32 devices in a mesh: section: 2 (over x), dp: 4 (over z), tensor: 4 (over y, core).
Axes of the slice: x: 2, y: 2, z: 4, core: 2. Of those that a mesh axis runs over, the one named last changes fastest.
Arguments:
- boundary: bfloat16 [2, 8, 1024, 1024], P('section', 'dp', 'tensor'), may hold values from -6 to 6
- norm_gain: float32 [2, 2, 1024], P('section'), may hold values from 0.5 to 1.5
- mix_in: bfloat16 [2, 1024, 2048], P('section', 'dp', 'tensor'), may hold values from -0.1875 to 0.1875
- mix_out: bfloat16 [2, 1024, 1024], P('section', 'tensor', 'dp'), may hold values from -0.375 to 0.375
- w_gate: bfloat16 [2, 1024, 4608], P('section', 'dp', 'tensor'), may hold values from -0.1875 to 0.1875
- w_up: bfloat16 [2, 1024, 4608], P('section', 'dp', 'tensor'), may hold values from -0.1875 to 0.1875
- w_down: bfloat16 [2, 4608, 1024], P('section', 'tensor', 'dp'), may hold values from -0.09375 to 0.09375
- conv_x: bfloat16 [1024, 1024], P(('section', 'dp'), 'tensor'), may hold values from -0.1875 to 0.1875
- conv_kernel: float32 [3, 1024], P(None, 'tensor'), may hold values from -3 to 3
- qk_gain: float32 [2, 64], replicated, may hold values from 0.7 to 1.6, as said below
Outputs:
- result: bfloat16 [2, 8, 1024, 1024], P('section', 'dp', 'tensor')
- grad_norm_gain: float32 [2, 2, 1024], P('section')
- grad_mix_in: float32 [2, 1024, 2048], P('section', 'dp', 'tensor')
- grad_mix_out: float32 [2, 1024, 1024], P('section', 'tensor', 'dp')
- grad_w_gate: float32 [2, 1024, 4608], P('section', 'dp', 'tensor')
- grad_w_up: float32 [2, 1024, 4608], P('section', 'dp', 'tensor')
- grad_w_down: float32 [2, 4608, 1024], P('section', 'tensor', 'dp')
- grad_conv_x: float32 [1024, 1024], P(('section', 'dp'), 'tensor')
- grad_conv_kernel: float32 [3, 1024], P(None, 'tensor')
- grad_qk_gain: float32 [2, 64], replicated
The draws below stay inside these ranges and needn't reach their ends.
Inputs may be any that keep to these rules, and one draw needn't show every extreme that they name: `qk_gain`: positive per-entry gains.
All inputs are finite; a program needn't handle non-finite values.
Results may differ from the reference program's by a relative error of at most 0.018.
The reference program's roundings to bfloat16 on the way count: a program that leaves them out, or rounds other values in their place, can miss the bound.
Values may be sent and summed in bfloat16 or wider, within the bound.
A program may use at most 192 MiB of HBM per device.

```python
import jax
import jax.numpy as jnp
from jax import lax

D = 1024
FF = 4608
HEADS = 16
KV_HEADS = 8
HEAD = 64
KERNEL = 3
SEQ = 1024
SEQS = 8
N_TENSOR = 4


def draw_qk_gain(key, part):
    return jnp.exp(jax.random.uniform(key, (2, HEAD), jnp.float32, jnp.log(0.7), jnp.log(1.6)))


def shard_levels(own_key, dims, pieces, low, largest):
    def one(position, shards_of):
        heights = jax.random.uniform(jax.random.fold_in(jax.random.fold_in(own_key, 6), position), (shards_of,), jnp.float32, low / len(pieces), largest / len(pieces))
        return jnp.repeat(jnp.exp(heights), dims[position] // shards_of).reshape((-1,) + (1,) * (len(dims) - position - 1))

    level = one(*pieces[0])
    for cut in pieces[1:]:
        level = level * one(*cut)
    return level


def noise(key, extent, width, bound, cuts=(), held_as=jnp.bfloat16):
    values = jax.random.normal(key, extent, jnp.float32) * width
    if len(cuts) > 0:
        values = shard_levels(key, extent, cuts, -0.22, 0.18) * values
    return jnp.clip(values, min=-bound, max=bound).astype(held_as)


def setup_inputs(seed: int = 0) -> dict:
    streams_of = jax.random.split(jax.random.key(seed), 11)
    boundary = noise(streams_of[0], (2, SEQS, SEQ, D), 1.0, 6.0, ((0, 2), (1, 4), (2, 4)))
    norm_gain = jnp.clip(1.0 + 0.1 * jax.random.normal(streams_of[1], (2, 2, D), jnp.float32), 0.5, 1.5)
    mix_in = noise(streams_of[2], (2, D, 2 * D), D ** -0.5, 0.1875, ((0, 2), (1, 4), (2, 4)))
    mix_out = noise(streams_of[3], (2, D, D), (D // 4) ** -0.5, 0.375, ((0, 2), (1, 4), (2, 4)))
    w_gate = noise(streams_of[4], (2, D, FF), D ** -0.5, 0.1875, ((0, 2), (1, 4), (2, 4)))
    w_up = noise(streams_of[5], (2, D, FF), D ** -0.5, 0.1875, ((0, 2), (1, 4), (2, 4)))
    w_down = noise(streams_of[6], (2, FF, D), FF ** -0.5, 0.09375, ((0, 2), (1, 4), (2, 4)))
    conv_x = noise(streams_of[7], (D, D), D ** -0.5, 0.1875, ((0, 8), (1, 4)))
    conv_kernel = noise(streams_of[8], (KERNEL, D), 0.6, 3.0, ((1, 4),), jnp.float32)
    qk_gain = draw_qk_gain(jax.random.fold_in(streams_of[10], 71), 0)
    return dict(boundary=boundary, norm_gain=norm_gain, mix_in=mix_in, mix_out=mix_out, w_gate=w_gate, w_up=w_up, w_down=w_down, conv_x=conv_x, conv_kernel=conv_kernel, qk_gain=qk_gain)


EPS = 1e-05
ROPE_BASE = 1000000.0
HIGHEST = lax.Precision.HIGHEST

@jax.custom_vjp
def low(v):
    return lax.optimization_barrier(v.astype(jnp.bfloat16)).astype(jnp.float32)

@jax.custom_vjp
def low_back(v):
    return v

def low_keep(v):
    return (low(v), None)

def low_pass(kept, grad):
    return (grad,)

def back_keep(v):
    return (v, None)

def back_low(kept, grad):
    return (low(grad),)
low.defvjp(low_keep, low_pass)
low_back.defvjp(back_keep, back_low)

def matmul(left_op, right_op):
    return jnp.dot(left_op, right_op, preferred_element_type=jnp.float32, precision=HIGHEST)

def norm_rows(values, gain):
    return values * lax.rsqrt(lax.optimization_barrier(jnp.mean(values * values, axis=-1, keepdims=True)) + EPS) * gain

def rotation(length, head_size):
    half_size = head_size // 2
    frequency = ROPE_BASE ** (-(jnp.arange(half_size, dtype=jnp.float32) * 2.0 / head_size))
    angles = jnp.arange(length, dtype=jnp.float32)[:, None] * frequency[None, :]
    cosine_table = jnp.concatenate([jnp.cos(angles), jnp.cos(angles)], axis=1)
    sine_table = jnp.concatenate([jnp.sin(angles), jnp.sin(angles)], axis=1)
    return (cosine_table, sine_table)

def rotate(values, cosine_table, sine_table):
    half_size = values.shape[-1] // 2
    turned = jnp.concatenate([-values[..., half_size:], values[..., :half_size]], axis=-1)
    return values * cosine_table + turned * sine_table

def delayed(values, delay_by):
    if delay_by == 0:
        return values
    return jnp.concatenate([jnp.zeros((delay_by, values.shape[1]), values.dtype), values[:-delay_by]], axis=0)

def feed_forward(middle, gain, gate_w, up_w, down_w):
    normed_mid = low(norm_rows(middle, gain))
    gate_pre = low_back(matmul(normed_mid, gate_w))
    up_pre = low_back(matmul(normed_mid, up_w))
    hidden = low(jax.nn.silu(gate_pre) * up_pre)
    return middle + low_back(matmul(hidden, down_w))

def conv_block(block_in, gains, w_in, w_cols, kernel, w_out, gate_w, up_w, down_w):
    length = block_in.shape[0]
    channels = D // N_TENSOR
    normed_in = low(norm_rows(block_in, gains[0]))
    projected = low_back(matmul(normed_in, w_in)).reshape(length, N_TENSOR, 2, channels)
    b_gate = projected[:, :, 0, :].reshape(length, D)
    c_gate = projected[:, :, 1, :].reshape(length, D)
    x_value = low_back(matmul(normed_in, w_cols))
    product = b_gate * x_value
    tap_count = kernel.shape[0]
    causal = jnp.zeros_like(product)
    for offset in range(tap_count):
        causal = causal + kernel[offset] * delayed(product, tap_count - 1 - offset)
    mixer_out = low(c_gate * causal)
    middle = block_in + low_back(matmul(mixer_out, w_out))
    return feed_forward(middle, gains[1], gate_w, up_w, down_w)

def attention_block(block_in, gains, w_in, head_gain, w_out, gate_w, up_w, down_w):
    length = block_in.shape[0]
    group_width = D // N_TENSOR
    group_size = HEADS // KV_HEADS
    normed_in = low(norm_rows(block_in, gains[0]))
    projected = low_back(matmul(normed_in, w_in)).reshape(length, N_TENSOR, 2 * group_width)
    queries = projected[:, :, :group_width].reshape(length, KV_HEADS, group_size, HEAD)
    key_part = projected[:, :, group_width:group_width + group_width // 2].reshape(length, KV_HEADS, HEAD)
    values = projected[:, :, group_width + group_width // 2:].reshape(length, KV_HEADS, HEAD)
    cosine_table, sine_table = rotation(length, HEAD)
    q_rot = low(rotate(norm_rows(queries, head_gain[0]), cosine_table[:, None, None, :], sine_table[:, None, None, :]))
    k_rot = low(rotate(norm_rows(key_part, head_gain[1]), cosine_table[:, None, :], sine_table[:, None, :]))
    v_low = low(values)
    row_block = min(512, length)
    score_scale = HEAD ** (-0.5)

    def attend(block_index):
        first_row = (block_index * row_block).astype(jnp.int32)
        q_piece = lax.dynamic_slice_in_dim(q_rot, first_row, row_block, 0)
        scores = low_back(jnp.einsum('ahgd,bhd->hgab', q_piece, k_rot, precision=HIGHEST) * score_scale)
        query_pos = first_row + jnp.arange(row_block, dtype=jnp.int32)
        allowed = jnp.arange(length, dtype=jnp.int32)[None, :] <= query_pos[:, None]
        scores = jnp.where(allowed[None, None], scores, -jnp.inf)
        weights = low(jax.nn.softmax(scores, axis=-1))
        return jnp.einsum('hgab,bhd->ahgd', weights, v_low, precision=HIGHEST).reshape(row_block, D)
    attended = lax.map(jax.checkpoint(attend), jnp.arange(length // row_block, dtype=jnp.int32))
    mixer_out = low_back(low(attended.reshape(length, D)))
    middle = block_in + low_back(matmul(mixer_out, w_out))
    return feed_forward(middle, gains[1], gate_w, up_w, down_w)

def both_blocks(params, block_in):
    norm_gains, w_in, w_out, gate_w, up_w, down_w, w_cols, kernel, head_gain = params
    between = conv_block(block_in, norm_gains[0], w_in[0], w_cols, kernel, w_out[0], gate_w[0], up_w[0], down_w[0])
    between = low(low_back(between))
    return attention_block(between, norm_gains[1], w_in[1], head_gain, w_out[1], gate_w[1], up_w[1], down_w[1])

def reference(boundary, norm_gain, mix_in, mix_out, w_gate, w_up, w_down, conv_x, conv_kernel, qk_gain):
    params = tuple((weight_arg.astype(jnp.float32) for weight_arg in (norm_gain, mix_in, mix_out, w_gate, w_up, w_down, conv_x, conv_kernel, qk_gain)))
    inputs = boundary[0].astype(jnp.float32)
    cotangents = boundary[1].astype(jnp.float32)

    def one_sequence(grad_sums, seq_pair):
        sequence, cotangent = seq_pair
        output, pullback = jax.vjp(both_blocks, params, sequence)
        param_grads, input_grad = pullback(cotangent)
        grad_sums = jax.tree.map(lambda total_sum, new_term: total_sum + new_term, grad_sums, param_grads)
        return (grad_sums, (input_grad.astype(jnp.bfloat16), output.astype(jnp.bfloat16)))
    start_sums = tuple((jnp.zeros_like(weight_arg) for weight_arg in params))
    grad_sums, (input_grads, outputs) = lax.scan(one_sequence, start_sums, (inputs, cotangents))
    result = jnp.stack([input_grads, outputs])
    return (result, grad_sums[0], grad_sums[1], grad_sums[2], grad_sums[3], grad_sums[4], grad_sums[5], grad_sums[6], grad_sums[7], grad_sums[8])
```

```python
import functools

import jax
import jax.numpy as jnp
from jax import lax
from jax.experimental import pallas as pl
from jax.experimental.pallas import tpu as pltpu
from jax.sharding import PartitionSpec as P

HEADS = 16
KV_HEADS = 8

EPS = 1e-05
ROPE_BASE = 1000000.0
MASKED = -1e30

MESH = pl.DeviceIdType.MESH
ANY = pl.BlockSpec(memory_space=pl.ANY)
VM = pl.BlockSpec(memory_space=pltpu.VMEM)
DMA = pltpu.SemaphoreType.DMA
VMEM_BYTES = 62 * 1024 * 1024
BF = jnp.bfloat16
F32 = jnp.float32


def contract(left_op, right_op, left_dim, right_dim):
    return lax.dot_general(
        left_op, right_op, (((left_dim,), (right_dim,)), ((), ())), preferred_element_type=F32
    )


def contract_rows(left_op, right_op):
    return contract(left_op, right_op, 0, 0)


def norm_rows(values, gain):
    return values * lax.rsqrt(jnp.mean(values * values, axis=-1, keepdims=True) + EPS) * gain


def norm_back(values, gain, grad_in):
    row_scale = lax.rsqrt(jnp.mean(values * values, axis=-1, keepdims=True) + EPS)
    normed = values * row_scale
    feature_count = values.shape[-1]
    gain_grad = jnp.sum((grad_in * normed).reshape(-1, feature_count), axis=0)
    scaled = grad_in * gain
    value_grad = row_scale * (scaled - normed * jnp.mean(scaled * normed, axis=-1, keepdims=True))
    return (value_grad, gain_grad)


def rotation(length, head_size):
    half_size = head_size // 2
    frequency = ROPE_BASE ** (-(jnp.arange(half_size, dtype=jnp.float32) * 2.0 / head_size))
    angles = jnp.arange(length, dtype=jnp.float32)[:, None] * frequency[None, :]
    cosine_table = jnp.concatenate([jnp.cos(angles), jnp.cos(angles)], axis=1)
    sine_table = jnp.concatenate([jnp.sin(angles), jnp.sin(angles)], axis=1)
    return (cosine_table, sine_table)


def rotate(values, cosine_table, sine_table):
    half_size = values.shape[-1] // 2
    turned = jnp.concatenate([-values[..., half_size:], values[..., :half_size]], axis=-1)
    return values * cosine_table + turned * sine_table


def rotate_back(grad_in, cosine_table, sine_table):
    half_size = grad_in.shape[-1] // 2
    shifted_grad = grad_in * sine_table
    return grad_in * cosine_table + jnp.concatenate(
        [shifted_grad[..., half_size:], -shifted_grad[..., :half_size]], axis=-1
    )


def delayed(values, delay_by):
    if delay_by == 0:
        return values
    return jnp.concatenate(
        [jnp.zeros((delay_by, values.shape[1]), values.dtype), values[:-delay_by]], axis=0
    )


def advanced(values, delay_by):
    if delay_by == 0:
        return values
    return jnp.concatenate(
        [values[delay_by:], jnp.zeros((delay_by, values.shape[1]), values.dtype)], axis=0
    )


def places():
    me = lax.axis_index("tensor")
    sib = me + 1 - 2 * (me % 2)
    cross = (me + 2) % 4
    diag = (sib + 2) % 4
    return me, sib, cross, diag


def greet(sib, cross):
    barrier = pltpu.get_barrier_semaphore()
    for peer in (sib, cross):
        pl.semaphore_signal(barrier, inc=1, device_id={"tensor": peer}, device_id_type=MESH)
    pl.semaphore_wait(barrier, 2)


def remote(src, dst, send_sem, recv_sem, peer):
    return pltpu.make_async_remote_copy(
        src_ref=src, dst_ref=dst, send_sem=send_sem, recv_sem=recv_sem,
        device_id={"tensor": peer}, device_id_type=MESH,
    )


def silu_parts(gate):
    sig = 1.0 / (1.0 + jnp.exp(-gate))
    return sig, gate * sig


def gather_kernel(cfg, *refs):
    norm, n_w, n_x, trans, epilogue = cfg
    it = iter(refs)
    x_ref = next(it)
    gain_ref = next(it) if norm else None
    w_hbm = [next(it) for _ in range(n_w)]
    e_hbm = [next(it) for _ in range(n_x)]
    a_hbm = next(it)
    n_out = {"plain": n_w, "ffn": 3, "ffn_back": 2}[epilogue]
    o_hbm = [next(it) for _ in range(n_out)]
    full = next(it)
    w_v = [next(it) for _ in range(n_w)]
    e_v = [next(it) for _ in range(n_x)]
    o_v = [next(it) for _ in range(n_out)]
    in_sem, out_sem, a_sem, xs, xr, ss, sr, ls, lr = it

    me, sib, cross, diag = places()
    rows = x_ref.shape[0]
    half = rows // 2
    loads = [
        pltpu.make_async_copy(src, dst, in_sem.at[i])
        for i, (src, dst) in enumerate(zip(w_hbm + e_hbm, w_v + e_v))
    ]
    for load in loads:
        load.start()
    greet(sib, cross)

    def span(owner, sub):
        return pl.ds(pl.multiple_of(owner * rows + sub * half, half), half)

    def to_cross(i):
        return remote(full.at[span(me, i)], full.at[span(me, i)], xs.at[i], xr.at[i], cross)

    def to_sib(i):
        return remote(full.at[span(me, i)], full.at[span(me, i)], ss.at[i], sr.at[i], sib)

    def relay(i):
        return remote(full.at[span(cross, i)], full.at[span(cross, i)], ls.at[i], lr.at[i], sib)

    for i in range(2):
        part = x_ref[pl.ds(i * half, half), :]
        if norm:
            part = norm_rows(part, gain_ref[...])
        full[span(me, i), :] = part.astype(BF)
        to_cross(i).start()
        to_sib(i).start()
    for load in loads:
        load.wait()

    def step(p, carry):
        far, sub = p // 2, p % 2
        near = (1 - sub) * me + sub * sib
        first = (1 - far) * near * rows + far * (cross * rows + sub * half)
        second = (1 - far) * (near * rows + half) + far * (diag * rows + sub * half)
        pair = [pl.ds(pl.multiple_of(first, half), half), pl.ds(pl.multiple_of(second, half), half)]

        @pl.when(p == 1)
        def _():
            to_sib(0).wait_recv()
            to_sib(1).wait_recv()

        for i in range(2):

            @pl.when(p == 2 + i)
            def _():
                to_cross(i).wait_recv()
                relay(i).start()
                relay(i).wait_recv()

        a = jnp.concatenate([full[pair[0], :], full[pair[1], :]], axis=0)
        prods = [contract(a, w[...], 1, 1 if trans else 0) for w in w_v]
        if epilogue == "plain":
            values = prods
        elif epilogue == "ffn":
            sig, silu = silu_parts(prods[0])
            values = [prods[0], prods[1], silu * prods[1]]
        else:
            gate = jnp.concatenate([e_v[0][q, :] for q in pair], axis=0).astype(F32)
            up = jnp.concatenate([e_v[1][q, :] for q in pair], axis=0).astype(F32)
            sig, silu = silu_parts(gate)
            values = [prods[0] * up * sig * (1.0 + gate * (1.0 - sig)), prods[0] * silu]
        for j, value in enumerate(values):
            value = value.astype(o_v[j].dtype)
            for k in range(2):
                o_v[j][pair[k], :] = value[k * half : (k + 1) * half]
                pltpu.make_async_copy(
                    o_v[j].at[pair[k]], o_hbm[j].at[pair[k]], out_sem.at[p, k, j]
                ).start()
        for k in range(2):
            pltpu.make_async_copy(full.at[pair[k]], a_hbm.at[pair[k]], a_sem.at[p, k]).start()
        return carry

    lax.fori_loop(0, 4, step, 0)
    for i in range(2):
        to_cross(i).wait_send()
        to_sib(i).wait_send()
        relay(i).wait_send()
    for p in range(4):
        for k in range(2):
            for j in range(n_out):
                pltpu.make_async_copy(
                    o_v[j].at[pl.ds(0, half)], o_hbm[j].at[pl.ds(0, half)], out_sem.at[p, k, j]
                ).wait()
            pltpu.make_async_copy(
                full.at[pl.ds(0, half)], a_hbm.at[pl.ds(0, half)], a_sem.at[p, k]
            ).wait()


def gather_mm(x_rows, gain, weights, extras=(), trans=False, epilogue="plain", cid=0, out_type=F32):
    rows, width = x_rows.shape
    length = rows * 4
    cols = [w.shape[0] if trans else w.shape[1] for w in weights]
    if epilogue == "plain":
        outs = [(c, out_type) for c in cols]
    else:
        outs = [(cols[0], BF)] * (3 if epilogue == "ffn" else 2)
    norm = gain is not None
    cfg = (norm, len(weights), len(extras), trans, epilogue)
    operands = [x_rows] + ([gain.reshape(1, width)] if norm else []) + list(weights) + list(extras)
    flops = sum(2 * length * width * c for c in cols)
    moved = sum(w.size * 2 for w in weights) + sum(length * c * 2 for c, _ in outs) + length * width * 4
    return pl.pallas_call(
        functools.partial(gather_kernel, cfg),
        out_shape=[jax.ShapeDtypeStruct((length, width), BF)]
        + [jax.ShapeDtypeStruct((length, c), t) for c, t in outs],
        in_specs=[VM] * (2 if norm else 1) + [ANY] * (len(weights) + len(extras)),
        out_specs=[ANY] * (1 + len(outs)),
        scratch_shapes=[pltpu.VMEM((length, width), BF)]
        + [pltpu.VMEM(w.shape, BF) for w in weights]
        + [pltpu.VMEM(e.shape, e.dtype) for e in extras]
        + [pltpu.VMEM((length, c), t) for c, t in outs]
        + [DMA((len(weights) + len(extras),)), DMA((4, 2, len(outs))), DMA((4, 2))]
        + [DMA((2,))] * 6,
        compiler_params=pltpu.CompilerParams(
            collective_id=cid, has_side_effects=True, vmem_limit_bytes=VMEM_BYTES
        ),
        cost_estimate=pl.CostEstimate(flops=flops, bytes_accessed=moved * 4, transcendentals=0),
        name=f"gather{cid}",
    )(*operands)


def scatter_kernel(cfg, *refs):
    n_y, trans, epilogue = cfg
    it = iter(refs)
    y_hbm = [next(it) for _ in range(n_y)]
    w_hbm = [next(it) for _ in range(n_y)]
    resid_ref = next(it)
    if epilogue == "back":
        value_ref, gain_ref = next(it), next(it)
    out_ref = next(it)
    if epilogue == "back":
        gain_out = next(it)
    y_v = [next(it) for _ in range(n_y)]
    w_v = [next(it) for _ in range(n_y)]
    keep, own, to_s, from_s, to_c, from_c, to_o, from_o = (next(it) for _ in range(8))
    in_sem, ds, dr, cs, cr, os_, or_ = it

    me, sib, cross, diag = places()
    rows = resid_ref.shape[0]
    half = rows // 2
    loads = [
        pltpu.make_async_copy(src, dst, in_sem.at[i])
        for i, (src, dst) in enumerate(zip(y_hbm + w_hbm, y_v + w_v))
    ]
    for load in loads:
        load.start()
    greet(sib, cross)
    for load in loads:
        load.wait()

    def send_diag(i):
        return remote(to_s.at[i], from_s.at[i], ds.at[i], dr.at[i], sib)

    def send_cross(i):
        return remote(to_c.at[i], from_c.at[i], cs.at[i], cr.at[i], cross)

    send_near = remote(to_o, from_o, os_, or_, sib)

    def pass_on(i):
        send_diag(i).wait_recv()
        to_c[i] = (keep[i] + from_s[i].astype(F32)).astype(BF)
        send_cross(i).start()

    def step(p, carry):
        near, sub = p // 2, p % 2
        base = near * ((1 - sub) * sib + sub * me) * rows
        first = base + (1 - near) * (cross * rows + sub * half)
        second = base + near * half + (1 - near) * (diag * rows + sub * half)
        pair = [pl.ds(pl.multiple_of(first, half), half), pl.ds(pl.multiple_of(second, half), half)]
        total = None
        for y, w in zip(y_v, w_v):
            a = jnp.concatenate([y[pair[0], :], y[pair[1], :]], axis=0)
            prod = contract(a, w[...], 1, 1 if trans else 0)
            total = prod if total is None else total + prod

        for i in range(2):

            @pl.when(p == i)
            def _():
                keep[i] = total[:half]
                to_s[i] = total[half:].astype(BF)
                send_diag(i).start()

        @pl.when(p == 1)
        def _():
            pass_on(0)

        @pl.when(p == 2)
        def _():
            to_o[...] = total.astype(BF)
            send_near.start()
            pass_on(1)

        @pl.when(p == 3)
        def _():
            own[...] = total

        return carry

    lax.fori_loop(0, 4, step, 0)
    send_near.wait_recv()
    gain_sum = None
    for i in range(2):
        part = pl.ds(i * half, half)
        send_cross(i).wait_recv()
        total = own[part, :] + from_o[part, :].astype(F32) + from_c[i].astype(F32)
        resid = resid_ref[part, :].astype(F32)
        if epilogue == "back":
            value_grad, gain_grad = norm_back(value_ref[part, :], gain_ref[...], total)
            out_ref[part, :] = resid + value_grad
            gain_sum = gain_grad if gain_sum is None else gain_sum + gain_grad
        else:
            out_ref[part, :] = resid + total
    if epilogue == "back":
        gain_out[...] = gain_sum.reshape(gain_out.shape)
    send_near.wait_send()
    for i in range(2):
        send_diag(i).wait_send()
        send_cross(i).wait_send()


def scatter_mm(operands, weights, resid, back=None, trans=False, cid=0):
    rows, width = resid.shape
    half = rows // 2
    epilogue = "plain" if back is None else "back"
    extra = [] if back is None else [back[0], back[1].reshape(1, width)]
    out_shape = [jax.ShapeDtypeStruct((rows, width), F32)]
    if back is not None:
        out_shape.append(jax.ShapeDtypeStruct((1, width), F32))
    flops = sum(2 * y.size * width for y in operands)
    moved = sum(2 * (y.size + w.size) for y, w in zip(operands, weights)) + rows * width * 12
    result = pl.pallas_call(
        functools.partial(scatter_kernel, (len(operands), trans, epilogue)),
        out_shape=out_shape,
        in_specs=[ANY] * (2 * len(operands)) + [VM] * (1 + len(extra)),
        out_specs=[VM] * len(out_shape),
        scratch_shapes=[pltpu.VMEM(y.shape, BF) for y in operands]
        + [pltpu.VMEM(w.shape, BF) for w in weights]
        + [pltpu.VMEM((2, half, width), F32), pltpu.VMEM((rows, width), F32)]
        + [pltpu.VMEM((2, half, width), BF)] * 4
        + [pltpu.VMEM((rows, width), BF)] * 2
        + [DMA((2 * len(operands),))]
        + [DMA((2,))] * 4
        + [DMA] * 2,
        compiler_params=pltpu.CompilerParams(
            collective_id=cid, has_side_effects=True, vmem_limit_bytes=VMEM_BYTES
        ),
        cost_estimate=pl.CostEstimate(flops=flops, bytes_accessed=moved * 4, transcendentals=0),
        name=f"scatter{cid}",
    )(*operands, *weights, resid, *extra)
    return result[0] if back is None else result


def conv_core(projected, x_value, kernel):
    channels = x_value.shape[1]
    b_gate = projected[:, :channels]
    c_gate = projected[:, channels:]
    product = b_gate * x_value
    tap_count = kernel.shape[0]
    causal = jnp.zeros_like(product)
    for offset in range(tap_count):
        causal = causal + kernel[offset] * delayed(product, tap_count - 1 - offset)
    return (b_gate, c_gate, product, causal)


def conv_back(projected, x_value, kernel, grad_y):
    b_gate, c_gate, product, causal = conv_core(projected, x_value, kernel)
    grad_c = grad_y * causal
    grad_causal = grad_y * c_gate
    tap_count = kernel.shape[0]
    kernel_rows = []
    grad_product = jnp.zeros_like(product)
    for offset in range(tap_count):
        delay_by = tap_count - 1 - offset
        kernel_rows.append(jnp.sum(grad_causal * delayed(product, delay_by), axis=0))
        grad_product = grad_product + kernel[offset] * advanced(grad_causal, delay_by)
    grad_proj = jnp.concatenate([grad_product * x_value, grad_c], axis=1).astype(BF)
    grad_value = (grad_product * b_gate).astype(BF)
    return (grad_proj, grad_value, jnp.stack(kernel_rows))


def attention_inputs(projected, head_gain):
    length = projected.shape[0]
    group_width = projected.shape[1] // 2
    head_size = head_gain.shape[1]
    group_size = HEADS // KV_HEADS
    kv_local = group_width // head_size // group_size
    queries = projected[:, :group_width].reshape(length, kv_local, group_size, head_size)
    key_part = projected[:, group_width : group_width + group_width // 2].reshape(
        length, kv_local, head_size
    )
    values = projected[:, group_width + group_width // 2 :].reshape(length, kv_local, head_size)
    cosine_table, sine_table = rotation(length, head_size)
    q_rot = rotate(
        norm_rows(queries, head_gain[0]),
        cosine_table[:, None, None, :],
        sine_table[:, None, None, :],
    ).astype(BF)
    k_rot = rotate(
        norm_rows(key_part, head_gain[1]), cosine_table[:, None, :], sine_table[:, None, :]
    ).astype(BF)
    return (queries, key_part, q_rot, k_rot, values.astype(BF), cosine_table, sine_table)


def masked_scores(q_piece, k_rot, first_row, length):
    row_block = q_piece.shape[0]
    score_scale = q_piece.shape[-1] ** (-0.5)
    scores = jnp.einsum("ahgd,bhd->hgab", q_piece, k_rot, preferred_element_type=F32) * score_scale
    query_pos = first_row + jnp.arange(row_block, dtype=jnp.int32)
    key_pos = jnp.arange(length, dtype=jnp.int32)
    allowed = key_pos[None, :] <= query_pos[:, None]
    return jnp.where(allowed, scores, MASKED)


def attention_forward(parts):
    q_rot, k_rot, v_low = (parts[2], parts[3], parts[4])
    length = q_rot.shape[0]
    row_block = min(512, length)
    out_blocks = []
    total_blocks = []
    for first_row in range(0, length, row_block):
        scores = masked_scores(q_rot[first_row : first_row + row_block], k_rot, first_row, length)
        row_max = jnp.max(scores, axis=-1, keepdims=True)
        exp_scores = jnp.exp(scores - row_max)
        row_sum = jnp.sum(exp_scores, axis=-1, keepdims=True)
        weights = (exp_scores / row_sum).astype(BF)
        attended = jnp.einsum("hgab,bhd->ahgd", weights, v_low, preferred_element_type=F32)
        out_blocks.append(attended.reshape(row_block, -1))
        total_blocks.append((row_max + jnp.log(row_sum))[..., 0])
    return (jnp.concatenate(out_blocks, axis=0).astype(BF), jnp.concatenate(total_blocks, axis=-1))


def attention_back(parts, log_total, head_gain, grad_y):
    queries, key_part, q_rot, k_rot, v_low, cosine_table, sine_table = parts
    length, kv_local, group_size, head_size = queries.shape
    score_scale = head_size ** (-0.5)
    row_block = min(512, length)
    grad_low = grad_y.astype(BF).reshape(length, kv_local, group_size, head_size)
    q_grads = []
    key_grad = jnp.zeros((length, kv_local, head_size), F32)
    value_grad = jnp.zeros((length, kv_local, head_size), F32)
    for first_row in range(0, length, row_block):
        q_piece = q_rot[first_row : first_row + row_block]
        scores = masked_scores(q_piece, k_rot, first_row, length)
        probability = jnp.exp(scores - log_total[:, :, first_row : first_row + row_block, None])
        weights = probability.astype(BF)
        grad_piece = grad_low[first_row : first_row + row_block]
        grad_weights = jnp.einsum("ahgd,bhd->hgab", grad_piece, v_low, preferred_element_type=F32)
        value_grad = value_grad + jnp.einsum(
            "hgab,ahgd->bhd", weights, grad_piece, preferred_element_type=F32
        )
        grad_scores = probability * (
            grad_weights - jnp.sum(probability * grad_weights, axis=-1, keepdims=True)
        )
        grad_scores = grad_scores.astype(BF)
        q_grads.append(
            jnp.einsum("hgab,bhd->ahgd", grad_scores, k_rot, preferred_element_type=F32)
            * score_scale
        )
        key_grad = (
            key_grad
            + jnp.einsum("hgab,ahgd->bhd", grad_scores, q_piece, preferred_element_type=F32)
            * score_scale
        )
    query_grad = jnp.concatenate(q_grads, axis=0)
    query_grad = rotate_back(
        query_grad, cosine_table[:, None, None, :], sine_table[:, None, None, :]
    )
    key_grad = rotate_back(key_grad, cosine_table[:, None, :], sine_table[:, None, :])
    query_raw, q_gain_grad = norm_back(queries, head_gain[0], query_grad)
    key_raw, k_gain_grad = norm_back(key_part, head_gain[1], key_grad)
    grad_proj = jnp.concatenate(
        [
            query_raw.reshape(length, -1),
            key_raw.reshape(length, -1),
            value_grad.reshape(length, -1),
        ],
        axis=1,
    ).astype(BF)
    return (grad_proj, jnp.stack([q_gain_grad, k_gain_grad]))


SWAP = [(0, 1), (1, 0)]
WHOLE = ("section", "dp")


def gather_rows(shard):
    both = lax.all_gather(shard, WHOLE, axis=0, tiled=True)
    size = both.shape[0] // 2
    return both[:size], both[size:]


def gather_cols(shard):
    both = lax.all_gather(shard, WHOLE, axis=0, tiled=False)
    count, rows, cols = both.shape
    both = both.reshape(2, count // 2, rows, cols).transpose(0, 2, 1, 3)
    both = both.reshape(2, rows, count // 2 * cols)
    return both[0], both[1]


def body(boundary, norm_gain, mix_in, mix_out, w_gate, w_up, w_down, conv_x, conv_kernel, qk_gain):
    section = lax.axis_index("section")
    first = section == 0
    model_width = boundary.shape[3]
    channels = mix_out.shape[1]

    slots = boundary[0]
    mine = jnp.where(first, slots[0], slots[1])
    theirs = jnp.where(first, slots[1], slots[0])
    moved = lax.ppermute(theirs, "section", SWAP)
    x_low = jnp.where(first, mine, moved)
    cot = jnp.where(first, moved, mine)
    gain_other = lax.ppermute(norm_gain[0], "section", SWAP)
    gains = (
        jnp.where(first, norm_gain[0], gain_other),
        jnp.where(first, gain_other, norm_gain[0]),
    )

    w_in = gather_rows(mix_in[0])
    w_cols = lax.all_gather(conv_x, WHOLE, axis=0, tiled=True)
    w_out = gather_cols(mix_out[0])
    gate_w = gather_rows(w_gate[0])
    up_w = gather_rows(w_up[0])
    down_w = gather_cols(w_down[0])

    x_rows = x_low.astype(F32)
    a0, proj0, value0 = gather_mm(x_rows, gains[0][0], [w_in[0], w_cols], cid=0)
    b_gate, c_gate, product, causal = conv_core(proj0, value0, conv_kernel)
    y0 = (c_gate * causal).astype(BF)
    mid0 = scatter_mm([y0], [w_out[0]], x_rows, cid=1)
    m0, gate0, up0, hid0 = gather_mm(
        mid0, gains[0][1], [gate_w[0], up_w[0]], epilogue="ffn", cid=2
    )
    z_rows = scatter_mm([hid0], [down_w[0]], mid0, cid=3).astype(BF).astype(F32)
    a1, proj1 = gather_mm(z_rows, gains[1][0], [w_in[1]], cid=4)
    parts = attention_inputs(proj1, qk_gain)
    y1, log_total = attention_forward(parts)
    mid1 = scatter_mm([y1], [w_out[1]], z_rows, cid=5)
    m1, gate1, up1, hid1 = gather_mm(
        mid1, gains[1][1], [gate_w[1], up_w[1]], epilogue="ffn", cid=6
    )
    y_rows = scatter_mm([hid1], [down_w[1]], mid1, cid=7).astype(BF)

    def low_grad(left_op, right_op):
        return contract_rows(left_op, right_op).astype(BF)

    def ffn_back(dout, middle, gain, m, gate, up, hid, block, cid):
        d_full, d_gate, d_up = gather_mm(
            dout, None, [down_w[block]], [gate, up], trans=True, epilogue="ffn_back", cid=cid
        )
        grads = (low_grad(m, d_gate), low_grad(m, d_up), low_grad(hid, d_full))
        d_mid, d_gain = scatter_mm(
            [d_gate, d_up], [gate_w[block], up_w[block]], dout, (middle, gain), True, cid + 1
        )
        return d_mid, d_gain, grads

    def out_back(d_mid, block, y, cid):
        d_full, d_y = gather_mm(d_mid, None, [w_out[block]], trans=True, cid=cid)
        return d_y, low_grad(y, d_full)

    def owned(rows_first, rows_second, dim):
        return [
            lax.psum_scatter(g, "dp", scatter_dimension=dim, tiled=True)
            for g in (rows_first, rows_second)
        ]

    d_mid1, gain11, (g_gate1, g_up1, g_down1) = ffn_back(
        cot, mid1, gains[1][1], m1, gate1, up1, hid1, 1, 8
    )
    d_y1, g_out1 = out_back(d_mid1, 1, y1, 10)
    d_proj1, head_grad = attention_back(parts, log_total, qk_gain, d_y1)
    g_in1 = low_grad(a1, d_proj1)
    d_z, gain10 = scatter_mm(
        [d_proj1], [w_in[1]], d_mid1, (z_rows, gains[1][0]), True, 11
    )
    d_z = d_z.astype(BF)
    d_mid0, gain01, (g_gate0, g_up0, g_down0) = ffn_back(
        d_z, mid0, gains[0][1], m0, gate0, up0, hid0, 0, 12
    )
    d_y0, g_out0 = out_back(d_mid0, 0, y0, 14)
    d_proj0, d_value0, kernel_grad = conv_back(proj0, value0, conv_kernel, d_y0)
    g_in0 = low_grad(a0, d_proj0)
    g_cols = low_grad(a0, d_value0)
    d_x, gain00 = scatter_mm(
        [d_proj0, d_value0], [w_in[0], w_cols], d_mid0, (x_rows, gains[0][0]), True, 15
    )
    d_x = d_x.astype(BF)

    pairs = [
        owned(g_in0, g_in1, 0),
        owned(g_out0, g_out1, 1),
        owned(g_gate0, g_gate1, 0),
        owned(g_up0, g_up1, 0),
        owned(g_down0, g_down1, 1),
    ]
    weight_grads = []
    for zero, one in pairs:
        kept = jnp.where(first, zero, one)
        sent = jnp.where(first, one, zero)
        other = lax.ppermute(sent, "section", SWAP)
        weight_grads.append((kept.astype(F32) + other.astype(F32))[None])
    cols_part = lax.psum_scatter(g_cols, WHOLE, scatter_dimension=0, tiled=True).astype(F32)

    moved_out = lax.ppermute(jnp.where(first, y_rows, d_x), "section", SWAP)
    kept_out = jnp.where(first, d_x, y_rows)
    result = jnp.stack(
        [jnp.where(first, kept_out, moved_out), jnp.where(first, moved_out, kept_out)]
    )

    tensor_index = lax.axis_index("tensor")
    kernel_full = lax.dynamic_update_slice_in_dim(
        jnp.zeros((conv_kernel.shape[0], model_width), F32), kernel_grad, tensor_index * channels, 1
    )
    gains_full = jnp.concatenate([gain00, gain01, gain10, gain11], axis=0)
    gains_total, kernel_total, head_total = lax.psum(
        (gains_full, kernel_full, head_grad), ("section", "dp", "tensor")
    )
    gain_out = lax.dynamic_slice_in_dim(gains_total.reshape(2, 2, model_width), section, 1, 0)
    kernel_out = lax.dynamic_slice_in_dim(kernel_total, tensor_index * channels, channels, 1)
    return (
        result[None],
        gain_out,
        *weight_grads,
        cols_part,
        kernel_out,
        head_total,
    )


def solution(mesh):
    in_specs = (
        P("section", "dp", "tensor", None),
        P("section", None, None),
        P("section", "dp", "tensor"),
        P("section", "tensor", "dp"),
        P("section", "dp", "tensor"),
        P("section", "dp", "tensor"),
        P("section", "tensor", "dp"),
        P(("section", "dp"), "tensor"),
        P(None, "tensor"),
        P(),
    )
    out_specs = (
        P("section", "dp", "tensor", None),
        P("section", None, None),
        P("section", "dp", "tensor"),
        P("section", "tensor", "dp"),
        P("section", "dp", "tensor"),
        P("section", "dp", "tensor"),
        P("section", "tensor", "dp"),
        P(("section", "dp"), "tensor"),
        P(None, "tensor"),
        P(),
    )
    return jax.shard_map(body, mesh=mesh, in_specs=in_specs, out_specs=out_specs, check_vma=False)
```

```python
import functools

import jax
import jax.numpy as jnp
from jax import lax
from jax.experimental import pallas as pl
from jax.experimental.pallas import tpu as pltpu
from jax.sharding import PartitionSpec as P

HEADS = 16
KV_HEADS = 8

EPS = 1e-05
ROPE_BASE = 1000000.0
MASKED = -1e30

MESH = pl.DeviceIdType.MESH
ANY = pl.BlockSpec(memory_space=pl.ANY)
VM = pl.BlockSpec(memory_space=pltpu.VMEM)
DMA = pltpu.SemaphoreType.DMA
VMEM_BYTES = 62 * 1024 * 1024
BF = jnp.bfloat16
F32 = jnp.float32


def contract(left_op, right_op, left_dim, right_dim):
    return lax.dot_general(
        left_op, right_op, (((left_dim,), (right_dim,)), ((), ())), preferred_element_type=F32
    )


def contract_rows(left_op, right_op):
    return contract(left_op, right_op, 0, 0)


def norm_rows(values, gain):
    return values * lax.rsqrt(jnp.mean(values * values, axis=-1, keepdims=True) + EPS) * gain


def norm_back(values, gain, grad_in):
    row_scale = lax.rsqrt(jnp.mean(values * values, axis=-1, keepdims=True) + EPS)
    normed = values * row_scale
    feature_count = values.shape[-1]
    gain_grad = jnp.sum((grad_in * normed).reshape(-1, feature_count), axis=0)
    scaled = grad_in * gain
    value_grad = row_scale * (scaled - normed * jnp.mean(scaled * normed, axis=-1, keepdims=True))
    return (value_grad, gain_grad)


def rotation(length, head_size):
    half_size = head_size // 2
    frequency = ROPE_BASE ** (-(jnp.arange(half_size, dtype=jnp.float32) * 2.0 / head_size))
    angles = jnp.arange(length, dtype=jnp.float32)[:, None] * frequency[None, :]
    cosine_table = jnp.concatenate([jnp.cos(angles), jnp.cos(angles)], axis=1)
    sine_table = jnp.concatenate([jnp.sin(angles), jnp.sin(angles)], axis=1)
    return (cosine_table, sine_table)


def rotate(values, cosine_table, sine_table):
    half_size = values.shape[-1] // 2
    turned = jnp.concatenate([-values[..., half_size:], values[..., :half_size]], axis=-1)
    return values * cosine_table + turned * sine_table


def rotate_back(grad_in, cosine_table, sine_table):
    half_size = grad_in.shape[-1] // 2
    shifted_grad = grad_in * sine_table
    return grad_in * cosine_table + jnp.concatenate(
        [shifted_grad[..., half_size:], -shifted_grad[..., :half_size]], axis=-1
    )


def delayed(values, delay_by):
    if delay_by == 0:
        return values
    return jnp.concatenate(
        [jnp.zeros((delay_by, values.shape[1]), values.dtype), values[:-delay_by]], axis=0
    )


def advanced(values, delay_by):
    if delay_by == 0:
        return values
    return jnp.concatenate(
        [values[delay_by:], jnp.zeros((delay_by, values.shape[1]), values.dtype)], axis=0
    )


def places():
    me = lax.axis_index("tensor")
    sib = me + 1 - 2 * (me % 2)
    cross = (me + 2) % 4
    diag = (sib + 2) % 4
    return me, sib, cross, diag


def greet(peers):
    barrier = pltpu.get_barrier_semaphore()
    for peer in peers:
        pl.semaphore_signal(barrier, inc=1, device_id=peer, device_id_type=MESH)
    pl.semaphore_wait(barrier, len(peers))


def remote(src, dst, send_sem, recv_sem, peer):
    return pltpu.make_async_remote_copy(
        src_ref=src, dst_ref=dst, send_sem=send_sem, recv_sem=recv_sem,
        device_id=peer, device_id_type=MESH,
    )


class Task:
    def __init__(self, inputs, out, axis, count, copies, sender=None):
        self.inputs, self.out, self.axis, self.count = inputs, out, axis, count
        self.copies, self.sender = copies, sender


def sizes():
    return lax.axis_size("section"), lax.axis_size("dp")


def slots(value):
    return jax.ShapeDtypeStruct((lax.axis_size("dp"),) + value.shape, value.dtype)


def same(value):
    return jax.ShapeDtypeStruct(value.shape, value.dtype)


def z_gather(piece):
    count = lax.axis_size("dp")

    def copies(ins, out, s, d, t):
        return [(ins[0], out.at[d], {"dp": (d + k) % count}) for k in range(1, count)]

    return Task([piece], slots(piece), "dp", count - 1, copies)


def x_gather(piece, held):
    count = lax.axis_size("dp")

    def copies(ins, out, s, d, t):
        peer = {"section": 1 - s}
        moves = [(ins[0], out.at[d], peer)]
        for k in range(1, count):
            other = (d + k) % count
            moves.append((ins[1].at[other], out.at[other], peer))
        return moves

    return Task([piece, held], slots(piece), "section", count, copies)


def x_half(shard):
    out = jax.ShapeDtypeStruct(shard.shape[1:], shard.dtype)

    def copies(ins, out, s, d, t):
        return [(ins[0].at[1 - s], out, {"section": 1 - s})]

    return Task([shard], out, "section", 1, copies)


def x_swap(value):
    def copies(ins, out, s, d, t):
        return [(ins[0], out, {"section": 1 - s})]

    return Task([value], same(value), "section", 1, copies)


def x_rows_of(grads):
    count = lax.axis_size("dp")
    out = jax.ShapeDtypeStruct((count,) + grads.shape[2:], grads.dtype)

    def copies(ins, out, s, d, t):
        peer = {"section": 1 - s}
        return [(ins[0].at[k, 1 - s], out.at[k], peer) for k in range(count)]

    return Task([grads], out, "section", count, copies)


def z_scatter(pieces):
    count = lax.axis_size("dp")

    def copies(ins, out, s, d, t):
        moves = []
        for k in range(1, count):
            other = (d + k) % count
            moves.append((ins[0].at[other], out.at[d], {"dp": other}))
        return moves

    return Task([pieces], same(pieces), "dp", count - 1, copies)


def x_final(piece, block):
    def copies(ins, out, s, d, t):
        return [(ins[0], out, {"section": 1 - s})]

    return Task([piece], same(piece), "section", 1, copies, sender=1 - block)


def t_share(value):
    out = jax.ShapeDtypeStruct((4,) + value.shape, value.dtype)

    def copies(ins, out, s, d, t):
        return [(ins[0], out.at[t], {"tensor": (t + k) % 4}) for k in range(1, 4)]

    return Task([value], out, "tensor", 3, copies)


class Background:
    def __init__(self, tasks):
        self.tasks = list(tasks)
        self.inputs = [v for task in self.tasks for v in task.inputs]
        self.outs = [task.out for task in self.tasks]
        self.count = sum(task.count for task in self.tasks)
        self.scratch = [DMA((max(self.count, 1),)), DMA((max(self.count, 1),))]

    def bind(self, it_in, it_out):
        self.in_refs = [next(it_in) for _ in self.inputs]
        self.out_refs = [next(it_out) for _ in self.outs]

    def peers(self, tensor):
        _, count = sizes()
        s, d, t = (lax.axis_index(a) for a in ("section", "dp", "tensor"))
        axes = {task.axis for task in self.tasks}
        found = []
        if "section" in axes:
            found.append({"section": 1 - s})
        if "dp" in axes:
            found += [{"dp": (d + k) % count} for k in range(1, count)]
        if "tensor" in axes:
            found += [{"tensor": (t + k) % 4} for k in range(1, 4)]
        else:
            found += tensor
        return found

    def plan(self, sems):
        send, recv = sems
        s, d, t = (lax.axis_index(a) for a in ("section", "dp", "tensor"))
        at, i, moves = 0, 0, []
        for task, out in zip(self.tasks, self.out_refs):
            ins = self.in_refs[at : at + len(task.inputs)]
            at += len(task.inputs)
            for from_ref, to_ref, peer in task.copies(ins, out, s, d, t):
                moves.append((remote(from_ref, to_ref, send.at[i], recv.at[i], peer), task.sender))
                i += 1
        return s, moves

    def start(self, sems):
        s, moves = self.plan(sems)
        for move, sender in moves:
            if sender is None:
                move.start()
            else:
                pl.when(s == sender)(move.start)

    def finish(self, sems):
        s, moves = self.plan(sems)
        for move, sender in moves:
            if sender is None:
                move.wait_recv()
                move.wait_send()
            else:
                pl.when(s == sender)(move.wait_send)
                pl.when(s == 1 - sender)(move.wait_recv)


def exchange_kernel(bg, *refs):
    ins = iter(refs[: len(bg.inputs)])
    outs = iter(refs[len(bg.inputs) : len(bg.inputs) + len(bg.outs)])
    sems = refs[len(bg.inputs) + len(bg.outs) :]
    bg.bind(ins, outs)
    greet(bg.peers([]))
    bg.start(sems)
    bg.finish(sems)


def exchange(tasks, cid):
    bg = Background(tasks)
    return pl.pallas_call(
        functools.partial(exchange_kernel, bg),
        out_shape=bg.outs,
        in_specs=[ANY] * len(bg.inputs),
        out_specs=[ANY] * len(bg.outs),
        scratch_shapes=bg.scratch,
        compiler_params=pltpu.CompilerParams(
            collective_id=cid, has_side_effects=True, vmem_limit_bytes=VMEM_BYTES
        ),
        name=f"exchange{cid}",
    )(*bg.inputs)


class Weight:
    def __init__(self, kind, piece, near, far):
        count = lax.axis_size("dp")
        rows, cols = piece.shape
        if kind == "cols":
            self.shape = (2 * rows, count * cols)
        else:
            self.shape = (2 * count * rows, cols)
        self.size = self.shape[0] * self.shape[1]
        if kind == "cols" and cols % 128:
            s, d = lax.axis_index("section"), lax.axis_index("dp")
            near = lax.dynamic_update_index_in_dim(near, piece, d, 0)
            both = jnp.stack([jnp.where(s == 0, near, far), jnp.where(s == 0, far, near)])
            self.parts = [both.transpose(0, 2, 1, 3).reshape(self.shape)]
            self.kind, self.loads = "whole", 1
        else:
            self.kind, self.parts, self.loads = kind, [piece, near, far], 2 * count

    def copies(self, refs, dst, sem):
        if self.kind == "whole":
            return [pltpu.make_async_copy(refs[0], dst, sem.at[0])]
        s, d = lax.axis_index("section"), lax.axis_index("dp")
        count = lax.axis_size("dp")
        rows, cols = self.parts[0].shape

        def place(sec, own):
            if self.kind == "cols":
                top = pl.multiple_of(sec * rows, rows)
                return dst.at[pl.ds(top, rows), pl.ds(pl.multiple_of(own * cols, cols), cols)]
            slot = own * 2 + sec if self.kind == "rows" else sec * count + own
            return dst.at[pl.ds(pl.multiple_of(slot * rows, rows), rows)]

        moves = []
        for k in range(count):
            other = (d + k) % count
            near = refs[0] if k == 0 else refs[1].at[other]
            moves.append(pltpu.make_async_copy(near, place(s, other), sem.at[2 * k]))
            moves.append(
                pltpu.make_async_copy(refs[2].at[other], place(1 - s, other), sem.at[2 * k + 1])
            )
        return moves


def silu_parts(gate):
    sig = 1.0 / (1.0 + jnp.exp(-gate))
    return sig, gate * sig


def gather_kernel(cfg, weights, bg, *refs):
    norm, n_w, n_x, trans, epilogue = cfg
    it = iter(refs)
    x_ref = next(it)
    gain_ref = next(it) if norm else None
    w_hbm = [[next(it) for _ in w.parts] for w in weights]
    e_hbm = [next(it) for _ in range(n_x)]
    bg_in = [next(it) for _ in bg.inputs]
    a_hbm = next(it)
    n_out = {"plain": n_w, "ffn": 3, "ffn_back": 2}[epilogue]
    o_hbm = [next(it) for _ in range(n_out)]
    bg.bind(iter(bg_in), it)
    full = next(it)
    w_v = [next(it) for _ in range(n_w)]
    e_v = [next(it) for _ in range(n_x)]
    o_v = [next(it) for _ in range(n_out)]
    w_sem, in_sem, out_sem, a_sem, xs, xr, ss, sr, ls, lr, *bg_sems = it

    me, sib, cross, diag = places()
    rows = x_ref.shape[0]
    half = rows // 2
    loads = [
        pltpu.make_async_copy(src, dst, in_sem.at[i])
        for i, (src, dst) in enumerate(zip(e_hbm, e_v))
    ]
    for i, w in enumerate(weights):
        loads += w.copies(w_hbm[i], w_v[i], w_sem.at[i])
    for load in loads:
        load.start()
    greet(bg.peers([{"tensor": sib}, {"tensor": cross}]))

    def span(owner, sub):
        return pl.ds(pl.multiple_of(owner * rows + sub * half, half), half)

    def to_cross(i):
        return remote(full.at[span(me, i)], full.at[span(me, i)], xs.at[i], xr.at[i], {"tensor": cross})

    def to_sib(i):
        return remote(full.at[span(me, i)], full.at[span(me, i)], ss.at[i], sr.at[i], {"tensor": sib})

    def relay(i):
        return remote(full.at[span(cross, i)], full.at[span(cross, i)], ls.at[i], lr.at[i], {"tensor": sib})

    for i in range(2):
        part = x_ref[pl.ds(i * half, half), :]
        if norm:
            part = norm_rows(part, gain_ref[...])
        full[span(me, i), :] = part.astype(BF)
        to_cross(i).start()
        to_sib(i).start()
    bg.start(bg_sems)
    for load in loads:
        load.wait()

    def step(p, carry):
        far, sub = p // 2, p % 2
        near = (1 - sub) * me + sub * sib
        first = (1 - far) * near * rows + far * (cross * rows + sub * half)
        second = (1 - far) * (near * rows + half) + far * (diag * rows + sub * half)
        pair = [pl.ds(pl.multiple_of(first, half), half), pl.ds(pl.multiple_of(second, half), half)]

        @pl.when(p == 1)
        def _():
            to_sib(0).wait_recv()
            to_sib(1).wait_recv()

        for i in range(2):

            @pl.when(p == 2 + i)
            def _():
                to_cross(i).wait_recv()
                relay(i).start()
                relay(i).wait_recv()

        a = jnp.concatenate([full[pair[0], :], full[pair[1], :]], axis=0)
        prods = [contract(a, w[...], 1, 1 if trans else 0) for w in w_v]
        if epilogue == "plain":
            values = prods
        elif epilogue == "ffn":
            sig, silu = silu_parts(prods[0])
            values = [prods[0], prods[1], silu * prods[1]]
        else:
            gate = jnp.concatenate([e_v[0][q, :] for q in pair], axis=0).astype(F32)
            up = jnp.concatenate([e_v[1][q, :] for q in pair], axis=0).astype(F32)
            sig, silu = silu_parts(gate)
            values = [prods[0] * up * sig * (1.0 + gate * (1.0 - sig)), prods[0] * silu]
        for j, value in enumerate(values):
            value = value.astype(o_v[j].dtype)
            for k in range(2):
                o_v[j][pair[k], :] = value[k * half : (k + 1) * half]
                pltpu.make_async_copy(
                    o_v[j].at[pair[k]], o_hbm[j].at[pair[k]], out_sem.at[p, k, j]
                ).start()
        for k in range(2):
            pltpu.make_async_copy(full.at[pair[k]], a_hbm.at[pair[k]], a_sem.at[p, k]).start()
        return carry

    lax.fori_loop(0, 4, step, 0)
    for i in range(2):
        to_cross(i).wait_send()
        to_sib(i).wait_send()
        relay(i).wait_send()
    for p in range(4):
        for k in range(2):
            for j in range(n_out):
                pltpu.make_async_copy(
                    o_v[j].at[pl.ds(0, half)], o_hbm[j].at[pl.ds(0, half)], out_sem.at[p, k, j]
                ).wait()
            pltpu.make_async_copy(
                full.at[pl.ds(0, half)], a_hbm.at[pl.ds(0, half)], a_sem.at[p, k]
            ).wait()
    bg.finish(bg_sems)


def gather_mm(x_rows, gain, weights, extras=(), trans=False, epilogue="plain", cid=0, tasks=()):
    rows, width = x_rows.shape
    length = rows * 4
    cols = [w.shape[0] if trans else w.shape[1] for w in weights]
    if epilogue == "plain":
        outs = [(c, F32) for c in cols]
    else:
        outs = [(cols[0], BF)] * (3 if epilogue == "ffn" else 2)
    norm = gain is not None
    cfg = (norm, len(weights), len(extras), trans, epilogue)
    bg = Background(tasks)
    parts = [part for w in weights for part in w.parts]
    operands = [x_rows] + ([gain.reshape(1, width)] if norm else []) + parts + list(extras)
    n_out = 1 + len(outs)
    flops = sum(2 * length * width * c for c in cols)
    moved = sum(w.size * 2 for w in weights) + sum(length * c * 2 for c, _ in outs) + length * width * 4
    result = pl.pallas_call(
        functools.partial(gather_kernel, cfg, weights, bg),
        out_shape=[jax.ShapeDtypeStruct((length, width), BF)]
        + [jax.ShapeDtypeStruct((length, c), t) for c, t in outs]
        + bg.outs,
        in_specs=[VM] * (2 if norm else 1) + [ANY] * (len(parts) + len(extras) + len(bg.inputs)),
        out_specs=[ANY] * (n_out + len(bg.outs)),
        scratch_shapes=[pltpu.VMEM((length, width), BF)]
        + [pltpu.VMEM(w.shape, BF) for w in weights]
        + [pltpu.VMEM(e.shape, e.dtype) for e in extras]
        + [pltpu.VMEM((length, c), t) for c, t in outs]
        + [DMA((len(weights), max(w.loads for w in weights)))]
        + [DMA((max(len(extras), 1),)), DMA((4, 2, len(outs))), DMA((4, 2))]
        + [DMA((2,))] * 6
        + bg.scratch,
        compiler_params=pltpu.CompilerParams(
            collective_id=cid, has_side_effects=True, vmem_limit_bytes=VMEM_BYTES
        ),
        cost_estimate=pl.CostEstimate(flops=flops, bytes_accessed=moved * 4, transcendentals=0),
        name=f"gather{cid}",
    )(*operands, *bg.inputs)
    return result[:n_out], result[n_out:]


def scatter_kernel(cfg, weights, bg, *refs):
    n_y, trans, epilogue = cfg
    it = iter(refs)
    y_hbm = [next(it) for _ in range(n_y)]
    w_hbm = [[next(it) for _ in w.parts] for w in weights]
    resid_ref = next(it)
    if epilogue == "back":
        value_ref, gain_ref = next(it), next(it)
    bg_in = [next(it) for _ in bg.inputs]
    out_ref = next(it)
    if epilogue == "back":
        gain_out = next(it)
    bg.bind(iter(bg_in), it)
    y_v = [next(it) for _ in range(n_y)]
    w_v = [next(it) for _ in range(n_y)]
    keep, own, to_s, from_s, to_c, from_c, to_o, from_o = (next(it) for _ in range(8))
    w_sem, in_sem, ds, dr, cs, cr, os_, or_, *bg_sems = it

    me, sib, cross, diag = places()
    rows = resid_ref.shape[0]
    half = rows // 2
    loads = [
        pltpu.make_async_copy(src, dst, in_sem.at[i])
        for i, (src, dst) in enumerate(zip(y_hbm, y_v))
    ]
    for i, w in enumerate(weights):
        loads += w.copies(w_hbm[i], w_v[i], w_sem.at[i])
    for load in loads:
        load.start()
    greet(bg.peers([{"tensor": sib}, {"tensor": cross}]))
    bg.start(bg_sems)
    for load in loads:
        load.wait()

    def send_diag(i):
        return remote(to_s.at[i], from_s.at[i], ds.at[i], dr.at[i], {"tensor": sib})

    def send_cross(i):
        return remote(to_c.at[i], from_c.at[i], cs.at[i], cr.at[i], {"tensor": cross})

    send_near = remote(to_o, from_o, os_, or_, {"tensor": sib})

    def pass_on(i):
        send_diag(i).wait_recv()
        to_c[i] = (keep[i] + from_s[i].astype(F32)).astype(BF)
        send_cross(i).start()

    def step(p, carry):
        near, sub = p // 2, p % 2
        base = near * ((1 - sub) * sib + sub * me) * rows
        first = base + (1 - near) * (cross * rows + sub * half)
        second = base + near * half + (1 - near) * (diag * rows + sub * half)
        pair = [pl.ds(pl.multiple_of(first, half), half), pl.ds(pl.multiple_of(second, half), half)]
        total = None
        for y, w in zip(y_v, w_v):
            a = jnp.concatenate([y[pair[0], :], y[pair[1], :]], axis=0)
            prod = contract(a, w[...], 1, 1 if trans else 0)
            total = prod if total is None else total + prod

        for i in range(2):

            @pl.when(p == i)
            def _():
                keep[i] = total[:half]
                to_s[i] = total[half:].astype(BF)
                send_diag(i).start()

        @pl.when(p == 1)
        def _():
            pass_on(0)

        @pl.when(p == 2)
        def _():
            to_o[...] = total.astype(BF)
            send_near.start()
            pass_on(1)

        @pl.when(p == 3)
        def _():
            own[...] = total

        return carry

    lax.fori_loop(0, 4, step, 0)
    send_near.wait_recv()
    gain_sum = None
    for i in range(2):
        part = pl.ds(i * half, half)
        send_cross(i).wait_recv()
        total = own[part, :] + from_o[part, :].astype(F32) + from_c[i].astype(F32)
        resid = resid_ref[part, :].astype(F32)
        if epilogue == "back":
            value_grad, gain_grad = norm_back(value_ref[part, :], gain_ref[...], total)
            out_ref[part, :] = resid + value_grad
            gain_sum = gain_grad if gain_sum is None else gain_sum + gain_grad
        else:
            out_ref[part, :] = resid + total
    if epilogue == "back":
        gain_out[...] = gain_sum.reshape(gain_out.shape)
    send_near.wait_send()
    for i in range(2):
        send_diag(i).wait_send()
        send_cross(i).wait_send()
    bg.finish(bg_sems)


def scatter_mm(operands, weights, resid, back=None, trans=False, cid=0, tasks=()):
    rows, width = resid.shape
    half = rows // 2
    epilogue = "plain" if back is None else "back"
    extra = [] if back is None else [back[0], back[1].reshape(1, width)]
    out_shape = [jax.ShapeDtypeStruct((rows, width), F32)]
    if back is not None:
        out_shape.append(jax.ShapeDtypeStruct((1, width), F32))
    n_out = len(out_shape)
    bg = Background(tasks)
    parts = [part for w in weights for part in w.parts]
    flops = sum(2 * y.size * width for y in operands)
    moved = sum(2 * (y.size + w.size) for y, w in zip(operands, weights)) + rows * width * 12
    result = pl.pallas_call(
        functools.partial(scatter_kernel, (len(operands), trans, epilogue), weights, bg),
        out_shape=out_shape + bg.outs,
        in_specs=[ANY] * (len(operands) + len(parts))
        + [VM] * (1 + len(extra))
        + [ANY] * len(bg.inputs),
        out_specs=[VM] * n_out + [ANY] * len(bg.outs),
        scratch_shapes=[pltpu.VMEM(y.shape, BF) for y in operands]
        + [pltpu.VMEM(w.shape, BF) for w in weights]
        + [pltpu.VMEM((2, half, width), F32), pltpu.VMEM((rows, width), F32)]
        + [pltpu.VMEM((2, half, width), BF)] * 4
        + [pltpu.VMEM((rows, width), BF)] * 2
        + [DMA((len(weights), max(w.loads for w in weights))), DMA((len(operands),))]
        + [DMA((2,))] * 4
        + [DMA] * 2
        + bg.scratch,
        compiler_params=pltpu.CompilerParams(
            collective_id=cid, has_side_effects=True, vmem_limit_bytes=VMEM_BYTES
        ),
        cost_estimate=pl.CostEstimate(flops=flops, bytes_accessed=moved * 4, transcendentals=0),
        name=f"scatter{cid}",
    )(*operands, *parts, resid, *extra, *bg.inputs)
    return result[:n_out], result[n_out:]


def conv_core(projected, x_value, kernel):
    channels = x_value.shape[1]
    b_gate = projected[:, :channels]
    c_gate = projected[:, channels:]
    product = b_gate * x_value
    tap_count = kernel.shape[0]
    causal = jnp.zeros_like(product)
    for offset in range(tap_count):
        causal = causal + kernel[offset] * delayed(product, tap_count - 1 - offset)
    return (b_gate, c_gate, product, causal)


def conv_back(projected, x_value, kernel, grad_y):
    b_gate, c_gate, product, causal = conv_core(projected, x_value, kernel)
    grad_c = grad_y * causal
    grad_causal = grad_y * c_gate
    tap_count = kernel.shape[0]
    kernel_rows = []
    grad_product = jnp.zeros_like(product)
    for offset in range(tap_count):
        delay_by = tap_count - 1 - offset
        kernel_rows.append(jnp.sum(grad_causal * delayed(product, delay_by), axis=0))
        grad_product = grad_product + kernel[offset] * advanced(grad_causal, delay_by)
    grad_proj = jnp.concatenate([grad_product * x_value, grad_c], axis=1).astype(BF)
    grad_value = (grad_product * b_gate).astype(BF)
    return (grad_proj, grad_value, jnp.stack(kernel_rows))


def attention_inputs(projected, head_gain):
    length = projected.shape[0]
    group_width = projected.shape[1] // 2
    head_size = head_gain.shape[1]
    group_size = HEADS // KV_HEADS
    kv_local = group_width // head_size // group_size
    queries = projected[:, :group_width].reshape(length, kv_local, group_size, head_size)
    key_part = projected[:, group_width : group_width + group_width // 2].reshape(
        length, kv_local, head_size
    )
    values = projected[:, group_width + group_width // 2 :].reshape(length, kv_local, head_size)
    cosine_table, sine_table = rotation(length, head_size)
    q_rot = rotate(
        norm_rows(queries, head_gain[0]),
        cosine_table[:, None, None, :],
        sine_table[:, None, None, :],
    ).astype(BF)
    k_rot = rotate(
        norm_rows(key_part, head_gain[1]), cosine_table[:, None, :], sine_table[:, None, :]
    ).astype(BF)
    return (queries, key_part, q_rot, k_rot, values.astype(BF), cosine_table, sine_table)


def masked_scores(q_piece, k_rot, first_row, length):
    row_block = q_piece.shape[0]
    score_scale = q_piece.shape[-1] ** (-0.5)
    scores = jnp.einsum("ahgd,bhd->hgab", q_piece, k_rot, preferred_element_type=F32) * score_scale
    query_pos = first_row + jnp.arange(row_block, dtype=jnp.int32)
    key_pos = jnp.arange(length, dtype=jnp.int32)
    allowed = key_pos[None, :] <= query_pos[:, None]
    return jnp.where(allowed, scores, MASKED)


def attention_forward(parts):
    q_rot, k_rot, v_low = (parts[2], parts[3], parts[4])
    length = q_rot.shape[0]
    row_block = min(512, length)
    out_blocks = []
    total_blocks = []
    for first_row in range(0, length, row_block):
        scores = masked_scores(q_rot[first_row : first_row + row_block], k_rot, first_row, length)
        row_max = jnp.max(scores, axis=-1, keepdims=True)
        exp_scores = jnp.exp(scores - row_max)
        row_sum = jnp.sum(exp_scores, axis=-1, keepdims=True)
        weights = (exp_scores / row_sum).astype(BF)
        attended = jnp.einsum("hgab,bhd->ahgd", weights, v_low, preferred_element_type=F32)
        out_blocks.append(attended.reshape(row_block, -1))
        total_blocks.append((row_max + jnp.log(row_sum))[..., 0])
    return (jnp.concatenate(out_blocks, axis=0).astype(BF), jnp.concatenate(total_blocks, axis=-1))


def attention_back(parts, log_total, head_gain, grad_y):
    queries, key_part, q_rot, k_rot, v_low, cosine_table, sine_table = parts
    length, kv_local, group_size, head_size = queries.shape
    score_scale = head_size ** (-0.5)
    row_block = min(512, length)
    grad_low = grad_y.astype(BF).reshape(length, kv_local, group_size, head_size)
    q_grads = []
    key_grad = jnp.zeros((length, kv_local, head_size), F32)
    value_grad = jnp.zeros((length, kv_local, head_size), F32)
    for first_row in range(0, length, row_block):
        q_piece = q_rot[first_row : first_row + row_block]
        scores = masked_scores(q_piece, k_rot, first_row, length)
        probability = jnp.exp(scores - log_total[:, :, first_row : first_row + row_block, None])
        weights = probability.astype(BF)
        grad_piece = grad_low[first_row : first_row + row_block]
        grad_weights = jnp.einsum("ahgd,bhd->hgab", grad_piece, v_low, preferred_element_type=F32)
        value_grad = value_grad + jnp.einsum(
            "hgab,ahgd->bhd", weights, grad_piece, preferred_element_type=F32
        )
        grad_scores = probability * (
            grad_weights - jnp.sum(probability * grad_weights, axis=-1, keepdims=True)
        )
        grad_scores = grad_scores.astype(BF)
        q_grads.append(
            jnp.einsum("hgab,bhd->ahgd", grad_scores, k_rot, preferred_element_type=F32)
            * score_scale
        )
        key_grad = (
            key_grad
            + jnp.einsum("hgab,ahgd->bhd", grad_scores, q_piece, preferred_element_type=F32)
            * score_scale
        )
    query_grad = jnp.concatenate(q_grads, axis=0)
    query_grad = rotate_back(
        query_grad, cosine_table[:, None, None, :], sine_table[:, None, None, :]
    )
    key_grad = rotate_back(key_grad, cosine_table[:, None, :], sine_table[:, None, :])
    query_raw, q_gain_grad = norm_back(queries, head_gain[0], query_grad)
    key_raw, k_gain_grad = norm_back(key_part, head_gain[1], key_grad)
    grad_proj = jnp.concatenate(
        [
            query_raw.reshape(length, -1),
            key_raw.reshape(length, -1),
            value_grad.reshape(length, -1),
        ],
        axis=1,
    ).astype(BF)
    return (grad_proj, jnp.stack([q_gain_grad, k_gain_grad]))


def low_grad(left_op, right_op):
    return contract_rows(left_op, right_op).astype(BF)


def body(boundary, norm_gain, mix_in, mix_out, w_gate, w_up, w_down, conv_x, conv_kernel, qk_gain):
    s, d, t = (lax.axis_index(a) for a in ("section", "dp", "tensor"))
    first = s == 0
    count = lax.axis_size("dp")
    model_width = boundary.shape[3]
    channels = mix_out.shape[1]

    def halves(shard):
        rows, cols = shard.shape
        return shard.reshape(2, rows // 2, cols)

    def pick(pair, index):
        return lax.dynamic_index_in_dim(pair, index, 0, keepdims=False)

    def by_block(kept, moved):
        return (jnp.where(first, kept, moved), jnp.where(first, moved, kept))

    def blocks_of(shards, moved):
        return [by_block(pick(shard, s), other) for shard, other in zip(shards, moved)]

    seqs = boundary[0]
    mix_shards = [halves(mix_in[0]), halves(mix_out[0])]
    ffn_shards = [halves(w_gate[0]), halves(w_up[0]), halves(w_down[0])]
    moved, gain_moved, *mix_moved = exchange(
        [x_half(seqs), x_swap(norm_gain[0])] + [x_half(v) for v in mix_shards], 16
    )
    x_low, cot = by_block(pick(seqs, s), moved)
    gains = by_block(norm_gain[0], gain_moved)
    h_in, h_out = blocks_of(mix_shards, mix_moved)

    z_in0, z_cols, z_out0, *ffn_moved = exchange(
        [z_gather(v) for v in (h_in[0], conv_x, h_out[0])] + [x_half(v) for v in ffn_shards], 17
    )
    h_gate, h_up, h_down = blocks_of(ffn_shards, ffn_moved)
    x_in0, x_cols, x_out0, z_gate0 = exchange(
        [x_gather(h_in[0], z_in0), x_gather(conv_x, z_cols), x_gather(h_out[0], z_out0)]
        + [z_gather(h_gate[0])],
        18,
    )
    in0 = Weight("rows", h_in[0], z_in0, x_in0)
    cols = Weight("conv", conv_x, z_cols, x_cols)
    out0 = Weight("cols", h_out[0], z_out0, x_out0)

    x_rows = x_low.astype(F32)
    (a0, proj0, value0), (x_gate0, z_up0) = gather_mm(
        x_rows, gains[0][0], [in0, cols], cid=0, tasks=[x_gather(h_gate[0], z_gate0), z_gather(h_up[0])]
    )
    gate_w0 = Weight("rows", h_gate[0], z_gate0, x_gate0)
    b_gate, c_gate, product, causal = conv_core(proj0, value0, conv_kernel)
    y0 = (c_gate * causal).astype(BF)
    (mid0,), (x_up0, z_down0) = scatter_mm(
        [y0], [out0], x_rows, cid=1, tasks=[x_gather(h_up[0], z_up0), z_gather(h_down[0])]
    )
    up_w0 = Weight("rows", h_up[0], z_up0, x_up0)
    (m0, gate0, up0, hid0), (x_down0, z_in1, z_out1) = gather_mm(
        mid0, gains[0][1], [gate_w0, up_w0], epilogue="ffn", cid=2,
        tasks=[x_gather(h_down[0], z_down0), z_gather(h_in[1]), z_gather(h_out[1])],
    )
    down_w0 = Weight("cols", h_down[0], z_down0, x_down0)
    (z_rows,), (x_in1, x_out1, z_gate1) = scatter_mm(
        [hid0], [down_w0], mid0, cid=3,
        tasks=[x_gather(h_in[1], z_in1), x_gather(h_out[1], z_out1), z_gather(h_gate[1])],
    )
    z_rows = z_rows.astype(BF).astype(F32)
    in1 = Weight("rows", h_in[1], z_in1, x_in1)
    out1 = Weight("cols", h_out[1], z_out1, x_out1)
    (a1, proj1), (x_gate1, z_up1) = gather_mm(
        z_rows, gains[1][0], [in1], cid=4, tasks=[x_gather(h_gate[1], z_gate1), z_gather(h_up[1])]
    )
    gate_w1 = Weight("rows", h_gate[1], z_gate1, x_gate1)
    parts = attention_inputs(proj1, qk_gain)
    y1, log_total = attention_forward(parts)
    (mid1,), (x_up1, z_down1) = scatter_mm(
        [y1], [out1], z_rows, cid=5, tasks=[x_gather(h_up[1], z_up1), z_gather(h_down[1])]
    )
    up_w1 = Weight("rows", h_up[1], z_up1, x_up1)
    (m1, gate1, up1, hid1), (x_down1,) = gather_mm(
        mid1, gains[1][1], [gate_w1, up_w1], epilogue="ffn", cid=6,
        tasks=[x_gather(h_down[1], z_down1)],
    )
    down_w1 = Weight("cols", h_down[1], z_down1, x_down1)
    (y_rows,), _ = scatter_mm([hid1], [down_w1], mid1, cid=7)
    y_rows = y_rows.astype(BF)

    def split_rows(grad):
        rows, width = grad.shape
        return grad.reshape(count, 2, rows // (2 * count), width)

    def sum_rows(grad, other):
        kept = lax.dynamic_index_in_dim(grad, s, 1, keepdims=False)
        return (kept.astype(F32) + other.astype(F32)).astype(BF)

    def split_cols(grad):
        rows, width = grad.shape
        return grad.reshape(2, rows // 2, width)

    def sum_cols(grad, other):
        total = (pick(grad, s).astype(F32) + other.astype(F32)).astype(BF)
        rows, width = total.shape
        return total.reshape(rows, count, width // count).transpose(1, 0, 2)

    def gathered(kept, others):
        own = (jnp.arange(count) == d).reshape((count,) + (1,) * (others.ndim - 1))
        return jnp.sum(jnp.where(own, kept, others).astype(F32), axis=0)

    (d_full1, d_gate1, d_up1), _ = gather_mm(
        cot, None, [down_w1], [gate1, up1], trans=True, epilogue="ffn_back", cid=8
    )
    g_down1 = split_cols(low_grad(hid1, d_full1))
    (d_mid1, gain11), (r_down1,) = scatter_mm(
        [d_gate1, d_up1], [gate_w1, up_w1], cot, (mid1, gains[1][1]), True, 9,
        tasks=[x_half(g_down1)],
    )
    g_gate1 = split_rows(low_grad(m1, d_gate1))
    s_down1 = sum_cols(g_down1, r_down1)
    (d_full, d_y1), (q_down1, r_gate1) = gather_mm(
        d_mid1, None, [out1], trans=True, cid=10, tasks=[z_scatter(s_down1), x_rows_of(g_gate1)]
    )
    g_out1 = split_cols(low_grad(y1, d_full))
    g_up1 = split_rows(low_grad(m1, d_up1))
    s_gate1 = sum_rows(g_gate1, r_gate1)
    d_proj1, head_grad = attention_back(parts, log_total, qk_gain, d_y1)
    (d_z, gain10), (q_gate1, r_up1) = scatter_mm(
        [d_proj1], [in1], d_mid1, (z_rows, gains[1][0]), True, 11,
        tasks=[z_scatter(s_gate1), x_rows_of(g_up1)],
    )
    d_z = d_z.astype(BF)
    g_in1 = split_rows(low_grad(a1, d_proj1))
    s_up1 = sum_rows(g_up1, r_up1)
    f_down1 = gathered(s_down1, q_down1).astype(BF)

    (d_full0, d_gate0, d_up0), (q_up1, r_in1, r_out1) = gather_mm(
        d_z, None, [down_w0], [gate0, up0], trans=True, epilogue="ffn_back", cid=12,
        tasks=[z_scatter(s_up1), x_rows_of(g_in1), x_half(g_out1)],
    )
    g_down0 = split_cols(low_grad(hid0, d_full0))
    s_in1, s_out1 = sum_rows(g_in1, r_in1), sum_cols(g_out1, r_out1)
    f_gate1 = gathered(s_gate1, q_gate1).astype(BF)
    (d_mid0, gain01), (q_in1, q_out1, r_down0, e_down1) = scatter_mm(
        [d_gate0, d_up0], [gate_w0, up_w0], d_z, (mid0, gains[0][1]), True, 13,
        tasks=[z_scatter(s_in1), z_scatter(s_out1), x_half(g_down0), x_final(f_down1, 1)],
    )
    g_gate0 = split_rows(low_grad(m0, d_gate0))
    s_down0 = sum_cols(g_down0, r_down0)
    f_up1 = gathered(s_up1, q_up1).astype(BF)
    (d_full, d_y0), (q_down0, r_gate0, e_gate1) = gather_mm(
        d_mid0, None, [out0], trans=True, cid=14,
        tasks=[z_scatter(s_down0), x_rows_of(g_gate0), x_final(f_gate1, 1)],
    )
    g_up0 = split_rows(low_grad(m0, d_up0))
    s_gate0 = sum_rows(g_gate0, r_gate0)
    d_proj0, d_value0, kernel_grad = conv_back(proj0, value0, conv_kernel, d_y0)
    f_in1 = gathered(s_in1, q_in1).astype(BF)
    f_out1 = gathered(s_out1, q_out1).astype(BF)
    (d_x, gain00), (q_gate0, r_up0, e_up1) = scatter_mm(
        [d_proj0, d_value0], [in0, cols], d_mid0, (x_rows, gains[0][0]), True, 15,
        tasks=[z_scatter(s_gate0), x_rows_of(g_up0), x_final(f_up1, 1)],
    )
    d_x = d_x.astype(BF)
    g_out0 = split_cols(low_grad(y0, d_full))
    g_in0 = split_rows(low_grad(a0, d_proj0))
    g_cols = low_grad(a0, d_value0).reshape(2, count, conv_x.shape[0], channels)
    s_up0 = sum_rows(g_up0, r_up0)
    f_down0 = gathered(s_down0, q_down0).astype(BF)

    small = jnp.concatenate(
        [
            gain00,
            gain01,
            gain10,
            gain11,
            lax.dynamic_update_slice_in_dim(
                jnp.zeros((conv_kernel.shape[0], model_width), F32), kernel_grad, t * channels, 1
            ),
            jnp.pad(head_grad.reshape(1, -1), ((0, 0), (0, model_width - head_grad.size))),
        ],
        axis=0,
    )
    out_sent = jnp.where(first, y_rows, d_x)
    q_up0, r_in0, r_cols, r_out0, small_x, out_moved, e_in1, e_out1, e_down0 = exchange(
        [z_scatter(s_up0), x_rows_of(g_in0), x_half(g_cols), x_half(g_out0), x_swap(small)]
        + [x_swap(out_sent), x_final(f_in1, 1), x_final(f_out1, 1), x_final(f_down0, 0)],
        19,
    )
    s_in0, s_out0 = sum_rows(g_in0, r_in0), sum_cols(g_out0, r_out0)
    s_cols = (pick(g_cols, s).astype(F32) + r_cols.astype(F32)).astype(BF)
    f_gate0 = gathered(s_gate0, q_gate0).astype(BF)
    f_up0 = gathered(s_up0, q_up0).astype(BF)
    small = small + small_x
    q_in0, q_cols, q_out0, small_z, e_gate0, e_up0 = exchange(
        [z_scatter(v) for v in (s_in0, s_cols, s_out0)]
        + [z_gather(small), x_final(f_gate0, 0), x_final(f_up0, 0)],
        20,
    )
    f_in0 = gathered(s_in0, q_in0).astype(BF)
    f_out0 = gathered(s_out0, q_out0).astype(BF)
    cols_part = gathered(s_cols, q_cols)
    small = gathered(small[None], small_z)
    e_in0, e_out0, small_t = exchange([x_final(f_in0, 0), x_final(f_out0, 0), t_share(small)], 21)
    own = (jnp.arange(4) == t).reshape(4, 1, 1)
    small = jnp.sum(jnp.where(own, small[None], small_t), axis=0)

    def whole(zero, zero_other, one, one_other):
        kept = jnp.where(first, zero, one)
        moved = jnp.where(first, zero_other, one_other)
        rows, width = kept.shape
        lower, upper = jnp.where(first, kept, moved), jnp.where(first, moved, kept)
        return jnp.concatenate([lower, upper], axis=0).astype(F32)[None]

    result = jnp.where(first, jnp.stack([d_x, out_moved]), jnp.stack([out_moved, y_rows]))
    gains_total = small[:4].reshape(2, 2, model_width)
    gain_out = lax.dynamic_slice_in_dim(gains_total, s, 1, 0)
    kernel_rows = small[4 : 4 + conv_kernel.shape[0]]
    kernel_out = lax.dynamic_slice_in_dim(kernel_rows, t * channels, channels, 1)
    head_total = small[-1, : qk_gain.size].reshape(qk_gain.shape)
    return (
        result[None],
        gain_out,
        whole(f_in0, e_in0, f_in1, e_in1),
        whole(f_out0, e_out0, f_out1, e_out1),
        whole(f_gate0, e_gate0, f_gate1, e_gate1),
        whole(f_up0, e_up0, f_up1, e_up1),
        whole(f_down0, e_down0, f_down1, e_down1),
        cols_part,
        kernel_out,
        head_total,
    )


def solution(mesh):
    in_specs = (
        P("section", "dp", "tensor", None),
        P("section", None, None),
        P("section", "dp", "tensor"),
        P("section", "tensor", "dp"),
        P("section", "dp", "tensor"),
        P("section", "dp", "tensor"),
        P("section", "tensor", "dp"),
        P(("section", "dp"), "tensor"),
        P(None, "tensor"),
        P(),
    )
    out_specs = (
        P("section", "dp", "tensor", None),
        P("section", None, None),
        P("section", "dp", "tensor"),
        P("section", "tensor", "dp"),
        P("section", "dp", "tensor"),
        P("section", "dp", "tensor"),
        P("section", "tensor", "dp"),
        P(("section", "dp"), "tensor"),
        P(None, "tensor"),
        P(),
    )
    return jax.shard_map(body, mesh=mesh, in_specs=in_specs, out_specs=out_specs, check_vma=False)
```

```python
import functools

import jax
import jax.numpy as jnp
from jax import lax
from jax.experimental import pallas as pl
from jax.experimental.pallas import tpu as pltpu
from jax.sharding import PartitionSpec as P

HEADS = 16
KV_HEADS = 8

EPS = 1e-05
ROPE_BASE = 1000000.0
MASKED = -1e30

MESH = pl.DeviceIdType.MESH
ANY = pl.BlockSpec(memory_space=pl.ANY)
VM = pl.BlockSpec(memory_space=pltpu.VMEM)
DMA = pltpu.SemaphoreType.DMA
VMEM_BYTES = 62 * 1024 * 1024
BF = jnp.bfloat16
F32 = jnp.float32


def contract(left_op, right_op, left_dim, right_dim):
    return lax.dot_general(
        left_op, right_op, (((left_dim,), (right_dim,)), ((), ())), preferred_element_type=F32
    )


def norm_rows(values, gain):
    return values * lax.rsqrt(jnp.mean(values * values, axis=-1, keepdims=True) + EPS) * gain


def norm_back(values, gain, grad_in):
    row_scale = lax.rsqrt(jnp.mean(values * values, axis=-1, keepdims=True) + EPS)
    normed = values * row_scale
    feature_count = values.shape[-1]
    gain_grad = jnp.sum((grad_in * normed).reshape(-1, feature_count), axis=0)
    scaled = grad_in * gain
    value_grad = row_scale * (scaled - normed * jnp.mean(scaled * normed, axis=-1, keepdims=True))
    return (value_grad, gain_grad)


def rotation(length, head_size):
    half_size = head_size // 2
    frequency = ROPE_BASE ** (-(jnp.arange(half_size, dtype=jnp.float32) * 2.0 / head_size))
    angles = jnp.arange(length, dtype=jnp.float32)[:, None] * frequency[None, :]
    cosine_table = jnp.concatenate([jnp.cos(angles), jnp.cos(angles)], axis=1)
    sine_table = jnp.concatenate([jnp.sin(angles), jnp.sin(angles)], axis=1)
    return (cosine_table, sine_table)


def delayed(values, delay_by):
    if delay_by == 0:
        return values
    return jnp.concatenate(
        [jnp.zeros((delay_by, values.shape[1]), values.dtype), values[:-delay_by]], axis=0
    )


def advanced(values, delay_by):
    if delay_by == 0:
        return values
    return jnp.concatenate(
        [values[delay_by:], jnp.zeros((delay_by, values.shape[1]), values.dtype)], axis=0
    )


def places():
    me = lax.axis_index("tensor")
    sib = me + 1 - 2 * (me % 2)
    cross = (me + 2) % 4
    diag = (sib + 2) % 4
    return me, sib, cross, diag


def greet(peers):
    barrier = pltpu.get_barrier_semaphore()
    for peer in peers:
        pl.semaphore_signal(barrier, inc=1, device_id=peer, device_id_type=MESH)
    pl.semaphore_wait(barrier, len(peers))


def remote(src, dst, send_sem, recv_sem, peer):
    return pltpu.make_async_remote_copy(
        src_ref=src, dst_ref=dst, send_sem=send_sem, recv_sem=recv_sem,
        device_id=peer, device_id_type=MESH,
    )


class Task:
    def __init__(self, inputs, out, axis, moves, count, final=None, room=()):
        self.inputs, self.out, self.axis, self.count = inputs, out, axis, count
        self.make, self.final, self.room = moves, final, list(room)
        self.scratch = [DMA((count,)), DMA((count,)), DMA((2 + dp_size(),))] + self.room

    def bind(self, ins, out, scratch):
        self.ins, self.out_ref = ins, out
        self.send_sem, self.recv_sem, self.local_sem, *self.bufs = scratch

    def at(self):
        return tuple(lax.axis_index(a) for a in ("section", "dp", "tensor"))

    def local(self, src, dst, i):
        return pltpu.make_async_copy(src, dst, self.local_sem.at[i])

    def load(self):
        pass

    def pairs(self):
        remotes, locals_ = self.make(self, *self.at())
        far = [
            [(cond, remote(src, dst, self.send_sem.at[i], self.recv_sem.at[i], peer))
             for cond, src in sources]
            for i, (sources, dst, peer) in enumerate(remotes)
        ]
        near = [
            [(cond, self.local(src, dst, i)) for cond, src in sources]
            for i, (sources, dst) in enumerate(locals_)
        ]
        return far, near

    def send(self):
        far, near = self.pairs()
        s = lax.axis_index("section")
        for variants in far:
            for cond, move in variants:
                if self.final is not None:
                    cond = s == 1 - self.final
                if cond is None:
                    move.start()
                else:
                    pl.when(cond)(move.start)
        for variants in near:
            for cond, move in variants:
                if cond is None:
                    move.start()
                else:
                    pl.when(cond)(move.start)

    def wait(self):
        far, near = self.pairs()
        s = lax.axis_index("section")
        for variants in far:
            move = variants[0][1]
            if self.final is None:
                move.wait_recv()
                move.wait_send()
            else:
                pl.when(s == 1 - self.final)(move.wait_send)
                pl.when(s == self.final)(move.wait_recv)
        for variants in near:
            variants[0][1].wait()


def dp_size():
    return lax.axis_size("dp")


def like(shape, value):
    return jax.ShapeDtypeStruct(shape, value.dtype)


def z_gather(piece):
    count = dp_size()

    def moves(task, s, d, t):
        far = [([(None, task.ins[0])], task.out_ref.at[d], {"dp": (d + k) % count}) for k in range(1, count)]
        return far, [([(None, task.ins[0])], task.out_ref.at[d])]

    return Task([piece], like((count,) + piece.shape, piece), "dp", moves, count - 1)


def z_gather_half(shard, moved, block):
    count = dp_size()

    def moves(task, s, d, t):
        sources = [(s == block, task.ins[0].at[block]), (s == 1 - block, task.ins[1])]
        far = [(sources, task.out_ref.at[d], {"dp": (d + k) % count}) for k in range(1, count)]
        return far, [(sources, task.out_ref.at[d])]

    return Task([shard, moved], like((count,) + shard.shape[1:], shard), "dp", moves, count - 1)


def x_move(value, index=None):
    def moves(task, s, d, t):
        src = task.ins[0] if index is None else task.ins[0].at[1 - s]
        return [([(None, src)], task.out_ref, {"section": 1 - s})], []

    out = value.out if isinstance(value, Task) else value
    shape = out.shape if index is None else out.shape[1:]
    return Task([value], jax.ShapeDtypeStruct(shape, out.dtype), "section", moves, 1)


def x_half(shard):
    return x_move(shard, 0)


def x_rows_of(grads):
    count = dp_size()

    def moves(task, s, d, t):
        return [
            ([(None, task.ins[0].at[k, 1 - s])], task.out_ref.at[k], {"section": 1 - s})
            for k in range(count)
        ], []

    return Task([grads], like((count,) + grads.shape[2:], grads), "section", moves, count)


def t_share(value):
    def moves(task, s, d, t):
        far = [([(None, task.ins[0])], task.out_ref.at[t], {"tensor": (t + k) % 4}) for k in range(1, 4)]
        return far, [([(None, task.ins[0])], task.out_ref.at[t])]

    return Task([value], like((4,) + value.shape, value), "tensor", moves, 3)


class SumScatter(Task):
    def __init__(self, kind, grads, received):
        count = dp_size()
        if kind == "cols":
            rows, width = grads.shape[1:]
            cols, held = width // count, (rows, width)
        else:
            rows, cols = grads.shape[2:]
            held = (count, rows, cols)
        self.kind, self.cols, self.n = kind, cols, count

        def moves(task, s, d, t):
            total = task.bufs[2]
            far = []
            for k in range(1, count):
                other = (d + k) % count
                far.append(([(None, total.at[other])], task.out_ref.at[d], {"dp": other}))
            return far, [([(None, total.at[d])], task.out_ref.at[d])]

        room = [pltpu.VMEM(held, BF)] * 2 + [pltpu.VMEM((count, rows, cols), BF)]
        super().__init__(
            [grads, received], like((count, rows, cols), grads), "dp", moves, count - 1, room=room
        )

    def loads(self):
        s = lax.axis_index("section")
        kept, got = self.bufs[:2]
        if self.kind == "rows":
            moves = [self.local(self.ins[0].at[k, s], kept.at[k], 2 + k) for k in range(self.n)]
        else:
            moves = [self.local(self.ins[0].at[s], kept, 2)]
        return moves + [self.local(self.ins[1], got, 1)]

    def load(self):
        for move in self.loads():
            move.start()

    def send(self):
        for move in self.loads():
            move.wait()
        kept, got, total = self.bufs
        for k in range(self.n):
            if self.kind == "cols":
                part = (slice(None), slice(k * self.cols, (k + 1) * self.cols))
            else:
                part = k
            total[k] = (kept[part].astype(F32) + got[part].astype(F32)).astype(BF)
        super().send()


class Finish(Task):
    def __init__(self, pieces, block):
        out = pieces.out if isinstance(pieces, Task) else pieces
        count, rows, cols = out.shape
        self.n = count

        def moves(task, s, d, t):
            total = task.bufs[1]
            far = [([(None, total)], task.out_ref.at[s], {"section": 1 - s})]
            return far, [([(None, total)], task.out_ref.at[s])]

        room = [pltpu.VMEM((count, rows, cols), BF), pltpu.VMEM((rows, cols), BF)]
        super().__init__(
            [pieces], like((2, rows, cols), out), "section", moves, 1, final=block, room=room
        )

    def load(self):
        self.local(self.ins[0], self.bufs[0], 1).start()

    def send(self):
        self.local(self.ins[0], self.bufs[0], 1).wait()
        held, total = self.bufs
        acc = held[0].astype(F32)
        for k in range(1, self.n):
            acc = acc + held[k].astype(F32)
        total[...] = acc.astype(BF)
        super().send()


class Background:
    def __init__(self, tasks):
        self.tasks = list(tasks)
        self.inputs = [v for task in self.tasks for v in task.inputs if not isinstance(v, Task)]
        self.outs = [task.out for task in self.tasks]
        self.scratch = [room for task in self.tasks for room in task.scratch]

    def bind(self, it_in, it_out):
        self.in_refs = [next(it_in) for _ in self.inputs]
        self.out_refs = [next(it_out) for _ in self.outs]

    def hold(self, scratch):
        scratch, ins = iter(scratch), iter(self.in_refs)
        for task, out in zip(self.tasks, self.out_refs):
            task.out_ref = out
        for task, out in zip(self.tasks, self.out_refs):
            refs = [v.out_ref if isinstance(v, Task) else next(ins) for v in task.inputs]
            task.bind(refs, out, [next(scratch) for _ in task.scratch])

    def peers(self, tensor):
        count = dp_size()
        s, d, t = (lax.axis_index(a) for a in ("section", "dp", "tensor"))
        axes = {task.axis for task in self.tasks}
        found = []
        if "section" in axes:
            found.append({"section": 1 - s})
        if "dp" in axes:
            found += [{"dp": (d + k) % count} for k in range(1, count)]
        if "tensor" in axes:
            found += [{"tensor": (t + k) % 4} for k in range(1, 4)]
        else:
            found += tensor
        return found

    def load(self):
        for task in self.tasks:
            task.load()

    def start(self):
        for task in sorted(self.tasks, key=lambda v: isinstance(v, (SumScatter, Finish))):
            task.send()

    def finish(self):
        for task in self.tasks:
            task.wait()

    def open(self, scratch):
        self.hold(scratch)
        if self.tasks:
            self.load()
            greet(self.peers([]))
            self.start()

    def close(self):
        self.finish()

    def params(self, cid):
        if not self.tasks:
            return pltpu.CompilerParams(vmem_limit_bytes=VMEM_BYTES)
        return pltpu.CompilerParams(
            collective_id=cid, has_side_effects=True, vmem_limit_bytes=VMEM_BYTES
        )


def exchange_kernel(bg, program, *refs):
    ins = iter(refs[: len(bg.inputs)])
    outs = iter(refs[len(bg.inputs) : len(bg.inputs) + len(bg.outs)])
    bg.bind(ins, outs)
    bg.hold(refs[len(bg.inputs) + len(bg.outs) :])
    for act, task in program:
        if act == "load":
            task.load()
    greet(bg.peers([]))
    for act, task in program:
        if act == "reload":
            task.load()
        elif act == "send":
            task.send()
        elif act == "wait":
            task.wait()


def exchange(tasks, program, cid):
    bg = Background(tasks)
    return pl.pallas_call(
        functools.partial(exchange_kernel, bg, program),
        out_shape=bg.outs,
        in_specs=[ANY] * len(bg.inputs),
        out_specs=[ANY] * len(bg.outs),
        scratch_shapes=bg.scratch,
        compiler_params=bg.params(cid),
        name=f"exchange{cid}",
    )(*bg.inputs)


class Weight:
    def __init__(self, kind, near, far):
        count, rows, cols = near.shape
        if kind == "cols":
            self.shape = (2 * rows, count * cols)
        else:
            self.shape = (2 * count * rows, cols)
        self.size = self.shape[0] * self.shape[1]
        if kind == "cols" and cols % 128:
            s = lax.axis_index("section")
            both = jnp.stack([jnp.where(s == 0, near, far), jnp.where(s == 0, far, near)])
            self.parts = [both.transpose(0, 2, 1, 3).reshape(self.shape)]
            self.kind, self.loads = "whole", 1
        else:
            self.kind, self.parts, self.loads = kind, [near, far], 2 * count

    def copies(self, refs, dst, sem):
        if self.kind == "whole":
            return [pltpu.make_async_copy(refs[0], dst, sem.at[0])]
        s = lax.axis_index("section")
        count, rows, cols = self.parts[0].shape

        def place(sec, own):
            if self.kind == "cols":
                top = pl.multiple_of(sec * rows, rows)
                return dst.at[pl.ds(top, rows), pl.ds(own * cols, cols)]
            slot = own * 2 + sec if self.kind == "rows" else sec * count + own
            return dst.at[pl.ds(pl.multiple_of(slot * rows, rows), rows)]

        moves = []
        for k in range(count):
            for i, sec in enumerate((s, 1 - s)):
                moves.append(pltpu.make_async_copy(refs[i].at[k], place(sec, k), sem.at[2 * k + i]))
        return moves


def grad_chunk(cols):
    return 384 if cols % 384 == 0 else 256


def grad_copies(dst_v, dst_hbm, sem):
    chunk = grad_chunk(dst_v.shape[0])
    return [
        pltpu.make_async_copy(
            dst_v.at[pl.ds(i * chunk, chunk)], dst_hbm.at[pl.ds(i * chunk, chunk)], sem.at[i]
        )
        for i in range(dst_v.shape[0] // chunk)
    ]


def grad_products(left, right, dst_v, dst_hbm, sem):
    cols = left.shape[1]
    chunk = grad_chunk(cols)

    def step(i, carry):
        part = pl.ds(pl.multiple_of(i * chunk, chunk), chunk)
        dst_v[part, :] = contract(left[:, part], right[...], 0, 0).astype(BF)
        pltpu.make_async_copy(dst_v.at[part], dst_hbm.at[part], sem.at[i]).start()
        return carry

    lax.fori_loop(0, cols // chunk, step, 0)


def silu_parts(gate):
    sig = 1.0 / (1.0 + jnp.exp(-gate))
    return sig, gate * sig


def gather_kernel(cfg, weights, bg, *refs):
    norm, n_w, n_x, trans, epilogue, with_grad = cfg
    it = iter(refs)
    x_ref = next(it)
    gain_ref = next(it) if norm else None
    w_hbm = [[next(it) for _ in w.parts] for w in weights]
    e_hbm = [next(it) for _ in range(n_x)]
    left_hbm = next(it) if with_grad else None
    bg_in = [next(it) for _ in bg.inputs]
    a_hbm = next(it)
    n_out = {"plain": n_w, "ffn": 3, "ffn_back": 2}[epilogue]
    o_hbm = [next(it) for _ in range(n_out)]
    grad_hbm = next(it) if with_grad else None
    bg.bind(iter(bg_in), it)
    full = next(it)
    w_v = [next(it) for _ in range(n_w)]
    e_v = [next(it) for _ in range(n_x)]
    o_v = [next(it) for _ in range(n_out)]
    if with_grad:
        left, grad_v, left_sem, grad_sem = (next(it) for _ in range(4))
        left_load = pltpu.make_async_copy(left_hbm, left, left_sem)
    w_sem, in_sem, out_sem, a_sem, xs, xr, ss, sr, ls, lr, *bg_room = it
    bg.hold(bg_room)

    me, sib, cross, diag = places()
    rows = x_ref.shape[0]
    half = rows // 2
    loads = [
        pltpu.make_async_copy(src, dst, in_sem.at[i])
        for i, (src, dst) in enumerate(zip(e_hbm, e_v))
    ]
    for i, w in enumerate(weights):
        loads += w.copies(w_hbm[i], w_v[i], w_sem.at[i])
    for load in loads:
        load.start()
    if with_grad:
        left_load.start()
    bg.load()
    greet(bg.peers([{"tensor": sib}, {"tensor": cross}]))

    def span(owner, sub):
        return pl.ds(pl.multiple_of(owner * rows + sub * half, half), half)

    def to_cross(i):
        return remote(full.at[span(me, i)], full.at[span(me, i)], xs.at[i], xr.at[i], {"tensor": cross})

    def to_sib(i):
        return remote(full.at[span(me, i)], full.at[span(me, i)], ss.at[i], sr.at[i], {"tensor": sib})

    def relay(i):
        return remote(full.at[span(cross, i)], full.at[span(cross, i)], ls.at[i], lr.at[i], {"tensor": sib})

    for i in range(2):
        part = x_ref[pl.ds(i * half, half), :]
        if norm:
            part = norm_rows(part, gain_ref[...])
        full[span(me, i), :] = part.astype(BF)
        to_cross(i).start()
        to_sib(i).start()
    bg.start()
    for load in loads:
        load.wait()

    def step(p, carry):
        far, sub = p // 2, p % 2
        near = (1 - sub) * me + sub * sib
        first = (1 - far) * near * rows + far * (cross * rows + sub * half)
        second = (1 - far) * (near * rows + half) + far * (diag * rows + sub * half)
        pair = [pl.ds(pl.multiple_of(first, half), half), pl.ds(pl.multiple_of(second, half), half)]

        @pl.when(p == 1)
        def _():
            to_sib(0).wait_recv()
            to_sib(1).wait_recv()

        for i in range(2):

            @pl.when(p == 2 + i)
            def _():
                to_cross(i).wait_recv()
                relay(i).start()
                relay(i).wait_recv()

        a = jnp.concatenate([full[pair[0], :], full[pair[1], :]], axis=0)
        prods = [contract(a, w[...], 1, 1 if trans else 0) for w in w_v]
        if epilogue == "plain":
            values = prods
        elif epilogue == "ffn":
            sig, silu = silu_parts(prods[0])
            values = [prods[0], prods[1], silu * prods[1]]
        else:
            gate = jnp.concatenate([e_v[0][q, :] for q in pair], axis=0).astype(F32)
            up = jnp.concatenate([e_v[1][q, :] for q in pair], axis=0).astype(F32)
            sig, silu = silu_parts(gate)
            values = [prods[0] * up * sig * (1.0 + gate * (1.0 - sig)), prods[0] * silu]
        for j, value in enumerate(values):
            value = value.astype(o_v[j].dtype)
            for k in range(2):
                o_v[j][pair[k], :] = value[k * half : (k + 1) * half]
                pltpu.make_async_copy(
                    o_v[j].at[pair[k]], o_hbm[j].at[pair[k]], out_sem.at[p, k, j]
                ).start()
        for k in range(2):
            pltpu.make_async_copy(full.at[pair[k]], a_hbm.at[pair[k]], a_sem.at[p, k]).start()
        return carry

    lax.fori_loop(0, 4, step, 0)
    if with_grad:
        left_load.wait()
        grad_products(left, full, grad_v, grad_hbm, grad_sem)
        for copy in grad_copies(grad_v, grad_hbm, grad_sem):
            copy.wait()
    for i in range(2):
        to_cross(i).wait_send()
        to_sib(i).wait_send()
        relay(i).wait_send()
    for p in range(4):
        for k in range(2):
            for j in range(n_out):
                pltpu.make_async_copy(
                    o_v[j].at[pl.ds(0, half)], o_hbm[j].at[pl.ds(0, half)], out_sem.at[p, k, j]
                ).wait()
            pltpu.make_async_copy(
                full.at[pl.ds(0, half)], a_hbm.at[pl.ds(0, half)], a_sem.at[p, k]
            ).wait()
    bg.finish()


def gather_mm(x_rows, gain, weights, extras=(), trans=False, epilogue="plain", cid=0, tasks=(), left=None):
    rows, width = x_rows.shape
    length = rows * 4
    cols = [w.shape[0] if trans else w.shape[1] for w in weights]
    if epilogue == "plain":
        outs = [(c, F32) for c in cols]
    else:
        outs = [(cols[0], BF)] * (3 if epilogue == "ffn" else 2)
    norm = gain is not None
    cfg = (norm, len(weights), len(extras), trans, epilogue, left is not None)
    bg = Background(tasks)
    parts = [part for w in weights for part in w.parts]
    operands = [x_rows] + ([gain.reshape(1, width)] if norm else []) + parts + list(extras)
    n_out = 1 + len(outs)
    grad_out, grad_room = [], []
    if left is not None:
        operands.append(left)
        grad_out = [jax.ShapeDtypeStruct((left.shape[1], width), BF)]
        grad_room = [pltpu.VMEM(left.shape, BF), pltpu.VMEM((left.shape[1], width), BF), DMA]
        grad_room.append(DMA((left.shape[1] // grad_chunk(left.shape[1]),)))
        n_out += 1
    flops = sum(2 * length * width * c for c in cols)
    moved = sum(w.size * 2 for w in weights) + sum(length * c * 2 for c, _ in outs) + length * width * 4
    result = pl.pallas_call(
        functools.partial(gather_kernel, cfg, weights, bg),
        out_shape=[jax.ShapeDtypeStruct((length, width), BF)]
        + [jax.ShapeDtypeStruct((length, c), t) for c, t in outs]
        + grad_out
        + bg.outs,
        in_specs=[VM] * (2 if norm else 1)
        + [ANY] * (len(operands) - (2 if norm else 1) + len(bg.inputs)),
        out_specs=[ANY] * (n_out + len(bg.outs)),
        scratch_shapes=[pltpu.VMEM((length, width), BF)]
        + [pltpu.VMEM(w.shape, BF) for w in weights]
        + [pltpu.VMEM(e.shape, e.dtype) for e in extras]
        + [pltpu.VMEM((length, c), t) for c, t in outs]
        + grad_room
        + [DMA((len(weights), max(w.loads for w in weights)))]
        + [DMA((max(len(extras), 1),)), DMA((4, 2, len(outs))), DMA((4, 2))]
        + [DMA((2,))] * 6
        + bg.scratch,
        compiler_params=pltpu.CompilerParams(
            collective_id=cid, has_side_effects=True, vmem_limit_bytes=VMEM_BYTES
        ),
        cost_estimate=pl.CostEstimate(flops=flops, bytes_accessed=moved * 4, transcendentals=0),
        name=f"gather{cid}",
    )(*operands, *bg.inputs)
    return result[:n_out], result[n_out:]


def scatter_kernel(cfg, weights, bg, *refs):
    n_y, trans, epilogue, with_grad = cfg
    it = iter(refs)
    y_hbm = [next(it) for _ in range(n_y)]
    w_hbm = [[next(it) for _ in w.parts] for w in weights]
    resid_ref = next(it)
    if epilogue == "back":
        value_ref, gain_ref = next(it), next(it)
    left_hbm = next(it) if with_grad else None
    bg_in = [next(it) for _ in bg.inputs]
    out_ref = next(it)
    if epilogue == "back":
        gain_out = next(it)
    grad_hbm = [next(it) for _ in range(n_y)] if with_grad else []
    bg.bind(iter(bg_in), it)
    y_v = [next(it) for _ in range(n_y)]
    w_v = [next(it) for _ in range(n_y)]
    keep, own, to_s, from_s, to_c, from_c, to_o, from_o = (next(it) for _ in range(8))
    if with_grad:
        left, left_sem, grad_sem = (next(it) for _ in range(3))
        grad_v = [next(it) for _ in range(n_y)]
        left_load = pltpu.make_async_copy(left_hbm, left, left_sem)
    w_sem, in_sem, ds, dr, cs, cr, os_, or_, *bg_room = it
    bg.hold(bg_room)

    me, sib, cross, diag = places()
    rows = resid_ref.shape[0]
    half = rows // 2
    loads = [
        pltpu.make_async_copy(src, dst, in_sem.at[i])
        for i, (src, dst) in enumerate(zip(y_hbm, y_v))
    ]
    for i, w in enumerate(weights):
        loads += w.copies(w_hbm[i], w_v[i], w_sem.at[i])
    for load in loads:
        load.start()
    if with_grad:
        left_load.start()
    bg.load()
    greet(bg.peers([{"tensor": sib}, {"tensor": cross}]))
    bg.start()
    for load in loads:
        load.wait()

    def send_diag(i):
        return remote(to_s.at[i], from_s.at[i], ds.at[i], dr.at[i], {"tensor": sib})

    def send_cross(i):
        return remote(to_c.at[i], from_c.at[i], cs.at[i], cr.at[i], {"tensor": cross})

    send_near = remote(to_o, from_o, os_, or_, {"tensor": sib})

    def pass_on(i):
        send_diag(i).wait_recv()
        to_c[i] = (keep[i] + from_s[i].astype(F32)).astype(BF)
        send_cross(i).start()

    def step(p, carry):
        near, sub = p // 2, p % 2
        base = near * ((1 - sub) * sib + sub * me) * rows
        first = base + (1 - near) * (cross * rows + sub * half)
        second = base + near * half + (1 - near) * (diag * rows + sub * half)
        pair = [pl.ds(pl.multiple_of(first, half), half), pl.ds(pl.multiple_of(second, half), half)]
        total = None
        for y, w in zip(y_v, w_v):
            a = jnp.concatenate([y[pair[0], :], y[pair[1], :]], axis=0)
            prod = contract(a, w[...], 1, 1 if trans else 0)
            total = prod if total is None else total + prod

        for i in range(2):

            @pl.when(p == i)
            def _():
                keep[i] = total[:half]
                to_s[i] = total[half:].astype(BF)
                send_diag(i).start()

        @pl.when(p == 1)
        def _():
            pass_on(0)

        @pl.when(p == 2)
        def _():
            to_o[...] = total.astype(BF)
            send_near.start()
            pass_on(1)

        @pl.when(p == 3)
        def _():
            own[...] = total

        return carry

    lax.fori_loop(0, 4, step, 0)
    if with_grad:
        left_load.wait()
        for j in range(n_y):
            grad_products(left, y_v[j], grad_v[j], grad_hbm[j], grad_sem.at[j])
    send_near.wait_recv()
    gain_sum = None
    for i in range(2):
        part = pl.ds(i * half, half)
        send_cross(i).wait_recv()
        total = own[part, :] + from_o[part, :].astype(F32) + from_c[i].astype(F32)
        resid = resid_ref[part, :].astype(F32)
        if epilogue == "back":
            value_grad, gain_grad = norm_back(value_ref[part, :], gain_ref[...], total)
            out_ref[part, :] = resid + value_grad
            gain_sum = gain_grad if gain_sum is None else gain_sum + gain_grad
        else:
            out_ref[part, :] = resid + total
    if epilogue == "back":
        gain_out[...] = gain_sum.reshape(gain_out.shape)
    send_near.wait_send()
    for i in range(2):
        send_diag(i).wait_send()
        send_cross(i).wait_send()
    for j in range(n_y if with_grad else 0):
        for copy in grad_copies(grad_v[j], grad_hbm[j], grad_sem.at[j]):
            copy.wait()
    bg.finish()


def scatter_mm(operands, weights, resid, back=None, trans=False, cid=0, tasks=(), left=None):
    rows, width = resid.shape
    half = rows // 2
    epilogue = "plain" if back is None else "back"
    extra = [] if back is None else [back[0], back[1].reshape(1, width)]
    out_shape = [jax.ShapeDtypeStruct((rows, width), F32)]
    if back is not None:
        out_shape.append(jax.ShapeDtypeStruct((1, width), F32))
    n_out = len(out_shape)
    grad_out, grad_room, operand_left = [], [], []
    if left is not None:
        operand_left = [left]
        chunks = left.shape[1] // grad_chunk(left.shape[1])
        grad_out = [jax.ShapeDtypeStruct((left.shape[1], y.shape[1]), BF) for y in operands]
        grad_room = [pltpu.VMEM(left.shape, BF), DMA, DMA((len(operands), chunks))]
        grad_room += [pltpu.VMEM(g.shape, BF) for g in grad_out]
    bg = Background(tasks)
    parts = [part for w in weights for part in w.parts]
    flops = sum(2 * y.size * width for y in operands)
    moved = sum(2 * (y.size + w.size) for y, w in zip(operands, weights)) + rows * width * 12
    result = pl.pallas_call(
        functools.partial(scatter_kernel, (len(operands), trans, epilogue, left is not None), weights, bg),
        out_shape=out_shape + grad_out + bg.outs,
        in_specs=[ANY] * (len(operands) + len(parts))
        + [VM] * (1 + len(extra))
        + [ANY] * (len(operand_left) + len(bg.inputs)),
        out_specs=[VM] * n_out + [ANY] * (len(grad_out) + len(bg.outs)),
        scratch_shapes=[pltpu.VMEM(y.shape, BF) for y in operands]
        + [pltpu.VMEM(w.shape, BF) for w in weights]
        + [pltpu.VMEM((2, half, width), F32), pltpu.VMEM((rows, width), F32)]
        + [pltpu.VMEM((2, half, width), BF)] * 4
        + [pltpu.VMEM((rows, width), BF)] * 2
        + grad_room
        + [DMA((len(weights), max(w.loads for w in weights))), DMA((len(operands),))]
        + [DMA((2,))] * 4
        + [DMA] * 2
        + bg.scratch,
        compiler_params=pltpu.CompilerParams(
            collective_id=cid, has_side_effects=True, vmem_limit_bytes=VMEM_BYTES
        ),
        cost_estimate=pl.CostEstimate(flops=flops, bytes_accessed=moved * 4, transcendentals=0),
        name=f"scatter{cid}",
    )(*operands, *parts, resid, *extra, *operand_left, *bg.inputs)
    n_out += len(grad_out)
    return result[:n_out], result[n_out:]


def conv_core(projected, x_value, kernel):
    channels = x_value.shape[1]
    b_gate = projected[:, :channels]
    c_gate = projected[:, channels:]
    product = b_gate * x_value
    tap_count = kernel.shape[0]
    causal = jnp.zeros_like(product)
    for offset in range(tap_count):
        causal = causal + kernel[offset] * delayed(product, tap_count - 1 - offset)
    return (b_gate, c_gate, product, causal)


def conv_back(projected, x_value, kernel, grad_y):
    b_gate, c_gate, product, causal = conv_core(projected, x_value, kernel)
    grad_c = grad_y * causal
    grad_causal = grad_y * c_gate
    tap_count = kernel.shape[0]
    kernel_rows = []
    grad_product = jnp.zeros_like(product)
    for offset in range(tap_count):
        delay_by = tap_count - 1 - offset
        kernel_rows.append(jnp.sum(grad_causal * delayed(product, delay_by), axis=0))
        grad_product = grad_product + kernel[offset] * advanced(grad_causal, delay_by)
    grad_proj = jnp.concatenate([grad_product * x_value, grad_c], axis=1).astype(BF)
    grad_value = (grad_product * b_gate).astype(BF)
    return (grad_proj, grad_value, jnp.stack(kernel_rows))


def head_mean(values, head_size):
    width = values.shape[1]
    row = lax.broadcasted_iota(jnp.int32, (width, width), 0) // head_size
    col = lax.broadcasted_iota(jnp.int32, (width, width), 1) // head_size
    group = jnp.where(row == col, 1.0 / head_size, 0.0).astype(F32)
    return lax.dot_general(
        values, group, (((1,), (0,)), ((), ())),
        precision=lax.Precision.HIGHEST, preferred_element_type=F32,
    )


def turn(values, head_size, back):
    width, half = values.shape[1], head_size // 2
    lane = lax.broadcasted_iota(jnp.int32, values.shape, 1) % head_size
    upper = pltpu.roll(values, width - half, 1)
    lower = pltpu.roll(values, half, 1)
    return jnp.where(lane < half, upper, -lower) if back else jnp.where(lane < half, -upper, lower)


def head_norm(values, gain, head_size):
    return values * lax.rsqrt(head_mean(values * values, head_size) + EPS) * gain


def head_norm_back(values, gain, grad_in, head_size):
    row_scale = lax.rsqrt(head_mean(values * values, head_size) + EPS)
    normed = values * row_scale
    gain_grad = jnp.sum(grad_in * normed, axis=0, keepdims=True)
    scaled = grad_in * gain
    return row_scale * (scaled - normed * head_mean(scaled * normed, head_size)), gain_grad


ROW_BLOCK = 256


def block_weights(q_rows, k_rows, first_row):
    rows, length = q_rows.shape[0], k_rows.shape[0]
    scores = contract(q_rows, k_rows, 1, 1) * (q_rows.shape[1] ** -0.5)
    query = first_row + lax.broadcasted_iota(jnp.int32, (rows, length), 0)
    key = lax.broadcasted_iota(jnp.int32, (rows, length), 1)
    scores = jnp.where(key <= query, scores, MASKED)
    exps = jnp.exp(scores - jnp.max(scores, axis=1, keepdims=True))
    return exps * (1.0 / jnp.sum(exps, axis=1, keepdims=True))


def attend_kernel(dims, bg, *refs):
    length, heads, kv_heads, size = dims
    it = iter(refs)
    proj, gain, cos, sin = (next(it) for _ in range(4))
    bg_in = [next(it) for _ in bg.inputs]
    y_out, q_out, k_out = (next(it) for _ in range(3))
    bg.bind(iter(bg_in), it)
    q_h, k_h, v_h, y_h, *room = it
    bg.open(room)
    q_cols, k_cols = heads * size, kv_heads * size

    def prepare(p, carry):
        rows = pl.ds(pl.multiple_of(p * ROW_BLOCK, ROW_BLOCK), ROW_BLOCK)
        c, n = cos[rows, :], sin[rows, :]
        q = head_norm(proj[rows, :q_cols], gain[0:1, :], size)
        q = (q * c + turn(q, size, False) * n).astype(BF)
        k = head_norm(proj[rows, q_cols : q_cols + k_cols], gain[1:2, :k_cols], size)
        k = (k * c[:, :k_cols] + turn(k, size, False) * n[:, :k_cols]).astype(BF)
        q_out[rows, :] = q
        k_out[rows, :] = k
        for h in range(heads):
            q_h[h, rows, :] = q[:, h * size : (h + 1) * size]
        v = proj[rows, q_cols + k_cols :].astype(BF)
        for g in range(kv_heads):
            k_h[g, rows, :] = k[:, g * size : (g + 1) * size]
            v_h[g, rows, :] = v[:, g * size : (g + 1) * size]
        return carry

    lax.fori_loop(0, length // ROW_BLOCK, prepare, 0)

    def head(h, carry):
        g = h // (heads // kv_heads)
        for i in range(length // ROW_BLOCK):
            rows, seen = pl.ds(i * ROW_BLOCK, ROW_BLOCK), pl.ds(0, (i + 1) * ROW_BLOCK)
            weights = block_weights(q_h[h, rows, :], k_h[g, seen, :], i * ROW_BLOCK)
            y_h[h, rows, :] = contract(weights.astype(BF), v_h[g, seen, :], 1, 0).astype(BF)
        return carry

    lax.fori_loop(0, heads, head, 0)
    y_out[...] = jnp.concatenate([y_h[h] for h in range(heads)], axis=1)
    bg.close()


def attend_back_kernel(dims, bg, *refs):
    length, heads, kv_heads, size = dims
    it = iter(refs)
    proj, q_rot, k_rot, dy, gain, cos, sin = (next(it) for _ in range(7))
    bg_in = [next(it) for _ in bg.inputs]
    d_proj, q_gain, k_gain = (next(it) for _ in range(3))
    bg.bind(iter(bg_in), it)
    q_h, k_h, v_h, dy_h, dq_h, dk_h, dv_h, *room = it
    bg.open(room)
    q_cols, k_cols = heads * size, kv_heads * size
    scale = size**-0.5

    def prepare(p, carry):
        rows = pl.ds(pl.multiple_of(p * ROW_BLOCK, ROW_BLOCK), ROW_BLOCK)
        low = dy[rows, :].astype(BF)
        q, k, v = q_rot[rows, :], k_rot[rows, :], proj[rows, q_cols + k_cols :].astype(BF)
        for h in range(heads):
            q_h[h, rows, :] = q[:, h * size : (h + 1) * size]
            dy_h[h, rows, :] = low[:, h * size : (h + 1) * size]
        for g in range(kv_heads):
            k_h[g, rows, :] = k[:, g * size : (g + 1) * size]
            v_h[g, rows, :] = v[:, g * size : (g + 1) * size]
        return carry

    lax.fori_loop(0, length // ROW_BLOCK, prepare, 0)
    dk_h[...] = jnp.zeros_like(dk_h)
    dv_h[...] = jnp.zeros_like(dv_h)

    def head(h, carry):
        g = h // (heads // kv_heads)
        for i in range(length // ROW_BLOCK):
            rows, seen = pl.ds(i * ROW_BLOCK, ROW_BLOCK), pl.ds(0, (i + 1) * ROW_BLOCK)
            q, low, k = q_h[h, rows, :], dy_h[h, rows, :], k_h[g, seen, :]
            prob = block_weights(q, k, i * ROW_BLOCK)
            d_weights = contract(low, v_h[g, seen, :], 1, 1)
            dv_h[g, seen, :] += contract(prob.astype(BF), low, 0, 0)
            inner = jnp.sum(prob * d_weights, axis=1, keepdims=True)
            d_scores = (prob * (d_weights - inner)).astype(BF)
            dq_h[h, rows, :] = contract(d_scores, k, 1, 0) * scale
            dk_h[g, seen, :] += contract(d_scores, q, 0, 0) * scale
        return carry

    lax.fori_loop(0, heads, head, 0)
    q_gain[...] = jnp.zeros_like(q_gain)
    k_gain[...] = jnp.zeros_like(k_gain)

    def finish(p, carry):
        rows = pl.ds(pl.multiple_of(p * ROW_BLOCK, ROW_BLOCK), ROW_BLOCK)
        c, n = cos[rows, :], sin[rows, :]
        dq = jnp.concatenate([dq_h[h, rows, :] for h in range(heads)], axis=1)
        dk = jnp.concatenate([dk_h[g, rows, :] for g in range(kv_heads)], axis=1)
        dv = jnp.concatenate([dv_h[g, rows, :] for g in range(kv_heads)], axis=1)
        dq = dq * c + turn(dq * n, size, True)
        dk = dk * c[:, :k_cols] + turn(dk * n[:, :k_cols], size, True)
        dq, q_sum = head_norm_back(proj[rows, :q_cols], gain[0:1, :], dq, size)
        dk, k_sum = head_norm_back(
            proj[rows, q_cols : q_cols + k_cols], gain[1:2, :k_cols], dk, size
        )
        q_gain[...] += q_sum
        k_gain[...] += k_sum
        d_proj[rows, :q_cols] = dq.astype(BF)
        d_proj[rows, q_cols : q_cols + k_cols] = dk.astype(BF)
        d_proj[rows, q_cols + k_cols :] = dv.astype(BF)
        return carry

    lax.fori_loop(0, length // ROW_BLOCK, finish, 0)
    bg.close()


def attention_dims(proj, qk_gain):
    length, width = proj.shape
    size = qk_gain.shape[1]
    heads = width // 2 // size
    return length, heads, heads // (HEADS // KV_HEADS), size


def attention_tables(width, length, qk_gain):
    size = qk_gain.shape[1]
    heads = width // 2 // size
    cosine_table, sine_table = rotation(length, size)
    return [jnp.tile(v, (1, heads)) for v in (qk_gain, cosine_table, sine_table)]


def attend(proj, qk_gain, tables, cid, tasks=()):
    dims = attention_dims(proj, qk_gain)
    length, heads, kv_heads, size = dims
    bg = Background(tasks)
    out = [jax.ShapeDtypeStruct((length, heads * size), BF)] * 2
    out.append(jax.ShapeDtypeStruct((length, kv_heads * size), BF))
    result = pl.pallas_call(
        functools.partial(attend_kernel, dims, bg),
        out_shape=out + bg.outs,
        in_specs=[VM] * 4 + [ANY] * len(bg.inputs),
        out_specs=[VM] * 3 + [ANY] * len(bg.outs),
        scratch_shapes=[
            pltpu.VMEM((n, length, size), BF) for n in (heads, kv_heads, kv_heads, heads)
        ]
        + bg.scratch,
        compiler_params=bg.params(cid),
        name=f"attend{cid}",
    )(proj, *tables, *bg.inputs)
    return result[:3], result[3:]


def attend_back(proj, rotated, d_y, qk_gain, tables, cid, tasks=()):
    dims = attention_dims(proj, qk_gain)
    length, heads, kv_heads, size = dims
    bg = Background(tasks)
    out = [
        jax.ShapeDtypeStruct(proj.shape, BF),
        jax.ShapeDtypeStruct((1, heads * size), F32),
        jax.ShapeDtypeStruct((1, kv_heads * size), F32),
    ]
    shapes = [(heads, BF), (kv_heads, BF), (kv_heads, BF), (heads, BF), (heads, F32)]
    shapes += [(kv_heads, F32)] * 2
    (d_proj, q_gain, k_gain), rest = (lambda r: (r[:3], r[3:]))(
        pl.pallas_call(
            functools.partial(attend_back_kernel, dims, bg),
            out_shape=out + bg.outs,
            in_specs=[VM] * 7 + [ANY] * len(bg.inputs),
            out_specs=[VM] * 3 + [ANY] * len(bg.outs),
            scratch_shapes=[pltpu.VMEM((n, length, size), kind) for n, kind in shapes]
            + bg.scratch,
            compiler_params=bg.params(cid),
            name=f"attend_back{cid}",
        )(proj, *rotated, d_y, *tables, *bg.inputs)
    )
    head_grad = jnp.stack(
        [jnp.sum(v.reshape(-1, size), axis=0) for v in (q_gain, k_gain)]
    )
    return (d_proj, head_grad), rest


def body(boundary, norm_gain, mix_in, mix_out, w_gate, w_up, w_down, conv_x, conv_kernel, qk_gain):
    s, d, t = (lax.axis_index(a) for a in ("section", "dp", "tensor"))
    first = s == 0
    count = dp_size()
    model_width = boundary.shape[3]
    channels = mix_out.shape[1]

    def halves(shard):
        rows, cols = shard.shape
        return shard.reshape(2, rows // 2, cols)

    def pick(pair, index):
        return lax.dynamic_index_in_dim(pair, index, 0, keepdims=False)

    def by_block(kept, moved):
        return (jnp.where(first, kept, moved), jnp.where(first, moved, kept))

    seqs = boundary[0]
    sh_in, sh_out, sh_gate, sh_up, sh_down = (
        halves(v[0]) for v in (mix_in, mix_out, w_gate, w_up, w_down)
    )
    t_in, t_out, t_gate, t_seq, t_up, t_down = (
        x_half(v) for v in (sh_in, sh_out, sh_gate, seqs, sh_up, sh_down)
    )
    t_gain, zt_cols = x_move(norm_gain[0]), z_gather(conv_x)
    zt_in, zt_out, zt_gate = (
        z_gather_half(a, b, 0) for a, b in ((sh_in, t_in), (sh_out, t_out), (sh_gate, t_gate))
    )
    xt_cols, xt_in, xt_out = x_move(zt_cols), x_move(zt_in), x_move(zt_out)
    program = [("send", v) for v in (t_in, t_out, zt_cols, t_gate, t_gain, t_seq)]
    program += [("wait", t_in), ("send", zt_in), ("wait", t_out), ("send", zt_out)]
    program += [("send", t_up), ("wait", t_gate), ("send", zt_gate)]
    program += [("wait", zt_cols), ("send", xt_cols), ("wait", zt_in), ("send", xt_in)]
    program += [("wait", zt_out), ("send", xt_out), ("send", t_down)]
    rest = [t_gain, t_seq, t_up, t_down, zt_gate, xt_cols, xt_in, xt_out]
    program += [("wait", v) for v in rest]
    order = [t_in, t_out, t_gate, t_seq, t_up, t_down, t_gain]
    order += [zt_cols, zt_in, zt_out, zt_gate, xt_cols, xt_in, xt_out]
    (m_in, m_out, m_gate, m_seq, m_up, m_down, m_gain), (
        z_cols, z_in0, z_out0, z_gate0, x_cols, x_in0, x_out0
    ) = (lambda r: (r[:7], r[7:]))(exchange(order, program, 16))

    x_low, cot = by_block(pick(seqs, s), m_seq)
    gains = by_block(norm_gain[0], m_gain)
    in0, cols = Weight("rows", z_in0, x_in0), Weight("conv", z_cols, x_cols)
    out0 = Weight("cols", z_out0, x_out0)
    tables = attention_tables(2 * channels, boundary.shape[2] * 4, qk_gain)

    x_rows = x_low.astype(F32)
    (a0, proj0, value0), (x_gate0, z_up0) = gather_mm(
        x_rows, gains[0][0], [in0, cols], cid=0,
        tasks=[x_move(z_gate0), z_gather_half(sh_up, m_up, 0)],
    )
    gate_w0 = Weight("rows", z_gate0, x_gate0)
    b_gate, c_gate, product, causal = conv_core(proj0, value0, conv_kernel)
    y0 = (c_gate * causal).astype(BF)
    (mid0,), (x_up0, z_down0) = scatter_mm(
        [y0], [out0], x_rows, cid=1, tasks=[x_move(z_up0), z_gather_half(sh_down, m_down, 0)]
    )
    up_w0 = Weight("rows", z_up0, x_up0)
    (m0, gate0, up0, hid0), (x_down0, z_in1, z_out1) = gather_mm(
        mid0, gains[0][1], [gate_w0, up_w0], epilogue="ffn", cid=2,
        tasks=[x_move(z_down0), z_gather_half(sh_in, m_in, 1), z_gather_half(sh_out, m_out, 1)],
    )
    down_w0 = Weight("cols", z_down0, x_down0)
    (z_rows,), (x_in1, x_out1, z_gate1) = scatter_mm(
        [hid0], [down_w0], mid0, cid=3,
        tasks=[x_move(z_in1), x_move(z_out1), z_gather_half(sh_gate, m_gate, 1)],
    )
    z_rows = z_rows.astype(BF).astype(F32)
    in1, out1 = Weight("rows", z_in1, x_in1), Weight("cols", z_out1, x_out1)
    (a1, proj1), (x_gate1, z_up1) = gather_mm(
        z_rows, gains[1][0], [in1], cid=4,
        tasks=[x_move(z_gate1), z_gather_half(sh_up, m_up, 1)],
    )
    gate_w1 = Weight("rows", z_gate1, x_gate1)
    (y1, *rotated), (x_up1, z_down1) = attend(
        proj1, qk_gain, tables, 22, tasks=[x_move(z_up1), z_gather_half(sh_down, m_down, 1)]
    )
    up_w1 = Weight("rows", z_up1, x_up1)
    (mid1,), (x_down1,) = scatter_mm([y1], [out1], z_rows, cid=5, tasks=[x_move(z_down1)])
    down_w1 = Weight("cols", z_down1, x_down1)
    (m1, gate1, up1, hid1), _ = gather_mm(
        mid1, gains[1][1], [gate_w1, up_w1], epilogue="ffn", cid=6
    )
    (y_rows,), _ = scatter_mm([hid1], [down_w1], mid1, cid=7)
    y_rows = y_rows.astype(BF)

    def split_rows(grad):
        rows, width = grad.shape
        return grad.reshape(count, 2, rows // (2 * count), width)

    def sum_rows(grad, other):
        return SumScatter("rows", grad, other)

    def sum_cols(grad, other):
        return SumScatter("cols", grad, other)

    (_, d_gate1, d_up1, g_down1), _ = gather_mm(
        cot, None, [down_w1], [gate1, up1], trans=True, epilogue="ffn_back", cid=8, left=hid1
    )
    g_down1 = halves(g_down1)
    (d_mid1, gain11, g_gate1, g_up1), (r_down1,) = scatter_mm(
        [d_gate1, d_up1], [gate_w1, up_w1], cot, (mid1, gains[1][1]), True, 9, left=m1,
        tasks=[x_half(g_down1)],
    )
    g_gate1, g_up1 = split_rows(g_gate1), split_rows(g_up1)
    (_, d_y1, g_out1), (q_down1, r_gate1) = gather_mm(
        d_mid1, None, [out1], trans=True, cid=10, left=y1,
        tasks=[sum_cols(g_down1, r_down1), x_rows_of(g_gate1)],
    )
    g_out1 = halves(g_out1)
    (d_proj1, head_grad), (q_gate1, r_up1) = attend_back(
        proj1, rotated, d_y1, qk_gain, tables, 23,
        tasks=[sum_rows(g_gate1, r_gate1), x_rows_of(g_up1)],
    )
    (d_z, gain10, g_in1), (q_up1, r_out1, e_down1) = scatter_mm(
        [d_proj1], [in1], d_mid1, (z_rows, gains[1][0]), True, 11, left=a1,
        tasks=[sum_rows(g_up1, r_up1), x_half(g_out1), Finish(q_down1, 1)],
    )
    g_in1 = split_rows(g_in1)
    d_z = d_z.astype(BF)

    (_, d_gate0, d_up0, g_down0), (q_out1, r_in1, e_gate1) = gather_mm(
        d_z, None, [down_w0], [gate0, up0], trans=True, epilogue="ffn_back", cid=12, left=hid0,
        tasks=[sum_cols(g_out1, r_out1), x_rows_of(g_in1), Finish(q_gate1, 1)],
    )
    g_down0 = halves(g_down0)
    (d_mid0, gain01, g_gate0, g_up0), (q_in1, r_down0, e_up1) = scatter_mm(
        [d_gate0, d_up0], [gate_w0, up_w0], d_z, (mid0, gains[0][1]), True, 13, left=m0,
        tasks=[sum_rows(g_in1, r_in1), x_half(g_down0), Finish(q_up1, 1)],
    )
    g_gate0, g_up0 = split_rows(g_gate0), split_rows(g_up0)
    (_, d_y0, g_out0), (q_down0, r_gate0, e_out1) = gather_mm(
        d_mid0, None, [out0], trans=True, cid=14, left=y0,
        tasks=[sum_cols(g_down0, r_down0), x_rows_of(g_gate0), Finish(q_out1, 1)],
    )
    g_out0 = halves(g_out0)
    d_proj0, d_value0, kernel_grad = conv_back(proj0, value0, conv_kernel, d_y0)
    (d_x, gain00, g_in0, g_cols), (q_gate0, r_up0, e_in1) = scatter_mm(
        [d_proj0, d_value0], [in0, cols], d_mid0, (x_rows, gains[0][0]), True, 15, left=a0,
        tasks=[sum_rows(g_gate0, r_gate0), x_rows_of(g_up0), Finish(q_in1, 1)],
    )
    d_x = d_x.astype(BF)
    g_in0 = split_rows(g_in0)
    g_cols = g_cols.reshape(2, count, conv_x.shape[0], channels)

    small = jnp.concatenate(
        [
            gain00,
            gain01,
            gain10,
            gain11,
            lax.dynamic_update_slice_in_dim(
                jnp.zeros((conv_kernel.shape[0], model_width), F32), kernel_grad, t * channels, 1
            ),
            jnp.pad(head_grad.reshape(1, -1), ((0, 0), (0, model_width - head_grad.size))),
        ],
        axis=0,
    )
    s_up = sum_rows(g_up0, r_up0)
    t_in0, t_cols, t_out0 = x_rows_of(g_in0), x_half(g_cols), x_half(g_out0)
    s_in, s_out = sum_rows(g_in0, t_in0), sum_cols(g_out0, t_out0)
    s_cols = SumScatter("slots", g_cols, t_cols)
    f_gate, f_down, f_up = Finish(q_gate0, 0), Finish(q_down0, 0), Finish(s_up, 0)
    f_in, f_out = Finish(s_in, 0), Finish(s_out, 0)
    t_small, t_result = x_move(small), x_move(jnp.where(first, y_rows, d_x))
    program = [("load", v) for v in (s_up, f_gate, f_down)]
    program += [("send", v) for v in (t_in0, t_small, t_cols, t_out0, s_up, t_result)]
    program += [("send", f_down), ("send", f_gate)]
    program += [("wait", t_in0), ("reload", s_in), ("send", s_in)]
    program += [("wait", t_cols), ("reload", s_cols), ("wait", t_out0), ("reload", s_out)]
    program += [("send", s_out), ("send", s_cols)]
    program += [("wait", s_up), ("reload", f_up), ("send", f_up)]
    program += [("wait", s_in), ("reload", f_in), ("send", f_in)]
    program += [("wait", s_out), ("reload", f_out), ("send", f_out)]
    rest = [s_cols, t_small, t_result, f_gate, f_down, f_up, f_in, f_out]
    program += [("wait", v) for v in rest]
    order = [t_in0, t_cols, t_out0, s_up, s_in, s_out, s_cols, f_gate, f_down, f_up, f_in, f_out]
    order += [t_small, t_result]
    *_, q_cols, e_gate0, e_down0, e_up0, e_in0, e_out0, small_x, out_moved = exchange(
        order, program, 17
    )
    small = small + small_x
    t_z = z_gather(small)
    (small_z,) = exchange([t_z], [("send", t_z), ("wait", t_z)], 18)
    small = jnp.sum(small_z, axis=0)
    t_t = t_share(small)
    (small_t,) = exchange([t_t], [("send", t_t), ("wait", t_t)], 19)
    small = jnp.sum(small_t, axis=0)

    def whole(zero, one):
        kept = jnp.where(first, zero, one)
        return kept.reshape(1, -1, kept.shape[-1]).astype(F32)

    result = jnp.where(first, jnp.stack([d_x, out_moved]), jnp.stack([out_moved, y_rows]))
    gains_total = small[:4].reshape(2, 2, model_width)
    gain_out = lax.dynamic_slice_in_dim(gains_total, s, 1, 0)
    kernel_rows = small[4 : 4 + conv_kernel.shape[0]]
    kernel_out = lax.dynamic_slice_in_dim(kernel_rows, t * channels, channels, 1)
    head_total = small[-1, : qk_gain.size].reshape(qk_gain.shape)
    return (
        result[None],
        gain_out,
        whole(e_in0, e_in1),
        whole(e_out0, e_out1),
        whole(e_gate0, e_gate1),
        whole(e_up0, e_up1),
        whole(e_down0, e_down1),
        jnp.sum(q_cols.astype(F32), axis=0),
        kernel_out,
        head_total,
    )


def solution(mesh):
    in_specs = (
        P("section", "dp", "tensor", None),
        P("section", None, None),
        P("section", "dp", "tensor"),
        P("section", "tensor", "dp"),
        P("section", "dp", "tensor"),
        P("section", "dp", "tensor"),
        P("section", "tensor", "dp"),
        P(("section", "dp"), "tensor"),
        P(None, "tensor"),
        P(),
    )
    out_specs = (
        P("section", "dp", "tensor", None),
        P("section", None, None),
        P("section", "dp", "tensor"),
        P("section", "tensor", "dp"),
        P("section", "dp", "tensor"),
        P("section", "dp", "tensor"),
        P("section", "tensor", "dp"),
        P(("section", "dp"), "tensor"),
        P(None, "tensor"),
        P(),
    )
    return jax.shard_map(body, mesh=mesh, in_specs=in_specs, out_specs=out_specs, check_vma=False)
```

```python
import functools

import jax
import jax.numpy as jnp
from jax import lax
from jax.experimental import pallas as pl
from jax.experimental.pallas import tpu as pltpu
from jax.sharding import PartitionSpec as P

HEADS = 16
KV_HEADS = 8

EPS = 1e-05
ROPE_BASE = 1000000.0
MASKED = -1e30

MESH = pl.DeviceIdType.MESH
ANY = pl.BlockSpec(memory_space=pl.ANY)
VM = pl.BlockSpec(memory_space=pltpu.VMEM)
DMA = pltpu.SemaphoreType.DMA
VMEM_BYTES = 62 * 1024 * 1024
BF = jnp.bfloat16
F32 = jnp.float32


def contract(left_op, right_op, left_dim, right_dim):
    return lax.dot_general(
        left_op, right_op, (((left_dim,), (right_dim,)), ((), ())), preferred_element_type=F32
    )


def norm_rows(values, gain):
    return values * lax.rsqrt(jnp.mean(values * values, axis=-1, keepdims=True) + EPS) * gain


def norm_back(values, gain, grad_in):
    row_scale = lax.rsqrt(jnp.mean(values * values, axis=-1, keepdims=True) + EPS)
    normed = values * row_scale
    feature_count = values.shape[-1]
    gain_grad = jnp.sum((grad_in * normed).reshape(-1, feature_count), axis=0)
    scaled = grad_in * gain
    value_grad = row_scale * (scaled - normed * jnp.mean(scaled * normed, axis=-1, keepdims=True))
    return (value_grad, gain_grad)


def rotation(length, head_size):
    half_size = head_size // 2
    frequency = ROPE_BASE ** (-(jnp.arange(half_size, dtype=jnp.float32) * 2.0 / head_size))
    angles = jnp.arange(length, dtype=jnp.float32)[:, None] * frequency[None, :]
    cosine_table = jnp.concatenate([jnp.cos(angles), jnp.cos(angles)], axis=1)
    sine_table = jnp.concatenate([jnp.sin(angles), jnp.sin(angles)], axis=1)
    return (cosine_table, sine_table)


def delayed(values, delay_by):
    if delay_by == 0:
        return values
    return jnp.concatenate(
        [jnp.zeros((delay_by, values.shape[1]), values.dtype), values[:-delay_by]], axis=0
    )


def advanced(values, delay_by):
    if delay_by == 0:
        return values
    return jnp.concatenate(
        [values[delay_by:], jnp.zeros((delay_by, values.shape[1]), values.dtype)], axis=0
    )


def places():
    me = lax.axis_index("tensor")
    sib = me + 1 - 2 * (me % 2)
    cross = (me + 2) % 4
    diag = (sib + 2) % 4
    return me, sib, cross, diag


def greet(peers):
    barrier = pltpu.get_barrier_semaphore()
    for peer in peers:
        pl.semaphore_signal(barrier, inc=1, device_id=peer, device_id_type=MESH)
    pl.semaphore_wait(barrier, len(peers))


def remote(src, dst, send_sem, recv_sem, peer):
    return pltpu.make_async_remote_copy(
        src_ref=src, dst_ref=dst, send_sem=send_sem, recv_sem=recv_sem,
        device_id=peer, device_id_type=MESH,
    )


class Task:
    summed = False

    def __init__(self, inputs, out, axis, moves, count, final=None, room=()):
        self.inputs, self.out, self.axis, self.count = inputs, out, axis, count
        self.make, self.final, self.room = moves, final, list(room)
        self.scratch = [DMA((count,)), DMA((count,)), DMA((2 + dp_size(),))] + self.room

    def bind(self, ins, out, scratch):
        self.ins, self.out_ref = ins, out
        self.send_sem, self.recv_sem, self.local_sem, *self.bufs = scratch

    def at(self):
        return tuple(lax.axis_index(a) for a in ("section", "dp", "tensor"))

    def local(self, src, dst, i):
        return pltpu.make_async_copy(src, dst, self.local_sem.at[i])

    def load(self):
        pass

    def pairs(self):
        remotes, locals_ = self.make(self, *self.at())
        far = [
            [(cond, remote(src, dst, self.send_sem.at[i], self.recv_sem.at[i], peer))
             for cond, src in sources]
            for i, (sources, dst, peer) in enumerate(remotes)
        ]
        near = [
            [(cond, self.local(src, dst, i)) for cond, src in sources]
            for i, (sources, dst) in enumerate(locals_)
        ]
        return far, near

    def send(self):
        far, near = self.pairs()
        s = lax.axis_index("section")
        for variants in far:
            for cond, move in variants:
                if self.final is not None:
                    cond = s == 1 - self.final
                if cond is None:
                    move.start()
                else:
                    pl.when(cond)(move.start)
        for variants in near:
            for cond, move in variants:
                if cond is None:
                    move.start()
                else:
                    pl.when(cond)(move.start)

    def wait(self):
        far, near = self.pairs()
        s = lax.axis_index("section")
        for variants in far:
            move = variants[0][1]
            if self.final is None:
                move.wait_recv()
                move.wait_send()
            else:
                pl.when(s == 1 - self.final)(move.wait_send)
                pl.when(s == self.final)(move.wait_recv)
        for variants in near:
            variants[0][1].wait()


def dp_size():
    return lax.axis_size("dp")


def like(shape, value):
    return jax.ShapeDtypeStruct(shape, value.dtype)


def z_gather(piece):
    count = dp_size()

    def moves(task, s, d, t):
        far = [([(None, task.ins[0])], task.out_ref.at[d], {"dp": (d + k) % count}) for k in range(1, count)]
        return far, [([(None, task.ins[0])], task.out_ref.at[d])]

    return Task([piece], like((count,) + piece.shape, piece), "dp", moves, count - 1)


def z_gather_half(shard, moved, block):
    count = dp_size()

    def moves(task, s, d, t):
        sources = [(s == block, task.ins[0].at[block]), (s == 1 - block, task.ins[1])]
        far = [(sources, task.out_ref.at[d], {"dp": (d + k) % count}) for k in range(1, count)]
        return far, [(sources, task.out_ref.at[d])]

    return Task([shard, moved], like((count,) + shard.shape[1:], shard), "dp", moves, count - 1)


def x_move(value, index=None):
    def moves(task, s, d, t):
        src = task.ins[0] if index is None else task.ins[0].at[1 - s]
        return [([(None, src)], task.out_ref, {"section": 1 - s})], []

    out = value.out if isinstance(value, Task) else value
    shape = out.shape if index is None else out.shape[1:]
    return Task([value], jax.ShapeDtypeStruct(shape, out.dtype), "section", moves, 1)


def x_part(value, lo, hi):
    def moves(task, s, d, t):
        part = pl.ds(lo, hi - lo)
        return [([(None, task.ins[0].at[part])], task.out_ref, {"section": 1 - s})], []

    return Task([value], like((hi - lo,) + value.shape[1:], value), "section", moves, 1)


def x_half(shard):
    return x_move(shard, 0)


def x_rows_of(grads):
    count = dp_size()

    def moves(task, s, d, t):
        return [
            ([(None, task.ins[0].at[k, 1 - s])], task.out_ref.at[k], {"section": 1 - s})
            for k in range(count)
        ], []

    return Task([grads], like((count,) + grads.shape[2:], grads), "section", moves, count)


class SumScatter(Task):
    summed = True

    def __init__(self, kind, grads, received):
        count = dp_size()
        if kind == "cols":
            rows, width = grads.shape[1:]
            cols, held = width // count, (rows, width)
        else:
            rows, cols = grads.shape[2:]
            held = (count, rows, cols)
        self.kind, self.cols, self.n = kind, cols, count

        def moves(task, s, d, t):
            total = task.bufs[2]
            far = []
            for k in range(1, count):
                other = (d + k) % count
                far.append(([(None, total.at[other])], task.out_ref.at[d], {"dp": other}))
            return far, [([(None, total.at[d])], task.out_ref.at[d])]

        room = [pltpu.VMEM(held, BF)] * 2 + [pltpu.VMEM((count, rows, cols), BF)]
        super().__init__(
            [grads, received], like((count, rows, cols), grads), "dp", moves, count - 1, room=room
        )

    def loads(self):
        s = lax.axis_index("section")
        kept, got = self.bufs[:2]
        if self.kind == "rows":
            moves = [self.local(self.ins[0].at[k, s], kept.at[k], 2 + k) for k in range(self.n)]
        else:
            moves = [self.local(self.ins[0].at[s], kept, 2)]
        return moves + [self.local(self.ins[1], got, 1)]

    def load(self):
        for move in self.loads():
            move.start()

    def send(self):
        for move in self.loads():
            move.wait()
        kept, got, total = self.bufs
        for k in range(self.n):
            if self.kind == "cols":
                part = (slice(None), slice(k * self.cols, (k + 1) * self.cols))
            else:
                part = k
            total[k] = (kept[part].astype(F32) + got[part].astype(F32)).astype(BF)
        super().send()


class Finish(Task):
    summed = True

    def __init__(self, pieces, block):
        out = pieces.out if isinstance(pieces, Task) else pieces
        count, rows, cols = out.shape
        self.n = count

        def moves(task, s, d, t):
            total = task.bufs[1]
            far = [([(None, total)], task.out_ref.at[s], {"section": 1 - s})]
            return far, [([(None, total)], task.out_ref.at[s])]

        room = [pltpu.VMEM((count, rows, cols), BF), pltpu.VMEM((rows, cols), BF)]
        super().__init__(
            [pieces], like((2, rows, cols), out), "section", moves, 1, final=block, room=room
        )

    def load(self):
        self.local(self.ins[0], self.bufs[0], 1).start()

    def send(self):
        self.local(self.ins[0], self.bufs[0], 1).wait()
        held, total = self.bufs
        acc = held[0].astype(F32)
        for k in range(1, self.n):
            acc = acc + held[k].astype(F32)
        total[...] = acc.astype(BF)
        super().send()


class SumShare(Task):
    summed = True

    def __init__(self, terms, axis, slotted=False):
        first = terms[0].out if isinstance(terms[0], Task) else terms[0]
        shape = first.shape[1:] if slotted else first.shape
        count = dp_size() if axis == "dp" else 4
        self.slotted, self.n = slotted, len(terms)

        def moves(task, s, d, t):
            total, me = task.bufs[-1], d if axis == "dp" else t
            far = [
                ([(None, total)], task.out_ref.at[me], {axis: (me + k) % count})
                for k in range(1, count)
            ]
            return far, [([(None, total)], task.out_ref.at[me])]

        room = [pltpu.VMEM(first.shape, F32) for _ in terms] + [pltpu.VMEM(shape, F32)]
        super().__init__(
            terms, jax.ShapeDtypeStruct((count,) + shape, F32), axis, moves, count - 1, room=room
        )

    def send(self):
        loads = [self.local(self.ins[i], self.bufs[i], 1 + i) for i in range(self.n)]
        for load in loads:
            load.start()
        for load in loads:
            load.wait()
        if self.slotted:
            parts = [self.bufs[0][k] for k in range(self.bufs[0].shape[0])]
        else:
            parts = [buf[...] for buf in self.bufs[: self.n]]
        acc = parts[0]
        for part in parts[1:]:
            acc = acc + part
        self.bufs[-1][...] = acc
        super().send()


class Background:
    def __init__(self, tasks):
        self.tasks = list(tasks)
        self.inputs = [v for task in self.tasks for v in task.inputs if not isinstance(v, Task)]
        self.outs = [task.out for task in self.tasks]
        self.scratch = [room for task in self.tasks for room in task.scratch]

    def bind(self, it_in, it_out):
        self.in_refs = [next(it_in) for _ in self.inputs]
        self.out_refs = [next(it_out) for _ in self.outs]

    def hold(self, scratch):
        scratch, ins = iter(scratch), iter(self.in_refs)
        for task, out in zip(self.tasks, self.out_refs):
            task.out_ref = out
        for task, out in zip(self.tasks, self.out_refs):
            refs = [v.out_ref if isinstance(v, Task) else next(ins) for v in task.inputs]
            task.bind(refs, out, [next(scratch) for _ in task.scratch])

    def peers(self, tensor):
        count = dp_size()
        s, d, t = (lax.axis_index(a) for a in ("section", "dp", "tensor"))
        axes = {task.axis for task in self.tasks}
        found = []
        if "section" in axes:
            found.append({"section": 1 - s})
        if "dp" in axes:
            found += [{"dp": (d + k) % count} for k in range(1, count)]
        if "tensor" in axes:
            found += [{"tensor": (t + k) % 4} for k in range(1, 4)]
        else:
            found += tensor
        return found

    def load(self):
        for task in self.tasks:
            task.load()

    def start(self, summed):
        for task in self.tasks:
            if task.summed == summed:
                task.send()

    def finish(self):
        for task in self.tasks:
            task.wait()

    def open(self, scratch):
        self.hold(scratch)
        if self.tasks:
            self.load()
            greet(self.peers([]))
            self.start(False)
            self.start(True)

    def close(self):
        self.finish()

    def params(self, cid):
        if not self.tasks:
            return pltpu.CompilerParams(vmem_limit_bytes=VMEM_BYTES)
        return pltpu.CompilerParams(
            collective_id=cid, has_side_effects=True, vmem_limit_bytes=VMEM_BYTES
        )


def exchange_kernel(bg, program, *refs):
    ins = iter(refs[: len(bg.inputs)])
    outs = iter(refs[len(bg.inputs) : len(bg.inputs) + len(bg.outs)])
    bg.bind(ins, outs)
    bg.hold(refs[len(bg.inputs) + len(bg.outs) :])
    for act, task in program:
        if act == "load":
            task.load()
    greet(bg.peers([]))
    for act, task in program:
        if act == "reload":
            task.load()
        elif act == "send":
            task.send()
        elif act == "wait":
            task.wait()


def exchange(tasks, program, cid):
    bg = Background(tasks)
    return pl.pallas_call(
        functools.partial(exchange_kernel, bg, program),
        out_shape=bg.outs,
        in_specs=[ANY] * len(bg.inputs),
        out_specs=[ANY] * len(bg.outs),
        scratch_shapes=bg.scratch,
        compiler_params=bg.params(cid),
        name=f"exchange{cid}",
    )(*bg.inputs)


class Weight:
    def __init__(self, kind, near, *far):
        count, rows, cols = near.shape
        self.rows, self.cols = rows, cols
        if kind == "cols":
            self.shape = (2 * rows, count * cols)
        else:
            self.shape = (2 * count * rows, cols)
        self.size = self.shape[0] * self.shape[1]
        if kind == "cols" and cols % 128:
            s = lax.axis_index("section")
            far = jnp.concatenate(far, axis=0)
            both = jnp.stack([jnp.where(s == 0, near, far), jnp.where(s == 0, far, near)])
            self.parts = [both.transpose(0, 2, 1, 3).reshape(self.shape)]
            self.kind, self.loads = "whole", 1
        else:
            self.kind, self.parts, self.loads = kind, [near, *far], 2 * count
            self.far_at = [(i + 1, k) for i, f in enumerate(far) for k in range(f.shape[0])]

    def copies(self, refs, dst, sem):
        if self.kind == "whole":
            return [pltpu.make_async_copy(refs[0], dst, sem.at[0])]
        s = lax.axis_index("section")
        rows, cols, count = self.rows, self.cols, len(self.far_at)

        def place(sec, own):
            if self.kind == "cols":
                top = pl.multiple_of(sec * rows, rows)
                return dst.at[pl.ds(top, rows), pl.ds(own * cols, cols)]
            slot = own * 2 + sec if self.kind == "rows" else sec * count + own
            return dst.at[pl.ds(pl.multiple_of(slot * rows, rows), rows)]

        moves = []
        for k, (i, far) in enumerate(self.far_at):
            near = refs[0].at[k]
            moves.append(pltpu.make_async_copy(near, place(s, k), sem.at[2 * k]))
            moves.append(
                pltpu.make_async_copy(refs[i].at[far], place(1 - s, k), sem.at[2 * k + 1])
            )
        return moves


def grad_chunk(cols):
    return 384 if cols % 384 == 0 else 256


def grad_copies(dst_v, dst_hbm, sem):
    chunk = grad_chunk(dst_v.shape[0])
    return [
        pltpu.make_async_copy(
            dst_v.at[pl.ds(i * chunk, chunk)], dst_hbm.at[pl.ds(i * chunk, chunk)], sem.at[i]
        )
        for i in range(dst_v.shape[0] // chunk)
    ]


def grad_products(left, right, dst_v, dst_hbm, sem):
    cols = left.shape[1]
    chunk = grad_chunk(cols)

    def step(i, carry):
        part = pl.ds(pl.multiple_of(i * chunk, chunk), chunk)
        dst_v[part, :] = contract(left[:, part], right[...], 0, 0).astype(BF)
        pltpu.make_async_copy(dst_v.at[part], dst_hbm.at[part], sem.at[i]).start()
        return carry

    lax.fori_loop(0, cols // chunk, step, 0)


def silu_parts(gate):
    sig = 1.0 / (1.0 + jnp.exp(-gate))
    return sig, gate * sig


def gather_kernel(cfg, weights, bg, *refs):
    norm, n_w, n_x, trans, epilogue, n_left, grads = cfg
    it = iter(refs)
    x_ref = next(it)
    gain_ref = next(it) if norm else None
    w_hbm = [[next(it) for _ in w.parts] for w in weights]
    e_hbm = [next(it) for _ in range(n_x)]
    left_hbm = [next(it) for _ in range(n_left)]
    bg_in = [next(it) for _ in bg.inputs]
    a_hbm = next(it)
    n_out = {"plain": n_w, "ffn": 3, "ffn_back": 2}[epilogue]
    o_hbm = [next(it) for _ in range(n_out)]
    grad_hbm = [next(it) for _ in grads]
    bg.bind(iter(bg_in), it)
    full = next(it)
    w_v = [next(it) for _ in range(n_w)]
    e_v = [next(it) for _ in range(n_x)]
    o_v = [next(it) for _ in range(n_out)]
    left_v = [next(it) for _ in range(n_left)]
    grad_v = [next(it) for _ in grads]
    grad_sem = [next(it) for _ in grads]
    left_sem = next(it)
    left_loads = [
        pltpu.make_async_copy(src, dst, left_sem.at[i])
        for i, (src, dst) in enumerate(zip(left_hbm, left_v))
    ]
    w_sem, in_sem, out_sem, a_sem, xs, xr, ss, sr, ls, lr, *bg_room = it
    bg.hold(bg_room)

    me, sib, cross, diag = places()
    rows = x_ref.shape[0]
    half = rows // 2
    loads = [
        pltpu.make_async_copy(src, dst, in_sem.at[i])
        for i, (src, dst) in enumerate(zip(e_hbm, e_v))
    ]
    for i, w in enumerate(weights):
        loads += w.copies(w_hbm[i], w_v[i], w_sem.at[i])
    for load in loads:
        load.start()
    for load in left_loads:
        load.start()
    bg.load()
    greet(bg.peers([{"tensor": sib}, {"tensor": cross}]))
    bg.start(False)

    def span(owner, sub):
        return pl.ds(pl.multiple_of(owner * rows + sub * half, half), half)

    def to_cross(i):
        return remote(full.at[span(me, i)], full.at[span(me, i)], xs.at[i], xr.at[i], {"tensor": cross})

    def to_sib(i):
        return remote(full.at[span(me, i)], full.at[span(me, i)], ss.at[i], sr.at[i], {"tensor": sib})

    def relay(i):
        return remote(full.at[span(cross, i)], full.at[span(cross, i)], ls.at[i], lr.at[i], {"tensor": sib})

    for i in range(2):
        part = x_ref[pl.ds(i * half, half), :]
        if norm:
            part = norm_rows(part, gain_ref[...])
        full[span(me, i), :] = part.astype(BF)
        to_cross(i).start()
        to_sib(i).start()
    bg.start(True)
    for load in loads:
        load.wait()

    def step(p, carry):
        far, sub = p // 2, p % 2
        near = (1 - sub) * me + sub * sib
        first = (1 - far) * near * rows + far * (cross * rows + sub * half)
        second = (1 - far) * (near * rows + half) + far * (diag * rows + sub * half)
        pair = [pl.ds(pl.multiple_of(first, half), half), pl.ds(pl.multiple_of(second, half), half)]

        @pl.when(p == 1)
        def _():
            to_sib(0).wait_recv()
            to_sib(1).wait_recv()

        for i in range(2):

            @pl.when(p == 2 + i)
            def _():
                to_cross(i).wait_recv()
                relay(i).start()
                relay(i).wait_recv()

        a = jnp.concatenate([full[pair[0], :], full[pair[1], :]], axis=0)
        prods = [contract(a, w[...], 1, 1 if trans else 0) for w in w_v]
        if epilogue == "plain":
            values = prods
        elif epilogue == "ffn":
            sig, silu = silu_parts(prods[0])
            values = [prods[0], prods[1], silu * prods[1]]
        else:
            gate = jnp.concatenate([e_v[0][q, :] for q in pair], axis=0).astype(F32)
            up = jnp.concatenate([e_v[1][q, :] for q in pair], axis=0).astype(F32)
            sig, silu = silu_parts(gate)
            values = [prods[0] * up * sig * (1.0 + gate * (1.0 - sig)), prods[0] * silu]
        for j, value in enumerate(values):
            value = value.astype(o_v[j].dtype)
            for k in range(2):
                o_v[j][pair[k], :] = value[k * half : (k + 1) * half]
                pltpu.make_async_copy(
                    o_v[j].at[pair[k]], o_hbm[j].at[pair[k]], out_sem.at[p, k, j]
                ).start()
        for k in range(2):
            pltpu.make_async_copy(full.at[pair[k]], a_hbm.at[pair[k]], a_sem.at[p, k]).start()
        return carry

    lax.fori_loop(0, 4, step, 0)
    for load in left_loads:
        load.wait()
    for j, (i, right) in enumerate(grads):
        right_v = full if right is None else o_v[right]
        grad_products(left_v[i], right_v, grad_v[j], grad_hbm[j], grad_sem[j])
    for j in range(len(grads)):
        for copy in grad_copies(grad_v[j], grad_hbm[j], grad_sem[j]):
            copy.wait()
    for i in range(2):
        to_cross(i).wait_send()
        to_sib(i).wait_send()
        relay(i).wait_send()
    for p in range(4):
        for k in range(2):
            for j in range(n_out):
                pltpu.make_async_copy(
                    o_v[j].at[pl.ds(0, half)], o_hbm[j].at[pl.ds(0, half)], out_sem.at[p, k, j]
                ).wait()
            pltpu.make_async_copy(
                full.at[pl.ds(0, half)], a_hbm.at[pl.ds(0, half)], a_sem.at[p, k]
            ).wait()
    bg.finish()


def gather_mm(x_rows, gain, weights, extras=(), trans=False, epilogue="plain", cid=0, tasks=(), lefts=(), grads=()):
    rows, width = x_rows.shape
    length = rows * 4
    cols = [w.shape[0] if trans else w.shape[1] for w in weights]
    if epilogue == "plain":
        outs = [(c, F32) for c in cols]
    else:
        outs = [(cols[0], BF)] * (3 if epilogue == "ffn" else 2)
    norm = gain is not None
    cfg = (norm, len(weights), len(extras), trans, epilogue, len(lefts), tuple(grads))
    bg = Background(tasks)
    parts = [part for w in weights for part in w.parts]
    operands = [x_rows] + ([gain.reshape(1, width)] if norm else []) + parts + list(extras)
    n_out = 1 + len(outs)
    operands += lefts
    grad_out = [
        jax.ShapeDtypeStruct((lefts[i].shape[1], width if j is None else outs[j][0]), BF)
        for i, j in grads
    ]
    grad_room = [pltpu.VMEM(v.shape, BF) for v in list(lefts) + grad_out]
    grad_room += [DMA((g.shape[0] // grad_chunk(g.shape[0]),)) for g in grad_out]
    grad_room.append(DMA((max(len(lefts), 1),)))
    n_out += len(grad_out)
    flops = sum(2 * length * width * c for c in cols)
    moved = sum(w.size * 2 for w in weights) + sum(length * c * 2 for c, _ in outs) + length * width * 4
    result = pl.pallas_call(
        functools.partial(gather_kernel, cfg, weights, bg),
        out_shape=[jax.ShapeDtypeStruct((length, width), BF)]
        + [jax.ShapeDtypeStruct((length, c), t) for c, t in outs]
        + grad_out
        + bg.outs,
        in_specs=[VM] * (2 if norm else 1)
        + [ANY] * (len(operands) - (2 if norm else 1) + len(bg.inputs)),
        out_specs=[ANY] * (n_out + len(bg.outs)),
        scratch_shapes=[pltpu.VMEM((length, width), BF)]
        + [pltpu.VMEM(w.shape, BF) for w in weights]
        + [pltpu.VMEM(e.shape, e.dtype) for e in extras]
        + [pltpu.VMEM((length, c), t) for c, t in outs]
        + grad_room
        + [DMA((len(weights), max(w.loads for w in weights)))]
        + [DMA((max(len(extras), 1),)), DMA((4, 2, len(outs))), DMA((4, 2))]
        + [DMA((2,))] * 6
        + bg.scratch,
        compiler_params=pltpu.CompilerParams(
            collective_id=cid, has_side_effects=True, vmem_limit_bytes=VMEM_BYTES
        ),
        cost_estimate=pl.CostEstimate(flops=flops, bytes_accessed=moved * 4, transcendentals=0),
        name=f"gather{cid}",
    )(*operands, *bg.inputs)
    return result[:n_out], result[n_out:]


def scatter_kernel(cfg, weights, bg, *refs):
    n_y, trans, epilogue, with_grad = cfg
    it = iter(refs)
    y_hbm = [next(it) for _ in range(n_y)]
    w_hbm = [[next(it) for _ in w.parts] for w in weights]
    resid_ref = next(it)
    if epilogue == "back":
        value_ref, gain_ref = next(it), next(it)
    left_hbm = next(it) if with_grad else None
    bg_in = [next(it) for _ in bg.inputs]
    out_ref = next(it)
    if epilogue == "back":
        gain_out = next(it)
    grad_hbm = [next(it) for _ in range(n_y)] if with_grad else []
    bg.bind(iter(bg_in), it)
    y_v = [next(it) for _ in range(n_y)]
    w_v = [next(it) for _ in range(n_y)]
    keep, own, to_s, from_s, to_c, from_c, to_o, from_o = (next(it) for _ in range(8))
    if with_grad:
        left, left_sem, grad_sem = (next(it) for _ in range(3))
        grad_v = [next(it) for _ in range(n_y)]
        left_load = pltpu.make_async_copy(left_hbm, left, left_sem)
    w_sem, in_sem, ds, dr, cs, cr, os_, or_, *bg_room = it
    bg.hold(bg_room)

    me, sib, cross, diag = places()
    rows = resid_ref.shape[0]
    half = rows // 2
    loads = [
        pltpu.make_async_copy(src, dst, in_sem.at[i])
        for i, (src, dst) in enumerate(zip(y_hbm, y_v))
    ]
    for i, w in enumerate(weights):
        loads += w.copies(w_hbm[i], w_v[i], w_sem.at[i])
    for load in loads:
        load.start()
    if with_grad:
        left_load.start()
    bg.load()
    greet(bg.peers([{"tensor": sib}, {"tensor": cross}]))
    bg.start(False)
    for load in loads:
        load.wait()

    def send_diag(i):
        return remote(to_s.at[i], from_s.at[i], ds.at[i], dr.at[i], {"tensor": sib})

    def send_cross(i):
        return remote(to_c.at[i], from_c.at[i], cs.at[i], cr.at[i], {"tensor": cross})

    send_near = remote(to_o, from_o, os_, or_, {"tensor": sib})

    def pass_on(i):
        send_diag(i).wait_recv()
        to_c[i] = (keep[i] + from_s[i].astype(F32)).astype(BF)
        send_cross(i).start()

    bg.start(True)

    def step(p, carry):
        near, sub = p // 2, p % 2
        base = near * ((1 - sub) * sib + sub * me) * rows
        first = base + (1 - near) * (cross * rows + sub * half)
        second = base + near * half + (1 - near) * (diag * rows + sub * half)
        pair = [pl.ds(pl.multiple_of(first, half), half), pl.ds(pl.multiple_of(second, half), half)]
        total = None
        for y, w in zip(y_v, w_v):
            a = jnp.concatenate([y[pair[0], :], y[pair[1], :]], axis=0)
            prod = contract(a, w[...], 1, 1 if trans else 0)
            total = prod if total is None else total + prod

        for i in range(2):

            @pl.when(p == i)
            def _():
                keep[i] = total[:half]
                to_s[i] = total[half:].astype(BF)
                send_diag(i).start()

        @pl.when(p == 1)
        def _():
            pass_on(0)

        @pl.when(p == 2)
        def _():
            to_o[...] = total.astype(BF)
            send_near.start()
            pass_on(1)

        @pl.when(p == 3)
        def _():
            own[...] = total

        return carry

    lax.fori_loop(0, 4, step, 0)
    if with_grad:
        left_load.wait()
        for j in range(n_y):
            grad_products(left, y_v[j], grad_v[j], grad_hbm[j], grad_sem.at[j])
    send_near.wait_recv()
    gain_sum = None
    for i in range(2):
        part = pl.ds(i * half, half)
        send_cross(i).wait_recv()
        total = own[part, :] + from_o[part, :].astype(F32) + from_c[i].astype(F32)
        resid = resid_ref[part, :].astype(F32)
        if epilogue == "back":
            value_grad, gain_grad = norm_back(value_ref[part, :], gain_ref[...], total)
            out_ref[part, :] = resid + value_grad
            gain_sum = gain_grad if gain_sum is None else gain_sum + gain_grad
        else:
            out_ref[part, :] = resid + total
    if epilogue == "back":
        gain_out[...] = gain_sum.reshape(gain_out.shape)
    send_near.wait_send()
    for i in range(2):
        send_diag(i).wait_send()
        send_cross(i).wait_send()
    for j in range(n_y if with_grad else 0):
        for copy in grad_copies(grad_v[j], grad_hbm[j], grad_sem.at[j]):
            copy.wait()
    bg.finish()


def scatter_mm(operands, weights, resid, back=None, trans=False, cid=0, tasks=(), left=None):
    rows, width = resid.shape
    half = rows // 2
    epilogue = "plain" if back is None else "back"
    extra = [] if back is None else [back[0], back[1].reshape(1, width)]
    out_shape = [jax.ShapeDtypeStruct((rows, width), F32)]
    if back is not None:
        out_shape.append(jax.ShapeDtypeStruct((1, width), F32))
    n_out = len(out_shape)
    grad_out, grad_room, operand_left = [], [], []
    if left is not None:
        operand_left = [left]
        chunks = left.shape[1] // grad_chunk(left.shape[1])
        grad_out = [jax.ShapeDtypeStruct((left.shape[1], y.shape[1]), BF) for y in operands]
        grad_room = [pltpu.VMEM(left.shape, BF), DMA, DMA((len(operands), chunks))]
        grad_room += [pltpu.VMEM(g.shape, BF) for g in grad_out]
    bg = Background(tasks)
    parts = [part for w in weights for part in w.parts]
    flops = sum(2 * y.size * width for y in operands)
    moved = sum(2 * (y.size + w.size) for y, w in zip(operands, weights)) + rows * width * 12
    result = pl.pallas_call(
        functools.partial(scatter_kernel, (len(operands), trans, epilogue, left is not None), weights, bg),
        out_shape=out_shape + grad_out + bg.outs,
        in_specs=[ANY] * (len(operands) + len(parts))
        + [VM] * (1 + len(extra))
        + [ANY] * (len(operand_left) + len(bg.inputs)),
        out_specs=[VM] * n_out + [ANY] * (len(grad_out) + len(bg.outs)),
        scratch_shapes=[pltpu.VMEM(y.shape, BF) for y in operands]
        + [pltpu.VMEM(w.shape, BF) for w in weights]
        + [pltpu.VMEM((2, half, width), F32), pltpu.VMEM((rows, width), F32)]
        + [pltpu.VMEM((2, half, width), BF)] * 4
        + [pltpu.VMEM((rows, width), BF)] * 2
        + grad_room
        + [DMA((len(weights), max(w.loads for w in weights))), DMA((len(operands),))]
        + [DMA((2,))] * 4
        + [DMA] * 2
        + bg.scratch,
        compiler_params=pltpu.CompilerParams(
            collective_id=cid, has_side_effects=True, vmem_limit_bytes=VMEM_BYTES
        ),
        cost_estimate=pl.CostEstimate(flops=flops, bytes_accessed=moved * 4, transcendentals=0),
        name=f"scatter{cid}",
    )(*operands, *parts, resid, *extra, *operand_left, *bg.inputs)
    n_out += len(grad_out)
    return result[:n_out], result[n_out:]


def conv_core(projected, x_value, kernel):
    channels = x_value.shape[1]
    b_gate = projected[:, :channels]
    c_gate = projected[:, channels:]
    product = b_gate * x_value
    tap_count = kernel.shape[0]
    causal = jnp.zeros_like(product)
    for offset in range(tap_count):
        causal = causal + kernel[offset] * delayed(product, tap_count - 1 - offset)
    return (b_gate, c_gate, product, causal)


def conv_back(projected, x_value, kernel, grad_y):
    b_gate, c_gate, product, causal = conv_core(projected, x_value, kernel)
    grad_c = grad_y * causal
    grad_causal = grad_y * c_gate
    tap_count = kernel.shape[0]
    kernel_rows = []
    grad_product = jnp.zeros_like(product)
    for offset in range(tap_count):
        delay_by = tap_count - 1 - offset
        kernel_rows.append(jnp.sum(grad_causal * delayed(product, delay_by), axis=0))
        grad_product = grad_product + kernel[offset] * advanced(grad_causal, delay_by)
    grad_proj = jnp.concatenate([grad_product * x_value, grad_c], axis=1).astype(BF)
    grad_value = (grad_product * b_gate).astype(BF)
    return (grad_proj, grad_value, jnp.stack(kernel_rows))


def head_mean(values, head_size):
    width = values.shape[1]
    row = lax.broadcasted_iota(jnp.int32, (width, width), 0) // head_size
    col = lax.broadcasted_iota(jnp.int32, (width, width), 1) // head_size
    group = jnp.where(row == col, 1.0 / head_size, 0.0).astype(F32)
    return lax.dot_general(
        values, group, (((1,), (0,)), ((), ())),
        precision=lax.Precision.HIGHEST, preferred_element_type=F32,
    )


def turn(values, head_size, back):
    width, half = values.shape[1], head_size // 2
    lane = lax.broadcasted_iota(jnp.int32, values.shape, 1) % head_size
    upper = pltpu.roll(values, width - half, 1)
    lower = pltpu.roll(values, half, 1)
    return jnp.where(lane < half, upper, -lower) if back else jnp.where(lane < half, -upper, lower)


def head_norm(values, gain, head_size):
    return values * lax.rsqrt(head_mean(values * values, head_size) + EPS) * gain


def head_norm_back(values, gain, grad_in, head_size):
    row_scale = lax.rsqrt(head_mean(values * values, head_size) + EPS)
    normed = values * row_scale
    gain_grad = jnp.sum(grad_in * normed, axis=0, keepdims=True)
    scaled = grad_in * gain
    return row_scale * (scaled - normed * head_mean(scaled * normed, head_size)), gain_grad


ROW_BLOCK = 256


def block_weights(q_rows, k_rows, first_row):
    rows, length = q_rows.shape[0], k_rows.shape[0]
    scores = contract(q_rows, k_rows, 1, 1) * (q_rows.shape[1] ** -0.5)
    query = first_row + lax.broadcasted_iota(jnp.int32, (rows, length), 0)
    key = lax.broadcasted_iota(jnp.int32, (rows, length), 1)
    scores = jnp.where(key <= query, scores, MASKED)
    exps = jnp.exp(scores - jnp.max(scores, axis=1, keepdims=True))
    return exps * (1.0 / jnp.sum(exps, axis=1, keepdims=True))


def attend_kernel(dims, bg, *refs):
    length, heads, kv_heads, size = dims
    it = iter(refs)
    proj, gain, cos, sin = (next(it) for _ in range(4))
    bg_in = [next(it) for _ in bg.inputs]
    y_out, q_out, k_out = (next(it) for _ in range(3))
    bg.bind(iter(bg_in), it)
    q_h, k_h, v_h, y_h, *room = it
    bg.open(room)
    q_cols, k_cols = heads * size, kv_heads * size

    def prepare(p, carry):
        rows = pl.ds(pl.multiple_of(p * ROW_BLOCK, ROW_BLOCK), ROW_BLOCK)
        c, n = cos[rows, :], sin[rows, :]
        q = head_norm(proj[rows, :q_cols], gain[0:1, :], size)
        q = (q * c + turn(q, size, False) * n).astype(BF)
        k = head_norm(proj[rows, q_cols : q_cols + k_cols], gain[1:2, :k_cols], size)
        k = (k * c[:, :k_cols] + turn(k, size, False) * n[:, :k_cols]).astype(BF)
        q_out[rows, :] = q
        k_out[rows, :] = k
        for h in range(heads):
            q_h[h, rows, :] = q[:, h * size : (h + 1) * size]
        v = proj[rows, q_cols + k_cols :].astype(BF)
        for g in range(kv_heads):
            k_h[g, rows, :] = k[:, g * size : (g + 1) * size]
            v_h[g, rows, :] = v[:, g * size : (g + 1) * size]
        return carry

    lax.fori_loop(0, length // ROW_BLOCK, prepare, 0)

    def head(h, carry):
        g = h // (heads // kv_heads)
        for i in range(length // ROW_BLOCK):
            rows, seen = pl.ds(i * ROW_BLOCK, ROW_BLOCK), pl.ds(0, (i + 1) * ROW_BLOCK)
            weights = block_weights(q_h[h, rows, :], k_h[g, seen, :], i * ROW_BLOCK)
            y_h[h, rows, :] = contract(weights.astype(BF), v_h[g, seen, :], 1, 0).astype(BF)
        return carry

    lax.fori_loop(0, heads, head, 0)
    y_out[...] = jnp.concatenate([y_h[h] for h in range(heads)], axis=1)
    bg.close()


def attend_back_kernel(dims, bg, *refs):
    length, heads, kv_heads, size = dims
    it = iter(refs)
    proj, q_rot, k_rot, dy, gain, cos, sin, left_hbm = (next(it) for _ in range(8))
    bg_in = [next(it) for _ in bg.inputs]
    d_proj, q_gain, k_gain, grad_hbm = (next(it) for _ in range(4))
    bg.bind(iter(bg_in), it)
    q_h, k_h, v_h, dy_h, dq_h, dk_h, dv_h, left, grad_v, left_sem, grad_sem, *room = it
    left_load = pltpu.make_async_copy(left_hbm, left, left_sem)
    left_load.start()
    bg.open(room)
    q_cols, k_cols = heads * size, kv_heads * size
    scale = size**-0.5

    def prepare(p, carry):
        rows = pl.ds(pl.multiple_of(p * ROW_BLOCK, ROW_BLOCK), ROW_BLOCK)
        low = dy[rows, :].astype(BF)
        q, k, v = q_rot[rows, :], k_rot[rows, :], proj[rows, q_cols + k_cols :].astype(BF)
        for h in range(heads):
            q_h[h, rows, :] = q[:, h * size : (h + 1) * size]
            dy_h[h, rows, :] = low[:, h * size : (h + 1) * size]
        for g in range(kv_heads):
            k_h[g, rows, :] = k[:, g * size : (g + 1) * size]
            v_h[g, rows, :] = v[:, g * size : (g + 1) * size]
        return carry

    lax.fori_loop(0, length // ROW_BLOCK, prepare, 0)
    dk_h[...] = jnp.zeros_like(dk_h)
    dv_h[...] = jnp.zeros_like(dv_h)

    def head(h, carry):
        g = h // (heads // kv_heads)
        for i in range(length // ROW_BLOCK):
            rows, seen = pl.ds(i * ROW_BLOCK, ROW_BLOCK), pl.ds(0, (i + 1) * ROW_BLOCK)
            q, low, k = q_h[h, rows, :], dy_h[h, rows, :], k_h[g, seen, :]
            prob = block_weights(q, k, i * ROW_BLOCK)
            d_weights = contract(low, v_h[g, seen, :], 1, 1)
            dv_h[g, seen, :] += contract(prob.astype(BF), low, 0, 0)
            inner = jnp.sum(prob * d_weights, axis=1, keepdims=True)
            d_scores = (prob * (d_weights - inner)).astype(BF)
            dq_h[h, rows, :] = contract(d_scores, k, 1, 0) * scale
            dk_h[g, seen, :] += contract(d_scores, q, 0, 0) * scale
        return carry

    lax.fori_loop(0, heads, head, 0)
    q_gain[...] = jnp.zeros_like(q_gain)
    k_gain[...] = jnp.zeros_like(k_gain)

    def finish(p, carry):
        rows = pl.ds(pl.multiple_of(p * ROW_BLOCK, ROW_BLOCK), ROW_BLOCK)
        c, n = cos[rows, :], sin[rows, :]
        dq = jnp.concatenate([dq_h[h, rows, :] for h in range(heads)], axis=1)
        dk = jnp.concatenate([dk_h[g, rows, :] for g in range(kv_heads)], axis=1)
        dv = jnp.concatenate([dv_h[g, rows, :] for g in range(kv_heads)], axis=1)
        dq = dq * c + turn(dq * n, size, True)
        dk = dk * c[:, :k_cols] + turn(dk * n[:, :k_cols], size, True)
        dq, q_sum = head_norm_back(proj[rows, :q_cols], gain[0:1, :], dq, size)
        dk, k_sum = head_norm_back(
            proj[rows, q_cols : q_cols + k_cols], gain[1:2, :k_cols], dk, size
        )
        q_gain[...] += q_sum
        k_gain[...] += k_sum
        d_proj[rows, :q_cols] = dq.astype(BF)
        d_proj[rows, q_cols : q_cols + k_cols] = dk.astype(BF)
        d_proj[rows, q_cols + k_cols :] = dv.astype(BF)
        return carry

    lax.fori_loop(0, length // ROW_BLOCK, finish, 0)
    left_load.wait()
    grad_products(left, d_proj, grad_v, grad_hbm, grad_sem)
    for copy in grad_copies(grad_v, grad_hbm, grad_sem):
        copy.wait()
    bg.close()


def attention_dims(proj, qk_gain):
    length, width = proj.shape
    size = qk_gain.shape[1]
    heads = width // 2 // size
    return length, heads, heads // (HEADS // KV_HEADS), size


def attention_tables(width, length, qk_gain):
    size = qk_gain.shape[1]
    heads = width // 2 // size
    cosine_table, sine_table = rotation(length, size)
    return [jnp.tile(v, (1, heads)) for v in (qk_gain, cosine_table, sine_table)]


def attend(proj, qk_gain, tables, cid, tasks=()):
    dims = attention_dims(proj, qk_gain)
    length, heads, kv_heads, size = dims
    bg = Background(tasks)
    out = [jax.ShapeDtypeStruct((length, heads * size), BF)] * 2
    out.append(jax.ShapeDtypeStruct((length, kv_heads * size), BF))
    result = pl.pallas_call(
        functools.partial(attend_kernel, dims, bg),
        out_shape=out + bg.outs,
        in_specs=[VM] * 4 + [ANY] * len(bg.inputs),
        out_specs=[VM] * 3 + [ANY] * len(bg.outs),
        scratch_shapes=[
            pltpu.VMEM((n, length, size), BF) for n in (heads, kv_heads, kv_heads, heads)
        ]
        + bg.scratch,
        compiler_params=bg.params(cid),
        name=f"attend{cid}",
    )(proj, *tables, *bg.inputs)
    return result[:3], result[3:]


def attend_back(proj, rotated, d_y, qk_gain, tables, left, cid, tasks=()):
    dims = attention_dims(proj, qk_gain)
    length, heads, kv_heads, size = dims
    bg = Background(tasks)
    grad = (left.shape[1], proj.shape[1])
    out = [
        jax.ShapeDtypeStruct(proj.shape, BF),
        jax.ShapeDtypeStruct((1, heads * size), F32),
        jax.ShapeDtypeStruct((1, kv_heads * size), F32),
        jax.ShapeDtypeStruct(grad, BF),
    ]
    shapes = [(heads, BF), (kv_heads, BF), (kv_heads, BF), (heads, BF), (heads, F32)]
    shapes += [(kv_heads, F32)] * 2
    result = pl.pallas_call(
        functools.partial(attend_back_kernel, dims, bg),
        out_shape=out + bg.outs,
        in_specs=[VM] * 7 + [ANY] * (1 + len(bg.inputs)),
        out_specs=[VM] * 3 + [ANY] * (1 + len(bg.outs)),
        scratch_shapes=[pltpu.VMEM((n, length, size), kind) for n, kind in shapes]
        + [pltpu.VMEM(left.shape, BF), pltpu.VMEM(grad, BF), DMA]
        + [DMA((grad[0] // grad_chunk(grad[0]),))]
        + bg.scratch,
        compiler_params=bg.params(cid),
        name=f"attend_back{cid}",
    )(proj, *rotated, d_y, *tables, left, *bg.inputs)
    d_proj, q_gain, k_gain, d_left = result[:4]
    head_grad = jnp.stack([jnp.sum(v.reshape(-1, size), axis=0) for v in (q_gain, k_gain)])
    return (d_proj, head_grad, d_left), result[4:]


def body(boundary, norm_gain, mix_in, mix_out, w_gate, w_up, w_down, conv_x, conv_kernel, qk_gain):
    s, d, t = (lax.axis_index(a) for a in ("section", "dp", "tensor"))
    first = s == 0
    count = dp_size()
    model_width = boundary.shape[3]
    channels = mix_out.shape[1]

    def halves(shard):
        rows, cols = shard.shape
        return shard.reshape(2, rows // 2, cols)

    def pick(pair, index):
        return lax.dynamic_index_in_dim(pair, index, 0, keepdims=False)

    def by_block(kept, moved):
        return (jnp.where(first, kept, moved), jnp.where(first, moved, kept))

    seqs = boundary[0]
    sh_in, sh_out, sh_gate, sh_up, sh_down = (
        halves(v[0]) for v in (mix_in, mix_out, w_gate, w_up, w_down)
    )
    t_in, t_out, t_gate, t_seq, t_up, t_down = (
        x_half(v) for v in (sh_in, sh_out, sh_gate, seqs, sh_up, sh_down)
    )
    t_gain, zt_cols = x_move(norm_gain[0]), z_gather(conv_x)
    zt_in, zt_out, zt_gate = (
        z_gather_half(a, b, 0) for a, b in ((sh_in, t_in), (sh_out, t_out), (sh_gate, t_gate))
    )
    xt_cols, xt_in, xt_out = x_move(zt_cols), x_move(zt_in), x_move(zt_out)
    program = [("send", v) for v in (t_in, t_out, zt_cols, t_gate, t_gain, t_seq)]
    program += [("wait", t_in), ("send", zt_in), ("wait", t_out), ("send", zt_out)]
    program += [("send", t_up), ("wait", t_gate), ("send", zt_gate)]
    program += [("wait", zt_cols), ("send", xt_cols), ("wait", zt_in), ("send", xt_in)]
    program += [("wait", zt_out), ("send", xt_out), ("send", t_down)]
    rest = [t_gain, t_seq, t_up, t_down, zt_gate, xt_cols, xt_in, xt_out]
    program += [("wait", v) for v in rest]
    order = [t_in, t_out, t_gate, t_seq, t_up, t_down, t_gain]
    order += [zt_cols, zt_in, zt_out, zt_gate, xt_cols, xt_in, xt_out]
    (m_in, m_out, m_gate, m_seq, m_up, m_down, m_gain), (
        z_cols, z_in0, z_out0, z_gate0, x_cols, x_in0, x_out0
    ) = (lambda r: (r[:7], r[7:]))(exchange(order, program, 16))

    x_low, cot = by_block(pick(seqs, s), m_seq)
    gains = by_block(norm_gain[0], m_gain)
    in0, cols = Weight("rows", z_in0, x_in0), Weight("conv", z_cols, x_cols)
    out0 = Weight("cols", z_out0, x_out0)
    tables = attention_tables(2 * channels, boundary.shape[2] * 4, qk_gain)

    x_rows = x_low.astype(F32)
    (a0, proj0, value0), (x_gate0, z_up0) = gather_mm(
        x_rows, gains[0][0], [in0, cols], cid=0,
        tasks=[x_move(z_gate0), z_gather_half(sh_up, m_up, 0)],
    )
    gate_w0 = Weight("rows", z_gate0, x_gate0)
    b_gate, c_gate, product, causal = conv_core(proj0, value0, conv_kernel)
    y0 = (c_gate * causal).astype(BF)
    (mid0,), (x_up0, z_down0) = scatter_mm(
        [y0], [out0], x_rows, cid=1, tasks=[x_move(z_up0), z_gather_half(sh_down, m_down, 0)]
    )
    up_w0 = Weight("rows", z_up0, x_up0)
    (m0, gate0, up0, hid0), (x_down0, z_in1, z_out1) = gather_mm(
        mid0, gains[0][1], [gate_w0, up_w0], epilogue="ffn", cid=2,
        tasks=[x_move(z_down0), z_gather_half(sh_in, m_in, 1), z_gather_half(sh_out, m_out, 1)],
    )
    down_w0 = Weight("cols", z_down0, x_down0)
    (z_rows,), (x_in1, x_out1, z_gate1) = scatter_mm(
        [hid0], [down_w0], mid0, cid=3,
        tasks=[x_move(z_in1), x_move(z_out1), z_gather_half(sh_gate, m_gate, 1)],
    )
    z_rows = z_rows.astype(BF).astype(F32)
    in1, out1 = Weight("rows", z_in1, x_in1), Weight("cols", z_out1, x_out1)
    (a1, proj1), (x_gate1, z_up1) = gather_mm(
        z_rows, gains[1][0], [in1], cid=4,
        tasks=[x_move(z_gate1), z_gather_half(sh_up, m_up, 1)],
    )
    gate_w1 = Weight("rows", z_gate1, x_gate1)
    (y1, *rotated), (x_up1, z_down1) = attend(
        proj1, qk_gain, tables, 22, tasks=[x_move(z_up1), z_gather_half(sh_down, m_down, 1)]
    )
    up_w1 = Weight("rows", z_up1, x_up1)
    (mid1,), (x_down1,) = scatter_mm(
        [y1], [out1], z_rows, cid=5, tasks=[x_part(z_down1, 0, count // 2)]
    )
    (m1, gate1, up1, hid1), (x_down1b,) = gather_mm(
        mid1, gains[1][1], [gate_w1, up_w1], epilogue="ffn", cid=6,
        tasks=[x_part(z_down1, count // 2, count)],
    )
    down_w1 = Weight("cols", z_down1, x_down1, x_down1b)

    def split_rows(grad):
        rows, width = grad.shape
        return grad.reshape(count, 2, rows // (2 * count), width)

    def sum_rows(grad, other):
        return SumScatter("rows", grad, other)

    def sum_cols(grad, other):
        return SumScatter("cols", grad, other)

    ffn_grads = [(0, None), (1, 0), (1, 1)]
    (_, d_gate1, d_up1, g_down1, g_gate1, g_up1), _ = gather_mm(
        cot, None, [down_w1], [gate1, up1], trans=True, epilogue="ffn_back", cid=8,
        lefts=[hid1, m1], grads=ffn_grads,
    )
    g_down1, g_gate1, g_up1 = halves(g_down1), split_rows(g_gate1), split_rows(g_up1)
    (y_rows,), (r_down1,) = scatter_mm([hid1], [down_w1], mid1, cid=7, tasks=[x_half(g_down1)])
    y_rows = y_rows.astype(BF)
    (d_mid1, gain11), (q_down1, r_gate1) = scatter_mm(
        [d_gate1, d_up1], [gate_w1, up_w1], cot, (mid1, gains[1][1]), True, 9,
        tasks=[sum_cols(g_down1, r_down1), x_rows_of(g_gate1)],
    )
    (_, d_y1, g_out1), (q_gate1, r_up1) = gather_mm(
        d_mid1, None, [out1], trans=True, cid=10, lefts=[y1], grads=[(0, None)],
        tasks=[sum_rows(g_gate1, r_gate1), x_rows_of(g_up1)],
    )
    g_out1 = halves(g_out1)
    (d_proj1, head_grad, g_in1), (q_up1, r_out1, e_down1) = attend_back(
        proj1, rotated, d_y1, qk_gain, tables, a1, 23,
        tasks=[sum_rows(g_up1, r_up1), x_half(g_out1), Finish(q_down1, 1)],
    )
    g_in1 = split_rows(g_in1)
    (d_z, gain10), (q_out1, r_in1, e_gate1) = scatter_mm(
        [d_proj1], [in1], d_mid1, (z_rows, gains[1][0]), True, 11,
        tasks=[sum_cols(g_out1, r_out1), x_rows_of(g_in1), Finish(q_gate1, 1)],
    )
    d_z = d_z.astype(BF)

    (_, d_gate0, d_up0, g_down0, g_gate0, g_up0), (q_in1, e_up1, e_out1) = gather_mm(
        d_z, None, [down_w0], [gate0, up0], trans=True, epilogue="ffn_back", cid=12,
        lefts=[hid0, m0], grads=ffn_grads,
        tasks=[sum_rows(g_in1, r_in1), Finish(q_up1, 1), Finish(q_out1, 1)],
    )
    g_down0, g_gate0, g_up0 = halves(g_down0), split_rows(g_gate0), split_rows(g_up0)
    (d_mid0, gain01), (r_down0, e_in1) = scatter_mm(
        [d_gate0, d_up0], [gate_w0, up_w0], d_z, (mid0, gains[0][1]), True, 13,
        tasks=[x_half(g_down0), Finish(q_in1, 1)],
    )
    (_, d_y0, g_out0), (q_down0, r_gate0) = gather_mm(
        d_mid0, None, [out0], trans=True, cid=14, lefts=[y0], grads=[(0, None)],
        tasks=[sum_cols(g_down0, r_down0), x_rows_of(g_gate0)],
    )
    g_out0 = halves(g_out0)
    d_proj0, d_value0, kernel_grad = conv_back(proj0, value0, conv_kernel, d_y0)
    (d_x, gain00, g_in0, g_cols), (q_gate0, r_up0) = scatter_mm(
        [d_proj0, d_value0], [in0, cols], d_mid0, (x_rows, gains[0][0]), True, 15, left=a0,
        tasks=[sum_rows(g_gate0, r_gate0), x_rows_of(g_up0)],
    )
    d_x = d_x.astype(BF)
    g_in0 = split_rows(g_in0)
    g_cols = g_cols.reshape(2, count, conv_x.shape[0], channels)

    small = jnp.concatenate(
        [
            gain00,
            gain01,
            gain10,
            gain11,
            lax.dynamic_update_slice_in_dim(
                jnp.zeros((conv_kernel.shape[0], model_width), F32), kernel_grad, t * channels, 1
            ),
            jnp.pad(head_grad.reshape(1, -1), ((0, 0), (0, model_width - head_grad.size))),
        ],
        axis=0,
    )
    s_up = sum_rows(g_up0, r_up0)
    t_in0, t_cols, t_out0 = x_rows_of(g_in0), x_half(g_cols), x_half(g_out0)
    s_in, s_out = sum_rows(g_in0, t_in0), sum_cols(g_out0, t_out0)
    s_cols = SumScatter("slots", g_cols, t_cols)
    f_gate, f_down, f_up = Finish(q_gate0, 0), Finish(q_down0, 0), Finish(s_up, 0)
    f_in, f_out = Finish(s_in, 0), Finish(s_out, 0)
    t_small, t_result = x_move(small), x_move(jnp.where(first, y_rows, d_x))
    z_small = SumShare([small, t_small], "dp")
    tp_small = SumShare([z_small], "tensor", slotted=True)
    program = [("load", v) for v in (s_up, f_gate, f_down)]
    program += [("send", v) for v in (t_in0, t_small, t_cols, t_out0, s_up, t_result)]
    program += [("send", f_down), ("send", f_gate)]
    program += [("wait", t_in0), ("reload", s_in), ("send", s_in)]
    program += [("wait", t_cols), ("reload", s_cols), ("wait", t_out0), ("reload", s_out)]
    program += [("send", s_out), ("send", s_cols), ("wait", t_small), ("send", z_small)]
    program += [("wait", s_up), ("reload", f_up), ("send", f_up)]
    program += [("wait", s_in), ("reload", f_in), ("send", f_in)]
    program += [("wait", z_small), ("send", tp_small)]
    program += [("wait", s_out), ("reload", f_out), ("send", f_out)]
    rest = [s_cols, tp_small, t_result, f_gate, f_down, f_up, f_in, f_out]
    program += [("wait", v) for v in rest]
    order = [t_in0, t_cols, t_out0, s_up, s_in, s_out, s_cols, f_gate, f_down, f_up, f_in, f_out]
    order += [t_small, z_small, tp_small, t_result]
    *_, q_cols, e_gate0, e_down0, e_up0, e_in0, e_out0, _, _, small_t, out_moved = exchange(
        order, program, 17
    )
    small = jnp.sum(small_t, axis=0)

    def whole(zero, one):
        kept = jnp.where(first, zero, one)
        return kept.reshape(1, -1, kept.shape[-1]).astype(F32)

    result = jnp.where(first, jnp.stack([d_x, out_moved]), jnp.stack([out_moved, y_rows]))
    gains_total = small[:4].reshape(2, 2, model_width)
    gain_out = lax.dynamic_slice_in_dim(gains_total, s, 1, 0)
    kernel_rows = small[4 : 4 + conv_kernel.shape[0]]
    kernel_out = lax.dynamic_slice_in_dim(kernel_rows, t * channels, channels, 1)
    head_total = small[-1, : qk_gain.size].reshape(qk_gain.shape)
    return (
        result[None],
        gain_out,
        whole(e_in0, e_in1),
        whole(e_out0, e_out1),
        whole(e_gate0, e_gate1),
        whole(e_up0, e_up1),
        whole(e_down0, e_down1),
        jnp.sum(q_cols.astype(F32), axis=0),
        kernel_out,
        head_total,
    )


def solution(mesh):
    in_specs = (
        P("section", "dp", "tensor", None),
        P("section", None, None),
        P("section", "dp", "tensor"),
        P("section", "tensor", "dp"),
        P("section", "dp", "tensor"),
        P("section", "dp", "tensor"),
        P("section", "tensor", "dp"),
        P(("section", "dp"), "tensor"),
        P(None, "tensor"),
        P(),
    )
    out_specs = (
        P("section", "dp", "tensor", None),
        P("section", None, None),
        P("section", "dp", "tensor"),
        P("section", "tensor", "dp"),
        P("section", "dp", "tensor"),
        P("section", "dp", "tensor"),
        P("section", "tensor", "dp"),
        P(("section", "dp"), "tensor"),
        P(None, "tensor"),
        P(),
    )
    return jax.shard_map(body, mesh=mesh, in_specs=in_specs, out_specs=out_specs, check_vma=False)
```

```python
import functools

import jax
import jax.numpy as jnp
from jax import lax
from jax.experimental import pallas as pl
from jax.experimental.pallas import tpu as pltpu
from jax.sharding import PartitionSpec as P

HEADS = 16
KV_HEADS = 8

EPS = 1e-05
ROPE_BASE = 1000000.0
MASKED = -1e30

MESH = pl.DeviceIdType.MESH
ANY = pl.BlockSpec(memory_space=pl.ANY)
DMA = pltpu.SemaphoreType.DMA
VMEM_BYTES = 63 * 1024 * 1024
BF = jnp.bfloat16
F32 = jnp.float32
ROW_BLOCK = 256


def contract(left_op, right_op, left_dim, right_dim):
    return lax.dot_general(
        left_op, right_op, (((left_dim,), (right_dim,)), ((), ())), preferred_element_type=F32
    )


def norm_rows(values, gain):
    return values * lax.rsqrt(jnp.mean(values * values, axis=-1, keepdims=True) + EPS) * gain


def norm_back(values, gain, grad_in):
    row_scale = lax.rsqrt(jnp.mean(values * values, axis=-1, keepdims=True) + EPS)
    normed = values * row_scale
    gain_grad = jnp.sum(grad_in * normed, axis=0, keepdims=True)
    scaled = grad_in * gain
    value_grad = row_scale * (scaled - normed * jnp.mean(scaled * normed, axis=-1, keepdims=True))
    return (value_grad, gain_grad)


def rotation(length, head_size):
    half_size = head_size // 2
    frequency = ROPE_BASE ** (-(jnp.arange(half_size, dtype=jnp.float32) * 2.0 / head_size))
    angles = jnp.arange(length, dtype=jnp.float32)[:, None] * frequency[None, :]
    cosine_table = jnp.concatenate([jnp.cos(angles), jnp.cos(angles)], axis=1)
    sine_table = jnp.concatenate([jnp.sin(angles), jnp.sin(angles)], axis=1)
    return (cosine_table, sine_table)


def silu_parts(gate):
    sig = 1.0 / (1.0 + jnp.exp(-gate))
    return sig, gate * sig


def dp_size():
    return lax.axis_size("dp")


def spot():
    return tuple(lax.axis_index(a) for a in ("section", "dp", "tensor"))


def block_of(index, size):
    return pl.ds(pl.multiple_of(index * size, size), size)


class Val:
    def __init__(self, shape, dtype):
        self.shape, self.dtype = tuple(shape), dtype
        self.ref = self.array = None


class Kernel:
    def __init__(self, cid):
        self.cid, self.ins, self.arrays, self.outs, self.room = cid, [], [], [], []
        self.early, self.steps, self.late, self.axes = [], [], [], {"tensor"}
        self.once = []

    def input(self, array):
        array = array.array if isinstance(array, Val) else array
        for val, known in zip(self.ins, self.arrays):
            if known is array:
                return val
        val = Val(array.shape, array.dtype)
        self.ins.append(val)
        self.arrays.append(array)
        return val

    def output(self, shape, dtype):
        val = Val(shape, dtype)
        self.outs.append(val)
        return val

    def vmem(self, shape, dtype):
        val = Val(shape, dtype)
        self.room.append((val, pltpu.VMEM(tuple(shape), dtype)))
        return val

    def sem(self, *shape):
        val = Val(shape, None)
        self.room.append((val, DMA(shape)))
        return val

    def do(self, *steps):
        self.steps += steps

    def body(self, *refs):
        vals = self.ins + self.outs + [val for val, _ in self.room]
        for val, ref in zip(vals, refs):
            val.ref = ref
        for item in self.once:
            item.waited = False
        for step in self.early:
            step()
        self.greet()
        for step in self.steps + self.late:
            step()

    def greet(self):
        s, d, t = spot()
        peers = []
        if "section" in self.axes:
            peers.append({"section": 1 - s})
        if "dp" in self.axes:
            peers += [{"dp": (d + k) % dp_size()} for k in range(1, dp_size())]
        peers += [{"tensor": (t + k) % 4} for k in range(1, 4)]
        barrier = pltpu.get_barrier_semaphore()
        for peer in peers:
            pl.semaphore_signal(barrier, inc=1, device_id=peer, device_id_type=MESH)
        pl.semaphore_wait(barrier, len(peers))

    def build(self):
        result = pl.pallas_call(
            self.body,
            out_shape=[jax.ShapeDtypeStruct(v.shape, v.dtype) for v in self.outs],
            in_specs=[ANY] * len(self.ins),
            out_specs=[ANY] * len(self.outs),
            scratch_shapes=[room for _, room in self.room],
            compiler_params=pltpu.CompilerParams(
                collective_id=self.cid, has_side_effects=True, vmem_limit_bytes=VMEM_BYTES
            ),
            name=f"stage{self.cid}",
        )(*self.arrays)
        for val, array in zip(self.outs, result):
            val.array = array


def remote(src, dst, send_sem, recv_sem, peer):
    return pltpu.make_async_remote_copy(
        src_ref=src, dst_ref=dst, send_sem=send_sem, recv_sem=recv_sem,
        device_id=peer, device_id_type=MESH,
    )


class Load:
    def __init__(self, k, sources, shape, dtype, early=False):
        self.k, self.sources, self.waited = k, sources, False
        self.buf, self.sem = k.vmem(shape, dtype), k.sem(1)
        k.once.append(self)
        if early:
            k.early.append(self.start)

    def moves(self):
        for cond, source in self.sources(*spot()):
            yield cond, pltpu.make_async_copy(source, self.buf.ref, self.sem.ref.at[0])

    def start(self):
        for cond, move in self.moves():
            if cond is None:
                move.start()
            else:
                pl.when(cond)(move.start)

    def wait(self):
        if not self.waited:
            self.waited = True
            next(self.moves())[1].wait()


def load_all(k, array, early=True):
    val = k.input(array)
    return Load(k, lambda s, d, t: [(None, val.ref)], val.shape, val.dtype, early)


class Save:
    def __init__(self, k, buf):
        self.buf, self.out, self.sem = buf, k.output(buf.shape, buf.dtype), k.sem(1)
        self.waited = False
        k.once.append(self)
        k.late.append(self.wait)

    def move(self):
        return pltpu.make_async_copy(self.buf.ref, self.out.ref, self.sem.ref.at[0])

    def start(self):
        self.move().start()

    def wait(self):
        if not self.waited:
            self.waited = True
            self.move().wait()


class Task:
    final = None

    def __init__(self, k, out, axis, moves, count, n_local=1, out_dtype=BF):
        self.k, self.axis, self.make = k, axis, moves
        self.out = k.output(out, out_dtype)
        self.send_sem, self.recv_sem, self.local_sem = k.sem(count), k.sem(count), k.sem(n_local)
        self.waited = False
        k.axes.add(axis)
        k.once.append(self)

    def local(self, src, dst, i):
        return pltpu.make_async_copy(src, dst, self.local_sem.ref.at[i])

    def pairs(self, every):
        far, near = self.make(*spot())
        for i, (sources, dst, peer) in enumerate(far):
            for cond, src in sources if every else sources[:1]:
                yield cond, True, remote(
                    src, dst, self.send_sem.ref.at[i], self.recv_sem.ref.at[i], peer
                )
        for i, (sources, dst) in enumerate(near):
            for cond, src in sources if every else sources[:1]:
                yield cond, False, self.local(src, dst, i)

    def send(self):
        for cond, far, move in self.pairs(True):
            if far and self.final is not None:
                cond = lax.axis_index("section") == 1 - self.final
            if cond is None:
                move.start()
            else:
                pl.when(cond)(move.start)

    def wait(self):
        if self.waited:
            return
        self.waited = True
        s = lax.axis_index("section")
        for _, far, move in self.pairs(False):
            if not far:
                move.wait()
            elif self.final is None:
                move.wait_recv()
                move.wait_send()
            else:
                pl.when(s == 1 - self.final)(move.wait_send)
                pl.when(s == self.final)(move.wait_recv)


def as_val(k, value):
    value = value.out if isinstance(value, Task) else value
    known = isinstance(value, Val) and (value.array is None)
    return value if known else k.input(value)


def z_gather(k, value):
    val, count = as_val(k, value), dp_size()

    def moves(s, d, t):
        source = [(None, val.ref)]
        dst = task.out.ref.at[d]
        return [(source, dst, {"dp": (d + i) % count}) for i in range(1, count)], [(source, dst)]

    task = Task(k, (count,) + val.shape, "dp", moves, count - 1, out_dtype=val.dtype)
    return task


def z_gather_half(k, shard, moved, block):
    shard, moved, count = as_val(k, shard), as_val(k, moved), dp_size()
    rows = shard.shape[0] // 2

    def moves(s, d, t):
        sources = [
            (s == block, shard.ref.at[pl.ds(block * rows, rows)]),
            (s == 1 - block, moved.ref),
        ]
        dst = task.out.ref.at[d]
        return [(sources, dst, {"dp": (d + i) % count}) for i in range(1, count)], [(sources, dst)]

    task = Task(k, (count,) + moved.shape, "dp", moves, count - 1)
    return task


def x_move(k, value):
    val = as_val(k, value)

    def moves(s, d, t):
        return [([(None, val.ref)], task.out.ref, {"section": 1 - s})], []

    task = Task(k, val.shape, "section", moves, 1, out_dtype=val.dtype)
    return task


def x_half(k, value):
    val = as_val(k, value)
    rows = val.shape[0] // 2

    def moves(s, d, t):
        src = val.ref.at[block_of(1 - s, rows)]
        return [([(None, src)], task.out.ref, {"section": 1 - s})], []

    task = Task(k, (rows,) + val.shape[1:], "section", moves, 1, out_dtype=val.dtype)
    return task


def x_slots(k, value, kind):
    val, count = as_val(k, value), dp_size()
    rows = val.shape[0] // (2 * count)

    def moves(s, d, t):
        far = []
        for i in range(count):
            slot = 2 * i + 1 - s if kind == "rows" else (1 - s) * count + i
            src = val.ref.at[block_of(slot, rows)]
            far.append(([(None, src)], task.out.ref.at[i], {"section": 1 - s}))
        return far, []

    task = Task(k, (count, rows) + val.shape[1:], "section", moves, count)
    return task


class SumScatter(Task):
    def __init__(self, k, kind, grads, received):
        count = dp_size()
        self.grads, self.got_val = as_val(k, grads), as_val(k, received)
        if kind == "cols":
            rows, cols = self.grads.shape[0] // 2, self.grads.shape[1] // count
            held = (rows, self.grads.shape[1])
        else:
            rows, cols = self.grads.shape[0] // (2 * count), self.grads.shape[1]
            held = (count, rows, cols)
        self.kind, self.rows, self.cols, self.n = kind, rows, cols, count
        self.kept, self.got = k.vmem(held, BF), k.vmem(held, BF)
        self.total = k.vmem((count, rows, cols), BF)

        def moves(s, d, t):
            total = self.total.ref
            far = []
            for i in range(1, count):
                other = (d + i) % count
                far.append(([(None, total.at[other])], self.out.ref.at[d], {"dp": other}))
            return far, [([(None, total.at[d])], self.out.ref.at[d])]

        super().__init__(k, (count, rows, cols), "dp", moves, count - 1, 2 + count)

    def loads(self):
        s, grads, kept = lax.axis_index("section"), self.grads.ref, self.kept.ref
        if self.kind == "cols":
            moves = [self.local(grads.at[block_of(s, self.rows)], kept, 2)]
        else:
            moves = []
            for i in range(self.n):
                slot = 2 * i + s if self.kind == "rows" else s * self.n + i
                moves.append(self.local(grads.at[block_of(slot, self.rows)], kept.at[i], 2 + i))
        return moves + [self.local(self.got_val.ref, self.got.ref, 1)]

    def load(self):
        for move in self.loads():
            move.start()

    def send(self):
        for move in self.loads():
            move.wait()
        kept, got, total = self.kept.ref, self.got.ref, self.total.ref
        for i in range(self.n):
            if self.kind == "cols":
                part = (slice(None), slice(i * self.cols, (i + 1) * self.cols))
            else:
                part = i
            total[i] = (kept[part].astype(F32) + got[part].astype(F32)).astype(BF)
        super().send()

    def add(self):
        self.load()
        self.send()


class Finish(Task):
    def __init__(self, k, pieces, block):
        self.pieces, self.final = as_val(k, pieces), block
        self.n, rows, cols = self.pieces.shape
        self.held, self.total = k.vmem(self.pieces.shape, BF), k.vmem((rows, cols), BF)

        def moves(s, d, t):
            source, dst = [(None, self.total.ref)], self.out.ref.at[s]
            return [(source, dst, {"section": 1 - s})], [(source, dst)]

        super().__init__(k, (2, rows, cols), "section", moves, 1, 2)

    def load(self):
        self.local(self.pieces.ref, self.held.ref, 1).start()

    def send(self):
        self.local(self.pieces.ref, self.held.ref, 1).wait()
        held = self.held.ref
        acc = held[0].astype(F32)
        for i in range(1, self.n):
            acc = acc + held[i].astype(F32)
        self.total.ref[...] = acc.astype(BF)
        super().send()

    def add(self):
        self.load()
        self.send()


class SumShare(Task):
    def __init__(self, k, terms, axis, slotted=False):
        self.terms = [as_val(k, v) for v in terms]
        shape = self.terms[0].shape[1:] if slotted else self.terms[0].shape
        count = dp_size() if axis == "dp" else 4
        self.slotted = slotted
        self.bufs = [k.vmem(v.shape, F32) for v in self.terms]
        self.total = k.vmem(shape, F32)

        def moves(s, d, t):
            source, me = [(None, self.total.ref)], d if axis == "dp" else t
            dst = self.out.ref.at[me]
            far = [(source, dst, {axis: (me + i) % count}) for i in range(1, count)]
            return far, [(source, dst)]

        super().__init__(k, (count,) + shape, axis, moves, count - 1, 3, out_dtype=F32)

    def add(self):
        loads = [self.local(v.ref, b.ref, 1 + i) for i, (v, b) in enumerate(zip(self.terms, self.bufs))]
        for load in loads:
            load.start()
        for load in loads:
            load.wait()
        if self.slotted:
            parts = [self.bufs[0].ref[i] for i in range(self.terms[0].shape[0])]
        else:
            parts = [buf.ref[...] for buf in self.bufs]
        acc = parts[0]
        for part in parts[1:]:
            acc = acc + part
        self.total.ref[...] = acc
        self.send()


class Weight:
    def __init__(self, k, kind, near, far, early=False):
        near, far = as_val(k, near), as_val(k, far)
        self.count, self.rows, self.cols = near.shape
        self.kind, self.near, self.far, self.waited = kind, near, far, False
        if kind == "cols":
            shape = (2 * self.rows, self.count * self.cols)
        else:
            shape = (2 * self.count * self.rows, self.cols)
        self.aside = kind == "cols" and self.cols % 128 != 0
        self.buf, self.sem = k.vmem(shape, BF), k.sem(2 * self.count)
        if self.aside:
            self.held = [k.vmem(near.shape, BF), k.vmem(near.shape, BF)]
        k.once.append(self)
        if early:
            k.early.append(self.start)

    def moves(self):
        s, dst = lax.axis_index("section"), self.buf.ref
        rows, cols = self.rows, self.cols

        def place(sec, own):
            if self.aside:
                return None
            if self.kind == "cols":
                return dst.at[block_of(sec, rows), pl.ds(own * cols, cols)]
            slot = own * 2 + sec if self.kind == "rows" else sec * self.count + own
            return dst.at[block_of(slot, rows)]

        for i in range(self.count):
            for j, (val, sec) in enumerate(((self.near, s), (self.far, 1 - s))):
                to = self.held[j].ref.at[i] if self.aside else place(sec, i)
                yield pltpu.make_async_copy(val.ref.at[i], to, self.sem.ref.at[2 * i + j])

    def start(self):
        for move in self.moves():
            move.start()

    def wait(self):
        if self.waited:
            return
        self.waited = True
        for move in self.moves():
            move.wait()
        if self.aside:
            s = lax.axis_index("section")
            for j, sec in enumerate((s, 1 - s)):
                whole = jnp.concatenate([self.held[j].ref[i] for i in range(self.count)], axis=1)
                self.buf.ref[block_of(sec, self.rows), :] = whole


class Product:
    def __init__(self, k, left, right):
        self.left, self.right = left, right
        rows = left.shape[1]
        self.chunk = 384 if rows % 384 == 0 else 256
        self.count = rows // self.chunk
        self.buf = k.vmem((rows, right.shape[1]), BF)
        self.out, self.sem = k.output(self.buf.shape, BF), k.sem(self.count)

    def copy(self, i):
        part = block_of(i, self.chunk)
        return pltpu.make_async_copy(self.buf.ref.at[part], self.out.ref.at[part], self.sem.ref.at[i])

    def run(self):
        def step(i, carry):
            part = block_of(i, self.chunk)
            value = contract(self.left.ref[:, part], self.right.ref[...], 0, 0)
            self.buf.ref[part, :] = value.astype(BF)
            self.copy(i).start()
            return carry

        lax.fori_loop(0, self.count, step, 0)

    def wait(self):
        for i in range(self.count):
            self.copy(i).wait()


def places():
    me = lax.axis_index("tensor")
    sib = me + 1 - 2 * (me % 2)
    cross = (me + 2) % 4
    diag = (sib + 2) % 4
    return me, sib, cross, diag


class Gather:
    def __init__(self, k, x, gain, weights, extras=(), trans=False, epilogue="plain", save=()):
        rows, width = x.shape
        length = 4 * rows
        self.k, self.x, self.gain, self.weights, self.extras = k, x, gain, weights, extras
        self.trans, self.epilogue, self.rows, self.half = trans, epilogue, rows, rows // 2
        cols = [w.buf.shape[0 if trans else 1] for w in weights]
        kinds = {
            "plain": [(c, F32) for c in cols],
            "ffn": [(cols[0], BF)] * 3,
            "ffn_back": [(cols[0], BF)] * 2,
        }[epilogue]
        self.full = k.vmem((length, width), BF)
        self.values = [k.vmem((length, c), kind) for c, kind in kinds]
        kept = [self.full] + self.values
        self.saved = [(v, k.output(v.shape, v.dtype), k.sem(4, 2)) for v in kept if kept.index(v) in save]
        self.sems = [k.sem(2) for _ in range(6)]
        k.late.append(self.end)

    def span(self, owner, sub):
        return pl.ds(pl.multiple_of(owner * self.rows + sub * self.half, self.half), self.half)

    def move(self, kind, i):
        me, sib, cross, _ = places()
        full = self.full.ref
        owner, peer, at = {"cross": (me, cross, 0), "sib": (me, sib, 2), "relay": (cross, sib, 4)}[kind]
        part = full.at[self.span(owner, i)]
        return remote(
            part, part, self.sems[at].ref.at[i], self.sems[at + 1].ref.at[i], {"tensor": peer}
        )

    def begin(self):
        me = places()[0]
        for i in range(2):
            part = self.x.ref[pl.ds(i * self.half, self.half), :].astype(F32)
            if self.gain is not None:
                val, row = self.gain
                part = norm_rows(part, val.ref[row : row + 1, :])
            self.full.ref[self.span(me, i), :] = part.astype(BF)
            self.move("cross", i).start()
            self.move("sib", i).start()

    def loop(self):
        me, sib, cross, diag = places()
        rows, half = self.rows, self.half
        for w in self.weights:
            w.wait()

        def step(p, carry):
            far, sub = p // 2, p % 2
            near = (1 - sub) * me + sub * sib
            first = (1 - far) * near * rows + far * (cross * rows + sub * half)
            second = (1 - far) * (near * rows + half) + far * (diag * rows + sub * half)
            pair = [pl.ds(pl.multiple_of(v, half), half) for v in (first, second)]

            @pl.when(p == 1)
            def _():
                self.move("sib", 0).wait_recv()
                self.move("sib", 1).wait_recv()

            for i in range(2):

                @pl.when(p == 2 + i)
                def _():
                    self.move("cross", i).wait_recv()
                    self.move("relay", i).start()
                    self.move("relay", i).wait_recv()

            def both(val):
                return jnp.concatenate([val.ref[pair[0], :], val.ref[pair[1], :]], axis=0)

            a = both(self.full)
            prods = [contract(a, w.buf.ref[...], 1, 1 if self.trans else 0) for w in self.weights]
            if self.epilogue == "plain":
                values = prods
            elif self.epilogue == "ffn":
                sig, silu = silu_parts(prods[0])
                values = [prods[0], prods[1], silu * prods[1]]
            else:
                gate, up = (both(v).astype(F32) for v in self.extras)
                sig, silu = silu_parts(gate)
                values = [prods[0] * up * sig * (1.0 + gate * (1.0 - sig)), prods[0] * silu]
            for val, value in zip(self.values, values):
                value = value.astype(val.dtype)
                for j in range(2):
                    val.ref[pair[j], :] = value[j * half : (j + 1) * half]
            for val, out, sem in self.saved:
                for j in range(2):
                    pltpu.make_async_copy(
                        val.ref.at[pair[j]], out.ref.at[pair[j]], sem.ref.at[p, j]
                    ).start()
            return carry

        lax.fori_loop(0, 4, step, 0)

    def end(self):
        for i in range(2):
            for kind in ("cross", "sib", "relay"):
                self.move(kind, i).wait_send()
        part = pl.ds(0, self.half)
        for val, out, sem in self.saved:
            for p in range(4):
                for j in range(2):
                    pltpu.make_async_copy(val.ref.at[part], out.ref.at[part], sem.ref.at[p, j]).wait()


class Scatter:
    def __init__(self, k, operands, weights, resid, back=None, trans=False, low=False):
        rows, width = resid.shape
        half = rows // 2
        self.operands, self.weights, self.resid, self.back = operands, weights, resid, back
        self.trans, self.low, self.rows, self.half = trans, low, rows, half
        self.keep, self.own = k.vmem((2, half, width), F32), k.vmem((rows, width), F32)
        self.to_s, self.from_s, self.to_c, self.from_c = (
            k.vmem((2, half, width), BF) for _ in range(4)
        )
        self.to_o, self.from_o = k.vmem((rows, width), BF), k.vmem((rows, width), BF)
        self.out = k.vmem((rows, width), BF if low else F32)
        self.gain_grad = k.vmem((1, width), F32) if back else None
        self.sems = [k.sem(2) for _ in range(4)] + [k.sem(1) for _ in range(2)]
        k.late.append(self.end)

    def move(self, kind, i=0):
        _, sib, cross, _ = places()
        at, src, dst, peer = {
            "diag": (0, self.to_s, self.from_s, sib),
            "cross": (2, self.to_c, self.from_c, cross),
            "near": (4, self.to_o, self.from_o, sib),
        }[kind]
        src, dst = (src.ref, dst.ref) if kind == "near" else (src.ref.at[i], dst.ref.at[i])
        return remote(
            src, dst, self.sems[at].ref.at[i], self.sems[at + 1].ref.at[i], {"tensor": peer}
        )

    def pass_on(self, i):
        self.move("diag", i).wait_recv()
        total = self.keep.ref[i] + self.from_s.ref[i].astype(F32)
        self.to_c.ref[i] = total.astype(BF)
        self.move("cross", i).start()

    def loop(self):
        me, sib, cross, diag = places()
        rows, half = self.rows, self.half
        for w in self.weights:
            w.wait()

        def step(p, carry):
            near, sub = p // 2, p % 2
            base = near * ((1 - sub) * sib + sub * me) * rows
            first = base + (1 - near) * (cross * rows + sub * half)
            second = base + near * half + (1 - near) * (diag * rows + sub * half)
            pair = [pl.ds(pl.multiple_of(v, half), half) for v in (first, second)]
            total = None
            for y, w in zip(self.operands, self.weights):
                a = jnp.concatenate([y.ref[pair[0], :], y.ref[pair[1], :]], axis=0)
                prod = contract(a, w.buf.ref[...], 1, 1 if self.trans else 0)
                total = prod if total is None else total + prod

            for i in range(2):

                @pl.when(p == i)
                def _():
                    self.keep.ref[i] = total[:half]
                    self.to_s.ref[i] = total[half:].astype(BF)
                    self.move("diag", i).start()

            @pl.when(p == 1)
            def _():
                self.pass_on(0)

            @pl.when(p == 2)
            def _():
                self.to_o.ref[...] = total.astype(BF)
                self.move("near").start()
                self.pass_on(1)

            @pl.when(p == 3)
            def _():
                self.own.ref[...] = total

            return carry

        lax.fori_loop(0, 4, step, 0)

    def finish(self):
        self.move("near").wait_recv()
        gain_sum = None
        for i in range(2):
            part = pl.ds(i * self.half, self.half)
            self.move("cross", i).wait_recv()
            total = self.own.ref[part, :] + self.from_o.ref[part, :].astype(F32)
            total = total + self.from_c.ref[i].astype(F32)
            resid = self.resid.ref[part, :].astype(F32)
            if self.back:
                value, (gain, row) = self.back
                value_grad, gain_grad = norm_back(
                    value.ref[part, :].astype(F32), gain.ref[row : row + 1, :], total
                )
                total = value_grad
                gain_sum = gain_grad if gain_sum is None else gain_sum + gain_grad
            self.out.ref[part, :] = (resid + total).astype(self.out.dtype)
        if self.back:
            self.gain_grad.ref[...] = gain_sum

    def end(self):
        self.move("near").wait_send()
        for i in range(2):
            self.move("diag", i).wait_send()
            self.move("cross", i).wait_send()


def delayed(values, by):
    if by == 0:
        return values
    row = lax.broadcasted_iota(jnp.int32, values.shape, 0)
    return jnp.where(row < by, 0.0, pltpu.roll(values, by, 0))


def advanced(values, by):
    if by == 0:
        return values
    length = values.shape[0]
    row = lax.broadcasted_iota(jnp.int32, values.shape, 0)
    return jnp.where(row >= length - by, 0.0, pltpu.roll(values, length - by, 0))


CONV_COLS = 128


class Conv:
    def __init__(self, k, projected, value, kernel):
        self.projected, self.value, self.kernel = projected, value, kernel
        self.y = k.vmem(value.shape, BF)

    def parts(self, j):
        channels = self.value.shape[1]
        at = slice(j * CONV_COLS, (j + 1) * CONV_COLS)
        b_gate = self.projected.ref[:, at]
        c_gate = self.projected.ref[:, channels + at.start : channels + at.stop]
        x_value, taps = self.value.ref[:, at], self.kernel.ref[:, at]
        product = b_gate * x_value
        count = taps.shape[0]
        causal = jnp.zeros_like(product)
        for i in range(count):
            causal = causal + taps[i : i + 1] * delayed(product, count - 1 - i)
        return at, b_gate, c_gate, x_value, taps, product, causal

    def run(self):
        for j in range(self.value.shape[1] // CONV_COLS):
            at, _, c_gate, _, _, _, causal = self.parts(j)
            self.y.ref[:, at] = (c_gate * causal).astype(BF)


class ConvBack(Conv):
    def __init__(self, k, projected, value, kernel, d_y):
        self.projected, self.value, self.kernel, self.d_y = projected, value, kernel, d_y
        self.d_proj = k.vmem(projected.shape, BF)
        self.d_value = k.vmem(value.shape, BF)
        self.d_kernel = k.vmem(kernel.shape, F32)

    def run(self):
        channels = self.value.shape[1]
        for j in range(channels // CONV_COLS):
            at, b_gate, c_gate, x_value, taps, product, causal = self.parts(j)
            d_y = self.d_y.ref[:, at]
            d_causal = d_y * c_gate
            count = taps.shape[0]
            d_product = jnp.zeros_like(product)
            for i in range(count):
                by = count - 1 - i
                row = jnp.sum(d_causal * delayed(product, by), axis=0, keepdims=True)
                self.d_kernel.ref[i : i + 1, at] = row
                d_product = d_product + taps[i : i + 1] * advanced(d_causal, by)
            self.d_proj.ref[:, at] = (d_product * x_value).astype(BF)
            self.d_proj.ref[:, channels + at.start : channels + at.stop] = (d_y * causal).astype(BF)
            self.d_value.ref[:, at] = (d_product * b_gate).astype(BF)


def head_mean(values, head_size):
    width = values.shape[1]
    row = lax.broadcasted_iota(jnp.int32, (width, width), 0) // head_size
    col = lax.broadcasted_iota(jnp.int32, (width, width), 1) // head_size
    group = jnp.where(row == col, 1.0 / head_size, 0.0).astype(F32)
    return lax.dot_general(
        values, group, (((1,), (0,)), ((), ())),
        precision=lax.Precision.HIGHEST, preferred_element_type=F32,
    )


def turn(values, head_size, back):
    width, half = values.shape[1], head_size // 2
    lane = lax.broadcasted_iota(jnp.int32, values.shape, 1) % head_size
    upper = pltpu.roll(values, width - half, 1)
    lower = pltpu.roll(values, half, 1)
    return jnp.where(lane < half, upper, -lower) if back else jnp.where(lane < half, -upper, lower)


def head_norm(values, gain, head_size):
    return values * lax.rsqrt(head_mean(values * values, head_size) + EPS) * gain


def head_norm_back(values, gain, grad_in, head_size):
    row_scale = lax.rsqrt(head_mean(values * values, head_size) + EPS)
    normed = values * row_scale
    gain_grad = jnp.sum(grad_in * normed, axis=0, keepdims=True)
    scaled = grad_in * gain
    return row_scale * (scaled - normed * head_mean(scaled * normed, head_size)), gain_grad


def block_weights(q_rows, k_rows, first_row):
    rows, length = q_rows.shape[0], k_rows.shape[0]
    scores = contract(q_rows, k_rows, 1, 1) * (q_rows.shape[1] ** -0.5)
    query = first_row + lax.broadcasted_iota(jnp.int32, (rows, length), 0)
    key = lax.broadcasted_iota(jnp.int32, (rows, length), 1)
    scores = jnp.where(key <= query, scores, MASKED)
    exps = jnp.exp(scores - jnp.max(scores, axis=1, keepdims=True))
    return exps * (1.0 / jnp.sum(exps, axis=1, keepdims=True))


class Heads:
    def __init__(self, projected, tables, size):
        self.projected, self.size = projected, size
        self.gain, self.cos, self.sin = (v.buf for v in tables)
        self.loads = tables
        self.length, width = projected.shape
        self.q_cols, self.k_cols = width // 2, width // 4
        self.heads, self.kv_heads = self.q_cols // size, self.k_cols // size
        self.share = self.heads // self.kv_heads

    def per_head(self, k, count, kind):
        return k.vmem((count, self.length, self.size), kind)

    def split(self, val, rows, values):
        for h in range(val.shape[0]):
            val.ref[h, rows, :] = values[:, h * self.size : (h + 1) * self.size]

    def join(self, val, rows):
        return jnp.concatenate([val.ref[h, rows, :] for h in range(val.shape[0])], axis=1)

    def blocks(self, step):
        lax.fori_loop(0, self.length // ROW_BLOCK, lambda p, c: step(block_of(p, ROW_BLOCK)) or c, 0)


class Attend(Heads):
    def __init__(self, k, projected, tables, size):
        super().__init__(projected, tables, size)
        self.q_rot = k.vmem((self.length, self.q_cols), BF)
        self.k_rot = k.vmem((self.length, self.k_cols), BF)
        self.y = k.vmem((self.length, self.q_cols), BF)
        self.q_h, self.y_h = (self.per_head(k, self.heads, BF) for _ in range(2))
        self.k_h, self.v_h = (self.per_head(k, self.kv_heads, BF) for _ in range(2))

    def run(self, *between):
        for load in self.loads:
            load.wait()
        size, q_cols, k_cols, proj = self.size, self.q_cols, self.k_cols, self.projected.ref

        def prepare(rows):
            c, n = self.cos.ref[rows, :], self.sin.ref[rows, :]
            q = head_norm(proj[rows, :q_cols], self.gain.ref[0:1, :], size)
            q = (q * c + turn(q, size, False) * n).astype(BF)
            k = head_norm(proj[rows, q_cols : q_cols + k_cols], self.gain.ref[1:2, :k_cols], size)
            k = (k * c[:, :k_cols] + turn(k, size, False) * n[:, :k_cols]).astype(BF)
            self.q_rot.ref[rows, :] = q
            self.k_rot.ref[rows, :] = k
            self.split(self.q_h, rows, q)
            self.split(self.k_h, rows, k)
            self.split(self.v_h, rows, proj[rows, q_cols + k_cols :].astype(BF))

        self.blocks(prepare)

        def head(h, carry):
            g = h // self.share
            for i in range(self.length // ROW_BLOCK):
                rows, seen = pl.ds(i * ROW_BLOCK, ROW_BLOCK), pl.ds(0, (i + 1) * ROW_BLOCK)
                weights = block_weights(
                    self.q_h.ref[h, rows, :], self.k_h.ref[g, seen, :], i * ROW_BLOCK
                )
                value = contract(weights.astype(BF), self.v_h.ref[g, seen, :], 1, 0)
                self.y_h.ref[h, rows, :] = value.astype(BF)
            return carry

        lax.fori_loop(0, self.heads // 2, head, 0)
        for step in between:
            step()
        lax.fori_loop(self.heads // 2, self.heads, head, 0)
        self.y.ref[...] = self.join(self.y_h, slice(None))


class AttendBack(Heads):
    def __init__(self, k, projected, tables, size, q_rot, k_rot, d_y):
        super().__init__(projected, tables, size)
        self.q_rot, self.k_rot, self.d_y = q_rot, k_rot, d_y
        self.q_h, self.dy_h = (self.per_head(k, self.heads, BF) for _ in range(2))
        self.k_h, self.v_h = (self.per_head(k, self.kv_heads, BF) for _ in range(2))
        self.dq_h = self.per_head(k, self.heads, F32)
        self.dk_h, self.dv_h = (self.per_head(k, self.kv_heads, F32) for _ in range(2))
        self.d_proj = k.vmem(projected.shape, BF)
        self.q_gain, self.k_gain = k.vmem((1, self.q_cols), F32), k.vmem((1, self.k_cols), F32)

    def run(self):
        for load in self.loads:
            load.wait()
        size, q_cols, k_cols, proj = self.size, self.q_cols, self.k_cols, self.projected.ref
        scale = size**-0.5
        dq_h, dk_h, dv_h = self.dq_h.ref, self.dk_h.ref, self.dv_h.ref

        def prepare(rows):
            self.split(self.q_h, rows, self.q_rot.ref[rows, :])
            self.split(self.dy_h, rows, self.d_y.ref[rows, :].astype(BF))
            self.split(self.k_h, rows, self.k_rot.ref[rows, :])
            self.split(self.v_h, rows, proj[rows, q_cols + k_cols :].astype(BF))

        self.blocks(prepare)
        dk_h[...] = jnp.zeros_like(dk_h)
        dv_h[...] = jnp.zeros_like(dv_h)

        def head(h, carry):
            g = h // self.share
            for i in range(self.length // ROW_BLOCK):
                rows, seen = pl.ds(i * ROW_BLOCK, ROW_BLOCK), pl.ds(0, (i + 1) * ROW_BLOCK)
                q, low = self.q_h.ref[h, rows, :], self.dy_h.ref[h, rows, :]
                k = self.k_h.ref[g, seen, :]
                prob = block_weights(q, k, i * ROW_BLOCK)
                d_weights = contract(low, self.v_h.ref[g, seen, :], 1, 1)
                dv_h[g, seen, :] += contract(prob.astype(BF), low, 0, 0)
                inner = jnp.sum(prob * d_weights, axis=1, keepdims=True)
                d_scores = (prob * (d_weights - inner)).astype(BF)
                dq_h[h, rows, :] = contract(d_scores, k, 1, 0) * scale
                dk_h[g, seen, :] += contract(d_scores, q, 0, 0) * scale
            return carry

        lax.fori_loop(0, self.heads, head, 0)
        self.q_gain.ref[...] = jnp.zeros_like(self.q_gain.ref)
        self.k_gain.ref[...] = jnp.zeros_like(self.k_gain.ref)

        def finish(rows):
            c, n = self.cos.ref[rows, :], self.sin.ref[rows, :]
            dq, dk, dv = (self.join(v, rows) for v in (self.dq_h, self.dk_h, self.dv_h))
            dq = dq * c + turn(dq * n, size, True)
            dk = dk * c[:, :k_cols] + turn(dk * n[:, :k_cols], size, True)
            dq, q_sum = head_norm_back(proj[rows, :q_cols], self.gain.ref[0:1, :], dq, size)
            dk, k_sum = head_norm_back(
                proj[rows, q_cols : q_cols + k_cols], self.gain.ref[1:2, :k_cols], dk, size
            )
            self.q_gain.ref[...] += q_sum
            self.k_gain.ref[...] += k_sum
            self.d_proj.ref[rows, :q_cols] = dq.astype(BF)
            self.d_proj.ref[rows, q_cols : q_cols + k_cols] = dk.astype(BF)
            self.d_proj.ref[rows, q_cols + k_cols :] = dv.astype(BF)

        self.blocks(finish)


def body(boundary, norm_gain, mix_in, mix_out, w_gate, w_up, w_down, conv_x, conv_kernel, qk_gain):
    first = lax.axis_index("section") == 0
    tensor_index = lax.axis_index("tensor")
    model_width = boundary.shape[3]
    channels = mix_out.shape[1]
    row_shape = boundary.shape[2:]
    length, size = 4 * row_shape[0], qk_gain.shape[1]

    seqs, own_gain = boundary[0], norm_gain[0]
    sh_in, sh_out, sh_gate, sh_up, sh_down = (v[0] for v in (mix_in, mix_out, w_gate, w_up, w_down))
    cosine_table, sine_table = rotation(length, size)
    heads = channels // size
    table_arrays = [jnp.tile(v, (1, heads)) for v in (qk_gain, cosine_table, sine_table)]

    def gains_of(k, block, other, early=True):
        own, moved = k.input(own_gain), as_val(k, other)
        sources = lambda s, d, t: [(s == block, own.ref), (s == 1 - block, moved.ref)]
        return Load(k, sources, own.shape, F32, early)

    def start_rows(k, slot, other, early=True):
        own, moved = k.input(seqs), as_val(k, other)
        sources = lambda s, d, t: [(s == slot, own.ref.at[slot]), (s == 1 - slot, moved.ref)]
        return Load(k, sources, row_shape, BF, early)

    def wait(*items):
        return [item.wait for item in items]

    k = Kernel(0)
    t_seq = None
    seq_val = k.input(seqs)

    def seq_moves(s, d, t):
        return [([(None, seq_val.ref.at[1 - s])], t_seq.out.ref, {"section": 1 - s})], []

    t_in, t_out, t_gate, t_up, t_down = (
        x_half(k, v) for v in (sh_in, sh_out, sh_gate, sh_up, sh_down)
    )
    t_seq = Task(k, row_shape, "section", seq_moves, 1)
    t_gain, z_cols = x_move(k, own_gain), z_gather(k, conv_x)
    z_in0, z_out0 = z_gather_half(k, sh_in, t_in.out, 0), z_gather_half(k, sh_out, t_out.out, 0)
    z_gate0, z_up0 = z_gather_half(k, sh_gate, t_gate.out, 0), z_gather_half(k, sh_up, t_up.out, 0)
    x_cols, x_in0, x_out0, x_gate0 = (x_move(k, v.out) for v in (z_cols, z_in0, z_out0, z_gate0))
    x_load, gain_load = start_rows(k, 0, t_seq.out, False), gains_of(k, 0, t_gain.out, False)
    taps = load_all(k, conv_kernel)
    w_in0, w_cols = Weight(k, "rows", z_in0.out, x_in0.out), Weight(k, "conv", z_cols.out, x_cols.out)
    w_out0 = Weight(k, "cols", z_out0.out, x_out0.out)
    g0 = Gather(k, x_load.buf, (gain_load.buf, 0), [w_in0, w_cols], save=(0, 1, 2))
    conv = Conv(k, g0.values[0], g0.values[1], taps.buf)
    y0 = Save(k, conv.y)
    s1 = Scatter(k, [conv.y], [w_out0], x_load.buf)
    mid0 = Save(k, s1.out)
    k.do(t_in.send, t_out.send, z_cols.send, t_gate.send, t_gain.send, t_seq.send)
    k.do(t_in.wait, z_in0.send, t_out.wait, z_out0.send, t_up.send)
    k.do(t_gain.wait, gain_load.start, t_seq.wait, x_load.start)
    k.do(gain_load.wait, x_load.wait, g0.begin)
    k.do(t_gate.wait, z_gate0.send)
    k.do(z_cols.wait, x_cols.send, z_in0.wait, x_in0.send, z_out0.wait, x_out0.send, t_down.send)
    k.do(t_up.wait, z_up0.send)
    k.do(x_cols.wait, w_cols.start, x_in0.wait, w_in0.start)
    k.do(z_gate0.wait, x_gate0.send)
    k.do(g0.loop, taps.wait, conv.run, y0.start)
    k.do(x_out0.wait, w_out0.start, s1.loop, s1.finish, mid0.start)
    k.do(*wait(t_down, x_gate0, z_up0))
    k.build()
    a0, proj0, value0 = (out for _, out, _ in g0.saved)
    y0, mid0 = y0.out, mid0.out

    k = Kernel(1)
    x_up0, z_down0 = x_move(k, z_up0.out), z_gather_half(k, sh_down, t_down.out, 0)
    z_in1, z_out1 = z_gather_half(k, sh_in, t_in.out, 1), z_gather_half(k, sh_out, t_out.out, 1)
    z_gate1 = z_gather_half(k, sh_gate, t_gate.out, 1)
    x_down0, x_in1, x_out1 = (x_move(k, v.out) for v in (z_down0, z_in1, z_out1))
    rows, gain_load = load_all(k, mid0), gains_of(k, 0, t_gain.out)
    w_gate0 = Weight(k, "rows", z_gate0.out, x_gate0.out, True)
    w_up0 = Weight(k, "rows", z_up0.out, x_up0.out)
    w_down0 = Weight(k, "cols", z_down0.out, x_down0.out)
    g2 = Gather(
        k, rows.buf, (gain_load.buf, 1), [w_gate0, w_up0], epilogue="ffn", save=(0, 1, 2, 3)
    )
    s3 = Scatter(k, [g2.values[2]], [w_down0], rows.buf, low=True)
    z_rows = Save(k, s3.out)
    k.do(x_up0.send, z_down0.send, z_in1.send, z_out1.send, z_gate1.send)
    k.do(rows.wait, gain_load.wait, g2.begin)
    k.do(z_down0.wait, x_down0.send, x_up0.wait, w_up0.start, g2.loop)
    k.do(z_in1.wait, x_in1.send, z_out1.wait, x_out1.send)
    k.do(x_down0.wait, w_down0.start, s3.loop, s3.finish, z_rows.start)
    k.do(*wait(x_in1, x_out1, z_gate1))
    k.build()
    m0, gate0, up0, hid0 = (out for _, out, _ in g2.saved)
    z_rows = z_rows.out

    k = Kernel(2)
    x_gate1, z_up1 = x_move(k, z_gate1.out), z_gather_half(k, sh_up, t_up.out, 1)
    z_down1, x_up1 = z_gather_half(k, sh_down, t_down.out, 1), x_move(k, z_up1.out)
    rows, gain_load = load_all(k, z_rows), gains_of(k, 1, t_gain.out)
    tables = [load_all(k, v) for v in table_arrays]
    w_in1 = Weight(k, "rows", z_in1.out, x_in1.out, True)
    w_out1 = Weight(k, "cols", z_out1.out, x_out1.out, True)
    g4 = Gather(k, rows.buf, (gain_load.buf, 0), [w_in1], save=(0, 1))
    attend = Attend(k, g4.values[0], tables, size)
    kept = [Save(k, v) for v in (attend.q_rot, attend.k_rot, attend.y)]
    s5 = Scatter(k, [attend.y], [w_out1], rows.buf)
    mid1 = Save(k, s5.out)
    k.do(x_gate1.send, z_up1.send, z_down1.send)
    k.do(rows.wait, gain_load.wait, g4.begin, g4.loop)
    k.do(lambda: attend.run(z_up1.wait, x_up1.send))
    k.do(*(v.start for v in kept))
    k.do(s5.loop, s5.finish, mid1.start)
    k.do(*wait(x_gate1, x_up1, z_down1))
    k.build()
    a1, proj1 = (out for _, out, _ in g4.saved)
    q_rot, k_rot, y1 = (v.out for v in kept)
    mid1 = mid1.out

    k = Kernel(3)
    x_down1 = x_move(k, z_down1.out)
    rows, gain_load = load_all(k, mid1), gains_of(k, 1, t_gain.out)
    cot = start_rows(k, 1, t_seq.out)
    w_gate1 = Weight(k, "rows", z_gate1.out, x_gate1.out, True)
    w_up1 = Weight(k, "rows", z_up1.out, x_up1.out, True)
    w_down1 = Weight(k, "cols", z_down1.out, x_down1.out)
    g6 = Gather(k, rows.buf, (gain_load.buf, 1), [w_gate1, w_up1], epilogue="ffn")
    g8 = Gather(
        k, cot.buf, None, [w_down1], [g6.values[0], g6.values[1]], trans=True, epilogue="ffn_back"
    )
    p_down1 = Product(k, g6.values[2], g8.full)
    p_gate1, p_up1 = Product(k, g6.full, g8.values[0]), Product(k, g6.full, g8.values[1])
    r_down1 = x_half(k, p_down1.out)
    s7 = Scatter(k, [g6.values[2]], [w_down1], rows.buf, low=True)
    s9 = Scatter(k, g8.values, [w_gate1, w_up1], cot.buf, (rows.buf, (gain_load.buf, 1)), True)
    y_rows, d_mid1, gain11 = Save(k, s7.out), Save(k, s9.out), Save(k, s9.gain_grad)
    k.do(x_down1.send, rows.wait, gain_load.wait, g6.begin, cot.wait, g8.begin, g6.loop)
    k.do(x_down1.wait, w_down1.start, g8.loop, p_down1.run, p_down1.wait, r_down1.send)
    k.do(s9.loop, p_gate1.run, p_up1.run, s9.finish, d_mid1.start, gain11.start)
    k.do(s7.loop, s7.finish, y_rows.start, p_gate1.wait, p_up1.wait)
    k.do(*wait(r_down1))
    k.build()
    y_rows, d_mid1, gain11 = y_rows.out, d_mid1.out, gain11.out

    k = Kernel(4)
    q_down1 = SumScatter(k, "cols", p_down1.out, r_down1.out)
    r_gate1, r_up1 = x_slots(k, p_gate1.out, "rows"), x_slots(k, p_up1.out, "rows")
    q_gate1 = SumScatter(k, "rows", p_gate1.out, r_gate1.out)
    rows, gain_load = load_all(k, d_mid1), gains_of(k, 1, t_gain.out)
    value = load_all(k, z_rows)
    tables = [load_all(k, v) for v in table_arrays]
    proj, q_load, k_load, y_load, a_load = (load_all(k, v) for v in (proj1, q_rot, k_rot, y1, a1))
    w_in1 = Weight(k, "rows", z_in1.out, x_in1.out, True)
    w_out1 = Weight(k, "cols", z_out1.out, x_out1.out, True)
    g10 = Gather(k, rows.buf, None, [w_out1], trans=True)
    p_out1 = Product(k, y_load.buf, g10.full)
    back = AttendBack(k, proj.buf, tables, size, q_load.buf, k_load.buf, g10.values[0])
    p_in1 = Product(k, a_load.buf, back.d_proj)
    r_out1 = x_half(k, p_out1.out)
    s11 = Scatter(
        k, [back.d_proj], [w_in1], rows.buf, (value.buf, (gain_load.buf, 0)), True, low=True
    )
    d_z, gain10 = Save(k, s11.out), Save(k, s11.gain_grad)
    head_gains = [Save(k, back.q_gain), Save(k, back.k_gain)]
    k.early.append(q_down1.load)
    k.do(r_gate1.send, r_up1.send, rows.wait, g10.begin, q_down1.send, g10.loop)
    k.do(y_load.wait, p_out1.run, p_out1.wait, r_out1.send)
    k.do(r_gate1.wait, q_gate1.add)
    k.do(proj.wait, q_load.wait, k_load.wait, back.run, *(v.start for v in head_gains))
    k.do(gain_load.wait, value.wait, s11.loop, a_load.wait, p_in1.run)
    k.do(s11.finish, d_z.start, gain10.start, p_in1.wait)
    k.do(*wait(q_down1, q_gate1, r_up1, r_out1))
    k.build()
    d_z, gain10 = d_z.out, gain10.out
    q_gain, k_gain = (v.out.array for v in head_gains)

    k = Kernel(5)
    q_up1 = SumScatter(k, "rows", p_up1.out, r_up1.out)
    q_out1 = SumScatter(k, "cols", p_out1.out, r_out1.out)
    r_in1 = x_slots(k, p_in1.out, "rows")
    q_in1 = SumScatter(k, "rows", p_in1.out, r_in1.out)
    e_down1, e_gate1 = Finish(k, q_down1.out, 1), Finish(k, q_gate1.out, 1)
    rows, value, gain_load = load_all(k, d_z), load_all(k, mid0), gains_of(k, 0, t_gain.out)
    gate_load, up_load, hid_load, m_load = (load_all(k, v) for v in (gate0, up0, hid0, m0))
    w_gate0 = Weight(k, "rows", z_gate0.out, x_gate0.out, True)
    w_up0 = Weight(k, "rows", z_up0.out, x_up0.out, True)
    w_down0 = Weight(k, "cols", z_down0.out, x_down0.out, True)
    g12 = Gather(
        k, rows.buf, None, [w_down0], [gate_load.buf, up_load.buf], trans=True, epilogue="ffn_back"
    )
    p_down0 = Product(k, hid_load.buf, g12.full)
    p_gate0, p_up0 = Product(k, m_load.buf, g12.values[0]), Product(k, m_load.buf, g12.values[1])
    r_down0 = x_half(k, p_down0.out)
    s13 = Scatter(
        k, g12.values, [w_gate0, w_up0], rows.buf, (value.buf, (gain_load.buf, 1)), True
    )
    d_mid0, gain01 = Save(k, s13.out), Save(k, s13.gain_grad)
    k.early += [q_up1.load, q_out1.load, e_down1.load, e_gate1.load]
    k.do(r_in1.send, rows.wait, g12.begin, q_up1.send, q_out1.send, e_down1.send, e_gate1.send)
    k.do(gate_load.wait, up_load.wait, g12.loop)
    k.do(hid_load.wait, p_down0.run, p_down0.wait, r_down0.send)
    k.do(r_in1.wait, q_in1.add)
    k.do(s13.loop, m_load.wait, p_gate0.run, p_up0.run)
    k.do(value.wait, gain_load.wait, s13.finish, d_mid0.start, gain01.start)
    k.do(p_gate0.wait, p_up0.wait)
    k.do(*wait(q_up1, q_out1, q_in1, e_down1, e_gate1, r_down0))
    k.build()
    d_mid0, gain01 = d_mid0.out, gain01.out

    k = Kernel(6)
    r_gate0, r_up0 = x_slots(k, p_gate0.out, "rows"), x_slots(k, p_up0.out, "rows")
    q_down0 = SumScatter(k, "cols", p_down0.out, r_down0.out)
    q_gate0 = SumScatter(k, "rows", p_gate0.out, r_gate0.out)
    q_up0 = SumScatter(k, "rows", p_up0.out, r_up0.out)
    e_up1, e_out1, e_in1 = (Finish(k, v.out, 1) for v in (q_up1, q_out1, q_in1))
    rows, gain_load = load_all(k, d_mid0), gains_of(k, 0, t_gain.out)
    x_load, taps = start_rows(k, 0, t_seq.out), load_all(k, conv_kernel)
    y_load, a_load, proj, value = (load_all(k, v) for v in (y0, a0, proj0, value0))
    w_in0 = Weight(k, "rows", z_in0.out, x_in0.out, True)
    w_cols = Weight(k, "conv", z_cols.out, x_cols.out, True)
    w_out0 = Weight(k, "cols", z_out0.out, x_out0.out, True)
    g14 = Gather(k, rows.buf, None, [w_out0], trans=True)
    p_out0 = Product(k, y_load.buf, g14.full)
    back = ConvBack(k, proj.buf, value.buf, taps.buf, g14.values[0])
    p_in0, p_cols = Product(k, a_load.buf, back.d_proj), Product(k, a_load.buf, back.d_value)
    r_out0, r_in0 = x_half(k, p_out0.out), x_slots(k, p_in0.out, "rows")
    r_cols = x_slots(k, p_cols.out, "conv")
    q_out0, q_in0 = SumScatter(k, "cols", p_out0.out, r_out0.out), SumScatter(k, "rows", p_in0.out, r_in0.out)
    q_cols = SumScatter(k, "conv", p_cols.out, r_cols.out)
    e_down0, e_gate0, e_up0, e_out0, e_in0 = (
        Finish(k, v.out, 0) for v in (q_down0, q_gate0, q_up0, q_out0, q_in0)
    )
    s15 = Scatter(
        k, [back.d_proj, back.d_value], [w_in0, w_cols], rows.buf,
        (x_load.buf, (gain_load.buf, 0)), True, low=True,
    )
    d_x = Save(k, s15.out)
    tap_rows = conv_kernel.shape[0]
    small = k.vmem((8, model_width), F32)
    small_out = Save(k, small)
    ready = [load_all(k, v) for v in (gain01, gain10, gain11)]
    head_row = jnp.pad(
        jnp.stack([jnp.sum(v.reshape(-1, size), axis=0) for v in (q_gain, k_gain)]).reshape(1, -1),
        ((0, 0), (0, model_width - 2 * size)),
    )
    head_load = load_all(k, head_row)

    def fill_small():
        t = lax.axis_index("tensor")
        small.ref[...] = jnp.zeros_like(small.ref)
        small.ref[0:1, :] = s15.gain_grad.ref[...]
        for i, load in enumerate(ready):
            load.wait()
            small.ref[i + 1 : i + 2, :] = load.buf.ref[...]
        small.ref[4 : 4 + tap_rows, block_of(t, channels)] = back.d_kernel.ref[...]
        head_load.wait()
        small.ref[7:8, :] = head_load.buf.ref[...]
        small_out.start()

    t_small = x_move(k, small_out.out)
    z_small = SumShare(k, [small_out.out, t_small.out], "dp")
    t_total = SumShare(k, [z_small.out], "tensor", slotted=True)
    y_val, dx_val = k.input(y_rows), d_x.out

    def result_moves(s, d, t):
        sources = [(s == 0, y_val.ref), (s == 1, dx_val.ref)]
        return [(sources, t_result.out.ref, {"section": 1 - s})], []

    t_result = Task(k, row_shape, "section", result_moves, 1)
    k.early += [q_down0.load, e_up1.load, e_out1.load, e_in1.load]
    k.do(r_gate0.send, r_up0.send, rows.wait, g14.begin, q_down0.send)
    k.do(e_up1.send, e_out1.send, e_in1.send, g14.loop)
    k.do(y_load.wait, p_out0.run, p_out0.wait, r_out0.send)
    k.do(proj.wait, value.wait, taps.wait, back.run, a_load.wait)
    k.do(p_in0.run, p_cols.run, p_in0.wait, r_in0.send, p_cols.wait, r_cols.send)
    k.do(r_gate0.wait, q_gate0.add)
    k.do(x_load.wait, gain_load.wait, s15.loop, s15.finish, d_x.start)
    k.do(fill_small, d_x.wait, t_result.send)
    k.do(small_out.wait, t_small.send)
    k.do(r_up0.wait, q_up0.add)
    k.do(r_out0.wait, q_out0.add, r_in0.wait, q_in0.add, r_cols.wait, q_cols.add)
    k.do(q_down0.wait, e_down0.add, t_small.wait, z_small.add, q_gate0.wait, e_gate0.add)
    k.do(z_small.wait, t_total.add)
    k.do(q_up0.wait, e_up0.add, q_out0.wait, e_out0.add, q_in0.wait, e_in0.add)
    rest = (e_up1, e_out1, e_in1, q_cols, e_down0, e_gate0, e_up0, e_out0, e_in0)
    k.do(*wait(*rest, t_total, t_result))
    k.build()

    def whole(zero, one):
        kept = jnp.where(first, zero.out.array, one.out.array)
        return kept.reshape(1, -1, kept.shape[-1]).astype(F32)

    d_x, y_rows, moved = d_x.out.array, y_rows.array, t_result.out.array
    result = jnp.where(first, jnp.stack([d_x, moved]), jnp.stack([moved, y_rows]))
    small = jnp.sum(t_total.out.array, axis=0)
    gains_total = small[:4].reshape(2, 2, model_width)
    gain_out = lax.dynamic_slice_in_dim(gains_total, lax.axis_index("section"), 1, 0)
    kernel_out = lax.dynamic_slice_in_dim(
        small[4 : 4 + tap_rows], tensor_index * channels, channels, 1
    )
    head_total = small[7, : qk_gain.size].reshape(qk_gain.shape)
    return (
        result[None],
        gain_out,
        whole(e_in0, e_in1),
        whole(e_out0, e_out1),
        whole(e_gate0, e_gate1),
        whole(e_up0, e_up1),
        whole(e_down0, e_down1),
        jnp.sum(q_cols.out.array.astype(F32), axis=0),
        kernel_out,
        head_total,
    )


def solution(mesh):
    in_specs = (
        P("section", "dp", "tensor", None),
        P("section", None, None),
        P("section", "dp", "tensor"),
        P("section", "tensor", "dp"),
        P("section", "dp", "tensor"),
        P("section", "dp", "tensor"),
        P("section", "tensor", "dp"),
        P(("section", "dp"), "tensor"),
        P(None, "tensor"),
        P(),
    )
    out_specs = (
        P("section", "dp", "tensor", None),
        P("section", None, None),
        P("section", "dp", "tensor"),
        P("section", "tensor", "dp"),
        P("section", "dp", "tensor"),
        P("section", "dp", "tensor"),
        P("section", "tensor", "dp"),
        P(("section", "dp"), "tensor"),
        P(None, "tensor"),
        P(),
    )
    return jax.shard_map(body, mesh=mesh, in_specs=in_specs, out_specs=out_specs, check_vma=False)
```

```python
import functools

import jax
import jax.numpy as jnp
from jax import lax
from jax.experimental import pallas as pl
from jax.experimental.pallas import tpu as pltpu
from jax.sharding import PartitionSpec as P

HEADS = 16
KV_HEADS = 8

EPS = 1e-05
ROPE_BASE = 1000000.0
MASKED = -1e30

MESH = pl.DeviceIdType.MESH
ANY = pl.BlockSpec(memory_space=pl.ANY)
DMA = pltpu.SemaphoreType.DMA
VMEM_BYTES = 63 * 1024 * 1024
BF = jnp.bfloat16
F32 = jnp.float32
ROW_BLOCK = 256


def contract(left_op, right_op, left_dim, right_dim):
    return lax.dot_general(
        left_op, right_op, (((left_dim,), (right_dim,)), ((), ())), preferred_element_type=F32
    )


def norm_rows(values, gain):
    return values * lax.rsqrt(jnp.mean(values * values, axis=-1, keepdims=True) + EPS) * gain


def norm_back(values, gain, grad_in):
    row_scale = lax.rsqrt(jnp.mean(values * values, axis=-1, keepdims=True) + EPS)
    normed = values * row_scale
    gain_grad = jnp.sum(grad_in * normed, axis=0, keepdims=True)
    scaled = grad_in * gain
    value_grad = row_scale * (scaled - normed * jnp.mean(scaled * normed, axis=-1, keepdims=True))
    return (value_grad, gain_grad)


def rotation(length, head_size):
    half_size = head_size // 2
    frequency = ROPE_BASE ** (-(jnp.arange(half_size, dtype=jnp.float32) * 2.0 / head_size))
    angles = jnp.arange(length, dtype=jnp.float32)[:, None] * frequency[None, :]
    cosine_table = jnp.concatenate([jnp.cos(angles), jnp.cos(angles)], axis=1)
    sine_table = jnp.concatenate([jnp.sin(angles), jnp.sin(angles)], axis=1)
    return (cosine_table, sine_table)


def silu_parts(gate):
    sig = 1.0 / (1.0 + jnp.exp(-gate))
    return sig, gate * sig


def dp_size():
    return lax.axis_size("dp")


def spot():
    return tuple(lax.axis_index(a) for a in ("section", "dp", "tensor"))


def block_of(index, size):
    return pl.ds(pl.multiple_of(index * size, size), size)


class Val:
    def __init__(self, shape, dtype):
        self.shape, self.dtype = tuple(shape), dtype
        self.ref = self.array = None


class Kernel:
    def __init__(self, cid):
        self.cid, self.ins, self.arrays, self.outs, self.room = cid, [], [], [], []
        self.early, self.steps, self.late, self.axes = [], [], [], {"tensor"}
        self.once = []

    def input(self, array):
        array = array.array if isinstance(array, Val) else array
        for val, known in zip(self.ins, self.arrays):
            if known is array:
                return val
        val = Val(array.shape, array.dtype)
        self.ins.append(val)
        self.arrays.append(array)
        return val

    def output(self, shape, dtype):
        val = Val(shape, dtype)
        self.outs.append(val)
        return val

    def vmem(self, shape, dtype):
        val = Val(shape, dtype)
        self.room.append((val, pltpu.VMEM(tuple(shape), dtype)))
        return val

    def sem(self, *shape):
        val = Val(shape, None)
        self.room.append((val, DMA(shape)))
        return val

    def do(self, *steps):
        self.steps += steps

    def body(self, *refs):
        vals = self.ins + self.outs + [val for val, _ in self.room]
        for val, ref in zip(vals, refs):
            val.ref = ref
        for item in self.once:
            item.waited = False
            item.phase = 0
        for step in self.early:
            step()
        self.greet()
        for step in self.steps + self.late:
            step()

    def greet(self):
        s, d, t = spot()
        peers = []
        if "section" in self.axes:
            peers.append({"section": 1 - s})
        if "dp" in self.axes:
            peers += [{"dp": (d + k) % dp_size()} for k in range(1, dp_size())]
        peers += [{"tensor": (t + k) % 4} for k in range(1, 4)]
        barrier = pltpu.get_barrier_semaphore()
        for peer in peers:
            pl.semaphore_signal(barrier, inc=1, device_id=peer, device_id_type=MESH)
        pl.semaphore_wait(barrier, len(peers))

    def build(self):
        result = pl.pallas_call(
            self.body,
            out_shape=[jax.ShapeDtypeStruct(v.shape, v.dtype) for v in self.outs],
            in_specs=[ANY] * len(self.ins),
            out_specs=[ANY] * len(self.outs),
            scratch_shapes=[room for _, room in self.room],
            compiler_params=pltpu.CompilerParams(
                collective_id=self.cid, has_side_effects=True, vmem_limit_bytes=VMEM_BYTES
            ),
            name=f"stage{self.cid}",
        )(*self.arrays)
        for val, array in zip(self.outs, result):
            val.array = array


def remote(src, dst, send_sem, recv_sem, peer):
    return pltpu.make_async_remote_copy(
        src_ref=src, dst_ref=dst, send_sem=send_sem, recv_sem=recv_sem,
        device_id=peer, device_id_type=MESH,
    )


class Load:
    def __init__(self, k, sources, shape, dtype, early=False):
        self.k, self.sources, self.waited = k, sources, False
        self.buf, self.sem = k.vmem(shape, dtype), k.sem(1)
        k.once.append(self)
        if early:
            k.early.append(self.start)

    def moves(self):
        for cond, source in self.sources(*spot()):
            yield cond, pltpu.make_async_copy(source, self.buf.ref, self.sem.ref.at[0])

    def start(self):
        for cond, move in self.moves():
            if cond is None:
                move.start()
            else:
                pl.when(cond)(move.start)

    def wait(self):
        if not self.waited:
            self.waited = True
            next(self.moves())[1].wait()


def load_all(k, array, early=True):
    val = k.input(array)
    return Load(k, lambda s, d, t: [(None, val.ref)], val.shape, val.dtype, early)


class Save:
    def __init__(self, k, buf):
        self.buf, self.out, self.sem = buf, k.output(buf.shape, buf.dtype), k.sem(1)
        self.waited = False
        k.once.append(self)
        k.late.append(self.wait)

    def move(self):
        return pltpu.make_async_copy(self.buf.ref, self.out.ref, self.sem.ref.at[0])

    def start(self):
        self.move().start()

    def wait(self):
        if not self.waited:
            self.waited = True
            self.move().wait()


class Task:
    final = None

    def __init__(self, k, out, axis, moves, count, n_local=1, out_dtype=BF):
        self.k, self.axis, self.make = k, axis, moves
        self.out = k.output(out, out_dtype)
        self.send_sem, self.recv_sem, self.local_sem = k.sem(count), k.sem(count), k.sem(n_local)
        self.waited = False
        k.axes.add(axis)
        k.once.append(self)

    def local(self, src, dst, i):
        return pltpu.make_async_copy(src, dst, self.local_sem.ref.at[i])

    def pairs(self, every):
        far, near = self.make(*spot())
        for i, (sources, dst, peer) in enumerate(far):
            for cond, src in sources if every else sources[:1]:
                yield cond, True, remote(
                    src, dst, self.send_sem.ref.at[i], self.recv_sem.ref.at[i], peer
                )
        for i, (sources, dst) in enumerate(near):
            for cond, src in sources if every else sources[:1]:
                yield cond, False, self.local(src, dst, i)

    def step(self):
        pass

    def send(self):
        for cond, far, move in self.pairs(True):
            if far and self.final is not None:
                cond = lax.axis_index("section") == 1 - self.final
            if cond is None:
                move.start()
            else:
                pl.when(cond)(move.start)

    def wait(self):
        if self.waited:
            return
        self.waited = True
        s = lax.axis_index("section")
        for _, far, move in self.pairs(False):
            if not far:
                move.wait()
            elif self.final is None:
                move.wait_recv()
                move.wait_send()
            else:
                pl.when(s == 1 - self.final)(move.wait_send)
                pl.when(s == self.final)(move.wait_recv)


def as_val(k, value):
    value = value.out if isinstance(value, Task) else value
    known = isinstance(value, Val) and (value.array is None)
    return value if known else k.input(value)


class Line(Task):
    def __init__(self, k, out, out_dtype=BF, n_local=1):
        super().__init__(k, out, "dp", None, 6, n_local, out_dtype)
        self.send_sem, self.recv_sem = k.sem(2, 3), k.sem(2, 3)
        self.phase = 0

    def hop(self, j, way, src, dst):
        d = lax.axis_index("dp")
        peer = {"dp": (d + 1 if way == 0 else d + 3) % 4}
        return remote(src, dst, self.send_sem.ref.at[way, j], self.recv_sem.ref.at[way, j], peer)


class LineGather(Line):
    def __init__(self, k, sources, shape, dtype):
        super().__init__(k, (4,) + shape, dtype)
        self.sources = sources

    def ends(self, j, way):
        d = lax.axis_index("dp")
        if way == 0:
            return (d >= j) & (d < 3), d >= j + 1
        return (d <= 3 - j) & (d > 0), d <= 2 - j

    def copy(self, j, way, src=None):
        d = lax.axis_index("dp")
        slot = (d + 4 - j if way == 0 else d + j) % 4
        piece = self.out.ref.at[slot]
        return self.hop(j, way, piece if src is None else src, piece)

    def send(self):
        self.phase = 0
        for cond, src in self.sources(*spot()):
            own = self.local(src, self.out.ref.at[lax.axis_index("dp")], 0)
            moves = [(True if cond is None else cond, own)]
            for way in range(2):
                sends = self.ends(0, way)[0]
                moves.append((sends if cond is None else sends & cond, self.copy(0, way, src)))
            for when, move in moves:
                if when is True:
                    move.start()
                else:
                    pl.when(when)(move.start)

    def arrive(self, j):
        for way in range(2):
            pl.when(self.ends(j, way)[1])(self.copy(j, way).wait_recv)

    def step(self):
        self.arrive(self.phase)
        self.phase += 1
        for way in range(2):
            pl.when(self.ends(self.phase, way)[0])(self.copy(self.phase, way).start)

    def wait(self):
        if self.waited:
            return
        self.waited = True
        while self.phase < 2:
            self.step()
        self.arrive(2)
        for j in range(3):
            for way in range(2):
                pl.when(self.ends(j, way)[0])(self.copy(j, way).wait_send)
        d = lax.axis_index("dp")
        self.local(self.sources(*spot())[0][1], self.out.ref.at[d], 0).wait()


def z_gather_from(k, sources, shape, dtype):
    count = dp_size()
    if count == 4:
        return LineGather(k, sources, shape, dtype)

    def moves(s, d, t):
        dst, found = task.out.ref.at[d], sources(s, d, t)
        return [(found, dst, {"dp": (d + i) % count}) for i in range(1, count)], [(found, dst)]

    task = Task(k, (count,) + shape, "dp", moves, count - 1, out_dtype=dtype)
    return task


def z_gather(k, value):
    val = as_val(k, value)
    return z_gather_from(k, lambda s, d, t: [(None, val.ref)], val.shape, val.dtype)


def z_gather_half(k, shard, moved, block):
    shard, moved = as_val(k, shard), as_val(k, moved)
    rows = shard.shape[0] // 2

    def sources(s, d, t):
        own = shard.ref.at[pl.ds(block * rows, rows)]
        return [(s == block, own), (s == 1 - block, moved.ref)]

    return z_gather_from(k, sources, moved.shape, shard.dtype)


def x_move(k, value):
    val = as_val(k, value)

    def moves(s, d, t):
        return [([(None, val.ref)], task.out.ref, {"section": 1 - s})], []

    task = Task(k, val.shape, "section", moves, 1, out_dtype=val.dtype)
    return task


def x_half(k, value):
    val = as_val(k, value)
    rows = val.shape[0] // 2

    def moves(s, d, t):
        src = val.ref.at[block_of(1 - s, rows)]
        return [([(None, src)], task.out.ref, {"section": 1 - s})], []

    task = Task(k, (rows,) + val.shape[1:], "section", moves, 1, out_dtype=val.dtype)
    return task


def x_slots(k, value, kind):
    val, count = as_val(k, value), dp_size()
    rows = val.shape[0] // (2 * count)

    def moves(s, d, t):
        far = []
        for i in range(count):
            slot = 2 * i + 1 - s if kind == "rows" else (1 - s) * count + i
            src = val.ref.at[block_of(slot, rows)]
            far.append(([(None, src)], task.out.ref.at[i], {"section": 1 - s}))
        return far, []

    task = Task(k, (count, rows) + val.shape[1:], "section", moves, count)
    return task


class Terms:
    def __init__(self, k, kind, grads, received, local):
        self.grads, self.received, self.local = as_val(k, grads), as_val(k, received), local
        self.kind, self.n = kind, dp_size()
        if kind == "cols":
            self.rows, self.cols = self.grads.shape[0] // 2, self.grads.shape[1] // self.n
            held = (self.rows, self.grads.shape[1])
        else:
            self.rows, self.cols = self.grads.shape[0] // (2 * self.n), self.grads.shape[1]
            held = (self.n, self.rows, self.cols)
        self.kept, self.got = k.vmem(held, BF), k.vmem(held, BF)
        self.shape = (self.n, self.rows, self.cols)
        self.total = k.vmem(self.shape, BF) if kind == "cols" else self.kept

    def loads(self):
        s, grads, kept = lax.axis_index("section"), self.grads.ref, self.kept.ref
        if self.kind == "cols":
            moves = [self.local(grads.at[block_of(s, self.rows)], kept, 2)]
        else:
            moves = []
            for i in range(self.n):
                slot = 2 * i + s if self.kind == "rows" else s * self.n + i
                moves.append(self.local(grads.at[block_of(slot, self.rows)], kept.at[i], 2 + i))
        return moves + [self.local(self.received.ref, self.got.ref, 1)]

    def load(self):
        for move in self.loads():
            move.start()

    def add(self):
        for move in self.loads():
            move.wait()
        kept, got, total = self.kept.ref, self.got.ref, self.total.ref
        for i in range(self.n):
            if self.kind == "cols":
                part = (slice(None), slice(i * self.cols, (i + 1) * self.cols))
            else:
                part = i
            total[i] = (kept[part].astype(F32) + got[part].astype(F32)).astype(BF)


class DirectScatter(Task):
    def __init__(self, k, kind, grads, received):
        self.terms = Terms(k, kind, grads, received, lambda *a: self.local(*a))
        count = dp_size()

        def moves(s, d, t):
            total = self.terms.total.ref
            far = []
            for i in range(1, count):
                other = (d + i) % count
                far.append(([(None, total.at[other])], self.out.ref.at[d], {"dp": other}))
            return far, [([(None, total.at[d])], self.out.ref.at[d])]

        super().__init__(k, self.terms.shape, "dp", moves, count - 1, 2 + count)
        self.load = self.terms.load

    def send(self):
        self.terms.add()
        super().send()

    def add(self):
        self.load()
        self.send()


class LineScatter(Line):
    def __init__(self, k, kind, grads, received):
        self.terms = Terms(k, kind, grads, received, lambda *a: self.local(*a))
        super().__init__(k, self.terms.shape[1:], BF, 6)
        self.got = k.vmem((2, 3) + self.terms.shape[1:], BF)
        self.load = self.terms.load

    def ends(self, j, way):
        d = lax.axis_index("dp")
        if way == 0:
            return (d <= j) & (d < 3), (d >= 1) & (d <= j + 1)
        return (d >= 3 - j) & (d > 0), (d <= 2) & (d >= 2 - j)

    def copy(self, j, way):
        d = lax.axis_index("dp")
        to = (d + 3 - j if way == 0 else d + 1 + j) % 4
        return self.hop(j, way, self.terms.total.ref.at[to], self.got.ref.at[way, j])

    def send(self):
        self.phase = 0
        self.terms.add()
        for way in range(2):
            pl.when(self.ends(0, way)[0])(self.copy(0, way).start)

    def take(self, j, way):
        d = lax.axis_index("dp")
        to = (d + 2 - j if way == 0 else d + 2 + j) % 4
        self.copy(j, way).wait_recv()
        total = self.terms.total.ref
        total[to] = (total[to].astype(F32) + self.got.ref[way, j].astype(F32)).astype(BF)

    def arrive(self, j):
        for way in range(2):
            pl.when(self.ends(j, way)[1])(functools.partial(self.take, j, way))

    def step(self):
        self.arrive(self.phase)
        self.phase += 1
        for way in range(2):
            pl.when(self.ends(self.phase, way)[0])(self.copy(self.phase, way).start)

    def wait(self):
        if self.waited:
            return
        self.waited = True
        while self.phase < 2:
            self.step()
        self.arrive(2)
        done = self.local(self.terms.total.ref.at[lax.axis_index("dp")], self.out.ref, 0)
        done.start()
        for j in range(3):
            for way in range(2):
                pl.when(self.ends(j, way)[0])(self.copy(j, way).wait_send)
        done.wait()

    def add(self):
        self.load()
        self.send()


def sum_scatter(k, kind, grads, received):
    return (LineScatter if dp_size() == 4 else DirectScatter)(k, kind, grads, received)


class Finish(Task):
    def __init__(self, k, pieces, block):
        self.pieces, self.final = as_val(k, pieces), block
        *slots, rows, cols = self.pieces.shape
        self.slots = slots[0] if slots else 0
        if slots:
            self.held, self.total = k.vmem(self.pieces.shape, BF), k.vmem((rows, cols), BF)
        else:
            self.total = self.pieces

        def moves(s, d, t):
            source, dst = [(None, self.total.ref)], self.out.ref.at[s]
            return [(source, dst, {"section": 1 - s})], [(source, dst)]

        super().__init__(k, (2, rows, cols), "section", moves, 1, 2)

    def load(self):
        if self.slots:
            self.local(self.pieces.ref, self.held.ref, 1).start()

    def send(self):
        if self.slots:
            self.local(self.pieces.ref, self.held.ref, 1).wait()
            acc = self.held.ref[0].astype(F32)
            for i in range(1, self.slots):
                acc = acc + self.held.ref[i].astype(F32)
            self.total.ref[...] = acc.astype(BF)
        super().send()

    def add(self):
        self.load()
        self.send()


class SumShare(Task):
    def __init__(self, k, terms, axis, slotted=False):
        self.terms = [as_val(k, v) for v in terms]
        shape = self.terms[0].shape[1:] if slotted else self.terms[0].shape
        count = dp_size() if axis == "dp" else 4
        self.slotted = slotted
        self.bufs = [k.vmem(v.shape, F32) for v in self.terms]
        self.total = k.vmem(shape, F32)

        def moves(s, d, t):
            source, me = [(None, self.total.ref)], d if axis == "dp" else t
            dst = self.out.ref.at[me]
            far = [(source, dst, {axis: (me + i) % count}) for i in range(1, count)]
            return far, [(source, dst)]

        super().__init__(k, (count,) + shape, axis, moves, count - 1, 3, out_dtype=F32)

    def add(self):
        loads = [self.local(v.ref, b.ref, 1 + i) for i, (v, b) in enumerate(zip(self.terms, self.bufs))]
        for load in loads:
            load.start()
        for load in loads:
            load.wait()
        if self.slotted:
            parts = [self.bufs[0].ref[i] for i in range(self.terms[0].shape[0])]
        else:
            parts = [buf.ref[...] for buf in self.bufs]
        acc = parts[0]
        for part in parts[1:]:
            acc = acc + part
        self.total.ref[...] = acc
        self.send()


class Weight:
    def __init__(self, k, kind, near, far, early=False):
        near, far = as_val(k, near), as_val(k, far)
        self.count, self.rows, self.cols = near.shape
        self.kind, self.near, self.far, self.waited = kind, near, far, False
        if kind == "cols":
            shape = (2 * self.rows, self.count * self.cols)
        else:
            shape = (2 * self.count * self.rows, self.cols)
        self.aside = kind == "cols" and self.cols % 128 != 0
        self.buf, self.sem = k.vmem(shape, BF), k.sem(2 * self.count)
        if self.aside:
            self.held = [k.vmem(near.shape, BF), k.vmem(near.shape, BF)]
        k.once.append(self)
        if early:
            k.early.append(self.start)

    def moves(self):
        s, dst = lax.axis_index("section"), self.buf.ref
        rows, cols = self.rows, self.cols

        def place(sec, own):
            if self.aside:
                return None
            if self.kind == "cols":
                return dst.at[block_of(sec, rows), pl.ds(own * cols, cols)]
            slot = own * 2 + sec if self.kind == "rows" else sec * self.count + own
            return dst.at[block_of(slot, rows)]

        for i in range(self.count):
            for j, (val, sec) in enumerate(((self.near, s), (self.far, 1 - s))):
                to = self.held[j].ref.at[i] if self.aside else place(sec, i)
                yield pltpu.make_async_copy(val.ref.at[i], to, self.sem.ref.at[2 * i + j])

    def start(self):
        for move in self.moves():
            move.start()

    def wait(self):
        if self.waited:
            return
        self.waited = True
        for move in self.moves():
            move.wait()
        if self.aside:
            s = lax.axis_index("section")
            for j, sec in enumerate((s, 1 - s)):
                whole = jnp.concatenate([self.held[j].ref[i] for i in range(self.count)], axis=1)
                self.buf.ref[block_of(sec, self.rows), :] = whole


class Product:
    def __init__(self, k, left, right):
        self.left, self.right = left, right
        rows = left.shape[1]
        self.chunk = 384 if rows % 384 == 0 else 256
        self.count = rows // self.chunk
        self.buf = k.vmem((rows, right.shape[1]), BF)
        self.out, self.sem = k.output(self.buf.shape, BF), k.sem(self.count)

    def copy(self, i):
        part = block_of(i, self.chunk)
        return pltpu.make_async_copy(self.buf.ref.at[part], self.out.ref.at[part], self.sem.ref.at[i])

    def run(self):
        def step(i, carry):
            part = block_of(i, self.chunk)
            value = contract(self.left.ref[:, part], self.right.ref[...], 0, 0)
            self.buf.ref[part, :] = value.astype(BF)
            self.copy(i).start()
            return carry

        lax.fori_loop(0, self.count, step, 0)

    def wait(self):
        for i in range(self.count):
            self.copy(i).wait()


def places():
    me = lax.axis_index("tensor")
    sib = me + 1 - 2 * (me % 2)
    cross = (me + 2) % 4
    diag = (sib + 2) % 4
    return me, sib, cross, diag


class Gather:
    def __init__(self, k, x, gain, weights, extras=(), trans=False, epilogue="plain", save=()):
        rows, width = x.shape
        length = 4 * rows
        self.k, self.x, self.gain, self.weights, self.extras = k, x, gain, weights, extras
        self.trans, self.epilogue, self.rows, self.half = trans, epilogue, rows, rows // 2
        cols = [w.buf.shape[0 if trans else 1] for w in weights]
        kinds = {
            "plain": [(c, F32) for c in cols],
            "ffn": [(cols[0], BF)] * 3,
            "ffn_back": [(cols[0], BF)] * 2,
        }[epilogue]
        self.full = k.vmem((length, width), BF)
        self.values = [k.vmem((length, c), kind) for c, kind in kinds]
        kept = [self.full] + self.values
        self.saved = [(v, k.output(v.shape, v.dtype), k.sem(4, 2)) for v in kept if kept.index(v) in save]
        self.sems = [k.sem(2) for _ in range(6)]
        k.late.append(self.end)

    def span(self, owner, sub):
        return pl.ds(pl.multiple_of(owner * self.rows + sub * self.half, self.half), self.half)

    def move(self, kind, i):
        me, sib, cross, _ = places()
        full = self.full.ref
        owner, peer, at = {"cross": (me, cross, 0), "sib": (me, sib, 2), "relay": (cross, sib, 4)}[kind]
        part = full.at[self.span(owner, i)]
        return remote(
            part, part, self.sems[at].ref.at[i], self.sems[at + 1].ref.at[i], {"tensor": peer}
        )

    def begin(self):
        me = places()[0]
        for i in range(2):
            part = self.x.ref[pl.ds(i * self.half, self.half), :].astype(F32)
            if self.gain is not None:
                val, row = self.gain
                part = norm_rows(part, val.ref[row : row + 1, :])
            self.full.ref[self.span(me, i), :] = part.astype(BF)
            self.move("cross", i).start()
            self.move("sib", i).start()

    def loop(self):
        me, sib, cross, diag = places()
        rows, half = self.rows, self.half
        for w in self.weights:
            w.wait()

        def step(p, carry):
            far, sub = p // 2, p % 2
            near = (1 - sub) * me + sub * sib
            first = (1 - far) * near * rows + far * (cross * rows + sub * half)
            second = (1 - far) * (near * rows + half) + far * (diag * rows + sub * half)
            pair = [pl.ds(pl.multiple_of(v, half), half) for v in (first, second)]

            @pl.when(p == 1)
            def _():
                self.move("sib", 0).wait_recv()
                self.move("sib", 1).wait_recv()

            for i in range(2):

                @pl.when(p == 2 + i)
                def _():
                    self.move("cross", i).wait_recv()
                    self.move("relay", i).start()
                    self.move("relay", i).wait_recv()

            def both(val):
                return jnp.concatenate([val.ref[pair[0], :], val.ref[pair[1], :]], axis=0)

            a = both(self.full)
            prods = [contract(a, w.buf.ref[...], 1, 1 if self.trans else 0) for w in self.weights]
            if self.epilogue == "plain":
                values = prods
            elif self.epilogue == "ffn":
                sig, silu = silu_parts(prods[0])
                values = [prods[0], prods[1], silu * prods[1]]
            else:
                gate, up = (both(v).astype(F32) for v in self.extras)
                sig, silu = silu_parts(gate)
                values = [prods[0] * up * sig * (1.0 + gate * (1.0 - sig)), prods[0] * silu]
            for val, value in zip(self.values, values):
                value = value.astype(val.dtype)
                for j in range(2):
                    val.ref[pair[j], :] = value[j * half : (j + 1) * half]
            for val, out, sem in self.saved:
                for j in range(2):
                    pltpu.make_async_copy(
                        val.ref.at[pair[j]], out.ref.at[pair[j]], sem.ref.at[p, j]
                    ).start()
            return carry

        lax.fori_loop(0, 4, step, 0)

    def end(self):
        for i in range(2):
            for kind in ("cross", "sib", "relay"):
                self.move(kind, i).wait_send()
        part = pl.ds(0, self.half)
        for val, out, sem in self.saved:
            for p in range(4):
                for j in range(2):
                    pltpu.make_async_copy(val.ref.at[part], out.ref.at[part], sem.ref.at[p, j]).wait()


class Scatter:
    def __init__(self, k, operands, weights, resid, back=None, trans=False, low=False):
        rows, width = resid.shape
        half = rows // 2
        self.operands, self.weights, self.resid, self.back = operands, weights, resid, back
        self.trans, self.low, self.rows, self.half = trans, low, rows, half
        self.keep, self.own = k.vmem((2, half, width), F32), k.vmem((rows, width), F32)
        self.to_s, self.from_s, self.to_c, self.from_c = (
            k.vmem((2, half, width), BF) for _ in range(4)
        )
        self.to_o, self.from_o = k.vmem((rows, width), BF), k.vmem((rows, width), BF)
        self.out = k.vmem((rows, width), BF if low else F32)
        self.gain_grad = k.vmem((1, width), F32) if back else None
        self.sems = [k.sem(2) for _ in range(4)] + [k.sem(1) for _ in range(2)]
        k.late.append(self.end)

    def move(self, kind, i=0):
        _, sib, cross, _ = places()
        at, src, dst, peer = {
            "diag": (0, self.to_s, self.from_s, sib),
            "cross": (2, self.to_c, self.from_c, cross),
            "near": (4, self.to_o, self.from_o, sib),
        }[kind]
        src, dst = (src.ref, dst.ref) if kind == "near" else (src.ref.at[i], dst.ref.at[i])
        return remote(
            src, dst, self.sems[at].ref.at[i], self.sems[at + 1].ref.at[i], {"tensor": peer}
        )

    def pass_on(self, i):
        self.move("diag", i).wait_recv()
        total = self.keep.ref[i] + self.from_s.ref[i].astype(F32)
        self.to_c.ref[i] = total.astype(BF)
        self.move("cross", i).start()

    def loop(self):
        me, sib, cross, diag = places()
        rows, half = self.rows, self.half
        for w in self.weights:
            w.wait()

        def step(p, carry):
            near, sub = p // 2, p % 2
            base = near * ((1 - sub) * sib + sub * me) * rows
            first = base + (1 - near) * (cross * rows + sub * half)
            second = base + near * half + (1 - near) * (diag * rows + sub * half)
            pair = [pl.ds(pl.multiple_of(v, half), half) for v in (first, second)]
            total = None
            for y, w in zip(self.operands, self.weights):
                a = jnp.concatenate([y.ref[pair[0], :], y.ref[pair[1], :]], axis=0)
                prod = contract(a, w.buf.ref[...], 1, 1 if self.trans else 0)
                total = prod if total is None else total + prod

            for i in range(2):

                @pl.when(p == i)
                def _():
                    self.keep.ref[i] = total[:half]
                    self.to_s.ref[i] = total[half:].astype(BF)
                    self.move("diag", i).start()

            @pl.when(p == 1)
            def _():
                self.pass_on(0)

            @pl.when(p == 2)
            def _():
                self.to_o.ref[...] = total.astype(BF)
                self.move("near").start()
                self.pass_on(1)

            @pl.when(p == 3)
            def _():
                self.own.ref[...] = total

            return carry

        lax.fori_loop(0, 4, step, 0)

    def finish(self):
        self.move("near").wait_recv()
        gain_sum = None
        for i in range(2):
            part = pl.ds(i * self.half, self.half)
            self.move("cross", i).wait_recv()
            total = self.own.ref[part, :] + self.from_o.ref[part, :].astype(F32)
            total = total + self.from_c.ref[i].astype(F32)
            resid = self.resid.ref[part, :].astype(F32)
            if self.back:
                value, (gain, row) = self.back
                value_grad, gain_grad = norm_back(
                    value.ref[part, :].astype(F32), gain.ref[row : row + 1, :], total
                )
                total = value_grad
                gain_sum = gain_grad if gain_sum is None else gain_sum + gain_grad
            self.out.ref[part, :] = (resid + total).astype(self.out.dtype)
        if self.back:
            self.gain_grad.ref[...] = gain_sum

    def end(self):
        self.move("near").wait_send()
        for i in range(2):
            self.move("diag", i).wait_send()
            self.move("cross", i).wait_send()


def delayed(values, by):
    if by == 0:
        return values
    row = lax.broadcasted_iota(jnp.int32, values.shape, 0)
    return jnp.where(row < by, 0.0, pltpu.roll(values, by, 0))


def advanced(values, by):
    if by == 0:
        return values
    length = values.shape[0]
    row = lax.broadcasted_iota(jnp.int32, values.shape, 0)
    return jnp.where(row >= length - by, 0.0, pltpu.roll(values, length - by, 0))


CONV_COLS = 128


class Conv:
    def __init__(self, k, projected, value, kernel):
        self.projected, self.value, self.kernel = projected, value, kernel
        self.y = k.vmem(value.shape, BF)

    def parts(self, j):
        channels = self.value.shape[1]
        at = slice(j * CONV_COLS, (j + 1) * CONV_COLS)
        b_gate = self.projected.ref[:, at]
        c_gate = self.projected.ref[:, channels + at.start : channels + at.stop]
        x_value, taps = self.value.ref[:, at], self.kernel.ref[:, at]
        product = b_gate * x_value
        count = taps.shape[0]
        causal = jnp.zeros_like(product)
        for i in range(count):
            causal = causal + taps[i : i + 1] * delayed(product, count - 1 - i)
        return at, b_gate, c_gate, x_value, taps, product, causal

    def run(self):
        for j in range(self.value.shape[1] // CONV_COLS):
            at, _, c_gate, _, _, _, causal = self.parts(j)
            self.y.ref[:, at] = (c_gate * causal).astype(BF)


class ConvBack(Conv):
    def __init__(self, k, projected, value, kernel, d_y):
        self.projected, self.value, self.kernel, self.d_y = projected, value, kernel, d_y
        self.d_proj = k.vmem(projected.shape, BF)
        self.d_value = k.vmem(value.shape, BF)
        self.d_kernel = k.vmem(kernel.shape, F32)

    def run(self):
        channels = self.value.shape[1]
        for j in range(channels // CONV_COLS):
            at, b_gate, c_gate, x_value, taps, product, causal = self.parts(j)
            d_y = self.d_y.ref[:, at]
            d_causal = d_y * c_gate
            count = taps.shape[0]
            d_product = jnp.zeros_like(product)
            for i in range(count):
                by = count - 1 - i
                row = jnp.sum(d_causal * delayed(product, by), axis=0, keepdims=True)
                self.d_kernel.ref[i : i + 1, at] = row
                d_product = d_product + taps[i : i + 1] * advanced(d_causal, by)
            self.d_proj.ref[:, at] = (d_product * x_value).astype(BF)
            self.d_proj.ref[:, channels + at.start : channels + at.stop] = (d_y * causal).astype(BF)
            self.d_value.ref[:, at] = (d_product * b_gate).astype(BF)


def head_mean(values, head_size):
    width = values.shape[1]
    row = lax.broadcasted_iota(jnp.int32, (width, width), 0) // head_size
    col = lax.broadcasted_iota(jnp.int32, (width, width), 1) // head_size
    group = jnp.where(row == col, 1.0 / head_size, 0.0).astype(F32)
    return lax.dot_general(
        values, group, (((1,), (0,)), ((), ())),
        precision=lax.Precision.HIGHEST, preferred_element_type=F32,
    )


def turn(values, head_size, back):
    width, half = values.shape[1], head_size // 2
    lane = lax.broadcasted_iota(jnp.int32, values.shape, 1) % head_size
    upper = pltpu.roll(values, width - half, 1)
    lower = pltpu.roll(values, half, 1)
    return jnp.where(lane < half, upper, -lower) if back else jnp.where(lane < half, -upper, lower)


def head_norm(values, gain, head_size):
    return values * lax.rsqrt(head_mean(values * values, head_size) + EPS) * gain


def head_norm_back(values, gain, grad_in, head_size):
    row_scale = lax.rsqrt(head_mean(values * values, head_size) + EPS)
    normed = values * row_scale
    gain_grad = jnp.sum(grad_in * normed, axis=0, keepdims=True)
    scaled = grad_in * gain
    return row_scale * (scaled - normed * head_mean(scaled * normed, head_size)), gain_grad


def block_weights(q_rows, k_rows, first_row):
    rows, length = q_rows.shape[0], k_rows.shape[0]
    scores = contract(q_rows, k_rows, 1, 1) * (q_rows.shape[1] ** -0.5)
    query = first_row + lax.broadcasted_iota(jnp.int32, (rows, length), 0)
    key = lax.broadcasted_iota(jnp.int32, (rows, length), 1)
    scores = jnp.where(key <= query, scores, MASKED)
    exps = jnp.exp(scores - jnp.max(scores, axis=1, keepdims=True))
    return exps * (1.0 / jnp.sum(exps, axis=1, keepdims=True))


class Heads:
    def __init__(self, projected, tables, size):
        self.projected, self.size = projected, size
        self.gain, self.cos, self.sin = (v.buf for v in tables)
        self.loads = tables
        self.length, width = projected.shape
        self.q_cols, self.k_cols = width // 2, width // 4
        self.heads, self.kv_heads = self.q_cols // size, self.k_cols // size
        self.share = self.heads // self.kv_heads

    def per_head(self, k, count, kind):
        return k.vmem((count, self.length, self.size), kind)

    def split(self, val, rows, values):
        for h in range(val.shape[0]):
            val.ref[h, rows, :] = values[:, h * self.size : (h + 1) * self.size]

    def join(self, val, rows):
        return jnp.concatenate([val.ref[h, rows, :] for h in range(val.shape[0])], axis=1)

    def blocks(self, step):
        lax.fori_loop(0, self.length // ROW_BLOCK, lambda p, c: step(block_of(p, ROW_BLOCK)) or c, 0)


class Attend(Heads):
    def __init__(self, k, projected, tables, size):
        super().__init__(projected, tables, size)
        self.q_rot = k.vmem((self.length, self.q_cols), BF)
        self.k_rot = k.vmem((self.length, self.k_cols), BF)
        self.y = k.vmem((self.length, self.q_cols), BF)
        self.q_h, self.y_h = (self.per_head(k, self.heads, BF) for _ in range(2))
        self.k_h, self.v_h = (self.per_head(k, self.kv_heads, BF) for _ in range(2))

    def run(self, *between):
        for load in self.loads:
            load.wait()
        size, q_cols, k_cols, proj = self.size, self.q_cols, self.k_cols, self.projected.ref

        def prepare(rows):
            c, n = self.cos.ref[rows, :], self.sin.ref[rows, :]
            q = head_norm(proj[rows, :q_cols], self.gain.ref[0:1, :], size)
            q = (q * c + turn(q, size, False) * n).astype(BF)
            k = head_norm(proj[rows, q_cols : q_cols + k_cols], self.gain.ref[1:2, :k_cols], size)
            k = (k * c[:, :k_cols] + turn(k, size, False) * n[:, :k_cols]).astype(BF)
            self.q_rot.ref[rows, :] = q
            self.k_rot.ref[rows, :] = k
            self.split(self.q_h, rows, q)
            self.split(self.k_h, rows, k)
            self.split(self.v_h, rows, proj[rows, q_cols + k_cols :].astype(BF))

        self.blocks(prepare)

        def head(h, carry):
            g = h // self.share
            for i in range(self.length // ROW_BLOCK):
                rows, seen = pl.ds(i * ROW_BLOCK, ROW_BLOCK), pl.ds(0, (i + 1) * ROW_BLOCK)
                weights = block_weights(
                    self.q_h.ref[h, rows, :], self.k_h.ref[g, seen, :], i * ROW_BLOCK
                )
                value = contract(weights.astype(BF), self.v_h.ref[g, seen, :], 1, 0)
                self.y_h.ref[h, rows, :] = value.astype(BF)
            return carry

        lax.fori_loop(0, self.heads // 2, head, 0)
        for step in between:
            step()
        lax.fori_loop(self.heads // 2, self.heads, head, 0)
        self.y.ref[...] = self.join(self.y_h, slice(None))


class AttendBack(Heads):
    def __init__(self, k, projected, tables, size, q_rot, k_rot, d_y):
        super().__init__(projected, tables, size)
        self.q_rot, self.k_rot, self.d_y = q_rot, k_rot, d_y
        self.q_h, self.dy_h = (self.per_head(k, self.heads, BF) for _ in range(2))
        self.k_h, self.v_h = (self.per_head(k, self.kv_heads, BF) for _ in range(2))
        self.dq_h = self.per_head(k, self.heads, F32)
        self.dk_h, self.dv_h = (self.per_head(k, self.kv_heads, F32) for _ in range(2))
        self.d_proj = k.vmem(projected.shape, BF)
        self.q_gain, self.k_gain = k.vmem((1, self.q_cols), F32), k.vmem((1, self.k_cols), F32)

    def run(self, *between):
        for load in self.loads:
            load.wait()
        size, q_cols, k_cols, proj = self.size, self.q_cols, self.k_cols, self.projected.ref
        scale = size**-0.5
        dq_h, dk_h, dv_h = self.dq_h.ref, self.dk_h.ref, self.dv_h.ref

        def prepare(rows):
            self.split(self.q_h, rows, self.q_rot.ref[rows, :])
            self.split(self.dy_h, rows, self.d_y.ref[rows, :].astype(BF))
            self.split(self.k_h, rows, self.k_rot.ref[rows, :])
            self.split(self.v_h, rows, proj[rows, q_cols + k_cols :].astype(BF))

        self.blocks(prepare)
        dk_h[...] = jnp.zeros_like(dk_h)
        dv_h[...] = jnp.zeros_like(dv_h)

        def head(h, carry):
            g = h // self.share
            for i in range(self.length // ROW_BLOCK):
                rows, seen = pl.ds(i * ROW_BLOCK, ROW_BLOCK), pl.ds(0, (i + 1) * ROW_BLOCK)
                q, low = self.q_h.ref[h, rows, :], self.dy_h.ref[h, rows, :]
                k = self.k_h.ref[g, seen, :]
                prob = block_weights(q, k, i * ROW_BLOCK)
                d_weights = contract(low, self.v_h.ref[g, seen, :], 1, 1)
                dv_h[g, seen, :] += contract(prob.astype(BF), low, 0, 0)
                inner = jnp.sum(prob * d_weights, axis=1, keepdims=True)
                d_scores = (prob * (d_weights - inner)).astype(BF)
                dq_h[h, rows, :] = contract(d_scores, k, 1, 0) * scale
                dk_h[g, seen, :] += contract(d_scores, q, 0, 0) * scale
            return carry

        lax.fori_loop(0, self.heads // 2, head, 0)
        for step in between:
            step()
        lax.fori_loop(self.heads // 2, self.heads, head, 0)
        self.q_gain.ref[...] = jnp.zeros_like(self.q_gain.ref)
        self.k_gain.ref[...] = jnp.zeros_like(self.k_gain.ref)

        def finish(rows):
            c, n = self.cos.ref[rows, :], self.sin.ref[rows, :]
            dq, dk, dv = (self.join(v, rows) for v in (self.dq_h, self.dk_h, self.dv_h))
            dq = dq * c + turn(dq * n, size, True)
            dk = dk * c[:, :k_cols] + turn(dk * n[:, :k_cols], size, True)
            dq, q_sum = head_norm_back(proj[rows, :q_cols], self.gain.ref[0:1, :], dq, size)
            dk, k_sum = head_norm_back(
                proj[rows, q_cols : q_cols + k_cols], self.gain.ref[1:2, :k_cols], dk, size
            )
            self.q_gain.ref[...] += q_sum
            self.k_gain.ref[...] += k_sum
            self.d_proj.ref[rows, :q_cols] = dq.astype(BF)
            self.d_proj.ref[rows, q_cols : q_cols + k_cols] = dk.astype(BF)
            self.d_proj.ref[rows, q_cols + k_cols :] = dv.astype(BF)

        self.blocks(finish)


def body(boundary, norm_gain, mix_in, mix_out, w_gate, w_up, w_down, conv_x, conv_kernel, qk_gain):
    first = lax.axis_index("section") == 0
    tensor_index = lax.axis_index("tensor")
    model_width = boundary.shape[3]
    channels = mix_out.shape[1]
    row_shape = boundary.shape[2:]
    length, size = 4 * row_shape[0], qk_gain.shape[1]

    seqs, own_gain = boundary[0], norm_gain[0]
    sh_in, sh_out, sh_gate, sh_up, sh_down = (v[0] for v in (mix_in, mix_out, w_gate, w_up, w_down))
    cosine_table, sine_table = rotation(length, size)
    heads = channels // size
    table_arrays = [jnp.tile(v, (1, heads)) for v in (qk_gain, cosine_table, sine_table)]

    def gains_of(k, block, other, early=True):
        own, moved = k.input(own_gain), as_val(k, other)
        sources = lambda s, d, t: [(s == block, own.ref), (s == 1 - block, moved.ref)]
        return Load(k, sources, own.shape, F32, early)

    def start_rows(k, slot, other, early=True):
        own, moved = k.input(seqs), as_val(k, other)
        sources = lambda s, d, t: [(s == slot, own.ref.at[slot]), (s == 1 - slot, moved.ref)]
        return Load(k, sources, row_shape, BF, early)

    def wait(*items):
        return [item.wait for item in items]

    k = Kernel(0)
    t_seq = None
    seq_val = k.input(seqs)

    def seq_moves(s, d, t):
        return [([(None, seq_val.ref.at[1 - s])], t_seq.out.ref, {"section": 1 - s})], []

    t_in, t_out, t_gate, t_up, t_down = (
        x_half(k, v) for v in (sh_in, sh_out, sh_gate, sh_up, sh_down)
    )
    t_seq = Task(k, row_shape, "section", seq_moves, 1)
    t_gain, z_cols = x_move(k, own_gain), z_gather(k, conv_x)
    z_in0, z_out0 = z_gather_half(k, sh_in, t_in.out, 0), z_gather_half(k, sh_out, t_out.out, 0)
    z_gate0, z_up0 = z_gather_half(k, sh_gate, t_gate.out, 0), z_gather_half(k, sh_up, t_up.out, 0)
    x_cols, x_in0, x_out0, x_gate0 = (x_move(k, v.out) for v in (z_cols, z_in0, z_out0, z_gate0))
    x_load, gain_load = start_rows(k, 0, t_seq.out, False), gains_of(k, 0, t_gain.out, False)
    taps = load_all(k, conv_kernel)
    w_in0, w_cols = Weight(k, "rows", z_in0.out, x_in0.out), Weight(k, "conv", z_cols.out, x_cols.out)
    w_out0 = Weight(k, "cols", z_out0.out, x_out0.out)
    g0 = Gather(k, x_load.buf, (gain_load.buf, 0), [w_in0, w_cols], save=(0, 1, 2))
    conv = Conv(k, g0.values[0], g0.values[1], taps.buf)
    y0 = Save(k, conv.y)
    s1 = Scatter(k, [conv.y], [w_out0], x_load.buf)
    mid0 = Save(k, s1.out)
    k.do(t_in.send, t_out.send, z_cols.send, t_gate.send, t_gain.send, t_seq.send)
    k.do(t_in.wait, z_in0.send, t_out.wait, z_out0.send, t_up.send)
    k.do(z_cols.step, z_in0.step, z_out0.step, t_gate.wait, z_gate0.send)
    k.do(z_cols.step, z_in0.step, z_out0.step)
    k.do(t_gain.wait, gain_load.start, t_seq.wait, x_load.start)
    k.do(gain_load.wait, x_load.wait, g0.begin)
    k.do(z_cols.wait, x_cols.send, z_in0.wait, x_in0.send, z_out0.wait, x_out0.send, t_down.send)
    k.do(z_gate0.step, t_up.wait, z_up0.send, z_gate0.step, z_up0.step, z_gate0.wait, x_gate0.send)
    k.do(x_cols.wait, w_cols.start, x_in0.wait, w_in0.start, z_up0.step)
    k.do(g0.loop, taps.wait, conv.run, y0.start)
    k.do(x_out0.wait, w_out0.start, s1.loop, s1.finish, mid0.start)
    k.do(*wait(t_down, x_gate0, z_up0))
    k.build()
    a0, proj0, value0 = (out for _, out, _ in g0.saved)
    y0, mid0 = y0.out, mid0.out

    k = Kernel(1)
    x_up0, z_down0 = x_move(k, z_up0.out), z_gather_half(k, sh_down, t_down.out, 0)
    z_in1, z_out1 = z_gather_half(k, sh_in, t_in.out, 1), z_gather_half(k, sh_out, t_out.out, 1)
    z_gate1 = z_gather_half(k, sh_gate, t_gate.out, 1)
    x_down0, x_in1, x_out1 = (x_move(k, v.out) for v in (z_down0, z_in1, z_out1))
    rows, gain_load = load_all(k, mid0), gains_of(k, 0, t_gain.out)
    w_gate0 = Weight(k, "rows", z_gate0.out, x_gate0.out, True)
    w_up0 = Weight(k, "rows", z_up0.out, x_up0.out)
    w_down0 = Weight(k, "cols", z_down0.out, x_down0.out)
    g2 = Gather(
        k, rows.buf, (gain_load.buf, 1), [w_gate0, w_up0], epilogue="ffn", save=(0, 1, 2, 3)
    )
    s3 = Scatter(k, [g2.values[2]], [w_down0], rows.buf, low=True)
    z_rows = Save(k, s3.out)
    k.do(x_up0.send, z_down0.send, z_in1.send, z_out1.send)
    k.do(rows.wait, gain_load.wait, g2.begin)
    k.do(z_down0.step, z_in1.step, z_out1.step, z_down0.step, z_gate1.send, z_in1.step, z_out1.step)
    k.do(z_down0.wait, x_down0.send, x_up0.wait, w_up0.start, z_gate1.step, g2.loop)
    k.do(z_gate1.step, z_in1.wait, x_in1.send, z_out1.wait, x_out1.send)
    k.do(x_down0.wait, w_down0.start, s3.loop, s3.finish, z_rows.start)
    k.do(*wait(x_in1, x_out1, z_gate1))
    k.build()
    m0, gate0, up0, hid0 = (out for _, out, _ in g2.saved)
    z_rows = z_rows.out

    k = Kernel(2)
    x_gate1, z_up1 = x_move(k, z_gate1.out), z_gather_half(k, sh_up, t_up.out, 1)
    z_down1, x_up1 = z_gather_half(k, sh_down, t_down.out, 1), x_move(k, z_up1.out)
    rows, gain_load = load_all(k, z_rows), gains_of(k, 1, t_gain.out)
    tables = [load_all(k, v) for v in table_arrays]
    w_in1 = Weight(k, "rows", z_in1.out, x_in1.out, True)
    w_out1 = Weight(k, "cols", z_out1.out, x_out1.out, True)
    g4 = Gather(k, rows.buf, (gain_load.buf, 0), [w_in1], save=(0, 1))
    attend = Attend(k, g4.values[0], tables, size)
    kept = [Save(k, v) for v in (attend.q_rot, attend.k_rot, attend.y)]
    s5 = Scatter(k, [attend.y], [w_out1], rows.buf)
    mid1 = Save(k, s5.out)
    k.do(x_gate1.send, z_up1.send, z_down1.send)
    k.do(rows.wait, gain_load.wait, g4.begin, z_up1.step, g4.loop, z_up1.step, z_down1.step)
    k.do(lambda: attend.run(z_up1.wait, x_up1.send, z_down1.step))
    k.do(*(v.start for v in kept))
    k.do(s5.loop, s5.finish, mid1.start)
    k.do(*wait(x_gate1, x_up1, z_down1))
    k.build()
    a1, proj1 = (out for _, out, _ in g4.saved)
    q_rot, k_rot, y1 = (v.out for v in kept)
    mid1 = mid1.out

    k = Kernel(3)
    x_down1 = x_move(k, z_down1.out)
    rows, gain_load = load_all(k, mid1), gains_of(k, 1, t_gain.out)
    cot = start_rows(k, 1, t_seq.out)
    w_gate1 = Weight(k, "rows", z_gate1.out, x_gate1.out, True)
    w_up1 = Weight(k, "rows", z_up1.out, x_up1.out, True)
    w_down1 = Weight(k, "cols", z_down1.out, x_down1.out)
    g6 = Gather(k, rows.buf, (gain_load.buf, 1), [w_gate1, w_up1], epilogue="ffn")
    g8 = Gather(
        k, cot.buf, None, [w_down1], [g6.values[0], g6.values[1]], trans=True, epilogue="ffn_back"
    )
    p_down1 = Product(k, g6.values[2], g8.full)
    p_gate1, p_up1 = Product(k, g6.full, g8.values[0]), Product(k, g6.full, g8.values[1])
    r_down1 = x_half(k, p_down1.out)
    s7 = Scatter(k, [g6.values[2]], [w_down1], rows.buf, low=True)
    s9 = Scatter(k, g8.values, [w_gate1, w_up1], cot.buf, (rows.buf, (gain_load.buf, 1)), True)
    y_rows, d_mid1, gain11 = Save(k, s7.out), Save(k, s9.out), Save(k, s9.gain_grad)
    k.do(x_down1.send, rows.wait, gain_load.wait, g6.begin, cot.wait, g8.begin, g6.loop)
    k.do(x_down1.wait, w_down1.start, g8.loop, p_down1.run, p_down1.wait, r_down1.send)
    k.do(s9.loop, p_gate1.run, p_up1.run, s9.finish, d_mid1.start, gain11.start)
    k.do(s7.loop, s7.finish, y_rows.start, p_gate1.wait, p_up1.wait)
    k.do(*wait(r_down1))
    k.build()
    y_rows, d_mid1, gain11 = y_rows.out, d_mid1.out, gain11.out

    k = Kernel(4)
    q_down1 = sum_scatter(k, "cols", p_down1.out, r_down1.out)
    r_gate1, r_up1 = x_slots(k, p_gate1.out, "rows"), x_slots(k, p_up1.out, "rows")
    q_gate1 = sum_scatter(k, "rows", p_gate1.out, r_gate1.out)
    rows, gain_load = load_all(k, d_mid1), gains_of(k, 1, t_gain.out)
    value = load_all(k, z_rows)
    tables = [load_all(k, v) for v in table_arrays]
    proj, q_load, k_load, y_load, a_load = (load_all(k, v) for v in (proj1, q_rot, k_rot, y1, a1))
    w_in1 = Weight(k, "rows", z_in1.out, x_in1.out, True)
    w_out1 = Weight(k, "cols", z_out1.out, x_out1.out, True)
    g10 = Gather(k, rows.buf, None, [w_out1], trans=True)
    p_out1 = Product(k, y_load.buf, g10.full)
    back = AttendBack(k, proj.buf, tables, size, q_load.buf, k_load.buf, g10.values[0])
    p_in1 = Product(k, a_load.buf, back.d_proj)
    r_out1 = x_half(k, p_out1.out)
    s11 = Scatter(
        k, [back.d_proj], [w_in1], rows.buf, (value.buf, (gain_load.buf, 0)), True, low=True
    )
    d_z, gain10 = Save(k, s11.out), Save(k, s11.gain_grad)
    head_gains = [Save(k, back.q_gain), Save(k, back.k_gain)]
    k.early.append(q_down1.load)
    k.do(r_gate1.send, r_up1.send, rows.wait, g10.begin, q_down1.send, g10.loop)
    k.do(q_down1.step, y_load.wait, p_out1.run, p_out1.wait, r_out1.send, q_down1.step)
    k.do(r_gate1.wait, q_gate1.add)
    k.do(proj.wait, q_load.wait, k_load.wait, lambda: back.run(q_gate1.step))
    k.do(q_gate1.step, *(v.start for v in head_gains))
    k.do(gain_load.wait, value.wait, s11.loop, a_load.wait, p_in1.run)
    k.do(s11.finish, d_z.start, gain10.start, p_in1.wait)
    k.do(*wait(q_down1, q_gate1, r_up1, r_out1))
    k.build()
    d_z, gain10 = d_z.out, gain10.out
    q_gain, k_gain = (v.out.array for v in head_gains)

    k = Kernel(5)
    q_up1 = sum_scatter(k, "rows", p_up1.out, r_up1.out)
    q_out1 = sum_scatter(k, "cols", p_out1.out, r_out1.out)
    r_in1 = x_slots(k, p_in1.out, "rows")
    q_in1 = sum_scatter(k, "rows", p_in1.out, r_in1.out)
    e_down1, e_gate1 = Finish(k, q_down1.out, 1), Finish(k, q_gate1.out, 1)
    rows, value, gain_load = load_all(k, d_z), load_all(k, mid0), gains_of(k, 0, t_gain.out)
    gate_load, up_load, hid_load, m_load = (load_all(k, v) for v in (gate0, up0, hid0, m0))
    w_gate0 = Weight(k, "rows", z_gate0.out, x_gate0.out, True)
    w_up0 = Weight(k, "rows", z_up0.out, x_up0.out, True)
    w_down0 = Weight(k, "cols", z_down0.out, x_down0.out, True)
    g12 = Gather(
        k, rows.buf, None, [w_down0], [gate_load.buf, up_load.buf], trans=True, epilogue="ffn_back"
    )
    p_down0 = Product(k, hid_load.buf, g12.full)
    p_gate0, p_up0 = Product(k, m_load.buf, g12.values[0]), Product(k, m_load.buf, g12.values[1])
    r_down0 = x_half(k, p_down0.out)
    s13 = Scatter(
        k, g12.values, [w_gate0, w_up0], rows.buf, (value.buf, (gain_load.buf, 1)), True
    )
    d_mid0, gain01 = Save(k, s13.out), Save(k, s13.gain_grad)
    k.early += [q_up1.load, q_out1.load, e_down1.load, e_gate1.load]
    k.do(r_in1.send, rows.wait, g12.begin, q_up1.send, q_out1.send, e_down1.send, e_gate1.send)
    k.do(gate_load.wait, up_load.wait, g12.loop)
    k.do(q_up1.step, q_out1.step, hid_load.wait, p_down0.run, p_down0.wait, r_down0.send)
    k.do(q_up1.step, q_out1.step, r_in1.wait, q_in1.add)
    k.do(s13.loop, q_in1.step, m_load.wait, p_gate0.run, q_in1.step, p_up0.run)
    k.do(value.wait, gain_load.wait, s13.finish, d_mid0.start, gain01.start)
    k.do(p_gate0.wait, p_up0.wait)
    k.do(*wait(q_up1, q_out1, q_in1, e_down1, e_gate1, r_down0))
    k.build()
    d_mid0, gain01 = d_mid0.out, gain01.out

    k = Kernel(6)
    r_gate0, r_up0 = x_slots(k, p_gate0.out, "rows"), x_slots(k, p_up0.out, "rows")
    q_down0 = sum_scatter(k, "cols", p_down0.out, r_down0.out)
    q_gate0 = sum_scatter(k, "rows", p_gate0.out, r_gate0.out)
    q_up0 = sum_scatter(k, "rows", p_up0.out, r_up0.out)
    e_up1, e_out1, e_in1 = (Finish(k, v.out, 1) for v in (q_up1, q_out1, q_in1))
    rows, gain_load = load_all(k, d_mid0), gains_of(k, 0, t_gain.out)
    x_load, taps = start_rows(k, 0, t_seq.out), load_all(k, conv_kernel)
    y_load, a_load, proj, value = (load_all(k, v) for v in (y0, a0, proj0, value0))
    w_in0 = Weight(k, "rows", z_in0.out, x_in0.out, True)
    w_cols = Weight(k, "conv", z_cols.out, x_cols.out, True)
    w_out0 = Weight(k, "cols", z_out0.out, x_out0.out, True)
    g14 = Gather(k, rows.buf, None, [w_out0], trans=True)
    p_out0 = Product(k, y_load.buf, g14.full)
    back = ConvBack(k, proj.buf, value.buf, taps.buf, g14.values[0])
    p_in0, p_cols = Product(k, a_load.buf, back.d_proj), Product(k, a_load.buf, back.d_value)
    r_out0, r_in0 = x_half(k, p_out0.out), x_slots(k, p_in0.out, "rows")
    r_cols = x_slots(k, p_cols.out, "conv")
    q_out0, q_in0 = sum_scatter(k, "cols", p_out0.out, r_out0.out), sum_scatter(k, "rows", p_in0.out, r_in0.out)
    q_cols = sum_scatter(k, "conv", p_cols.out, r_cols.out)
    e_down0, e_gate0, e_up0, e_out0, e_in0 = (
        Finish(k, v.out, 0) for v in (q_down0, q_gate0, q_up0, q_out0, q_in0)
    )
    s15 = Scatter(
        k, [back.d_proj, back.d_value], [w_in0, w_cols], rows.buf,
        (x_load.buf, (gain_load.buf, 0)), True, low=True,
    )
    d_x = Save(k, s15.out)
    tap_rows = conv_kernel.shape[0]
    small = k.vmem((8, model_width), F32)
    small_out = Save(k, small)
    ready = [load_all(k, v) for v in (gain01, gain10, gain11)]
    head_row = jnp.pad(
        jnp.stack([jnp.sum(v.reshape(-1, size), axis=0) for v in (q_gain, k_gain)]).reshape(1, -1),
        ((0, 0), (0, model_width - 2 * size)),
    )
    head_load = load_all(k, head_row)

    def fill_small():
        t = lax.axis_index("tensor")
        small.ref[...] = jnp.zeros_like(small.ref)
        small.ref[0:1, :] = s15.gain_grad.ref[...]
        for i, load in enumerate(ready):
            load.wait()
            small.ref[i + 1 : i + 2, :] = load.buf.ref[...]
        small.ref[4 : 4 + tap_rows, block_of(t, channels)] = back.d_kernel.ref[...]
        head_load.wait()
        small.ref[7:8, :] = head_load.buf.ref[...]
        small_out.start()

    t_small = x_move(k, small_out.out)
    z_small = SumShare(k, [small_out.out, t_small.out], "dp")
    t_total = SumShare(k, [z_small.out], "tensor", slotted=True)
    y_val, dx_val = k.input(y_rows), d_x.out

    def result_moves(s, d, t):
        sources = [(s == 0, y_val.ref), (s == 1, dx_val.ref)]
        return [(sources, t_result.out.ref, {"section": 1 - s})], []

    t_result = Task(k, row_shape, "section", result_moves, 1)
    k.early += [q_down0.load, e_up1.load, e_out1.load, e_in1.load]
    k.do(r_gate0.send, r_up0.send, rows.wait, g14.begin, q_down0.send)
    k.do(e_up1.send, e_out1.send, e_in1.send, g14.loop)
    k.do(q_down0.step, y_load.wait, p_out0.run, p_out0.wait, r_out0.send, q_down0.step)
    k.do(proj.wait, value.wait, taps.wait, back.run, a_load.wait)
    k.do(p_in0.run, p_cols.run, p_in0.wait, r_in0.send, p_cols.wait, r_cols.send)
    k.do(r_gate0.wait, q_gate0.add)
    k.do(x_load.wait, gain_load.wait, s15.loop, q_gate0.step, s15.finish, d_x.start, q_gate0.step)
    k.do(fill_small, d_x.wait, t_result.send)
    k.do(small_out.wait, t_small.send)
    k.do(q_down0.wait, e_down0.add, q_gate0.wait, e_gate0.add)
    k.do(r_up0.wait, q_up0.add, r_out0.wait, q_out0.add, r_in0.wait, q_in0.add)
    k.do(q_up0.step, r_cols.wait, q_cols.add, q_out0.step, q_in0.step, t_small.wait, z_small.add)
    k.do(q_up0.step, q_cols.step, q_out0.step, q_in0.step, z_small.wait, t_total.add)
    k.do(q_up0.wait, e_up0.add, q_cols.step, q_out0.wait, e_out0.add, q_in0.wait, e_in0.add)
    rest = (e_up1, e_out1, e_in1, q_cols, e_down0, e_gate0, e_up0, e_out0, e_in0)
    k.do(*wait(*rest, t_total, t_result))
    k.build()

    def whole(zero, one):
        kept = jnp.where(first, zero.out.array, one.out.array)
        return kept.reshape(1, -1, kept.shape[-1]).astype(F32)

    d_x, y_rows, moved = d_x.out.array, y_rows.array, t_result.out.array
    result = jnp.where(first, jnp.stack([d_x, moved]), jnp.stack([moved, y_rows]))
    small = jnp.sum(t_total.out.array, axis=0)
    gains_total = small[:4].reshape(2, 2, model_width)
    gain_out = lax.dynamic_slice_in_dim(gains_total, lax.axis_index("section"), 1, 0)
    kernel_out = lax.dynamic_slice_in_dim(
        small[4 : 4 + tap_rows], tensor_index * channels, channels, 1
    )
    cols_grad = q_cols.out.array.astype(F32)
    if cols_grad.ndim == 3:
        cols_grad = jnp.sum(cols_grad, axis=0)
    head_total = small[7, : qk_gain.size].reshape(qk_gain.shape)
    return (
        result[None],
        gain_out,
        whole(e_in0, e_in1),
        whole(e_out0, e_out1),
        whole(e_gate0, e_gate1),
        whole(e_up0, e_up1),
        whole(e_down0, e_down1),
        cols_grad,
        kernel_out,
        head_total,
    )


def solution(mesh):
    in_specs = (
        P("section", "dp", "tensor", None),
        P("section", None, None),
        P("section", "dp", "tensor"),
        P("section", "tensor", "dp"),
        P("section", "dp", "tensor"),
        P("section", "dp", "tensor"),
        P("section", "tensor", "dp"),
        P(("section", "dp"), "tensor"),
        P(None, "tensor"),
        P(),
    )
    out_specs = (
        P("section", "dp", "tensor", None),
        P("section", None, None),
        P("section", "dp", "tensor"),
        P("section", "tensor", "dp"),
        P("section", "dp", "tensor"),
        P("section", "dp", "tensor"),
        P("section", "tensor", "dp"),
        P(("section", "dp"), "tensor"),
        P(None, "tensor"),
        P(),
    )
    return jax.shard_map(body, mesh=mesh, in_specs=in_specs, out_specs=out_specs, check_vma=False)
```

```python
import functools

import jax
import jax.numpy as jnp
from jax import lax
from jax.experimental import pallas as pl
from jax.experimental.pallas import tpu as pltpu
from jax.sharding import PartitionSpec as P

HEADS = 16
KV_HEADS = 8

EPS = 1e-05
ROPE_BASE = 1000000.0
MASKED = -1e30

MESH = pl.DeviceIdType.MESH
ANY = pl.BlockSpec(memory_space=pl.ANY)
DMA = pltpu.SemaphoreType.DMA
VMEM_BYTES = 63 * 1024 * 1024
BF = jnp.bfloat16
F32 = jnp.float32
ROW_BLOCK = 256


def contract(left_op, right_op, left_dim, right_dim):
    return lax.dot_general(
        left_op, right_op, (((left_dim,), (right_dim,)), ((), ())), preferred_element_type=F32
    )


def norm_rows(values, gain):
    return values * lax.rsqrt(jnp.mean(values * values, axis=-1, keepdims=True) + EPS) * gain


def norm_back(values, gain, grad_in):
    row_scale = lax.rsqrt(jnp.mean(values * values, axis=-1, keepdims=True) + EPS)
    normed = values * row_scale
    gain_grad = jnp.sum(grad_in * normed, axis=0, keepdims=True)
    scaled = grad_in * gain
    value_grad = row_scale * (scaled - normed * jnp.mean(scaled * normed, axis=-1, keepdims=True))
    return (value_grad, gain_grad)


def rotation(length, head_size, width):
    half_size = head_size // 2
    column = (jnp.arange(width) % half_size).astype(F32)
    frequency = ROPE_BASE ** (-(column * 2.0 / head_size))
    angles = jnp.arange(length, dtype=F32)[:, None] * frequency[None, :]
    return jnp.cos(angles), jnp.sin(angles)


def silu_parts(gate):
    sig = 1.0 / (1.0 + jnp.exp(-gate))
    return sig, gate * sig


def dp_size():
    return lax.axis_size("dp")


def spot():
    return tuple(lax.axis_index(a) for a in ("section", "dp", "tensor"))


def block_of(index, size):
    return pl.ds(pl.multiple_of(index * size, size), size)


class Val:
    def __init__(self, shape, dtype):
        self.shape, self.dtype = tuple(shape), dtype
        self.ref = self.array = None


class Kernel:
    def __init__(self, cid):
        self.cid, self.ins, self.arrays, self.outs, self.room = cid, [], [], [], []
        self.early, self.steps, self.late, self.axes = [], [], [], {"tensor"}
        self.once = []

    def input(self, array):
        array = array.array if isinstance(array, Val) else array
        for val, known in zip(self.ins, self.arrays):
            if known is array:
                return val
        val = Val(array.shape, array.dtype)
        self.ins.append(val)
        self.arrays.append(array)
        return val

    def output(self, shape, dtype):
        val = Val(shape, dtype)
        self.outs.append(val)
        return val

    def vmem(self, shape, dtype):
        val = Val(shape, dtype)
        self.room.append((val, pltpu.VMEM(tuple(shape), dtype)))
        return val

    def sem(self, *shape):
        val = Val(shape, None)
        self.room.append((val, DMA(shape)))
        return val

    def do(self, *steps):
        self.steps += steps

    def body(self, *refs):
        vals = self.ins + self.outs + [val for val, _ in self.room]
        for val, ref in zip(vals, refs):
            val.ref = ref
        for item in self.once:
            item.waited = False
            item.phase = 0
        for step in self.early:
            step()
        self.greet()
        for step in self.steps + self.late:
            step()

    def greet(self):
        s, d, t = spot()
        peers = []
        if "section" in self.axes:
            peers.append({"section": 1 - s})
        if "dp" in self.axes:
            peers += [{"dp": (d + k) % dp_size()} for k in range(1, dp_size())]
        peers += [{"tensor": (t + k) % 4} for k in range(1, 4)]
        barrier = pltpu.get_barrier_semaphore()
        for peer in peers:
            pl.semaphore_signal(barrier, inc=1, device_id=peer, device_id_type=MESH)
        pl.semaphore_wait(barrier, len(peers))

    def build(self):
        result = pl.pallas_call(
            self.body,
            out_shape=[jax.ShapeDtypeStruct(v.shape, v.dtype) for v in self.outs],
            in_specs=[ANY] * len(self.ins),
            out_specs=[ANY] * len(self.outs),
            scratch_shapes=[room for _, room in self.room],
            compiler_params=pltpu.CompilerParams(
                collective_id=self.cid, has_side_effects=True, vmem_limit_bytes=VMEM_BYTES
            ),
            name=f"stage{self.cid}",
        )(*self.arrays)
        for val, array in zip(self.outs, result):
            val.array = array


def remote(src, dst, send_sem, recv_sem, peer):
    return pltpu.make_async_remote_copy(
        src_ref=src, dst_ref=dst, send_sem=send_sem, recv_sem=recv_sem,
        device_id=peer, device_id_type=MESH,
    )


class Load:
    def __init__(self, k, sources, shape, dtype, early=False):
        self.k, self.sources, self.waited = k, sources, False
        self.buf, self.sem = k.vmem(shape, dtype), k.sem(1)
        k.once.append(self)
        if early:
            k.early.append(self.start)

    def moves(self):
        for cond, source in self.sources(*spot()):
            yield cond, pltpu.make_async_copy(source, self.buf.ref, self.sem.ref.at[0])

    def start(self):
        for cond, move in self.moves():
            if cond is None:
                move.start()
            else:
                pl.when(cond)(move.start)

    def wait(self):
        if not self.waited:
            self.waited = True
            next(self.moves())[1].wait()


def load_all(k, array, early=True):
    val = k.input(array)
    return Load(k, lambda s, d, t: [(None, val.ref)], val.shape, val.dtype, early)


class Save:
    def __init__(self, k, buf):
        self.buf, self.out, self.sem = buf, k.output(buf.shape, buf.dtype), k.sem(1)
        self.waited = False
        k.once.append(self)
        k.late.append(self.wait)

    def move(self):
        return pltpu.make_async_copy(self.buf.ref, self.out.ref, self.sem.ref.at[0])

    def start(self):
        self.move().start()

    def wait(self):
        if not self.waited:
            self.waited = True
            self.move().wait()


class Task:
    final = None

    def __init__(self, k, out, axis, moves, count, n_local=1, out_dtype=BF):
        self.k, self.axis, self.make = k, axis, moves
        self.out = k.output(out, out_dtype)
        self.send_sem, self.recv_sem, self.local_sem = k.sem(count), k.sem(count), k.sem(n_local)
        self.waited = False
        k.axes.add(axis)
        k.once.append(self)

    def local(self, src, dst, i):
        return pltpu.make_async_copy(src, dst, self.local_sem.ref.at[i])

    def pairs(self, every):
        far, near = self.make(*spot())
        for i, (sources, dst, peer) in enumerate(far):
            for cond, src in sources if every else sources[:1]:
                yield cond, True, remote(
                    src, dst, self.send_sem.ref.at[i], self.recv_sem.ref.at[i], peer
                )
        for i, (sources, dst) in enumerate(near):
            for cond, src in sources if every else sources[:1]:
                yield cond, False, self.local(src, dst, i)

    def step(self):
        pass

    def send(self):
        for cond, far, move in self.pairs(True):
            if far and self.final is not None:
                cond = lax.axis_index("section") == 1 - self.final
            if cond is None:
                move.start()
            else:
                pl.when(cond)(move.start)

    def wait(self):
        if self.waited:
            return
        self.waited = True
        s = lax.axis_index("section")
        for _, far, move in self.pairs(False):
            if not far:
                move.wait()
            elif self.final is None:
                move.wait_recv()
                move.wait_send()
            else:
                pl.when(s == 1 - self.final)(move.wait_send)
                pl.when(s == self.final)(move.wait_recv)


def as_val(k, value):
    value = value.out if isinstance(value, Task) else value
    known = isinstance(value, Val) and (value.array is None)
    return value if known else k.input(value)


class Line(Task):
    def __init__(self, k, out, out_dtype=BF, n_local=1):
        super().__init__(k, out, "dp", None, 6, n_local, out_dtype)
        self.send_sem, self.recv_sem = k.sem(2, 3), k.sem(2, 3)
        self.phase = 0

    def hop(self, j, way, src, dst):
        d = lax.axis_index("dp")
        peer = {"dp": (d + 1 if way == 0 else d + 3) % 4}
        return remote(src, dst, self.send_sem.ref.at[way, j], self.recv_sem.ref.at[way, j], peer)


class LineGather(Line):
    def __init__(self, k, sources, shape, dtype):
        super().__init__(k, (4,) + shape, dtype)
        self.sources = sources

    def ends(self, j, way):
        d = lax.axis_index("dp")
        if way == 0:
            return (d >= j) & (d < 3), d >= j + 1
        return (d <= 3 - j) & (d > 0), d <= 2 - j

    def copy(self, j, way, src=None):
        d = lax.axis_index("dp")
        slot = (d + 4 - j if way == 0 else d + j) % 4
        piece = self.out.ref.at[slot]
        return self.hop(j, way, piece if src is None else src, piece)

    def send(self):
        self.phase = 0
        for cond, src in self.sources(*spot()):
            own = self.local(src, self.out.ref.at[lax.axis_index("dp")], 0)
            moves = [(True if cond is None else cond, own)]
            for way in range(2):
                sends = self.ends(0, way)[0]
                moves.append((sends if cond is None else sends & cond, self.copy(0, way, src)))
            for when, move in moves:
                if when is True:
                    move.start()
                else:
                    pl.when(when)(move.start)

    def arrive(self, j):
        for way in range(2):
            pl.when(self.ends(j, way)[1])(self.copy(j, way).wait_recv)

    def step(self):
        self.arrive(self.phase)
        self.phase += 1
        for way in range(2):
            pl.when(self.ends(self.phase, way)[0])(self.copy(self.phase, way).start)

    def wait(self):
        if self.waited:
            return
        self.waited = True
        while self.phase < 2:
            self.step()
        self.arrive(2)
        for j in range(3):
            for way in range(2):
                pl.when(self.ends(j, way)[0])(self.copy(j, way).wait_send)
        d = lax.axis_index("dp")
        self.local(self.sources(*spot())[0][1], self.out.ref.at[d], 0).wait()


def z_gather_from(k, sources, shape, dtype):
    count = dp_size()
    if count == 4:
        return LineGather(k, sources, shape, dtype)

    def moves(s, d, t):
        dst, found = task.out.ref.at[d], sources(s, d, t)
        return [(found, dst, {"dp": (d + i) % count}) for i in range(1, count)], [(found, dst)]

    task = Task(k, (count,) + shape, "dp", moves, count - 1, out_dtype=dtype)
    return task


def z_gather(k, value):
    val = as_val(k, value)
    return z_gather_from(k, lambda s, d, t: [(None, val.ref)], val.shape, val.dtype)


def z_gather_half(k, shard, moved, block):
    shard, moved = as_val(k, shard), as_val(k, moved)
    rows = shard.shape[0] // 2

    def sources(s, d, t):
        own = shard.ref.at[pl.ds(block * rows, rows)]
        return [(s == block, own), (s == 1 - block, moved.ref)]

    return z_gather_from(k, sources, moved.shape, shard.dtype)


def one_way(task, sender):
    task.final = None if sender is None else 1 - sender
    return task


def z_gather_whole(k, shard, moved, block):
    shard, moved = as_val(k, shard), as_val(k, moved)

    def sources(s, d, t):
        return [(s == block, shard.ref), (s == 1 - block, moved.ref)]

    return z_gather_from(k, sources, shard.shape, shard.dtype)


def x_move(k, value, sender=None):
    val = as_val(k, value)

    def moves(s, d, t):
        return [([(None, val.ref)], task.out.ref, {"section": 1 - s})], []

    task = Task(k, val.shape, "section", moves, 1, out_dtype=val.dtype)
    return one_way(task, sender)


def x_half(k, value, sender=None):
    val = as_val(k, value)
    rows = val.shape[0] // 2

    def moves(s, d, t):
        src = val.ref.at[block_of(1 - s, rows)]
        return [([(None, src)], task.out.ref, {"section": 1 - s})], []

    task = Task(k, (rows,) + val.shape[1:], "section", moves, 1, out_dtype=val.dtype)
    return one_way(task, sender)


def x_slots(k, value, kind):
    val, count = as_val(k, value), dp_size()
    rows = val.shape[0] // (2 * count)

    def moves(s, d, t):
        far = []
        for i in range(count):
            slot = 2 * i + 1 - s if kind == "rows" else (1 - s) * count + i
            src = val.ref.at[block_of(slot, rows)]
            far.append(([(None, src)], task.out.ref.at[i], {"section": 1 - s}))
        return far, []

    task = Task(k, (count, rows) + val.shape[1:], "section", moves, count)
    return task


class Terms:
    def __init__(self, k, kind, grads, received, local):
        self.grads, self.local = as_val(k, grads), local
        self.kind, self.n = kind, dp_size()
        self.whole = received is None
        if self.whole:
            self.rows, self.cols = self.grads.shape[0] // self.n, self.grads.shape[1]
            self.shape = (self.n, self.rows, self.cols)
            self.kept = self.total = k.vmem(self.shape, BF)
            return
        self.received = as_val(k, received)
        if kind == "cols":
            self.rows, self.cols = self.grads.shape[0] // 2, self.grads.shape[1] // self.n
            held = (self.rows, self.grads.shape[1])
        else:
            self.rows, self.cols = self.grads.shape[0] // (2 * self.n), self.grads.shape[1]
            held = (self.n, self.rows, self.cols)
        self.kept, self.got = k.vmem(held, BF), k.vmem(held, BF)
        self.shape = (self.n, self.rows, self.cols)
        self.total = k.vmem(self.shape, BF) if kind == "cols" else self.kept

    def loads(self):
        s, grads, kept = lax.axis_index("section"), self.grads.ref, self.kept.ref
        if self.whole:
            return [
                self.local(grads.at[block_of(i, self.rows)], kept.at[i], 2 + i) for i in range(self.n)
            ]
        if self.kind == "cols":
            moves = [self.local(grads.at[block_of(s, self.rows)], kept, 2)]
        else:
            moves = []
            for i in range(self.n):
                slot = 2 * i + s if self.kind == "rows" else s * self.n + i
                moves.append(self.local(grads.at[block_of(slot, self.rows)], kept.at[i], 2 + i))
        return moves + [self.local(self.received.ref, self.got.ref, 1)]

    def load(self):
        for move in self.loads():
            move.start()

    def add(self):
        for move in self.loads():
            move.wait()
        if self.whole:
            return
        kept, got, total = self.kept.ref, self.got.ref, self.total.ref
        for i in range(self.n):
            if self.kind == "cols":
                part = (slice(None), slice(i * self.cols, (i + 1) * self.cols))
            else:
                part = i
            total[i] = (kept[part].astype(F32) + got[part].astype(F32)).astype(BF)


class DirectScatter(Task):
    def __init__(self, k, kind, grads, received):
        self.terms = Terms(k, kind, grads, received, lambda *a: self.local(*a))
        count = dp_size()

        def moves(s, d, t):
            total = self.terms.total.ref
            far = []
            for i in range(1, count):
                other = (d + i) % count
                far.append(([(None, total.at[other])], self.out.ref.at[d], {"dp": other}))
            return far, [([(None, total.at[d])], self.out.ref.at[d])]

        super().__init__(k, self.terms.shape, "dp", moves, count - 1, 2 + count)
        self.load = self.terms.load

    def send(self):
        self.terms.add()
        super().send()

    def add(self):
        self.load()
        self.send()


class LineScatter(Line):
    def __init__(self, k, kind, grads, received):
        self.terms = Terms(k, kind, grads, received, lambda *a: self.local(*a))
        super().__init__(k, self.terms.shape[1:], BF, 6)
        self.got = k.vmem((2, 3) + self.terms.shape[1:], BF)
        self.load = self.terms.load

    def ends(self, j, way):
        d = lax.axis_index("dp")
        if way == 0:
            return (d <= j) & (d < 3), (d >= 1) & (d <= j + 1)
        return (d >= 3 - j) & (d > 0), (d <= 2) & (d >= 2 - j)

    def copy(self, j, way):
        d = lax.axis_index("dp")
        to = (d + 3 - j if way == 0 else d + 1 + j) % 4
        return self.hop(j, way, self.terms.total.ref.at[to], self.got.ref.at[way, j])

    def send(self):
        self.phase = 0
        self.terms.add()
        for way in range(2):
            pl.when(self.ends(0, way)[0])(self.copy(0, way).start)

    def take(self, j, way):
        d = lax.axis_index("dp")
        to = (d + 2 - j if way == 0 else d + 2 + j) % 4
        self.copy(j, way).wait_recv()
        total = self.terms.total.ref
        total[to] = (total[to].astype(F32) + self.got.ref[way, j].astype(F32)).astype(BF)

    def arrive(self, j):
        for way in range(2):
            pl.when(self.ends(j, way)[1])(functools.partial(self.take, j, way))

    def step(self):
        self.arrive(self.phase)
        self.phase += 1
        for way in range(2):
            pl.when(self.ends(self.phase, way)[0])(self.copy(self.phase, way).start)

    def wait(self):
        if self.waited:
            return
        self.waited = True
        while self.phase < 2:
            self.step()
        self.arrive(2)
        done = self.local(self.terms.total.ref.at[lax.axis_index("dp")], self.out.ref, 0)
        done.start()
        for j in range(3):
            for way in range(2):
                pl.when(self.ends(j, way)[0])(self.copy(j, way).wait_send)
        done.wait()

    def add(self):
        self.load()
        self.send()


def sum_scatter(k, kind, grads, received=None):
    return (LineScatter if dp_size() == 4 else DirectScatter)(k, kind, grads, received)


class Finish(Task):
    def __init__(self, k, pieces, block):
        self.pieces, self.final = as_val(k, pieces), block
        *slots, rows, cols = self.pieces.shape
        self.slots = slots[0] if slots else 0
        if slots:
            self.held, self.total = k.vmem(self.pieces.shape, BF), k.vmem((rows, cols), BF)
        else:
            self.total = self.pieces

        def moves(s, d, t):
            source, dst = [(None, self.total.ref)], self.out.ref.at[s]
            return [(source, dst, {"section": 1 - s})], [(source, dst)]

        super().__init__(k, (2, rows, cols), "section", moves, 1, 2)

    def load(self):
        if self.slots:
            self.local(self.pieces.ref, self.held.ref, 1).start()

    def send(self):
        if self.slots:
            self.local(self.pieces.ref, self.held.ref, 1).wait()
            acc = self.held.ref[0].astype(F32)
            for i in range(1, self.slots):
                acc = acc + self.held.ref[i].astype(F32)
            self.total.ref[...] = acc.astype(BF)
        super().send()

    def add(self):
        self.load()
        self.send()


class SumShare(Task):
    def __init__(self, k, terms, axis, slotted=False):
        self.terms = [as_val(k, v) for v in terms]
        shape = self.terms[0].shape[1:] if slotted else self.terms[0].shape
        count = dp_size() if axis == "dp" else 4
        self.slotted = slotted
        self.bufs = [k.vmem(v.shape, F32) for v in self.terms]
        self.total = k.vmem(shape, F32)

        def moves(s, d, t):
            source, me = [(None, self.total.ref)], d if axis == "dp" else t
            dst = self.out.ref.at[me]
            far = [(source, dst, {axis: (me + i) % count}) for i in range(1, count)]
            return far, [(source, dst)]

        super().__init__(k, (count,) + shape, axis, moves, count - 1, 3, out_dtype=F32)

    def add(self):
        loads = [self.local(v.ref, b.ref, 1 + i) for i, (v, b) in enumerate(zip(self.terms, self.bufs))]
        for load in loads:
            load.start()
        for load in loads:
            load.wait()
        if self.slotted:
            parts = [self.bufs[0].ref[i] for i in range(self.terms[0].shape[0])]
        else:
            parts = [buf.ref[...] for buf in self.bufs]
        acc = parts[0]
        for part in parts[1:]:
            acc = acc + part
        self.total.ref[...] = acc
        self.send()


class Weight:
    def __init__(self, k, kind, near, far=None, early=False):
        near, far = as_val(k, near), None if far is None else as_val(k, far)
        self.count, self.rows, self.cols = near.shape
        self.kind, self.near, self.far, self.waited = kind, near, far, False
        sides = 1 if far is None else 2
        if kind == "cols":
            shape = (sides * self.rows, self.count * self.cols)
        else:
            shape = (sides * self.count * self.rows, self.cols)
        self.aside = kind == "cols" and self.cols % 128 != 0
        self.buf, self.sem = k.vmem(shape, BF), k.sem(2 * self.count)
        if self.aside:
            self.held = [k.vmem(near.shape, BF), k.vmem(near.shape, BF)]
        k.once.append(self)
        if early:
            k.early.append(self.start)

    def moves(self):
        s, dst = lax.axis_index("section"), self.buf.ref
        rows, cols = self.rows, self.cols

        def place(sec, own):
            if self.aside:
                return None
            if self.kind == "cols":
                return dst.at[block_of(sec, rows), pl.ds(own * cols, cols)]
            slot = own * 2 + sec if self.kind == "rows" else sec * self.count + own
            return dst.at[block_of(slot, rows)]

        if self.far is None:
            for i in range(self.count):
                if self.kind == "cols":
                    to = dst.at[:, pl.ds(i * cols, cols)]
                else:
                    to = dst.at[pl.ds(i * rows, rows)]
                to = self.held[0].ref.at[i] if self.aside else to
                yield pltpu.make_async_copy(self.near.ref.at[i], to, self.sem.ref.at[2 * i])
            return
        for i in range(self.count):
            for j, (val, sec) in enumerate(((self.near, s), (self.far, 1 - s))):
                to = self.held[j].ref.at[i] if self.aside else place(sec, i)
                yield pltpu.make_async_copy(val.ref.at[i], to, self.sem.ref.at[2 * i + j])

    def start(self):
        for move in self.moves():
            move.start()

    def wait(self):
        if self.waited:
            return
        self.waited = True
        for move in self.moves():
            move.wait()
        if self.aside:
            s = lax.axis_index("section")
            for j, sec in enumerate((s, 1 - s) if self.far is not None else (0,)):
                whole = jnp.concatenate([self.held[j].ref[i] for i in range(self.count)], axis=1)
                self.buf.ref[block_of(sec, self.rows), :] = whole


class Product:
    def __init__(self, k, left, right):
        self.left, self.right = left, right
        rows = left.shape[1]
        self.chunk = 384 if rows % 384 == 0 else 256
        self.count = rows // self.chunk
        self.buf = k.vmem((rows, right.shape[1]), BF)
        self.out, self.sem = k.output(self.buf.shape, BF), k.sem(self.count)

    def copy(self, i):
        part = block_of(i, self.chunk)
        return pltpu.make_async_copy(self.buf.ref.at[part], self.out.ref.at[part], self.sem.ref.at[i])

    def run(self):
        def step(i, carry):
            part = block_of(i, self.chunk)
            value = contract(self.left.ref[:, part], self.right.ref[...], 0, 0)
            self.buf.ref[part, :] = value.astype(BF)
            self.copy(i).start()
            return carry

        lax.fori_loop(0, self.count, step, 0)

    def wait(self):
        for i in range(self.count):
            self.copy(i).wait()


def places():
    me = lax.axis_index("tensor")
    sib = me + 1 - 2 * (me % 2)
    cross = (me + 2) % 4
    diag = (sib + 2) % 4
    return me, sib, cross, diag


class Gather:
    def __init__(self, k, x, gain, weights, extras=(), trans=False, epilogue="plain", save=()):
        rows, width = x.shape
        length = 4 * rows
        self.k, self.x, self.gain, self.weights, self.extras = k, x, gain, weights, extras
        self.trans, self.epilogue, self.rows, self.half = trans, epilogue, rows, rows // 2
        cols = [w.buf.shape[0 if trans else 1] for w in weights]
        kinds = {
            "plain": [(c, F32) for c in cols],
            "ffn": [(cols[0], BF)] * 3,
            "ffn_back": [(cols[0], BF)] * 2,
        }[epilogue]
        self.full = k.vmem((length, width), BF)
        self.values = [k.vmem((length, c), kind) for c, kind in kinds]
        kept = [self.full] + self.values
        self.saved = [(v, k.output(v.shape, v.dtype), k.sem(4, 2)) for v in kept if kept.index(v) in save]
        self.sems = [k.sem(2) for _ in range(6)]
        k.late.append(self.end)

    def span(self, owner, sub):
        return pl.ds(pl.multiple_of(owner * self.rows + sub * self.half, self.half), self.half)

    def move(self, kind, i):
        me, sib, cross, _ = places()
        full = self.full.ref
        owner, peer, at = {"cross": (me, cross, 0), "sib": (me, sib, 2), "relay": (cross, sib, 4)}[kind]
        part = full.at[self.span(owner, i)]
        return remote(
            part, part, self.sems[at].ref.at[i], self.sems[at + 1].ref.at[i], {"tensor": peer}
        )

    def begin(self):
        me = places()[0]
        for i in range(2):
            part = self.x.ref[pl.ds(i * self.half, self.half), :].astype(F32)
            if self.gain is not None:
                val, row = self.gain
                part = norm_rows(part, val.ref[row : row + 1, :])
            self.full.ref[self.span(me, i), :] = part.astype(BF)
            self.move("cross", i).start()
            self.move("sib", i).start()

    def loop(self):
        me, sib, cross, diag = places()
        rows, half = self.rows, self.half
        for w in self.weights:
            w.wait()

        def step(p, carry):
            far, sub = p // 2, p % 2
            near = (1 - sub) * me + sub * sib
            first = (1 - far) * near * rows + far * (cross * rows + sub * half)
            second = (1 - far) * (near * rows + half) + far * (diag * rows + sub * half)
            pair = [pl.ds(pl.multiple_of(v, half), half) for v in (first, second)]

            @pl.when(p == 1)
            def _():
                self.move("sib", 0).wait_recv()
                self.move("sib", 1).wait_recv()

            for i in range(2):

                @pl.when(p == 2 + i)
                def _():
                    self.move("cross", i).wait_recv()
                    self.move("relay", i).start()
                    self.move("relay", i).wait_recv()

            def both(val):
                return jnp.concatenate([val.ref[pair[0], :], val.ref[pair[1], :]], axis=0)

            a = both(self.full)
            prods = [contract(a, w.buf.ref[...], 1, 1 if self.trans else 0) for w in self.weights]
            if self.epilogue == "plain":
                values = prods
            elif self.epilogue == "ffn":
                sig, silu = silu_parts(prods[0])
                values = [prods[0], prods[1], silu * prods[1]]
            else:
                gate, up = (both(v).astype(F32) for v in self.extras)
                sig, silu = silu_parts(gate)
                values = [prods[0] * up * sig * (1.0 + gate * (1.0 - sig)), prods[0] * silu]
            for val, value in zip(self.values, values):
                value = value.astype(val.dtype)
                for j in range(2):
                    val.ref[pair[j], :] = value[j * half : (j + 1) * half]
            for val, out, sem in self.saved:
                for j in range(2):
                    pltpu.make_async_copy(
                        val.ref.at[pair[j]], out.ref.at[pair[j]], sem.ref.at[p, j]
                    ).start()
            return carry

        lax.fori_loop(0, 4, step, 0)

    def end(self):
        for i in range(2):
            for kind in ("cross", "sib", "relay"):
                self.move(kind, i).wait_send()
        part = pl.ds(0, self.half)
        for val, out, sem in self.saved:
            for p in range(4):
                for j in range(2):
                    pltpu.make_async_copy(val.ref.at[part], out.ref.at[part], sem.ref.at[p, j]).wait()


class Scatter:
    def __init__(self, k, operands, weights, resid, back=None, trans=False, low=False):
        rows, width = resid.shape
        half = rows // 2
        self.operands, self.weights, self.resid, self.back = operands, weights, resid, back
        self.trans, self.low, self.rows, self.half = trans, low, rows, half
        self.keep, self.own = k.vmem((2, half, width), F32), k.vmem((rows, width), F32)
        self.to_s, self.from_s, self.to_c, self.from_c = (
            k.vmem((2, half, width), BF) for _ in range(4)
        )
        self.to_o, self.from_o = k.vmem((rows, width), BF), k.vmem((rows, width), BF)
        self.out = k.vmem((rows, width), BF if low else F32)
        self.gain_grad = k.vmem((1, width), F32) if back else None
        self.sems = [k.sem(2) for _ in range(4)] + [k.sem(1) for _ in range(2)]
        k.late.append(self.end)

    def move(self, kind, i=0):
        _, sib, cross, _ = places()
        at, src, dst, peer = {
            "diag": (0, self.to_s, self.from_s, sib),
            "cross": (2, self.to_c, self.from_c, cross),
            "near": (4, self.to_o, self.from_o, sib),
        }[kind]
        src, dst = (src.ref, dst.ref) if kind == "near" else (src.ref.at[i], dst.ref.at[i])
        return remote(
            src, dst, self.sems[at].ref.at[i], self.sems[at + 1].ref.at[i], {"tensor": peer}
        )

    def pass_on(self, i):
        self.move("diag", i).wait_recv()
        total = self.keep.ref[i] + self.from_s.ref[i].astype(F32)
        self.to_c.ref[i] = total.astype(BF)
        self.move("cross", i).start()

    def loop(self):
        me, sib, cross, diag = places()
        rows, half = self.rows, self.half
        for w in self.weights:
            w.wait()

        def step(p, carry):
            near, sub = p // 2, p % 2
            base = near * ((1 - sub) * sib + sub * me) * rows
            first = base + (1 - near) * (cross * rows + sub * half)
            second = base + near * half + (1 - near) * (diag * rows + sub * half)
            pair = [pl.ds(pl.multiple_of(v, half), half) for v in (first, second)]
            total = None
            for y, w in zip(self.operands, self.weights):
                a = jnp.concatenate([y.ref[pair[0], :], y.ref[pair[1], :]], axis=0)
                prod = contract(a, w.buf.ref[...], 1, 1 if self.trans else 0)
                total = prod if total is None else total + prod

            for i in range(2):

                @pl.when(p == i)
                def _():
                    self.keep.ref[i] = total[:half]
                    self.to_s.ref[i] = total[half:].astype(BF)
                    self.move("diag", i).start()

            @pl.when(p == 1)
            def _():
                self.pass_on(0)

            @pl.when(p == 2)
            def _():
                self.to_o.ref[...] = total.astype(BF)
                self.move("near").start()
                self.pass_on(1)

            @pl.when(p == 3)
            def _():
                self.own.ref[...] = total

            return carry

        lax.fori_loop(0, 4, step, 0)

    def finish(self):
        self.move("near").wait_recv()
        gain_sum = None
        for i in range(2):
            part = pl.ds(i * self.half, self.half)
            self.move("cross", i).wait_recv()
            total = self.own.ref[part, :] + self.from_o.ref[part, :].astype(F32)
            total = total + self.from_c.ref[i].astype(F32)
            resid = self.resid.ref[part, :].astype(F32)
            if self.back:
                value, (gain, row) = self.back
                value_grad, gain_grad = norm_back(
                    value.ref[part, :].astype(F32), gain.ref[row : row + 1, :], total
                )
                total = value_grad
                gain_sum = gain_grad if gain_sum is None else gain_sum + gain_grad
            self.out.ref[part, :] = (resid + total).astype(self.out.dtype)
        if self.back:
            self.gain_grad.ref[...] = gain_sum

    def end(self):
        self.move("near").wait_send()
        for i in range(2):
            self.move("diag", i).wait_send()
            self.move("cross", i).wait_send()


def delayed(values, by):
    if by == 0:
        return values
    row = lax.broadcasted_iota(jnp.int32, values.shape, 0)
    return jnp.where(row < by, 0.0, pltpu.roll(values, by, 0))


def advanced(values, by):
    if by == 0:
        return values
    length = values.shape[0]
    row = lax.broadcasted_iota(jnp.int32, values.shape, 0)
    return jnp.where(row >= length - by, 0.0, pltpu.roll(values, length - by, 0))


CONV_COLS = 128


class Conv:
    def __init__(self, k, projected, value, kernel):
        self.projected, self.value, self.kernel = projected, value, kernel
        self.y = k.vmem(value.shape, BF)

    def parts(self, j):
        channels = self.value.shape[1]
        at = slice(j * CONV_COLS, (j + 1) * CONV_COLS)
        b_gate = self.projected.ref[:, at]
        c_gate = self.projected.ref[:, channels + at.start : channels + at.stop]
        x_value, taps = self.value.ref[:, at], self.kernel.ref[:, at]
        product = b_gate * x_value
        count = taps.shape[0]
        causal = jnp.zeros_like(product)
        for i in range(count):
            causal = causal + taps[i : i + 1] * delayed(product, count - 1 - i)
        return at, b_gate, c_gate, x_value, taps, product, causal

    def run(self):
        for j in range(self.value.shape[1] // CONV_COLS):
            at, _, c_gate, _, _, _, causal = self.parts(j)
            self.y.ref[:, at] = (c_gate * causal).astype(BF)


class ConvBack(Conv):
    def __init__(self, k, projected, value, kernel, d_y):
        self.projected, self.value, self.kernel, self.d_y = projected, value, kernel, d_y
        self.d_proj = k.vmem(projected.shape, BF)
        self.d_value = k.vmem(value.shape, BF)
        self.d_kernel = k.vmem(kernel.shape, F32)

    def run(self):
        channels = self.value.shape[1]
        for j in range(channels // CONV_COLS):
            at, b_gate, c_gate, x_value, taps, product, causal = self.parts(j)
            d_y = self.d_y.ref[:, at]
            d_causal = d_y * c_gate
            count = taps.shape[0]
            d_product = jnp.zeros_like(product)
            for i in range(count):
                by = count - 1 - i
                row = jnp.sum(d_causal * delayed(product, by), axis=0, keepdims=True)
                self.d_kernel.ref[i : i + 1, at] = row
                d_product = d_product + taps[i : i + 1] * advanced(d_causal, by)
            self.d_proj.ref[:, at] = (d_product * x_value).astype(BF)
            self.d_proj.ref[:, channels + at.start : channels + at.stop] = (d_y * causal).astype(BF)
            self.d_value.ref[:, at] = (d_product * b_gate).astype(BF)


def head_mean(values, head_size):
    width = values.shape[1]
    row = lax.broadcasted_iota(jnp.int32, (width, width), 0) // head_size
    col = lax.broadcasted_iota(jnp.int32, (width, width), 1) // head_size
    group = jnp.where(row == col, 1.0 / head_size, 0.0).astype(F32)
    return lax.dot_general(
        values, group, (((1,), (0,)), ((), ())),
        precision=lax.Precision.HIGHEST, preferred_element_type=F32,
    )


def turn(values, head_size, back):
    width, half = values.shape[1], head_size // 2
    lane = lax.broadcasted_iota(jnp.int32, values.shape, 1) % head_size
    upper = pltpu.roll(values, width - half, 1)
    lower = pltpu.roll(values, half, 1)
    return jnp.where(lane < half, upper, -lower) if back else jnp.where(lane < half, -upper, lower)


def head_norm(values, gain, head_size):
    return values * lax.rsqrt(head_mean(values * values, head_size) + EPS) * gain


def head_norm_back(values, gain, grad_in, head_size):
    row_scale = lax.rsqrt(head_mean(values * values, head_size) + EPS)
    normed = values * row_scale
    gain_grad = jnp.sum(grad_in * normed, axis=0, keepdims=True)
    scaled = grad_in * gain
    return row_scale * (scaled - normed * head_mean(scaled * normed, head_size)), gain_grad


def block_weights(q_rows, k_rows, first_row):
    rows, length = q_rows.shape[0], k_rows.shape[0]
    scores = contract(q_rows, k_rows, 1, 1) * (q_rows.shape[1] ** -0.5)
    query = first_row + lax.broadcasted_iota(jnp.int32, (rows, length), 0)
    key = lax.broadcasted_iota(jnp.int32, (rows, length), 1)
    scores = jnp.where(key <= query, scores, MASKED)
    exps = jnp.exp(scores - jnp.max(scores, axis=1, keepdims=True))
    return exps * (1.0 / jnp.sum(exps, axis=1, keepdims=True))


class Heads:
    def __init__(self, projected, tables, size):
        self.projected, self.size = projected, size
        self.gain, self.cos, self.sin = (v.buf for v in tables)
        self.loads = tables
        self.length, width = projected.shape
        self.q_cols, self.k_cols = width // 2, width // 4
        self.heads, self.kv_heads = self.q_cols // size, self.k_cols // size
        self.share = self.heads // self.kv_heads

    def per_head(self, k, count, kind):
        return k.vmem((count, self.length, self.size), kind)

    def split(self, val, rows, values):
        for h in range(val.shape[0]):
            val.ref[h, rows, :] = values[:, h * self.size : (h + 1) * self.size]

    def join(self, val, rows):
        return jnp.concatenate([val.ref[h, rows, :] for h in range(val.shape[0])], axis=1)

    def angles(self, rows):
        c, n = self.cos.ref[rows, :], self.sin.ref[rows, :]
        repeat = self.q_cols // c.shape[1]
        return jnp.concatenate([c] * repeat, axis=1), jnp.concatenate([n] * repeat, axis=1)

    def blocks(self, step):
        lax.fori_loop(0, self.length // ROW_BLOCK, lambda p, c: step(block_of(p, ROW_BLOCK)) or c, 0)


class Attend(Heads):
    def __init__(self, k, projected, tables, size):
        super().__init__(projected, tables, size)
        self.q_rot = k.vmem((self.length, self.q_cols), BF)
        self.k_rot = k.vmem((self.length, self.k_cols), BF)
        self.y = k.vmem((self.length, self.q_cols), BF)
        self.q_h, self.y_h = (self.per_head(k, self.heads, BF) for _ in range(2))
        self.k_h, self.v_h = (self.per_head(k, self.kv_heads, BF) for _ in range(2))

    def run(self, *between):
        for load in self.loads:
            load.wait()
        size, q_cols, k_cols, proj = self.size, self.q_cols, self.k_cols, self.projected.ref

        def prepare(rows):
            c, n = self.angles(rows)
            q = head_norm(proj[rows, :q_cols], self.gain.ref[0:1, :], size)
            q = (q * c + turn(q, size, False) * n).astype(BF)
            k = head_norm(proj[rows, q_cols : q_cols + k_cols], self.gain.ref[1:2, :k_cols], size)
            k = (k * c[:, :k_cols] + turn(k, size, False) * n[:, :k_cols]).astype(BF)
            self.q_rot.ref[rows, :] = q
            self.k_rot.ref[rows, :] = k
            self.split(self.q_h, rows, q)
            self.split(self.k_h, rows, k)
            self.split(self.v_h, rows, proj[rows, q_cols + k_cols :].astype(BF))

        self.blocks(prepare)

        def head(h, carry):
            g = h // self.share
            for i in range(self.length // ROW_BLOCK):
                rows, seen = pl.ds(i * ROW_BLOCK, ROW_BLOCK), pl.ds(0, (i + 1) * ROW_BLOCK)
                weights = block_weights(
                    self.q_h.ref[h, rows, :], self.k_h.ref[g, seen, :], i * ROW_BLOCK
                )
                value = contract(weights.astype(BF), self.v_h.ref[g, seen, :], 1, 0)
                self.y_h.ref[h, rows, :] = value.astype(BF)
            return carry

        lax.fori_loop(0, self.heads // 2, head, 0)
        for step in between:
            step()
        lax.fori_loop(self.heads // 2, self.heads, head, 0)
        self.y.ref[...] = self.join(self.y_h, slice(None))


class AttendBack(Heads):
    def __init__(self, k, projected, tables, size, q_rot, k_rot, d_y):
        super().__init__(projected, tables, size)
        self.q_rot, self.k_rot, self.d_y = q_rot, k_rot, d_y
        self.q_h, self.dy_h = (self.per_head(k, self.heads, BF) for _ in range(2))
        self.k_h, self.v_h = (self.per_head(k, self.kv_heads, BF) for _ in range(2))
        self.dq_h = self.per_head(k, self.heads, F32)
        self.dk_h, self.dv_h = (self.per_head(k, self.kv_heads, F32) for _ in range(2))
        self.d_proj = k.vmem(projected.shape, BF)
        self.q_gain, self.k_gain = k.vmem((1, self.q_cols), F32), k.vmem((1, self.k_cols), F32)

    def run(self, *between):
        for load in self.loads:
            load.wait()
        size, q_cols, k_cols, proj = self.size, self.q_cols, self.k_cols, self.projected.ref
        scale = size**-0.5
        dq_h, dk_h, dv_h = self.dq_h.ref, self.dk_h.ref, self.dv_h.ref

        def prepare(rows):
            self.split(self.q_h, rows, self.q_rot.ref[rows, :])
            self.split(self.dy_h, rows, self.d_y.ref[rows, :].astype(BF))
            self.split(self.k_h, rows, self.k_rot.ref[rows, :])
            self.split(self.v_h, rows, proj[rows, q_cols + k_cols :].astype(BF))

        self.blocks(prepare)
        dk_h[...] = jnp.zeros_like(dk_h)
        dv_h[...] = jnp.zeros_like(dv_h)

        def head(h, carry):
            g = h // self.share
            for i in range(self.length // ROW_BLOCK):
                rows, seen = pl.ds(i * ROW_BLOCK, ROW_BLOCK), pl.ds(0, (i + 1) * ROW_BLOCK)
                q, low = self.q_h.ref[h, rows, :], self.dy_h.ref[h, rows, :]
                k = self.k_h.ref[g, seen, :]
                prob = block_weights(q, k, i * ROW_BLOCK)
                d_weights = contract(low, self.v_h.ref[g, seen, :], 1, 1)
                dv_h[g, seen, :] += contract(prob.astype(BF), low, 0, 0)
                inner = jnp.sum(prob * d_weights, axis=1, keepdims=True)
                d_scores = (prob * (d_weights - inner)).astype(BF)
                dq_h[h, rows, :] = contract(d_scores, k, 1, 0) * scale
                dk_h[g, seen, :] += contract(d_scores, q, 0, 0) * scale
            return carry

        lax.fori_loop(0, self.heads // 2, head, 0)
        for step in between:
            step()
        lax.fori_loop(self.heads // 2, self.heads, head, 0)
        self.q_gain.ref[...] = jnp.zeros_like(self.q_gain.ref)
        self.k_gain.ref[...] = jnp.zeros_like(self.k_gain.ref)

        def finish(rows):
            c, n = self.angles(rows)
            dq, dk, dv = (self.join(v, rows) for v in (self.dq_h, self.dk_h, self.dv_h))
            dq = dq * c + turn(dq * n, size, True)
            dk = dk * c[:, :k_cols] + turn(dk * n[:, :k_cols], size, True)
            dq, q_sum = head_norm_back(proj[rows, :q_cols], self.gain.ref[0:1, :], dq, size)
            dk, k_sum = head_norm_back(
                proj[rows, q_cols : q_cols + k_cols], self.gain.ref[1:2, :k_cols], dk, size
            )
            self.q_gain.ref[...] += q_sum
            self.k_gain.ref[...] += k_sum
            self.d_proj.ref[rows, :q_cols] = dq.astype(BF)
            self.d_proj.ref[rows, q_cols : q_cols + k_cols] = dk.astype(BF)
            self.d_proj.ref[rows, q_cols + k_cols :] = dv.astype(BF)

        self.blocks(finish)


def body(boundary, norm_gain, mix_in, mix_out, w_gate, w_up, w_down, conv_x, conv_kernel, qk_gain):
    first = lax.axis_index("section") == 0
    tensor_index = lax.axis_index("tensor")
    model_width = boundary.shape[3]
    channels = mix_out.shape[1]
    row_shape = boundary.shape[2:]
    length, size = 4 * row_shape[0], qk_gain.shape[1]

    seqs, own_gain = boundary[0], norm_gain[0]
    sh_in, sh_out, sh_gate, sh_up, sh_down = (v[0] for v in (mix_in, mix_out, w_gate, w_up, w_down))
    table_arrays = [jnp.tile(qk_gain, (1, channels // size)), *rotation(length, size, 128)]

    def gains_of(k, block, other, early=True):
        own, moved = k.input(own_gain), as_val(k, other)
        sources = lambda s, d, t: [(s == block, own.ref), (s == 1 - block, moved.ref)]
        return Load(k, sources, own.shape, F32, early)

    def start_rows(k, slot, other, early=True):
        own, moved = k.input(seqs), as_val(k, other)
        sources = lambda s, d, t: [(s == slot, own.ref.at[slot]), (s == 1 - slot, moved.ref)]
        return Load(k, sources, row_shape, BF, early)

    def wait(*items):
        return [item.wait for item in items]

    k = Kernel(0)
    t_seq = None
    seq_val = k.input(seqs)

    def seq_moves(s, d, t):
        return [([(None, seq_val.ref.at[1 - s])], t_seq.out.ref, {"section": 1 - s})], []

    t_in, t_out, t_up = (x_half(k, v) for v in (sh_in, sh_out, sh_up))
    t_gate0, t_down0 = x_move(k, sh_gate, 0), x_half(k, sh_down, 0)
    t_gate1, t_down1 = x_half(k, sh_gate, 1), x_move(k, sh_down, 1)
    t_seq = Task(k, row_shape, "section", seq_moves, 1)
    t_gain, z_cols = x_move(k, own_gain), z_gather(k, conv_x)
    z_in0, z_out0 = z_gather_half(k, sh_in, t_in.out, 0), z_gather_half(k, sh_out, t_out.out, 0)
    z_gate0 = z_gather_whole(k, sh_gate, t_gate0.out, 0)
    z_up0 = z_gather_half(k, sh_up, t_up.out, 0)
    x_cols, x_in0, x_out0 = (x_move(k, v.out) for v in (z_cols, z_in0, z_out0))
    x_load, gain_load = start_rows(k, 0, t_seq.out, False), gains_of(k, 0, t_gain.out, False)
    taps = load_all(k, conv_kernel)
    w_in0, w_cols = Weight(k, "rows", z_in0.out, x_in0.out), Weight(k, "conv", z_cols.out, x_cols.out)
    w_out0 = Weight(k, "cols", z_out0.out, x_out0.out)
    g0 = Gather(k, x_load.buf, (gain_load.buf, 0), [w_in0, w_cols], save=(0, 1, 2))
    conv = Conv(k, g0.values[0], g0.values[1], taps.buf)
    y0 = Save(k, conv.y)
    s1 = Scatter(k, [conv.y], [w_out0], x_load.buf)
    mid0 = Save(k, s1.out)
    k.do(t_in.send, t_out.send, z_cols.send, t_gate0.send, t_gate1.send, t_gain.send, t_seq.send)
    k.do(t_in.wait, z_in0.send, t_out.wait, z_out0.send, t_up.send)
    k.do(z_cols.step, z_in0.step, z_out0.step, t_gate0.wait, z_gate0.send)
    k.do(z_cols.step, z_in0.step, z_out0.step)
    k.do(t_gain.wait, gain_load.start, t_seq.wait, x_load.start)
    k.do(gain_load.wait, x_load.wait, g0.begin)
    k.do(z_cols.wait, x_cols.send, z_in0.wait, x_in0.send, z_out0.wait, x_out0.send)
    k.do(t_down0.send, t_down1.send, t_up.wait, z_up0.send, z_gate0.step, z_up0.step)
    k.do(x_cols.wait, w_cols.start, x_in0.wait, w_in0.start, z_gate0.step)
    k.do(g0.loop, taps.wait, conv.run, y0.start)
    k.do(z_up0.step, x_out0.wait, w_out0.start, s1.loop, s1.finish, mid0.start)
    k.do(*wait(t_gate1, t_down0, t_down1, z_gate0, z_up0))
    k.build()
    a0, proj0, value0 = (out for _, out, _ in g0.saved)
    y0, mid0 = y0.out, mid0.out

    k = Kernel(1)
    x_up0, z_down0 = x_move(k, z_up0.out), z_gather_half(k, sh_down, t_down0.out, 0)
    z_in1, z_out1 = z_gather_half(k, sh_in, t_in.out, 1), z_gather_half(k, sh_out, t_out.out, 1)
    z_gate1 = z_gather_half(k, sh_gate, t_gate1.out, 1)
    x_down0, x_in1, x_out1 = (x_move(k, v.out) for v in (z_down0, z_in1, z_out1))
    rows, gain_load = load_all(k, mid0), gains_of(k, 0, t_gain.out)
    w_gate0 = Weight(k, "rows", z_gate0.out, None, True)
    w_up0 = Weight(k, "rows", z_up0.out, x_up0.out)
    w_down0 = Weight(k, "cols", z_down0.out, x_down0.out)
    g2 = Gather(
        k, rows.buf, (gain_load.buf, 1), [w_gate0, w_up0], epilogue="ffn", save=(0, 1, 2, 3)
    )
    s3 = Scatter(k, [g2.values[2]], [w_down0], rows.buf, low=True)
    z_rows = Save(k, s3.out)
    k.do(x_up0.send, z_down0.send, z_in1.send, z_out1.send)
    k.do(rows.wait, gain_load.wait, g2.begin)
    k.do(z_down0.step, z_in1.step, z_out1.step, z_down0.step, z_gate1.send, z_in1.step, z_out1.step)
    k.do(z_down0.wait, x_down0.send, x_up0.wait, w_up0.start, z_gate1.step, g2.loop)
    k.do(z_gate1.step, z_in1.wait, x_in1.send, z_out1.wait, x_out1.send)
    k.do(x_down0.wait, w_down0.start, s3.loop, s3.finish, z_rows.start)
    k.do(*wait(x_in1, x_out1, z_gate1))
    k.build()
    m0, gate0, up0, hid0 = (out for _, out, _ in g2.saved)
    z_rows = z_rows.out

    k = Kernel(2)
    x_gate1, z_up1 = x_move(k, z_gate1.out), z_gather_half(k, sh_up, t_up.out, 1)
    z_down1, x_up1 = z_gather_whole(k, sh_down, t_down1.out, 1), x_move(k, z_up1.out)
    rows, gain_load = load_all(k, z_rows), gains_of(k, 1, t_gain.out)
    tables = [load_all(k, v) for v in table_arrays]
    w_in1 = Weight(k, "rows", z_in1.out, x_in1.out, True)
    w_out1 = Weight(k, "cols", z_out1.out, x_out1.out, True)
    g4 = Gather(k, rows.buf, (gain_load.buf, 0), [w_in1], save=(0, 1))
    attend = Attend(k, g4.values[0], tables, size)
    kept = [Save(k, v) for v in (attend.q_rot, attend.k_rot, attend.y)]
    s5 = Scatter(k, [attend.y], [w_out1], rows.buf)
    mid1 = Save(k, s5.out)
    k.do(x_gate1.send, z_up1.send, z_down1.send)
    k.do(rows.wait, gain_load.wait, g4.begin, z_up1.step, g4.loop, z_up1.step)
    k.do(lambda: attend.run(z_up1.wait, x_up1.send, z_down1.step))
    k.do(*(v.start for v in kept))
    k.do(s5.loop, z_down1.step, s5.finish, mid1.start)
    k.do(*wait(x_gate1, x_up1, z_down1))
    k.build()
    a1, proj1 = (out for _, out, _ in g4.saved)
    q_rot, k_rot, y1 = (v.out for v in kept)
    mid1 = mid1.out

    k = Kernel(3)
    rows, gain_load = load_all(k, mid1), gains_of(k, 1, t_gain.out)
    cot = start_rows(k, 1, t_seq.out)
    w_gate1 = Weight(k, "rows", z_gate1.out, x_gate1.out, True)
    w_up1 = Weight(k, "rows", z_up1.out, x_up1.out, True)
    w_down1 = Weight(k, "cols", z_down1.out, None, True)
    g6 = Gather(k, rows.buf, (gain_load.buf, 1), [w_gate1, w_up1], epilogue="ffn")
    g8 = Gather(
        k, cot.buf, None, [w_down1], [g6.values[0], g6.values[1]], trans=True, epilogue="ffn_back"
    )
    p_down1 = Product(k, g6.values[2], g8.full)
    p_gate1, p_up1 = Product(k, g6.full, g8.values[0]), Product(k, g6.full, g8.values[1])
    r_down1 = x_half(k, p_down1.out)
    s7 = Scatter(k, [g6.values[2]], [w_down1], rows.buf, low=True)
    s9 = Scatter(k, g8.values, [w_gate1, w_up1], cot.buf, (rows.buf, (gain_load.buf, 1)), True)
    y_rows, d_mid1, gain11 = Save(k, s7.out), Save(k, s9.out), Save(k, s9.gain_grad)
    k.do(rows.wait, gain_load.wait, g6.begin, cot.wait, g8.begin, g6.loop)
    k.do(g8.loop, p_down1.run, p_down1.wait, r_down1.send)
    k.do(s9.loop, s7.loop, p_gate1.run, p_up1.run, s9.finish, d_mid1.start, gain11.start)
    k.do(s7.finish, y_rows.start, p_gate1.wait, p_up1.wait)
    k.do(*wait(r_down1))
    k.build()
    y_rows, d_mid1, gain11 = y_rows.out, d_mid1.out, gain11.out

    k = Kernel(4)
    q_down1 = sum_scatter(k, "cols", p_down1.out, r_down1.out)
    r_gate1, q_up1 = x_slots(k, p_gate1.out, "rows"), sum_scatter(k, "rows", p_up1.out)
    rows, gain_load = load_all(k, d_mid1), gains_of(k, 1, t_gain.out)
    value = load_all(k, z_rows)
    tables = [load_all(k, v) for v in table_arrays]
    proj, q_load, k_load, y_load, a_load = (load_all(k, v) for v in (proj1, q_rot, k_rot, y1, a1))
    w_in1 = Weight(k, "rows", z_in1.out, x_in1.out, True)
    w_out1 = Weight(k, "cols", z_out1.out, x_out1.out, True)
    g10 = Gather(k, rows.buf, None, [w_out1], trans=True)
    p_out1 = Product(k, y_load.buf, g10.full)
    back = AttendBack(k, proj.buf, tables, size, q_load.buf, k_load.buf, g10.values[0])
    p_in1 = Product(k, a_load.buf, back.d_proj)
    r_out1 = x_half(k, p_out1.out)
    s11 = Scatter(
        k, [back.d_proj], [w_in1], rows.buf, (value.buf, (gain_load.buf, 0)), True, low=True
    )
    d_z, gain10 = Save(k, s11.out), Save(k, s11.gain_grad)
    head_gains = [Save(k, back.q_gain), Save(k, back.k_gain)]
    k.early += [q_up1.load, q_down1.load]
    k.do(r_gate1.send, rows.wait, g10.begin, q_up1.send, q_down1.send, g10.loop)
    k.do(q_up1.step, q_down1.step, y_load.wait, p_out1.run, p_out1.wait, r_out1.send)
    k.do(proj.wait, q_load.wait, k_load.wait, lambda: back.run(q_up1.step, q_down1.step))
    k.do(q_up1.wait, *(v.start for v in head_gains))
    k.do(gain_load.wait, value.wait, s11.loop, a_load.wait, p_in1.run)
    k.do(s11.finish, d_z.start, gain10.start, p_in1.wait)
    k.do(*wait(q_down1, q_up1, r_gate1, r_out1))
    k.build()
    d_z, gain10 = d_z.out, gain10.out
    q_gain, k_gain = (v.out for v in head_gains)

    k = Kernel(5)
    q_gate1, m_up1 = sum_scatter(k, "rows", p_gate1.out, r_gate1.out), x_move(k, q_up1.out, 0)
    q_out1 = sum_scatter(k, "cols", p_out1.out, r_out1.out)
    r_in1 = x_slots(k, p_in1.out, "rows")
    q_in1 = sum_scatter(k, "rows", p_in1.out, r_in1.out)
    e_down1 = Finish(k, q_down1.out, 1)
    rows, value, gain_load = load_all(k, d_z), load_all(k, mid0), gains_of(k, 0, t_gain.out)
    gate_load, up_load, hid_load, m_load = (load_all(k, v) for v in (gate0, up0, hid0, m0))
    w_gate0 = Weight(k, "rows", z_gate0.out, None, True)
    w_up0 = Weight(k, "rows", z_up0.out, x_up0.out, True)
    w_down0 = Weight(k, "cols", z_down0.out, x_down0.out, True)
    g12 = Gather(
        k, rows.buf, None, [w_down0], [gate_load.buf, up_load.buf], trans=True, epilogue="ffn_back"
    )
    p_down0 = Product(k, hid_load.buf, g12.full)
    p_gate0, p_up0 = Product(k, m_load.buf, g12.values[0]), Product(k, m_load.buf, g12.values[1])
    r_down0 = x_half(k, p_down0.out)
    s13 = Scatter(
        k, g12.values, [w_gate0, w_up0], rows.buf, (value.buf, (gain_load.buf, 1)), True
    )
    d_mid0, gain01 = Save(k, s13.out), Save(k, s13.gain_grad)
    k.early += [q_gate1.load, q_out1.load, e_down1.load]
    k.do(r_in1.send, rows.wait, g12.begin, q_gate1.send, q_out1.send, m_up1.send, e_down1.send)
    k.do(gate_load.wait, up_load.wait, g12.loop)
    k.do(q_gate1.step, q_out1.step, hid_load.wait, p_down0.run, p_down0.wait, r_down0.send)
    k.do(q_gate1.step, q_out1.step, r_in1.wait, q_in1.add)
    k.do(s13.loop, q_in1.step, m_load.wait, p_gate0.run, q_in1.step, p_up0.run)
    k.do(value.wait, gain_load.wait, s13.finish, d_mid0.start, gain01.start)
    k.do(p_gate0.wait, p_up0.wait)
    k.do(*wait(q_gate1, q_out1, q_in1, e_down1, m_up1, r_down0))
    k.build()
    d_mid0, gain01 = d_mid0.out, gain01.out

    k = Kernel(6)
    r_gate0 = x_slots(k, p_gate0.out, "rows")
    q_down0 = sum_scatter(k, "cols", p_down0.out, r_down0.out)
    q_gate0 = sum_scatter(k, "rows", p_gate0.out, r_gate0.out)
    q_up0 = sum_scatter(k, "rows", p_up0.out)
    m_up0 = x_move(k, q_up0.out, 1)
    e_gate1, e_out1, e_in1 = (Finish(k, v.out, 1) for v in (q_gate1, q_out1, q_in1))
    rows, gain_load = load_all(k, d_mid0), gains_of(k, 0, t_gain.out)
    x_load, taps = start_rows(k, 0, t_seq.out), load_all(k, conv_kernel)
    y_load, a_load, proj, value = (load_all(k, v) for v in (y0, a0, proj0, value0))
    w_in0 = Weight(k, "rows", z_in0.out, x_in0.out, True)
    w_cols = Weight(k, "conv", z_cols.out, x_cols.out, True)
    w_out0 = Weight(k, "cols", z_out0.out, x_out0.out, True)
    g14 = Gather(k, rows.buf, None, [w_out0], trans=True)
    p_out0 = Product(k, y_load.buf, g14.full)
    back = ConvBack(k, proj.buf, value.buf, taps.buf, g14.values[0])
    p_in0, p_cols = Product(k, a_load.buf, back.d_proj), Product(k, a_load.buf, back.d_value)
    r_out0, r_in0 = x_half(k, p_out0.out), x_slots(k, p_in0.out, "rows")
    r_cols = x_slots(k, p_cols.out, "conv")
    q_out0, q_in0 = sum_scatter(k, "cols", p_out0.out, r_out0.out), sum_scatter(k, "rows", p_in0.out, r_in0.out)
    q_cols = sum_scatter(k, "conv", p_cols.out, r_cols.out)
    e_down0, e_gate0, e_out0, e_in0 = (
        Finish(k, v.out, 0) for v in (q_down0, q_gate0, q_out0, q_in0)
    )
    s15 = Scatter(
        k, [back.d_proj, back.d_value], [w_in0, w_cols], rows.buf,
        (x_load.buf, (gain_load.buf, 0)), True, low=True,
    )
    d_x = Save(k, s15.out)
    tap_rows = conv_kernel.shape[0]
    small = k.vmem((8, model_width), F32)
    small_out = Save(k, small)
    ready = [load_all(k, v) for v in (gain01, gain10, gain11)]
    head_loads = [load_all(k, v) for v in (q_gain, k_gain)]

    def fill_small():
        t = lax.axis_index("tensor")
        small.ref[...] = jnp.zeros_like(small.ref)
        small.ref[0:1, :] = s15.gain_grad.ref[...]
        for i, load in enumerate(ready):
            load.wait()
            small.ref[i + 1 : i + 2, :] = load.buf.ref[...]
        small.ref[4 : 4 + tap_rows, block_of(t, channels)] = back.d_kernel.ref[...]
        at = 0
        for load in head_loads:
            load.wait()
            width = load.buf.shape[1]
            small.ref[7:8, at : at + width] = load.buf.ref[...]
            at += width
        small_out.start()

    t_small = x_move(k, small_out.out)
    z_small = SumShare(k, [small_out.out, t_small.out], "dp")
    t_total = SumShare(k, [z_small.out], "tensor", slotted=True)
    y_val, dx_val = k.input(y_rows), d_x.out

    def result_moves(s, d, t):
        sources = [(s == 0, y_val.ref), (s == 1, dx_val.ref)]
        return [(sources, t_result.out.ref, {"section": 1 - s})], []

    t_result = Task(k, row_shape, "section", result_moves, 1)
    k.early += [q_up0.load, q_down0.load, e_gate1.load, e_out1.load, e_in1.load]
    k.do(r_gate0.send, rows.wait, g14.begin, q_up0.send, q_down0.send)
    k.do(e_gate1.send, e_out1.send, e_in1.send, g14.loop)
    k.do(q_up0.step, q_down0.step, y_load.wait, p_out0.run, p_out0.wait, r_out0.send)
    k.do(proj.wait, value.wait, taps.wait, back.run, a_load.wait)
    k.do(p_in0.run, p_cols.run, p_in0.wait, r_in0.send, p_cols.wait, r_cols.send)
    k.do(r_gate0.wait, q_gate0.add, q_up0.step, q_down0.step)
    k.do(x_load.wait, gain_load.wait, s15.loop, q_gate0.step, s15.finish, d_x.start)
    k.do(fill_small, d_x.wait, t_result.send, small_out.wait, t_small.send)
    k.do(q_up0.wait, m_up0.send, r_out0.wait, q_out0.add, r_in0.wait, q_in0.add)
    k.do(r_cols.wait, q_cols.add, q_gate0.step, q_down0.wait, e_down0.add)
    k.do(q_out0.step, q_in0.step, q_cols.step, t_small.wait, z_small.add)
    k.do(q_gate0.wait, e_gate0.add, q_out0.step, q_in0.step, q_cols.step)
    k.do(z_small.wait, t_total.add, q_out0.wait, e_out0.add, q_in0.wait, e_in0.add)
    rest = (e_gate1, e_out1, e_in1, q_cols, e_down0, e_gate0, m_up0, e_out0, e_in0)
    k.do(*wait(*rest, t_total, t_result))
    k.build()

    def whole(zero, one):
        kept = jnp.where(first, zero.out.array, one.out.array)
        return kept.reshape(1, -1, kept.shape[-1]).astype(F32)

    def slot_sum(value):
        value = value.out.array.astype(F32)
        return value if value.ndim == 2 else jnp.sum(value, axis=0)

    up_zero, up_one = slot_sum(q_up0) + slot_sum(m_up0), slot_sum(q_up1) + slot_sum(m_up1)
    d_x, y_rows, moved = d_x.out.array, y_rows.array, t_result.out.array
    result = jnp.where(first, jnp.stack([d_x, moved]), jnp.stack([moved, y_rows]))
    small = jnp.sum(t_total.out.array, axis=0)
    gains_total = small[:4].reshape(2, 2, model_width)
    gain_out = lax.dynamic_slice_in_dim(gains_total, lax.axis_index("section"), 1, 0)
    kernel_out = lax.dynamic_slice_in_dim(
        small[4 : 4 + tap_rows], tensor_index * channels, channels, 1
    )
    cols_grad = slot_sum(q_cols)
    split = channels + channels // 2
    head_total = jnp.stack(
        [
            jnp.sum(v.reshape(-1, size), axis=0)
            for v in (small[7, :channels], small[7, channels:split])
        ]
    )
    return (
        result[None],
        gain_out,
        whole(e_in0, e_in1),
        whole(e_out0, e_out1),
        whole(e_gate0, e_gate1),
        jnp.where(first, up_zero, up_one)[None],
        whole(e_down0, e_down1),
        cols_grad,
        kernel_out,
        head_total,
    )


def solution(mesh):
    in_specs = (
        P("section", "dp", "tensor", None),
        P("section", None, None),
        P("section", "dp", "tensor"),
        P("section", "tensor", "dp"),
        P("section", "dp", "tensor"),
        P("section", "dp", "tensor"),
        P("section", "tensor", "dp"),
        P(("section", "dp"), "tensor"),
        P(None, "tensor"),
        P(),
    )
    out_specs = (
        P("section", "dp", "tensor", None),
        P("section", None, None),
        P("section", "dp", "tensor"),
        P("section", "tensor", "dp"),
        P("section", "dp", "tensor"),
        P("section", "dp", "tensor"),
        P("section", "tensor", "dp"),
        P(("section", "dp"), "tensor"),
        P(None, "tensor"),
        P(),
    )
    return jax.shard_map(body, mesh=mesh, in_specs=in_specs, out_specs=out_specs, check_vma=False)
```

```python
import functools

import jax
import jax.numpy as jnp
from jax import lax
from jax.experimental import pallas as pl
from jax.experimental.pallas import tpu as pltpu
from jax.sharding import PartitionSpec as P

HEADS = 16
KV_HEADS = 8

EPS = 1e-05
ROPE_BASE = 1000000.0
MASKED = -1e30

MESH = pl.DeviceIdType.MESH
ANY = pl.BlockSpec(memory_space=pl.ANY)
DMA = pltpu.SemaphoreType.DMA
VMEM_BYTES = 63 * 1024 * 1024
BF = jnp.bfloat16
F32 = jnp.float32
ROW_BLOCK = 256


def contract(left_op, right_op, left_dim, right_dim):
    return lax.dot_general(
        left_op, right_op, (((left_dim,), (right_dim,)), ((), ())), preferred_element_type=F32
    )


def norm_rows(values, gain):
    return values * lax.rsqrt(jnp.mean(values * values, axis=-1, keepdims=True) + EPS) * gain


def norm_back(values, gain, grad_in):
    row_scale = lax.rsqrt(jnp.mean(values * values, axis=-1, keepdims=True) + EPS)
    normed = values * row_scale
    gain_grad = jnp.sum(grad_in * normed, axis=0, keepdims=True)
    scaled = grad_in * gain
    value_grad = row_scale * (scaled - normed * jnp.mean(scaled * normed, axis=-1, keepdims=True))
    return (value_grad, gain_grad)


class Angles:
    def __init__(self, k, length, head_size, width):
        self.half = head_size // 2
        self.tables = [k.vmem((length, width), F32) for _ in range(2)]
        self.saves = [Save(k, v) for v in self.tables]

    def run(self):
        cos, sin = self.tables
        shape = (ROW_BLOCK, cos.shape[1])
        column = (lax.broadcasted_iota(jnp.int32, shape, 1) % self.half).astype(F32)
        frequency = ROPE_BASE ** (-(column / self.half))
        row = lax.broadcasted_iota(jnp.int32, shape, 0)

        def step(i, carry):
            rows = block_of(i, ROW_BLOCK)
            angle = (row + i * ROW_BLOCK).astype(F32) * frequency
            cos.ref[rows, :] = jnp.cos(angle)
            sin.ref[rows, :] = jnp.sin(angle)
            return carry

        lax.fori_loop(0, cos.shape[0] // ROW_BLOCK, step, 0)
        for save in self.saves:
            save.start()


def silu_parts(gate):
    sig = 1.0 / (1.0 + jnp.exp(-gate))
    return sig, gate * sig


def dp_size():
    return lax.axis_size("dp")


def spot():
    return tuple(lax.axis_index(a) for a in ("section", "dp", "tensor"))


def block_of(index, size):
    return pl.ds(pl.multiple_of(index * size, size), size)


class Val:
    def __init__(self, shape, dtype):
        self.shape, self.dtype = tuple(shape), dtype
        self.ref = self.array = None


class Kernel:
    def __init__(self, cid):
        self.cid, self.ins, self.arrays, self.outs, self.room = cid, [], [], [], []
        self.early, self.steps, self.late, self.axes = [], [], [], {"tensor"}
        self.once = []

    def input(self, array):
        array = array.array if isinstance(array, Val) else array
        for val, known in zip(self.ins, self.arrays):
            if known is array:
                return val
        val = Val(array.shape, array.dtype)
        self.ins.append(val)
        self.arrays.append(array)
        return val

    def output(self, shape, dtype):
        val = Val(shape, dtype)
        self.outs.append(val)
        return val

    def vmem(self, shape, dtype):
        val = Val(shape, dtype)
        self.room.append((val, pltpu.VMEM(tuple(shape), dtype)))
        return val

    def sem(self, *shape):
        val = Val(shape, None)
        self.room.append((val, DMA(shape)))
        return val

    def do(self, *steps):
        self.steps += steps

    def body(self, *refs):
        vals = self.ins + self.outs + [val for val, _ in self.room]
        for val, ref in zip(vals, refs):
            val.ref = ref
        for item in self.once:
            item.waited = False
            item.phase = 0
        for step in self.early:
            step()
        self.greet()
        for step in self.steps + self.late:
            step()

    def greet(self):
        s, d, t = spot()
        peers = []
        if "section" in self.axes:
            peers.append({"section": 1 - s})
        if "dp" in self.axes:
            peers += [{"dp": (d + k) % dp_size()} for k in range(1, dp_size())]
        peers += [{"tensor": (t + k) % 4} for k in range(1, 4)]
        barrier = pltpu.get_barrier_semaphore()
        for peer in peers:
            pl.semaphore_signal(barrier, inc=1, device_id=peer, device_id_type=MESH)
        pl.semaphore_wait(barrier, len(peers))

    def build(self):
        result = pl.pallas_call(
            self.body,
            out_shape=[jax.ShapeDtypeStruct(v.shape, v.dtype) for v in self.outs],
            in_specs=[ANY] * len(self.ins),
            out_specs=[ANY] * len(self.outs),
            scratch_shapes=[room for _, room in self.room],
            compiler_params=pltpu.CompilerParams(
                collective_id=self.cid, has_side_effects=True, vmem_limit_bytes=VMEM_BYTES
            ),
            name=f"stage{self.cid}",
        )(*self.arrays)
        for val, array in zip(self.outs, result):
            val.array = array


def remote(src, dst, send_sem, recv_sem, peer):
    return pltpu.make_async_remote_copy(
        src_ref=src, dst_ref=dst, send_sem=send_sem, recv_sem=recv_sem,
        device_id=peer, device_id_type=MESH,
    )


class Load:
    def __init__(self, k, sources, shape, dtype, early=False):
        self.k, self.sources, self.waited = k, sources, False
        self.buf, self.sem = k.vmem(shape, dtype), k.sem(1)
        k.once.append(self)
        if early:
            k.early.append(self.start)

    def moves(self):
        for cond, source in self.sources(*spot()):
            yield cond, pltpu.make_async_copy(source, self.buf.ref, self.sem.ref.at[0])

    def start(self):
        for cond, move in self.moves():
            if cond is None:
                move.start()
            else:
                pl.when(cond)(move.start)

    def wait(self):
        if not self.waited:
            self.waited = True
            next(self.moves())[1].wait()


def load_all(k, array, early=True):
    val = k.input(array)
    return Load(k, lambda s, d, t: [(None, val.ref)], val.shape, val.dtype, early)


class Save:
    def __init__(self, k, buf):
        self.buf, self.out, self.sem = buf, k.output(buf.shape, buf.dtype), k.sem(1)
        self.waited = False
        k.once.append(self)
        k.late.append(self.wait)

    def move(self):
        return pltpu.make_async_copy(self.buf.ref, self.out.ref, self.sem.ref.at[0])

    def start(self):
        self.move().start()

    def wait(self):
        if not self.waited:
            self.waited = True
            self.move().wait()


class Task:
    final = None

    def __init__(self, k, out, axis, moves, count, n_local=1, out_dtype=BF):
        self.k, self.axis, self.make = k, axis, moves
        self.out = k.output(out, out_dtype)
        self.send_sem, self.recv_sem, self.local_sem = k.sem(count), k.sem(count), k.sem(n_local)
        self.waited = False
        k.axes.add(axis)
        k.once.append(self)

    def local(self, src, dst, i):
        return pltpu.make_async_copy(src, dst, self.local_sem.ref.at[i])

    def pairs(self, every):
        far, near = self.make(*spot())
        for i, (sources, dst, peer) in enumerate(far):
            for cond, src in sources if every else sources[:1]:
                yield cond, True, remote(
                    src, dst, self.send_sem.ref.at[i], self.recv_sem.ref.at[i], peer
                )
        for i, (sources, dst) in enumerate(near):
            for cond, src in sources if every else sources[:1]:
                yield cond, False, self.local(src, dst, i)

    def step(self):
        pass

    def send(self):
        for cond, far, move in self.pairs(True):
            if far and self.final is not None:
                cond = lax.axis_index("section") == 1 - self.final
            if cond is None:
                move.start()
            else:
                pl.when(cond)(move.start)

    def wait(self):
        if self.waited:
            return
        self.waited = True
        s = lax.axis_index("section")
        for _, far, move in self.pairs(False):
            if not far:
                move.wait()
            elif self.final is None:
                move.wait_recv()
                move.wait_send()
            else:
                pl.when(s == 1 - self.final)(move.wait_send)
                pl.when(s == self.final)(move.wait_recv)


def as_val(k, value):
    value = value.out if isinstance(value, Task) else value
    known = isinstance(value, Val) and (value.array is None)
    return value if known else k.input(value)


class Line(Task):
    def __init__(self, k, out, out_dtype=BF, n_local=1):
        super().__init__(k, out, "dp", None, 6, n_local, out_dtype)
        self.send_sem, self.recv_sem = k.sem(2, 3), k.sem(2, 3)
        self.phase = 0

    def hop(self, j, way, src, dst):
        d = lax.axis_index("dp")
        peer = {"dp": (d + 1 if way == 0 else d + 3) % 4}
        return remote(src, dst, self.send_sem.ref.at[way, j], self.recv_sem.ref.at[way, j], peer)


class LineGather(Line):
    def __init__(self, k, sources, shape, dtype):
        super().__init__(k, (4,) + shape, dtype)
        self.sources = sources

    def ends(self, j, way):
        d = lax.axis_index("dp")
        if way == 0:
            return (d >= j) & (d < 3), d >= j + 1
        return (d <= 3 - j) & (d > 0), d <= 2 - j

    def copy(self, j, way, src=None):
        d = lax.axis_index("dp")
        slot = (d + 4 - j if way == 0 else d + j) % 4
        piece = self.out.ref.at[slot]
        return self.hop(j, way, piece if src is None else src, piece)

    def send(self):
        self.phase = 0
        for cond, src in self.sources(*spot()):
            own = self.local(src, self.out.ref.at[lax.axis_index("dp")], 0)
            moves = [(True if cond is None else cond, own)]
            for way in range(2):
                sends = self.ends(0, way)[0]
                moves.append((sends if cond is None else sends & cond, self.copy(0, way, src)))
            for when, move in moves:
                if when is True:
                    move.start()
                else:
                    pl.when(when)(move.start)

    def arrive(self, j):
        for way in range(2):
            pl.when(self.ends(j, way)[1])(self.copy(j, way).wait_recv)

    def step(self):
        self.arrive(self.phase)
        self.phase += 1
        for way in range(2):
            pl.when(self.ends(self.phase, way)[0])(self.copy(self.phase, way).start)

    def wait(self):
        if self.waited:
            return
        self.waited = True
        while self.phase < 2:
            self.step()
        self.arrive(2)
        for j in range(3):
            for way in range(2):
                pl.when(self.ends(j, way)[0])(self.copy(j, way).wait_send)
        d = lax.axis_index("dp")
        self.local(self.sources(*spot())[0][1], self.out.ref.at[d], 0).wait()


def z_gather_from(k, sources, shape, dtype):
    count = dp_size()
    if count == 4:
        return LineGather(k, sources, shape, dtype)

    def moves(s, d, t):
        dst, found = task.out.ref.at[d], sources(s, d, t)
        return [(found, dst, {"dp": (d + i) % count}) for i in range(1, count)], [(found, dst)]

    task = Task(k, (count,) + shape, "dp", moves, count - 1, out_dtype=dtype)
    return task


def z_gather(k, value):
    val = as_val(k, value)
    return z_gather_from(k, lambda s, d, t: [(None, val.ref)], val.shape, val.dtype)


def z_gather_half(k, shard, moved, block):
    shard, moved = as_val(k, shard), as_val(k, moved)
    rows = shard.shape[0] // 2

    def sources(s, d, t):
        own = shard.ref.at[pl.ds(block * rows, rows)]
        return [(s == block, own), (s == 1 - block, moved.ref)]

    return z_gather_from(k, sources, moved.shape, shard.dtype)


def one_way(task, sender):
    task.final = None if sender is None else 1 - sender
    return task


def z_gather_whole(k, shard, moved, block, half=None):
    shard, moved = as_val(k, shard), as_val(k, moved)
    rows = shard.shape[0] if half is None else shard.shape[0] // 2
    part = pl.ds(0 if half is None else half * rows, rows)

    def sources(s, d, t):
        return [(s == block, shard.ref.at[part]), (s == 1 - block, moved.ref.at[part])]

    return z_gather_from(k, sources, (rows,) + shard.shape[1:], shard.dtype)


def x_move(k, value, sender=None):
    val = as_val(k, value)

    def moves(s, d, t):
        return [([(None, val.ref)], task.out.ref, {"section": 1 - s})], []

    task = Task(k, val.shape, "section", moves, 1, out_dtype=val.dtype)
    return one_way(task, sender)


def x_half(k, value, sender=None):
    val = as_val(k, value)
    rows = val.shape[0] // 2

    def moves(s, d, t):
        src = val.ref.at[block_of(1 - s, rows)]
        return [([(None, src)], task.out.ref, {"section": 1 - s})], []

    task = Task(k, (rows,) + val.shape[1:], "section", moves, 1, out_dtype=val.dtype)
    return one_way(task, sender)


def x_slots(k, value, kind):
    val, count = as_val(k, value), dp_size()
    rows = val.shape[0] // (2 * count)

    def moves(s, d, t):
        far = []
        for i in range(count):
            slot = 2 * i + 1 - s if kind == "rows" else (1 - s) * count + i
            src = val.ref.at[block_of(slot, rows)]
            far.append(([(None, src)], task.out.ref.at[i], {"section": 1 - s}))
        return far, []

    task = Task(k, (count, rows) + val.shape[1:], "section", moves, count)
    return task


class Terms:
    def __init__(self, k, kind, grads, received, local):
        self.grads, self.local = as_val(k, grads), local
        self.kind, self.n = kind, dp_size()
        self.whole = received is None
        if self.whole:
            rows, cols = self.grads.shape
            self.rows = rows if kind == "cols" else rows // self.n
            self.cols = cols // self.n if kind == "cols" else cols
            self.shape = (self.n, self.rows, self.cols)
            self.aside = kind == "cols" and self.cols % 128 != 0
            self.total = k.vmem(self.shape, BF)
            self.kept = k.vmem(self.grads.shape, BF) if self.aside else self.total
            return
        self.received = as_val(k, received)
        if kind == "cols":
            self.rows, self.cols = self.grads.shape[0] // 2, self.grads.shape[1] // self.n
            held = (self.rows, self.grads.shape[1])
        else:
            self.rows, self.cols = self.grads.shape[0] // (2 * self.n), self.grads.shape[1]
            held = (self.n, self.rows, self.cols)
        self.kept, self.got = k.vmem(held, BF), k.vmem(held, BF)
        self.shape = (self.n, self.rows, self.cols)
        self.total = k.vmem(self.shape, BF) if kind == "cols" else self.kept

    def loads(self):
        s, grads, kept = lax.axis_index("section"), self.grads.ref, self.kept.ref
        if self.whole and self.aside:
            return [self.local(grads, kept, 2)]
        if self.whole:
            parts = [
                grads.at[:, pl.ds(i * self.cols, self.cols)]
                if self.kind == "cols"
                else grads.at[block_of(i, self.rows)]
                for i in range(self.n)
            ]
            return [self.local(part, kept.at[i], 2 + i) for i, part in enumerate(parts)]
        if self.kind == "cols":
            moves = [self.local(grads.at[block_of(s, self.rows)], kept, 2)]
        else:
            moves = []
            for i in range(self.n):
                slot = 2 * i + s if self.kind == "rows" else s * self.n + i
                moves.append(self.local(grads.at[block_of(slot, self.rows)], kept.at[i], 2 + i))
        return moves + [self.local(self.received.ref, self.got.ref, 1)]

    def load(self):
        for move in self.loads():
            move.start()

    def add(self):
        for move in self.loads():
            move.wait()
        if self.whole and self.aside:
            for i in range(self.n):
                self.total.ref[i] = self.kept.ref[:, i * self.cols : (i + 1) * self.cols]
        if self.whole:
            return
        kept, got, total = self.kept.ref, self.got.ref, self.total.ref
        for i in range(self.n):
            if self.kind == "cols":
                part = (slice(None), slice(i * self.cols, (i + 1) * self.cols))
            else:
                part = i
            total[i] = (kept[part].astype(F32) + got[part].astype(F32)).astype(BF)


class DirectScatter(Task):
    def __init__(self, k, kind, grads, received):
        self.terms = Terms(k, kind, grads, received, lambda *a: self.local(*a))
        count = dp_size()

        def moves(s, d, t):
            total = self.terms.total.ref
            far = []
            for i in range(1, count):
                other = (d + i) % count
                far.append(([(None, total.at[other])], self.out.ref.at[d], {"dp": other}))
            return far, [([(None, total.at[d])], self.out.ref.at[d])]

        super().__init__(k, self.terms.shape, "dp", moves, count - 1, 2 + count)
        self.load = self.terms.load

    def send(self):
        self.terms.add()
        super().send()

    def add(self):
        self.load()
        self.send()


class LineScatter(Line):
    def __init__(self, k, kind, grads, received):
        self.terms = Terms(k, kind, grads, received, lambda *a: self.local(*a))
        super().__init__(k, self.terms.shape[1:], BF, 6)
        self.got = k.vmem((2, 3) + self.terms.shape[1:], BF)
        self.load = self.terms.load

    def ends(self, j, way):
        d = lax.axis_index("dp")
        if way == 0:
            return (d <= j) & (d < 3), (d >= 1) & (d <= j + 1)
        return (d >= 3 - j) & (d > 0), (d <= 2) & (d >= 2 - j)

    def copy(self, j, way):
        d = lax.axis_index("dp")
        to = (d + 3 - j if way == 0 else d + 1 + j) % 4
        return self.hop(j, way, self.terms.total.ref.at[to], self.got.ref.at[way, j])

    def send(self):
        self.phase = 0
        self.terms.add()
        for way in range(2):
            pl.when(self.ends(0, way)[0])(self.copy(0, way).start)

    def take(self, j, way):
        d = lax.axis_index("dp")
        to = (d + 2 - j if way == 0 else d + 2 + j) % 4
        self.copy(j, way).wait_recv()
        total = self.terms.total.ref
        total[to] = (total[to].astype(F32) + self.got.ref[way, j].astype(F32)).astype(BF)

    def arrive(self, j):
        for way in range(2):
            pl.when(self.ends(j, way)[1])(functools.partial(self.take, j, way))

    def step(self):
        self.arrive(self.phase)
        self.phase += 1
        for way in range(2):
            pl.when(self.ends(self.phase, way)[0])(self.copy(self.phase, way).start)

    def wait(self):
        if self.waited:
            return
        self.waited = True
        while self.phase < 2:
            self.step()
        self.arrive(2)
        done = self.local(self.terms.total.ref.at[lax.axis_index("dp")], self.out.ref, 0)
        done.start()
        for j in range(3):
            for way in range(2):
                pl.when(self.ends(j, way)[0])(self.copy(j, way).wait_send)
        done.wait()

    def add(self):
        self.load()
        self.send()


def sum_scatter(k, kind, grads, received=None):
    return (LineScatter if dp_size() == 4 else DirectScatter)(k, kind, grads, received)


class Finish(Task):
    def __init__(self, k, pieces, block):
        self.pieces, self.final = as_val(k, pieces), block
        *slots, rows, cols = self.pieces.shape
        self.slots = slots[0] if slots else 0
        if slots:
            self.held, self.total = k.vmem(self.pieces.shape, BF), k.vmem((rows, cols), BF)
        else:
            self.total = self.pieces

        def moves(s, d, t):
            source, dst = [(None, self.total.ref)], self.out.ref.at[s]
            return [(source, dst, {"section": 1 - s})], [(source, dst)]

        super().__init__(k, (2, rows, cols), "section", moves, 1, 2)

    def load(self):
        if self.slots:
            self.local(self.pieces.ref, self.held.ref, 1).start()

    def send(self):
        if self.slots:
            self.local(self.pieces.ref, self.held.ref, 1).wait()
            acc = self.held.ref[0].astype(F32)
            for i in range(1, self.slots):
                acc = acc + self.held.ref[i].astype(F32)
            self.total.ref[...] = acc.astype(BF)
        super().send()

    def add(self):
        self.load()
        self.send()


class SumShare(Task):
    def __init__(self, k, terms, axis, slotted=False):
        self.terms = [as_val(k, v) for v in terms]
        shape = self.terms[0].shape[1:] if slotted else self.terms[0].shape
        count = dp_size() if axis == "dp" else 4
        self.slotted = slotted
        self.bufs = [k.vmem(v.shape, F32) for v in self.terms]
        self.total = k.vmem(shape, F32)

        def moves(s, d, t):
            source, me = [(None, self.total.ref)], d if axis == "dp" else t
            dst = self.out.ref.at[me]
            far = [(source, dst, {axis: (me + i) % count}) for i in range(1, count)]
            return far, [(source, dst)]

        super().__init__(k, (count,) + shape, axis, moves, count - 1, 3, out_dtype=F32)

    def add(self):
        loads = [self.local(v.ref, b.ref, 1 + i) for i, (v, b) in enumerate(zip(self.terms, self.bufs))]
        for load in loads:
            load.start()
        for load in loads:
            load.wait()
        if self.slotted:
            parts = [self.bufs[0].ref[i] for i in range(self.terms[0].shape[0])]
        else:
            parts = [buf.ref[...] for buf in self.bufs]
        acc = parts[0]
        for part in parts[1:]:
            acc = acc + part
        self.total.ref[...] = acc
        self.send()


class Weight:
    def __init__(self, k, kind, near, far=None, early=False, fixed=False):
        near, far = as_val(k, near), None if far is None else as_val(k, far)
        self.count, self.rows, self.cols = near.shape
        self.kind, self.near, self.far, self.waited = kind, near, far, False
        sides, self.fixed = 1 if far is None else 2, fixed
        if kind == "cols":
            shape = (sides * self.rows, self.count * self.cols)
        else:
            shape = (sides * self.count * self.rows, self.cols)
        self.aside = kind == "cols" and self.cols % 128 != 0
        self.buf, self.sem = k.vmem(shape, BF), k.sem(2 * self.count)
        if self.aside:
            self.held = [k.vmem(near.shape, BF), k.vmem(near.shape, BF)]
        k.once.append(self)
        if early:
            k.early.append(self.start)

    def moves(self):
        s, dst = 0 if self.fixed else lax.axis_index("section"), self.buf.ref
        rows, cols = self.rows, self.cols

        def place(sec, own):
            if self.aside:
                return None
            if self.kind == "cols":
                return dst.at[block_of(sec, rows), pl.ds(own * cols, cols)]
            slot = own * 2 + sec if self.kind == "rows" else sec * self.count + own
            return dst.at[block_of(slot, rows)]

        if self.far is None:
            for i in range(self.count):
                if self.kind == "cols":
                    to = dst.at[:, pl.ds(i * cols, cols)]
                else:
                    to = dst.at[pl.ds(i * rows, rows)]
                to = self.held[0].ref.at[i] if self.aside else to
                yield pltpu.make_async_copy(self.near.ref.at[i], to, self.sem.ref.at[2 * i])
            return
        for i in range(self.count):
            for j, (val, sec) in enumerate(((self.near, s), (self.far, 1 - s))):
                to = self.held[j].ref.at[i] if self.aside else place(sec, i)
                yield pltpu.make_async_copy(val.ref.at[i], to, self.sem.ref.at[2 * i + j])

    def start(self):
        for move in self.moves():
            move.start()

    def wait(self):
        if self.waited:
            return
        self.waited = True
        for move in self.moves():
            move.wait()
        if self.aside:
            s = 0 if self.fixed else lax.axis_index("section")
            for j, sec in enumerate((s, 1 - s) if self.far is not None else (0,)):
                whole = jnp.concatenate([self.held[j].ref[i] for i in range(self.count)], axis=1)
                self.buf.ref[block_of(sec, self.rows), :] = whole


class Product:
    def __init__(self, k, left, right):
        self.left, self.right = left, right
        rows = left.shape[1]
        self.chunk = 384 if rows % 384 == 0 else 256
        self.count = rows // self.chunk
        self.buf = k.vmem((rows, right.shape[1]), BF)
        self.out, self.sem = k.output(self.buf.shape, BF), k.sem(self.count)

    def copy(self, i):
        part = block_of(i, self.chunk)
        return pltpu.make_async_copy(self.buf.ref.at[part], self.out.ref.at[part], self.sem.ref.at[i])

    def run(self):
        def step(i, carry):
            part = block_of(i, self.chunk)
            value = contract(self.left.ref[:, part], self.right.ref[...], 0, 0)
            self.buf.ref[part, :] = value.astype(BF)
            self.copy(i).start()
            return carry

        lax.fori_loop(0, self.count, step, 0)

    def wait(self):
        for i in range(self.count):
            self.copy(i).wait()


def places():
    me = lax.axis_index("tensor")
    sib = me + 1 - 2 * (me % 2)
    cross = (me + 2) % 4
    diag = (sib + 2) % 4
    return me, sib, cross, diag


class Gather:
    def __init__(self, k, x, gain, weights, extras=(), trans=False, epilogue="plain", save=()):
        rows, width = x.shape
        length = 4 * rows
        self.k, self.x, self.gain, self.weights, self.extras = k, x, gain, weights, extras
        self.trans, self.epilogue, self.rows, self.half = trans, epilogue, rows, rows // 2
        cols = [w.buf.shape[0 if trans else 1] for w in weights]
        kinds = {
            "plain": [(c, F32) for c in cols],
            "ffn": [(cols[0], BF)] * 3,
            "ffn_back": [(cols[0], BF)] * 2,
        }[epilogue]
        self.full = k.vmem((length, width), BF)
        self.values = [k.vmem((length, c), kind) for c, kind in kinds]
        kept = [self.full] + self.values
        self.saved = [(v, k.output(v.shape, v.dtype), k.sem(4, 2)) for v in kept if kept.index(v) in save]
        self.sems = [k.sem(2) for _ in range(6)]
        k.late.append(self.end)

    def span(self, owner, sub):
        return pl.ds(pl.multiple_of(owner * self.rows + sub * self.half, self.half), self.half)

    def move(self, kind, i):
        me, sib, cross, _ = places()
        full = self.full.ref
        owner, peer, at = {"cross": (me, cross, 0), "sib": (me, sib, 2), "relay": (cross, sib, 4)}[kind]
        part = full.at[self.span(owner, i)]
        return remote(
            part, part, self.sems[at].ref.at[i], self.sems[at + 1].ref.at[i], {"tensor": peer}
        )

    def begin(self):
        me = places()[0]
        for i in range(2):
            part = self.x.ref[pl.ds(i * self.half, self.half), :].astype(F32)
            if self.gain is not None:
                val, row = self.gain
                part = norm_rows(part, val.ref[row : row + 1, :])
            self.full.ref[self.span(me, i), :] = part.astype(BF)
            self.move("cross", i).start()
            self.move("sib", i).start()

    def loop(self):
        me, sib, cross, diag = places()
        rows, half = self.rows, self.half
        for w in self.weights:
            w.wait()

        def step(p, carry):
            far, sub = p // 2, p % 2
            near = (1 - sub) * me + sub * sib
            first = (1 - far) * near * rows + far * (cross * rows + sub * half)
            second = (1 - far) * (near * rows + half) + far * (diag * rows + sub * half)
            pair = [pl.ds(pl.multiple_of(v, half), half) for v in (first, second)]

            @pl.when(p == 1)
            def _():
                self.move("sib", 0).wait_recv()
                self.move("sib", 1).wait_recv()

            for i in range(2):

                @pl.when(p == 2 + i)
                def _():
                    self.move("cross", i).wait_recv()
                    self.move("relay", i).start()
                    self.move("relay", i).wait_recv()

            def both(val):
                return jnp.concatenate([val.ref[pair[0], :], val.ref[pair[1], :]], axis=0)

            a = both(self.full)
            prods = [contract(a, w.buf.ref[...], 1, 1 if self.trans else 0) for w in self.weights]
            if self.epilogue == "plain":
                values = prods
            elif self.epilogue == "ffn":
                sig, silu = silu_parts(prods[0])
                values = [prods[0], prods[1], silu * prods[1]]
            else:
                gate, up = (both(v).astype(F32) for v in self.extras)
                sig, silu = silu_parts(gate)
                values = [prods[0] * up * sig * (1.0 + gate * (1.0 - sig)), prods[0] * silu]
            for val, value in zip(self.values, values):
                value = value.astype(val.dtype)
                for j in range(2):
                    val.ref[pair[j], :] = value[j * half : (j + 1) * half]
            for val, out, sem in self.saved:
                for j in range(2):
                    pltpu.make_async_copy(
                        val.ref.at[pair[j]], out.ref.at[pair[j]], sem.ref.at[p, j]
                    ).start()
            return carry

        lax.fori_loop(0, 4, step, 0)

    def end(self):
        for i in range(2):
            for kind in ("cross", "sib", "relay"):
                self.move(kind, i).wait_send()
        part = pl.ds(0, self.half)
        for val, out, sem in self.saved:
            for p in range(4):
                for j in range(2):
                    pltpu.make_async_copy(val.ref.at[part], out.ref.at[part], sem.ref.at[p, j]).wait()


class Scatter:
    def __init__(self, k, operands, weights, resid, back=None, trans=False, low=False):
        rows, width = resid.shape
        half = rows // 2
        self.operands, self.weights, self.resid, self.back = operands, weights, resid, back
        self.trans, self.low, self.rows, self.half = trans, low, rows, half
        self.keep, self.own = k.vmem((2, half, width), F32), k.vmem((rows, width), F32)
        self.to_s, self.from_s, self.to_c, self.from_c = (
            k.vmem((2, half, width), BF) for _ in range(4)
        )
        self.to_o, self.from_o = k.vmem((rows, width), BF), k.vmem((rows, width), BF)
        self.out = k.vmem((rows, width), BF if low else F32)
        self.gain_grad = k.vmem((1, width), F32) if back else None
        self.sems = [k.sem(2) for _ in range(4)] + [k.sem(1) for _ in range(2)]
        k.late.append(self.end)

    def move(self, kind, i=0):
        _, sib, cross, _ = places()
        at, src, dst, peer = {
            "diag": (0, self.to_s, self.from_s, sib),
            "cross": (2, self.to_c, self.from_c, cross),
            "near": (4, self.to_o, self.from_o, sib),
        }[kind]
        src, dst = (src.ref, dst.ref) if kind == "near" else (src.ref.at[i], dst.ref.at[i])
        return remote(
            src, dst, self.sems[at].ref.at[i], self.sems[at + 1].ref.at[i], {"tensor": peer}
        )

    def pass_on(self, i):
        self.move("diag", i).wait_recv()
        total = self.keep.ref[i] + self.from_s.ref[i].astype(F32)
        self.to_c.ref[i] = total.astype(BF)
        self.move("cross", i).start()

    def loop(self):
        me, sib, cross, diag = places()
        rows, half = self.rows, self.half
        for w in self.weights:
            w.wait()

        def step(p, carry):
            near, sub = p // 2, p % 2
            base = near * ((1 - sub) * sib + sub * me) * rows
            first = base + (1 - near) * (cross * rows + sub * half)
            second = base + near * half + (1 - near) * (diag * rows + sub * half)
            pair = [pl.ds(pl.multiple_of(v, half), half) for v in (first, second)]
            total = None
            for y, w in zip(self.operands, self.weights):
                a = jnp.concatenate([y.ref[pair[0], :], y.ref[pair[1], :]], axis=0)
                prod = contract(a, w.buf.ref[...], 1, 1 if self.trans else 0)
                total = prod if total is None else total + prod

            for i in range(2):

                @pl.when(p == i)
                def _():
                    self.keep.ref[i] = total[:half]
                    self.to_s.ref[i] = total[half:].astype(BF)
                    self.move("diag", i).start()

            @pl.when(p == 1)
            def _():
                self.pass_on(0)

            @pl.when(p == 2)
            def _():
                self.to_o.ref[...] = total.astype(BF)
                self.move("near").start()
                self.pass_on(1)

            @pl.when(p == 3)
            def _():
                self.own.ref[...] = total

            return carry

        lax.fori_loop(0, 4, step, 0)

    def finish(self):
        self.move("near").wait_recv()
        gain_sum = None
        for i in range(2):
            part = pl.ds(i * self.half, self.half)
            self.move("cross", i).wait_recv()
            total = self.own.ref[part, :] + self.from_o.ref[part, :].astype(F32)
            total = total + self.from_c.ref[i].astype(F32)
            resid = self.resid.ref[part, :].astype(F32)
            if self.back:
                value, (gain, row) = self.back
                value_grad, gain_grad = norm_back(
                    value.ref[part, :].astype(F32), gain.ref[row : row + 1, :], total
                )
                total = value_grad
                gain_sum = gain_grad if gain_sum is None else gain_sum + gain_grad
            self.out.ref[part, :] = (resid + total).astype(self.out.dtype)
        if self.back:
            self.gain_grad.ref[...] = gain_sum

    def end(self):
        self.move("near").wait_send()
        for i in range(2):
            self.move("diag", i).wait_send()
            self.move("cross", i).wait_send()


def delayed(values, by):
    if by == 0:
        return values
    row = lax.broadcasted_iota(jnp.int32, values.shape, 0)
    return jnp.where(row < by, 0.0, pltpu.roll(values, by, 0))


def advanced(values, by):
    if by == 0:
        return values
    length = values.shape[0]
    row = lax.broadcasted_iota(jnp.int32, values.shape, 0)
    return jnp.where(row >= length - by, 0.0, pltpu.roll(values, length - by, 0))


CONV_COLS = 128


class Conv:
    def __init__(self, k, projected, value, kernel):
        self.projected, self.value, self.kernel = projected, value, kernel
        self.y = k.vmem(value.shape, BF)

    def parts(self, j):
        channels = self.value.shape[1]
        at = slice(j * CONV_COLS, (j + 1) * CONV_COLS)
        b_gate = self.projected.ref[:, at]
        c_gate = self.projected.ref[:, channels + at.start : channels + at.stop]
        x_value, taps = self.value.ref[:, at], self.kernel.ref[:, at]
        product = b_gate * x_value
        count = taps.shape[0]
        causal = jnp.zeros_like(product)
        for i in range(count):
            causal = causal + taps[i : i + 1] * delayed(product, count - 1 - i)
        return at, b_gate, c_gate, x_value, taps, product, causal

    def run(self):
        for j in range(self.value.shape[1] // CONV_COLS):
            at, _, c_gate, _, _, _, causal = self.parts(j)
            self.y.ref[:, at] = (c_gate * causal).astype(BF)


class ConvBack(Conv):
    def __init__(self, k, projected, value, kernel, d_y):
        self.projected, self.value, self.kernel, self.d_y = projected, value, kernel, d_y
        self.d_proj = k.vmem(projected.shape, BF)
        self.d_value = k.vmem(value.shape, BF)
        self.d_kernel = k.vmem(kernel.shape, F32)

    def run(self):
        channels = self.value.shape[1]
        for j in range(channels // CONV_COLS):
            at, b_gate, c_gate, x_value, taps, product, causal = self.parts(j)
            d_y = self.d_y.ref[:, at]
            d_causal = d_y * c_gate
            count = taps.shape[0]
            d_product = jnp.zeros_like(product)
            for i in range(count):
                by = count - 1 - i
                row = jnp.sum(d_causal * delayed(product, by), axis=0, keepdims=True)
                self.d_kernel.ref[i : i + 1, at] = row
                d_product = d_product + taps[i : i + 1] * advanced(d_causal, by)
            self.d_proj.ref[:, at] = (d_product * x_value).astype(BF)
            self.d_proj.ref[:, channels + at.start : channels + at.stop] = (d_y * causal).astype(BF)
            self.d_value.ref[:, at] = (d_product * b_gate).astype(BF)


def head_mean(values, head_size):
    width = values.shape[1]
    row = lax.broadcasted_iota(jnp.int32, (width, width), 0) // head_size
    col = lax.broadcasted_iota(jnp.int32, (width, width), 1) // head_size
    group = jnp.where(row == col, 1.0 / head_size, 0.0).astype(F32)
    return lax.dot_general(
        values, group, (((1,), (0,)), ((), ())),
        precision=lax.Precision.HIGHEST, preferred_element_type=F32,
    )


def turn(values, head_size, back):
    width, half = values.shape[1], head_size // 2
    lane = lax.broadcasted_iota(jnp.int32, values.shape, 1) % head_size
    upper = pltpu.roll(values, width - half, 1)
    lower = pltpu.roll(values, half, 1)
    return jnp.where(lane < half, upper, -lower) if back else jnp.where(lane < half, -upper, lower)


def head_norm(values, gain, head_size):
    return values * lax.rsqrt(head_mean(values * values, head_size) + EPS) * gain


def head_norm_back(values, gain, grad_in, head_size):
    row_scale = lax.rsqrt(head_mean(values * values, head_size) + EPS)
    normed = values * row_scale
    gain_grad = jnp.sum(grad_in * normed, axis=0, keepdims=True)
    scaled = grad_in * gain
    return row_scale * (scaled - normed * head_mean(scaled * normed, head_size)), gain_grad


def block_weights(q_rows, keys):
    scores = [contract(q_rows, k_rows, 1, 1) for k_rows in keys]
    query = lax.broadcasted_iota(jnp.int32, scores[-1].shape, 0)
    key = lax.broadcasted_iota(jnp.int32, scores[-1].shape, 1)
    scores[-1] = jnp.where(key <= query, scores[-1], MASKED)
    top = functools.reduce(
        jnp.maximum, [jnp.max(part, axis=1, keepdims=True) for part in scores]
    )
    exps = [jnp.exp(part - top) for part in scores]
    scale = 1.0 / sum(jnp.sum(part, axis=1, keepdims=True) for part in exps)
    return [part * scale for part in exps]


def key_blocks(i):
    blocks = [pl.ds(0, i * ROW_BLOCK)] if i else []
    return blocks + [pl.ds(i * ROW_BLOCK, ROW_BLOCK)]


class Heads:
    def __init__(self, projected, tables, size):
        assert size in (16, 64, 256), size
        self.projected, self.size = projected, size
        self.gain, self.cos, self.sin = (v.buf for v in tables)
        self.loads = tables
        self.length, width = projected.shape
        self.q_cols, self.k_cols = width // 2, width // 4
        self.heads, self.kv_heads = self.q_cols // size, self.k_cols // size
        self.share = self.heads // self.kv_heads

    def per_head(self, k, count, kind):
        return k.vmem((count, self.length, self.size), kind)

    def split(self, val, rows, values):
        for h in range(val.shape[0]):
            val.ref[h, rows, :] = values[:, h * self.size : (h + 1) * self.size]

    def join(self, val, rows):
        return jnp.concatenate([val.ref[h, rows, :] for h in range(val.shape[0])], axis=1)

    def angles(self, rows):
        c, n = self.cos.ref[rows, :], self.sin.ref[rows, :]
        repeat = self.q_cols // c.shape[1]
        return jnp.concatenate([c] * repeat, axis=1), jnp.concatenate([n] * repeat, axis=1)

    def blocks(self, step):
        lax.fori_loop(0, self.length // ROW_BLOCK, lambda p, c: step(block_of(p, ROW_BLOCK)) or c, 0)


class Attend(Heads):
    def __init__(self, k, projected, tables, size):
        super().__init__(projected, tables, size)
        self.q_rot = k.vmem((self.length, self.q_cols), BF)
        self.k_rot = k.vmem((self.length, self.k_cols), BF)
        self.y = k.vmem((self.length, self.q_cols), BF)
        self.q_h, self.y_h = (self.per_head(k, self.heads, BF) for _ in range(2))
        self.k_h, self.v_h = (self.per_head(k, self.kv_heads, BF) for _ in range(2))

    def run(self, *between):
        for load in self.loads:
            load.wait()
        size, q_cols, k_cols, proj = self.size, self.q_cols, self.k_cols, self.projected.ref

        def prepare(rows):
            c, n = self.angles(rows)
            q = head_norm(proj[rows, :q_cols], self.gain.ref[0:1, :], size)
            q = (q * c + turn(q, size, False) * n).astype(BF)
            k = head_norm(proj[rows, q_cols : q_cols + k_cols], self.gain.ref[1:2, :k_cols], size)
            k = (k * c[:, :k_cols] + turn(k, size, False) * n[:, :k_cols]).astype(BF)
            self.q_rot.ref[rows, :] = q
            self.k_rot.ref[rows, :] = k
            self.split(self.q_h, rows, (q.astype(F32) * size**-0.5).astype(BF))
            self.split(self.k_h, rows, k)
            self.split(self.v_h, rows, proj[rows, q_cols + k_cols :].astype(BF))

        self.blocks(prepare)

        def head(h, carry):
            g = h // self.share
            for i in range(self.length // ROW_BLOCK):
                rows, seen = pl.ds(i * ROW_BLOCK, ROW_BLOCK), key_blocks(i)
                weights = block_weights(
                    self.q_h.ref[h, rows, :], [self.k_h.ref[g, at, :] for at in seen]
                )
                value = sum(
                    contract(part.astype(BF), self.v_h.ref[g, at, :], 1, 0)
                    for part, at in zip(weights, seen)
                )
                self.y_h.ref[h, rows, :] = value.astype(BF)
            return carry

        lax.fori_loop(0, self.heads // 2, head, 0)
        for step in between:
            step()
        lax.fori_loop(self.heads // 2, self.heads, head, 0)
        self.y.ref[...] = self.join(self.y_h, slice(None))


class AttendBack(Heads):
    def __init__(self, k, projected, tables, size, q_rot, k_rot, d_y):
        super().__init__(projected, tables, size)
        self.q_rot, self.k_rot, self.d_y = q_rot, k_rot, d_y
        self.q_h, self.dy_h = (self.per_head(k, self.heads, BF) for _ in range(2))
        self.k_h, self.v_h = (self.per_head(k, self.kv_heads, BF) for _ in range(2))
        self.dq_h = self.per_head(k, self.heads, F32)
        self.dk_h, self.dv_h = (self.per_head(k, self.kv_heads, F32) for _ in range(2))
        self.d_proj = k.vmem(projected.shape, BF)
        self.q_gain, self.k_gain = k.vmem((1, self.q_cols), F32), k.vmem((1, self.k_cols), F32)

    def run(self, *between):
        for load in self.loads:
            load.wait()
        size, q_cols, k_cols, proj = self.size, self.q_cols, self.k_cols, self.projected.ref
        scale = size**-0.5
        dq_h, dk_h, dv_h = self.dq_h.ref, self.dk_h.ref, self.dv_h.ref

        def prepare(rows):
            self.split(self.q_h, rows, (self.q_rot.ref[rows, :].astype(F32) * scale).astype(BF))
            self.split(self.dy_h, rows, self.d_y.ref[rows, :].astype(BF))
            self.split(self.k_h, rows, self.k_rot.ref[rows, :])
            self.split(self.v_h, rows, proj[rows, q_cols + k_cols :].astype(BF))

        self.blocks(prepare)
        dk_h[...] = jnp.zeros_like(dk_h)
        dv_h[...] = jnp.zeros_like(dv_h)

        def head(h, carry):
            g = h // self.share
            for i in range(self.length // ROW_BLOCK):
                rows, seen = pl.ds(i * ROW_BLOCK, ROW_BLOCK), key_blocks(i)
                q, low = self.q_h.ref[h, rows, :], self.dy_h.ref[h, rows, :]
                keys = [self.k_h.ref[g, at, :] for at in seen]
                probs = block_weights(q, keys)
                d_weights = [contract(low, self.v_h.ref[g, at, :], 1, 1) for at in seen]
                inner = sum(
                    jnp.sum(a * b, axis=1, keepdims=True) for a, b in zip(probs, d_weights)
                )
                d_q = 0.0
                for at, k, prob, d_weight in zip(seen, keys, probs, d_weights):
                    dv_h[g, at, :] += contract(prob.astype(BF), low, 0, 0)
                    d_scores = (prob * (d_weight - inner)).astype(BF)
                    d_q = d_q + contract(d_scores, k, 1, 0)
                    dk_h[g, at, :] += contract(d_scores, q, 0, 0)
                dq_h[h, rows, :] = d_q * scale
            return carry

        lax.fori_loop(0, self.heads // 2, head, 0)
        for step in between:
            step()
        lax.fori_loop(self.heads // 2, self.heads, head, 0)
        self.q_gain.ref[...] = jnp.zeros_like(self.q_gain.ref)
        self.k_gain.ref[...] = jnp.zeros_like(self.k_gain.ref)

        def finish(rows):
            c, n = self.angles(rows)
            dq, dk, dv = (self.join(v, rows) for v in (self.dq_h, self.dk_h, self.dv_h))
            dq = dq * c + turn(dq * n, size, True)
            dk = dk * c[:, :k_cols] + turn(dk * n[:, :k_cols], size, True)
            dq, q_sum = head_norm_back(proj[rows, :q_cols], self.gain.ref[0:1, :], dq, size)
            dk, k_sum = head_norm_back(
                proj[rows, q_cols : q_cols + k_cols], self.gain.ref[1:2, :k_cols], dk, size
            )
            self.q_gain.ref[...] += q_sum
            self.k_gain.ref[...] += k_sum
            self.d_proj.ref[rows, :q_cols] = dq.astype(BF)
            self.d_proj.ref[rows, q_cols : q_cols + k_cols] = dk.astype(BF)
            self.d_proj.ref[rows, q_cols + k_cols :] = dv.astype(BF)

        self.blocks(finish)


def body(boundary, norm_gain, mix_in, mix_out, w_gate, w_up, w_down, conv_x, conv_kernel, qk_gain):
    first = lax.axis_index("section") == 0
    tensor_index = lax.axis_index("tensor")
    model_width = boundary.shape[3]
    channels = mix_out.shape[1]
    row_shape = boundary.shape[2:]
    length, size = 4 * row_shape[0], qk_gain.shape[1]

    seqs, own_gain = boundary[0], norm_gain[0]
    sh_in, sh_out, sh_gate, sh_up, sh_down = (v[0] for v in (mix_in, mix_out, w_gate, w_up, w_down))
    head_gain = jnp.tile(qk_gain, (1, channels // size))

    def gains_of(k, block, other, early=True):
        own, moved = k.input(own_gain), as_val(k, other)
        sources = lambda s, d, t: [(s == block, own.ref), (s == 1 - block, moved.ref)]
        return Load(k, sources, own.shape, F32, early)

    def start_rows(k, slot, other, early=True):
        own, moved = k.input(seqs), as_val(k, other)
        sources = lambda s, d, t: [(s == slot, own.ref.at[slot]), (s == 1 - slot, moved.ref)]
        return Load(k, sources, row_shape, BF, early)

    def wait(*items):
        return [item.wait for item in items]

    k = Kernel(0)
    t_seq = None
    seq_val = k.input(seqs)

    def seq_moves(s, d, t):
        return [([(None, seq_val.ref.at[1 - s])], t_seq.out.ref, {"section": 1 - s})], []

    t_in, t_out, t_up = (x_half(k, v) for v in (sh_in, sh_out, sh_up))
    t_gate0, t_down0 = x_move(k, sh_gate, 0), x_half(k, sh_down, 0)
    t_gate1, t_down1 = x_half(k, sh_gate, 1), x_move(k, sh_down, 1)
    t_seq = Task(k, row_shape, "section", seq_moves, 1)
    t_gain, z_cols = x_move(k, own_gain), z_gather(k, conv_x)
    z_in0, z_out0 = z_gather_half(k, sh_in, t_in.out, 0), z_gather_half(k, sh_out, t_out.out, 0)
    z_gate0 = z_gather_whole(k, sh_gate, t_gate0.out, 0)
    z_up0 = z_gather_half(k, sh_up, t_up.out, 0)
    x_cols, x_in0, x_out0, x_up0 = (x_move(k, v.out) for v in (z_cols, z_in0, z_out0, z_up0))
    x_load, gain_load = start_rows(k, 0, t_seq.out, False), gains_of(k, 0, t_gain.out, False)
    taps = load_all(k, conv_kernel)
    angles = Angles(k, length, size, 128)
    w_in0, w_cols = Weight(k, "rows", z_in0.out, x_in0.out), Weight(k, "conv", z_cols.out, x_cols.out)
    w_out0 = Weight(k, "cols", z_out0.out, x_out0.out)
    g0 = Gather(k, x_load.buf, (gain_load.buf, 0), [w_in0, w_cols], save=(0, 1, 2))
    conv = Conv(k, g0.values[0], g0.values[1], taps.buf)
    y0 = Save(k, conv.y)
    s1 = Scatter(k, [conv.y], [w_out0], x_load.buf)
    mid0 = Save(k, s1.out)
    k.do(t_in.send, t_out.send, z_cols.send, t_up.send, t_gain.send, t_seq.send)
    k.do(t_in.wait, z_in0.send, t_out.wait, z_out0.send)
    k.do(z_cols.step, z_in0.step, z_out0.step, t_up.wait, z_up0.send)
    k.do(z_cols.step, z_in0.step, z_out0.step, z_cols.wait, x_cols.send, z_in0.wait, x_in0.send)
    k.do(z_out0.wait, x_out0.send, t_gate0.send, t_gate1.send)
    k.do(t_gain.wait, gain_load.start, t_seq.wait, x_load.start, z_up0.step)
    k.do(gain_load.wait, x_load.wait, g0.begin, z_up0.step, angles.run)
    k.do(z_up0.wait, x_up0.send, t_down0.send, t_down1.send)
    k.do(x_cols.wait, w_cols.start, x_in0.wait, w_in0.start, t_gate0.wait, z_gate0.send)
    k.do(g0.loop, z_gate0.step, taps.wait, conv.run, y0.start)
    k.do(x_out0.wait, w_out0.start, s1.loop, z_gate0.step, s1.finish, mid0.start)
    k.do(*wait(t_gate1, t_down0, t_down1, z_gate0, x_up0))
    k.build()
    a0, proj0, value0 = (out for _, out, _ in g0.saved)
    table_arrays = [head_gain] + [v.out for v in angles.saves]
    y0, mid0 = y0.out, mid0.out

    k = Kernel(1)
    z_down0 = z_gather_half(k, sh_down, t_down0.out, 0)
    z_in1, z_out1 = z_gather_half(k, sh_in, t_in.out, 1), z_gather_half(k, sh_out, t_out.out, 1)
    z_gate1 = z_gather_half(k, sh_gate, t_gate1.out, 1)
    z_down1a = z_gather_whole(k, sh_down, t_down1.out, 1, 0)
    x_down0, x_in1, x_out1 = (x_move(k, v.out) for v in (z_down0, z_in1, z_out1))
    rows, gain_load = load_all(k, mid0), gains_of(k, 0, t_gain.out)
    w_gate0 = Weight(k, "rows", z_gate0.out, None, True)
    w_up0 = Weight(k, "rows", z_up0.out, x_up0.out, True)
    w_down0 = Weight(k, "cols", z_down0.out, x_down0.out)
    g2 = Gather(
        k, rows.buf, (gain_load.buf, 1), [w_gate0, w_up0], epilogue="ffn", save=(0, 1, 2, 3)
    )
    s3 = Scatter(k, [g2.values[2]], [w_down0], rows.buf, low=True)
    z_rows = Save(k, s3.out)
    k.do(z_down0.send, rows.wait, gain_load.wait, g2.begin, z_down0.step, z_in1.send, z_out1.send)
    k.do(z_down0.step, z_in1.step, z_out1.step, z_gate1.send, z_down0.wait, x_down0.send)
    k.do(g2.loop, z_in1.step, z_out1.step, z_gate1.step, z_down1a.send)
    k.do(z_in1.wait, x_in1.send, z_out1.wait, x_out1.send, z_gate1.step, z_down1a.step)
    k.do(x_down0.wait, w_down0.start, s3.loop, z_down1a.step, s3.finish, z_rows.start)
    k.do(*wait(x_in1, x_out1, z_gate1, z_down1a))
    k.build()
    m0, gate0, up0, hid0 = (out for _, out, _ in g2.saved)
    z_rows = z_rows.out

    k = Kernel(2)
    x_gate1, z_up1 = x_move(k, z_gate1.out), z_gather_half(k, sh_up, t_up.out, 1)
    z_down1, x_up1 = z_gather_whole(k, sh_down, t_down1.out, 1, 1), x_move(k, z_up1.out)
    rows, gain_load = load_all(k, z_rows), gains_of(k, 1, t_gain.out)
    tables = [load_all(k, v) for v in table_arrays]
    w_in1 = Weight(k, "rows", z_in1.out, x_in1.out, True)
    w_out1 = Weight(k, "cols", z_out1.out, x_out1.out, True)
    g4 = Gather(k, rows.buf, (gain_load.buf, 0), [w_in1], save=(0, 1))
    attend = Attend(k, g4.values[0], tables, size)
    kept = [Save(k, v) for v in (attend.q_rot, attend.k_rot, attend.y)]
    s5 = Scatter(k, [attend.y], [w_out1], rows.buf)
    mid1 = Save(k, s5.out)
    k.do(x_gate1.send, z_up1.send, z_down1.send)
    k.do(rows.wait, gain_load.wait, g4.begin, z_up1.step, g4.loop, z_up1.step)
    k.do(lambda: attend.run(z_up1.wait, x_up1.send, z_down1.step))
    k.do(*(v.start for v in kept))
    k.do(s5.loop, z_down1.step, s5.finish, mid1.start)
    k.do(*wait(x_gate1, x_up1, z_down1))
    k.build()
    a1, proj1 = (out for _, out, _ in g4.saved)
    q_rot, k_rot, y1 = (v.out for v in kept)
    mid1 = mid1.out

    k = Kernel(3)
    rows, gain_load = load_all(k, mid1), gains_of(k, 1, t_gain.out)
    cot = start_rows(k, 1, t_seq.out)
    w_gate1 = Weight(k, "rows", z_gate1.out, x_gate1.out, True)
    w_up1 = Weight(k, "rows", z_up1.out, x_up1.out, True)
    w_down1 = Weight(k, "cols", z_down1a.out, z_down1.out, True, True)
    g6 = Gather(k, rows.buf, (gain_load.buf, 1), [w_gate1, w_up1], epilogue="ffn")
    g8 = Gather(
        k, cot.buf, None, [w_down1], [g6.values[0], g6.values[1]], trans=True, epilogue="ffn_back"
    )
    p_down1 = Product(k, g6.values[2], g8.full)
    p_gate1, p_up1 = Product(k, g6.full, g8.values[0]), Product(k, g6.full, g8.values[1])
    r_down1 = x_half(k, p_down1.out)
    s7 = Scatter(k, [g6.values[2]], [w_down1], rows.buf, low=True)
    s9 = Scatter(k, g8.values, [w_gate1, w_up1], cot.buf, (rows.buf, (gain_load.buf, 1)), True)
    y_rows, d_mid1, gain11 = Save(k, s7.out), Save(k, s9.out), Save(k, s9.gain_grad)
    k.do(rows.wait, gain_load.wait, g6.begin, cot.wait, g8.begin, g6.loop)
    k.do(g8.loop, p_down1.run, p_down1.wait, r_down1.send)
    k.do(s9.loop, s7.loop, p_gate1.run, p_up1.run, s9.finish, d_mid1.start, gain11.start)
    k.do(s7.finish, y_rows.start, p_gate1.wait, p_up1.wait)
    k.do(*wait(r_down1))
    k.build()
    y_rows, d_mid1, gain11 = y_rows.out, d_mid1.out, gain11.out

    k = Kernel(4)
    q_down1 = sum_scatter(k, "cols", p_down1.out, r_down1.out)
    r_gate1, q_up1 = x_slots(k, p_gate1.out, "rows"), sum_scatter(k, "rows", p_up1.out)
    rows, gain_load = load_all(k, d_mid1), gains_of(k, 1, t_gain.out)
    value = load_all(k, z_rows)
    tables = [load_all(k, v) for v in table_arrays]
    proj, q_load, k_load, y_load, a_load = (load_all(k, v) for v in (proj1, q_rot, k_rot, y1, a1))
    w_in1 = Weight(k, "rows", z_in1.out, x_in1.out, True)
    w_out1 = Weight(k, "cols", z_out1.out, x_out1.out, True)
    g10 = Gather(k, rows.buf, None, [w_out1], trans=True)
    p_out1 = Product(k, y_load.buf, g10.full)
    back = AttendBack(k, proj.buf, tables, size, q_load.buf, k_load.buf, g10.values[0])
    p_in1 = Product(k, a_load.buf, back.d_proj)
    r_out1 = x_half(k, p_out1.out)
    s11 = Scatter(
        k, [back.d_proj], [w_in1], rows.buf, (value.buf, (gain_load.buf, 0)), True, low=True
    )
    d_z, gain10 = Save(k, s11.out), Save(k, s11.gain_grad)
    head_gains = [Save(k, back.q_gain), Save(k, back.k_gain)]
    k.early += [q_up1.load, q_down1.load]
    k.do(r_gate1.send, rows.wait, g10.begin, q_up1.send, q_down1.send, g10.loop)
    k.do(q_up1.step, q_down1.step, y_load.wait, p_out1.run, p_out1.wait, r_out1.send)
    k.do(proj.wait, q_load.wait, k_load.wait, lambda: back.run(q_up1.step, q_down1.step))
    k.do(*(v.start for v in head_gains))
    k.do(gain_load.wait, value.wait, s11.loop, a_load.wait, p_in1.run)
    k.do(s11.finish, d_z.start, gain10.start, p_in1.wait)
    k.do(*wait(q_down1, q_up1, r_gate1, r_out1))
    k.build()
    d_z, gain10 = d_z.out, gain10.out
    q_gain, k_gain = (v.out for v in head_gains)

    k = Kernel(5)
    q_gate1, m_up1 = sum_scatter(k, "rows", p_gate1.out, r_gate1.out), x_move(k, q_up1.out, 0)
    q_out1 = sum_scatter(k, "cols", p_out1.out, r_out1.out)
    r_in1 = x_slots(k, p_in1.out, "rows")
    q_in1 = sum_scatter(k, "rows", p_in1.out, r_in1.out)
    e_down1 = Finish(k, q_down1.out, 1)
    rows, value, gain_load = load_all(k, d_z), load_all(k, mid0), gains_of(k, 0, t_gain.out)
    gate_load, up_load, hid_load, m_load = (load_all(k, v) for v in (gate0, up0, hid0, m0))
    w_gate0 = Weight(k, "rows", z_gate0.out, None, True)
    w_up0 = Weight(k, "rows", z_up0.out, x_up0.out, True)
    w_down0 = Weight(k, "cols", z_down0.out, x_down0.out, True)
    g12 = Gather(
        k, rows.buf, None, [w_down0], [gate_load.buf, up_load.buf], trans=True, epilogue="ffn_back"
    )
    p_down0 = Product(k, hid_load.buf, g12.full)
    p_gate0, p_up0 = Product(k, m_load.buf, g12.values[0]), Product(k, m_load.buf, g12.values[1])
    q_down0, r_gate0 = sum_scatter(k, "cols", p_down0.out), x_slots(k, p_gate0.out, "rows")
    s13 = Scatter(
        k, g12.values, [w_gate0, w_up0], rows.buf, (value.buf, (gain_load.buf, 1)), True
    )
    d_mid0, gain01 = Save(k, s13.out), Save(k, s13.gain_grad)
    k.early += [q_gate1.load, q_out1.load, e_down1.load]
    k.do(r_in1.send, rows.wait, g12.begin, q_gate1.send, q_out1.send, m_up1.send, e_down1.send)
    k.do(gate_load.wait, up_load.wait, q_gate1.step, q_out1.step, g12.loop, q_gate1.step)
    k.do(q_out1.step, hid_load.wait, p_down0.run, p_down0.wait, q_down0.add)
    k.do(r_in1.wait, q_in1.add, s13.loop, m_load.wait, p_gate0.run, p_gate0.wait, r_gate0.send)
    k.do(q_in1.step, q_down0.step, p_up0.run, q_in1.step)
    k.do(value.wait, gain_load.wait, s13.finish, d_mid0.start, gain01.start)
    k.do(q_down0.step, p_up0.wait)
    k.do(*wait(q_gate1, q_out1, q_in1, e_down1, m_up1, q_down0, r_gate0))
    k.build()
    d_mid0, gain01 = d_mid0.out, gain01.out

    k = Kernel(6)
    q_gate0 = sum_scatter(k, "rows", p_gate0.out, r_gate0.out)
    q_up0 = sum_scatter(k, "rows", p_up0.out)
    m_up0, m_down0 = x_move(k, q_up0.out, 1), x_move(k, q_down0.out, 1)
    e_gate1, e_out1, e_in1 = (Finish(k, v.out, 1) for v in (q_gate1, q_out1, q_in1))
    rows, gain_load = load_all(k, d_mid0), gains_of(k, 0, t_gain.out)
    x_load, taps = start_rows(k, 0, t_seq.out), load_all(k, conv_kernel)
    y_load, a_load, proj, value = (load_all(k, v) for v in (y0, a0, proj0, value0))
    w_in0 = Weight(k, "rows", z_in0.out, x_in0.out, True)
    w_cols = Weight(k, "conv", z_cols.out, x_cols.out, True)
    w_out0 = Weight(k, "cols", z_out0.out, x_out0.out, True)
    g14 = Gather(k, rows.buf, None, [w_out0], trans=True)
    p_out0 = Product(k, y_load.buf, g14.full)
    back = ConvBack(k, proj.buf, value.buf, taps.buf, g14.values[0])
    p_in0, p_cols = Product(k, a_load.buf, back.d_proj), Product(k, a_load.buf, back.d_value)
    r_out0, r_in0 = x_half(k, p_out0.out), x_slots(k, p_in0.out, "rows")
    r_cols = x_slots(k, p_cols.out, "conv")
    q_out0, q_in0 = sum_scatter(k, "cols", p_out0.out, r_out0.out), sum_scatter(k, "rows", p_in0.out, r_in0.out)
    q_cols = sum_scatter(k, "conv", p_cols.out, r_cols.out)
    e_gate0, e_out0, e_in0 = (Finish(k, v.out, 0) for v in (q_gate0, q_out0, q_in0))
    s15 = Scatter(
        k, [back.d_proj, back.d_value], [w_in0, w_cols], rows.buf,
        (x_load.buf, (gain_load.buf, 0)), True, low=True,
    )
    d_x = Save(k, s15.out)
    tap_rows = conv_kernel.shape[0]
    small = k.vmem((8, model_width), F32)
    small_out = Save(k, small)
    ready = [load_all(k, v) for v in (gain01, gain10, gain11)]
    head_loads = [load_all(k, v) for v in (q_gain, k_gain)]

    def fill_small():
        t = lax.axis_index("tensor")
        small.ref[...] = jnp.zeros_like(small.ref)
        small.ref[0:1, :] = s15.gain_grad.ref[...]
        for i, load in enumerate(ready):
            load.wait()
            small.ref[i + 1 : i + 2, :] = load.buf.ref[...]
        small.ref[4 : 4 + tap_rows, block_of(t, channels)] = back.d_kernel.ref[...]
        at = 0
        for load in head_loads:
            load.wait()
            width = load.buf.shape[1]
            small.ref[7:8, at : at + width] = load.buf.ref[...]
            at += width
        small_out.start()

    t_small = x_move(k, small_out.out)
    z_small = SumShare(k, [small_out.out, t_small.out], "dp")
    t_total = SumShare(k, [z_small.out], "tensor", slotted=True)
    y_val, dx_val = k.input(y_rows), d_x.out

    def result_moves(s, d, t):
        sources = [(s == 0, y_val.ref), (s == 1, dx_val.ref)]
        return [(sources, t_result.out.ref, {"section": 1 - s})], []

    t_result = Task(k, row_shape, "section", result_moves, 1)
    k.early += [q_gate0.load, q_up0.load, e_gate1.load, e_out1.load, e_in1.load]
    k.do(m_down0.send, rows.wait, g14.begin, q_gate0.send, q_up0.send)
    k.do(e_gate1.send, e_out1.send, e_in1.send, q_gate0.step, g14.loop)
    k.do(q_up0.step, q_gate0.step, y_load.wait, p_out0.run, p_out0.wait, r_out0.send)
    k.do(proj.wait, value.wait, taps.wait, back.run, a_load.wait)
    k.do(p_in0.run, p_cols.run, p_in0.wait, r_in0.send, p_cols.wait, r_cols.send)
    k.do(q_gate0.wait, e_gate0.add, q_up0.step, r_out0.wait, q_out0.add)
    k.do(x_load.wait, gain_load.wait, s15.loop, q_out0.step, s15.finish, d_x.start)
    k.do(fill_small, d_x.wait, t_result.send, small_out.wait, t_small.send)
    k.do(r_in0.wait, q_in0.add, r_cols.wait, q_cols.add, q_up0.wait, m_up0.send, q_out0.step)
    k.do(q_in0.step, q_cols.step, t_small.wait, z_small.add, q_in0.step, q_cols.step)
    k.do(q_out0.wait, e_out0.add, z_small.wait, t_total.add, q_in0.wait, e_in0.add)
    rest = (e_gate1, e_out1, e_in1, q_cols, m_down0, e_gate0, m_up0, e_out0, e_in0)
    k.do(*wait(*rest, t_total, t_result))
    k.build()

    owned = [
        ([e_in0], [e_in1], 1),
        ([e_out0], [e_out1], 1),
        ([e_gate0], [e_gate1], 1),
        ([q_up0, m_up0], [q_up1, m_up1], 1),
        ([q_down0, m_down0], [e_down1], 1),
        ([q_cols], [q_cols], 0),
    ]
    return pack(
        [(zero, one, lead) for zero, one, lead in owned], t_total, d_x.out, y_rows, t_result,
        (norm_gain.shape, conv_kernel.shape, qk_gain.shape),
    )


def slot_free(val, shape):
    value = val.out.array
    if value.ndim == 3 and value.shape[0] * value.shape[1] != shape[0]:
        value = jnp.sum(value.astype(F32), axis=0).astype(BF)
    return value.reshape(shape)


def pack_kernel(plan, *refs):
    n_in, leads, terms, tap_rows = plan
    ins, rest = refs[:n_in], refs[n_in:]
    result, gain_out, *grads, cols, taps, heads = rest[: len(leads) + 4]
    grads = [*grads, cols]
    room = iter(rest[len(leads) + 4 :])
    own_v, moved_v, small_v, *bufs = (next(room) for _ in range(3 + len(terms)))
    out_v = [next(room) for _ in leads]
    load_sem, store_sem = room
    s, t = lax.axis_index("section"), lax.axis_index("tensor")
    small, d_x, y_rows, moved, *parts = ins

    def either(cond, zero, one, dst, sem):
        if zero is not None:
            pl.when(cond)(pltpu.make_async_copy(zero, dst, sem).start)
        if one is not None:
            pl.when(jnp.logical_not(cond))(pltpu.make_async_copy(one, dst, sem).start)

    first = s == 0
    either(first, d_x, y_rows, own_v, load_sem.at[0])
    pltpu.make_async_copy(moved, moved_v, load_sem.at[1]).start()
    pltpu.make_async_copy(small, small_v, load_sem.at[2]).start()
    for j, (zero, one, _) in enumerate(terms):
        either(
            first,
            None if zero is None else parts[zero],
            None if one is None else parts[one],
            bufs[j],
            load_sem.at[3 + j],
        )
    for j, (zero, one, i) in enumerate(terms):
        arrive = pltpu.make_async_copy(parts[one if zero is None else zero], bufs[j], load_sem.at[3 + j])
        begins = j == 0 or terms[j - 1][2] != i

        def put(j=j, i=i, begins=begins):
            value = bufs[j][...].astype(F32)
            value = value if begins else out_v[i][...] + value
            out_v[i][...] = value

        if zero is None or one is None:
            cond = first if one is None else jnp.logical_not(first)

            @pl.when(cond)
            def _(arrive=arrive, put=put):
                arrive.wait()
                put()
        else:
            arrive.wait()
            put()
        if j + 1 == len(terms) or terms[j + 1][2] != i:
            dst = grads[i].at[0] if leads[i] else grads[i]
            pltpu.make_async_copy(out_v[i], dst, store_sem.at[i]).start()
    pltpu.make_async_copy(d_x, own_v, load_sem.at[0]).wait()
    pltpu.make_async_copy(moved, moved_v, load_sem.at[1]).wait()
    n = len(leads)
    stores = [
        pltpu.make_async_copy(own_v, result.at[0, s], store_sem.at[n]),
        pltpu.make_async_copy(moved_v, result.at[0, 1 - s], store_sem.at[n + 1]),
    ]
    for store in stores:
        store.start()
    pltpu.make_async_copy(small, small_v, load_sem.at[2]).wait()
    total = small_v[0]
    for i in range(1, small_v.shape[0]):
        total = total + small_v[i]
    gain_out[0] = jnp.where(first, total[0:2], total[2:4])
    channels, size = taps.shape[1], heads.shape[1]
    chosen = total[4 : 4 + tap_rows, 0:channels]
    for i in range(1, total.shape[1] // channels):
        chosen = jnp.where(t == i, total[4 : 4 + tap_rows, i * channels : (i + 1) * channels], chosen)
    taps[...] = chosen
    at = 0
    for row, width in enumerate((channels, channels // 2)):
        value = total[7:8, at : at + size]
        for i in range(1, width // size):
            value = value + total[7:8, at + i * size : at + (i + 1) * size]
        heads[row : row + 1, :] = value
        at += width
    for i, store in enumerate(leads):
        dst = grads[i].at[0] if store else grads[i]
        pltpu.make_async_copy(out_v[i], dst, store_sem.at[i]).wait()
    for store in stores:
        store.wait()


def pack(owned, small, d_x, y_rows, moved, shapes):
    gain_shape, tap_shape, head_shape = shapes
    parts, terms, leads, out_shapes = [], [], [], []
    for i, (zero, one, lead) in enumerate(owned):
        whole = zero[0].out.shape
        if lead and len(whole) == 3 and isinstance(zero[0], Finish):
            shape = (whole[0] * whole[1], whole[2])
        else:
            shape = whole[-2:]
        shape = tuple(shape)
        leads.append(lead)
        out_shapes.append(shape)
        for j in range(max(len(zero), len(one))):
            pair = []
            for side in (zero, one):
                if j < len(side):
                    parts.append(slot_free(side[j], shape))
                    pair.append(len(parts) - 1)
                else:
                    pair.append(None)
            terms.append((*pair, i))
    operands = [small.out.array, d_x.array, y_rows.array, moved.out.array, *parts]
    rows = d_x.shape
    smem = pl.BlockSpec(memory_space=pltpu.VMEM)
    out_shape = [jax.ShapeDtypeStruct((1, 2) + rows, BF), jax.ShapeDtypeStruct(gain_shape, F32)]
    out_shape += [
        jax.ShapeDtypeStruct((1,) + v if lead else v, F32) for v, lead in zip(out_shapes, leads)
    ]
    out_shape += [jax.ShapeDtypeStruct(v, F32) for v in (tap_shape, head_shape)]
    n = len(leads)
    return tuple(
        pl.pallas_call(
            functools.partial(
                pack_kernel, (len(operands), tuple(leads), tuple(terms), tap_shape[0])
            ),
            out_shape=out_shape,
            in_specs=[ANY] * len(operands),
            out_specs=[ANY, smem] + [ANY] * n + [smem] * 2,
            scratch_shapes=[pltpu.VMEM(rows, BF)] * 2
            + [pltpu.VMEM(small.out.shape, F32)]
            + [pltpu.VMEM(out_shapes[i], BF) for _, _, i in terms]
            + [pltpu.VMEM(v, F32) for v in out_shapes]
            + [DMA((3 + len(terms),)), DMA((n + 2,))],
            compiler_params=pltpu.CompilerParams(vmem_limit_bytes=VMEM_BYTES),
            name="pack",
        )(*operands)
    )


def solution(mesh):
    in_specs = (
        P("section", "dp", "tensor", None),
        P("section", None, None),
        P("section", "dp", "tensor"),
        P("section", "tensor", "dp"),
        P("section", "dp", "tensor"),
        P("section", "dp", "tensor"),
        P("section", "tensor", "dp"),
        P(("section", "dp"), "tensor"),
        P(None, "tensor"),
        P(),
    )
    out_specs = (
        P("section", "dp", "tensor", None),
        P("section", None, None),
        P("section", "dp", "tensor"),
        P("section", "tensor", "dp"),
        P("section", "dp", "tensor"),
        P("section", "dp", "tensor"),
        P("section", "tensor", "dp"),
        P(("section", "dp"), "tensor"),
        P(None, "tensor"),
        P(),
    )
    return jax.shard_map(body, mesh=mesh, in_specs=in_specs, out_specs=out_specs, check_vma=False)
```

```python
import functools

import jax
import jax.numpy as jnp
from jax import lax
from jax.experimental import pallas as pl
from jax.experimental.pallas import tpu as pltpu
from jax.sharding import PartitionSpec as P

HEADS = 16
KV_HEADS = 8

EPS = 1e-05
ROPE_BASE = 1000000.0
MASKED = -1e30

MESH = pl.DeviceIdType.MESH
ANY = pl.BlockSpec(memory_space=pl.ANY)
DMA = pltpu.SemaphoreType.DMA
VMEM_BYTES = 63 * 1024 * 1024
BF = jnp.bfloat16
F32 = jnp.float32
ROW_BLOCK = 256


def contract(left_op, right_op, left_dim, right_dim):
    return lax.dot_general(
        left_op, right_op, (((left_dim,), (right_dim,)), ((), ())), preferred_element_type=F32
    )


def norm_rows(values, gain):
    return values * lax.rsqrt(jnp.mean(values * values, axis=-1, keepdims=True) + EPS) * gain


def norm_back(values, gain, grad_in):
    row_scale = lax.rsqrt(jnp.mean(values * values, axis=-1, keepdims=True) + EPS)
    normed = values * row_scale
    gain_grad = jnp.sum(grad_in * normed, axis=0, keepdims=True)
    scaled = grad_in * gain
    value_grad = row_scale * (scaled - normed * jnp.mean(scaled * normed, axis=-1, keepdims=True))
    return (value_grad, gain_grad)


class Angles:
    def __init__(self, k, length, head_size, width):
        self.half = head_size // 2
        self.tables = [k.vmem((length, width), F32) for _ in range(2)]
        self.saves = [Save(k, v) for v in self.tables]

    def run(self):
        cos, sin = self.tables
        shape = (ROW_BLOCK, cos.shape[1])
        column = (lax.broadcasted_iota(jnp.int32, shape, 1) % self.half).astype(F32)
        frequency = ROPE_BASE ** (-(column / self.half))
        row = lax.broadcasted_iota(jnp.int32, shape, 0)

        def step(i, carry):
            rows = block_of(i, ROW_BLOCK)
            angle = (row + i * ROW_BLOCK).astype(F32) * frequency
            cos.ref[rows, :] = jnp.cos(angle)
            sin.ref[rows, :] = jnp.sin(angle)
            return carry

        lax.fori_loop(0, cos.shape[0] // ROW_BLOCK, step, 0)
        for save in self.saves:
            save.start()


def silu_parts(gate):
    sig = 1.0 / (1.0 + jnp.exp(-gate))
    return sig, gate * sig


def dp_size():
    return lax.axis_size("dp")


def spot():
    return tuple(lax.axis_index(a) for a in ("section", "dp", "tensor"))


def block_of(index, size):
    return pl.ds(pl.multiple_of(index * size, size), size)


class Val:
    def __init__(self, shape, dtype):
        self.shape, self.dtype = tuple(shape), dtype
        self.ref = self.array = None


class Kernel:
    def __init__(self, cid):
        self.cid, self.ins, self.arrays, self.outs, self.room = cid, [], [], [], []
        self.early, self.steps, self.late, self.axes = [], [], [], {"tensor"}
        self.once = []

    def input(self, array):
        array = array.array if isinstance(array, Val) else array
        for val, known in zip(self.ins, self.arrays):
            if known is array:
                return val
        val = Val(array.shape, array.dtype)
        self.ins.append(val)
        self.arrays.append(array)
        return val

    def output(self, shape, dtype):
        val = Val(shape, dtype)
        self.outs.append(val)
        return val

    def vmem(self, shape, dtype):
        val = Val(shape, dtype)
        self.room.append((val, pltpu.VMEM(tuple(shape), dtype)))
        return val

    def sem(self, *shape):
        val = Val(shape, None)
        self.room.append((val, DMA(shape)))
        return val

    def do(self, *steps):
        self.steps += steps

    def body(self, *refs):
        vals = self.ins + self.outs + [val for val, _ in self.room]
        for val, ref in zip(vals, refs):
            val.ref = ref
        for item in self.once:
            item.waited = False
            item.phase = 0
        for step in self.early:
            step()
        self.greet()
        for step in self.steps + self.late:
            step()

    def greet(self):
        s, d, t = spot()
        peers = []
        if "section" in self.axes:
            peers.append({"section": 1 - s})
        if "dp" in self.axes:
            peers += [{"dp": (d + k) % dp_size()} for k in range(1, dp_size())]
        peers += [{"tensor": (t + k) % 4} for k in range(1, 4)]
        barrier = pltpu.get_barrier_semaphore()
        for peer in peers:
            pl.semaphore_signal(barrier, inc=1, device_id=peer, device_id_type=MESH)
        pl.semaphore_wait(barrier, len(peers))

    def build(self):
        result = pl.pallas_call(
            self.body,
            out_shape=[jax.ShapeDtypeStruct(v.shape, v.dtype) for v in self.outs],
            in_specs=[ANY] * len(self.ins),
            out_specs=[ANY] * len(self.outs),
            scratch_shapes=[room for _, room in self.room],
            compiler_params=pltpu.CompilerParams(
                collective_id=self.cid, has_side_effects=True, vmem_limit_bytes=VMEM_BYTES
            ),
            name=f"stage{self.cid}",
        )(*self.arrays)
        for val, array in zip(self.outs, result):
            val.array = array


def remote(src, dst, send_sem, recv_sem, peer):
    return pltpu.make_async_remote_copy(
        src_ref=src, dst_ref=dst, send_sem=send_sem, recv_sem=recv_sem,
        device_id=peer, device_id_type=MESH,
    )


class Load:
    def __init__(self, k, sources, shape, dtype, early=False):
        self.k, self.sources, self.waited = k, sources, False
        self.buf, self.sem = k.vmem(shape, dtype), k.sem(1)
        k.once.append(self)
        if early:
            k.early.append(self.start)

    def moves(self):
        for cond, source in self.sources(*spot()):
            yield cond, pltpu.make_async_copy(source, self.buf.ref, self.sem.ref.at[0])

    def start(self):
        for cond, move in self.moves():
            if cond is None:
                move.start()
            else:
                pl.when(cond)(move.start)

    def wait(self):
        if not self.waited:
            self.waited = True
            next(self.moves())[1].wait()


def load_all(k, array, early=True):
    val = k.input(array)
    return Load(k, lambda s, d, t: [(None, val.ref)], val.shape, val.dtype, early)


class Save:
    def __init__(self, k, buf):
        self.buf, self.out, self.sem = buf, k.output(buf.shape, buf.dtype), k.sem(1)
        self.waited = False
        k.once.append(self)
        k.late.append(self.wait)

    def move(self):
        return pltpu.make_async_copy(self.buf.ref, self.out.ref, self.sem.ref.at[0])

    def start(self):
        self.move().start()

    def wait(self):
        if not self.waited:
            self.waited = True
            self.move().wait()


class Task:
    final = None

    def __init__(self, k, out, axis, moves, count, n_local=1, out_dtype=BF):
        self.k, self.axis, self.make = k, axis, moves
        self.out = k.output(out, out_dtype)
        self.send_sem, self.recv_sem, self.local_sem = k.sem(count), k.sem(count), k.sem(n_local)
        self.waited = False
        k.axes.add(axis)
        k.once.append(self)

    def local(self, src, dst, i):
        return pltpu.make_async_copy(src, dst, self.local_sem.ref.at[i])

    def pairs(self, every):
        far, near = self.make(*spot())
        for i, (sources, dst, peer) in enumerate(far):
            for cond, src in sources if every else sources[:1]:
                yield cond, True, remote(
                    src, dst, self.send_sem.ref.at[i], self.recv_sem.ref.at[i], peer
                )
        for i, (sources, dst) in enumerate(near):
            for cond, src in sources if every else sources[:1]:
                yield cond, False, self.local(src, dst, i)

    def step(self):
        pass

    def send(self):
        for cond, far, move in self.pairs(True):
            if far and self.final is not None:
                cond = lax.axis_index("section") == 1 - self.final
            if cond is None:
                move.start()
            else:
                pl.when(cond)(move.start)

    def wait(self):
        if self.waited:
            return
        self.waited = True
        s = lax.axis_index("section")
        for _, far, move in self.pairs(False):
            if not far:
                move.wait()
            elif self.final is None:
                move.wait_recv()
                move.wait_send()
            else:
                pl.when(s == 1 - self.final)(move.wait_send)
                pl.when(s == self.final)(move.wait_recv)


def as_val(k, value):
    value = value.out if isinstance(value, Task) else value
    known = isinstance(value, Val) and (value.array is None)
    return value if known else k.input(value)


class Line(Task):
    def __init__(self, k, out, out_dtype=BF, n_local=1):
        super().__init__(k, out, "dp", None, 6, n_local, out_dtype)
        self.send_sem, self.recv_sem = k.sem(2, 3), k.sem(2, 3)
        self.phase = 0

    def hop(self, j, way, src, dst):
        d = lax.axis_index("dp")
        peer = {"dp": (d + 1 if way == 0 else d + 3) % 4}
        return remote(src, dst, self.send_sem.ref.at[way, j], self.recv_sem.ref.at[way, j], peer)


class LineGather(Line):
    def __init__(self, k, sources, shape, dtype):
        super().__init__(k, (4,) + shape, dtype)
        self.sources = sources

    def ends(self, j, way):
        d = lax.axis_index("dp")
        if way == 0:
            return (d >= j) & (d < 3), d >= j + 1
        return (d <= 3 - j) & (d > 0), d <= 2 - j

    def copy(self, j, way, src=None):
        d = lax.axis_index("dp")
        slot = (d + 4 - j if way == 0 else d + j) % 4
        piece = self.out.ref.at[slot]
        return self.hop(j, way, piece if src is None else src, piece)

    def send(self):
        self.phase = 0
        for cond, src in self.sources(*spot()):
            own = self.local(src, self.out.ref.at[lax.axis_index("dp")], 0)
            moves = [(True if cond is None else cond, own)]
            for way in range(2):
                sends = self.ends(0, way)[0]
                moves.append((sends if cond is None else sends & cond, self.copy(0, way, src)))
            for when, move in moves:
                if when is True:
                    move.start()
                else:
                    pl.when(when)(move.start)

    def arrive(self, j):
        for way in range(2):
            pl.when(self.ends(j, way)[1])(self.copy(j, way).wait_recv)

    def step(self):
        self.arrive(self.phase)
        self.phase += 1
        for way in range(2):
            pl.when(self.ends(self.phase, way)[0])(self.copy(self.phase, way).start)

    def wait(self):
        if self.waited:
            return
        self.waited = True
        while self.phase < 2:
            self.step()
        self.arrive(2)
        for j in range(3):
            for way in range(2):
                pl.when(self.ends(j, way)[0])(self.copy(j, way).wait_send)
        d = lax.axis_index("dp")
        self.local(self.sources(*spot())[0][1], self.out.ref.at[d], 0).wait()


def z_gather_from(k, sources, shape, dtype):
    count = dp_size()
    if count == 4:
        return LineGather(k, sources, shape, dtype)

    def moves(s, d, t):
        dst, found = task.out.ref.at[d], sources(s, d, t)
        return [(found, dst, {"dp": (d + i) % count}) for i in range(1, count)], [(found, dst)]

    task = Task(k, (count,) + shape, "dp", moves, count - 1, out_dtype=dtype)
    return task


def z_gather(k, value):
    val = as_val(k, value)
    return z_gather_from(k, lambda s, d, t: [(None, val.ref)], val.shape, val.dtype)


def z_gather_half(k, shard, moved, block):
    shard, moved = as_val(k, shard), as_val(k, moved)
    rows = shard.shape[0] // 2

    def sources(s, d, t):
        own = shard.ref.at[pl.ds(block * rows, rows)]
        return [(s == block, own), (s == 1 - block, moved.ref)]

    return z_gather_from(k, sources, moved.shape, shard.dtype)


def one_way(task, sender):
    task.final = None if sender is None else 1 - sender
    return task


def z_gather_whole(k, shard, moved, block, half=None):
    shard, moved = as_val(k, shard), as_val(k, moved)
    rows = shard.shape[0] if half is None else shard.shape[0] // 2
    part = pl.ds(0 if half is None else half * rows, rows)

    def sources(s, d, t):
        return [(s == block, shard.ref.at[part]), (s == 1 - block, moved.ref.at[part])]

    return z_gather_from(k, sources, (rows,) + shard.shape[1:], shard.dtype)


def x_move(k, value, sender=None):
    val = as_val(k, value)

    def moves(s, d, t):
        return [([(None, val.ref)], task.out.ref, {"section": 1 - s})], []

    task = Task(k, val.shape, "section", moves, 1, out_dtype=val.dtype)
    return one_way(task, sender)


def x_half(k, value, sender=None):
    val = as_val(k, value)
    rows = val.shape[0] // 2

    def moves(s, d, t):
        src = val.ref.at[block_of(1 - s, rows)]
        return [([(None, src)], task.out.ref, {"section": 1 - s})], []

    task = Task(k, (rows,) + val.shape[1:], "section", moves, 1, out_dtype=val.dtype)
    return one_way(task, sender)


def x_slots(k, value, kind):
    val, count = as_val(k, value), dp_size()
    rows = val.shape[0] // (2 * count)

    def moves(s, d, t):
        far = []
        for i in range(count):
            slot = 2 * i + 1 - s if kind == "rows" else (1 - s) * count + i
            src = val.ref.at[block_of(slot, rows)]
            far.append(([(None, src)], task.out.ref.at[i], {"section": 1 - s}))
        return far, []

    task = Task(k, (count, rows) + val.shape[1:], "section", moves, count)
    return task


class Terms:
    def __init__(self, k, kind, grads, received, local):
        self.grads, self.local = as_val(k, grads), local
        self.kind, self.n = kind, dp_size()
        self.whole = received is None
        if self.whole:
            rows, cols = self.grads.shape
            self.rows = rows if kind == "cols" else rows // self.n
            self.cols = cols // self.n if kind == "cols" else cols
            self.shape = (self.n, self.rows, self.cols)
            self.aside = kind == "cols" and self.cols % 128 != 0
            self.total = k.vmem(self.shape, BF)
            self.kept = k.vmem(self.grads.shape, BF) if self.aside else self.total
            return
        self.received = as_val(k, received)
        if kind == "cols":
            self.rows, self.cols = self.grads.shape[0] // 2, self.grads.shape[1] // self.n
            held = (self.rows, self.grads.shape[1])
        else:
            self.rows, self.cols = self.grads.shape[0] // (2 * self.n), self.grads.shape[1]
            held = (self.n, self.rows, self.cols)
        self.kept, self.got = k.vmem(held, BF), k.vmem(held, BF)
        self.shape = (self.n, self.rows, self.cols)
        self.total = k.vmem(self.shape, BF) if kind == "cols" else self.kept

    def loads(self):
        s, grads, kept = lax.axis_index("section"), self.grads.ref, self.kept.ref
        if self.whole and self.aside:
            return [self.local(grads, kept, 2)]
        if self.whole:
            parts = [
                grads.at[:, pl.ds(i * self.cols, self.cols)]
                if self.kind == "cols"
                else grads.at[block_of(i, self.rows)]
                for i in range(self.n)
            ]
            return [self.local(part, kept.at[i], 2 + i) for i, part in enumerate(parts)]
        if self.kind == "cols":
            moves = [self.local(grads.at[block_of(s, self.rows)], kept, 2)]
        else:
            moves = []
            for i in range(self.n):
                slot = 2 * i + s if self.kind == "rows" else s * self.n + i
                moves.append(self.local(grads.at[block_of(slot, self.rows)], kept.at[i], 2 + i))
        return moves + [self.local(self.received.ref, self.got.ref, 1)]

    def load(self):
        for move in self.loads():
            move.start()

    def add(self):
        for move in self.loads():
            move.wait()
        if self.whole and self.aside:
            for i in range(self.n):
                self.total.ref[i] = self.kept.ref[:, i * self.cols : (i + 1) * self.cols]
        if self.whole:
            return
        kept, got, total = self.kept.ref, self.got.ref, self.total.ref
        for i in range(self.n):
            if self.kind == "cols":
                part = (slice(None), slice(i * self.cols, (i + 1) * self.cols))
            else:
                part = i
            total[i] = (kept[part].astype(F32) + got[part].astype(F32)).astype(BF)


class DirectScatter(Task):
    def __init__(self, k, kind, grads, received):
        self.terms = Terms(k, kind, grads, received, lambda *a: self.local(*a))
        count = dp_size()

        def moves(s, d, t):
            total = self.terms.total.ref
            far = []
            for i in range(1, count):
                other = (d + i) % count
                far.append(([(None, total.at[other])], self.out.ref.at[d], {"dp": other}))
            return far, [([(None, total.at[d])], self.out.ref.at[d])]

        super().__init__(k, self.terms.shape, "dp", moves, count - 1, 2 + count)
        self.load = self.terms.load

    def send(self):
        self.terms.add()
        super().send()

    def add(self):
        self.load()
        self.send()


class LineScatter(Line):
    def __init__(self, k, kind, grads, received):
        self.terms = Terms(k, kind, grads, received, lambda *a: self.local(*a))
        super().__init__(k, self.terms.shape[1:], BF, 6)
        self.got = k.vmem((2, 3) + self.terms.shape[1:], BF)
        self.load = self.terms.load

    def ends(self, j, way):
        d = lax.axis_index("dp")
        if way == 0:
            return (d <= j) & (d < 3), (d >= 1) & (d <= j + 1)
        return (d >= 3 - j) & (d > 0), (d <= 2) & (d >= 2 - j)

    def copy(self, j, way):
        d = lax.axis_index("dp")
        to = (d + 3 - j if way == 0 else d + 1 + j) % 4
        return self.hop(j, way, self.terms.total.ref.at[to], self.got.ref.at[way, j])

    def send(self):
        self.phase = 0
        self.terms.add()
        for way in range(2):
            pl.when(self.ends(0, way)[0])(self.copy(0, way).start)

    def take(self, j, way):
        d = lax.axis_index("dp")
        to = (d + 2 - j if way == 0 else d + 2 + j) % 4
        self.copy(j, way).wait_recv()
        total = self.terms.total.ref
        total[to] = (total[to].astype(F32) + self.got.ref[way, j].astype(F32)).astype(BF)

    def arrive(self, j):
        for way in range(2):
            pl.when(self.ends(j, way)[1])(functools.partial(self.take, j, way))

    def step(self):
        self.arrive(self.phase)
        self.phase += 1
        for way in range(2):
            pl.when(self.ends(self.phase, way)[0])(self.copy(self.phase, way).start)

    def wait(self):
        if self.waited:
            return
        self.waited = True
        while self.phase < 2:
            self.step()
        self.arrive(2)
        done = self.local(self.terms.total.ref.at[lax.axis_index("dp")], self.out.ref, 0)
        done.start()
        for j in range(3):
            for way in range(2):
                pl.when(self.ends(j, way)[0])(self.copy(j, way).wait_send)
        done.wait()

    def add(self):
        self.load()
        self.send()


def sum_scatter(k, kind, grads, received=None):
    return (LineScatter if dp_size() == 4 else DirectScatter)(k, kind, grads, received)


class Finish(Task):
    def __init__(self, k, pieces, block):
        self.pieces, self.final = as_val(k, pieces), block
        *slots, rows, cols = self.pieces.shape
        self.slots = slots[0] if slots else 0
        if slots:
            self.held, self.total = k.vmem(self.pieces.shape, BF), k.vmem((rows, cols), BF)
        else:
            self.total = self.pieces

        def moves(s, d, t):
            source, dst = [(None, self.total.ref)], self.out.ref.at[s]
            return [(source, dst, {"section": 1 - s})], [(source, dst)]

        super().__init__(k, (2, rows, cols), "section", moves, 1, 2)

    def load(self):
        if self.slots:
            self.local(self.pieces.ref, self.held.ref, 1).start()

    def send(self):
        if self.slots:
            self.local(self.pieces.ref, self.held.ref, 1).wait()
            acc = self.held.ref[0].astype(F32)
            for i in range(1, self.slots):
                acc = acc + self.held.ref[i].astype(F32)
            self.total.ref[...] = acc.astype(BF)
        super().send()

    def add(self):
        self.load()
        self.send()


class SumShare(Task):
    def __init__(self, k, terms, axis, slotted=False):
        self.terms = [as_val(k, v) for v in terms]
        shape = self.terms[0].shape[1:] if slotted else self.terms[0].shape
        count = dp_size() if axis == "dp" else 4
        self.slotted = slotted
        self.bufs = [k.vmem(v.shape, F32) for v in self.terms]
        self.total = k.vmem(shape, F32)

        def moves(s, d, t):
            source, me = [(None, self.total.ref)], d if axis == "dp" else t
            dst = self.out.ref.at[me]
            far = [(source, dst, {axis: (me + i) % count}) for i in range(1, count)]
            return far, [(source, dst)]

        super().__init__(k, (count,) + shape, axis, moves, count - 1, 3, out_dtype=F32)

    def add(self):
        loads = [self.local(v.ref, b.ref, 1 + i) for i, (v, b) in enumerate(zip(self.terms, self.bufs))]
        for load in loads:
            load.start()
        for load in loads:
            load.wait()
        if self.slotted:
            parts = [self.bufs[0].ref[i] for i in range(self.terms[0].shape[0])]
        else:
            parts = [buf.ref[...] for buf in self.bufs]
        acc = parts[0]
        for part in parts[1:]:
            acc = acc + part
        self.total.ref[...] = acc
        self.send()


class Weight:
    def __init__(self, k, kind, near, far=None, early=False, fixed=False):
        near, far = as_val(k, near), None if far is None else as_val(k, far)
        self.count, self.rows, self.cols = near.shape
        self.kind, self.near, self.far, self.waited = kind, near, far, False
        sides, self.fixed = 1 if far is None else 2, fixed
        if kind == "cols":
            shape = (sides * self.rows, self.count * self.cols)
        else:
            shape = (sides * self.count * self.rows, self.cols)
        self.aside = kind == "cols" and self.cols % 128 != 0
        self.buf, self.sem = k.vmem(shape, BF), k.sem(2 * self.count)
        if self.aside:
            self.held = [k.vmem(near.shape, BF), k.vmem(near.shape, BF)]
        k.once.append(self)
        if early:
            k.early.append(self.start)

    def moves(self):
        s, dst = 0 if self.fixed else lax.axis_index("section"), self.buf.ref
        rows, cols = self.rows, self.cols

        def place(sec, own):
            if self.aside:
                return None
            if self.kind == "cols":
                return dst.at[block_of(sec, rows), pl.ds(own * cols, cols)]
            slot = own * 2 + sec if self.kind == "rows" else sec * self.count + own
            return dst.at[block_of(slot, rows)]

        if self.far is None:
            for i in range(self.count):
                if self.kind == "cols":
                    to = dst.at[:, pl.ds(i * cols, cols)]
                else:
                    to = dst.at[pl.ds(i * rows, rows)]
                to = self.held[0].ref.at[i] if self.aside else to
                yield pltpu.make_async_copy(self.near.ref.at[i], to, self.sem.ref.at[2 * i])
            return
        for i in range(self.count):
            for j, (val, sec) in enumerate(((self.near, s), (self.far, 1 - s))):
                to = self.held[j].ref.at[i] if self.aside else place(sec, i)
                yield pltpu.make_async_copy(val.ref.at[i], to, self.sem.ref.at[2 * i + j])

    def start(self):
        for move in self.moves():
            move.start()

    def wait(self):
        if self.waited:
            return
        self.waited = True
        for move in self.moves():
            move.wait()
        if self.aside:
            s = 0 if self.fixed else lax.axis_index("section")
            for j, sec in enumerate((s, 1 - s) if self.far is not None else (0,)):
                whole = jnp.concatenate([self.held[j].ref[i] for i in range(self.count)], axis=1)
                self.buf.ref[block_of(sec, self.rows), :] = whole


class Product:
    def __init__(self, k, left, right):
        self.left, self.right = left, right
        rows = left.shape[1]
        self.chunk = 384 if rows % 384 == 0 else 256
        self.count = rows // self.chunk
        self.buf = k.vmem((rows, right.shape[1]), BF)
        self.out, self.sem = k.output(self.buf.shape, BF), k.sem(self.count)

    def copy(self, i):
        part = block_of(i, self.chunk)
        return pltpu.make_async_copy(self.buf.ref.at[part], self.out.ref.at[part], self.sem.ref.at[i])

    def run(self):
        def step(i, carry):
            part = block_of(i, self.chunk)
            value = contract(self.left.ref[:, part], self.right.ref[...], 0, 0)
            self.buf.ref[part, :] = value.astype(BF)
            self.copy(i).start()
            return carry

        lax.fori_loop(0, self.count, step, 0)

    def wait(self):
        for i in range(self.count):
            self.copy(i).wait()


def places():
    me = lax.axis_index("tensor")
    sib = me + 1 - 2 * (me % 2)
    cross = (me + 2) % 4
    diag = (sib + 2) % 4
    return me, sib, cross, diag


class Gather:
    def __init__(self, k, x, gain, weights, extras=(), trans=False, epilogue="plain", save=()):
        rows, width = x.shape
        length = 4 * rows
        self.k, self.x, self.gain, self.weights, self.extras = k, x, gain, weights, extras
        self.trans, self.epilogue, self.rows, self.half = trans, epilogue, rows, rows // 2
        cols = [w.buf.shape[0 if trans else 1] for w in weights]
        kinds = {
            "plain": [(c, F32) for c in cols],
            "ffn": [(cols[0], BF)] * 3,
            "ffn_back": [(cols[0], BF)] * 2,
        }[epilogue]
        self.full = k.vmem((length, width), BF)
        self.values = [k.vmem((length, c), kind) for c, kind in kinds]
        kept = [self.full] + self.values
        self.saved = [(v, k.output(v.shape, v.dtype), k.sem(4, 2)) for v in kept if kept.index(v) in save]
        self.sems = [k.sem(2) for _ in range(6)]
        k.late.append(self.end)

    def span(self, owner, sub):
        return pl.ds(pl.multiple_of(owner * self.rows + sub * self.half, self.half), self.half)

    def move(self, kind, i):
        me, sib, cross, _ = places()
        full = self.full.ref
        owner, peer, at = {"cross": (me, cross, 0), "sib": (me, sib, 2), "relay": (cross, sib, 4)}[kind]
        part = full.at[self.span(owner, i)]
        return remote(
            part, part, self.sems[at].ref.at[i], self.sems[at + 1].ref.at[i], {"tensor": peer}
        )

    def begin(self):
        me = places()[0]
        for i in range(2):
            part = self.x.ref[pl.ds(i * self.half, self.half), :].astype(F32)
            if self.gain is not None:
                val, row = self.gain
                part = norm_rows(part, val.ref[row : row + 1, :])
            self.full.ref[self.span(me, i), :] = part.astype(BF)
            self.move("cross", i).start()
            self.move("sib", i).start()

    def loop(self):
        me, sib, cross, diag = places()
        rows, half = self.rows, self.half
        for w in self.weights:
            w.wait()

        def step(p, carry):
            far, sub = p // 2, p % 2
            near = (1 - sub) * me + sub * sib
            first = (1 - far) * near * rows + far * (cross * rows + sub * half)
            second = (1 - far) * (near * rows + half) + far * (diag * rows + sub * half)
            pair = [pl.ds(pl.multiple_of(v, half), half) for v in (first, second)]

            @pl.when(p == 1)
            def _():
                self.move("sib", 0).wait_recv()
                self.move("sib", 1).wait_recv()

            for i in range(2):

                @pl.when(p == 2 + i)
                def _():
                    self.move("cross", i).wait_recv()
                    self.move("relay", i).start()
                    self.move("relay", i).wait_recv()

            def both(val):
                return jnp.concatenate([val.ref[pair[0], :], val.ref[pair[1], :]], axis=0)

            a = both(self.full)
            prods = [contract(a, w.buf.ref[...], 1, 1 if self.trans else 0) for w in self.weights]
            if self.epilogue == "plain":
                values = prods
            elif self.epilogue == "ffn":
                sig, silu = silu_parts(prods[0])
                values = [prods[0], prods[1], silu * prods[1]]
            else:
                gate, up = (both(v).astype(F32) for v in self.extras)
                sig, silu = silu_parts(gate)
                values = [prods[0] * up * sig * (1.0 + gate * (1.0 - sig)), prods[0] * silu]
            for val, value in zip(self.values, values):
                value = value.astype(val.dtype)
                for j in range(2):
                    val.ref[pair[j], :] = value[j * half : (j + 1) * half]
            for val, out, sem in self.saved:
                for j in range(2):
                    pltpu.make_async_copy(
                        val.ref.at[pair[j]], out.ref.at[pair[j]], sem.ref.at[p, j]
                    ).start()
            return carry

        lax.fori_loop(0, 4, step, 0)

    def end(self):
        for i in range(2):
            for kind in ("cross", "sib", "relay"):
                self.move(kind, i).wait_send()
        part = pl.ds(0, self.half)
        for val, out, sem in self.saved:
            for p in range(4):
                for j in range(2):
                    pltpu.make_async_copy(val.ref.at[part], out.ref.at[part], sem.ref.at[p, j]).wait()


class Scatter:
    def __init__(self, k, operands, weights, resid, back=None, trans=False, low=False):
        rows, width = resid.shape
        half = rows // 2
        self.operands, self.weights, self.resid, self.back = operands, weights, resid, back
        self.trans, self.low, self.rows, self.half = trans, low, rows, half
        self.keep, self.own = k.vmem((2, half, width), F32), k.vmem((rows, width), F32)
        self.to_s, self.from_s, self.to_c, self.from_c = (
            k.vmem((2, half, width), BF) for _ in range(4)
        )
        self.to_o, self.from_o = k.vmem((rows, width), BF), k.vmem((rows, width), BF)
        self.out = k.vmem((rows, width), BF if low else F32)
        self.gain_grad = k.vmem((1, width), F32) if back else None
        self.sems = [k.sem(2) for _ in range(4)] + [k.sem(1) for _ in range(2)]
        k.late.append(self.end)

    def move(self, kind, i=0):
        _, sib, cross, _ = places()
        at, src, dst, peer = {
            "diag": (0, self.to_s, self.from_s, sib),
            "cross": (2, self.to_c, self.from_c, cross),
            "near": (4, self.to_o, self.from_o, sib),
        }[kind]
        src, dst = (src.ref, dst.ref) if kind == "near" else (src.ref.at[i], dst.ref.at[i])
        return remote(
            src, dst, self.sems[at].ref.at[i], self.sems[at + 1].ref.at[i], {"tensor": peer}
        )

    def pass_on(self, i):
        self.move("diag", i).wait_recv()
        total = self.keep.ref[i] + self.from_s.ref[i].astype(F32)
        self.to_c.ref[i] = total.astype(BF)
        self.move("cross", i).start()

    def loop(self):
        me, sib, cross, diag = places()
        rows, half = self.rows, self.half
        for w in self.weights:
            w.wait()

        def step(p, carry):
            near, sub = p // 2, p % 2
            base = near * ((1 - sub) * sib + sub * me) * rows
            first = base + (1 - near) * (cross * rows + sub * half)
            second = base + near * half + (1 - near) * (diag * rows + sub * half)
            pair = [pl.ds(pl.multiple_of(v, half), half) for v in (first, second)]
            total = None
            for y, w in zip(self.operands, self.weights):
                a = jnp.concatenate([y.ref[pair[0], :], y.ref[pair[1], :]], axis=0)
                prod = contract(a, w.buf.ref[...], 1, 1 if self.trans else 0)
                total = prod if total is None else total + prod

            for i in range(2):

                @pl.when(p == i)
                def _():
                    self.keep.ref[i] = total[:half]
                    self.to_s.ref[i] = total[half:].astype(BF)
                    self.move("diag", i).start()

            @pl.when(p == 1)
            def _():
                self.pass_on(0)

            @pl.when(p == 2)
            def _():
                self.to_o.ref[...] = total.astype(BF)
                self.move("near").start()
                self.pass_on(1)

            @pl.when(p == 3)
            def _():
                self.own.ref[...] = total

            return carry

        lax.fori_loop(0, 4, step, 0)

    def finish(self):
        self.move("near").wait_recv()
        gain_sum = None
        for i in range(2):
            part = pl.ds(i * self.half, self.half)
            self.move("cross", i).wait_recv()
            total = self.own.ref[part, :] + self.from_o.ref[part, :].astype(F32)
            total = total + self.from_c.ref[i].astype(F32)
            resid = self.resid.ref[part, :].astype(F32)
            if self.back:
                value, (gain, row) = self.back
                value_grad, gain_grad = norm_back(
                    value.ref[part, :].astype(F32), gain.ref[row : row + 1, :], total
                )
                total = value_grad
                gain_sum = gain_grad if gain_sum is None else gain_sum + gain_grad
            self.out.ref[part, :] = (resid + total).astype(self.out.dtype)
        if self.back:
            self.gain_grad.ref[...] = gain_sum

    def end(self):
        self.move("near").wait_send()
        for i in range(2):
            self.move("diag", i).wait_send()
            self.move("cross", i).wait_send()


def delayed(values, by):
    if by == 0:
        return values
    row = lax.broadcasted_iota(jnp.int32, values.shape, 0)
    return jnp.where(row < by, 0.0, pltpu.roll(values, by, 0))


def advanced(values, by):
    if by == 0:
        return values
    length = values.shape[0]
    row = lax.broadcasted_iota(jnp.int32, values.shape, 0)
    return jnp.where(row >= length - by, 0.0, pltpu.roll(values, length - by, 0))


CONV_COLS = 128


class Conv:
    def __init__(self, k, projected, value, kernel):
        self.projected, self.value, self.kernel = projected, value, kernel
        self.y = k.vmem(value.shape, BF)

    def parts(self, j):
        channels = self.value.shape[1]
        at = slice(j * CONV_COLS, (j + 1) * CONV_COLS)
        b_gate = self.projected.ref[:, at]
        c_gate = self.projected.ref[:, channels + at.start : channels + at.stop]
        x_value, taps = self.value.ref[:, at], self.kernel.ref[:, at]
        product = b_gate * x_value
        count = taps.shape[0]
        causal = jnp.zeros_like(product)
        for i in range(count):
            causal = causal + taps[i : i + 1] * delayed(product, count - 1 - i)
        return at, b_gate, c_gate, x_value, taps, product, causal

    def run(self):
        for j in range(self.value.shape[1] // CONV_COLS):
            at, _, c_gate, _, _, _, causal = self.parts(j)
            self.y.ref[:, at] = (c_gate * causal).astype(BF)


class ConvBack(Conv):
    def __init__(self, k, projected, value, kernel, d_y):
        self.projected, self.value, self.kernel, self.d_y = projected, value, kernel, d_y
        self.d_proj = k.vmem(projected.shape, BF)
        self.d_value = k.vmem(value.shape, BF)
        self.d_kernel = k.vmem(kernel.shape, F32)

    def run(self):
        channels = self.value.shape[1]
        for j in range(channels // CONV_COLS):
            at, b_gate, c_gate, x_value, taps, product, causal = self.parts(j)
            d_y = self.d_y.ref[:, at]
            d_causal = d_y * c_gate
            count = taps.shape[0]
            d_product = jnp.zeros_like(product)
            for i in range(count):
                by = count - 1 - i
                row = jnp.sum(d_causal * delayed(product, by), axis=0, keepdims=True)
                self.d_kernel.ref[i : i + 1, at] = row
                d_product = d_product + taps[i : i + 1] * advanced(d_causal, by)
            self.d_proj.ref[:, at] = (d_product * x_value).astype(BF)
            self.d_proj.ref[:, channels + at.start : channels + at.stop] = (d_y * causal).astype(BF)
            self.d_value.ref[:, at] = (d_product * b_gate).astype(BF)


def head_mean(values, head_size):
    width = values.shape[1]
    row = lax.broadcasted_iota(jnp.int32, (width, width), 0) // head_size
    col = lax.broadcasted_iota(jnp.int32, (width, width), 1) // head_size
    group = jnp.where(row == col, 1.0 / head_size, 0.0).astype(F32)
    return lax.dot_general(
        values, group, (((1,), (0,)), ((), ())),
        precision=lax.Precision.HIGHEST, preferred_element_type=F32,
    )


def turn(values, head_size, back):
    width, half = values.shape[1], head_size // 2
    lane = lax.broadcasted_iota(jnp.int32, values.shape, 1) % head_size
    upper = pltpu.roll(values, width - half, 1)
    lower = pltpu.roll(values, half, 1)
    return jnp.where(lane < half, upper, -lower) if back else jnp.where(lane < half, -upper, lower)


def head_norm(values, gain, head_size):
    return values * lax.rsqrt(head_mean(values * values, head_size) + EPS) * gain


def head_norm_back(values, gain, grad_in, head_size):
    row_scale = lax.rsqrt(head_mean(values * values, head_size) + EPS)
    normed = values * row_scale
    gain_grad = jnp.sum(grad_in * normed, axis=0, keepdims=True)
    scaled = grad_in * gain
    return row_scale * (scaled - normed * head_mean(scaled * normed, head_size)), gain_grad


def block_weights(q_rows, keys):
    scores = [contract(q_rows, k_rows, 1, 1) for k_rows in keys]
    query = lax.broadcasted_iota(jnp.int32, scores[-1].shape, 0)
    key = lax.broadcasted_iota(jnp.int32, scores[-1].shape, 1)
    scores[-1] = jnp.where(key <= query, scores[-1], MASKED)
    top = functools.reduce(
        jnp.maximum, [jnp.max(part, axis=1, keepdims=True) for part in scores]
    )
    exps = [jnp.exp(part - top) for part in scores]
    scale = 1.0 / sum(jnp.sum(part, axis=1, keepdims=True) for part in exps)
    return [part * scale for part in exps]


def key_blocks(i):
    blocks = [pl.ds(0, i * ROW_BLOCK)] if i else []
    return blocks + [pl.ds(i * ROW_BLOCK, ROW_BLOCK)]


class Heads:
    def __init__(self, projected, tables, size):
        assert size in (16, 64, 256), size
        self.projected, self.size = projected, size
        self.gain, self.cos, self.sin = (v.buf for v in tables)
        self.loads = tables
        self.length, width = projected.shape
        self.q_cols, self.k_cols = width // 2, width // 4
        self.heads, self.kv_heads = self.q_cols // size, self.k_cols // size
        self.share = self.heads // self.kv_heads

    def per_head(self, k, count, kind):
        return k.vmem((count, self.length, self.size), kind)

    def split(self, val, rows, values):
        for h in range(val.shape[0]):
            val.ref[h, rows, :] = values[:, h * self.size : (h + 1) * self.size]

    def join(self, val, rows):
        return jnp.concatenate([val.ref[h, rows, :] for h in range(val.shape[0])], axis=1)

    def angles(self, rows):
        c, n = self.cos.ref[rows, :], self.sin.ref[rows, :]
        repeat = self.q_cols // c.shape[1]
        return jnp.concatenate([c] * repeat, axis=1), jnp.concatenate([n] * repeat, axis=1)

    def blocks(self, step):
        lax.fori_loop(0, self.length // ROW_BLOCK, lambda p, c: step(block_of(p, ROW_BLOCK)) or c, 0)


class Attend(Heads):
    def __init__(self, k, projected, tables, size):
        super().__init__(projected, tables, size)
        self.q_rot = k.vmem((self.length, self.q_cols), BF)
        self.k_rot = k.vmem((self.length, self.k_cols), BF)
        self.y = k.vmem((self.length, self.q_cols), BF)
        self.q_h, self.y_h = (self.per_head(k, self.heads, BF) for _ in range(2))
        self.k_h, self.v_h = (self.per_head(k, self.kv_heads, BF) for _ in range(2))

    def run(self, *between):
        for load in self.loads:
            load.wait()
        size, q_cols, k_cols, proj = self.size, self.q_cols, self.k_cols, self.projected.ref

        def prepare(rows):
            c, n = self.angles(rows)
            q = head_norm(proj[rows, :q_cols], self.gain.ref[0:1, :], size)
            q = (q * c + turn(q, size, False) * n).astype(BF)
            k = head_norm(proj[rows, q_cols : q_cols + k_cols], self.gain.ref[1:2, :k_cols], size)
            k = (k * c[:, :k_cols] + turn(k, size, False) * n[:, :k_cols]).astype(BF)
            self.q_rot.ref[rows, :] = q
            self.k_rot.ref[rows, :] = k
            self.split(self.q_h, rows, (q.astype(F32) * size**-0.5).astype(BF))
            self.split(self.k_h, rows, k)
            self.split(self.v_h, rows, proj[rows, q_cols + k_cols :].astype(BF))

        self.blocks(prepare)

        def head(h, carry):
            g = h // self.share
            for i in range(self.length // ROW_BLOCK):
                rows, seen = pl.ds(i * ROW_BLOCK, ROW_BLOCK), key_blocks(i)
                weights = block_weights(
                    self.q_h.ref[h, rows, :], [self.k_h.ref[g, at, :] for at in seen]
                )
                value = sum(
                    contract(part.astype(BF), self.v_h.ref[g, at, :], 1, 0)
                    for part, at in zip(weights, seen)
                )
                self.y_h.ref[h, rows, :] = value.astype(BF)
            return carry

        lax.fori_loop(0, self.heads // 2, head, 0)
        for step in between:
            step()
        lax.fori_loop(self.heads // 2, self.heads, head, 0)
        self.y.ref[...] = self.join(self.y_h, slice(None))


class AttendBack(Heads):
    def __init__(self, k, projected, tables, size, q_rot, k_rot, d_y):
        super().__init__(projected, tables, size)
        self.q_rot, self.k_rot, self.d_y = q_rot, k_rot, d_y
        self.q_h, self.dy_h = (self.per_head(k, self.heads, BF) for _ in range(2))
        self.k_h, self.v_h = (self.per_head(k, self.kv_heads, BF) for _ in range(2))
        self.dq_h = self.per_head(k, self.heads, F32)
        self.dk_h, self.dv_h = (self.per_head(k, self.kv_heads, F32) for _ in range(2))
        self.d_proj = k.vmem(projected.shape, BF)
        self.q_gain, self.k_gain = k.vmem((1, self.q_cols), F32), k.vmem((1, self.k_cols), F32)

    def run(self, *between):
        for load in self.loads:
            load.wait()
        size, q_cols, k_cols, proj = self.size, self.q_cols, self.k_cols, self.projected.ref
        scale = size**-0.5
        dq_h, dk_h, dv_h = self.dq_h.ref, self.dk_h.ref, self.dv_h.ref

        def prepare(rows):
            self.split(self.q_h, rows, (self.q_rot.ref[rows, :].astype(F32) * scale).astype(BF))
            self.split(self.dy_h, rows, self.d_y.ref[rows, :].astype(BF))
            self.split(self.k_h, rows, self.k_rot.ref[rows, :])
            self.split(self.v_h, rows, proj[rows, q_cols + k_cols :].astype(BF))

        self.blocks(prepare)
        dk_h[...] = jnp.zeros_like(dk_h)
        dv_h[...] = jnp.zeros_like(dv_h)

        def head(h, carry):
            g = h // self.share
            for i in range(self.length // ROW_BLOCK):
                rows, seen = pl.ds(i * ROW_BLOCK, ROW_BLOCK), key_blocks(i)
                q, low = self.q_h.ref[h, rows, :], self.dy_h.ref[h, rows, :]
                keys = [self.k_h.ref[g, at, :] for at in seen]
                probs = block_weights(q, keys)
                d_weights = [contract(low, self.v_h.ref[g, at, :], 1, 1) for at in seen]
                inner = sum(
                    jnp.sum(a * b, axis=1, keepdims=True) for a, b in zip(probs, d_weights)
                )
                d_q = 0.0
                for at, k, prob, d_weight in zip(seen, keys, probs, d_weights):
                    dv_h[g, at, :] += contract(prob.astype(BF), low, 0, 0)
                    d_scores = (prob * (d_weight - inner)).astype(BF)
                    d_q = d_q + contract(d_scores, k, 1, 0)
                    dk_h[g, at, :] += contract(d_scores, q, 0, 0)
                dq_h[h, rows, :] = d_q * scale
            return carry

        lax.fori_loop(0, self.heads // 2, head, 0)
        for step in between:
            step()
        lax.fori_loop(self.heads // 2, self.heads, head, 0)
        self.q_gain.ref[...] = jnp.zeros_like(self.q_gain.ref)
        self.k_gain.ref[...] = jnp.zeros_like(self.k_gain.ref)

        def finish(rows):
            c, n = self.angles(rows)
            dq, dk, dv = (self.join(v, rows) for v in (self.dq_h, self.dk_h, self.dv_h))
            dq = dq * c + turn(dq * n, size, True)
            dk = dk * c[:, :k_cols] + turn(dk * n[:, :k_cols], size, True)
            dq, q_sum = head_norm_back(proj[rows, :q_cols], self.gain.ref[0:1, :], dq, size)
            dk, k_sum = head_norm_back(
                proj[rows, q_cols : q_cols + k_cols], self.gain.ref[1:2, :k_cols], dk, size
            )
            self.q_gain.ref[...] += q_sum
            self.k_gain.ref[...] += k_sum
            self.d_proj.ref[rows, :q_cols] = dq.astype(BF)
            self.d_proj.ref[rows, q_cols : q_cols + k_cols] = dk.astype(BF)
            self.d_proj.ref[rows, q_cols + k_cols :] = dv.astype(BF)

        self.blocks(finish)


def body(boundary, norm_gain, mix_in, mix_out, w_gate, w_up, w_down, conv_x, conv_kernel, qk_gain):
    first = lax.axis_index("section") == 0
    tensor_index = lax.axis_index("tensor")
    model_width = boundary.shape[3]
    channels = mix_out.shape[1]
    row_shape = boundary.shape[2:]
    length, size = 4 * row_shape[0], qk_gain.shape[1]

    seqs, own_gain = boundary[0], norm_gain[0]
    sh_in, sh_out, sh_gate, sh_up, sh_down = (v[0] for v in (mix_in, mix_out, w_gate, w_up, w_down))
    head_gain = jnp.tile(qk_gain, (1, channels // size))

    def gains_of(k, block, other, early=True):
        own, moved = k.input(own_gain), as_val(k, other)
        sources = lambda s, d, t: [(s == block, own.ref), (s == 1 - block, moved.ref)]
        return Load(k, sources, own.shape, F32, early)

    def start_rows(k, slot, other, early=True):
        own, moved = k.input(seqs), as_val(k, other)
        sources = lambda s, d, t: [(s == slot, own.ref.at[slot]), (s == 1 - slot, moved.ref)]
        return Load(k, sources, row_shape, BF, early)

    def wait(*items):
        return [item.wait for item in items]

    k = Kernel(0)
    t_seq = None
    seq_val = k.input(seqs)

    def seq_moves(s, d, t):
        return [([(None, seq_val.ref.at[1 - s])], t_seq.out.ref, {"section": 1 - s})], []

    t_in, t_out, t_up = (x_half(k, v) for v in (sh_in, sh_out, sh_up))
    t_gate0, t_down0 = x_move(k, sh_gate, 0), x_half(k, sh_down, 0)
    t_gate1, t_down1 = x_half(k, sh_gate, 1), x_move(k, sh_down, 1)
    t_seq = Task(k, row_shape, "section", seq_moves, 1)
    t_gain, z_cols = x_move(k, own_gain), z_gather(k, conv_x)
    z_in0, z_out0 = z_gather_half(k, sh_in, t_in.out, 0), z_gather_half(k, sh_out, t_out.out, 0)
    z_gate0 = z_gather_whole(k, sh_gate, t_gate0.out, 0)
    z_up0 = z_gather_half(k, sh_up, t_up.out, 0)
    x_cols, x_in0, x_out0 = (x_move(k, v.out) for v in (z_cols, z_in0, z_out0))
    x_load, gain_load = start_rows(k, 0, t_seq.out, False), gains_of(k, 0, t_gain.out, False)
    taps = load_all(k, conv_kernel)
    angles = Angles(k, length, size, 128)
    w_in0, w_cols = Weight(k, "rows", z_in0.out, x_in0.out), Weight(k, "conv", z_cols.out, x_cols.out)
    w_out0 = Weight(k, "cols", z_out0.out, x_out0.out)
    g0 = Gather(k, x_load.buf, (gain_load.buf, 0), [w_in0, w_cols], save=(0, 1, 2))
    conv = Conv(k, g0.values[0], g0.values[1], taps.buf)
    y0 = Save(k, conv.y)
    s1 = Scatter(k, [conv.y], [w_out0], x_load.buf)
    mid0 = Save(k, s1.out)
    k.do(t_in.send, t_out.send, z_cols.send, t_gate0.send, t_gate1.send, t_gain.send, t_seq.send)
    k.do(t_in.wait, z_in0.send, t_out.wait, z_out0.send, z_cols.step, z_in0.step, z_out0.step)
    k.do(z_cols.step, z_in0.step, z_out0.step, t_gate0.wait, z_gate0.send)
    k.do(z_cols.wait, x_cols.send, z_in0.wait, x_in0.send, z_out0.wait, x_out0.send)
    k.do(t_up.send, t_down0.send, t_down1.send)
    k.do(t_gain.wait, gain_load.start, t_seq.wait, x_load.start, gain_load.wait, x_load.wait)
    k.do(g0.begin, angles.run, z_gate0.step)
    k.do(x_cols.wait, w_cols.start, x_in0.wait, w_in0.start, z_gate0.step)
    k.do(g0.loop, t_up.wait, z_up0.send, taps.wait, conv.run, y0.start)
    k.do(x_out0.wait, w_out0.start, s1.loop, z_up0.step, s1.finish, mid0.start, z_up0.step)
    k.do(*wait(t_gate1, t_down0, t_down1, z_gate0, z_up0))
    k.build()
    a0, proj0, value0 = (out for _, out, _ in g0.saved)
    table_arrays = [head_gain] + [v.out for v in angles.saves]
    y0, mid0 = y0.out, mid0.out

    k = Kernel(1)
    x_up0, z_down0 = x_move(k, z_up0.out), z_gather_half(k, sh_down, t_down0.out, 0)
    z_in1, z_out1 = z_gather_half(k, sh_in, t_in.out, 1), z_gather_half(k, sh_out, t_out.out, 1)
    z_gate1 = z_gather_half(k, sh_gate, t_gate1.out, 1)
    z_down1a = z_gather_whole(k, sh_down, t_down1.out, 1, 0)
    x_down0, x_in1, x_out1 = (x_move(k, v.out) for v in (z_down0, z_in1, z_out1))
    rows, gain_load = load_all(k, mid0), gains_of(k, 0, t_gain.out)
    w_gate0 = Weight(k, "rows", z_gate0.out, None, True)
    w_up0 = Weight(k, "rows", z_up0.out, x_up0.out)
    w_down0 = Weight(k, "cols", z_down0.out, x_down0.out)
    g2 = Gather(
        k, rows.buf, (gain_load.buf, 1), [w_gate0, w_up0], epilogue="ffn", save=(0, 1, 2, 3)
    )
    s3 = Scatter(k, [g2.values[2]], [w_down0], rows.buf, low=True)
    z_rows = Save(k, s3.out)
    k.do(x_up0.send, z_down0.send, rows.wait, gain_load.wait, g2.begin, z_down0.step)
    k.do(z_in1.send, z_out1.send, z_down0.step, z_in1.step, z_out1.step, z_gate1.send)
    k.do(z_down0.wait, x_down0.send, z_down1a.send, x_up0.wait, w_up0.start, z_in1.step, z_out1.step)
    k.do(g2.loop, z_gate1.step, z_down1a.step, z_in1.wait, x_in1.send, z_out1.wait, x_out1.send)
    k.do(x_down0.wait, w_down0.start, s3.loop, z_gate1.step, z_down1a.step)
    k.do(s3.finish, z_rows.start, *wait(x_in1, x_out1, z_gate1, z_down1a))
    k.build()
    m0, gate0, up0, hid0 = (out for _, out, _ in g2.saved)
    z_rows = z_rows.out

    k = Kernel(2)
    x_gate1, z_up1 = x_move(k, z_gate1.out), z_gather_half(k, sh_up, t_up.out, 1)
    z_down1, x_up1 = z_gather_whole(k, sh_down, t_down1.out, 1, 1), x_move(k, z_up1.out)
    rows, gain_load = load_all(k, z_rows), gains_of(k, 1, t_gain.out)
    tables = [load_all(k, v) for v in table_arrays]
    w_in1 = Weight(k, "rows", z_in1.out, x_in1.out, True)
    w_out1 = Weight(k, "cols", z_out1.out, x_out1.out, True)
    g4 = Gather(k, rows.buf, (gain_load.buf, 0), [w_in1], save=(0, 1))
    attend = Attend(k, g4.values[0], tables, size)
    kept = [Save(k, v) for v in (attend.q_rot, attend.k_rot, attend.y)]
    s5 = Scatter(k, [attend.y], [w_out1], rows.buf)
    mid1 = Save(k, s5.out)
    k.do(x_gate1.send, z_up1.send, z_down1.send)
    k.do(rows.wait, gain_load.wait, g4.begin, z_up1.step, g4.loop, z_up1.step)
    k.do(lambda: attend.run(z_up1.wait, x_up1.send, z_down1.step))
    k.do(*(v.start for v in kept))
    k.do(s5.loop, z_down1.step, s5.finish, mid1.start)
    k.do(*wait(x_gate1, x_up1, z_down1))
    k.build()
    a1, proj1 = (out for _, out, _ in g4.saved)
    q_rot, k_rot, y1 = (v.out for v in kept)
    mid1 = mid1.out

    k = Kernel(3)
    rows, gain_load = load_all(k, mid1), gains_of(k, 1, t_gain.out)
    cot = start_rows(k, 1, t_seq.out)
    w_gate1 = Weight(k, "rows", z_gate1.out, x_gate1.out, True)
    w_up1 = Weight(k, "rows", z_up1.out, x_up1.out, True)
    w_down1 = Weight(k, "cols", z_down1a.out, z_down1.out, True, True)
    g6 = Gather(k, rows.buf, (gain_load.buf, 1), [w_gate1, w_up1], epilogue="ffn")
    g8 = Gather(
        k, cot.buf, None, [w_down1], [g6.values[0], g6.values[1]], trans=True, epilogue="ffn_back"
    )
    p_down1 = Product(k, g6.values[2], g8.full)
    p_gate1, p_up1 = Product(k, g6.full, g8.values[0]), Product(k, g6.full, g8.values[1])
    r_down1 = x_half(k, p_down1.out)
    s7 = Scatter(k, [g6.values[2]], [w_down1], rows.buf, low=True)
    s9 = Scatter(k, g8.values, [w_gate1, w_up1], cot.buf, (rows.buf, (gain_load.buf, 1)), True)
    y_rows, d_mid1, gain11 = Save(k, s7.out), Save(k, s9.out), Save(k, s9.gain_grad)
    k.do(rows.wait, gain_load.wait, g6.begin, cot.wait, g8.begin, g6.loop)
    k.do(g8.loop, p_down1.run, p_down1.wait, r_down1.send)
    k.do(s9.loop, s7.loop, p_gate1.run, p_up1.run, s9.finish, d_mid1.start, gain11.start)
    k.do(s7.finish, y_rows.start, p_gate1.wait, p_up1.wait)
    k.do(*wait(r_down1))
    k.build()
    y_rows, d_mid1, gain11 = y_rows.out, d_mid1.out, gain11.out

    k = Kernel(4)
    q_down1 = sum_scatter(k, "cols", p_down1.out, r_down1.out)
    r_gate1, q_up1 = x_slots(k, p_gate1.out, "rows"), sum_scatter(k, "rows", p_up1.out)
    rows, gain_load = load_all(k, d_mid1), gains_of(k, 1, t_gain.out)
    value = load_all(k, z_rows)
    tables = [load_all(k, v) for v in table_arrays]
    proj, q_load, k_load, y_load, a_load = (load_all(k, v) for v in (proj1, q_rot, k_rot, y1, a1))
    w_in1 = Weight(k, "rows", z_in1.out, x_in1.out, True)
    w_out1 = Weight(k, "cols", z_out1.out, x_out1.out, True)
    g10 = Gather(k, rows.buf, None, [w_out1], trans=True)
    p_out1 = Product(k, y_load.buf, g10.full)
    back = AttendBack(k, proj.buf, tables, size, q_load.buf, k_load.buf, g10.values[0])
    p_in1 = Product(k, a_load.buf, back.d_proj)
    r_out1 = x_half(k, p_out1.out)
    s11 = Scatter(
        k, [back.d_proj], [w_in1], rows.buf, (value.buf, (gain_load.buf, 0)), True, low=True
    )
    d_z, gain10 = Save(k, s11.out), Save(k, s11.gain_grad)
    head_gains = [Save(k, back.q_gain), Save(k, back.k_gain)]
    k.early += [q_down1.load, q_up1.load]
    k.do(r_gate1.send, rows.wait, g10.begin, q_down1.send, q_up1.send, g10.loop)
    k.do(q_down1.step, y_load.wait, p_out1.run, p_out1.wait, r_out1.send)
    k.do(proj.wait, q_load.wait, k_load.wait, lambda: back.run(q_up1.step, q_down1.step))
    k.do(q_up1.step, *(v.start for v in head_gains))
    k.do(gain_load.wait, value.wait, s11.loop, a_load.wait, p_in1.run)
    k.do(s11.finish, d_z.start, gain10.start, p_in1.wait)
    k.do(*wait(q_down1, q_up1, r_gate1, r_out1))
    k.build()
    d_z, gain10 = d_z.out, gain10.out
    q_gain, k_gain = (v.out for v in head_gains)

    k = Kernel(5)
    q_gate1, m_up1 = sum_scatter(k, "rows", p_gate1.out, r_gate1.out), x_move(k, q_up1.out, 0)
    q_out1 = sum_scatter(k, "cols", p_out1.out, r_out1.out)
    r_in1 = x_slots(k, p_in1.out, "rows")
    q_in1 = sum_scatter(k, "rows", p_in1.out, r_in1.out)
    e_down1 = Finish(k, q_down1.out, 1)
    rows, value, gain_load = load_all(k, d_z), load_all(k, mid0), gains_of(k, 0, t_gain.out)
    gate_load, up_load, hid_load, m_load = (load_all(k, v) for v in (gate0, up0, hid0, m0))
    w_gate0 = Weight(k, "rows", z_gate0.out, None, True)
    w_up0 = Weight(k, "rows", z_up0.out, x_up0.out, True)
    w_down0 = Weight(k, "cols", z_down0.out, x_down0.out, True)
    g12 = Gather(
        k, rows.buf, None, [w_down0], [gate_load.buf, up_load.buf], trans=True, epilogue="ffn_back"
    )
    p_down0 = Product(k, hid_load.buf, g12.full)
    p_gate0, p_up0 = Product(k, m_load.buf, g12.values[0]), Product(k, m_load.buf, g12.values[1])
    r_down0 = x_half(k, p_down0.out)
    s13 = Scatter(
        k, g12.values, [w_gate0, w_up0], rows.buf, (value.buf, (gain_load.buf, 1)), True
    )
    d_mid0, gain01 = Save(k, s13.out), Save(k, s13.gain_grad)
    k.early += [q_gate1.load, q_out1.load, e_down1.load]
    k.do(r_in1.send, rows.wait, g12.begin, q_gate1.send, q_out1.send, m_up1.send, e_down1.send)
    k.do(gate_load.wait, up_load.wait, g12.loop, q_gate1.step, q_out1.step)
    k.do(hid_load.wait, p_down0.run, p_down0.wait, r_down0.send, r_in1.wait, q_in1.add)
    k.do(s13.loop, q_gate1.step, q_out1.step, q_in1.step)
    k.do(m_load.wait, p_gate0.run, p_up0.run, q_in1.step, value.wait, gain_load.wait)
    k.do(s13.finish, d_mid0.start, gain01.start, p_gate0.wait, p_up0.wait)
    k.do(*wait(q_gate1, q_out1, q_in1, e_down1, m_up1, r_down0))
    k.build()
    d_mid0, gain01 = d_mid0.out, gain01.out

    k = Kernel(6)
    r_gate0 = x_slots(k, p_gate0.out, "rows")
    q_gate0 = sum_scatter(k, "rows", p_gate0.out, r_gate0.out)
    q_down0 = sum_scatter(k, "cols", p_down0.out, r_down0.out)
    q_up0 = sum_scatter(k, "rows", p_up0.out)
    m_up0 = x_move(k, q_up0.out, 1)
    e_gate1, e_out1, e_in1 = (Finish(k, v.out, 1) for v in (q_gate1, q_out1, q_in1))
    rows, gain_load = load_all(k, d_mid0), gains_of(k, 0, t_gain.out)
    x_load, taps = start_rows(k, 0, t_seq.out), load_all(k, conv_kernel)
    y_load, a_load, proj, value = (load_all(k, v) for v in (y0, a0, proj0, value0))
    w_in0 = Weight(k, "rows", z_in0.out, x_in0.out, True)
    w_cols = Weight(k, "conv", z_cols.out, x_cols.out, True)
    w_out0 = Weight(k, "cols", z_out0.out, x_out0.out, True)
    g14 = Gather(k, rows.buf, None, [w_out0], trans=True)
    p_out0 = Product(k, y_load.buf, g14.full)
    back = ConvBack(k, proj.buf, value.buf, taps.buf, g14.values[0])
    p_in0, p_cols = Product(k, a_load.buf, back.d_proj), Product(k, a_load.buf, back.d_value)
    r_out0, r_in0 = x_half(k, p_out0.out), x_slots(k, p_in0.out, "rows")
    r_cols = x_slots(k, p_cols.out, "conv")
    q_out0, q_in0 = sum_scatter(k, "cols", p_out0.out, r_out0.out), sum_scatter(k, "rows", p_in0.out, r_in0.out)
    q_cols = sum_scatter(k, "conv", p_cols.out, r_cols.out)
    e_down0, e_gate0, e_out0, e_in0 = (
        Finish(k, v.out, 0) for v in (q_down0, q_gate0, q_out0, q_in0)
    )
    s15 = Scatter(
        k, [back.d_proj, back.d_value], [w_in0, w_cols], rows.buf,
        (x_load.buf, (gain_load.buf, 0)), True, low=True,
    )
    d_x = Save(k, s15.out)
    tap_rows = conv_kernel.shape[0]
    small = k.vmem((8, model_width), F32)
    small_out = Save(k, small)
    ready = [load_all(k, v) for v in (gain01, gain10, gain11)]
    head_loads = [load_all(k, v) for v in (q_gain, k_gain)]

    def fill_small():
        t = lax.axis_index("tensor")
        small.ref[...] = jnp.zeros_like(small.ref)
        small.ref[0:1, :] = s15.gain_grad.ref[...]
        for i, load in enumerate(ready):
            load.wait()
            small.ref[i + 1 : i + 2, :] = load.buf.ref[...]
        small.ref[4 : 4 + tap_rows, block_of(t, channels)] = back.d_kernel.ref[...]
        at = 0
        for load in head_loads:
            load.wait()
            width = load.buf.shape[1]
            small.ref[7:8, at : at + width] = load.buf.ref[...]
            at += width
        small_out.start()

    t_small = x_move(k, small_out.out)
    z_small = SumShare(k, [small_out.out, t_small.out], "dp")
    t_total = SumShare(k, [z_small.out], "tensor", slotted=True)
    y_val, dx_val = k.input(y_rows), d_x.out

    def result_moves(s, d, t):
        sources = [(s == 0, y_val.ref), (s == 1, dx_val.ref)]
        return [(sources, t_result.out.ref, {"section": 1 - s})], []

    t_result = Task(k, row_shape, "section", result_moves, 1)
    k.early += [q_up0.load, q_down0.load, e_gate1.load, e_out1.load, e_in1.load]
    k.do(r_gate0.send, rows.wait, g14.begin, q_up0.send, q_down0.send)
    k.do(e_gate1.send, e_out1.send, e_in1.send, g14.loop)
    k.do(y_load.wait, p_out0.run, p_out0.wait, r_out0.send, q_up0.step)
    k.do(proj.wait, value.wait, taps.wait, back.run, q_down0.step, a_load.wait)
    k.do(p_in0.run, p_cols.run, p_in0.wait, r_in0.send, p_cols.wait, r_cols.send)
    k.do(r_gate0.wait, q_gate0.add, x_load.wait, gain_load.wait, s15.loop, q_up0.step)
    k.do(q_down0.step, s15.finish, d_x.start, fill_small, d_x.wait, t_result.send)
    k.do(small_out.wait, t_small.send, q_gate0.step, r_out0.wait, q_out0.add, r_in0.wait, q_in0.add)
    k.do(r_cols.wait, q_cols.add, q_up0.wait, m_up0.send, q_down0.wait, e_down0.add)
    k.do(q_gate0.step, q_out0.step, q_in0.step, q_cols.step, t_small.wait, z_small.add)
    k.do(q_gate0.wait, e_gate0.add, q_out0.step, q_in0.step, q_cols.step)
    k.do(z_small.wait, t_total.add, q_out0.wait, e_out0.add, q_in0.wait, e_in0.add)
    rest = (e_gate1, e_out1, e_in1, q_cols, e_down0, e_gate0, m_up0, e_out0, e_in0)
    k.do(*wait(*rest, t_total, t_result))
    k.build()

    owned = [
        ([e_in0], [e_in1], 1),
        ([e_out0], [e_out1], 1),
        ([e_gate0], [e_gate1], 1),
        ([q_up0, m_up0], [q_up1, m_up1], 1),
        ([e_down0], [e_down1], 1),
        ([q_cols], [q_cols], 0),
    ]
    return pack(
        [(zero, one, lead) for zero, one, lead in owned], t_total, d_x.out, y_rows, t_result,
        (norm_gain.shape, conv_kernel.shape, qk_gain.shape),
    )


def slot_free(val, shape):
    value = val.out.array
    if value.ndim == 3 and value.shape[0] * value.shape[1] != shape[0]:
        value = jnp.sum(value.astype(F32), axis=0).astype(BF)
    return value.reshape(shape)


def pack_kernel(plan, *refs):
    n_in, leads, terms, tap_rows = plan
    ins, rest = refs[:n_in], refs[n_in:]
    result, gain_out, *grads, cols, taps, heads = rest[: len(leads) + 4]
    grads = [*grads, cols]
    room = iter(rest[len(leads) + 4 :])
    own_v, moved_v, small_v, *bufs = (next(room) for _ in range(3 + len(terms)))
    out_v = [next(room) for _ in leads]
    load_sem, store_sem = room
    s, t = lax.axis_index("section"), lax.axis_index("tensor")
    small, d_x, y_rows, moved, *parts = ins

    def either(cond, zero, one, dst, sem):
        if zero is not None:
            pl.when(cond)(pltpu.make_async_copy(zero, dst, sem).start)
        if one is not None:
            pl.when(jnp.logical_not(cond))(pltpu.make_async_copy(one, dst, sem).start)

    first = s == 0
    either(first, d_x, y_rows, own_v, load_sem.at[0])
    pltpu.make_async_copy(moved, moved_v, load_sem.at[1]).start()
    pltpu.make_async_copy(small, small_v, load_sem.at[2]).start()
    for j, (zero, one, _) in enumerate(terms):
        either(
            first,
            None if zero is None else parts[zero],
            None if one is None else parts[one],
            bufs[j],
            load_sem.at[3 + j],
        )
    for j, (zero, one, i) in enumerate(terms):
        arrive = pltpu.make_async_copy(parts[one if zero is None else zero], bufs[j], load_sem.at[3 + j])
        begins = j == 0 or terms[j - 1][2] != i

        def put(j=j, i=i, begins=begins):
            value = bufs[j][...].astype(F32)
            value = value if begins else out_v[i][...] + value
            out_v[i][...] = value

        if zero is None or one is None:
            cond = first if one is None else jnp.logical_not(first)

            @pl.when(cond)
            def _(arrive=arrive, put=put):
                arrive.wait()
                put()
        else:
            arrive.wait()
            put()
        if j + 1 == len(terms) or terms[j + 1][2] != i:
            dst = grads[i].at[0] if leads[i] else grads[i]
            pltpu.make_async_copy(out_v[i], dst, store_sem.at[i]).start()
    pltpu.make_async_copy(d_x, own_v, load_sem.at[0]).wait()
    pltpu.make_async_copy(moved, moved_v, load_sem.at[1]).wait()
    n = len(leads)
    stores = [
        pltpu.make_async_copy(own_v, result.at[0, s], store_sem.at[n]),
        pltpu.make_async_copy(moved_v, result.at[0, 1 - s], store_sem.at[n + 1]),
    ]
    for store in stores:
        store.start()
    pltpu.make_async_copy(small, small_v, load_sem.at[2]).wait()
    total = small_v[0]
    for i in range(1, small_v.shape[0]):
        total = total + small_v[i]
    gain_out[0] = jnp.where(first, total[0:2], total[2:4])
    channels, size = taps.shape[1], heads.shape[1]
    chosen = total[4 : 4 + tap_rows, 0:channels]
    for i in range(1, total.shape[1] // channels):
        chosen = jnp.where(t == i, total[4 : 4 + tap_rows, i * channels : (i + 1) * channels], chosen)
    taps[...] = chosen
    at = 0
    for row, width in enumerate((channels, channels // 2)):
        value = total[7:8, at : at + size]
        for i in range(1, width // size):
            value = value + total[7:8, at + i * size : at + (i + 1) * size]
        heads[row : row + 1, :] = value
        at += width
    for i, store in enumerate(leads):
        dst = grads[i].at[0] if store else grads[i]
        pltpu.make_async_copy(out_v[i], dst, store_sem.at[i]).wait()
    for store in stores:
        store.wait()


def pack(owned, small, d_x, y_rows, moved, shapes):
    gain_shape, tap_shape, head_shape = shapes
    parts, terms, leads, out_shapes = [], [], [], []
    for i, (zero, one, lead) in enumerate(owned):
        whole = zero[0].out.shape
        if lead and len(whole) == 3 and isinstance(zero[0], Finish):
            shape = (whole[0] * whole[1], whole[2])
        else:
            shape = whole[-2:]
        shape = tuple(shape)
        leads.append(lead)
        out_shapes.append(shape)
        for j in range(max(len(zero), len(one))):
            pair = []
            for side in (zero, one):
                if j < len(side):
                    parts.append(slot_free(side[j], shape))
                    pair.append(len(parts) - 1)
                else:
                    pair.append(None)
            terms.append((*pair, i))
    operands = [small.out.array, d_x.array, y_rows.array, moved.out.array, *parts]
    rows = d_x.shape
    smem = pl.BlockSpec(memory_space=pltpu.VMEM)
    out_shape = [jax.ShapeDtypeStruct((1, 2) + rows, BF), jax.ShapeDtypeStruct(gain_shape, F32)]
    out_shape += [
        jax.ShapeDtypeStruct((1,) + v if lead else v, F32) for v, lead in zip(out_shapes, leads)
    ]
    out_shape += [jax.ShapeDtypeStruct(v, F32) for v in (tap_shape, head_shape)]
    n = len(leads)
    return tuple(
        pl.pallas_call(
            functools.partial(
                pack_kernel, (len(operands), tuple(leads), tuple(terms), tap_shape[0])
            ),
            out_shape=out_shape,
            in_specs=[ANY] * len(operands),
            out_specs=[ANY, smem] + [ANY] * n + [smem] * 2,
            scratch_shapes=[pltpu.VMEM(rows, BF)] * 2
            + [pltpu.VMEM(small.out.shape, F32)]
            + [pltpu.VMEM(out_shapes[i], BF) for _, _, i in terms]
            + [pltpu.VMEM(v, F32) for v in out_shapes]
            + [DMA((3 + len(terms),)), DMA((n + 2,))],
            compiler_params=pltpu.CompilerParams(vmem_limit_bytes=VMEM_BYTES),
            name="pack",
        )(*operands)
    )


def solution(mesh):
    in_specs = (
        P("section", "dp", "tensor", None),
        P("section", None, None),
        P("section", "dp", "tensor"),
        P("section", "tensor", "dp"),
        P("section", "dp", "tensor"),
        P("section", "dp", "tensor"),
        P("section", "tensor", "dp"),
        P(("section", "dp"), "tensor"),
        P(None, "tensor"),
        P(),
    )
    out_specs = (
        P("section", "dp", "tensor", None),
        P("section", None, None),
        P("section", "dp", "tensor"),
        P("section", "tensor", "dp"),
        P("section", "dp", "tensor"),
        P("section", "dp", "tensor"),
        P("section", "tensor", "dp"),
        P(("section", "dp"), "tensor"),
        P(None, "tensor"),
        P(),
    )
    return jax.shard_map(body, mesh=mesh, in_specs=in_specs, out_specs=out_specs, check_vma=False)
```

```python
import functools

import jax
import jax.numpy as jnp
from jax import lax
from jax.experimental import pallas as pl
from jax.experimental.pallas import tpu as pltpu
from jax.sharding import PartitionSpec as P

HEADS = 16
KV_HEADS = 8

EPS = 1e-05
ROPE_BASE = 1000000.0
MASKED = -1e30

MESH = pl.DeviceIdType.MESH
ANY = pl.BlockSpec(memory_space=pl.ANY)
DMA = pltpu.SemaphoreType.DMA
VMEM_BYTES = 63 * 1024 * 1024
BF = jnp.bfloat16
F32 = jnp.float32
ROW_BLOCK = 256


def contract(left_op, right_op, left_dim, right_dim):
    return lax.dot_general(
        left_op, right_op, (((left_dim,), (right_dim,)), ((), ())), preferred_element_type=F32
    )


def norm_rows(values, gain):
    return values * lax.rsqrt(jnp.mean(values * values, axis=-1, keepdims=True) + EPS) * gain


def norm_back(values, gain, grad_in):
    row_scale = lax.rsqrt(jnp.mean(values * values, axis=-1, keepdims=True) + EPS)
    normed = values * row_scale
    gain_grad = jnp.sum(grad_in * normed, axis=0, keepdims=True)
    scaled = grad_in * gain
    value_grad = row_scale * (scaled - normed * jnp.mean(scaled * normed, axis=-1, keepdims=True))
    return (value_grad, gain_grad)


class Angles:
    def __init__(self, k, length, head_size, width):
        self.half = head_size // 2
        self.tables = [k.vmem((length, width), F32) for _ in range(2)]
        self.saves = [Save(k, v) for v in self.tables]

    def run(self):
        cos, sin = self.tables
        shape = (ROW_BLOCK, cos.shape[1])
        column = (lax.broadcasted_iota(jnp.int32, shape, 1) % self.half).astype(F32)
        frequency = ROPE_BASE ** (-(column / self.half))
        row = lax.broadcasted_iota(jnp.int32, shape, 0)

        def step(i, carry):
            rows = block_of(i, ROW_BLOCK)
            angle = (row + i * ROW_BLOCK).astype(F32) * frequency
            cos.ref[rows, :] = jnp.cos(angle)
            sin.ref[rows, :] = jnp.sin(angle)
            return carry

        lax.fori_loop(0, cos.shape[0] // ROW_BLOCK, step, 0)
        for save in self.saves:
            save.start()


def silu_parts(gate):
    sig = 1.0 / (1.0 + jnp.exp(-gate))
    return sig, gate * sig


def dp_size():
    return lax.axis_size("dp")


def spot():
    return tuple(lax.axis_index(a) for a in ("section", "dp", "tensor"))


def block_of(index, size):
    return pl.ds(pl.multiple_of(index * size, size), size)


class Val:
    def __init__(self, shape, dtype):
        self.shape, self.dtype = tuple(shape), dtype
        self.ref = self.array = None


class Kernel:
    def __init__(self, cid):
        self.cid, self.ins, self.arrays, self.outs, self.room = cid, [], [], [], []
        self.early, self.steps, self.late, self.axes = [], [], [], set()
        self.once = []

    def input(self, array):
        array = array.array if isinstance(array, Val) else array
        for val, known in zip(self.ins, self.arrays):
            if known is array:
                return val
        val = Val(array.shape, array.dtype)
        self.ins.append(val)
        self.arrays.append(array)
        return val

    def output(self, shape, dtype):
        val = Val(shape, dtype)
        self.outs.append(val)
        return val

    def vmem(self, shape, dtype):
        val = Val(shape, dtype)
        self.room.append((val, pltpu.VMEM(tuple(shape), dtype)))
        return val

    def sem(self, *shape):
        val = Val(shape, None)
        self.room.append((val, DMA(shape)))
        return val

    def do(self, *steps):
        self.steps += steps

    def body(self, *refs):
        vals = self.ins + self.outs + [val for val, _ in self.room]
        for val, ref in zip(vals, refs):
            val.ref = ref
        for item in self.once:
            item.waited = False
            item.phase = 0
        for step in self.early:
            step()
        self.greet()
        for step in self.steps + self.late:
            step()

    def greet(self):
        s, d, t = spot()
        _, sib, cross, diag = places()
        barrier = pltpu.get_barrier_semaphore()
        peers = [{"tensor": sib}, {"tensor": cross}]
        if "tensor" in self.axes:
            peers.append({"tensor": diag})
        if "section" in self.axes:
            peers.append({"section": 1 - s})
        if "dp" in self.axes:
            peers += [{"dp": (d + i) % dp_size()} for i in range(1, dp_size())]

        def signal(peer):
            pl.semaphore_signal(barrier, inc=1, device_id=peer, device_id_type=MESH)

        for peer in peers:
            signal(peer)
        expected = len(peers)
        if "line" in self.axes and "dp" not in self.axes:
            pl.when(d < 3)(lambda: signal({"dp": (d + 1) % 4}))
            pl.when(d > 0)(lambda: signal({"dp": (d + 3) % 4}))
            expected = expected + (d + 2) // 3 + (5 - d) // 3
        pl.semaphore_wait(barrier, expected)

    def build(self):
        result = pl.pallas_call(
            self.body,
            out_shape=[jax.ShapeDtypeStruct(v.shape, v.dtype) for v in self.outs],
            in_specs=[ANY] * len(self.ins),
            out_specs=[ANY] * len(self.outs),
            scratch_shapes=[room for _, room in self.room],
            compiler_params=pltpu.CompilerParams(
                collective_id=self.cid, has_side_effects=True, vmem_limit_bytes=VMEM_BYTES
            ),
            name=f"stage{self.cid}",
        )(*self.arrays)
        for val, array in zip(self.outs, result):
            val.array = array


def remote(src, dst, send_sem, recv_sem, peer):
    return pltpu.make_async_remote_copy(
        src_ref=src, dst_ref=dst, send_sem=send_sem, recv_sem=recv_sem,
        device_id=peer, device_id_type=MESH,
    )


class Load:
    def __init__(self, k, sources, shape, dtype, early=False):
        self.k, self.sources, self.waited = k, sources, False
        self.buf, self.sem = k.vmem(shape, dtype), k.sem(1)
        k.once.append(self)
        if early:
            k.early.append(self.start)

    def moves(self):
        for cond, source in self.sources(*spot()):
            yield cond, pltpu.make_async_copy(source, self.buf.ref, self.sem.ref.at[0])

    def start(self):
        for cond, move in self.moves():
            if cond is None:
                move.start()
            else:
                pl.when(cond)(move.start)

    def wait(self):
        if not self.waited:
            self.waited = True
            next(self.moves())[1].wait()


def load_all(k, array, early=True):
    val = k.input(array)
    return Load(k, lambda s, d, t: [(None, val.ref)], val.shape, val.dtype, early)


class Save:
    def __init__(self, k, buf):
        self.buf, self.out, self.sem = buf, k.output(buf.shape, buf.dtype), k.sem(1)
        self.waited = False
        k.once.append(self)
        k.late.append(self.wait)

    def move(self):
        return pltpu.make_async_copy(self.buf.ref, self.out.ref, self.sem.ref.at[0])

    def start(self):
        self.move().start()

    def wait(self):
        if not self.waited:
            self.waited = True
            self.move().wait()


class Task:
    final = None

    def __init__(self, k, out, axis, moves, count, n_local=1, out_dtype=BF):
        self.k, self.axis, self.make = k, axis, moves
        self.out = k.output(out, out_dtype)
        self.send_sem, self.recv_sem, self.local_sem = k.sem(count), k.sem(count), k.sem(n_local)
        self.waited = False
        k.axes.add(axis)
        k.once.append(self)

    def local(self, src, dst, i):
        return pltpu.make_async_copy(src, dst, self.local_sem.ref.at[i])

    def pairs(self, every):
        far, near = self.make(*spot())
        for i, (sources, dst, peer) in enumerate(far):
            for cond, src in sources if every else sources[:1]:
                yield cond, True, remote(
                    src, dst, self.send_sem.ref.at[i], self.recv_sem.ref.at[i], peer
                )
        for i, (sources, dst) in enumerate(near):
            for cond, src in sources if every else sources[:1]:
                yield cond, False, self.local(src, dst, i)

    def step(self):
        pass

    def send(self):
        for cond, far, move in self.pairs(True):
            if far and self.final is not None:
                cond = lax.axis_index("section") == 1 - self.final
            if cond is None:
                move.start()
            else:
                pl.when(cond)(move.start)

    def wait(self):
        if self.waited:
            return
        self.waited = True
        s = lax.axis_index("section")
        for _, far, move in self.pairs(False):
            if not far:
                move.wait()
            elif self.final is None:
                move.wait_recv()
                move.wait_send()
            else:
                pl.when(s == 1 - self.final)(move.wait_send)
                pl.when(s == self.final)(move.wait_recv)


def as_val(k, value):
    value = value.out if isinstance(value, Task) else value
    known = isinstance(value, Val) and (value.array is None)
    return value if known else k.input(value)


class Line(Task):
    def __init__(self, k, out, out_dtype=BF, n_local=1):
        super().__init__(k, out, "line", None, 6, n_local, out_dtype)
        self.send_sem, self.recv_sem = k.sem(2, 3), k.sem(2, 3)
        self.phase = 0

    def hop(self, j, way, src, dst):
        d = lax.axis_index("dp")
        peer = {"dp": (d + 1 if way == 0 else d + 3) % 4}
        return remote(src, dst, self.send_sem.ref.at[way, j], self.recv_sem.ref.at[way, j], peer)


class LineGather(Line):
    def __init__(self, k, sources, shape, dtype):
        super().__init__(k, (4,) + shape, dtype)
        self.sources = sources

    def ends(self, j, way):
        d = lax.axis_index("dp")
        if way == 0:
            return (d >= j) & (d < 3), d >= j + 1
        return (d <= 3 - j) & (d > 0), d <= 2 - j

    def copy(self, j, way, src=None):
        d = lax.axis_index("dp")
        slot = (d + 4 - j if way == 0 else d + j) % 4
        piece = self.out.ref.at[slot]
        return self.hop(j, way, piece if src is None else src, piece)

    def send(self):
        self.phase = 0
        for cond, src in self.sources(*spot()):
            own = self.local(src, self.out.ref.at[lax.axis_index("dp")], 0)
            moves = [(True if cond is None else cond, own)]
            for way in range(2):
                sends = self.ends(0, way)[0]
                moves.append((sends if cond is None else sends & cond, self.copy(0, way, src)))
            for when, move in moves:
                if when is True:
                    move.start()
                else:
                    pl.when(when)(move.start)

    def arrive(self, j):
        for way in range(2):
            pl.when(self.ends(j, way)[1])(self.copy(j, way).wait_recv)

    def step(self):
        self.arrive(self.phase)
        self.phase += 1
        for way in range(2):
            pl.when(self.ends(self.phase, way)[0])(self.copy(self.phase, way).start)

    def wait(self):
        if self.waited:
            return
        self.waited = True
        while self.phase < 2:
            self.step()
        self.arrive(2)
        for j in range(3):
            for way in range(2):
                pl.when(self.ends(j, way)[0])(self.copy(j, way).wait_send)
        d = lax.axis_index("dp")
        self.local(self.sources(*spot())[0][1], self.out.ref.at[d], 0).wait()


def z_gather_from(k, sources, shape, dtype):
    count = dp_size()
    if count == 4:
        return LineGather(k, sources, shape, dtype)

    def moves(s, d, t):
        dst, found = task.out.ref.at[d], sources(s, d, t)
        return [(found, dst, {"dp": (d + i) % count}) for i in range(1, count)], [(found, dst)]

    task = Task(k, (count,) + shape, "dp", moves, count - 1, out_dtype=dtype)
    return task


def z_gather(k, value):
    val = as_val(k, value)
    return z_gather_from(k, lambda s, d, t: [(None, val.ref)], val.shape, val.dtype)


def z_gather_half(k, shard, moved, block):
    shard, moved = as_val(k, shard), as_val(k, moved)
    rows = shard.shape[0] // 2

    def sources(s, d, t):
        own = shard.ref.at[pl.ds(block * rows, rows)]
        return [(s == block, own), (s == 1 - block, moved.ref)]

    return z_gather_from(k, sources, moved.shape, shard.dtype)


def one_way(task, sender):
    task.final = None if sender is None else 1 - sender
    return task


def z_gather_whole(k, shard, moved, block, half=None):
    shard, moved = as_val(k, shard), as_val(k, moved)
    rows = shard.shape[0] if half is None else shard.shape[0] // 2
    part = pl.ds(0 if half is None else half * rows, rows)

    def sources(s, d, t):
        return [(s == block, shard.ref.at[part]), (s == 1 - block, moved.ref.at[part])]

    return z_gather_from(k, sources, (rows,) + shard.shape[1:], shard.dtype)


def x_move(k, value, sender=None):
    val = as_val(k, value)

    def moves(s, d, t):
        return [([(None, val.ref)], task.out.ref, {"section": 1 - s})], []

    task = Task(k, val.shape, "section", moves, 1, out_dtype=val.dtype)
    return one_way(task, sender)


def x_half(k, value, sender=None):
    val = as_val(k, value)
    rows = val.shape[0] // 2

    def moves(s, d, t):
        src = val.ref.at[block_of(1 - s, rows)]
        return [([(None, src)], task.out.ref, {"section": 1 - s})], []

    task = Task(k, (rows,) + val.shape[1:], "section", moves, 1, out_dtype=val.dtype)
    return one_way(task, sender)


def x_slots(k, value, kind):
    val, count = as_val(k, value), dp_size()
    rows = val.shape[0] // (2 * count)

    def moves(s, d, t):
        far = []
        for i in range(count):
            slot = 2 * i + 1 - s if kind == "rows" else (1 - s) * count + i
            src = val.ref.at[block_of(slot, rows)]
            far.append(([(None, src)], task.out.ref.at[i], {"section": 1 - s}))
        return far, []

    task = Task(k, (count, rows) + val.shape[1:], "section", moves, count)
    return task


class Terms:
    def __init__(self, k, kind, grads, received, local):
        self.grads, self.local = as_val(k, grads), local
        self.kind, self.n = kind, dp_size()
        self.whole = received is None
        if self.whole:
            rows, cols = self.grads.shape
            self.rows = rows if kind == "cols" else rows // self.n
            self.cols = cols // self.n if kind == "cols" else cols
            self.shape = (self.n, self.rows, self.cols)
            self.aside = kind == "cols" and self.cols % 128 != 0
            self.total = k.vmem(self.shape, BF)
            self.kept = k.vmem(self.grads.shape, BF) if self.aside else self.total
            return
        self.received = as_val(k, received)
        if kind == "cols":
            self.rows, self.cols = self.grads.shape[0] // 2, self.grads.shape[1] // self.n
            held = (self.rows, self.grads.shape[1])
        else:
            self.rows, self.cols = self.grads.shape[0] // (2 * self.n), self.grads.shape[1]
            held = (self.n, self.rows, self.cols)
        self.kept, self.got = k.vmem(held, BF), k.vmem(held, BF)
        self.shape = (self.n, self.rows, self.cols)
        self.total = k.vmem(self.shape, BF) if kind == "cols" else self.kept

    def loads(self):
        s, grads, kept = lax.axis_index("section"), self.grads.ref, self.kept.ref
        if self.whole and self.aside:
            return [self.local(grads, kept, 2)]
        if self.whole:
            parts = [
                grads.at[:, pl.ds(i * self.cols, self.cols)]
                if self.kind == "cols"
                else grads.at[block_of(i, self.rows)]
                for i in range(self.n)
            ]
            return [self.local(part, kept.at[i], 2 + i) for i, part in enumerate(parts)]
        if self.kind == "cols":
            moves = [self.local(grads.at[block_of(s, self.rows)], kept, 2)]
        else:
            moves = []
            for i in range(self.n):
                slot = 2 * i + s if self.kind == "rows" else s * self.n + i
                moves.append(self.local(grads.at[block_of(slot, self.rows)], kept.at[i], 2 + i))
        return moves + [self.local(self.received.ref, self.got.ref, 1)]

    def load(self):
        for move in self.loads():
            move.start()

    def add(self):
        for move in self.loads():
            move.wait()
        if self.whole and self.aside:
            for i in range(self.n):
                self.total.ref[i] = self.kept.ref[:, i * self.cols : (i + 1) * self.cols]
        if self.whole:
            return
        kept, got, total = self.kept.ref, self.got.ref, self.total.ref
        for i in range(self.n):
            if self.kind == "cols":
                part = (slice(None), slice(i * self.cols, (i + 1) * self.cols))
            else:
                part = i
            total[i] = (kept[part].astype(F32) + got[part].astype(F32)).astype(BF)


class DirectScatter(Task):
    def __init__(self, k, kind, grads, received):
        self.terms = Terms(k, kind, grads, received, lambda *a: self.local(*a))
        count = dp_size()

        def moves(s, d, t):
            total = self.terms.total.ref
            far = []
            for i in range(1, count):
                other = (d + i) % count
                far.append(([(None, total.at[other])], self.out.ref.at[d], {"dp": other}))
            return far, [([(None, total.at[d])], self.out.ref.at[d])]

        super().__init__(k, self.terms.shape, "dp", moves, count - 1, 2 + count)
        self.load = self.terms.load

    def send(self):
        self.terms.add()
        super().send()

    def add(self):
        self.load()
        self.send()


class LineScatter(Line):
    def __init__(self, k, kind, grads, received):
        self.terms = Terms(k, kind, grads, received, lambda *a: self.local(*a))
        super().__init__(k, self.terms.shape[1:], BF, 6)
        self.got = k.vmem((2, 3) + self.terms.shape[1:], BF)
        self.load = self.terms.load

    def ends(self, j, way):
        d = lax.axis_index("dp")
        if way == 0:
            return (d <= j) & (d < 3), (d >= 1) & (d <= j + 1)
        return (d >= 3 - j) & (d > 0), (d <= 2) & (d >= 2 - j)

    def copy(self, j, way):
        d = lax.axis_index("dp")
        to = (d + 3 - j if way == 0 else d + 1 + j) % 4
        return self.hop(j, way, self.terms.total.ref.at[to], self.got.ref.at[way, j])

    def send(self):
        self.phase = 0
        self.terms.add()
        for way in range(2):
            pl.when(self.ends(0, way)[0])(self.copy(0, way).start)

    def take(self, j, way):
        d = lax.axis_index("dp")
        to = (d + 2 - j if way == 0 else d + 2 + j) % 4
        self.copy(j, way).wait_recv()
        total = self.terms.total.ref
        total[to] = (total[to].astype(F32) + self.got.ref[way, j].astype(F32)).astype(BF)

    def arrive(self, j):
        for way in range(2):
            pl.when(self.ends(j, way)[1])(functools.partial(self.take, j, way))

    def step(self):
        self.arrive(self.phase)
        self.phase += 1
        for way in range(2):
            pl.when(self.ends(self.phase, way)[0])(self.copy(self.phase, way).start)

    def wait(self):
        if self.waited:
            return
        self.waited = True
        while self.phase < 2:
            self.step()
        self.arrive(2)
        done = self.local(self.terms.total.ref.at[lax.axis_index("dp")], self.out.ref, 0)
        done.start()
        for j in range(3):
            for way in range(2):
                pl.when(self.ends(j, way)[0])(self.copy(j, way).wait_send)
        done.wait()

    def add(self):
        self.load()
        self.send()


def sum_scatter(k, kind, grads, received=None):
    return (LineScatter if dp_size() == 4 else DirectScatter)(k, kind, grads, received)


class Finish(Task):
    def __init__(self, k, pieces, block):
        self.pieces, self.final = as_val(k, pieces), block
        *slots, rows, cols = self.pieces.shape
        self.slots = slots[0] if slots else 0
        if slots:
            self.held, self.total = k.vmem(self.pieces.shape, BF), k.vmem((rows, cols), BF)
        else:
            self.total = self.pieces

        def moves(s, d, t):
            source, dst = [(None, self.total.ref)], self.out.ref.at[s]
            return [(source, dst, {"section": 1 - s})], [(source, dst)]

        super().__init__(k, (2, rows, cols), "section", moves, 1, 2)

    def load(self):
        if self.slots:
            self.local(self.pieces.ref, self.held.ref, 1).start()

    def send(self):
        if self.slots:
            self.local(self.pieces.ref, self.held.ref, 1).wait()
            acc = self.held.ref[0].astype(F32)
            for i in range(1, self.slots):
                acc = acc + self.held.ref[i].astype(F32)
            self.total.ref[...] = acc.astype(BF)
        super().send()

    def add(self):
        self.load()
        self.send()


class SumShare(Task):
    def __init__(self, k, terms, axis, slotted=False):
        self.terms = [as_val(k, v) for v in terms]
        shape = self.terms[0].shape[1:] if slotted else self.terms[0].shape
        count = dp_size() if axis == "dp" else 4
        self.slotted = slotted
        self.bufs = [k.vmem(v.shape, F32) for v in self.terms]
        self.total = k.vmem(shape, F32)

        def moves(s, d, t):
            source, me = [(None, self.total.ref)], d if axis == "dp" else t
            dst = self.out.ref.at[me]
            far = [(source, dst, {axis: (me + i) % count}) for i in range(1, count)]
            return far, [(source, dst)]

        super().__init__(k, (count,) + shape, axis, moves, count - 1, 3, out_dtype=F32)

    def add(self):
        loads = [self.local(v.ref, b.ref, 1 + i) for i, (v, b) in enumerate(zip(self.terms, self.bufs))]
        for load in loads:
            load.start()
        for load in loads:
            load.wait()
        if self.slotted:
            parts = [self.bufs[0].ref[i] for i in range(self.terms[0].shape[0])]
        else:
            parts = [buf.ref[...] for buf in self.bufs]
        acc = parts[0]
        for part in parts[1:]:
            acc = acc + part
        self.total.ref[...] = acc
        self.send()


class Weight:
    def __init__(self, k, kind, near, far=None, early=False, fixed=False):
        near, far = as_val(k, near), None if far is None else as_val(k, far)
        self.count, self.rows, self.cols = near.shape
        self.kind, self.near, self.far, self.waited = kind, near, far, False
        sides, self.fixed = 1 if far is None else 2, fixed
        if kind == "cols":
            shape = (sides * self.rows, self.count * self.cols)
        else:
            shape = (sides * self.count * self.rows, self.cols)
        self.aside = kind == "cols" and self.cols % 128 != 0
        self.buf, self.sem = k.vmem(shape, BF), k.sem(2 * self.count)
        if self.aside:
            self.held = [k.vmem(near.shape, BF), k.vmem(near.shape, BF)]
        k.once.append(self)
        if early:
            k.early.append(self.start)

    def moves(self):
        s, dst = 0 if self.fixed else lax.axis_index("section"), self.buf.ref
        rows, cols = self.rows, self.cols

        def place(sec, own):
            if self.aside:
                return None
            if self.kind == "cols":
                return dst.at[block_of(sec, rows), pl.ds(own * cols, cols)]
            slot = own * 2 + sec if self.kind == "rows" else sec * self.count + own
            return dst.at[block_of(slot, rows)]

        if self.far is None:
            for i in range(self.count):
                if self.kind == "cols":
                    to = dst.at[:, pl.ds(i * cols, cols)]
                else:
                    to = dst.at[pl.ds(i * rows, rows)]
                to = self.held[0].ref.at[i] if self.aside else to
                yield pltpu.make_async_copy(self.near.ref.at[i], to, self.sem.ref.at[2 * i])
            return
        for i in range(self.count):
            for j, (val, sec) in enumerate(((self.near, s), (self.far, 1 - s))):
                to = self.held[j].ref.at[i] if self.aside else place(sec, i)
                yield pltpu.make_async_copy(val.ref.at[i], to, self.sem.ref.at[2 * i + j])

    def start(self):
        for move in self.moves():
            move.start()

    def wait(self):
        if self.waited:
            return
        self.waited = True
        for move in self.moves():
            move.wait()
        if self.aside:
            s = 0 if self.fixed else lax.axis_index("section")
            for j, sec in enumerate((s, 1 - s) if self.far is not None else (0,)):
                whole = jnp.concatenate([self.held[j].ref[i] for i in range(self.count)], axis=1)
                self.buf.ref[block_of(sec, self.rows), :] = whole


class Product:
    def __init__(self, k, left, right):
        self.left, self.right = left, right
        rows = left.shape[1]
        self.chunk = 384 if rows % 384 == 0 else 256
        self.count = rows // self.chunk
        self.buf = k.vmem((rows, right.shape[1]), BF)
        self.out, self.sem = k.output(self.buf.shape, BF), k.sem(self.count)

    def copy(self, i):
        part = block_of(i, self.chunk)
        return pltpu.make_async_copy(self.buf.ref.at[part], self.out.ref.at[part], self.sem.ref.at[i])

    def run(self):
        def step(i, carry):
            part = block_of(i, self.chunk)
            value = contract(self.left.ref[:, part], self.right.ref[...], 0, 0)
            self.buf.ref[part, :] = value.astype(BF)
            self.copy(i).start()
            return carry

        lax.fori_loop(0, self.count, step, 0)

    def wait(self):
        for i in range(self.count):
            self.copy(i).wait()


def places():
    me = lax.axis_index("tensor")
    sib = me + 1 - 2 * (me % 2)
    cross = (me + 2) % 4
    diag = (sib + 2) % 4
    return me, sib, cross, diag


class Gather:
    def __init__(self, k, x, gain, weights, extras=(), trans=False, epilogue="plain", save=()):
        rows, width = x.shape
        length = 4 * rows
        self.k, self.x, self.gain, self.weights, self.extras = k, x, gain, weights, extras
        self.trans, self.epilogue, self.rows, self.half = trans, epilogue, rows, rows // 2
        cols = [w.buf.shape[0 if trans else 1] for w in weights]
        kinds = {
            "plain": [(c, F32) for c in cols],
            "ffn": [(cols[0], BF)] * 3,
            "ffn_back": [(cols[0], BF)] * 2,
        }[epilogue]
        self.full = k.vmem((length, width), BF)
        self.values = [k.vmem((length, c), kind) for c, kind in kinds]
        kept = [self.full] + self.values
        self.saved = [(v, k.output(v.shape, v.dtype), k.sem(4, 2)) for v in kept if kept.index(v) in save]
        self.sems = [k.sem(2) for _ in range(6)]
        k.late.append(self.end)

    def span(self, owner, sub):
        return pl.ds(pl.multiple_of(owner * self.rows + sub * self.half, self.half), self.half)

    def move(self, kind, i):
        me, sib, cross, _ = places()
        full = self.full.ref
        owner, peer, at = {"cross": (me, cross, 0), "sib": (me, sib, 2), "relay": (cross, sib, 4)}[kind]
        part = full.at[self.span(owner, i)]
        return remote(
            part, part, self.sems[at].ref.at[i], self.sems[at + 1].ref.at[i], {"tensor": peer}
        )

    def begin(self):
        me = places()[0]
        for i in range(2):
            part = self.x.ref[pl.ds(i * self.half, self.half), :].astype(F32)
            if self.gain is not None:
                val, row = self.gain
                part = norm_rows(part, val.ref[row : row + 1, :])
            self.full.ref[self.span(me, i), :] = part.astype(BF)
            self.move("cross", i).start()
            self.move("sib", i).start()

    def loop(self):
        me, sib, cross, diag = places()
        rows, half = self.rows, self.half
        for w in self.weights:
            w.wait()

        def step(p, carry):
            far, sub = p // 2, p % 2
            near = (1 - sub) * me + sub * sib
            first = (1 - far) * near * rows + far * (cross * rows + sub * half)
            second = (1 - far) * (near * rows + half) + far * (diag * rows + sub * half)
            pair = [pl.ds(pl.multiple_of(v, half), half) for v in (first, second)]

            @pl.when(p == 1)
            def _():
                self.move("sib", 0).wait_recv()
                self.move("sib", 1).wait_recv()

            for i in range(2):

                @pl.when(p == 2 + i)
                def _():
                    self.move("cross", i).wait_recv()
                    self.move("relay", i).start()
                    self.move("relay", i).wait_recv()

            def both(val):
                return jnp.concatenate([val.ref[pair[0], :], val.ref[pair[1], :]], axis=0)

            a = both(self.full)
            prods = [contract(a, w.buf.ref[...], 1, 1 if self.trans else 0) for w in self.weights]
            if self.epilogue == "plain":
                values = prods
            elif self.epilogue == "ffn":
                sig, silu = silu_parts(prods[0])
                values = [prods[0], prods[1], silu * prods[1]]
            else:
                gate, up = (both(v).astype(F32) for v in self.extras)
                sig, silu = silu_parts(gate)
                values = [prods[0] * up * sig * (1.0 + gate * (1.0 - sig)), prods[0] * silu]
            for val, value in zip(self.values, values):
                value = value.astype(val.dtype)
                for j in range(2):
                    val.ref[pair[j], :] = value[j * half : (j + 1) * half]
            for val, out, sem in self.saved:
                for j in range(2):
                    pltpu.make_async_copy(
                        val.ref.at[pair[j]], out.ref.at[pair[j]], sem.ref.at[p, j]
                    ).start()
            return carry

        lax.fori_loop(0, 4, step, 0)

    def end(self):
        for i in range(2):
            for kind in ("cross", "sib", "relay"):
                self.move(kind, i).wait_send()
        part = pl.ds(0, self.half)
        for val, out, sem in self.saved:
            for p in range(4):
                for j in range(2):
                    pltpu.make_async_copy(val.ref.at[part], out.ref.at[part], sem.ref.at[p, j]).wait()


class Scatter:
    def __init__(self, k, operands, weights, resid, back=None, trans=False, low=False):
        rows, width = resid.shape
        half = rows // 2
        self.operands, self.weights, self.resid, self.back = operands, weights, resid, back
        self.trans, self.low, self.rows, self.half = trans, low, rows, half
        self.keep, self.own = k.vmem((2, half, width), F32), k.vmem((rows, width), F32)
        self.to_s, self.from_s, self.to_c, self.from_c = (
            k.vmem((2, half, width), BF) for _ in range(4)
        )
        self.to_o, self.from_o = k.vmem((rows, width), BF), k.vmem((rows, width), BF)
        self.out = k.vmem((rows, width), BF if low else F32)
        self.gain_grad = k.vmem((1, width), F32) if back else None
        self.sems = [k.sem(2) for _ in range(4)] + [k.sem(1) for _ in range(2)]
        k.late.append(self.end)

    def move(self, kind, i=0):
        _, sib, cross, _ = places()
        at, src, dst, peer = {
            "diag": (0, self.to_s, self.from_s, sib),
            "cross": (2, self.to_c, self.from_c, cross),
            "near": (4, self.to_o, self.from_o, sib),
        }[kind]
        src, dst = (src.ref, dst.ref) if kind == "near" else (src.ref.at[i], dst.ref.at[i])
        return remote(
            src, dst, self.sems[at].ref.at[i], self.sems[at + 1].ref.at[i], {"tensor": peer}
        )

    def pass_on(self, i):
        self.move("diag", i).wait_recv()
        total = self.keep.ref[i] + self.from_s.ref[i].astype(F32)
        self.to_c.ref[i] = total.astype(BF)
        self.move("cross", i).start()

    def loop(self):
        me, sib, cross, diag = places()
        rows, half = self.rows, self.half
        for w in self.weights:
            w.wait()

        def step(p, carry):
            near, sub = p // 2, p % 2
            base = near * ((1 - sub) * sib + sub * me) * rows
            first = base + (1 - near) * (cross * rows + sub * half)
            second = base + near * half + (1 - near) * (diag * rows + sub * half)
            pair = [pl.ds(pl.multiple_of(v, half), half) for v in (first, second)]
            total = None
            for y, w in zip(self.operands, self.weights):
                a = jnp.concatenate([y.ref[pair[0], :], y.ref[pair[1], :]], axis=0)
                prod = contract(a, w.buf.ref[...], 1, 1 if self.trans else 0)
                total = prod if total is None else total + prod

            for i in range(2):

                @pl.when(p == i)
                def _():
                    self.keep.ref[i] = total[:half]
                    self.to_s.ref[i] = total[half:].astype(BF)
                    self.move("diag", i).start()

            @pl.when(p == 1)
            def _():
                self.pass_on(0)

            @pl.when(p == 2)
            def _():
                self.to_o.ref[...] = total.astype(BF)
                self.move("near").start()
                self.pass_on(1)

            @pl.when(p == 3)
            def _():
                self.own.ref[...] = total

            return carry

        lax.fori_loop(0, 4, step, 0)

    def finish(self):
        self.move("near").wait_recv()
        gain_sum = None
        for i in range(2):
            part = pl.ds(i * self.half, self.half)
            self.move("cross", i).wait_recv()
            total = self.own.ref[part, :] + self.from_o.ref[part, :].astype(F32)
            total = total + self.from_c.ref[i].astype(F32)
            resid = self.resid.ref[part, :].astype(F32)
            if self.back:
                value, (gain, row) = self.back
                value_grad, gain_grad = norm_back(
                    value.ref[part, :].astype(F32), gain.ref[row : row + 1, :], total
                )
                total = value_grad
                gain_sum = gain_grad if gain_sum is None else gain_sum + gain_grad
            self.out.ref[part, :] = (resid + total).astype(self.out.dtype)
        if self.back:
            self.gain_grad.ref[...] = gain_sum

    def end(self):
        self.move("near").wait_send()
        for i in range(2):
            self.move("diag", i).wait_send()
            self.move("cross", i).wait_send()


def delayed(values, by):
    if by == 0:
        return values
    row = lax.broadcasted_iota(jnp.int32, values.shape, 0)
    return jnp.where(row < by, 0.0, pltpu.roll(values, by, 0))


def advanced(values, by):
    if by == 0:
        return values
    length = values.shape[0]
    row = lax.broadcasted_iota(jnp.int32, values.shape, 0)
    return jnp.where(row >= length - by, 0.0, pltpu.roll(values, length - by, 0))


CONV_COLS = 128


class Conv:
    def __init__(self, k, projected, value, kernel):
        self.projected, self.value, self.kernel = projected, value, kernel
        self.y = k.vmem(value.shape, BF)

    def parts(self, j):
        channels = self.value.shape[1]
        at = slice(j * CONV_COLS, (j + 1) * CONV_COLS)
        b_gate = self.projected.ref[:, at]
        c_gate = self.projected.ref[:, channels + at.start : channels + at.stop]
        x_value, taps = self.value.ref[:, at], self.kernel.ref[:, at]
        product = b_gate * x_value
        count = taps.shape[0]
        causal = jnp.zeros_like(product)
        for i in range(count):
            causal = causal + taps[i : i + 1] * delayed(product, count - 1 - i)
        return at, b_gate, c_gate, x_value, taps, product, causal

    def run(self):
        for j in range(self.value.shape[1] // CONV_COLS):
            at, _, c_gate, _, _, _, causal = self.parts(j)
            self.y.ref[:, at] = (c_gate * causal).astype(BF)


class ConvBack(Conv):
    def __init__(self, k, projected, value, kernel, d_y):
        self.projected, self.value, self.kernel, self.d_y = projected, value, kernel, d_y
        self.d_proj = k.vmem(projected.shape, BF)
        self.d_value = k.vmem(value.shape, BF)
        self.d_kernel = k.vmem(kernel.shape, F32)

    def run(self):
        channels = self.value.shape[1]
        for j in range(channels // CONV_COLS):
            at, b_gate, c_gate, x_value, taps, product, causal = self.parts(j)
            d_y = self.d_y.ref[:, at]
            d_causal = d_y * c_gate
            count = taps.shape[0]
            d_product = jnp.zeros_like(product)
            for i in range(count):
                by = count - 1 - i
                row = jnp.sum(d_causal * delayed(product, by), axis=0, keepdims=True)
                self.d_kernel.ref[i : i + 1, at] = row
                d_product = d_product + taps[i : i + 1] * advanced(d_causal, by)
            self.d_proj.ref[:, at] = (d_product * x_value).astype(BF)
            self.d_proj.ref[:, channels + at.start : channels + at.stop] = (d_y * causal).astype(BF)
            self.d_value.ref[:, at] = (d_product * b_gate).astype(BF)


def head_mean(values, head_size):
    width = values.shape[1]
    row = lax.broadcasted_iota(jnp.int32, (width, width), 0) // head_size
    col = lax.broadcasted_iota(jnp.int32, (width, width), 1) // head_size
    group = jnp.where(row == col, 1.0 / head_size, 0.0).astype(F32)
    return lax.dot_general(
        values, group, (((1,), (0,)), ((), ())),
        precision=lax.Precision.HIGHEST, preferred_element_type=F32,
    )


def turn(values, head_size, back):
    width, half = values.shape[1], head_size // 2
    lane = lax.broadcasted_iota(jnp.int32, values.shape, 1) % head_size
    upper = pltpu.roll(values, width - half, 1)
    lower = pltpu.roll(values, half, 1)
    return jnp.where(lane < half, upper, -lower) if back else jnp.where(lane < half, -upper, lower)


def head_norm(values, gain, head_size):
    return values * lax.rsqrt(head_mean(values * values, head_size) + EPS) * gain


def head_norm_back(values, gain, grad_in, head_size):
    row_scale = lax.rsqrt(head_mean(values * values, head_size) + EPS)
    normed = values * row_scale
    gain_grad = jnp.sum(grad_in * normed, axis=0, keepdims=True)
    scaled = grad_in * gain
    return row_scale * (scaled - normed * head_mean(scaled * normed, head_size)), gain_grad


def block_weights(q_rows, keys):
    scores = [contract(q_rows, k_rows, 1, 1) for k_rows in keys]
    query = lax.broadcasted_iota(jnp.int32, scores[-1].shape, 0)
    key = lax.broadcasted_iota(jnp.int32, scores[-1].shape, 1)
    scores[-1] = jnp.where(key <= query, scores[-1], MASKED)
    top = functools.reduce(
        jnp.maximum, [jnp.max(part, axis=1, keepdims=True) for part in scores]
    )
    exps = [jnp.exp(part - top) for part in scores]
    scale = 1.0 / sum(jnp.sum(part, axis=1, keepdims=True) for part in exps)
    return [part * scale for part in exps]


def key_blocks(i):
    blocks = [pl.ds(0, i * ROW_BLOCK)] if i else []
    return blocks + [pl.ds(i * ROW_BLOCK, ROW_BLOCK)]


class Heads:
    def __init__(self, projected, tables, size):
        assert size in (16, 64, 256), size
        self.projected, self.size = projected, size
        self.gain, self.cos, self.sin = (v.buf for v in tables)
        self.loads = tables
        self.length, width = projected.shape
        self.q_cols, self.k_cols = width // 2, width // 4
        self.heads, self.kv_heads = self.q_cols // size, self.k_cols // size
        self.share = self.heads // self.kv_heads

    def per_head(self, k, count, kind):
        return k.vmem((count, self.length, self.size), kind)

    def split(self, val, rows, values):
        for h in range(val.shape[0]):
            val.ref[h, rows, :] = values[:, h * self.size : (h + 1) * self.size]

    def join(self, val, rows):
        return jnp.concatenate([val.ref[h, rows, :] for h in range(val.shape[0])], axis=1)

    def angles(self, rows):
        c, n = self.cos.ref[rows, :], self.sin.ref[rows, :]
        repeat = self.q_cols // c.shape[1]
        return jnp.concatenate([c] * repeat, axis=1), jnp.concatenate([n] * repeat, axis=1)

    def blocks(self, step):
        lax.fori_loop(0, self.length // ROW_BLOCK, lambda p, c: step(block_of(p, ROW_BLOCK)) or c, 0)


class Attend(Heads):
    def __init__(self, k, projected, tables, size):
        super().__init__(projected, tables, size)
        self.q_rot = k.vmem((self.length, self.q_cols), BF)
        self.k_rot = k.vmem((self.length, self.k_cols), BF)
        self.y = k.vmem((self.length, self.q_cols), BF)
        self.q_h, self.y_h = (self.per_head(k, self.heads, BF) for _ in range(2))
        self.k_h, self.v_h = (self.per_head(k, self.kv_heads, BF) for _ in range(2))

    def run(self, *between):
        for load in self.loads:
            load.wait()
        size, q_cols, k_cols, proj = self.size, self.q_cols, self.k_cols, self.projected.ref

        def prepare(rows):
            c, n = self.angles(rows)
            q = head_norm(proj[rows, :q_cols], self.gain.ref[0:1, :], size)
            q = (q * c + turn(q, size, False) * n).astype(BF)
            k = head_norm(proj[rows, q_cols : q_cols + k_cols], self.gain.ref[1:2, :k_cols], size)
            k = (k * c[:, :k_cols] + turn(k, size, False) * n[:, :k_cols]).astype(BF)
            self.q_rot.ref[rows, :] = q
            self.k_rot.ref[rows, :] = k
            self.split(self.q_h, rows, (q.astype(F32) * size**-0.5).astype(BF))
            self.split(self.k_h, rows, k)
            self.split(self.v_h, rows, proj[rows, q_cols + k_cols :].astype(BF))

        self.blocks(prepare)

        def head(h, carry):
            g = h // self.share
            for i in range(self.length // ROW_BLOCK):
                rows, seen = pl.ds(i * ROW_BLOCK, ROW_BLOCK), key_blocks(i)
                weights = block_weights(
                    self.q_h.ref[h, rows, :], [self.k_h.ref[g, at, :] for at in seen]
                )
                value = sum(
                    contract(part.astype(BF), self.v_h.ref[g, at, :], 1, 0)
                    for part, at in zip(weights, seen)
                )
                self.y_h.ref[h, rows, :] = value.astype(BF)
            return carry

        lax.fori_loop(0, self.heads // 2, head, 0)
        for step in between:
            step()
        lax.fori_loop(self.heads // 2, self.heads, head, 0)
        self.y.ref[...] = self.join(self.y_h, slice(None))


class AttendBack(Heads):
    def __init__(self, k, projected, tables, size, q_rot, k_rot, d_y):
        super().__init__(projected, tables, size)
        self.q_rot, self.k_rot, self.d_y = q_rot, k_rot, d_y
        self.q_h, self.dy_h = (self.per_head(k, self.heads, BF) for _ in range(2))
        self.k_h, self.v_h = (self.per_head(k, self.kv_heads, BF) for _ in range(2))
        self.dq_h = self.per_head(k, self.heads, F32)
        self.dk_h, self.dv_h = (self.per_head(k, self.kv_heads, F32) for _ in range(2))
        self.d_proj = k.vmem(projected.shape, BF)
        self.q_gain, self.k_gain = k.vmem((1, self.q_cols), F32), k.vmem((1, self.k_cols), F32)

    def run(self, *between):
        for load in self.loads:
            load.wait()
        size, q_cols, k_cols, proj = self.size, self.q_cols, self.k_cols, self.projected.ref
        scale = size**-0.5
        dq_h, dk_h, dv_h = self.dq_h.ref, self.dk_h.ref, self.dv_h.ref

        def prepare(rows):
            self.split(self.q_h, rows, (self.q_rot.ref[rows, :].astype(F32) * scale).astype(BF))
            self.split(self.dy_h, rows, self.d_y.ref[rows, :].astype(BF))
            self.split(self.k_h, rows, self.k_rot.ref[rows, :])
            self.split(self.v_h, rows, proj[rows, q_cols + k_cols :].astype(BF))

        self.blocks(prepare)
        dk_h[...] = jnp.zeros_like(dk_h)
        dv_h[...] = jnp.zeros_like(dv_h)

        def head(h, carry):
            g = h // self.share
            for i in range(self.length // ROW_BLOCK):
                rows, seen = pl.ds(i * ROW_BLOCK, ROW_BLOCK), key_blocks(i)
                q, low = self.q_h.ref[h, rows, :], self.dy_h.ref[h, rows, :]
                keys = [self.k_h.ref[g, at, :] for at in seen]
                probs = block_weights(q, keys)
                d_weights = [contract(low, self.v_h.ref[g, at, :], 1, 1) for at in seen]
                inner = sum(
                    jnp.sum(a * b, axis=1, keepdims=True) for a, b in zip(probs, d_weights)
                )
                d_q = 0.0
                for at, k, prob, d_weight in zip(seen, keys, probs, d_weights):
                    dv_h[g, at, :] += contract(prob.astype(BF), low, 0, 0)
                    d_scores = (prob * (d_weight - inner)).astype(BF)
                    d_q = d_q + contract(d_scores, k, 1, 0)
                    dk_h[g, at, :] += contract(d_scores, q, 0, 0)
                dq_h[h, rows, :] = d_q * scale
            return carry

        lax.fori_loop(0, self.heads // 2, head, 0)
        for step in between:
            step()
        lax.fori_loop(self.heads // 2, self.heads, head, 0)
        self.q_gain.ref[...] = jnp.zeros_like(self.q_gain.ref)
        self.k_gain.ref[...] = jnp.zeros_like(self.k_gain.ref)

        def finish(rows):
            c, n = self.angles(rows)
            dq, dk, dv = (self.join(v, rows) for v in (self.dq_h, self.dk_h, self.dv_h))
            dq = dq * c + turn(dq * n, size, True)
            dk = dk * c[:, :k_cols] + turn(dk * n[:, :k_cols], size, True)
            dq, q_sum = head_norm_back(proj[rows, :q_cols], self.gain.ref[0:1, :], dq, size)
            dk, k_sum = head_norm_back(
                proj[rows, q_cols : q_cols + k_cols], self.gain.ref[1:2, :k_cols], dk, size
            )
            self.q_gain.ref[...] += q_sum
            self.k_gain.ref[...] += k_sum
            self.d_proj.ref[rows, :q_cols] = dq.astype(BF)
            self.d_proj.ref[rows, q_cols : q_cols + k_cols] = dk.astype(BF)
            self.d_proj.ref[rows, q_cols + k_cols :] = dv.astype(BF)

        self.blocks(finish)


def body(boundary, norm_gain, mix_in, mix_out, w_gate, w_up, w_down, conv_x, conv_kernel, qk_gain):
    first = lax.axis_index("section") == 0
    tensor_index = lax.axis_index("tensor")
    model_width = boundary.shape[3]
    channels = mix_out.shape[1]
    row_shape = boundary.shape[2:]
    length, size = 4 * row_shape[0], qk_gain.shape[1]

    seqs, own_gain = boundary[0], norm_gain[0]
    sh_in, sh_out, sh_gate, sh_up, sh_down = (v[0] for v in (mix_in, mix_out, w_gate, w_up, w_down))
    head_gain = jnp.tile(qk_gain, (1, channels // size))

    def gains_of(k, block, other, early=True):
        own, moved = k.input(own_gain), as_val(k, other)
        sources = lambda s, d, t: [(s == block, own.ref), (s == 1 - block, moved.ref)]
        return Load(k, sources, own.shape, F32, early)

    def start_rows(k, slot, other, early=True):
        own, moved = k.input(seqs), as_val(k, other)
        sources = lambda s, d, t: [(s == slot, own.ref.at[slot]), (s == 1 - slot, moved.ref)]
        return Load(k, sources, row_shape, BF, early)

    def wait(*items):
        return [item.wait for item in items]

    k = Kernel(0)
    t_seq = None
    seq_val = k.input(seqs)

    def seq_moves(s, d, t):
        return [([(None, seq_val.ref.at[1 - s])], t_seq.out.ref, {"section": 1 - s})], []

    t_in, t_out, t_up = (x_half(k, v) for v in (sh_in, sh_out, sh_up))
    t_gate0, t_down0 = x_move(k, sh_gate, 0), x_half(k, sh_down, 0)
    t_gate1, t_down1 = x_half(k, sh_gate, 1), x_move(k, sh_down, 1)
    t_seq = Task(k, row_shape, "section", seq_moves, 1)
    t_gain, z_cols = x_move(k, own_gain), z_gather(k, conv_x)
    z_in0, z_out0 = z_gather_half(k, sh_in, t_in.out, 0), z_gather_half(k, sh_out, t_out.out, 0)
    z_gate0 = z_gather_whole(k, sh_gate, t_gate0.out, 0)
    z_up0 = z_gather_half(k, sh_up, t_up.out, 0)
    x_cols, x_in0, x_out0 = (x_move(k, v.out) for v in (z_cols, z_in0, z_out0))
    x_load, gain_load = start_rows(k, 0, t_seq.out, False), gains_of(k, 0, t_gain.out, False)
    taps = load_all(k, conv_kernel)
    angles = Angles(k, length, size, 128)
    w_in0, w_cols = Weight(k, "rows", z_in0.out, x_in0.out), Weight(k, "conv", z_cols.out, x_cols.out)
    w_out0 = Weight(k, "cols", z_out0.out, x_out0.out)
    g0 = Gather(k, x_load.buf, (gain_load.buf, 0), [w_in0, w_cols], save=(0, 1, 2))
    conv = Conv(k, g0.values[0], g0.values[1], taps.buf)
    y0 = Save(k, conv.y)
    s1 = Scatter(k, [conv.y], [w_out0], x_load.buf)
    mid0 = Save(k, s1.out)
    k.do(t_in.send, t_out.send, z_cols.send, t_gate0.send, t_gate1.send, t_gain.send, t_seq.send)
    k.do(t_in.wait, z_in0.send, t_out.wait, z_out0.send, z_cols.step, z_in0.step, z_out0.step)
    k.do(z_cols.step, z_in0.step, z_out0.step, t_gate0.wait, z_gate0.send)
    k.do(z_cols.wait, x_cols.send, z_in0.wait, x_in0.send, z_out0.wait, x_out0.send)
    k.do(t_up.send, t_down0.send, t_down1.send)
    k.do(t_gain.wait, gain_load.start, t_seq.wait, x_load.start, gain_load.wait, x_load.wait)
    k.do(g0.begin, angles.run, z_gate0.step)
    k.do(x_cols.wait, w_cols.start, x_in0.wait, w_in0.start, z_gate0.step)
    k.do(g0.loop, t_up.wait, z_up0.send, taps.wait, conv.run, y0.start)
    k.do(x_out0.wait, w_out0.start, s1.loop, z_up0.step, s1.finish, mid0.start, z_up0.step)
    k.do(*wait(t_gate1, t_down0, t_down1, z_gate0, z_up0))
    k.build()
    a0, proj0, value0 = (out for _, out, _ in g0.saved)
    table_arrays = [head_gain] + [v.out for v in angles.saves]
    y0, mid0 = y0.out, mid0.out

    k = Kernel(1)
    x_up0, z_down0 = x_move(k, z_up0.out), z_gather_half(k, sh_down, t_down0.out, 0)
    z_in1, z_out1 = z_gather_half(k, sh_in, t_in.out, 1), z_gather_half(k, sh_out, t_out.out, 1)
    z_gate1 = z_gather_half(k, sh_gate, t_gate1.out, 1)
    z_down1a = z_gather_whole(k, sh_down, t_down1.out, 1, 0)
    x_down0, x_in1, x_out1 = (x_move(k, v.out) for v in (z_down0, z_in1, z_out1))
    rows, gain_load = load_all(k, mid0), gains_of(k, 0, t_gain.out)
    w_gate0 = Weight(k, "rows", z_gate0.out, None, True)
    w_up0 = Weight(k, "rows", z_up0.out, x_up0.out)
    w_down0 = Weight(k, "cols", z_down0.out, x_down0.out)
    g2 = Gather(
        k, rows.buf, (gain_load.buf, 1), [w_gate0, w_up0], epilogue="ffn", save=(0, 1, 2, 3)
    )
    s3 = Scatter(k, [g2.values[2]], [w_down0], rows.buf, low=True)
    z_rows = Save(k, s3.out)
    k.do(x_up0.send, z_down0.send, rows.wait, gain_load.wait, g2.begin, z_down0.step)
    k.do(z_in1.send, z_out1.send, z_down0.step, z_in1.step, z_out1.step, z_gate1.send)
    k.do(z_down0.wait, x_down0.send, z_down1a.send, x_up0.wait, w_up0.start, z_in1.step, z_out1.step)
    k.do(g2.loop, z_gate1.step, z_down1a.step, z_in1.wait, x_in1.send, z_out1.wait, x_out1.send)
    k.do(x_down0.wait, w_down0.start, s3.loop, z_gate1.step, z_down1a.step)
    k.do(s3.finish, z_rows.start, *wait(x_in1, x_out1, z_gate1, z_down1a))
    k.build()
    m0, gate0, up0, hid0 = (out for _, out, _ in g2.saved)
    z_rows = z_rows.out

    k = Kernel(2)
    x_gate1, z_up1 = x_move(k, z_gate1.out), z_gather_half(k, sh_up, t_up.out, 1)
    z_down1, x_up1 = z_gather_whole(k, sh_down, t_down1.out, 1, 1), x_move(k, z_up1.out)
    rows, gain_load = load_all(k, z_rows), gains_of(k, 1, t_gain.out)
    tables = [load_all(k, v) for v in table_arrays]
    w_in1 = Weight(k, "rows", z_in1.out, x_in1.out, True)
    w_out1 = Weight(k, "cols", z_out1.out, x_out1.out, True)
    g4 = Gather(k, rows.buf, (gain_load.buf, 0), [w_in1], save=(0, 1))
    attend = Attend(k, g4.values[0], tables, size)
    kept = [Save(k, v) for v in (attend.q_rot, attend.k_rot, attend.y)]
    s5 = Scatter(k, [attend.y], [w_out1], rows.buf)
    mid1 = Save(k, s5.out)
    k.do(x_gate1.send, z_up1.send, z_down1.send)
    k.do(rows.wait, gain_load.wait, g4.begin, z_up1.step, g4.loop, z_up1.step)
    k.do(lambda: attend.run(z_up1.wait, x_up1.send, z_down1.step))
    k.do(*(v.start for v in kept))
    k.do(s5.loop, z_down1.step, s5.finish, mid1.start)
    k.do(*wait(x_gate1, x_up1, z_down1))
    k.build()
    a1, proj1 = (out for _, out, _ in g4.saved)
    q_rot, k_rot, y1 = (v.out for v in kept)
    mid1 = mid1.out

    k = Kernel(3)
    rows, gain_load = load_all(k, mid1), gains_of(k, 1, t_gain.out)
    cot = start_rows(k, 1, t_seq.out)
    w_gate1 = Weight(k, "rows", z_gate1.out, x_gate1.out, True)
    w_up1 = Weight(k, "rows", z_up1.out, x_up1.out, True)
    w_down1 = Weight(k, "cols", z_down1a.out, z_down1.out, True, True)
    g6 = Gather(k, rows.buf, (gain_load.buf, 1), [w_gate1, w_up1], epilogue="ffn")
    g8 = Gather(
        k, cot.buf, None, [w_down1], [g6.values[0], g6.values[1]], trans=True, epilogue="ffn_back"
    )
    p_down1 = Product(k, g6.values[2], g8.full)
    p_gate1, p_up1 = Product(k, g6.full, g8.values[0]), Product(k, g6.full, g8.values[1])
    s7 = Scatter(k, [g6.values[2]], [w_down1], rows.buf, low=True)
    s9 = Scatter(k, g8.values, [w_gate1, w_up1], cot.buf, (rows.buf, (gain_load.buf, 1)), True)
    y_rows, d_mid1, gain11 = Save(k, s7.out), Save(k, s9.out), Save(k, s9.gain_grad)
    k.do(rows.wait, gain_load.wait, g6.begin, cot.wait, g8.begin, g6.loop, s7.loop, g8.loop)
    k.do(s9.loop, p_down1.run, s7.finish, y_rows.start, p_gate1.run, p_up1.run)
    k.do(s9.finish, d_mid1.start, gain11.start, p_down1.wait, p_gate1.wait, p_up1.wait)
    k.build()
    y_rows, d_mid1, gain11 = y_rows.out, d_mid1.out, gain11.out

    k = Kernel(4)
    r_down1 = x_half(k, p_down1.out)
    r_gate1, q_up1 = x_slots(k, p_gate1.out, "rows"), sum_scatter(k, "rows", p_up1.out)
    rows, gain_load = load_all(k, d_mid1), gains_of(k, 1, t_gain.out)
    value = load_all(k, z_rows)
    tables = [load_all(k, v) for v in table_arrays]
    proj, q_load, k_load, y_load, a_load = (load_all(k, v) for v in (proj1, q_rot, k_rot, y1, a1))
    w_in1 = Weight(k, "rows", z_in1.out, x_in1.out, True)
    w_out1 = Weight(k, "cols", z_out1.out, x_out1.out, True)
    g10 = Gather(k, rows.buf, None, [w_out1], trans=True)
    p_out1 = Product(k, y_load.buf, g10.full)
    back = AttendBack(k, proj.buf, tables, size, q_load.buf, k_load.buf, g10.values[0])
    p_in1 = Product(k, a_load.buf, back.d_proj)
    r_out1 = x_half(k, p_out1.out)
    s11 = Scatter(
        k, [back.d_proj], [w_in1], rows.buf, (value.buf, (gain_load.buf, 0)), True, low=True
    )
    d_z, gain10 = Save(k, s11.out), Save(k, s11.gain_grad)
    head_gains = [Save(k, back.q_gain), Save(k, back.k_gain)]
    k.early.append(q_up1.load)
    k.do(r_down1.send, r_gate1.send, rows.wait, g10.begin, q_up1.send, g10.loop)
    k.do(y_load.wait, p_out1.run, q_up1.step, p_out1.wait, r_out1.send)
    k.do(proj.wait, q_load.wait, k_load.wait, lambda: back.run(q_up1.step))
    k.do(*(v.start for v in head_gains))
    k.do(gain_load.wait, value.wait, s11.loop, a_load.wait, p_in1.run)
    k.do(s11.finish, d_z.start, gain10.start, p_in1.wait)
    k.do(*wait(r_down1, q_up1, r_gate1, r_out1))
    k.build()
    d_z, gain10 = d_z.out, gain10.out
    q_gain, k_gain = (v.out for v in head_gains)

    k = Kernel(5)
    q_gate1, m_up1 = sum_scatter(k, "rows", p_gate1.out, r_gate1.out), x_move(k, q_up1.out, 0)
    q_out1 = sum_scatter(k, "cols", p_out1.out, r_out1.out)
    r_in1 = x_slots(k, p_in1.out, "rows")
    q_in1 = sum_scatter(k, "rows", p_in1.out, r_in1.out)
    q_down1 = sum_scatter(k, "cols", p_down1.out, r_down1.out)
    rows, value, gain_load = load_all(k, d_z), load_all(k, mid0), gains_of(k, 0, t_gain.out)
    gate_load, up_load, hid_load, m_load = (load_all(k, v) for v in (gate0, up0, hid0, m0))
    w_gate0 = Weight(k, "rows", z_gate0.out, None, True)
    w_up0 = Weight(k, "rows", z_up0.out, x_up0.out, True)
    w_down0 = Weight(k, "cols", z_down0.out, x_down0.out, True)
    g12 = Gather(
        k, rows.buf, None, [w_down0], [gate_load.buf, up_load.buf], trans=True, epilogue="ffn_back"
    )
    p_down0 = Product(k, hid_load.buf, g12.full)
    p_gate0, p_up0 = Product(k, m_load.buf, g12.values[0]), Product(k, m_load.buf, g12.values[1])
    r_down0 = x_half(k, p_down0.out)
    s13 = Scatter(
        k, g12.values, [w_gate0, w_up0], rows.buf, (value.buf, (gain_load.buf, 1)), True
    )
    d_mid0, gain01 = Save(k, s13.out), Save(k, s13.gain_grad)
    k.early += [q_gate1.load, q_down1.load, q_out1.load]
    k.do(r_in1.send, m_up1.send, rows.wait, g12.begin, q_gate1.send, q_down1.send, q_out1.send)
    k.do(gate_load.wait, up_load.wait, g12.loop, q_gate1.step, q_down1.step, q_out1.step)
    k.do(hid_load.wait, p_down0.run, p_down0.wait, r_down0.send, r_in1.wait, q_in1.add)
    k.do(s13.loop, q_gate1.step, q_down1.step, q_out1.step)
    k.do(m_load.wait, p_gate0.run, q_in1.step, p_up0.run, value.wait, gain_load.wait)
    k.do(s13.finish, d_mid0.start, gain01.start, q_in1.step, p_gate0.wait, p_up0.wait)
    k.do(*wait(q_gate1, q_out1, q_in1, q_down1, m_up1, r_down0))
    k.build()
    d_mid0, gain01 = d_mid0.out, gain01.out

    k = Kernel(6)
    r_gate0 = x_slots(k, p_gate0.out, "rows")
    q_gate0 = sum_scatter(k, "rows", p_gate0.out, r_gate0.out)
    q_down0 = sum_scatter(k, "cols", p_down0.out, r_down0.out)
    q_up0 = sum_scatter(k, "rows", p_up0.out)
    m_up0 = x_move(k, q_up0.out, 1)
    e_down1 = Finish(k, q_down1.out, 1)
    e_gate1, e_out1, e_in1 = (Finish(k, v.out, 1) for v in (q_gate1, q_out1, q_in1))
    rows, gain_load = load_all(k, d_mid0), gains_of(k, 0, t_gain.out)
    x_load, taps = start_rows(k, 0, t_seq.out), load_all(k, conv_kernel)
    y_load, a_load, proj, value = (load_all(k, v) for v in (y0, a0, proj0, value0))
    w_in0 = Weight(k, "rows", z_in0.out, x_in0.out, True)
    w_cols = Weight(k, "conv", z_cols.out, x_cols.out, True)
    w_out0 = Weight(k, "cols", z_out0.out, x_out0.out, True)
    g14 = Gather(k, rows.buf, None, [w_out0], trans=True)
    p_out0 = Product(k, y_load.buf, g14.full)
    back = ConvBack(k, proj.buf, value.buf, taps.buf, g14.values[0])
    p_in0, p_cols = Product(k, a_load.buf, back.d_proj), Product(k, a_load.buf, back.d_value)
    r_out0, r_in0 = x_half(k, p_out0.out), x_slots(k, p_in0.out, "rows")
    r_cols = x_slots(k, p_cols.out, "conv")
    q_out0, q_in0 = sum_scatter(k, "cols", p_out0.out, r_out0.out), sum_scatter(k, "rows", p_in0.out, r_in0.out)
    q_cols = sum_scatter(k, "conv", p_cols.out, r_cols.out)
    e_down0, e_gate0, e_out0, e_in0 = (
        Finish(k, v.out, 0) for v in (q_down0, q_gate0, q_out0, q_in0)
    )
    s15 = Scatter(
        k, [back.d_proj, back.d_value], [w_in0, w_cols], rows.buf,
        (x_load.buf, (gain_load.buf, 0)), True, low=True,
    )
    d_x = Save(k, s15.out)
    tap_rows = conv_kernel.shape[0]
    small = k.vmem((8, model_width), F32)
    small_out = Save(k, small)
    ready = [load_all(k, v) for v in (gain01, gain10, gain11)]
    head_loads = [load_all(k, v) for v in (q_gain, k_gain)]

    def fill_small():
        t = lax.axis_index("tensor")
        small.ref[...] = jnp.zeros_like(small.ref)
        small.ref[0:1, :] = s15.gain_grad.ref[...]
        for i, load in enumerate(ready):
            load.wait()
            small.ref[i + 1 : i + 2, :] = load.buf.ref[...]
        small.ref[4 : 4 + tap_rows, block_of(t, channels)] = back.d_kernel.ref[...]
        at = 0
        for load in head_loads:
            load.wait()
            width = load.buf.shape[1]
            small.ref[7:8, at : at + width] = load.buf.ref[...]
            at += width
        small_out.start()

    t_small = x_move(k, small_out.out)
    z_small = SumShare(k, [small_out.out, t_small.out], "dp")
    t_total = SumShare(k, [z_small.out], "tensor", slotted=True)
    y_val, dx_val = k.input(y_rows), d_x.out

    def result_moves(s, d, t):
        sources = [(s == 0, y_val.ref), (s == 1, dx_val.ref)]
        return [(sources, t_result.out.ref, {"section": 1 - s})], []

    t_result = Task(k, row_shape, "section", result_moves, 1)
    k.early += [q_up0.load, q_down0.load]
    k.early += [v.load for v in (e_down1, e_gate1, e_out1, e_in1)]
    k.do(r_gate0.send, rows.wait, g14.begin, q_up0.send, q_down0.send)
    k.do(e_down1.send, e_gate1.send, e_out1.send, e_in1.send, g14.loop)
    k.do(y_load.wait, p_out0.run, p_out0.wait, r_out0.send, q_up0.step)
    k.do(proj.wait, value.wait, taps.wait, back.run, q_down0.step, a_load.wait)
    k.do(p_in0.run, p_cols.run, p_in0.wait, r_in0.send, p_cols.wait, r_cols.send)
    k.do(r_gate0.wait, q_gate0.add, x_load.wait, gain_load.wait, s15.loop, q_up0.step)
    k.do(q_down0.step, s15.finish, d_x.start, fill_small, d_x.wait, t_result.send)
    k.do(small_out.wait, t_small.send, q_gate0.step, r_out0.wait, q_out0.add, r_in0.wait, q_in0.add)
    k.do(r_cols.wait, q_cols.add, q_up0.wait, m_up0.send, q_down0.wait, e_down0.add)
    k.do(q_gate0.step, q_out0.step, q_in0.step, q_cols.step, t_small.wait, z_small.add)
    k.do(q_gate0.wait, e_gate0.add, q_out0.step, q_in0.step, q_cols.step)
    k.do(z_small.wait, t_total.add, q_out0.wait, e_out0.add, q_in0.wait, e_in0.add)
    rest = (e_down1, e_gate1, e_out1, e_in1, q_cols, e_down0, e_gate0, m_up0, e_out0, e_in0)
    k.do(*wait(*rest, t_total, t_result))
    k.build()

    owned = [
        ([e_in0], [e_in1], 1),
        ([e_out0], [e_out1], 1),
        ([e_gate0], [e_gate1], 1),
        ([q_up0, m_up0], [q_up1, m_up1], 1),
        ([e_down0], [e_down1], 1),
        ([q_cols], [q_cols], 0),
    ]
    return pack(
        [(zero, one, lead) for zero, one, lead in owned], t_total, d_x.out, y_rows, t_result,
        (norm_gain.shape, conv_kernel.shape, qk_gain.shape),
    )


def slot_free(val, shape):
    value = val.out.array
    if value.ndim == 3 and value.shape[0] * value.shape[1] != shape[0]:
        value = jnp.sum(value.astype(F32), axis=0).astype(BF)
    return value.reshape(shape)


def pack_kernel(plan, *refs):
    n_in, leads, terms, tap_rows = plan
    ins, rest = refs[:n_in], refs[n_in:]
    result, gain_out, *grads, cols, taps, heads = rest[: len(leads) + 4]
    grads = [*grads, cols]
    room = iter(rest[len(leads) + 4 :])
    own_v, moved_v, small_v, *bufs = (next(room) for _ in range(3 + len(terms)))
    out_v = [next(room) for _ in leads]
    load_sem, store_sem = room
    s, t = lax.axis_index("section"), lax.axis_index("tensor")
    small, d_x, y_rows, moved, *parts = ins

    def either(cond, zero, one, dst, sem):
        if zero is not None:
            pl.when(cond)(pltpu.make_async_copy(zero, dst, sem).start)
        if one is not None:
            pl.when(jnp.logical_not(cond))(pltpu.make_async_copy(one, dst, sem).start)

    first = s == 0
    either(first, d_x, y_rows, own_v, load_sem.at[0])
    pltpu.make_async_copy(moved, moved_v, load_sem.at[1]).start()
    pltpu.make_async_copy(small, small_v, load_sem.at[2]).start()
    for j, (zero, one, _) in enumerate(terms):
        either(
            first,
            None if zero is None else parts[zero],
            None if one is None else parts[one],
            bufs[j],
            load_sem.at[3 + j],
        )
    for j, (zero, one, i) in enumerate(terms):
        arrive = pltpu.make_async_copy(parts[one if zero is None else zero], bufs[j], load_sem.at[3 + j])
        begins = j == 0 or terms[j - 1][2] != i

        def put(j=j, i=i, begins=begins):
            value = bufs[j][...].astype(F32)
            value = value if begins else out_v[i][...] + value
            out_v[i][...] = value

        if zero is None or one is None:
            cond = first if one is None else jnp.logical_not(first)

            @pl.when(cond)
            def _(arrive=arrive, put=put):
                arrive.wait()
                put()
        else:
            arrive.wait()
            put()
        if j + 1 == len(terms) or terms[j + 1][2] != i:
            dst = grads[i].at[0] if leads[i] else grads[i]
            pltpu.make_async_copy(out_v[i], dst, store_sem.at[i]).start()
    pltpu.make_async_copy(d_x, own_v, load_sem.at[0]).wait()
    pltpu.make_async_copy(moved, moved_v, load_sem.at[1]).wait()
    n = len(leads)
    stores = [
        pltpu.make_async_copy(own_v, result.at[0, s], store_sem.at[n]),
        pltpu.make_async_copy(moved_v, result.at[0, 1 - s], store_sem.at[n + 1]),
    ]
    for store in stores:
        store.start()
    pltpu.make_async_copy(small, small_v, load_sem.at[2]).wait()
    total = small_v[0]
    for i in range(1, small_v.shape[0]):
        total = total + small_v[i]
    gain_out[0] = jnp.where(first, total[0:2], total[2:4])
    channels, size = taps.shape[1], heads.shape[1]
    chosen = total[4 : 4 + tap_rows, 0:channels]
    for i in range(1, total.shape[1] // channels):
        chosen = jnp.where(t == i, total[4 : 4 + tap_rows, i * channels : (i + 1) * channels], chosen)
    taps[...] = chosen
    at = 0
    for row, width in enumerate((channels, channels // 2)):
        value = total[7:8, at : at + size]
        for i in range(1, width // size):
            value = value + total[7:8, at + i * size : at + (i + 1) * size]
        heads[row : row + 1, :] = value
        at += width
    for i, store in enumerate(leads):
        dst = grads[i].at[0] if store else grads[i]
        pltpu.make_async_copy(out_v[i], dst, store_sem.at[i]).wait()
    for store in stores:
        store.wait()


def pack(owned, small, d_x, y_rows, moved, shapes):
    gain_shape, tap_shape, head_shape = shapes
    parts, terms, leads, out_shapes = [], [], [], []
    for i, (zero, one, lead) in enumerate(owned):
        whole = zero[0].out.shape
        if lead and len(whole) == 3 and isinstance(zero[0], Finish):
            shape = (whole[0] * whole[1], whole[2])
        else:
            shape = whole[-2:]
        shape = tuple(shape)
        leads.append(lead)
        out_shapes.append(shape)
        for j in range(max(len(zero), len(one))):
            pair = []
            for side in (zero, one):
                if j < len(side):
                    parts.append(slot_free(side[j], shape))
                    pair.append(len(parts) - 1)
                else:
                    pair.append(None)
            terms.append((*pair, i))
    operands = [small.out.array, d_x.array, y_rows.array, moved.out.array, *parts]
    rows = d_x.shape
    smem = pl.BlockSpec(memory_space=pltpu.VMEM)
    out_shape = [jax.ShapeDtypeStruct((1, 2) + rows, BF), jax.ShapeDtypeStruct(gain_shape, F32)]
    out_shape += [
        jax.ShapeDtypeStruct((1,) + v if lead else v, F32) for v, lead in zip(out_shapes, leads)
    ]
    out_shape += [jax.ShapeDtypeStruct(v, F32) for v in (tap_shape, head_shape)]
    n = len(leads)
    return tuple(
        pl.pallas_call(
            functools.partial(
                pack_kernel, (len(operands), tuple(leads), tuple(terms), tap_shape[0])
            ),
            out_shape=out_shape,
            in_specs=[ANY] * len(operands),
            out_specs=[ANY, smem] + [ANY] * n + [smem] * 2,
            scratch_shapes=[pltpu.VMEM(rows, BF)] * 2
            + [pltpu.VMEM(small.out.shape, F32)]
            + [pltpu.VMEM(out_shapes[i], BF) for _, _, i in terms]
            + [pltpu.VMEM(v, F32) for v in out_shapes]
            + [DMA((3 + len(terms),)), DMA((n + 2,))],
            compiler_params=pltpu.CompilerParams(vmem_limit_bytes=VMEM_BYTES),
            name="pack",
        )(*operands)
    )


def solution(mesh):
    in_specs = (
        P("section", "dp", "tensor", None),
        P("section", None, None),
        P("section", "dp", "tensor"),
        P("section", "tensor", "dp"),
        P("section", "dp", "tensor"),
        P("section", "dp", "tensor"),
        P("section", "tensor", "dp"),
        P(("section", "dp"), "tensor"),
        P(None, "tensor"),
        P(),
    )
    out_specs = (
        P("section", "dp", "tensor", None),
        P("section", None, None),
        P("section", "dp", "tensor"),
        P("section", "tensor", "dp"),
        P("section", "dp", "tensor"),
        P("section", "dp", "tensor"),
        P("section", "tensor", "dp"),
        P(("section", "dp"), "tensor"),
        P(None, "tensor"),
        P(),
    )
    return jax.shard_map(body, mesh=mesh, in_specs=in_specs, out_specs=out_specs, check_vma=False)
```

```python
import functools

import jax
import jax.numpy as jnp
from jax import lax
from jax.experimental import pallas as pl
from jax.experimental.pallas import tpu as pltpu
from jax.sharding import PartitionSpec as P

HEADS = 16
KV_HEADS = 8

EPS = 1e-05
ROPE_BASE = 1000000.0
MASKED = -1e30

MESH = pl.DeviceIdType.MESH
ANY = pl.BlockSpec(memory_space=pl.ANY)
DMA = pltpu.SemaphoreType.DMA
VMEM_BYTES = 63 * 1024 * 1024
BF = jnp.bfloat16
F32 = jnp.float32
ROW_BLOCK = 256


def contract(left_op, right_op, left_dim, right_dim):
    return lax.dot_general(
        left_op, right_op, (((left_dim,), (right_dim,)), ((), ())), preferred_element_type=F32
    )


def norm_rows(values, gain):
    return values * lax.rsqrt(jnp.mean(values * values, axis=-1, keepdims=True) + EPS) * gain


def norm_back(values, gain, grad_in):
    row_scale = lax.rsqrt(jnp.mean(values * values, axis=-1, keepdims=True) + EPS)
    normed = values * row_scale
    gain_grad = jnp.sum(grad_in * normed, axis=0, keepdims=True)
    scaled = grad_in * gain
    value_grad = row_scale * (scaled - normed * jnp.mean(scaled * normed, axis=-1, keepdims=True))
    return (value_grad, gain_grad)


class Angles:
    def __init__(self, k, length, head_size, width):
        self.half = head_size // 2
        self.tables = [k.vmem((length, width), F32) for _ in range(2)]
        self.saves = [Save(k, v) for v in self.tables]

    def run(self):
        cos, sin = self.tables
        shape = (ROW_BLOCK, cos.shape[1])
        column = (lax.broadcasted_iota(jnp.int32, shape, 1) % self.half).astype(F32)
        frequency = ROPE_BASE ** (-(column / self.half))
        row = lax.broadcasted_iota(jnp.int32, shape, 0)

        def step(i, carry):
            rows = block_of(i, ROW_BLOCK)
            angle = (row + i * ROW_BLOCK).astype(F32) * frequency
            cos.ref[rows, :] = jnp.cos(angle)
            sin.ref[rows, :] = jnp.sin(angle)
            return carry

        lax.fori_loop(0, cos.shape[0] // ROW_BLOCK, step, 0)
        for save in self.saves:
            save.start()


def silu_parts(gate):
    sig = 1.0 / (1.0 + jnp.exp(-gate))
    return sig, gate * sig


def dp_size():
    return lax.axis_size("dp")


def spot():
    return tuple(lax.axis_index(a) for a in ("section", "dp", "tensor"))


def block_of(index, size):
    return pl.ds(pl.multiple_of(index * size, size), size)


class Val:
    def __init__(self, shape, dtype):
        self.shape, self.dtype = tuple(shape), dtype
        self.ref = self.array = None


class Kernel:
    def __init__(self, cid):
        self.cid, self.ins, self.arrays, self.outs, self.room = cid, [], [], [], []
        self.early, self.steps, self.late, self.axes = [], [], [], set()
        self.once = []

    def input(self, array):
        array = array.array if isinstance(array, Val) else array
        for val, known in zip(self.ins, self.arrays):
            if known is array:
                return val
        val = Val(array.shape, array.dtype)
        self.ins.append(val)
        self.arrays.append(array)
        return val

    def output(self, shape, dtype):
        val = Val(shape, dtype)
        self.outs.append(val)
        return val

    def vmem(self, shape, dtype):
        val = Val(shape, dtype)
        self.room.append((val, pltpu.VMEM(tuple(shape), dtype)))
        return val

    def sem(self, *shape):
        val = Val(shape, None)
        self.room.append((val, DMA(shape)))
        return val

    def do(self, *steps):
        self.steps += steps

    def body(self, *refs):
        vals = self.ins + self.outs + [val for val, _ in self.room]
        for val, ref in zip(vals, refs):
            val.ref = ref
        for item in self.once:
            item.waited = False
            item.phase = 0
        for step in self.early:
            step()
        self.greet()
        for step in self.steps + self.late:
            step()

    def greet(self):
        s, d, t = spot()
        _, sib, cross, diag = places()
        barrier = pltpu.get_barrier_semaphore()
        peers = [{"tensor": sib}, {"tensor": cross}]
        if "tensor" in self.axes:
            peers.append({"tensor": diag})
        if "section" in self.axes:
            peers.append({"section": 1 - s})
        if "dp" in self.axes:
            peers += [{"dp": (d + i) % dp_size()} for i in range(1, dp_size())]

        def signal(peer):
            pl.semaphore_signal(barrier, inc=1, device_id=peer, device_id_type=MESH)

        for peer in peers:
            signal(peer)
        expected = len(peers)
        if "line" in self.axes and "dp" not in self.axes:
            pl.when(d < 3)(lambda: signal({"dp": (d + 1) % 4}))
            pl.when(d > 0)(lambda: signal({"dp": (d + 3) % 4}))
            expected = expected + (d + 2) // 3 + (5 - d) // 3
        pl.semaphore_wait(barrier, expected)

    def build(self):
        result = pl.pallas_call(
            self.body,
            out_shape=[jax.ShapeDtypeStruct(v.shape, v.dtype) for v in self.outs],
            in_specs=[ANY] * len(self.ins),
            out_specs=[ANY] * len(self.outs),
            scratch_shapes=[room for _, room in self.room],
            compiler_params=pltpu.CompilerParams(
                collective_id=self.cid, has_side_effects=True, vmem_limit_bytes=VMEM_BYTES
            ),
            name=f"stage{self.cid}",
        )(*self.arrays)
        for val, array in zip(self.outs, result):
            val.array = array


def remote(src, dst, send_sem, recv_sem, peer):
    return pltpu.make_async_remote_copy(
        src_ref=src, dst_ref=dst, send_sem=send_sem, recv_sem=recv_sem,
        device_id=peer, device_id_type=MESH,
    )


class Load:
    def __init__(self, k, sources, shape, dtype, early=False):
        self.k, self.sources, self.waited = k, sources, False
        self.buf, self.sem = k.vmem(shape, dtype), k.sem(1)
        k.once.append(self)
        if early:
            k.early.append(self.start)

    def moves(self):
        for cond, source in self.sources(*spot()):
            yield cond, pltpu.make_async_copy(source, self.buf.ref, self.sem.ref.at[0])

    def start(self):
        for cond, move in self.moves():
            if cond is None:
                move.start()
            else:
                pl.when(cond)(move.start)

    def wait(self):
        if not self.waited:
            self.waited = True
            next(self.moves())[1].wait()


def load_all(k, array, early=True):
    val = k.input(array)
    return Load(k, lambda s, d, t: [(None, val.ref)], val.shape, val.dtype, early)


class Save:
    def __init__(self, k, buf):
        self.buf, self.out, self.sem = buf, k.output(buf.shape, buf.dtype), k.sem(1)
        self.waited = False
        k.once.append(self)
        k.late.append(self.wait)

    def move(self):
        return pltpu.make_async_copy(self.buf.ref, self.out.ref, self.sem.ref.at[0])

    def start(self):
        self.move().start()

    def wait(self):
        if not self.waited:
            self.waited = True
            self.move().wait()


class Task:
    final = None

    def __init__(self, k, out, axis, moves, count, n_local=1, out_dtype=BF):
        self.k, self.axis, self.make = k, axis, moves
        self.out = k.output(out, out_dtype)
        self.send_sem, self.recv_sem, self.local_sem = k.sem(count), k.sem(count), k.sem(n_local)
        self.waited = False
        k.axes.add(axis)
        k.once.append(self)

    def local(self, src, dst, i):
        return pltpu.make_async_copy(src, dst, self.local_sem.ref.at[i])

    def pairs(self, every):
        far, near = self.make(*spot())
        for i, (sources, dst, peer) in enumerate(far):
            for cond, src in sources if every else sources[:1]:
                yield cond, True, remote(
                    src, dst, self.send_sem.ref.at[i], self.recv_sem.ref.at[i], peer
                )
        for i, (sources, dst) in enumerate(near):
            for cond, src in sources if every else sources[:1]:
                yield cond, False, self.local(src, dst, i)

    def step(self):
        pass

    def send(self):
        for cond, far, move in self.pairs(True):
            if far and self.final is not None:
                cond = lax.axis_index("section") == 1 - self.final
            if cond is None:
                move.start()
            else:
                pl.when(cond)(move.start)

    def wait(self):
        if self.waited:
            return
        self.waited = True
        s = lax.axis_index("section")
        for _, far, move in self.pairs(False):
            if not far:
                move.wait()
            elif self.final is None:
                move.wait_recv()
                move.wait_send()
            else:
                pl.when(s == 1 - self.final)(move.wait_send)
                pl.when(s == self.final)(move.wait_recv)


class Part:
    def __init__(self, base, start, rows):
        self.base, self.start, self.rows = base, start, rows
        self.shape, self.dtype = (rows,) + tuple(base.shape[1:]), base.dtype
        self.array = None

    @property
    def ref(self):
        return self.base.ref.at[pl.ds(self.start, self.rows)]


def as_val(k, value):
    if isinstance(value, Part):
        return Part(as_val(k, value.base), value.start, value.rows)
    value = value.out if isinstance(value, Task) else value
    known = isinstance(value, Val) and (value.array is None)
    return value if known else k.input(value)


class Line(Task):
    def __init__(self, k, out, out_dtype=BF, n_local=1):
        super().__init__(k, out, "line", None, 6, n_local, out_dtype)
        self.send_sem, self.recv_sem = k.sem(2, 3), k.sem(2, 3)
        self.phase = 0

    def hop(self, j, way, src, dst):
        d = lax.axis_index("dp")
        peer = {"dp": (d + 1 if way == 0 else d + 3) % 4}
        return remote(src, dst, self.send_sem.ref.at[way, j], self.recv_sem.ref.at[way, j], peer)


class LineGather(Line):
    def __init__(self, k, sources, shape, dtype):
        super().__init__(k, (4,) + shape, dtype)
        self.sources = sources

    def ends(self, j, way):
        d = lax.axis_index("dp")
        if way == 0:
            return (d >= j) & (d < 3), d >= j + 1
        return (d <= 3 - j) & (d > 0), d <= 2 - j

    def copy(self, j, way, src=None):
        d = lax.axis_index("dp")
        slot = (d + 4 - j if way == 0 else d + j) % 4
        piece = self.out.ref.at[slot]
        return self.hop(j, way, piece if src is None else src, piece)

    def send(self):
        self.phase = 0
        for cond, src in self.sources(*spot()):
            own = self.local(src, self.out.ref.at[lax.axis_index("dp")], 0)
            moves = [(True if cond is None else cond, own)]
            for way in range(2):
                sends = self.ends(0, way)[0]
                moves.append((sends if cond is None else sends & cond, self.copy(0, way, src)))
            for when, move in moves:
                if when is True:
                    move.start()
                else:
                    pl.when(when)(move.start)

    def arrive(self, j):
        for way in range(2):
            pl.when(self.ends(j, way)[1])(self.copy(j, way).wait_recv)

    def step(self):
        self.arrive(self.phase)
        self.phase += 1
        for way in range(2):
            pl.when(self.ends(self.phase, way)[0])(self.copy(self.phase, way).start)

    def wait(self):
        if self.waited:
            return
        self.waited = True
        while self.phase < 2:
            self.step()
        self.arrive(2)
        for j in range(3):
            for way in range(2):
                pl.when(self.ends(j, way)[0])(self.copy(j, way).wait_send)
        d = lax.axis_index("dp")
        self.local(self.sources(*spot())[0][1], self.out.ref.at[d], 0).wait()


def z_gather_from(k, sources, shape, dtype):
    count = dp_size()
    if count == 4:
        return LineGather(k, sources, shape, dtype)

    def moves(s, d, t):
        dst, found = task.out.ref.at[d], sources(s, d, t)
        return [(found, dst, {"dp": (d + i) % count}) for i in range(1, count)], [(found, dst)]

    task = Task(k, (count,) + shape, "dp", moves, count - 1, out_dtype=dtype)
    return task


def z_gather(k, value):
    val = as_val(k, value)
    return z_gather_from(k, lambda s, d, t: [(None, val.ref)], val.shape, val.dtype)


def z_gather_half(k, shard, moved, block):
    shard, moved = as_val(k, shard), as_val(k, moved)
    rows = shard.shape[0] // 2

    def sources(s, d, t):
        own = shard.ref.at[pl.ds(block * rows, rows)]
        return [(s == block, own), (s == 1 - block, moved.ref)]

    return z_gather_from(k, sources, moved.shape, shard.dtype)


def one_way(task, sender):
    task.final = None if sender is None else 1 - sender
    return task


def z_gather_whole(k, shard, moved, block, half=None):
    shard, moved = as_val(k, shard), as_val(k, moved)
    rows = shard.shape[0] if half is None else shard.shape[0] // 2
    part = pl.ds(0 if half is None else half * rows, rows)

    def sources(s, d, t):
        return [(s == block, shard.ref.at[part]), (s == 1 - block, moved.ref.at[part])]

    return z_gather_from(k, sources, (rows,) + shard.shape[1:], shard.dtype)


def x_move(k, value, sender=None):
    val = as_val(k, value)

    def moves(s, d, t):
        return [([(None, val.ref)], task.out.ref, {"section": 1 - s})], []

    task = Task(k, val.shape, "section", moves, 1, out_dtype=val.dtype)
    return one_way(task, sender)


def x_half(k, value, sender=None):
    val = as_val(k, value)
    rows = val.shape[0] // 2

    def moves(s, d, t):
        src = val.ref.at[block_of(1 - s, rows)]
        return [([(None, src)], task.out.ref, {"section": 1 - s})], []

    task = Task(k, (rows,) + val.shape[1:], "section", moves, 1, out_dtype=val.dtype)
    return one_way(task, sender)


def x_slots(k, value, kind):
    val, count = as_val(k, value), dp_size()
    rows = val.shape[0] // (2 * count)

    def moves(s, d, t):
        far = []
        for i in range(count):
            slot = 2 * i + 1 - s if kind == "rows" else (1 - s) * count + i
            src = val.ref.at[block_of(slot, rows)]
            far.append(([(None, src)], task.out.ref.at[i], {"section": 1 - s}))
        return far, []

    task = Task(k, (count, rows) + val.shape[1:], "section", moves, count)
    return task


class Terms:
    def __init__(self, k, kind, grads, received, local):
        self.grads, self.local = as_val(k, grads), local
        self.kind, self.n = kind, dp_size()
        self.whole = received is None
        if self.whole:
            rows, cols = self.grads.shape
            self.rows = rows if kind == "cols" else rows // self.n
            self.cols = cols // self.n if kind == "cols" else cols
            self.shape = (self.n, self.rows, self.cols)
            self.aside = kind == "cols" and self.cols % 128 != 0
            self.total = k.vmem(self.shape, BF)
            self.kept = k.vmem(self.grads.shape, BF) if self.aside else self.total
            return
        self.received = as_val(k, received)
        if kind == "cols":
            self.rows, self.cols = self.grads.shape[0] // 2, self.grads.shape[1] // self.n
            held = (self.rows, self.grads.shape[1])
        else:
            self.rows, self.cols = self.grads.shape[0] // (2 * self.n), self.grads.shape[1]
            held = (self.n, self.rows, self.cols)
        self.kept, self.got = k.vmem(held, BF), k.vmem(held, BF)
        self.shape = (self.n, self.rows, self.cols)
        self.total = k.vmem(self.shape, BF) if kind == "cols" else self.kept

    def loads(self):
        s, grads, kept = lax.axis_index("section"), self.grads.ref, self.kept.ref
        if self.whole and self.aside:
            return [self.local(grads, kept, 2)]
        if self.whole:
            parts = [
                grads.at[:, pl.ds(i * self.cols, self.cols)]
                if self.kind == "cols"
                else grads.at[block_of(i, self.rows)]
                for i in range(self.n)
            ]
            return [self.local(part, kept.at[i], 2 + i) for i, part in enumerate(parts)]
        if self.kind == "cols":
            moves = [self.local(grads.at[block_of(s, self.rows)], kept, 2)]
        else:
            moves = []
            for i in range(self.n):
                slot = 2 * i + s if self.kind == "rows" else s * self.n + i
                moves.append(self.local(grads.at[block_of(slot, self.rows)], kept.at[i], 2 + i))
        return moves + [self.local(self.received.ref, self.got.ref, 1)]

    def load(self):
        for move in self.loads():
            move.start()

    def add(self):
        for move in self.loads():
            move.wait()
        if self.whole and self.aside:
            for i in range(self.n):
                self.total.ref[i] = self.kept.ref[:, i * self.cols : (i + 1) * self.cols]
        if self.whole:
            return
        kept, got, total = self.kept.ref, self.got.ref, self.total.ref
        for i in range(self.n):
            if self.kind == "cols":
                part = (slice(None), slice(i * self.cols, (i + 1) * self.cols))
            else:
                part = i
            total[i] = (kept[part].astype(F32) + got[part].astype(F32)).astype(BF)


class DirectScatter(Task):
    def __init__(self, k, kind, grads, received):
        self.terms = Terms(k, kind, grads, received, lambda *a: self.local(*a))
        count = dp_size()

        def moves(s, d, t):
            total = self.terms.total.ref
            far = []
            for i in range(1, count):
                other = (d + i) % count
                far.append(([(None, total.at[other])], self.out.ref.at[d], {"dp": other}))
            return far, [([(None, total.at[d])], self.out.ref.at[d])]

        super().__init__(k, self.terms.shape, "dp", moves, count - 1, 2 + count)
        self.load = self.terms.load

    def send(self):
        self.terms.add()
        super().send()

    def add(self):
        self.load()
        self.send()


class LineScatter(Line):
    def __init__(self, k, kind, grads, received):
        self.terms = Terms(k, kind, grads, received, lambda *a: self.local(*a))
        super().__init__(k, self.terms.shape[1:], BF, 6)
        self.got = k.vmem((2, 3) + self.terms.shape[1:], BF)
        self.load = self.terms.load

    def ends(self, j, way):
        d = lax.axis_index("dp")
        if way == 0:
            return (d <= j) & (d < 3), (d >= 1) & (d <= j + 1)
        return (d >= 3 - j) & (d > 0), (d <= 2) & (d >= 2 - j)

    def copy(self, j, way):
        d = lax.axis_index("dp")
        to = (d + 3 - j if way == 0 else d + 1 + j) % 4
        return self.hop(j, way, self.terms.total.ref.at[to], self.got.ref.at[way, j])

    def send(self):
        self.phase = 0
        self.terms.add()
        for way in range(2):
            pl.when(self.ends(0, way)[0])(self.copy(0, way).start)

    def take(self, j, way):
        d = lax.axis_index("dp")
        to = (d + 2 - j if way == 0 else d + 2 + j) % 4
        self.copy(j, way).wait_recv()
        total = self.terms.total.ref
        total[to] = (total[to].astype(F32) + self.got.ref[way, j].astype(F32)).astype(BF)

    def arrive(self, j):
        for way in range(2):
            pl.when(self.ends(j, way)[1])(functools.partial(self.take, j, way))

    def step(self):
        self.arrive(self.phase)
        self.phase += 1
        for way in range(2):
            pl.when(self.ends(self.phase, way)[0])(self.copy(self.phase, way).start)

    def wait(self):
        if self.waited:
            return
        self.waited = True
        while self.phase < 2:
            self.step()
        self.arrive(2)
        done = self.local(self.terms.total.ref.at[lax.axis_index("dp")], self.out.ref, 0)
        done.start()
        for j in range(3):
            for way in range(2):
                pl.when(self.ends(j, way)[0])(self.copy(j, way).wait_send)
        done.wait()

    def add(self):
        self.load()
        self.send()


def sum_scatter(k, kind, grads, received=None):
    return (LineScatter if dp_size() == 4 else DirectScatter)(k, kind, grads, received)


class Finish(Task):
    def __init__(self, k, pieces, block):
        self.pieces, self.final = as_val(k, pieces), block
        *slots, rows, cols = self.pieces.shape
        self.slots = slots[0] if slots else 0
        if slots:
            self.held, self.total = k.vmem(self.pieces.shape, BF), k.vmem((rows, cols), BF)
        else:
            self.total = self.pieces

        def moves(s, d, t):
            source, dst = [(None, self.total.ref)], self.out.ref.at[s]
            return [(source, dst, {"section": 1 - s})], [(source, dst)]

        super().__init__(k, (2, rows, cols), "section", moves, 1, 2)

    def load(self):
        if self.slots:
            self.local(self.pieces.ref, self.held.ref, 1).start()

    def send(self):
        if self.slots:
            self.local(self.pieces.ref, self.held.ref, 1).wait()
            acc = self.held.ref[0].astype(F32)
            for i in range(1, self.slots):
                acc = acc + self.held.ref[i].astype(F32)
            self.total.ref[...] = acc.astype(BF)
        super().send()

    def add(self):
        self.load()
        self.send()


class SumShare(Task):
    def __init__(self, k, terms, axis, slotted=False):
        self.terms = [as_val(k, v) for v in terms]
        shape = self.terms[0].shape[1:] if slotted else self.terms[0].shape
        count = dp_size() if axis == "dp" else 4
        self.slotted = slotted
        self.bufs = [k.vmem(v.shape, F32) for v in self.terms]
        self.total = k.vmem(shape, F32)

        def moves(s, d, t):
            source, me = [(None, self.total.ref)], d if axis == "dp" else t
            dst = self.out.ref.at[me]
            far = [(source, dst, {axis: (me + i) % count}) for i in range(1, count)]
            return far, [(source, dst)]

        super().__init__(k, (count,) + shape, axis, moves, count - 1, 3, out_dtype=F32)

    def add(self):
        loads = [self.local(v.ref, b.ref, 1 + i) for i, (v, b) in enumerate(zip(self.terms, self.bufs))]
        for load in loads:
            load.start()
        for load in loads:
            load.wait()
        if self.slotted:
            parts = [self.bufs[0].ref[i] for i in range(self.terms[0].shape[0])]
        else:
            parts = [buf.ref[...] for buf in self.bufs]
        acc = parts[0]
        for part in parts[1:]:
            acc = acc + part
        self.total.ref[...] = acc
        self.send()


class Weight:
    def __init__(self, k, kind, *segments, early=False):
        self.kind, self.waited = kind, False
        self.segments, start = [], 0
        for near, far in segments:
            near, far = as_val(k, near), None if far is None else as_val(k, far)
            self.segments.append((near, far, start))
            start += near.shape[1] * (1 if far is None else 2)
        self.count, _, self.cols = self.segments[0][0].shape
        self.rows = start
        if kind == "cols":
            shape = (self.rows, self.count * self.cols)
        else:
            shape = (self.count * self.rows, self.cols)
        self.aside = kind == "cols" and self.cols % 128 != 0
        self.buf = k.vmem(shape, BF)
        sides = [v for near, far, _ in self.segments for v in (near, far) if v is not None]
        self.sem = k.sem(len(sides), self.count)
        if self.aside:
            self.held = [k.vmem(v.shape, BF) for v in sides]
        k.once.append(self)
        if early:
            k.early.append(self.start)

    def sides(self):
        s = lax.axis_index("section")
        for near, far, start in self.segments:
            rows = near.shape[1]
            if far is None:
                yield near, start, None
            else:
                yield near, start + s * rows, s
                yield far, start + (1 - s) * rows, 1 - s

    def moves(self):
        dst = self.buf.ref
        for j, (val, start, sec) in enumerate(self.sides()):
            rows = val.shape[1]
            for i in range(self.count):
                if self.aside:
                    to = self.held[j].ref.at[i]
                elif self.kind == "cols":
                    at = pl.ds(pl.multiple_of(start, 16), rows)
                    to = dst.at[at, pl.ds(i * self.cols, self.cols)]
                else:
                    top = (sec * self.count + i) * rows if self.kind == "conv" else i * self.rows + start
                    to = dst.at[pl.ds(pl.multiple_of(top, 16), rows)]
                yield pltpu.make_async_copy(val.ref.at[i], to, self.sem.ref.at[j, i])

    def start(self):
        for move in self.moves():
            move.start()

    def wait(self):
        if self.waited:
            return
        self.waited = True
        for move in self.moves():
            move.wait()
        if self.aside:
            for j, (val, start, _) in enumerate(self.sides()):
                whole = jnp.concatenate([self.held[j].ref[i] for i in range(self.count)], axis=1)
                self.buf.ref[pl.ds(pl.multiple_of(start, 16), val.shape[1]), :] = whole


class Product:
    def __init__(self, k, left, right):
        self.left, self.right = left, right
        rows = left.shape[1]
        self.chunk = 384 if rows % 384 == 0 else 256
        self.count = rows // self.chunk
        self.buf = k.vmem((rows, right.shape[1]), BF)
        self.out, self.sem = k.output(self.buf.shape, BF), k.sem(self.count)

    def copy(self, i):
        part = block_of(i, self.chunk)
        return pltpu.make_async_copy(self.buf.ref.at[part], self.out.ref.at[part], self.sem.ref.at[i])

    def run(self):
        def step(i, carry):
            part = block_of(i, self.chunk)
            value = contract(self.left.ref[:, part], self.right.ref[...], 0, 0)
            self.buf.ref[part, :] = value.astype(BF)
            self.copy(i).start()
            return carry

        lax.fori_loop(0, self.count, step, 0)

    def wait(self):
        for i in range(self.count):
            self.copy(i).wait()


def places():
    me = lax.axis_index("tensor")
    sib = me + 1 - 2 * (me % 2)
    cross = (me + 2) % 4
    diag = (sib + 2) % 4
    return me, sib, cross, diag


class Gather:
    def __init__(self, k, x, gain, weights, extras=(), trans=False, epilogue="plain", save=()):
        rows, width = x.shape
        length = 4 * rows
        self.k, self.x, self.gain, self.weights, self.extras = k, x, gain, weights, extras
        self.trans, self.epilogue, self.rows, self.half = trans, epilogue, rows, rows // 2
        cols = [w.buf.shape[0 if trans else 1] for w in weights]
        kinds = {
            "plain": [(c, F32) for c in cols],
            "ffn": [(cols[0], BF)] * 3,
            "ffn_back": [(cols[0], BF)] * 2,
        }[epilogue]
        self.full = k.vmem((length, width), BF)
        self.values = [k.vmem((length, c), kind) for c, kind in kinds]
        kept = [self.full] + self.values
        self.saved = [(v, k.output(v.shape, v.dtype), k.sem(4, 2)) for v in kept if kept.index(v) in save]
        self.sems = [k.sem(2) for _ in range(6)]
        k.late.append(self.end)

    def span(self, owner, sub):
        return pl.ds(pl.multiple_of(owner * self.rows + sub * self.half, self.half), self.half)

    def move(self, kind, i):
        me, sib, cross, _ = places()
        full = self.full.ref
        owner, peer, at = {"cross": (me, cross, 0), "sib": (me, sib, 2), "relay": (cross, sib, 4)}[kind]
        part = full.at[self.span(owner, i)]
        return remote(
            part, part, self.sems[at].ref.at[i], self.sems[at + 1].ref.at[i], {"tensor": peer}
        )

    def begin(self):
        me = places()[0]
        for i in range(2):
            part = self.x.ref[pl.ds(i * self.half, self.half), :].astype(F32)
            if self.gain is not None:
                val, row = self.gain
                part = norm_rows(part, val.ref[row : row + 1, :])
            self.full.ref[self.span(me, i), :] = part.astype(BF)
            self.move("cross", i).start()
            self.move("sib", i).start()

    def loop(self):
        me, sib, cross, diag = places()
        rows, half = self.rows, self.half
        for w in self.weights:
            w.wait()

        def step(p, carry):
            far, sub = p // 2, p % 2
            near = (1 - sub) * me + sub * sib
            first = (1 - far) * near * rows + far * (cross * rows + sub * half)
            second = (1 - far) * (near * rows + half) + far * (diag * rows + sub * half)
            pair = [pl.ds(pl.multiple_of(v, half), half) for v in (first, second)]

            @pl.when(p == 1)
            def _():
                self.move("sib", 0).wait_recv()
                self.move("sib", 1).wait_recv()

            for i in range(2):

                @pl.when(p == 2 + i)
                def _():
                    self.move("cross", i).wait_recv()
                    self.move("relay", i).start()
                    self.move("relay", i).wait_recv()

            def both(val):
                return jnp.concatenate([val.ref[pair[0], :], val.ref[pair[1], :]], axis=0)

            a = both(self.full)
            prods = [contract(a, w.buf.ref[...], 1, 1 if self.trans else 0) for w in self.weights]
            if self.epilogue == "plain":
                values = prods
            elif self.epilogue == "ffn":
                sig, silu = silu_parts(prods[0])
                values = [prods[0], prods[1], silu * prods[1]]
            else:
                gate, up = (both(v).astype(F32) for v in self.extras)
                sig, silu = silu_parts(gate)
                values = [prods[0] * up * sig * (1.0 + gate * (1.0 - sig)), prods[0] * silu]
            for val, value in zip(self.values, values):
                value = value.astype(val.dtype)
                for j in range(2):
                    val.ref[pair[j], :] = value[j * half : (j + 1) * half]
            for val, out, sem in self.saved:
                for j in range(2):
                    pltpu.make_async_copy(
                        val.ref.at[pair[j]], out.ref.at[pair[j]], sem.ref.at[p, j]
                    ).start()
            return carry

        lax.fori_loop(0, 4, step, 0)

    def end(self):
        for i in range(2):
            for kind in ("cross", "sib", "relay"):
                self.move(kind, i).wait_send()
        part = pl.ds(0, self.half)
        for val, out, sem in self.saved:
            for p in range(4):
                for j in range(2):
                    pltpu.make_async_copy(val.ref.at[part], out.ref.at[part], sem.ref.at[p, j]).wait()


class Scatter:
    def __init__(self, k, operands, weights, resid, back=None, trans=False, low=False):
        rows, width = resid.shape
        half = rows // 2
        self.operands, self.weights, self.resid, self.back = operands, weights, resid, back
        self.trans, self.low, self.rows, self.half = trans, low, rows, half
        self.keep, self.own = k.vmem((2, half, width), F32), k.vmem((rows, width), F32)
        self.to_s, self.from_s, self.to_c, self.from_c = (
            k.vmem((2, half, width), BF) for _ in range(4)
        )
        self.to_o, self.from_o = k.vmem((rows, width), BF), k.vmem((rows, width), BF)
        self.out = k.vmem((rows, width), BF if low else F32)
        self.gain_grad = k.vmem((1, width), F32) if back else None
        self.sems = [k.sem(2) for _ in range(4)] + [k.sem(1) for _ in range(2)]
        k.late.append(self.end)

    def move(self, kind, i=0):
        _, sib, cross, _ = places()
        at, src, dst, peer = {
            "diag": (0, self.to_s, self.from_s, sib),
            "cross": (2, self.to_c, self.from_c, cross),
            "near": (4, self.to_o, self.from_o, sib),
        }[kind]
        src, dst = (src.ref, dst.ref) if kind == "near" else (src.ref.at[i], dst.ref.at[i])
        return remote(
            src, dst, self.sems[at].ref.at[i], self.sems[at + 1].ref.at[i], {"tensor": peer}
        )

    def pass_on(self, i):
        self.move("diag", i).wait_recv()
        total = self.keep.ref[i] + self.from_s.ref[i].astype(F32)
        self.to_c.ref[i] = total.astype(BF)
        self.move("cross", i).start()

    def loop(self):
        me, sib, cross, diag = places()
        rows, half = self.rows, self.half
        for w in self.weights:
            w.wait()

        def step(p, carry):
            near, sub = p // 2, p % 2
            base = near * ((1 - sub) * sib + sub * me) * rows
            first = base + (1 - near) * (cross * rows + sub * half)
            second = base + near * half + (1 - near) * (diag * rows + sub * half)
            pair = [pl.ds(pl.multiple_of(v, half), half) for v in (first, second)]
            total = None
            for y, w in zip(self.operands, self.weights):
                a = jnp.concatenate([y.ref[pair[0], :], y.ref[pair[1], :]], axis=0)
                prod = contract(a, w.buf.ref[...], 1, 1 if self.trans else 0)
                total = prod if total is None else total + prod

            for i in range(2):

                @pl.when(p == i)
                def _():
                    self.keep.ref[i] = total[:half]
                    self.to_s.ref[i] = total[half:].astype(BF)
                    self.move("diag", i).start()

            @pl.when(p == 1)
            def _():
                self.pass_on(0)

            @pl.when(p == 2)
            def _():
                self.to_o.ref[...] = total.astype(BF)
                self.move("near").start()
                self.pass_on(1)

            @pl.when(p == 3)
            def _():
                self.own.ref[...] = total

            return carry

        lax.fori_loop(0, 4, step, 0)

    def finish(self):
        self.move("near").wait_recv()
        gain_sum = None
        for i in range(2):
            part = pl.ds(i * self.half, self.half)
            self.move("cross", i).wait_recv()
            total = self.own.ref[part, :] + self.from_o.ref[part, :].astype(F32)
            total = total + self.from_c.ref[i].astype(F32)
            resid = self.resid.ref[part, :].astype(F32)
            if self.back:
                value, (gain, row) = self.back
                value_grad, gain_grad = norm_back(
                    value.ref[part, :].astype(F32), gain.ref[row : row + 1, :], total
                )
                total = value_grad
                gain_sum = gain_grad if gain_sum is None else gain_sum + gain_grad
            self.out.ref[part, :] = (resid + total).astype(self.out.dtype)
        if self.back:
            self.gain_grad.ref[...] = gain_sum

    def end(self):
        self.move("near").wait_send()
        for i in range(2):
            self.move("diag", i).wait_send()
            self.move("cross", i).wait_send()


def delayed(values, by):
    if by == 0:
        return values
    row = lax.broadcasted_iota(jnp.int32, values.shape, 0)
    return jnp.where(row < by, 0.0, pltpu.roll(values, by, 0))


def advanced(values, by):
    if by == 0:
        return values
    length = values.shape[0]
    row = lax.broadcasted_iota(jnp.int32, values.shape, 0)
    return jnp.where(row >= length - by, 0.0, pltpu.roll(values, length - by, 0))


CONV_COLS = 128


class Conv:
    def __init__(self, k, projected, value, kernel):
        self.projected, self.value, self.kernel = projected, value, kernel
        self.y = k.vmem(value.shape, BF)

    def parts(self, j):
        channels = self.value.shape[1]
        at = slice(j * CONV_COLS, (j + 1) * CONV_COLS)
        b_gate = self.projected.ref[:, at]
        c_gate = self.projected.ref[:, channels + at.start : channels + at.stop]
        x_value, taps = self.value.ref[:, at], self.kernel.ref[:, at]
        product = b_gate * x_value
        count = taps.shape[0]
        causal = jnp.zeros_like(product)
        for i in range(count):
            causal = causal + taps[i : i + 1] * delayed(product, count - 1 - i)
        return at, b_gate, c_gate, x_value, taps, product, causal

    def run(self):
        for j in range(self.value.shape[1] // CONV_COLS):
            at, _, c_gate, _, _, _, causal = self.parts(j)
            self.y.ref[:, at] = (c_gate * causal).astype(BF)


class ConvBack(Conv):
    def __init__(self, k, projected, value, kernel, d_y):
        self.projected, self.value, self.kernel, self.d_y = projected, value, kernel, d_y
        self.d_proj = k.vmem(projected.shape, BF)
        self.d_value = k.vmem(value.shape, BF)
        self.d_kernel = k.vmem(kernel.shape, F32)

    def run(self):
        channels = self.value.shape[1]
        for j in range(channels // CONV_COLS):
            at, b_gate, c_gate, x_value, taps, product, causal = self.parts(j)
            d_y = self.d_y.ref[:, at]
            d_causal = d_y * c_gate
            count = taps.shape[0]
            d_product = jnp.zeros_like(product)
            for i in range(count):
                by = count - 1 - i
                row = jnp.sum(d_causal * delayed(product, by), axis=0, keepdims=True)
                self.d_kernel.ref[i : i + 1, at] = row
                d_product = d_product + taps[i : i + 1] * advanced(d_causal, by)
            self.d_proj.ref[:, at] = (d_product * x_value).astype(BF)
            self.d_proj.ref[:, channels + at.start : channels + at.stop] = (d_y * causal).astype(BF)
            self.d_value.ref[:, at] = (d_product * b_gate).astype(BF)


def head_mean(values, head_size):
    width = values.shape[1]
    row = lax.broadcasted_iota(jnp.int32, (width, width), 0) // head_size
    col = lax.broadcasted_iota(jnp.int32, (width, width), 1) // head_size
    group = jnp.where(row == col, 1.0 / head_size, 0.0).astype(F32)
    return lax.dot_general(
        values, group, (((1,), (0,)), ((), ())),
        precision=lax.Precision.HIGHEST, preferred_element_type=F32,
    )


def turn(values, head_size, back):
    width, half = values.shape[1], head_size // 2
    lane = lax.broadcasted_iota(jnp.int32, values.shape, 1) % head_size
    upper = pltpu.roll(values, width - half, 1)
    lower = pltpu.roll(values, half, 1)
    return jnp.where(lane < half, upper, -lower) if back else jnp.where(lane < half, -upper, lower)


def head_norm(values, gain, head_size):
    return values * lax.rsqrt(head_mean(values * values, head_size) + EPS) * gain


def head_norm_back(values, gain, grad_in, head_size):
    row_scale = lax.rsqrt(head_mean(values * values, head_size) + EPS)
    normed = values * row_scale
    gain_grad = jnp.sum(grad_in * normed, axis=0, keepdims=True)
    scaled = grad_in * gain
    return row_scale * (scaled - normed * head_mean(scaled * normed, head_size)), gain_grad


def block_weights(q_rows, keys):
    scores = [contract(q_rows, k_rows, 1, 1) for k_rows in keys]
    query = lax.broadcasted_iota(jnp.int32, scores[-1].shape, 0)
    key = lax.broadcasted_iota(jnp.int32, scores[-1].shape, 1)
    scores[-1] = jnp.where(key <= query, scores[-1], MASKED)
    top = functools.reduce(
        jnp.maximum, [jnp.max(part, axis=1, keepdims=True) for part in scores]
    )
    exps = [jnp.exp(part - top) for part in scores]
    scale = 1.0 / sum(jnp.sum(part, axis=1, keepdims=True) for part in exps)
    return [part * scale for part in exps]


def key_blocks(i):
    blocks = [pl.ds(0, i * ROW_BLOCK)] if i else []
    return blocks + [pl.ds(i * ROW_BLOCK, ROW_BLOCK)]


class Heads:
    def __init__(self, projected, tables, size):
        assert size in (16, 64, 256), size
        self.projected, self.size = projected, size
        self.gain, self.cos, self.sin = (v.buf for v in tables)
        self.loads = tables
        self.length, width = projected.shape
        self.q_cols, self.k_cols = width // 2, width // 4
        self.heads, self.kv_heads = self.q_cols // size, self.k_cols // size
        self.share = self.heads // self.kv_heads

    def per_head(self, k, count, kind):
        return k.vmem((count, self.length, self.size), kind)

    def split(self, val, rows, values):
        for h in range(val.shape[0]):
            val.ref[h, rows, :] = values[:, h * self.size : (h + 1) * self.size]

    def join(self, val, rows):
        return jnp.concatenate([val.ref[h, rows, :] for h in range(val.shape[0])], axis=1)

    def angles(self, rows):
        c, n = self.cos.ref[rows, :], self.sin.ref[rows, :]
        repeat = self.q_cols // c.shape[1]
        return jnp.concatenate([c] * repeat, axis=1), jnp.concatenate([n] * repeat, axis=1)

    def blocks(self, step):
        lax.fori_loop(0, self.length // ROW_BLOCK, lambda p, c: step(block_of(p, ROW_BLOCK)) or c, 0)


class Attend(Heads):
    def __init__(self, k, projected, tables, size):
        super().__init__(projected, tables, size)
        self.q_rot = k.vmem((self.length, self.q_cols), BF)
        self.k_rot = k.vmem((self.length, self.k_cols), BF)
        self.y = k.vmem((self.length, self.q_cols), BF)
        self.q_h, self.y_h = (self.per_head(k, self.heads, BF) for _ in range(2))
        self.k_h, self.v_h = (self.per_head(k, self.kv_heads, BF) for _ in range(2))

    def run(self, *between):
        for load in self.loads:
            load.wait()
        size, q_cols, k_cols, proj = self.size, self.q_cols, self.k_cols, self.projected.ref

        def prepare(rows):
            c, n = self.angles(rows)
            q = head_norm(proj[rows, :q_cols], self.gain.ref[0:1, :], size)
            q = (q * c + turn(q, size, False) * n).astype(BF)
            k = head_norm(proj[rows, q_cols : q_cols + k_cols], self.gain.ref[1:2, :k_cols], size)
            k = (k * c[:, :k_cols] + turn(k, size, False) * n[:, :k_cols]).astype(BF)
            self.q_rot.ref[rows, :] = q
            self.k_rot.ref[rows, :] = k
            self.split(self.q_h, rows, (q.astype(F32) * size**-0.5).astype(BF))
            self.split(self.k_h, rows, k)
            self.split(self.v_h, rows, proj[rows, q_cols + k_cols :].astype(BF))

        self.blocks(prepare)

        def head(h, carry):
            g = h // self.share
            for i in range(self.length // ROW_BLOCK):
                rows, seen = pl.ds(i * ROW_BLOCK, ROW_BLOCK), key_blocks(i)
                weights = block_weights(
                    self.q_h.ref[h, rows, :], [self.k_h.ref[g, at, :] for at in seen]
                )
                value = sum(
                    contract(part.astype(BF), self.v_h.ref[g, at, :], 1, 0)
                    for part, at in zip(weights, seen)
                )
                self.y_h.ref[h, rows, :] = value.astype(BF)
            return carry

        lax.fori_loop(0, self.heads // 2, head, 0)
        for step in between:
            step()
        lax.fori_loop(self.heads // 2, self.heads, head, 0)
        self.y.ref[...] = self.join(self.y_h, slice(None))


class AttendBack(Heads):
    def __init__(self, k, projected, tables, size, q_rot, k_rot, d_y):
        super().__init__(projected, tables, size)
        self.q_rot, self.k_rot, self.d_y = q_rot, k_rot, d_y
        self.q_h, self.dy_h = (self.per_head(k, self.heads, BF) for _ in range(2))
        self.k_h, self.v_h = (self.per_head(k, self.kv_heads, BF) for _ in range(2))
        self.dq_h = self.per_head(k, self.heads, F32)
        self.dk_h, self.dv_h = (self.per_head(k, self.kv_heads, F32) for _ in range(2))
        self.d_proj = k.vmem(projected.shape, BF)
        self.q_gain, self.k_gain = k.vmem((1, self.q_cols), F32), k.vmem((1, self.k_cols), F32)

    def run(self, *between):
        for load in self.loads:
            load.wait()
        size, q_cols, k_cols, proj = self.size, self.q_cols, self.k_cols, self.projected.ref
        scale = size**-0.5
        dq_h, dk_h, dv_h = self.dq_h.ref, self.dk_h.ref, self.dv_h.ref

        def prepare(rows):
            self.split(self.q_h, rows, (self.q_rot.ref[rows, :].astype(F32) * scale).astype(BF))
            self.split(self.dy_h, rows, self.d_y.ref[rows, :].astype(BF))
            self.split(self.k_h, rows, self.k_rot.ref[rows, :])
            self.split(self.v_h, rows, proj[rows, q_cols + k_cols :].astype(BF))

        self.blocks(prepare)
        dk_h[...] = jnp.zeros_like(dk_h)
        dv_h[...] = jnp.zeros_like(dv_h)

        def head(h, carry):
            g = h // self.share
            for i in range(self.length // ROW_BLOCK):
                rows, seen = pl.ds(i * ROW_BLOCK, ROW_BLOCK), key_blocks(i)
                q, low = self.q_h.ref[h, rows, :], self.dy_h.ref[h, rows, :]
                keys = [self.k_h.ref[g, at, :] for at in seen]
                probs = block_weights(q, keys)
                d_weights = [contract(low, self.v_h.ref[g, at, :], 1, 1) for at in seen]
                inner = sum(
                    jnp.sum(a * b, axis=1, keepdims=True) for a, b in zip(probs, d_weights)
                )
                d_q = 0.0
                for at, k, prob, d_weight in zip(seen, keys, probs, d_weights):
                    dv_h[g, at, :] += contract(prob.astype(BF), low, 0, 0)
                    d_scores = (prob * (d_weight - inner)).astype(BF)
                    d_q = d_q + contract(d_scores, k, 1, 0)
                    dk_h[g, at, :] += contract(d_scores, q, 0, 0)
                dq_h[h, rows, :] = d_q * scale
            return carry

        lax.fori_loop(0, self.heads // 2, head, 0)
        for step in between:
            step()
        lax.fori_loop(self.heads // 2, self.heads, head, 0)
        self.q_gain.ref[...] = jnp.zeros_like(self.q_gain.ref)
        self.k_gain.ref[...] = jnp.zeros_like(self.k_gain.ref)

        def finish(rows):
            c, n = self.angles(rows)
            dq, dk, dv = (self.join(v, rows) for v in (self.dq_h, self.dk_h, self.dv_h))
            dq = dq * c + turn(dq * n, size, True)
            dk = dk * c[:, :k_cols] + turn(dk * n[:, :k_cols], size, True)
            dq, q_sum = head_norm_back(proj[rows, :q_cols], self.gain.ref[0:1, :], dq, size)
            dk, k_sum = head_norm_back(
                proj[rows, q_cols : q_cols + k_cols], self.gain.ref[1:2, :k_cols], dk, size
            )
            self.q_gain.ref[...] += q_sum
            self.k_gain.ref[...] += k_sum
            self.d_proj.ref[rows, :q_cols] = dq.astype(BF)
            self.d_proj.ref[rows, q_cols : q_cols + k_cols] = dk.astype(BF)
            self.d_proj.ref[rows, q_cols + k_cols :] = dv.astype(BF)

        self.blocks(finish)


def body(boundary, norm_gain, mix_in, mix_out, w_gate, w_up, w_down, conv_x, conv_kernel, qk_gain):
    first = lax.axis_index("section") == 0
    tensor_index = lax.axis_index("tensor")
    model_width = boundary.shape[3]
    channels = mix_out.shape[1]
    row_shape = boundary.shape[2:]
    length, size = 4 * row_shape[0], qk_gain.shape[1]

    seqs, own_gain = boundary[0], norm_gain[0]
    sh_in, sh_out, sh_gate, sh_up, sh_down = (v[0] for v in (mix_in, mix_out, w_gate, w_up, w_down))
    head_gain = jnp.tile(qk_gain, (1, channels // size))

    def gains_of(k, block, other, early=True):
        own, moved = k.input(own_gain), as_val(k, other)
        sources = lambda s, d, t: [(s == block, own.ref), (s == 1 - block, moved.ref)]
        return Load(k, sources, own.shape, F32, early)

    def start_rows(k, slot, other, early=True):
        own, moved = k.input(seqs), as_val(k, other)
        sources = lambda s, d, t: [(s == slot, own.ref.at[slot]), (s == 1 - slot, moved.ref)]
        return Load(k, sources, row_shape, BF, early)

    def wait(*items):
        return [item.wait for item in items]

    k = Kernel(0)
    t_seq = None
    seq_val = k.input(seqs)

    def seq_moves(s, d, t):
        return [([(None, seq_val.ref.at[1 - s])], t_seq.out.ref, {"section": 1 - s})], []

    t_in, t_out, t_up = (x_half(k, v) for v in (sh_in, sh_out, sh_up))
    gate_lo, gate_hi = (Part(sh_gate, i * (sh_gate.shape[0] // 2), sh_gate.shape[0] // 2) for i in range(2))
    down_lo, down_hi = (Part(sh_down, i * (sh_down.shape[0] // 2), sh_down.shape[0] // 2) for i in range(2))
    t_gate0a, t_gate0b = x_half(k, gate_lo, 0), x_move(k, gate_hi, 0)
    t_down0a, t_down0b = x_half(k, down_lo, 0), x_move(k, down_hi, 0)
    t_gate1, t_down1 = x_half(k, sh_gate, 1), x_move(k, sh_down, 1)
    t_seq = Task(k, row_shape, "section", seq_moves, 1)
    t_gain, z_cols = x_move(k, own_gain), z_gather(k, conv_x)
    z_in0, z_out0 = z_gather_half(k, sh_in, t_in.out, 0), z_gather_half(k, sh_out, t_out.out, 0)
    z_gate0a = z_gather_half(k, gate_lo, t_gate0a.out, 0)
    z_gate0b, x_gate0a = z_gather_whole(k, gate_hi, t_gate0b.out, 0), x_move(k, z_gate0a.out)
    z_up0 = z_gather_half(k, sh_up, t_up.out, 0)
    x_cols, x_in0, x_out0 = (x_move(k, v.out) for v in (z_cols, z_in0, z_out0))
    x_load, gain_load = start_rows(k, 0, t_seq.out, False), gains_of(k, 0, t_gain.out, False)
    taps = load_all(k, conv_kernel)
    angles = Angles(k, length, size, 128)
    w_in0, w_cols = Weight(k, "rows", (z_in0.out, x_in0.out)), Weight(k, "conv", (z_cols.out, x_cols.out))
    w_out0 = Weight(k, "cols", (z_out0.out, x_out0.out))
    g0 = Gather(k, x_load.buf, (gain_load.buf, 0), [w_in0, w_cols], save=(0, 1, 2))
    conv = Conv(k, g0.values[0], g0.values[1], taps.buf)
    y0 = Save(k, conv.y)
    s1 = Scatter(k, [conv.y], [w_out0], x_load.buf)
    mid0 = Save(k, s1.out)
    k.do(t_in.send, t_out.send, z_cols.send, t_gate0b.send, t_gate0a.send, t_gate1.send)
    k.do(t_gain.send, t_seq.send)
    k.do(t_in.wait, z_in0.send, t_out.wait, z_out0.send, z_cols.step, z_in0.step, z_out0.step)
    k.do(z_cols.step, z_in0.step, z_out0.step, t_gate0b.wait, z_gate0b.send)
    k.do(t_gate0a.wait, z_gate0a.send)
    k.do(z_cols.wait, x_cols.send, z_in0.wait, x_in0.send, z_out0.wait, x_out0.send, t_up.send)
    k.do(t_gain.wait, gain_load.start, t_seq.wait, x_load.start, gain_load.wait, x_load.wait)
    k.do(g0.begin, z_gate0b.step, z_gate0a.step, angles.run, z_gate0b.step, z_gate0a.step)
    k.do(x_cols.wait, w_cols.start, x_in0.wait, w_in0.start, z_gate0a.wait, x_gate0a.send)
    k.do(t_down0b.send, t_down0a.send, t_down1.send, t_up.wait, z_up0.send)
    k.do(g0.loop, z_up0.step, taps.wait, conv.run, y0.start)
    k.do(x_out0.wait, w_out0.start, s1.loop, z_up0.step, s1.finish, mid0.start)
    k.do(*wait(t_gate1, t_down0a, t_down0b, t_down1, z_gate0b, x_gate0a, z_up0))
    k.build()
    a0, proj0, value0 = (out for _, out, _ in g0.saved)
    table_arrays = [head_gain] + [v.out for v in angles.saves]
    y0, mid0 = y0.out, mid0.out

    k = Kernel(1)
    x_up0, z_gate1 = x_move(k, z_up0.out), z_gather_half(k, sh_gate, t_gate1.out, 1)
    z_down0a = z_gather_half(k, down_lo, t_down0a.out, 0)
    z_down0b = z_gather_whole(k, down_hi, t_down0b.out, 0)
    z_in1, z_out1 = z_gather_half(k, sh_in, t_in.out, 1), z_gather_half(k, sh_out, t_out.out, 1)
    x_down0a, x_in1, x_out1 = (x_move(k, v.out) for v in (z_down0a, z_in1, z_out1))
    rows, gain_load = load_all(k, mid0), gains_of(k, 0, t_gain.out)
    w_gate0 = Weight(k, "rows", (z_gate0a.out, x_gate0a.out), (z_gate0b.out, None), early=True)
    w_up0 = Weight(k, "rows", (z_up0.out, x_up0.out))
    w_down0 = Weight(k, "cols", (z_down0a.out, x_down0a.out), (z_down0b.out, None))
    g2 = Gather(
        k, rows.buf, (gain_load.buf, 1), [w_gate0, w_up0], epilogue="ffn", save=(0, 1, 2, 3)
    )
    s3 = Scatter(k, [g2.values[2]], [w_down0], rows.buf, low=True)
    z_rows = Save(k, s3.out)
    k.do(x_up0.send, z_down0a.send, z_down0b.send, rows.wait, gain_load.wait, g2.begin)
    k.do(z_in1.send, z_out1.send, z_down0a.step, z_in1.step, z_out1.step, z_down0b.step)
    k.do(z_down0a.step, z_in1.step, z_out1.step, z_gate1.send, z_down0a.wait, x_down0a.send)
    k.do(x_up0.wait, w_up0.start, z_down0b.step, g2.loop, z_gate1.step)
    k.do(z_in1.wait, x_in1.send, z_out1.wait, x_out1.send, z_down0b.wait, x_down0a.wait)
    k.do(w_down0.start, s3.loop, z_gate1.step, s3.finish, z_rows.start)
    k.do(*wait(x_in1, x_out1, z_gate1))
    k.build()
    m0, gate0, up0, hid0 = (out for _, out, _ in g2.saved)
    z_rows = z_rows.out

    k = Kernel(2)
    x_gate1, z_up1 = x_move(k, z_gate1.out), z_gather_half(k, sh_up, t_up.out, 1)
    z_down1a, z_down1b = (z_gather_whole(k, sh_down, t_down1.out, 1, i) for i in range(2))
    x_up1 = x_move(k, z_up1.out)
    rows, gain_load = load_all(k, z_rows), gains_of(k, 1, t_gain.out)
    tables = [load_all(k, v) for v in table_arrays]
    w_in1 = Weight(k, "rows", (z_in1.out, x_in1.out), early=True)
    w_out1 = Weight(k, "cols", (z_out1.out, x_out1.out), early=True)
    g4 = Gather(k, rows.buf, (gain_load.buf, 0), [w_in1], save=(0, 1))
    attend = Attend(k, g4.values[0], tables, size)
    kept = [Save(k, v) for v in (attend.q_rot, attend.k_rot, attend.y)]
    s5 = Scatter(k, [attend.y], [w_out1], rows.buf)
    mid1 = Save(k, s5.out)
    k.do(x_gate1.send, z_up1.send, rows.wait, gain_load.wait, g4.begin, z_up1.step)
    k.do(z_down1a.send, g4.loop, z_up1.step, z_down1b.send)
    k.do(lambda: attend.run(z_up1.wait, x_up1.send, z_down1a.step))
    k.do(*(v.start for v in kept))
    k.do(z_down1b.step, s5.loop, z_down1a.step, z_down1b.step, s5.finish, mid1.start)
    k.do(*wait(x_gate1, x_up1, z_down1a, z_down1b))
    k.build()
    a1, proj1 = (out for _, out, _ in g4.saved)
    q_rot, k_rot, y1 = (v.out for v in kept)
    mid1 = mid1.out

    k = Kernel(3)
    rows, gain_load = load_all(k, mid1), gains_of(k, 1, t_gain.out)
    cot = start_rows(k, 1, t_seq.out)
    w_gate1 = Weight(k, "rows", (z_gate1.out, x_gate1.out), early=True)
    w_up1 = Weight(k, "rows", (z_up1.out, x_up1.out), early=True)
    w_down1 = Weight(k, "cols", (z_down1a.out, None), (z_down1b.out, None), early=True)
    g6 = Gather(k, rows.buf, (gain_load.buf, 1), [w_gate1, w_up1], epilogue="ffn")
    g8 = Gather(
        k, cot.buf, None, [w_down1], [g6.values[0], g6.values[1]], trans=True, epilogue="ffn_back"
    )
    p_down1 = Product(k, g6.values[2], g8.full)
    p_gate1, p_up1 = Product(k, g6.full, g8.values[0]), Product(k, g6.full, g8.values[1])
    s7 = Scatter(k, [g6.values[2]], [w_down1], rows.buf, low=True)
    s9 = Scatter(k, g8.values, [w_gate1, w_up1], cot.buf, (rows.buf, (gain_load.buf, 1)), True)
    y_rows, d_mid1, gain11 = Save(k, s7.out), Save(k, s9.out), Save(k, s9.gain_grad)
    k.do(rows.wait, gain_load.wait, g6.begin, cot.wait, g8.begin, g6.loop, s7.loop, g8.loop)
    k.do(s9.loop, p_down1.run, s7.finish, y_rows.start, p_gate1.run, p_up1.run)
    k.do(s9.finish, d_mid1.start, gain11.start, p_down1.wait, p_gate1.wait, p_up1.wait)
    k.build()
    y_rows, d_mid1, gain11 = y_rows.out, d_mid1.out, gain11.out

    k = Kernel(4)
    r_down1 = x_half(k, p_down1.out)
    r_gate1, q_up1 = x_slots(k, p_gate1.out, "rows"), sum_scatter(k, "rows", p_up1.out)
    rows, gain_load = load_all(k, d_mid1), gains_of(k, 1, t_gain.out)
    value = load_all(k, z_rows)
    tables = [load_all(k, v) for v in table_arrays]
    proj, q_load, k_load, y_load, a_load = (load_all(k, v) for v in (proj1, q_rot, k_rot, y1, a1))
    w_in1 = Weight(k, "rows", (z_in1.out, x_in1.out), early=True)
    w_out1 = Weight(k, "cols", (z_out1.out, x_out1.out), early=True)
    g10 = Gather(k, rows.buf, None, [w_out1], trans=True)
    p_out1 = Product(k, y_load.buf, g10.full)
    back = AttendBack(k, proj.buf, tables, size, q_load.buf, k_load.buf, g10.values[0])
    p_in1 = Product(k, a_load.buf, back.d_proj)
    r_out1 = x_half(k, p_out1.out)
    s11 = Scatter(
        k, [back.d_proj], [w_in1], rows.buf, (value.buf, (gain_load.buf, 0)), True, low=True
    )
    d_z, gain10 = Save(k, s11.out), Save(k, s11.gain_grad)
    head_gains = [Save(k, back.q_gain), Save(k, back.k_gain)]
    k.early.append(q_up1.load)
    k.do(r_down1.send, r_gate1.send, rows.wait, g10.begin, q_up1.send, g10.loop)
    k.do(y_load.wait, p_out1.run, q_up1.step, p_out1.wait, r_out1.send)
    k.do(proj.wait, q_load.wait, k_load.wait, lambda: back.run(q_up1.step))
    k.do(*(v.start for v in head_gains))
    k.do(gain_load.wait, value.wait, s11.loop, a_load.wait, p_in1.run)
    k.do(s11.finish, d_z.start, gain10.start, p_in1.wait)
    k.do(*wait(r_down1, q_up1, r_gate1, r_out1))
    k.build()
    d_z, gain10 = d_z.out, gain10.out
    q_gain, k_gain = (v.out for v in head_gains)

    k = Kernel(5)
    q_gate1, m_up1 = sum_scatter(k, "rows", p_gate1.out, r_gate1.out), x_move(k, q_up1.out, 0)
    q_out1 = sum_scatter(k, "cols", p_out1.out, r_out1.out)
    r_in1 = x_slots(k, p_in1.out, "rows")
    q_in1 = sum_scatter(k, "rows", p_in1.out, r_in1.out)
    q_down1 = sum_scatter(k, "cols", p_down1.out, r_down1.out)
    rows, value, gain_load = load_all(k, d_z), load_all(k, mid0), gains_of(k, 0, t_gain.out)
    gate_load, up_load, hid_load, m_load = (load_all(k, v) for v in (gate0, up0, hid0, m0))
    w_gate0 = Weight(k, "rows", (z_gate0a.out, x_gate0a.out), (z_gate0b.out, None), early=True)
    w_up0 = Weight(k, "rows", (z_up0.out, x_up0.out), early=True)
    w_down0 = Weight(k, "cols", (z_down0a.out, x_down0a.out), (z_down0b.out, None), early=True)
    g12 = Gather(
        k, rows.buf, None, [w_down0], [gate_load.buf, up_load.buf], trans=True, epilogue="ffn_back"
    )
    p_down0 = Product(k, hid_load.buf, g12.full)
    p_gate0, p_up0 = Product(k, m_load.buf, g12.values[0]), Product(k, m_load.buf, g12.values[1])
    r_down0 = x_half(k, p_down0.out)
    s13 = Scatter(
        k, g12.values, [w_gate0, w_up0], rows.buf, (value.buf, (gain_load.buf, 1)), True
    )
    d_mid0, gain01 = Save(k, s13.out), Save(k, s13.gain_grad)
    k.early += [q_gate1.load, q_down1.load, q_out1.load]
    k.do(r_in1.send, m_up1.send, rows.wait, g12.begin, q_gate1.send, q_down1.send, q_out1.send)
    k.do(gate_load.wait, up_load.wait, g12.loop, q_gate1.step, q_down1.step, q_out1.step)
    k.do(hid_load.wait, p_down0.run, p_down0.wait, r_down0.send, r_in1.wait, q_in1.add)
    k.do(s13.loop, q_gate1.step, q_down1.step, q_out1.step)
    k.do(m_load.wait, p_gate0.run, q_in1.step, p_up0.run, value.wait, gain_load.wait)
    k.do(s13.finish, d_mid0.start, gain01.start, q_in1.step, p_gate0.wait, p_up0.wait)
    k.do(*wait(q_gate1, q_out1, q_in1, q_down1, m_up1, r_down0))
    k.build()
    d_mid0, gain01 = d_mid0.out, gain01.out

    k = Kernel(6)
    r_gate0 = x_slots(k, p_gate0.out, "rows")
    q_gate0 = sum_scatter(k, "rows", p_gate0.out, r_gate0.out)
    q_down0 = sum_scatter(k, "cols", p_down0.out, r_down0.out)
    q_up0 = sum_scatter(k, "rows", p_up0.out)
    m_up0 = x_move(k, q_up0.out, 1)
    e_down1 = Finish(k, q_down1.out, 1)
    e_gate1, e_out1, e_in1 = (Finish(k, v.out, 1) for v in (q_gate1, q_out1, q_in1))
    rows, gain_load = load_all(k, d_mid0), gains_of(k, 0, t_gain.out)
    x_load, taps = start_rows(k, 0, t_seq.out), load_all(k, conv_kernel)
    y_load, a_load, proj, value = (load_all(k, v) for v in (y0, a0, proj0, value0))
    w_in0 = Weight(k, "rows", (z_in0.out, x_in0.out), early=True)
    w_cols = Weight(k, "conv", (z_cols.out, x_cols.out), early=True)
    w_out0 = Weight(k, "cols", (z_out0.out, x_out0.out), early=True)
    g14 = Gather(k, rows.buf, None, [w_out0], trans=True)
    p_out0 = Product(k, y_load.buf, g14.full)
    back = ConvBack(k, proj.buf, value.buf, taps.buf, g14.values[0])
    p_in0, p_cols = Product(k, a_load.buf, back.d_proj), Product(k, a_load.buf, back.d_value)
    r_out0, r_in0 = x_half(k, p_out0.out), x_slots(k, p_in0.out, "rows")
    r_cols = x_slots(k, p_cols.out, "conv")
    q_out0, q_in0 = sum_scatter(k, "cols", p_out0.out, r_out0.out), sum_scatter(k, "rows", p_in0.out, r_in0.out)
    q_cols = sum_scatter(k, "conv", p_cols.out, r_cols.out)
    e_down0, e_gate0, e_out0, e_in0 = (
        Finish(k, v.out, 0) for v in (q_down0, q_gate0, q_out0, q_in0)
    )
    s15 = Scatter(
        k, [back.d_proj, back.d_value], [w_in0, w_cols], rows.buf,
        (x_load.buf, (gain_load.buf, 0)), True, low=True,
    )
    d_x = Save(k, s15.out)
    tap_rows = conv_kernel.shape[0]
    small = k.vmem((8, model_width), F32)
    small_out = Save(k, small)
    ready = [load_all(k, v) for v in (gain01, gain10, gain11)]
    head_loads = [load_all(k, v) for v in (q_gain, k_gain)]

    def fill_small():
        t = lax.axis_index("tensor")
        small.ref[...] = jnp.zeros_like(small.ref)
        small.ref[0:1, :] = s15.gain_grad.ref[...]
        for i, load in enumerate(ready):
            load.wait()
            small.ref[i + 1 : i + 2, :] = load.buf.ref[...]
        small.ref[4 : 4 + tap_rows, block_of(t, channels)] = back.d_kernel.ref[...]
        at = 0
        for load in head_loads:
            load.wait()
            width = load.buf.shape[1]
            small.ref[7:8, at : at + width] = load.buf.ref[...]
            at += width
        small_out.start()

    t_small = x_move(k, small_out.out)
    z_small = SumShare(k, [small_out.out, t_small.out], "dp")
    t_total = SumShare(k, [z_small.out], "tensor", slotted=True)
    y_val, dx_val = k.input(y_rows), d_x.out

    def result_moves(s, d, t):
        sources = [(s == 0, y_val.ref), (s == 1, dx_val.ref)]
        return [(sources, t_result.out.ref, {"section": 1 - s})], []

    t_result = Task(k, row_shape, "section", result_moves, 1)
    k.early += [q_up0.load, q_down0.load]
    k.early += [v.load for v in (e_down1, e_gate1, e_out1, e_in1)]
    k.do(r_gate0.send, rows.wait, g14.begin, q_up0.send, q_down0.send)
    k.do(e_down1.send, e_gate1.send, e_out1.send, e_in1.send, g14.loop)
    k.do(y_load.wait, p_out0.run, p_out0.wait, r_out0.send, q_up0.step)
    k.do(proj.wait, value.wait, taps.wait, back.run, q_down0.step, a_load.wait)
    k.do(p_in0.run, p_cols.run, p_in0.wait, r_in0.send, p_cols.wait, r_cols.send)
    k.do(r_gate0.wait, q_gate0.add, x_load.wait, gain_load.wait, s15.loop, q_up0.step)
    k.do(q_down0.step, s15.finish, d_x.start, fill_small, d_x.wait, t_result.send)
    k.do(small_out.wait, t_small.send, q_gate0.step, r_out0.wait, q_out0.add, r_in0.wait, q_in0.add)
    k.do(r_cols.wait, q_cols.add, q_up0.wait, m_up0.send, q_down0.wait, e_down0.add)
    k.do(q_gate0.step, q_out0.step, q_in0.step, q_cols.step, t_small.wait, z_small.add)
    k.do(q_gate0.wait, e_gate0.add, q_out0.step, q_in0.step, q_cols.step)
    k.do(z_small.wait, t_total.add, q_out0.wait, e_out0.add, q_in0.wait, e_in0.add)
    rest = (e_down1, e_gate1, e_out1, e_in1, q_cols, e_down0, e_gate0, m_up0, e_out0, e_in0)
    k.do(*wait(*rest, t_total, t_result))
    k.build()

    owned = [
        ([e_in0], [e_in1], 1),
        ([e_out0], [e_out1], 1),
        ([e_gate0], [e_gate1], 1),
        ([q_up0, m_up0], [q_up1, m_up1], 1),
        ([e_down0], [e_down1], 1),
        ([q_cols], [q_cols], 0),
    ]
    return pack(
        [(zero, one, lead) for zero, one, lead in owned], t_total, d_x.out, y_rows, t_result,
        (norm_gain.shape, conv_kernel.shape, qk_gain.shape),
    )


def slot_free(val, shape):
    value = val.out.array
    if value.ndim == 3 and value.shape[0] * value.shape[1] != shape[0]:
        value = jnp.sum(value.astype(F32), axis=0).astype(BF)
    return value.reshape(shape)


def pack_kernel(plan, *refs):
    n_in, leads, terms, tap_rows = plan
    ins, rest = refs[:n_in], refs[n_in:]
    result, gain_out, *grads, cols, taps, heads = rest[: len(leads) + 4]
    grads = [*grads, cols]
    room = iter(rest[len(leads) + 4 :])
    own_v, moved_v, small_v, *bufs = (next(room) for _ in range(3 + len(terms)))
    out_v = [next(room) for _ in leads]
    load_sem, store_sem = room
    s, t = lax.axis_index("section"), lax.axis_index("tensor")
    small, d_x, y_rows, moved, *parts = ins

    def either(cond, zero, one, dst, sem):
        if zero is not None:
            pl.when(cond)(pltpu.make_async_copy(zero, dst, sem).start)
        if one is not None:
            pl.when(jnp.logical_not(cond))(pltpu.make_async_copy(one, dst, sem).start)

    first = s == 0
    either(first, d_x, y_rows, own_v, load_sem.at[0])
    pltpu.make_async_copy(moved, moved_v, load_sem.at[1]).start()
    pltpu.make_async_copy(small, small_v, load_sem.at[2]).start()
    for j, (zero, one, _) in enumerate(terms):
        either(
            first,
            None if zero is None else parts[zero],
            None if one is None else parts[one],
            bufs[j],
            load_sem.at[3 + j],
        )
    for j, (zero, one, i) in enumerate(terms):
        arrive = pltpu.make_async_copy(parts[one if zero is None else zero], bufs[j], load_sem.at[3 + j])
        begins = j == 0 or terms[j - 1][2] != i

        def put(j=j, i=i, begins=begins):
            value = bufs[j][...].astype(F32)
            value = value if begins else out_v[i][...] + value
            out_v[i][...] = value

        if zero is None or one is None:
            cond = first if one is None else jnp.logical_not(first)

            @pl.when(cond)
            def _(arrive=arrive, put=put):
                arrive.wait()
                put()
        else:
            arrive.wait()
            put()
        if j + 1 == len(terms) or terms[j + 1][2] != i:
            dst = grads[i].at[0] if leads[i] else grads[i]
            pltpu.make_async_copy(out_v[i], dst, store_sem.at[i]).start()
    pltpu.make_async_copy(d_x, own_v, load_sem.at[0]).wait()
    pltpu.make_async_copy(moved, moved_v, load_sem.at[1]).wait()
    n = len(leads)
    stores = [
        pltpu.make_async_copy(own_v, result.at[0, s], store_sem.at[n]),
        pltpu.make_async_copy(moved_v, result.at[0, 1 - s], store_sem.at[n + 1]),
    ]
    for store in stores:
        store.start()
    pltpu.make_async_copy(small, small_v, load_sem.at[2]).wait()
    total = small_v[0]
    for i in range(1, small_v.shape[0]):
        total = total + small_v[i]
    gain_out[0] = jnp.where(first, total[0:2], total[2:4])
    channels, size = taps.shape[1], heads.shape[1]
    chosen = total[4 : 4 + tap_rows, 0:channels]
    for i in range(1, total.shape[1] // channels):
        chosen = jnp.where(t == i, total[4 : 4 + tap_rows, i * channels : (i + 1) * channels], chosen)
    taps[...] = chosen
    at = 0
    for row, width in enumerate((channels, channels // 2)):
        value = total[7:8, at : at + size]
        for i in range(1, width // size):
            value = value + total[7:8, at + i * size : at + (i + 1) * size]
        heads[row : row + 1, :] = value
        at += width
    for i, store in enumerate(leads):
        dst = grads[i].at[0] if store else grads[i]
        pltpu.make_async_copy(out_v[i], dst, store_sem.at[i]).wait()
    for store in stores:
        store.wait()


def pack(owned, small, d_x, y_rows, moved, shapes):
    gain_shape, tap_shape, head_shape = shapes
    parts, terms, leads, out_shapes = [], [], [], []
    for i, (zero, one, lead) in enumerate(owned):
        whole = zero[0].out.shape
        if lead and len(whole) == 3 and isinstance(zero[0], Finish):
            shape = (whole[0] * whole[1], whole[2])
        else:
            shape = whole[-2:]
        shape = tuple(shape)
        leads.append(lead)
        out_shapes.append(shape)
        for j in range(max(len(zero), len(one))):
            pair = []
            for side in (zero, one):
                if j < len(side):
                    parts.append(slot_free(side[j], shape))
                    pair.append(len(parts) - 1)
                else:
                    pair.append(None)
            terms.append((*pair, i))
    operands = [small.out.array, d_x.array, y_rows.array, moved.out.array, *parts]
    rows = d_x.shape
    smem = pl.BlockSpec(memory_space=pltpu.VMEM)
    out_shape = [jax.ShapeDtypeStruct((1, 2) + rows, BF), jax.ShapeDtypeStruct(gain_shape, F32)]
    out_shape += [
        jax.ShapeDtypeStruct((1,) + v if lead else v, F32) for v, lead in zip(out_shapes, leads)
    ]
    out_shape += [jax.ShapeDtypeStruct(v, F32) for v in (tap_shape, head_shape)]
    n = len(leads)
    return tuple(
        pl.pallas_call(
            functools.partial(
                pack_kernel, (len(operands), tuple(leads), tuple(terms), tap_shape[0])
            ),
            out_shape=out_shape,
            in_specs=[ANY] * len(operands),
            out_specs=[ANY, smem] + [ANY] * n + [smem] * 2,
            scratch_shapes=[pltpu.VMEM(rows, BF)] * 2
            + [pltpu.VMEM(small.out.shape, F32)]
            + [pltpu.VMEM(out_shapes[i], BF) for _, _, i in terms]
            + [pltpu.VMEM(v, F32) for v in out_shapes]
            + [DMA((3 + len(terms),)), DMA((n + 2,))],
            compiler_params=pltpu.CompilerParams(vmem_limit_bytes=VMEM_BYTES),
            name="pack",
        )(*operands)
    )


def solution(mesh):
    in_specs = (
        P("section", "dp", "tensor", None),
        P("section", None, None),
        P("section", "dp", "tensor"),
        P("section", "tensor", "dp"),
        P("section", "dp", "tensor"),
        P("section", "dp", "tensor"),
        P("section", "tensor", "dp"),
        P(("section", "dp"), "tensor"),
        P(None, "tensor"),
        P(),
    )
    out_specs = (
        P("section", "dp", "tensor", None),
        P("section", None, None),
        P("section", "dp", "tensor"),
        P("section", "tensor", "dp"),
        P("section", "dp", "tensor"),
        P("section", "dp", "tensor"),
        P("section", "tensor", "dp"),
        P(("section", "dp"), "tensor"),
        P(None, "tensor"),
        P(),
    )
    return jax.shard_map(body, mesh=mesh, in_specs=in_specs, out_specs=out_specs, check_vma=False)
```

```python
import functools

import jax
import jax.numpy as jnp
from jax import lax
from jax.experimental import pallas as pl
from jax.experimental.pallas import tpu as pltpu
from jax.sharding import PartitionSpec as P

HEADS = 16
KV_HEADS = 8

EPS = 1e-05
ROPE_BASE = 1000000.0
MASKED = -1e30

MESH = pl.DeviceIdType.MESH
ANY = pl.BlockSpec(memory_space=pl.ANY)
DMA = pltpu.SemaphoreType.DMA
VMEM_BYTES = 63 * 1024 * 1024
BF = jnp.bfloat16
F32 = jnp.float32
ROW_BLOCK = 256


def contract(left_op, right_op, left_dim, right_dim):
    return lax.dot_general(
        left_op, right_op, (((left_dim,), (right_dim,)), ((), ())), preferred_element_type=F32
    )


def norm_rows(values, gain):
    return values * lax.rsqrt(jnp.mean(values * values, axis=-1, keepdims=True) + EPS) * gain


def norm_back(values, gain, grad_in):
    row_scale = lax.rsqrt(jnp.mean(values * values, axis=-1, keepdims=True) + EPS)
    normed = values * row_scale
    gain_grad = jnp.sum(grad_in * normed, axis=0, keepdims=True)
    scaled = grad_in * gain
    value_grad = row_scale * (scaled - normed * jnp.mean(scaled * normed, axis=-1, keepdims=True))
    return (value_grad, gain_grad)


class Angles:
    def __init__(self, k, length, head_size, width):
        self.half = head_size // 2
        self.tables = [k.vmem((length, width), F32) for _ in range(2)]
        self.saves = [Save(k, v) for v in self.tables]

    def run(self):
        cos, sin = self.tables
        shape = (ROW_BLOCK, cos.shape[1])
        column = (lax.broadcasted_iota(jnp.int32, shape, 1) % self.half).astype(F32)
        frequency = ROPE_BASE ** (-(column / self.half))
        row = lax.broadcasted_iota(jnp.int32, shape, 0)

        def step(i, carry):
            rows = block_of(i, ROW_BLOCK)
            angle = (row + i * ROW_BLOCK).astype(F32) * frequency
            cos.ref[rows, :] = jnp.cos(angle)
            sin.ref[rows, :] = jnp.sin(angle)
            return carry

        lax.fori_loop(0, cos.shape[0] // ROW_BLOCK, step, 0)
        for save in self.saves:
            save.start()


def silu_parts(gate):
    sig = 1.0 / (1.0 + jnp.exp(-gate))
    return sig, gate * sig


def dp_size():
    return lax.axis_size("dp")


def spot():
    return tuple(lax.axis_index(a) for a in ("section", "dp", "tensor"))


def block_of(index, size):
    return pl.ds(pl.multiple_of(index * size, size), size)


class Val:
    def __init__(self, shape, dtype):
        self.shape, self.dtype = tuple(shape), dtype
        self.ref = self.array = None


class Kernel:
    def __init__(self, cid):
        self.cid, self.ins, self.arrays, self.outs, self.room = cid, [], [], [], []
        self.early, self.steps, self.late, self.axes = [], [], [], set()
        self.once = []

    def input(self, array):
        array = array.array if isinstance(array, Val) else array
        for val, known in zip(self.ins, self.arrays):
            if known is array:
                return val
        val = Val(array.shape, array.dtype)
        self.ins.append(val)
        self.arrays.append(array)
        return val

    def output(self, shape, dtype):
        val = Val(shape, dtype)
        self.outs.append(val)
        return val

    def vmem(self, shape, dtype):
        val = Val(shape, dtype)
        self.room.append((val, pltpu.VMEM(tuple(shape), dtype)))
        return val

    def sem(self, *shape):
        val = Val(shape, None)
        self.room.append((val, DMA(shape)))
        return val

    def do(self, *steps):
        self.steps += steps

    def body(self, *refs):
        vals = self.ins + self.outs + [val for val, _ in self.room]
        for val, ref in zip(vals, refs):
            val.ref = ref
        for item in self.once:
            item.waited = False
            item.phase = 0
        for step in self.early:
            step()
        self.greet()
        for step in self.steps + self.late:
            step()

    def greet(self):
        s, d, t = spot()
        _, sib, cross, diag = places()
        barrier = pltpu.get_barrier_semaphore()
        peers = [{"tensor": sib}, {"tensor": cross}]
        if "tensor" in self.axes:
            peers.append({"tensor": diag})
        if "section" in self.axes:
            peers.append({"section": 1 - s})
        if "dp" in self.axes:
            peers += [{"dp": (d + i) % dp_size()} for i in range(1, dp_size())]

        def signal(peer):
            pl.semaphore_signal(barrier, inc=1, device_id=peer, device_id_type=MESH)

        for peer in peers:
            signal(peer)
        expected = len(peers)
        if "line" in self.axes and "dp" not in self.axes:
            pl.when(d < 3)(lambda: signal({"dp": (d + 1) % 4}))
            pl.when(d > 0)(lambda: signal({"dp": (d + 3) % 4}))
            expected = expected + (d + 2) // 3 + (5 - d) // 3
        pl.semaphore_wait(barrier, expected)

    def build(self):
        result = pl.pallas_call(
            self.body,
            out_shape=[jax.ShapeDtypeStruct(v.shape, v.dtype) for v in self.outs],
            in_specs=[ANY] * len(self.ins),
            out_specs=[ANY] * len(self.outs),
            scratch_shapes=[room for _, room in self.room],
            compiler_params=pltpu.CompilerParams(
                collective_id=self.cid, has_side_effects=True, vmem_limit_bytes=VMEM_BYTES
            ),
            name=f"stage{self.cid}",
        )(*self.arrays)
        for val, array in zip(self.outs, result):
            val.array = array


def remote(src, dst, send_sem, recv_sem, peer):
    return pltpu.make_async_remote_copy(
        src_ref=src, dst_ref=dst, send_sem=send_sem, recv_sem=recv_sem,
        device_id=peer, device_id_type=MESH,
    )


class Load:
    def __init__(self, k, sources, shape, dtype, early=False):
        self.k, self.sources, self.waited = k, sources, False
        self.buf, self.sem = k.vmem(shape, dtype), k.sem(1)
        k.once.append(self)
        if early:
            k.early.append(self.start)

    def moves(self):
        for cond, source in self.sources(*spot()):
            yield cond, pltpu.make_async_copy(source, self.buf.ref, self.sem.ref.at[0])

    def start(self):
        for cond, move in self.moves():
            if cond is None:
                move.start()
            else:
                pl.when(cond)(move.start)

    def wait(self):
        if not self.waited:
            self.waited = True
            next(self.moves())[1].wait()


def load_all(k, array, early=True):
    val = k.input(array)
    return Load(k, lambda s, d, t: [(None, val.ref)], val.shape, val.dtype, early)


class Save:
    def __init__(self, k, buf):
        self.buf, self.out, self.sem = buf, k.output(buf.shape, buf.dtype), k.sem(1)
        self.waited = False
        k.once.append(self)
        k.late.append(self.wait)

    def move(self):
        return pltpu.make_async_copy(self.buf.ref, self.out.ref, self.sem.ref.at[0])

    def start(self):
        self.move().start()

    def wait(self):
        if not self.waited:
            self.waited = True
            self.move().wait()


class Task:
    final = None

    def __init__(self, k, out, axis, moves, count, n_local=1, out_dtype=BF):
        self.k, self.axis, self.make = k, axis, moves
        self.out = k.output(out, out_dtype)
        self.send_sem, self.recv_sem, self.local_sem = k.sem(count), k.sem(count), k.sem(n_local)
        self.waited = False
        k.axes.add(axis)
        k.once.append(self)

    def local(self, src, dst, i):
        return pltpu.make_async_copy(src, dst, self.local_sem.ref.at[i])

    def pairs(self, every):
        far, near = self.make(*spot())
        for i, (sources, dst, peer) in enumerate(far):
            for cond, src in sources if every else sources[:1]:
                yield cond, True, remote(
                    src, dst, self.send_sem.ref.at[i], self.recv_sem.ref.at[i], peer
                )
        for i, (sources, dst) in enumerate(near):
            for cond, src in sources if every else sources[:1]:
                yield cond, False, self.local(src, dst, i)

    def step(self):
        pass

    def send(self):
        for cond, far, move in self.pairs(True):
            if far and self.final is not None:
                cond = lax.axis_index("section") == 1 - self.final
            if cond is None:
                move.start()
            else:
                pl.when(cond)(move.start)

    def wait(self):
        if self.waited:
            return
        self.waited = True
        s = lax.axis_index("section")
        for _, far, move in self.pairs(False):
            if not far:
                move.wait()
            elif self.final is None:
                move.wait_recv()
                move.wait_send()
            else:
                pl.when(s == 1 - self.final)(move.wait_send)
                pl.when(s == self.final)(move.wait_recv)


class Part:
    def __init__(self, base, start, rows):
        self.base, self.start, self.rows = base, start, rows
        self.shape, self.dtype = (rows,) + tuple(base.shape[1:]), base.dtype
        self.array = None

    @property
    def ref(self):
        return self.base.ref.at[pl.ds(self.start, self.rows)]


def as_val(k, value):
    if isinstance(value, Part):
        return Part(as_val(k, value.base), value.start, value.rows)
    value = value.out if isinstance(value, Task) else value
    known = isinstance(value, Val) and (value.array is None)
    return value if known else k.input(value)


class Line(Task):
    def __init__(self, k, out, out_dtype=BF, n_local=1):
        super().__init__(k, out, "line", None, 6, n_local, out_dtype)
        self.send_sem, self.recv_sem = k.sem(2, 3), k.sem(2, 3)
        self.phase = 0

    def hop(self, j, way, src, dst):
        d = lax.axis_index("dp")
        peer = {"dp": (d + 1 if way == 0 else d + 3) % 4}
        return remote(src, dst, self.send_sem.ref.at[way, j], self.recv_sem.ref.at[way, j], peer)


class LineGather(Line):
    def __init__(self, k, sources, shape, dtype):
        super().__init__(k, (4,) + shape, dtype)
        self.sources = sources

    def ends(self, j, way):
        d = lax.axis_index("dp")
        if way == 0:
            return (d >= j) & (d < 3), d >= j + 1
        return (d <= 3 - j) & (d > 0), d <= 2 - j

    def copy(self, j, way, src=None):
        d = lax.axis_index("dp")
        slot = (d + 4 - j if way == 0 else d + j) % 4
        piece = self.out.ref.at[slot]
        return self.hop(j, way, piece if src is None else src, piece)

    def send(self):
        self.phase = 0
        for cond, src in self.sources(*spot()):
            own = self.local(src, self.out.ref.at[lax.axis_index("dp")], 0)
            moves = [(True if cond is None else cond, own)]
            for way in range(2):
                sends = self.ends(0, way)[0]
                moves.append((sends if cond is None else sends & cond, self.copy(0, way, src)))
            for when, move in moves:
                if when is True:
                    move.start()
                else:
                    pl.when(when)(move.start)

    def arrive(self, j):
        for way in range(2):
            pl.when(self.ends(j, way)[1])(self.copy(j, way).wait_recv)

    def step(self):
        self.arrive(self.phase)
        self.phase += 1
        for way in range(2):
            pl.when(self.ends(self.phase, way)[0])(self.copy(self.phase, way).start)

    def wait(self):
        if self.waited:
            return
        self.waited = True
        while self.phase < 2:
            self.step()
        self.arrive(2)
        for j in range(3):
            for way in range(2):
                pl.when(self.ends(j, way)[0])(self.copy(j, way).wait_send)
        d = lax.axis_index("dp")
        self.local(self.sources(*spot())[0][1], self.out.ref.at[d], 0).wait()


def z_gather_from(k, sources, shape, dtype):
    count = dp_size()
    if count == 4:
        return LineGather(k, sources, shape, dtype)

    def moves(s, d, t):
        dst, found = task.out.ref.at[d], sources(s, d, t)
        return [(found, dst, {"dp": (d + i) % count}) for i in range(1, count)], [(found, dst)]

    task = Task(k, (count,) + shape, "dp", moves, count - 1, out_dtype=dtype)
    return task


def z_gather(k, value):
    val = as_val(k, value)
    return z_gather_from(k, lambda s, d, t: [(None, val.ref)], val.shape, val.dtype)


def z_gather_half(k, shard, moved, block):
    shard, moved = as_val(k, shard), as_val(k, moved)
    rows = shard.shape[0] // 2

    def sources(s, d, t):
        own = shard.ref.at[pl.ds(block * rows, rows)]
        return [(s == block, own), (s == 1 - block, moved.ref)]

    return z_gather_from(k, sources, moved.shape, shard.dtype)


def one_way(task, sender):
    task.final = None if sender is None else 1 - sender
    return task


def z_gather_whole(k, shard, moved, block, half=None):
    shard, moved = as_val(k, shard), as_val(k, moved)
    rows = shard.shape[0] if half is None else shard.shape[0] // 2
    part = pl.ds(0 if half is None else half * rows, rows)

    def sources(s, d, t):
        return [(s == block, shard.ref.at[part]), (s == 1 - block, moved.ref.at[part])]

    return z_gather_from(k, sources, (rows,) + shard.shape[1:], shard.dtype)


def x_move(k, value, sender=None):
    val = as_val(k, value)

    def moves(s, d, t):
        return [([(None, val.ref)], task.out.ref, {"section": 1 - s})], []

    task = Task(k, val.shape, "section", moves, 1, out_dtype=val.dtype)
    return one_way(task, sender)


def x_half(k, value, sender=None):
    val = as_val(k, value)
    rows = val.shape[0] // 2

    def moves(s, d, t):
        src = val.ref.at[block_of(1 - s, rows)]
        return [([(None, src)], task.out.ref, {"section": 1 - s})], []

    task = Task(k, (rows,) + val.shape[1:], "section", moves, 1, out_dtype=val.dtype)
    return one_way(task, sender)


def x_slots(k, value, kind):
    val, count = as_val(k, value), dp_size()
    rows = val.shape[0] // (2 * count)

    def moves(s, d, t):
        far = []
        for i in range(count):
            slot = 2 * i + 1 - s if kind == "rows" else (1 - s) * count + i
            src = val.ref.at[block_of(slot, rows)]
            far.append(([(None, src)], task.out.ref.at[i], {"section": 1 - s}))
        return far, []

    task = Task(k, (count, rows) + val.shape[1:], "section", moves, count)
    return task


class Terms:
    def __init__(self, k, kind, grads, received, local):
        self.grads, self.local = as_val(k, grads), local
        self.kind, self.n = kind, dp_size()
        self.whole = received is None
        if self.whole:
            rows, cols = self.grads.shape
            self.rows = rows if kind == "cols" else rows // self.n
            self.cols = cols // self.n if kind == "cols" else cols
            self.shape = (self.n, self.rows, self.cols)
            self.aside = kind == "cols" and self.cols % 128 != 0
            self.total = k.vmem(self.shape, BF)
            self.kept = k.vmem(self.grads.shape, BF) if self.aside else self.total
            return
        self.received = as_val(k, received)
        if kind == "cols":
            self.rows, self.cols = self.grads.shape[0] // 2, self.grads.shape[1] // self.n
            held = (self.rows, self.grads.shape[1])
        else:
            self.rows, self.cols = self.grads.shape[0] // (2 * self.n), self.grads.shape[1]
            held = (self.n, self.rows, self.cols)
        self.kept, self.got = k.vmem(held, BF), k.vmem(held, BF)
        self.shape = (self.n, self.rows, self.cols)
        self.total = k.vmem(self.shape, BF) if kind == "cols" else self.kept

    def loads(self):
        s, grads, kept = lax.axis_index("section"), self.grads.ref, self.kept.ref
        if self.whole and self.aside:
            return [self.local(grads, kept, 2)]
        if self.whole:
            parts = [
                grads.at[:, pl.ds(i * self.cols, self.cols)]
                if self.kind == "cols"
                else grads.at[block_of(i, self.rows)]
                for i in range(self.n)
            ]
            return [self.local(part, kept.at[i], 2 + i) for i, part in enumerate(parts)]
        if self.kind == "cols":
            moves = [self.local(grads.at[block_of(s, self.rows)], kept, 2)]
        else:
            moves = []
            for i in range(self.n):
                slot = 2 * i + s if self.kind == "rows" else s * self.n + i
                moves.append(self.local(grads.at[block_of(slot, self.rows)], kept.at[i], 2 + i))
        return moves + [self.local(self.received.ref, self.got.ref, 1)]

    def load(self):
        for move in self.loads():
            move.start()

    def add(self):
        for move in self.loads():
            move.wait()
        if self.whole and self.aside:
            for i in range(self.n):
                self.total.ref[i] = self.kept.ref[:, i * self.cols : (i + 1) * self.cols]
        if self.whole:
            return
        kept, got, total = self.kept.ref, self.got.ref, self.total.ref
        for i in range(self.n):
            if self.kind == "cols":
                part = (slice(None), slice(i * self.cols, (i + 1) * self.cols))
            else:
                part = i
            total[i] = (kept[part].astype(F32) + got[part].astype(F32)).astype(BF)


class DirectScatter(Task):
    def __init__(self, k, kind, grads, received):
        self.terms = Terms(k, kind, grads, received, lambda *a: self.local(*a))
        count = dp_size()

        def moves(s, d, t):
            total = self.terms.total.ref
            far = []
            for i in range(1, count):
                other = (d + i) % count
                far.append(([(None, total.at[other])], self.out.ref.at[d], {"dp": other}))
            return far, [([(None, total.at[d])], self.out.ref.at[d])]

        super().__init__(k, self.terms.shape, "dp", moves, count - 1, 2 + count)
        self.load = self.terms.load

    def send(self):
        self.terms.add()
        super().send()

    def add(self):
        self.load()
        self.send()


class LineScatter(Line):
    def __init__(self, k, kind, grads, received):
        self.terms = Terms(k, kind, grads, received, lambda *a: self.local(*a))
        super().__init__(k, self.terms.shape[1:], BF, 6)
        self.got = k.vmem((2, 3) + self.terms.shape[1:], BF)
        self.load = self.terms.load

    def ends(self, j, way):
        d = lax.axis_index("dp")
        if way == 0:
            return (d <= j) & (d < 3), (d >= 1) & (d <= j + 1)
        return (d >= 3 - j) & (d > 0), (d <= 2) & (d >= 2 - j)

    def copy(self, j, way):
        d = lax.axis_index("dp")
        to = (d + 3 - j if way == 0 else d + 1 + j) % 4
        return self.hop(j, way, self.terms.total.ref.at[to], self.got.ref.at[way, j])

    def send(self):
        self.phase = 0
        self.terms.add()
        for way in range(2):
            pl.when(self.ends(0, way)[0])(self.copy(0, way).start)

    def take(self, j, way):
        d = lax.axis_index("dp")
        to = (d + 2 - j if way == 0 else d + 2 + j) % 4
        self.copy(j, way).wait_recv()
        total = self.terms.total.ref
        total[to] = (total[to].astype(F32) + self.got.ref[way, j].astype(F32)).astype(BF)

    def arrive(self, j):
        for way in range(2):
            pl.when(self.ends(j, way)[1])(functools.partial(self.take, j, way))

    def step(self):
        self.arrive(self.phase)
        self.phase += 1
        for way in range(2):
            pl.when(self.ends(self.phase, way)[0])(self.copy(self.phase, way).start)

    def wait(self):
        if self.waited:
            return
        self.waited = True
        while self.phase < 2:
            self.step()
        self.arrive(2)
        done = self.local(self.terms.total.ref.at[lax.axis_index("dp")], self.out.ref, 0)
        done.start()
        for j in range(3):
            for way in range(2):
                pl.when(self.ends(j, way)[0])(self.copy(j, way).wait_send)
        done.wait()

    def add(self):
        self.load()
        self.send()


def sum_scatter(k, kind, grads, received=None):
    return (LineScatter if dp_size() == 4 else DirectScatter)(k, kind, grads, received)


class Finish(Task):
    def __init__(self, k, pieces, block):
        self.pieces, self.final = as_val(k, pieces), block
        *slots, rows, cols = self.pieces.shape
        self.slots = slots[0] if slots else 0
        if slots:
            self.held, self.total = k.vmem(self.pieces.shape, BF), k.vmem((rows, cols), BF)
        else:
            self.total = self.pieces

        def moves(s, d, t):
            source, dst = [(None, self.total.ref)], self.out.ref.at[s]
            return [(source, dst, {"section": 1 - s})], [(source, dst)]

        super().__init__(k, (2, rows, cols), "section", moves, 1, 2)

    def load(self):
        if self.slots:
            self.local(self.pieces.ref, self.held.ref, 1).start()

    def send(self):
        if self.slots:
            self.local(self.pieces.ref, self.held.ref, 1).wait()
            acc = self.held.ref[0].astype(F32)
            for i in range(1, self.slots):
                acc = acc + self.held.ref[i].astype(F32)
            self.total.ref[...] = acc.astype(BF)
        super().send()

    def add(self):
        self.load()
        self.send()


class SumShare(Task):
    def __init__(self, k, terms, axis, slotted=False):
        self.terms = [as_val(k, v) for v in terms]
        shape = self.terms[0].shape[1:] if slotted else self.terms[0].shape
        count = dp_size() if axis == "dp" else 4
        self.slotted = slotted
        self.bufs = [k.vmem(v.shape, F32) for v in self.terms]
        self.total = k.vmem(shape, F32)

        def moves(s, d, t):
            source, me = [(None, self.total.ref)], d if axis == "dp" else t
            dst = self.out.ref.at[me]
            far = [(source, dst, {axis: (me + i) % count}) for i in range(1, count)]
            return far, [(source, dst)]

        super().__init__(k, (count,) + shape, axis, moves, count - 1, 3, out_dtype=F32)

    def add(self):
        loads = [self.local(v.ref, b.ref, 1 + i) for i, (v, b) in enumerate(zip(self.terms, self.bufs))]
        for load in loads:
            load.start()
        for load in loads:
            load.wait()
        if self.slotted:
            parts = [self.bufs[0].ref[i] for i in range(self.terms[0].shape[0])]
        else:
            parts = [buf.ref[...] for buf in self.bufs]
        acc = parts[0]
        for part in parts[1:]:
            acc = acc + part
        self.total.ref[...] = acc
        self.send()


class Weight:
    def __init__(self, k, kind, *segments, early=False):
        self.kind, self.waited = kind, False
        self.segments, start = [], 0
        for near, far in segments:
            near, far = as_val(k, near), None if far is None else as_val(k, far)
            self.segments.append((near, far, start))
            start += near.shape[1] * (1 if far is None else 2)
        self.count, _, self.cols = self.segments[0][0].shape
        self.rows = start
        if kind == "cols":
            shape = (self.rows, self.count * self.cols)
        else:
            shape = (self.count * self.rows, self.cols)
        self.aside = kind == "cols" and self.cols % 128 != 0
        self.buf = k.vmem(shape, BF)
        sides = [v for near, far, _ in self.segments for v in (near, far) if v is not None]
        self.sem = k.sem(len(sides), self.count)
        if self.aside:
            self.held = [k.vmem(v.shape, BF) for v in sides]
        k.once.append(self)
        if early:
            k.early.append(self.start)

    def sides(self):
        s = lax.axis_index("section")
        for near, far, start in self.segments:
            rows = near.shape[1]
            if far is None:
                yield near, start, None
            else:
                yield near, start + s * rows, s
                yield far, start + (1 - s) * rows, 1 - s

    def moves(self):
        dst = self.buf.ref
        for j, (val, start, sec) in enumerate(self.sides()):
            rows = val.shape[1]
            for i in range(self.count):
                if self.aside:
                    to = self.held[j].ref.at[i]
                elif self.kind == "cols":
                    at = pl.ds(pl.multiple_of(start, 16), rows)
                    to = dst.at[at, pl.ds(i * self.cols, self.cols)]
                else:
                    top = (sec * self.count + i) * rows if self.kind == "conv" else i * self.rows + start
                    to = dst.at[pl.ds(pl.multiple_of(top, 16), rows)]
                yield pltpu.make_async_copy(val.ref.at[i], to, self.sem.ref.at[j, i])

    def start(self):
        for move in self.moves():
            move.start()

    def wait(self):
        if self.waited:
            return
        self.waited = True
        for move in self.moves():
            move.wait()
        if self.aside:
            for j, (val, start, _) in enumerate(self.sides()):
                whole = jnp.concatenate([self.held[j].ref[i] for i in range(self.count)], axis=1)
                self.buf.ref[pl.ds(pl.multiple_of(start, 16), val.shape[1]), :] = whole


class Product:
    def __init__(self, k, left, right):
        self.left, self.right = left, right
        rows = left.shape[1]
        self.chunk = 384 if rows % 384 == 0 else 256
        self.count = rows // self.chunk
        self.buf = k.vmem((rows, right.shape[1]), BF)
        self.out, self.sem = k.output(self.buf.shape, BF), k.sem(self.count)

    def copy(self, i):
        part = block_of(i, self.chunk)
        return pltpu.make_async_copy(self.buf.ref.at[part], self.out.ref.at[part], self.sem.ref.at[i])

    def run(self):
        def step(i, carry):
            part = block_of(i, self.chunk)
            value = contract(self.left.ref[:, part], self.right.ref[...], 0, 0)
            self.buf.ref[part, :] = value.astype(BF)
            self.copy(i).start()
            return carry

        lax.fori_loop(0, self.count, step, 0)

    def wait(self):
        for i in range(self.count):
            self.copy(i).wait()


def places():
    me = lax.axis_index("tensor")
    sib = me + 1 - 2 * (me % 2)
    cross = (me + 2) % 4
    diag = (sib + 2) % 4
    return me, sib, cross, diag


class Gather:
    def __init__(self, k, x, gain, weights, extras=(), trans=False, epilogue="plain", save=()):
        rows, width = x.shape
        length = 4 * rows
        self.k, self.x, self.gain, self.weights, self.extras = k, x, gain, weights, extras
        self.trans, self.epilogue, self.rows, self.half = trans, epilogue, rows, rows // 2
        cols = [w.buf.shape[0 if trans else 1] for w in weights]
        kinds = {
            "plain": [(c, F32) for c in cols],
            "ffn": [(cols[0], BF)] * 3,
            "ffn_back": [(cols[0], BF)] * 2,
        }[epilogue]
        self.full = k.vmem((length, width), BF)
        self.values = [k.vmem((length, c), kind) for c, kind in kinds]
        kept = [self.full] + self.values
        self.saved = [(v, k.output(v.shape, v.dtype), k.sem(4, 2)) for v in kept if kept.index(v) in save]
        self.sems = [k.sem(2) for _ in range(6)]
        k.late.append(self.end)

    def span(self, owner, sub):
        return pl.ds(pl.multiple_of(owner * self.rows + sub * self.half, self.half), self.half)

    def move(self, kind, i):
        me, sib, cross, _ = places()
        full = self.full.ref
        owner, peer, at = {"cross": (me, cross, 0), "sib": (me, sib, 2), "relay": (cross, sib, 4)}[kind]
        part = full.at[self.span(owner, i)]
        return remote(
            part, part, self.sems[at].ref.at[i], self.sems[at + 1].ref.at[i], {"tensor": peer}
        )

    def begin(self):
        me = places()[0]
        for i in range(2):
            part = self.x.ref[pl.ds(i * self.half, self.half), :].astype(F32)
            if self.gain is not None:
                val, row = self.gain
                part = norm_rows(part, val.ref[row : row + 1, :])
            self.full.ref[self.span(me, i), :] = part.astype(BF)
            self.move("cross", i).start()
            self.move("sib", i).start()

    def loop(self):
        me, sib, cross, diag = places()
        rows, half = self.rows, self.half
        for w in self.weights:
            w.wait()

        def step(p, carry):
            far, sub = p // 2, p % 2
            near = (1 - sub) * me + sub * sib
            first = (1 - far) * near * rows + far * (cross * rows + sub * half)
            second = (1 - far) * (near * rows + half) + far * (diag * rows + sub * half)
            pair = [pl.ds(pl.multiple_of(v, half), half) for v in (first, second)]

            @pl.when(p == 1)
            def _():
                self.move("sib", 0).wait_recv()
                self.move("sib", 1).wait_recv()

            for i in range(2):

                @pl.when(p == 2 + i)
                def _():
                    self.move("cross", i).wait_recv()
                    self.move("relay", i).start()
                    self.move("relay", i).wait_recv()

            def both(val):
                return jnp.concatenate([val.ref[pair[0], :], val.ref[pair[1], :]], axis=0)

            a = both(self.full)
            prods = [contract(a, w.buf.ref[...], 1, 1 if self.trans else 0) for w in self.weights]
            if self.epilogue == "plain":
                values = prods
            elif self.epilogue == "ffn":
                sig, silu = silu_parts(prods[0])
                values = [prods[0], prods[1], silu * prods[1]]
            else:
                gate, up = (both(v).astype(F32) for v in self.extras)
                sig, silu = silu_parts(gate)
                values = [prods[0] * up * sig * (1.0 + gate * (1.0 - sig)), prods[0] * silu]
            for val, value in zip(self.values, values):
                value = value.astype(val.dtype)
                for j in range(2):
                    val.ref[pair[j], :] = value[j * half : (j + 1) * half]
            for val, out, sem in self.saved:
                for j in range(2):
                    pltpu.make_async_copy(
                        val.ref.at[pair[j]], out.ref.at[pair[j]], sem.ref.at[p, j]
                    ).start()
            return carry

        lax.fori_loop(0, 4, step, 0)

    def end(self):
        for i in range(2):
            for kind in ("cross", "sib", "relay"):
                self.move(kind, i).wait_send()
        part = pl.ds(0, self.half)
        for val, out, sem in self.saved:
            for p in range(4):
                for j in range(2):
                    pltpu.make_async_copy(val.ref.at[part], out.ref.at[part], sem.ref.at[p, j]).wait()


class Scatter:
    def __init__(self, k, operands, weights, resid, back=None, trans=False, low=False):
        rows, width = resid.shape
        half = rows // 2
        self.operands, self.weights, self.resid, self.back = operands, weights, resid, back
        self.trans, self.low, self.rows, self.half = trans, low, rows, half
        self.keep, self.own = k.vmem((2, half, width), F32), k.vmem((rows, width), F32)
        self.to_s, self.from_s, self.to_c, self.from_c = (
            k.vmem((2, half, width), BF) for _ in range(4)
        )
        self.to_o, self.from_o = k.vmem((rows, width), BF), k.vmem((rows, width), BF)
        self.out = k.vmem((rows, width), BF if low else F32)
        self.gain_grad = k.vmem((1, width), F32) if back else None
        self.sems = [k.sem(2) for _ in range(4)] + [k.sem(1) for _ in range(2)]
        k.late.append(self.end)

    def move(self, kind, i=0):
        _, sib, cross, _ = places()
        at, src, dst, peer = {
            "diag": (0, self.to_s, self.from_s, sib),
            "cross": (2, self.to_c, self.from_c, cross),
            "near": (4, self.to_o, self.from_o, sib),
        }[kind]
        src, dst = (src.ref, dst.ref) if kind == "near" else (src.ref.at[i], dst.ref.at[i])
        return remote(
            src, dst, self.sems[at].ref.at[i], self.sems[at + 1].ref.at[i], {"tensor": peer}
        )

    def pass_on(self, i):
        self.move("diag", i).wait_recv()
        total = self.keep.ref[i] + self.from_s.ref[i].astype(F32)
        self.to_c.ref[i] = total.astype(BF)
        self.move("cross", i).start()

    def loop(self):
        me, sib, cross, diag = places()
        rows, half = self.rows, self.half
        for w in self.weights:
            w.wait()

        def step(p, carry):
            near, sub = p // 2, p % 2
            base = near * ((1 - sub) * sib + sub * me) * rows
            first = base + (1 - near) * (cross * rows + sub * half)
            second = base + near * half + (1 - near) * (diag * rows + sub * half)
            pair = [pl.ds(pl.multiple_of(v, half), half) for v in (first, second)]
            total = None
            for y, w in zip(self.operands, self.weights):
                a = jnp.concatenate([y.ref[pair[0], :], y.ref[pair[1], :]], axis=0)
                prod = contract(a, w.buf.ref[...], 1, 1 if self.trans else 0)
                total = prod if total is None else total + prod

            for i in range(2):

                @pl.when(p == i)
                def _():
                    self.keep.ref[i] = total[:half]
                    self.to_s.ref[i] = total[half:].astype(BF)
                    self.move("diag", i).start()

            @pl.when(p == 1)
            def _():
                self.pass_on(0)

            @pl.when(p == 2)
            def _():
                self.to_o.ref[...] = total.astype(BF)
                self.move("near").start()
                self.pass_on(1)

            @pl.when(p == 3)
            def _():
                self.own.ref[...] = total

            return carry

        lax.fori_loop(0, 4, step, 0)

    def finish(self):
        self.move("near").wait_recv()
        gain_sum = None
        for i in range(2):
            part = pl.ds(i * self.half, self.half)
            self.move("cross", i).wait_recv()
            total = self.own.ref[part, :] + self.from_o.ref[part, :].astype(F32)
            total = total + self.from_c.ref[i].astype(F32)
            resid = self.resid.ref[part, :].astype(F32)
            if self.back:
                value, (gain, row) = self.back
                value_grad, gain_grad = norm_back(
                    value.ref[part, :].astype(F32), gain.ref[row : row + 1, :], total
                )
                total = value_grad
                gain_sum = gain_grad if gain_sum is None else gain_sum + gain_grad
            self.out.ref[part, :] = (resid + total).astype(self.out.dtype)
        if self.back:
            self.gain_grad.ref[...] = gain_sum

    def end(self):
        self.move("near").wait_send()
        for i in range(2):
            self.move("diag", i).wait_send()
            self.move("cross", i).wait_send()


def delayed(values, by):
    if by == 0:
        return values
    row = lax.broadcasted_iota(jnp.int32, values.shape, 0)
    return jnp.where(row < by, 0.0, pltpu.roll(values, by, 0))


def advanced(values, by):
    if by == 0:
        return values
    length = values.shape[0]
    row = lax.broadcasted_iota(jnp.int32, values.shape, 0)
    return jnp.where(row >= length - by, 0.0, pltpu.roll(values, length - by, 0))


CONV_COLS = 128


class Conv:
    def __init__(self, k, projected, value, kernel):
        self.projected, self.value, self.kernel = projected, value, kernel
        self.y = k.vmem(value.shape, BF)

    def parts(self, j):
        channels = self.value.shape[1]
        at = slice(j * CONV_COLS, (j + 1) * CONV_COLS)
        b_gate = self.projected.ref[:, at]
        c_gate = self.projected.ref[:, channels + at.start : channels + at.stop]
        x_value, taps = self.value.ref[:, at], self.kernel.ref[:, at]
        product = b_gate * x_value
        count = taps.shape[0]
        causal = jnp.zeros_like(product)
        for i in range(count):
            causal = causal + taps[i : i + 1] * delayed(product, count - 1 - i)
        return at, b_gate, c_gate, x_value, taps, product, causal

    def run(self):
        for j in range(self.value.shape[1] // CONV_COLS):
            at, _, c_gate, _, _, _, causal = self.parts(j)
            self.y.ref[:, at] = (c_gate * causal).astype(BF)


class ConvBack(Conv):
    def __init__(self, k, projected, value, kernel, d_y):
        self.projected, self.value, self.kernel, self.d_y = projected, value, kernel, d_y
        self.d_proj = k.vmem(projected.shape, BF)
        self.d_value = k.vmem(value.shape, BF)
        self.d_kernel = k.vmem(kernel.shape, F32)

    def run(self):
        channels = self.value.shape[1]
        for j in range(channels // CONV_COLS):
            at, b_gate, c_gate, x_value, taps, product, causal = self.parts(j)
            d_y = self.d_y.ref[:, at]
            d_causal = d_y * c_gate
            count = taps.shape[0]
            d_product = jnp.zeros_like(product)
            for i in range(count):
                by = count - 1 - i
                row = jnp.sum(d_causal * delayed(product, by), axis=0, keepdims=True)
                self.d_kernel.ref[i : i + 1, at] = row
                d_product = d_product + taps[i : i + 1] * advanced(d_causal, by)
            self.d_proj.ref[:, at] = (d_product * x_value).astype(BF)
            self.d_proj.ref[:, channels + at.start : channels + at.stop] = (d_y * causal).astype(BF)
            self.d_value.ref[:, at] = (d_product * b_gate).astype(BF)


def head_mean(values, head_size):
    width = values.shape[1]
    row = lax.broadcasted_iota(jnp.int32, (width, width), 0) // head_size
    col = lax.broadcasted_iota(jnp.int32, (width, width), 1) // head_size
    group = jnp.where(row == col, 1.0 / head_size, 0.0).astype(F32)
    return lax.dot_general(
        values, group, (((1,), (0,)), ((), ())),
        precision=lax.Precision.HIGHEST, preferred_element_type=F32,
    )


def turn(values, head_size, back):
    width, half = values.shape[1], head_size // 2
    lane = lax.broadcasted_iota(jnp.int32, values.shape, 1) % head_size
    upper = pltpu.roll(values, width - half, 1)
    lower = pltpu.roll(values, half, 1)
    return jnp.where(lane < half, upper, -lower) if back else jnp.where(lane < half, -upper, lower)


def head_norm(values, gain, head_size):
    return values * lax.rsqrt(head_mean(values * values, head_size) + EPS) * gain


def head_norm_back(values, gain, grad_in, head_size):
    row_scale = lax.rsqrt(head_mean(values * values, head_size) + EPS)
    normed = values * row_scale
    gain_grad = jnp.sum(grad_in * normed, axis=0, keepdims=True)
    scaled = grad_in * gain
    return row_scale * (scaled - normed * head_mean(scaled * normed, head_size)), gain_grad


def block_weights(q_rows, keys):
    scores = [contract(q_rows, k_rows, 1, 1) for k_rows in keys]
    query = lax.broadcasted_iota(jnp.int32, scores[-1].shape, 0)
    key = lax.broadcasted_iota(jnp.int32, scores[-1].shape, 1)
    scores[-1] = jnp.where(key <= query, scores[-1], MASKED)
    top = functools.reduce(
        jnp.maximum, [jnp.max(part, axis=1, keepdims=True) for part in scores]
    )
    exps = [jnp.exp(part - top) for part in scores]
    scale = 1.0 / sum(jnp.sum(part, axis=1, keepdims=True) for part in exps)
    return [part * scale for part in exps]


def key_blocks(i):
    blocks = [pl.ds(0, i * ROW_BLOCK)] if i else []
    return blocks + [pl.ds(i * ROW_BLOCK, ROW_BLOCK)]


class Heads:
    def __init__(self, projected, tables, size):
        assert size in (16, 64, 256), size
        self.projected, self.size = projected, size
        self.gain, self.cos, self.sin = (v.buf for v in tables)
        self.loads = tables
        self.length, width = projected.shape
        self.q_cols, self.k_cols = width // 2, width // 4
        self.heads, self.kv_heads = self.q_cols // size, self.k_cols // size
        self.share = self.heads // self.kv_heads

    def per_head(self, k, count, kind):
        return k.vmem((count, self.length, self.size), kind)

    def split(self, val, rows, values):
        for h in range(val.shape[0]):
            val.ref[h, rows, :] = values[:, h * self.size : (h + 1) * self.size]

    def join(self, val, rows):
        return jnp.concatenate([val.ref[h, rows, :] for h in range(val.shape[0])], axis=1)

    def angles(self, rows):
        c, n = self.cos.ref[rows, :], self.sin.ref[rows, :]
        repeat = self.q_cols // c.shape[1]
        return jnp.concatenate([c] * repeat, axis=1), jnp.concatenate([n] * repeat, axis=1)

    def blocks(self, step):
        lax.fori_loop(0, self.length // ROW_BLOCK, lambda p, c: step(block_of(p, ROW_BLOCK)) or c, 0)


class Attend(Heads):
    def __init__(self, k, projected, tables, size):
        super().__init__(projected, tables, size)
        self.q_rot = k.vmem((self.length, self.q_cols), BF)
        self.k_rot = k.vmem((self.length, self.k_cols), BF)
        self.y = k.vmem((self.length, self.q_cols), BF)
        self.q_h, self.y_h = (self.per_head(k, self.heads, BF) for _ in range(2))
        self.k_h, self.v_h = (self.per_head(k, self.kv_heads, BF) for _ in range(2))

    def run(self, *between):
        for load in self.loads:
            load.wait()
        size, q_cols, k_cols, proj = self.size, self.q_cols, self.k_cols, self.projected.ref

        def prepare(rows):
            c, n = self.angles(rows)
            q = head_norm(proj[rows, :q_cols], self.gain.ref[0:1, :], size)
            q = (q * c + turn(q, size, False) * n).astype(BF)
            k = head_norm(proj[rows, q_cols : q_cols + k_cols], self.gain.ref[1:2, :k_cols], size)
            k = (k * c[:, :k_cols] + turn(k, size, False) * n[:, :k_cols]).astype(BF)
            self.q_rot.ref[rows, :] = q
            self.k_rot.ref[rows, :] = k
            self.split(self.q_h, rows, (q.astype(F32) * size**-0.5).astype(BF))
            self.split(self.k_h, rows, k)
            self.split(self.v_h, rows, proj[rows, q_cols + k_cols :].astype(BF))

        self.blocks(prepare)

        def head(h, carry):
            g = h // self.share
            for i in range(self.length // ROW_BLOCK):
                rows, seen = pl.ds(i * ROW_BLOCK, ROW_BLOCK), key_blocks(i)
                weights = block_weights(
                    self.q_h.ref[h, rows, :], [self.k_h.ref[g, at, :] for at in seen]
                )
                value = sum(
                    contract(part.astype(BF), self.v_h.ref[g, at, :], 1, 0)
                    for part, at in zip(weights, seen)
                )
                self.y_h.ref[h, rows, :] = value.astype(BF)
            return carry

        lax.fori_loop(0, self.heads // 2, head, 0)
        for step in between:
            step()
        lax.fori_loop(self.heads // 2, self.heads, head, 0)
        self.y.ref[...] = self.join(self.y_h, slice(None))


class AttendBack(Heads):
    def __init__(self, k, projected, tables, size, q_rot, k_rot, d_y):
        super().__init__(projected, tables, size)
        self.q_rot, self.k_rot, self.d_y = q_rot, k_rot, d_y
        self.q_h, self.dy_h = (self.per_head(k, self.heads, BF) for _ in range(2))
        self.k_h, self.v_h = (self.per_head(k, self.kv_heads, BF) for _ in range(2))
        self.dq_h = self.per_head(k, self.heads, F32)
        self.dk_h, self.dv_h = (self.per_head(k, self.kv_heads, F32) for _ in range(2))
        self.d_proj = k.vmem(projected.shape, BF)
        self.q_gain, self.k_gain = k.vmem((1, self.q_cols), F32), k.vmem((1, self.k_cols), F32)

    def run(self, *between):
        for load in self.loads:
            load.wait()
        size, q_cols, k_cols, proj = self.size, self.q_cols, self.k_cols, self.projected.ref
        scale = size**-0.5
        dq_h, dk_h, dv_h = self.dq_h.ref, self.dk_h.ref, self.dv_h.ref

        def prepare(rows):
            self.split(self.q_h, rows, (self.q_rot.ref[rows, :].astype(F32) * scale).astype(BF))
            self.split(self.dy_h, rows, self.d_y.ref[rows, :].astype(BF))
            self.split(self.k_h, rows, self.k_rot.ref[rows, :])
            self.split(self.v_h, rows, proj[rows, q_cols + k_cols :].astype(BF))

        self.blocks(prepare)
        dk_h[...] = jnp.zeros_like(dk_h)
        dv_h[...] = jnp.zeros_like(dv_h)

        def head(h, carry):
            g = h // self.share
            for i in range(self.length // ROW_BLOCK):
                rows, seen = pl.ds(i * ROW_BLOCK, ROW_BLOCK), key_blocks(i)
                q, low = self.q_h.ref[h, rows, :], self.dy_h.ref[h, rows, :]
                keys = [self.k_h.ref[g, at, :] for at in seen]
                probs = block_weights(q, keys)
                d_weights = [contract(low, self.v_h.ref[g, at, :], 1, 1) for at in seen]
                inner = sum(
                    jnp.sum(a * b, axis=1, keepdims=True) for a, b in zip(probs, d_weights)
                )
                d_q = 0.0
                for at, k, prob, d_weight in zip(seen, keys, probs, d_weights):
                    dv_h[g, at, :] += contract(prob.astype(BF), low, 0, 0)
                    d_scores = (prob * (d_weight - inner)).astype(BF)
                    d_q = d_q + contract(d_scores, k, 1, 0)
                    dk_h[g, at, :] += contract(d_scores, q, 0, 0)
                dq_h[h, rows, :] = d_q * scale
            return carry

        lax.fori_loop(0, self.heads // 2, head, 0)
        for step in between:
            step()
        lax.fori_loop(self.heads // 2, self.heads, head, 0)
        self.q_gain.ref[...] = jnp.zeros_like(self.q_gain.ref)
        self.k_gain.ref[...] = jnp.zeros_like(self.k_gain.ref)

        def finish(rows):
            c, n = self.angles(rows)
            dq, dk, dv = (self.join(v, rows) for v in (self.dq_h, self.dk_h, self.dv_h))
            dq = dq * c + turn(dq * n, size, True)
            dk = dk * c[:, :k_cols] + turn(dk * n[:, :k_cols], size, True)
            dq, q_sum = head_norm_back(proj[rows, :q_cols], self.gain.ref[0:1, :], dq, size)
            dk, k_sum = head_norm_back(
                proj[rows, q_cols : q_cols + k_cols], self.gain.ref[1:2, :k_cols], dk, size
            )
            self.q_gain.ref[...] += q_sum
            self.k_gain.ref[...] += k_sum
            self.d_proj.ref[rows, :q_cols] = dq.astype(BF)
            self.d_proj.ref[rows, q_cols : q_cols + k_cols] = dk.astype(BF)
            self.d_proj.ref[rows, q_cols + k_cols :] = dv.astype(BF)

        self.blocks(finish)


def body(boundary, norm_gain, mix_in, mix_out, w_gate, w_up, w_down, conv_x, conv_kernel, qk_gain):
    first = lax.axis_index("section") == 0
    tensor_index = lax.axis_index("tensor")
    model_width = boundary.shape[3]
    channels = mix_out.shape[1]
    row_shape = boundary.shape[2:]
    length, size = 4 * row_shape[0], qk_gain.shape[1]

    seqs, own_gain = boundary[0], norm_gain[0]
    sh_in, sh_out, sh_gate, sh_up, sh_down = (v[0] for v in (mix_in, mix_out, w_gate, w_up, w_down))
    head_gain = jnp.tile(qk_gain, (1, channels // size))

    def gains_of(k, block, other, early=True):
        own, moved = k.input(own_gain), as_val(k, other)
        sources = lambda s, d, t: [(s == block, own.ref), (s == 1 - block, moved.ref)]
        return Load(k, sources, own.shape, F32, early)

    def start_rows(k, slot, other, early=True):
        own, moved = k.input(seqs), as_val(k, other)
        sources = lambda s, d, t: [(s == slot, own.ref.at[slot]), (s == 1 - slot, moved.ref)]
        return Load(k, sources, row_shape, BF, early)

    def wait(*items):
        return [item.wait for item in items]

    k = Kernel(0)
    t_seq = None
    seq_val = k.input(seqs)

    def seq_moves(s, d, t):
        return [([(None, seq_val.ref.at[1 - s])], t_seq.out.ref, {"section": 1 - s})], []

    t_in, t_out, t_up = (x_half(k, v) for v in (sh_in, sh_out, sh_up))
    gate_lo, gate_hi = (Part(sh_gate, i * (sh_gate.shape[0] // 2), sh_gate.shape[0] // 2) for i in range(2))
    down_lo, down_hi = (Part(sh_down, i * (sh_down.shape[0] // 2), sh_down.shape[0] // 2) for i in range(2))
    t_gate0a, t_gate0b = x_half(k, gate_lo, 0), x_move(k, gate_hi, 0)
    t_down0a, t_down0b = x_half(k, down_lo, 0), x_move(k, down_hi, 0)
    t_gate1, t_down1 = x_half(k, sh_gate, 1), x_move(k, sh_down, 1)
    t_seq = Task(k, row_shape, "section", seq_moves, 1)
    t_gain, z_cols = x_move(k, own_gain), z_gather(k, conv_x)
    z_in0, z_out0 = z_gather_half(k, sh_in, t_in.out, 0), z_gather_half(k, sh_out, t_out.out, 0)
    z_gate0a = z_gather_half(k, gate_lo, t_gate0a.out, 0)
    z_gate0b, x_gate0a = z_gather_whole(k, gate_hi, t_gate0b.out, 0), x_move(k, z_gate0a.out)
    z_up0 = z_gather_half(k, sh_up, t_up.out, 0)
    x_cols, x_in0, x_out0 = (x_move(k, v.out) for v in (z_cols, z_in0, z_out0))
    x_load, gain_load = start_rows(k, 0, t_seq.out, False), gains_of(k, 0, t_gain.out, False)
    taps = load_all(k, conv_kernel)
    angles = Angles(k, length, size, 128)
    w_in0, w_cols = Weight(k, "rows", (z_in0.out, x_in0.out)), Weight(k, "conv", (z_cols.out, x_cols.out))
    w_out0 = Weight(k, "cols", (z_out0.out, x_out0.out))
    g0 = Gather(k, x_load.buf, (gain_load.buf, 0), [w_in0, w_cols], save=(0, 1, 2))
    conv = Conv(k, g0.values[0], g0.values[1], taps.buf)
    y0 = Save(k, conv.y)
    s1 = Scatter(k, [conv.y], [w_out0], x_load.buf)
    mid0 = Save(k, s1.out)
    x_up0, z_gate1 = x_move(k, z_up0.out), z_gather_half(k, sh_gate, t_gate1.out, 1)
    z_down0a = z_gather_half(k, down_lo, t_down0a.out, 0)
    z_down0b = z_gather_whole(k, down_hi, t_down0b.out, 0)
    z_in1, z_out1 = z_gather_half(k, sh_in, t_in.out, 1), z_gather_half(k, sh_out, t_out.out, 1)
    x_down0a, x_in1, x_out1 = (x_move(k, v.out) for v in (z_down0a, z_in1, z_out1))
    w_gate0 = Weight(k, "rows", (z_gate0a.out, x_gate0a.out), (z_gate0b.out, None))
    w_up0 = Weight(k, "rows", (z_up0.out, x_up0.out))
    w_down0 = Weight(k, "cols", (z_down0a.out, x_down0a.out), (z_down0b.out, None))
    g2 = Gather(k, s1.out, (gain_load.buf, 1), [w_gate0, w_up0], epilogue="ffn", save=(0, 1, 2, 3))
    s3 = Scatter(k, [g2.values[2]], [w_down0], s1.out, low=True)
    z_rows = Save(k, s3.out)
    k.do(t_in.send, t_out.send, z_cols.send, t_up.send, t_gain.send, t_seq.send)
    k.do(t_gate0a.send, t_gate1.send)
    k.do(t_in.wait, z_in0.send, t_out.wait, z_out0.send, z_cols.step, z_in0.step, z_out0.step)
    k.do(z_cols.step, z_in0.step, z_out0.step, t_up.wait, z_up0.send)
    k.do(z_cols.wait, x_cols.send, z_in0.wait, x_in0.send, z_out0.wait, x_out0.send)
    k.do(t_gate0b.send, t_down0a.send, t_down0b.send, t_down1.send)
    k.do(t_gain.wait, gain_load.start, t_seq.wait, x_load.start, gain_load.wait, x_load.wait)
    k.do(g0.begin, z_up0.step, t_gate0a.wait, z_gate0a.send, angles.run, z_up0.step, z_gate0a.step)
    k.do(z_in1.send, z_out1.send, x_cols.wait, w_cols.start, x_in0.wait, w_in0.start)
    k.do(g0.loop, z_gate0a.step, t_gate0b.wait, z_gate0b.send, z_in1.step, z_out1.step)
    k.do(z_gate0a.wait, x_gate0a.send, z_up0.wait, x_up0.send, taps.wait, conv.run, y0.start)
    k.do(x_out0.wait, w_out0.start, s1.loop, z_gate0b.step, t_down0a.wait, z_down0a.send)
    k.do(t_down0b.wait, z_down0b.send, z_in1.step, z_out1.step, s1.finish, mid0.start)
    k.do(g2.begin, z_gate0b.step, z_down0a.step, z_down0b.step, t_gate1.wait, z_gate1.send)
    k.do(z_down0a.step)
    k.do(z_down0b.step, z_down0a.wait, x_down0a.send, z_in1.wait, x_in1.send, z_out1.wait, x_out1.send)
    k.do(z_gate0b.wait, x_gate0a.wait, w_gate0.start, z_gate1.step, x_up0.wait, w_up0.start)
    k.do(z_gate1.step, g2.loop, z_down0b.wait, x_down0a.wait, w_down0.start)
    k.do(s3.loop, s3.finish, z_rows.start)
    k.do(*wait(t_down1, x_in1, x_out1, z_gate1))
    k.build()
    a0, proj0, value0 = (out for _, out, _ in g0.saved)
    table_arrays = [head_gain] + [v.out for v in angles.saves]
    y0, mid0 = y0.out, mid0.out
    m0, gate0, up0, hid0 = (out for _, out, _ in g2.saved)
    z_rows = z_rows.out

    k = Kernel(2)
    x_gate1, z_up1 = x_move(k, z_gate1.out), z_gather_half(k, sh_up, t_up.out, 1)
    z_down1a, z_down1b = (z_gather_whole(k, sh_down, t_down1.out, 1, i) for i in range(2))
    x_up1 = x_move(k, z_up1.out)
    rows, gain_load = load_all(k, z_rows), gains_of(k, 1, t_gain.out)
    tables = [load_all(k, v) for v in table_arrays]
    w_in1 = Weight(k, "rows", (z_in1.out, x_in1.out), early=True)
    w_out1 = Weight(k, "cols", (z_out1.out, x_out1.out), early=True)
    g4 = Gather(k, rows.buf, (gain_load.buf, 0), [w_in1], save=(0, 1))
    attend = Attend(k, g4.values[0], tables, size)
    kept = [Save(k, v) for v in (attend.q_rot, attend.k_rot, attend.y)]
    s5 = Scatter(k, [attend.y], [w_out1], rows.buf)
    mid1 = Save(k, s5.out)
    cot = start_rows(k, 1, t_seq.out)
    w_gate1 = Weight(k, "rows", (z_gate1.out, x_gate1.out))
    w_up1 = Weight(k, "rows", (z_up1.out, x_up1.out))
    w_down1 = Weight(k, "cols", (z_down1a.out, None), (z_down1b.out, None))
    g6 = Gather(k, s5.out, (gain_load.buf, 1), [w_gate1, w_up1], epilogue="ffn", save=(3,))
    g8 = Gather(
        k, cot.buf, None, [w_down1], [g6.values[0], g6.values[1]], trans=True, epilogue="ffn_back"
    )
    p_down1 = Product(k, g6.values[2], g8.full)
    p_gate1, p_up1 = Product(k, g6.full, g8.values[0]), Product(k, g6.full, g8.values[1])
    s9 = Scatter(k, g8.values, [w_gate1, w_up1], cot.buf, (s5.out, (gain_load.buf, 1)), True)
    d_mid1, gain11 = Save(k, s9.out), Save(k, s9.gain_grad)
    k.do(x_gate1.send, z_up1.send, rows.wait, gain_load.wait, g4.begin, z_up1.step)
    k.do(cot.wait, g8.begin, z_down1a.send, g4.loop, z_up1.step, z_down1b.send)
    k.do(lambda: attend.run(z_up1.wait, x_up1.send, z_down1a.step))
    k.do(*(v.start for v in kept))
    k.do(x_gate1.wait, w_gate1.start, z_down1b.step, s5.loop, z_down1a.step, s5.finish, mid1.start)
    k.do(g6.begin, z_down1b.step, x_up1.wait, w_up1.start, g6.loop)
    k.do(*wait(z_down1a, z_down1b), w_down1.start, g8.loop)
    k.do(s9.loop, p_down1.run, p_gate1.run, p_up1.run)
    k.do(s9.finish, d_mid1.start, gain11.start, p_down1.wait, p_gate1.wait, p_up1.wait)
    k.build()
    a1, proj1 = (out for _, out, _ in g4.saved)
    (hid1,) = (out for _, out, _ in g6.saved)
    q_rot, k_rot, y1 = (v.out for v in kept)
    mid1, d_mid1, gain11 = mid1.out, d_mid1.out, gain11.out

    k = Kernel(4)
    r_down1 = x_half(k, p_down1.out)
    r_gate1, q_up1 = x_slots(k, p_gate1.out, "rows"), sum_scatter(k, "rows", p_up1.out)
    rows, gain_load = load_all(k, d_mid1), gains_of(k, 1, t_gain.out)
    value = load_all(k, z_rows)
    tables = [load_all(k, v) for v in table_arrays]
    proj, q_load, k_load, y_load, a_load = (load_all(k, v) for v in (proj1, q_rot, k_rot, y1, a1))
    w_in1 = Weight(k, "rows", (z_in1.out, x_in1.out), early=True)
    w_out1 = Weight(k, "cols", (z_out1.out, x_out1.out), early=True)
    g10 = Gather(k, rows.buf, None, [w_out1], trans=True)
    p_out1 = Product(k, y_load.buf, g10.full)
    back = AttendBack(k, proj.buf, tables, size, q_load.buf, k_load.buf, g10.values[0])
    p_in1 = Product(k, a_load.buf, back.d_proj)
    r_out1 = x_half(k, p_out1.out)
    s11 = Scatter(
        k, [back.d_proj], [w_in1], rows.buf, (value.buf, (gain_load.buf, 0)), True, low=True
    )
    d_z, gain10 = Save(k, s11.out), Save(k, s11.gain_grad)
    head_gains = [Save(k, back.q_gain), Save(k, back.k_gain)]
    k.early.append(q_up1.load)
    k.do(r_down1.send, r_gate1.send, rows.wait, g10.begin, q_up1.send, g10.loop)
    k.do(y_load.wait, p_out1.run, q_up1.step, p_out1.wait, r_out1.send)
    k.do(proj.wait, q_load.wait, k_load.wait, lambda: back.run(q_up1.step))
    k.do(*(v.start for v in head_gains))
    k.do(gain_load.wait, value.wait, s11.loop, a_load.wait, p_in1.run)
    k.do(s11.finish, d_z.start, gain10.start, p_in1.wait)
    k.do(*wait(r_down1, q_up1, r_gate1, r_out1))
    k.build()
    d_z, gain10 = d_z.out, gain10.out
    q_gain, k_gain = (v.out for v in head_gains)

    k = Kernel(5)
    q_gate1, m_up1 = sum_scatter(k, "rows", p_gate1.out, r_gate1.out), x_move(k, q_up1.out, 0)
    q_out1 = sum_scatter(k, "cols", p_out1.out, r_out1.out)
    r_in1 = x_slots(k, p_in1.out, "rows")
    q_in1 = sum_scatter(k, "rows", p_in1.out, r_in1.out)
    q_down1 = sum_scatter(k, "cols", p_down1.out, r_down1.out)
    rows, value, gain_load = load_all(k, d_z), load_all(k, mid0), gains_of(k, 0, t_gain.out)
    gate_load, up_load, hid_load, m_load = (load_all(k, v) for v in (gate0, up0, hid0, m0))
    w_gate0 = Weight(k, "rows", (z_gate0a.out, x_gate0a.out), (z_gate0b.out, None), early=True)
    w_up0 = Weight(k, "rows", (z_up0.out, x_up0.out), early=True)
    w_down0 = Weight(k, "cols", (z_down0a.out, x_down0a.out), (z_down0b.out, None), early=True)
    g12 = Gather(
        k, rows.buf, None, [w_down0], [gate_load.buf, up_load.buf], trans=True, epilogue="ffn_back"
    )
    p_down0 = Product(k, hid_load.buf, g12.full)
    p_gate0, p_up0 = Product(k, m_load.buf, g12.values[0]), Product(k, m_load.buf, g12.values[1])
    r_down0 = x_half(k, p_down0.out)
    s13 = Scatter(
        k, g12.values, [w_gate0, w_up0], rows.buf, (value.buf, (gain_load.buf, 1)), True
    )
    d_mid0, gain01 = Save(k, s13.out), Save(k, s13.gain_grad)
    k.early += [q_gate1.load, q_down1.load, q_out1.load]
    k.do(r_in1.send, m_up1.send, rows.wait, g12.begin, q_gate1.send, q_down1.send, q_out1.send)
    k.do(gate_load.wait, up_load.wait, g12.loop, q_gate1.step, q_down1.step, q_out1.step)
    k.do(hid_load.wait, p_down0.run, p_down0.wait, r_down0.send, r_in1.wait, q_in1.add)
    k.do(s13.loop, q_gate1.step, q_down1.step, q_out1.step)
    k.do(m_load.wait, p_gate0.run, q_in1.step, p_up0.run, value.wait, gain_load.wait)
    k.do(s13.finish, d_mid0.start, gain01.start, q_in1.step, p_gate0.wait, p_up0.wait)
    k.do(*wait(q_gate1, q_out1, q_in1, q_down1, m_up1, r_down0))
    k.build()
    d_mid0, gain01 = d_mid0.out, gain01.out

    k = Kernel(6)
    r_gate0 = x_slots(k, p_gate0.out, "rows")
    q_gate0 = sum_scatter(k, "rows", p_gate0.out, r_gate0.out)
    q_down0 = sum_scatter(k, "cols", p_down0.out, r_down0.out)
    q_up0 = sum_scatter(k, "rows", p_up0.out)
    m_up0 = x_move(k, q_up0.out, 1)
    e_down1 = Finish(k, q_down1.out, 1)
    e_gate1, e_out1, e_in1 = (Finish(k, v.out, 1) for v in (q_gate1, q_out1, q_in1))
    rows, gain_load = load_all(k, d_mid0), gains_of(k, 0, t_gain.out)
    x_load, taps = start_rows(k, 0, t_seq.out), load_all(k, conv_kernel)
    y_load, a_load, proj, value = (load_all(k, v) for v in (y0, a0, proj0, value0))
    w_in0 = Weight(k, "rows", (z_in0.out, x_in0.out), early=True)
    w_cols = Weight(k, "conv", (z_cols.out, x_cols.out), early=True)
    w_out0 = Weight(k, "cols", (z_out0.out, x_out0.out), early=True)
    g14 = Gather(k, rows.buf, None, [w_out0], trans=True)
    p_out0 = Product(k, y_load.buf, g14.full)
    back = ConvBack(k, proj.buf, value.buf, taps.buf, g14.values[0])
    p_in0, p_cols = Product(k, a_load.buf, back.d_proj), Product(k, a_load.buf, back.d_value)
    r_out0, r_in0 = x_half(k, p_out0.out), x_slots(k, p_in0.out, "rows")
    r_cols = x_slots(k, p_cols.out, "conv")
    q_out0, q_in0 = sum_scatter(k, "cols", p_out0.out, r_out0.out), sum_scatter(k, "rows", p_in0.out, r_in0.out)
    q_cols = sum_scatter(k, "conv", p_cols.out, r_cols.out)
    e_down0, e_gate0, e_out0, e_in0 = (
        Finish(k, v.out, 0) for v in (q_down0, q_gate0, q_out0, q_in0)
    )
    s15 = Scatter(
        k, [back.d_proj, back.d_value], [w_in0, w_cols], rows.buf,
        (x_load.buf, (gain_load.buf, 0)), True, low=True,
    )
    d_x = Save(k, s15.out)
    tap_rows = conv_kernel.shape[0]
    small = k.vmem((8, model_width), F32)
    small_out = Save(k, small)
    ready = [load_all(k, v) for v in (gain01, gain10, gain11)]
    head_loads = [load_all(k, v) for v in (q_gain, k_gain)]

    def fill_small():
        t = lax.axis_index("tensor")
        small.ref[...] = jnp.zeros_like(small.ref)
        small.ref[0:1, :] = s15.gain_grad.ref[...]
        for i, load in enumerate(ready):
            load.wait()
            small.ref[i + 1 : i + 2, :] = load.buf.ref[...]
        small.ref[4 : 4 + tap_rows, block_of(t, channels)] = back.d_kernel.ref[...]
        at = 0
        for load in head_loads:
            load.wait()
            width = load.buf.shape[1]
            small.ref[7:8, at : at + width] = load.buf.ref[...]
            at += width
        small_out.start()

    t_small = x_move(k, small_out.out)
    z_small = SumShare(k, [small_out.out, t_small.out], "dp")
    t_total = SumShare(k, [z_small.out], "tensor", slotted=True)
    hid_load, mid_load = load_all(k, hid1), load_all(k, mid1)
    w_down1 = Weight(k, "cols", (z_down1a.out, None), (z_down1b.out, None), early=True)
    s7 = Scatter(k, [hid_load.buf], [w_down1], mid_load.buf, low=True)
    y_rows = Save(k, s7.out)
    t_x, t_y = x_move(k, d_x.out, 1), x_move(k, y_rows.out, 0)
    k.early += [q_up0.load, q_down0.load]
    k.early += [v.load for v in (e_down1, e_gate1, e_out1, e_in1)]
    k.do(r_gate0.send, rows.wait, g14.begin, q_up0.send, q_down0.send)
    k.do(e_down1.send, e_gate1.send, e_out1.send, e_in1.send, g14.loop)
    k.do(y_load.wait, p_out0.run, p_out0.wait, r_out0.send, q_up0.step)
    k.do(proj.wait, value.wait, taps.wait, back.run, q_down0.step, a_load.wait)
    k.do(p_in0.run, p_cols.run, p_in0.wait, r_in0.send, p_cols.wait, r_cols.send)
    k.do(r_gate0.wait, q_gate0.add, x_load.wait, gain_load.wait, s15.loop, q_up0.step)
    k.do(q_down0.step, s15.finish, d_x.start, fill_small, d_x.wait, t_x.send)
    k.do(small_out.wait, t_small.send, q_gate0.step, hid_load.wait, mid_load.wait, s7.loop)
    k.do(r_out0.wait, q_out0.add, r_in0.wait, q_in0.add)
    k.do(r_cols.wait, q_cols.add, q_up0.wait, m_up0.send, q_down0.wait, e_down0.add)
    k.do(s7.finish, y_rows.start, y_rows.wait, t_y.send)
    k.do(q_gate0.step, q_out0.step, q_in0.step, q_cols.step, t_small.wait, z_small.add)
    k.do(q_gate0.wait, e_gate0.add, q_out0.step, q_in0.step, q_cols.step)
    k.do(z_small.wait, t_total.add, q_out0.wait, e_out0.add, q_in0.wait, e_in0.add)
    rest = (e_down1, e_gate1, e_out1, e_in1, q_cols, e_down0, e_gate0, m_up0, e_out0, e_in0)
    k.do(*wait(*rest, t_total, t_x, t_y))
    k.build()

    owned = [
        ([e_in0], [e_in1], 1),
        ([e_out0], [e_out1], 1),
        ([e_gate0], [e_gate1], 1),
        ([q_up0, m_up0], [q_up1, m_up1], 1),
        ([e_down0], [e_down1], 1),
        ([q_cols], [q_cols], 0),
    ]
    return pack(
        [(zero, one, lead) for zero, one, lead in owned], t_total, d_x.out, y_rows.out, t_x, t_y,
        (norm_gain.shape, conv_kernel.shape, qk_gain.shape),
    )


def slot_free(val, shape):
    value = val.out.array
    if value.ndim == 3 and value.shape[0] * value.shape[1] != shape[0]:
        value = jnp.sum(value.astype(F32), axis=0).astype(BF)
    return value.reshape(shape)


def pack_kernel(plan, *refs):
    n_in, leads, terms, tap_rows = plan
    ins, rest = refs[:n_in], refs[n_in:]
    result, gain_out, *grads, cols, taps, heads = rest[: len(leads) + 4]
    grads = [*grads, cols]
    room = iter(rest[len(leads) + 4 :])
    own_v, moved_v, small_v, *bufs = (next(room) for _ in range(3 + len(terms)))
    out_v = [next(room) for _ in leads]
    load_sem, store_sem = room
    s, t = lax.axis_index("section"), lax.axis_index("tensor")
    small, d_x, y_rows, moved, moved_y, *parts = ins

    def either(cond, zero, one, dst, sem):
        if zero is not None:
            pl.when(cond)(pltpu.make_async_copy(zero, dst, sem).start)
        if one is not None:
            pl.when(jnp.logical_not(cond))(pltpu.make_async_copy(one, dst, sem).start)

    first = s == 0
    either(first, d_x, y_rows, own_v, load_sem.at[0])
    either(first, moved, moved_y, moved_v, load_sem.at[1])
    pltpu.make_async_copy(small, small_v, load_sem.at[2]).start()
    for j, (zero, one, _) in enumerate(terms):
        either(
            first,
            None if zero is None else parts[zero],
            None if one is None else parts[one],
            bufs[j],
            load_sem.at[3 + j],
        )
    for j, (zero, one, i) in enumerate(terms):
        arrive = pltpu.make_async_copy(parts[one if zero is None else zero], bufs[j], load_sem.at[3 + j])
        begins = j == 0 or terms[j - 1][2] != i

        def put(j=j, i=i, begins=begins):
            value = bufs[j][...].astype(F32)
            value = value if begins else out_v[i][...] + value
            out_v[i][...] = value

        if zero is None or one is None:
            cond = first if one is None else jnp.logical_not(first)

            @pl.when(cond)
            def _(arrive=arrive, put=put):
                arrive.wait()
                put()
        else:
            arrive.wait()
            put()
        if j + 1 == len(terms) or terms[j + 1][2] != i:
            dst = grads[i].at[0] if leads[i] else grads[i]
            pltpu.make_async_copy(out_v[i], dst, store_sem.at[i]).start()
    pltpu.make_async_copy(d_x, own_v, load_sem.at[0]).wait()
    pltpu.make_async_copy(moved, moved_v, load_sem.at[1]).wait()
    n = len(leads)
    stores = [
        pltpu.make_async_copy(own_v, result.at[0, s], store_sem.at[n]),
        pltpu.make_async_copy(moved_v, result.at[0, 1 - s], store_sem.at[n + 1]),
    ]
    for store in stores:
        store.start()
    pltpu.make_async_copy(small, small_v, load_sem.at[2]).wait()
    total = small_v[0]
    for i in range(1, small_v.shape[0]):
        total = total + small_v[i]
    gain_out[0] = jnp.where(first, total[0:2], total[2:4])
    channels, size = taps.shape[1], heads.shape[1]
    chosen = total[4 : 4 + tap_rows, 0:channels]
    for i in range(1, total.shape[1] // channels):
        chosen = jnp.where(t == i, total[4 : 4 + tap_rows, i * channels : (i + 1) * channels], chosen)
    taps[...] = chosen
    at = 0
    for row, width in enumerate((channels, channels // 2)):
        value = total[7:8, at : at + size]
        for i in range(1, width // size):
            value = value + total[7:8, at + i * size : at + (i + 1) * size]
        heads[row : row + 1, :] = value
        at += width
    for i, store in enumerate(leads):
        dst = grads[i].at[0] if store else grads[i]
        pltpu.make_async_copy(out_v[i], dst, store_sem.at[i]).wait()
    for store in stores:
        store.wait()


def pack(owned, small, d_x, y_rows, moved_x, moved_y, shapes):
    gain_shape, tap_shape, head_shape = shapes
    parts, terms, leads, out_shapes = [], [], [], []
    for i, (zero, one, lead) in enumerate(owned):
        whole = zero[0].out.shape
        if lead and len(whole) == 3 and isinstance(zero[0], Finish):
            shape = (whole[0] * whole[1], whole[2])
        else:
            shape = whole[-2:]
        shape = tuple(shape)
        leads.append(lead)
        out_shapes.append(shape)
        for j in range(max(len(zero), len(one))):
            pair = []
            for side in (zero, one):
                if j < len(side):
                    parts.append(slot_free(side[j], shape))
                    pair.append(len(parts) - 1)
                else:
                    pair.append(None)
            terms.append((*pair, i))
    operands = [v.array for v in (small.out, d_x, y_rows, moved_x.out, moved_y.out)] + parts
    rows = d_x.shape
    smem = pl.BlockSpec(memory_space=pltpu.VMEM)
    out_shape = [jax.ShapeDtypeStruct((1, 2) + rows, BF), jax.ShapeDtypeStruct(gain_shape, F32)]
    out_shape += [
        jax.ShapeDtypeStruct((1,) + v if lead else v, F32) for v, lead in zip(out_shapes, leads)
    ]
    out_shape += [jax.ShapeDtypeStruct(v, F32) for v in (tap_shape, head_shape)]
    n = len(leads)
    return tuple(
        pl.pallas_call(
            functools.partial(
                pack_kernel, (len(operands), tuple(leads), tuple(terms), tap_shape[0])
            ),
            out_shape=out_shape,
            in_specs=[ANY] * len(operands),
            out_specs=[ANY, smem] + [ANY] * n + [smem] * 2,
            scratch_shapes=[pltpu.VMEM(rows, BF)] * 2
            + [pltpu.VMEM(small.out.shape, F32)]
            + [pltpu.VMEM(out_shapes[i], BF) for _, _, i in terms]
            + [pltpu.VMEM(v, F32) for v in out_shapes]
            + [DMA((3 + len(terms),)), DMA((n + 2,))],
            compiler_params=pltpu.CompilerParams(vmem_limit_bytes=VMEM_BYTES),
            name="pack",
        )(*operands)
    )


def solution(mesh):
    in_specs = (
        P("section", "dp", "tensor", None),
        P("section", None, None),
        P("section", "dp", "tensor"),
        P("section", "tensor", "dp"),
        P("section", "dp", "tensor"),
        P("section", "dp", "tensor"),
        P("section", "tensor", "dp"),
        P(("section", "dp"), "tensor"),
        P(None, "tensor"),
        P(),
    )
    out_specs = (
        P("section", "dp", "tensor", None),
        P("section", None, None),
        P("section", "dp", "tensor"),
        P("section", "tensor", "dp"),
        P("section", "dp", "tensor"),
        P("section", "dp", "tensor"),
        P("section", "tensor", "dp"),
        P(("section", "dp"), "tensor"),
        P(None, "tensor"),
        P(),
    )
    return jax.shard_map(body, mesh=mesh, in_specs=in_specs, out_specs=out_specs, check_vma=False)
```

```python
import functools

import jax
import jax.numpy as jnp
from jax import lax
from jax.experimental import pallas as pl
from jax.experimental.pallas import tpu as pltpu
from jax.sharding import PartitionSpec as P

HEADS = 16
KV_HEADS = 8

EPS = 1e-05
ROPE_BASE = 1000000.0
MASKED = -1e30

MESH = pl.DeviceIdType.MESH
ANY = pl.BlockSpec(memory_space=pl.ANY)
DMA = pltpu.SemaphoreType.DMA
VMEM_BYTES = 63 * 1024 * 1024
BF = jnp.bfloat16
F32 = jnp.float32
ROW_BLOCK = 256


def contract(left_op, right_op, left_dim, right_dim):
    return lax.dot_general(
        left_op, right_op, (((left_dim,), (right_dim,)), ((), ())), preferred_element_type=F32
    )


def norm_rows(values, gain):
    return values * lax.rsqrt(jnp.mean(values * values, axis=-1, keepdims=True) + EPS) * gain


def norm_back(values, gain, grad_in):
    row_scale = lax.rsqrt(jnp.mean(values * values, axis=-1, keepdims=True) + EPS)
    normed = values * row_scale
    gain_grad = jnp.sum(grad_in * normed, axis=0, keepdims=True)
    scaled = grad_in * gain
    value_grad = row_scale * (scaled - normed * jnp.mean(scaled * normed, axis=-1, keepdims=True))
    return (value_grad, gain_grad)


class Angles:
    def __init__(self, k, length, head_size, width):
        self.half = head_size // 2
        self.tables = [k.vmem((length, width), F32) for _ in range(2)]
        self.saves = [Save(k, v) for v in self.tables]

    def run(self):
        cos, sin = self.tables
        shape = (ROW_BLOCK, cos.shape[1])
        column = (lax.broadcasted_iota(jnp.int32, shape, 1) % self.half).astype(F32)
        frequency = ROPE_BASE ** (-(column / self.half))
        row = lax.broadcasted_iota(jnp.int32, shape, 0)

        def step(i, carry):
            rows = block_of(i, ROW_BLOCK)
            angle = (row + i * ROW_BLOCK).astype(F32) * frequency
            cos.ref[rows, :] = jnp.cos(angle)
            sin.ref[rows, :] = jnp.sin(angle)
            return carry

        lax.fori_loop(0, cos.shape[0] // ROW_BLOCK, step, 0)
        for save in self.saves:
            save.start()


def silu_parts(gate):
    sig = 1.0 / (1.0 + jnp.exp(-gate))
    return sig, gate * sig


def chunked(rows, step):
    size = next((n for n in (32, 16) if rows % n == 0), rows)
    if size == rows:
        step(pl.ds(0, rows))
    else:
        lax.fori_loop(0, rows // size, lambda i, c: step(block_of(i, size)) or c, 0)


def dp_size():
    return lax.axis_size("dp")


def spot():
    return tuple(lax.axis_index(a) for a in ("section", "dp", "tensor"))


def block_of(index, size):
    return pl.ds(pl.multiple_of(index * size, size), size)


class Val:
    def __init__(self, shape, dtype):
        self.shape, self.dtype = tuple(shape), dtype
        self.ref = self.array = None


class Kernel:
    def __init__(self, cid):
        self.cid, self.ins, self.arrays, self.outs, self.room = cid, [], [], [], []
        self.early, self.steps, self.late, self.axes = [], [], [], set()
        self.once = []

    def input(self, array):
        array = array.array if isinstance(array, Val) else array
        for val, known in zip(self.ins, self.arrays):
            if known is array:
                return val
        val = Val(array.shape, array.dtype)
        self.ins.append(val)
        self.arrays.append(array)
        return val

    def output(self, shape, dtype):
        val = Val(shape, dtype)
        self.outs.append(val)
        return val

    def vmem(self, shape, dtype):
        val = Val(shape, dtype)
        self.room.append((val, pltpu.VMEM(tuple(shape), dtype)))
        return val

    def sem(self, *shape):
        val = Val(shape, None)
        self.room.append((val, DMA(shape)))
        return val

    def do(self, *steps):
        self.steps += steps

    def body(self, *refs):
        vals = self.ins + self.outs + [val for val, _ in self.room]
        for val, ref in zip(vals, refs):
            val.ref = ref
        for item in self.once:
            item.waited = False
            item.phase = 0
        for step in self.early:
            step()
        self.greet()
        for step in self.steps + self.late:
            step()

    def greet(self):
        s, d, t = spot()
        _, sib, cross, diag = places()
        barrier = pltpu.get_barrier_semaphore()
        peers = [{"tensor": sib}, {"tensor": cross}]
        if "tensor" in self.axes:
            peers.append({"tensor": diag})
        if "section" in self.axes:
            peers.append({"section": 1 - s})
        if "dp" in self.axes:
            peers += [{"dp": (d + i) % dp_size()} for i in range(1, dp_size())]

        def signal(peer):
            pl.semaphore_signal(barrier, inc=1, device_id=peer, device_id_type=MESH)

        for peer in peers:
            signal(peer)
        expected = len(peers)
        if "line" in self.axes and "dp" not in self.axes:
            pl.when(d < 3)(lambda: signal({"dp": (d + 1) % 4}))
            pl.when(d > 0)(lambda: signal({"dp": (d + 3) % 4}))
            expected = expected + (d + 2) // 3 + (5 - d) // 3
        pl.semaphore_wait(barrier, expected)

    def build(self):
        result = pl.pallas_call(
            self.body,
            out_shape=[jax.ShapeDtypeStruct(v.shape, v.dtype) for v in self.outs],
            in_specs=[ANY] * len(self.ins),
            out_specs=[ANY] * len(self.outs),
            scratch_shapes=[room for _, room in self.room],
            compiler_params=pltpu.CompilerParams(
                collective_id=self.cid, has_side_effects=True, vmem_limit_bytes=VMEM_BYTES
            ),
            name=f"stage{self.cid}",
        )(*self.arrays)
        for val, array in zip(self.outs, result):
            val.array = array


def remote(src, dst, send_sem, recv_sem, peer):
    return pltpu.make_async_remote_copy(
        src_ref=src, dst_ref=dst, send_sem=send_sem, recv_sem=recv_sem,
        device_id=peer, device_id_type=MESH,
    )


class Load:
    def __init__(self, k, sources, shape, dtype, early=False):
        self.k, self.sources, self.waited = k, sources, False
        self.buf, self.sem = k.vmem(shape, dtype), k.sem(1)
        k.once.append(self)
        if early:
            k.early.append(self.start)

    def moves(self):
        for cond, source in self.sources(*spot()):
            yield cond, pltpu.make_async_copy(source, self.buf.ref, self.sem.ref.at[0])

    def start(self):
        for cond, move in self.moves():
            if cond is None:
                move.start()
            else:
                pl.when(cond)(move.start)

    def wait(self):
        if not self.waited:
            self.waited = True
            next(self.moves())[1].wait()


def load_all(k, array, early=True):
    val = k.input(array)
    return Load(k, lambda s, d, t: [(None, val.ref)], val.shape, val.dtype, early)


class Save:
    def __init__(self, k, buf):
        self.buf, self.out, self.sem = buf, k.output(buf.shape, buf.dtype), k.sem(1)
        self.waited = False
        k.once.append(self)
        k.late.append(self.wait)

    def move(self):
        return pltpu.make_async_copy(self.buf.ref, self.out.ref, self.sem.ref.at[0])

    def start(self):
        self.move().start()

    def wait(self):
        if not self.waited:
            self.waited = True
            self.move().wait()


class Task:
    final = None

    def __init__(self, k, out, axis, moves, count, n_local=1, out_dtype=BF):
        self.k, self.axis, self.make = k, axis, moves
        self.out = k.output(out, out_dtype)
        self.send_sem, self.recv_sem, self.local_sem = k.sem(count), k.sem(count), k.sem(n_local)
        self.waited = False
        k.axes.add(axis)
        k.once.append(self)

    def local(self, src, dst, i):
        return pltpu.make_async_copy(src, dst, self.local_sem.ref.at[i])

    def pairs(self, every):
        far, near = self.make(*spot())
        for i, (sources, dst, peer) in enumerate(far):
            for cond, src in sources if every else sources[:1]:
                yield cond, True, remote(
                    src, dst, self.send_sem.ref.at[i], self.recv_sem.ref.at[i], peer
                )
        for i, (sources, dst) in enumerate(near):
            for cond, src in sources if every else sources[:1]:
                yield cond, False, self.local(src, dst, i)

    def step(self):
        pass

    def send(self):
        for cond, far, move in self.pairs(True):
            if far and self.final is not None:
                cond = lax.axis_index("section") == 1 - self.final
            if cond is None:
                move.start()
            else:
                pl.when(cond)(move.start)

    def wait(self):
        if self.waited:
            return
        self.waited = True
        s = lax.axis_index("section")
        for _, far, move in self.pairs(False):
            if not far:
                move.wait()
            elif self.final is None:
                move.wait_recv()
                move.wait_send()
            else:
                pl.when(s == 1 - self.final)(move.wait_send)
                pl.when(s == self.final)(move.wait_recv)


class Part:
    def __init__(self, base, start, rows):
        self.base, self.start, self.rows = base, start, rows
        self.shape, self.dtype = (rows,) + tuple(base.shape[1:]), base.dtype
        self.array = None

    @property
    def ref(self):
        return self.base.ref.at[pl.ds(self.start, self.rows)]


def as_val(k, value):
    if isinstance(value, Part):
        return Part(as_val(k, value.base), value.start, value.rows)
    value = value.out if isinstance(value, Task) else value
    known = isinstance(value, Val) and (value.array is None)
    return value if known else k.input(value)


class Line(Task):
    def __init__(self, k, out, out_dtype=BF, n_local=1):
        super().__init__(k, out, "line", None, 6, n_local, out_dtype)
        self.send_sem, self.recv_sem = k.sem(2, 3), k.sem(2, 3)
        self.phase = 0

    def hop(self, j, way, src, dst):
        d = lax.axis_index("dp")
        peer = {"dp": (d + 1 if way == 0 else d + 3) % 4}
        return remote(src, dst, self.send_sem.ref.at[way, j], self.recv_sem.ref.at[way, j], peer)


class LineGather(Line):
    def __init__(self, k, sources, shape, dtype):
        super().__init__(k, (4,) + shape, dtype)
        self.sources = sources

    def ends(self, j, way):
        d = lax.axis_index("dp")
        if way == 0:
            return (d >= j) & (d < 3), d >= j + 1
        return (d <= 3 - j) & (d > 0), d <= 2 - j

    def copy(self, j, way, src=None):
        d = lax.axis_index("dp")
        slot = (d + 4 - j if way == 0 else d + j) % 4
        piece = self.out.ref.at[slot]
        return self.hop(j, way, piece if src is None else src, piece)

    def send(self):
        self.phase = 0
        for cond, src in self.sources(*spot()):
            own = self.local(src, self.out.ref.at[lax.axis_index("dp")], 0)
            moves = [(True if cond is None else cond, own)]
            for way in range(2):
                sends = self.ends(0, way)[0]
                moves.append((sends if cond is None else sends & cond, self.copy(0, way, src)))
            for when, move in moves:
                if when is True:
                    move.start()
                else:
                    pl.when(when)(move.start)

    def arrive(self, j):
        for way in range(2):
            pl.when(self.ends(j, way)[1])(self.copy(j, way).wait_recv)

    def step(self):
        self.arrive(self.phase)
        self.phase += 1
        for way in range(2):
            pl.when(self.ends(self.phase, way)[0])(self.copy(self.phase, way).start)

    def wait(self):
        if self.waited:
            return
        self.waited = True
        while self.phase < 2:
            self.step()
        self.arrive(2)
        for j in range(3):
            for way in range(2):
                pl.when(self.ends(j, way)[0])(self.copy(j, way).wait_send)
        d = lax.axis_index("dp")
        self.local(self.sources(*spot())[0][1], self.out.ref.at[d], 0).wait()


def z_gather_from(k, sources, shape, dtype):
    count = dp_size()
    if count == 4:
        return LineGather(k, sources, shape, dtype)

    def moves(s, d, t):
        dst, found = task.out.ref.at[d], sources(s, d, t)
        return [(found, dst, {"dp": (d + i) % count}) for i in range(1, count)], [(found, dst)]

    task = Task(k, (count,) + shape, "dp", moves, count - 1, out_dtype=dtype)
    return task


def z_gather(k, value):
    val = as_val(k, value)
    return z_gather_from(k, lambda s, d, t: [(None, val.ref)], val.shape, val.dtype)


def z_gather_half(k, shard, moved, block):
    shard, moved = as_val(k, shard), as_val(k, moved)
    rows = shard.shape[0] // 2

    def sources(s, d, t):
        own = shard.ref.at[pl.ds(block * rows, rows)]
        return [(s == block, own), (s == 1 - block, moved.ref)]

    return z_gather_from(k, sources, moved.shape, shard.dtype)


def one_way(task, sender):
    task.final = None if sender is None else 1 - sender
    return task


def z_gather_whole(k, shard, moved, block, half=None):
    shard, moved = as_val(k, shard), as_val(k, moved)
    rows = shard.shape[0] if half is None else shard.shape[0] // 2
    part = pl.ds(0 if half is None else half * rows, rows)

    def sources(s, d, t):
        return [(s == block, shard.ref.at[part]), (s == 1 - block, moved.ref.at[part])]

    return z_gather_from(k, sources, (rows,) + shard.shape[1:], shard.dtype)


def x_move(k, value, sender=None):
    val = as_val(k, value)

    def moves(s, d, t):
        return [([(None, val.ref)], task.out.ref, {"section": 1 - s})], []

    task = Task(k, val.shape, "section", moves, 1, out_dtype=val.dtype)
    return one_way(task, sender)


def x_half(k, value, sender=None):
    val = as_val(k, value)
    rows = val.shape[0] // 2

    def moves(s, d, t):
        src = val.ref.at[block_of(1 - s, rows)]
        return [([(None, src)], task.out.ref, {"section": 1 - s})], []

    task = Task(k, (rows,) + val.shape[1:], "section", moves, 1, out_dtype=val.dtype)
    return one_way(task, sender)


def x_slots(k, value, kind):
    val, count = as_val(k, value), dp_size()
    rows = val.shape[0] // (2 * count)

    def moves(s, d, t):
        far = []
        for i in range(count):
            slot = 2 * i + 1 - s if kind == "rows" else (1 - s) * count + i
            src = val.ref.at[block_of(slot, rows)]
            far.append(([(None, src)], task.out.ref.at[i], {"section": 1 - s}))
        return far, []

    task = Task(k, (count, rows) + val.shape[1:], "section", moves, count)
    return task


class Terms:
    def __init__(self, k, kind, grads, received, local):
        self.grads, self.local = as_val(k, grads), local
        self.kind, self.n = kind, dp_size()
        self.whole = received is None
        if self.whole:
            rows, cols = self.grads.shape
            self.rows = rows if kind == "cols" else rows // self.n
            self.cols = cols // self.n if kind == "cols" else cols
            self.shape = (self.n, self.rows, self.cols)
            self.aside = kind == "cols" and self.cols % 128 != 0
            self.total = k.vmem(self.shape, BF)
            self.kept = k.vmem(self.grads.shape, BF) if self.aside else self.total
            return
        self.received = as_val(k, received)
        if kind == "cols":
            self.rows, self.cols = self.grads.shape[0] // 2, self.grads.shape[1] // self.n
            held = (self.rows, self.grads.shape[1])
        else:
            self.rows, self.cols = self.grads.shape[0] // (2 * self.n), self.grads.shape[1]
            held = (self.n, self.rows, self.cols)
        self.kept, self.got = k.vmem(held, BF), k.vmem(held, BF)
        self.shape = (self.n, self.rows, self.cols)
        self.total = k.vmem(self.shape, BF) if kind == "cols" else self.kept

    def loads(self):
        s, grads, kept = lax.axis_index("section"), self.grads.ref, self.kept.ref
        if self.whole and self.aside:
            return [self.local(grads, kept, 2)]
        if self.whole:
            parts = [
                grads.at[:, pl.ds(i * self.cols, self.cols)]
                if self.kind == "cols"
                else grads.at[block_of(i, self.rows)]
                for i in range(self.n)
            ]
            return [self.local(part, kept.at[i], 2 + i) for i, part in enumerate(parts)]
        if self.kind == "cols":
            moves = [self.local(grads.at[block_of(s, self.rows)], kept, 2)]
        else:
            moves = []
            for i in range(self.n):
                slot = 2 * i + s if self.kind == "rows" else s * self.n + i
                moves.append(self.local(grads.at[block_of(slot, self.rows)], kept.at[i], 2 + i))
        return moves + [self.local(self.received.ref, self.got.ref, 1)]

    def load(self):
        for move in self.loads():
            move.start()

    def add(self):
        for move in self.loads():
            move.wait()
        if self.whole and self.aside:
            for i in range(self.n):
                self.total.ref[i] = self.kept.ref[:, i * self.cols : (i + 1) * self.cols]
        if self.whole:
            return
        kept, got, total = self.kept.ref, self.got.ref, self.total.ref
        if self.kind != "cols":

            def piece(i, carry):
                chunked(self.rows, lambda at: total.__setitem__(
                    (i, at), (kept[i, at, :].astype(F32) + got[i, at, :].astype(F32)).astype(BF)
                ))
                return carry

            lax.fori_loop(0, self.n, piece, 0)
            return

        def add_rows(at):
            for i in range(self.n):
                part = slice(i * self.cols, (i + 1) * self.cols)
                value = kept[at, part].astype(F32) + got[at, part].astype(F32)
                total[i, at, :] = value.astype(BF)

        chunked(self.rows, add_rows)


class DirectScatter(Task):
    def __init__(self, k, kind, grads, received):
        self.terms = Terms(k, kind, grads, received, lambda *a: self.local(*a))
        count = dp_size()

        def moves(s, d, t):
            total = self.terms.total.ref
            far = []
            for i in range(1, count):
                other = (d + i) % count
                far.append(([(None, total.at[other])], self.out.ref.at[d], {"dp": other}))
            return far, [([(None, total.at[d])], self.out.ref.at[d])]

        super().__init__(k, self.terms.shape, "dp", moves, count - 1, 2 + count)
        self.load = self.terms.load

    def send(self):
        self.terms.add()
        super().send()

    def add(self):
        self.load()
        self.send()


class LineScatter(Line):
    def __init__(self, k, kind, grads, received):
        self.terms = Terms(k, kind, grads, received, lambda *a: self.local(*a))
        super().__init__(k, self.terms.shape[1:], BF, 6)
        self.got = k.vmem((2, 3) + self.terms.shape[1:], BF)
        self.load = self.terms.load

    def ends(self, j, way):
        d = lax.axis_index("dp")
        if way == 0:
            return (d <= j) & (d < 3), (d >= 1) & (d <= j + 1)
        return (d >= 3 - j) & (d > 0), (d <= 2) & (d >= 2 - j)

    def copy(self, j, way):
        d = lax.axis_index("dp")
        to = (d + 3 - j if way == 0 else d + 1 + j) % 4
        return self.hop(j, way, self.terms.total.ref.at[to], self.got.ref.at[way, j])

    def send(self):
        self.phase = 0
        self.terms.add()
        for way in range(2):
            pl.when(self.ends(0, way)[0])(self.copy(0, way).start)

    def take(self, j, way):
        d = lax.axis_index("dp")
        to = (d + 2 - j if way == 0 else d + 2 + j) % 4
        self.copy(j, way).wait_recv()
        total, got = self.terms.total.ref, self.got.ref

        def add_rows(at):
            value = total[to, at, :].astype(F32) + got[way, j, at, :].astype(F32)
            total[to, at, :] = value.astype(BF)

        chunked(self.terms.rows, add_rows)

    def arrive(self, j):
        for way in range(2):
            pl.when(self.ends(j, way)[1])(functools.partial(self.take, j, way))

    def step(self):
        self.arrive(self.phase)
        self.phase += 1
        for way in range(2):
            pl.when(self.ends(self.phase, way)[0])(self.copy(self.phase, way).start)

    def wait(self):
        if self.waited:
            return
        self.waited = True
        while self.phase < 2:
            self.step()
        self.arrive(2)
        done = self.local(self.terms.total.ref.at[lax.axis_index("dp")], self.out.ref, 0)
        done.start()
        for j in range(3):
            for way in range(2):
                pl.when(self.ends(j, way)[0])(self.copy(j, way).wait_send)
        done.wait()

    def add(self):
        self.load()
        self.send()


def sum_scatter(k, kind, grads, received=None):
    return (LineScatter if dp_size() == 4 else DirectScatter)(k, kind, grads, received)


class Finish(Task):
    def __init__(self, k, pieces, block):
        self.pieces, self.final = as_val(k, pieces), block
        *slots, rows, cols = self.pieces.shape
        self.slots = slots[0] if slots else 0
        if slots:
            self.held, self.total = k.vmem(self.pieces.shape, BF), k.vmem((rows, cols), BF)
        else:
            self.total = self.pieces

        def moves(s, d, t):
            source, dst = [(None, self.total.ref)], self.out.ref.at[s]
            return [(source, dst, {"section": 1 - s})], [(source, dst)]

        super().__init__(k, (2, rows, cols), "section", moves, 1, 2)

    def load(self):
        if self.slots:
            self.local(self.pieces.ref, self.held.ref, 1).start()

    def send(self):
        if self.slots:
            self.local(self.pieces.ref, self.held.ref, 1).wait()
            acc = self.held.ref[0].astype(F32)
            for i in range(1, self.slots):
                acc = acc + self.held.ref[i].astype(F32)
            self.total.ref[...] = acc.astype(BF)
        super().send()

    def add(self):
        self.load()
        self.send()


class SumShare(Task):
    def __init__(self, k, terms, axis, slotted=False):
        self.terms = [as_val(k, v) for v in terms]
        shape = self.terms[0].shape[1:] if slotted else self.terms[0].shape
        count = dp_size() if axis == "dp" else 4
        self.slotted = slotted
        self.bufs = [k.vmem(v.shape, F32) for v in self.terms]
        self.total = k.vmem(shape, F32)

        def moves(s, d, t):
            source, me = [(None, self.total.ref)], d if axis == "dp" else t
            dst = self.out.ref.at[me]
            far = [(source, dst, {axis: (me + i) % count}) for i in range(1, count)]
            return far, [(source, dst)]

        super().__init__(k, (count,) + shape, axis, moves, count - 1, 3, out_dtype=F32)

    def add(self):
        loads = [self.local(v.ref, b.ref, 1 + i) for i, (v, b) in enumerate(zip(self.terms, self.bufs))]
        for load in loads:
            load.start()
        for load in loads:
            load.wait()
        if self.slotted:
            parts = [self.bufs[0].ref[i] for i in range(self.terms[0].shape[0])]
        else:
            parts = [buf.ref[...] for buf in self.bufs]
        acc = parts[0]
        for part in parts[1:]:
            acc = acc + part
        self.total.ref[...] = acc
        self.send()


class Weight:
    def __init__(self, k, kind, *segments, early=False):
        self.kind, self.waited = kind, False
        self.segments, start = [], 0
        for near, far in segments:
            near, far = as_val(k, near), None if far is None else as_val(k, far)
            self.segments.append((near, far, start))
            start += near.shape[1] * (1 if far is None else 2)
        self.count, _, self.cols = self.segments[0][0].shape
        self.rows = start
        if kind == "cols":
            shape = (self.rows, self.count * self.cols)
        else:
            shape = (self.count * self.rows, self.cols)
        self.aside = kind == "cols" and self.cols % 128 != 0
        self.buf = k.vmem(shape, BF)
        sides = [v for near, far, _ in self.segments for v in (near, far) if v is not None]
        self.sem = k.sem(len(sides), self.count)
        if self.aside:
            self.held = [k.vmem(v.shape, BF) for v in sides]
        k.once.append(self)
        if early:
            k.early.append(self.start)

    def sides(self):
        s = lax.axis_index("section")
        for near, far, start in self.segments:
            rows = near.shape[1]
            if far is None:
                yield near, start, None
            else:
                yield near, start + s * rows, s
                yield far, start + (1 - s) * rows, 1 - s

    def moves(self):
        dst = self.buf.ref
        for j, (val, start, sec) in enumerate(self.sides()):
            rows = val.shape[1]
            for i in range(self.count):
                if self.aside:
                    to = self.held[j].ref.at[i]
                elif self.kind == "cols":
                    at = pl.ds(pl.multiple_of(start, 16), rows)
                    to = dst.at[at, pl.ds(i * self.cols, self.cols)]
                else:
                    top = (sec * self.count + i) * rows if self.kind == "conv" else i * self.rows + start
                    to = dst.at[pl.ds(pl.multiple_of(top, 16), rows)]
                yield pltpu.make_async_copy(val.ref.at[i], to, self.sem.ref.at[j, i])

    def start(self):
        for move in self.moves():
            move.start()

    def wait(self):
        if self.waited:
            return
        self.waited = True
        for move in self.moves():
            move.wait()
        if self.aside:
            for j, (val, start, _) in enumerate(self.sides()):
                whole = jnp.concatenate([self.held[j].ref[i] for i in range(self.count)], axis=1)
                self.buf.ref[pl.ds(pl.multiple_of(start, 16), val.shape[1]), :] = whole


class Product:
    def __init__(self, k, left, right):
        self.left, self.right = left, right
        rows = left.shape[1]
        self.chunk = 384 if rows % 384 == 0 else 256
        self.count = rows // self.chunk
        self.buf = k.vmem((rows, right.shape[1]), BF)
        self.out, self.sem = k.output(self.buf.shape, BF), k.sem(self.count)

    def copy(self, i):
        part = block_of(i, self.chunk)
        return pltpu.make_async_copy(self.buf.ref.at[part], self.out.ref.at[part], self.sem.ref.at[i])

    def run(self):
        def step(i, carry):
            part = block_of(i, self.chunk)
            value = contract(self.left.ref[:, part], self.right.ref[...], 0, 0)
            self.buf.ref[part, :] = value.astype(BF)
            self.copy(i).start()
            return carry

        lax.fori_loop(0, self.count, step, 0)

    def wait(self):
        for i in range(self.count):
            self.copy(i).wait()


def places():
    me = lax.axis_index("tensor")
    sib = me + 1 - 2 * (me % 2)
    cross = (me + 2) % 4
    diag = (sib + 2) % 4
    return me, sib, cross, diag


class Gather:
    def __init__(self, k, x, gain, weights, extras=(), trans=False, epilogue="plain", save=()):
        rows, width = x.shape
        length = 4 * rows
        self.k, self.x, self.gain, self.weights, self.extras = k, x, gain, weights, extras
        self.trans, self.epilogue, self.rows, self.half = trans, epilogue, rows, rows // 2
        cols = [w.buf.shape[0 if trans else 1] for w in weights]
        kinds = {
            "plain": [(c, F32) for c in cols],
            "ffn": [(cols[0], BF)] * 3,
            "ffn_back": [(cols[0], BF)] * 2,
        }[epilogue]
        self.full = k.vmem((length, width), BF)
        self.values = [k.vmem((length, c), kind) for c, kind in kinds]
        kept = [self.full] + self.values
        self.saved = [(v, k.output(v.shape, v.dtype), k.sem(4, 2)) for v in kept if kept.index(v) in save]
        self.sems = [k.sem(2) for _ in range(6)]
        k.late.append(self.end)

    def span(self, owner, sub):
        return pl.ds(pl.multiple_of(owner * self.rows + sub * self.half, self.half), self.half)

    def move(self, kind, i):
        me, sib, cross, _ = places()
        full = self.full.ref
        owner, peer, at = {"cross": (me, cross, 0), "sib": (me, sib, 2), "relay": (cross, sib, 4)}[kind]
        part = full.at[self.span(owner, i)]
        return remote(
            part, part, self.sems[at].ref.at[i], self.sems[at + 1].ref.at[i], {"tensor": peer}
        )

    def begin(self):
        me = places()[0]
        for i in range(2):

            def put(j, carry):
                at = i * self.half + j * 32
                part = self.x.ref[pl.ds(pl.multiple_of(at, 32), 32), :].astype(F32)
                if self.gain is not None:
                    val, row = self.gain
                    part = norm_rows(part, val.ref[row : row + 1, :])
                self.full.ref[pl.ds(pl.multiple_of(me * self.rows + at, 32), 32), :] = part.astype(BF)
                return carry

            lax.fori_loop(0, self.half // 32, put, 0)
            self.move("cross", i).start()
            self.move("sib", i).start()

    def loop(self):
        me, sib, cross, diag = places()
        rows, half = self.rows, self.half
        for w in self.weights:
            w.wait()

        def step(p, carry):
            far, sub = p // 2, p % 2
            near = (1 - sub) * me + sub * sib
            first = (1 - far) * near * rows + far * (cross * rows + sub * half)
            second = (1 - far) * (near * rows + half) + far * (diag * rows + sub * half)
            pair = [pl.ds(pl.multiple_of(v, half), half) for v in (first, second)]

            @pl.when(p == 1)
            def _():
                self.move("sib", 0).wait_recv()
                self.move("sib", 1).wait_recv()

            for i in range(2):

                @pl.when(p == 2 + i)
                def _():
                    self.move("cross", i).wait_recv()
                    self.move("relay", i).start()
                    self.move("relay", i).wait_recv()

            def both(val):
                return jnp.concatenate([val.ref[pair[0], :], val.ref[pair[1], :]], axis=0)

            a = both(self.full)
            prods = [contract(a, w.buf.ref[...], 1, 1 if self.trans else 0) for w in self.weights]
            if self.epilogue == "plain":
                values = prods
            elif self.epilogue == "ffn":
                sig, silu = silu_parts(prods[0])
                values = [prods[0], prods[1], silu * prods[1]]
            else:
                gate, up = (both(v).astype(F32) for v in self.extras)
                sig, silu = silu_parts(gate)
                values = [prods[0] * up * sig * (1.0 + gate * (1.0 - sig)), prods[0] * silu]
            for val, value in zip(self.values, values):
                value = value.astype(val.dtype)
                for j in range(2):
                    val.ref[pair[j], :] = value[j * half : (j + 1) * half]
            for val, out, sem in self.saved:
                for j in range(2):
                    pltpu.make_async_copy(
                        val.ref.at[pair[j]], out.ref.at[pair[j]], sem.ref.at[p, j]
                    ).start()
            return carry

        lax.fori_loop(0, 4, step, 0)

    def end(self):
        for i in range(2):
            for kind in ("cross", "sib", "relay"):
                self.move(kind, i).wait_send()
        part = pl.ds(0, self.half)
        for val, out, sem in self.saved:
            for p in range(4):
                for j in range(2):
                    pltpu.make_async_copy(val.ref.at[part], out.ref.at[part], sem.ref.at[p, j]).wait()


class Scatter:
    def __init__(self, k, operands, weights, resid, back=None, trans=False, low=False):
        rows, width = resid.shape
        half = rows // 2
        self.operands, self.weights, self.resid, self.back = operands, weights, resid, back
        self.trans, self.low, self.rows, self.half = trans, low, rows, half
        self.keep, self.own = k.vmem((2, half, width), F32), k.vmem((rows, width), F32)
        self.to_s, self.from_s, self.to_c, self.from_c = (
            k.vmem((2, half, width), BF) for _ in range(4)
        )
        self.to_o, self.from_o = k.vmem((rows, width), BF), k.vmem((rows, width), BF)
        self.out = k.vmem((rows, width), BF if low else F32)
        self.gain_grad = k.vmem((1, width), F32) if back else None
        self.sems = [k.sem(2) for _ in range(4)] + [k.sem(1) for _ in range(2)]
        k.late.append(self.end)

    def move(self, kind, i=0):
        _, sib, cross, _ = places()
        at, src, dst, peer = {
            "diag": (0, self.to_s, self.from_s, sib),
            "cross": (2, self.to_c, self.from_c, cross),
            "near": (4, self.to_o, self.from_o, sib),
        }[kind]
        src, dst = (src.ref, dst.ref) if kind == "near" else (src.ref.at[i], dst.ref.at[i])
        return remote(
            src, dst, self.sems[at].ref.at[i], self.sems[at + 1].ref.at[i], {"tensor": peer}
        )

    def pass_on(self, i):
        self.move("diag", i).wait_recv()

        def add_rows(at):
            total = self.keep.ref[i, at, :] + self.from_s.ref[i, at, :].astype(F32)
            self.to_c.ref[i, at, :] = total.astype(BF)

        chunked(self.half, add_rows)
        self.move("cross", i).start()

    def loop(self):
        me, sib, cross, diag = places()
        rows, half = self.rows, self.half
        for w in self.weights:
            w.wait()

        def step(p, carry):
            near, sub = p // 2, p % 2
            base = near * ((1 - sub) * sib + sub * me) * rows
            first = base + (1 - near) * (cross * rows + sub * half)
            second = base + near * half + (1 - near) * (diag * rows + sub * half)
            pair = [pl.ds(pl.multiple_of(v, half), half) for v in (first, second)]
            total = None
            for y, w in zip(self.operands, self.weights):
                a = jnp.concatenate([y.ref[pair[0], :], y.ref[pair[1], :]], axis=0)
                prod = contract(a, w.buf.ref[...], 1, 1 if self.trans else 0)
                total = prod if total is None else total + prod

            self.own.ref[...] = total

            @pl.when(p < 2)
            def _():
                def put(at):
                    self.keep.ref[p, at, :] = self.own.ref[at, :]
                    lower = pl.ds(pl.multiple_of(at.start + half, 16), at.size)
                    self.to_s.ref[p, at, :] = self.own.ref[lower, :].astype(BF)

                chunked(half, put)
                self.move("diag", p).start()

            @pl.when(p == 2)
            def _():
                def put(at):
                    self.to_o.ref[at, :] = self.own.ref[at, :].astype(BF)

                chunked(rows, put)
                self.move("near").start()

            @pl.when((p == 1) | (p == 2))
            def _():
                self.pass_on(p - 1)

            return carry

        lax.fori_loop(0, 4, step, 0)

    def finish(self):
        self.move("near").wait_recv()
        if self.back:
            self.gain_grad.ref[...] = jnp.zeros_like(self.gain_grad.ref)
        for i in range(2):
            self.move("cross", i).wait_recv()

            def add_rows(j, carry):
                inner = pl.ds(pl.multiple_of(j * 32, 32), 32)
                part = pl.ds(pl.multiple_of(i * self.half + j * 32, 32), 32)
                total = self.own.ref[part, :] + self.from_o.ref[part, :].astype(F32)
                total = total + self.from_c.ref[i, inner, :].astype(F32)
                resid = self.resid.ref[part, :].astype(F32)
                if self.back:
                    value, (gain, row) = self.back
                    total, gain_grad = norm_back(
                        value.ref[part, :].astype(F32), gain.ref[row : row + 1, :], total
                    )
                    self.gain_grad.ref[...] += gain_grad
                self.out.ref[part, :] = (resid + total).astype(self.out.dtype)
                return carry

            lax.fori_loop(0, self.half // 32, add_rows, 0)

    def end(self):
        self.move("near").wait_send()
        for i in range(2):
            self.move("diag", i).wait_send()
            self.move("cross", i).wait_send()


def delayed(values, by):
    if by == 0:
        return values
    row = lax.broadcasted_iota(jnp.int32, values.shape, 0)
    return jnp.where(row < by, 0.0, pltpu.roll(values, by, 0))


def advanced(values, by):
    if by == 0:
        return values
    length = values.shape[0]
    row = lax.broadcasted_iota(jnp.int32, values.shape, 0)
    return jnp.where(row >= length - by, 0.0, pltpu.roll(values, length - by, 0))


CONV_COLS = 128


class Conv:
    def __init__(self, k, projected, value, kernel):
        self.projected, self.value, self.kernel = projected, value, kernel
        self.y = k.vmem(value.shape, BF)

    def parts(self, j):
        channels = self.value.shape[1]
        at = block_of(j, CONV_COLS)
        b_gate = self.projected.ref[:, at]
        c_gate = self.projected.ref[:, block_of(j + channels // CONV_COLS, CONV_COLS)]
        x_value, taps = self.value.ref[:, at], self.kernel.ref[:, at]
        product = b_gate * x_value
        count = taps.shape[0]
        causal = jnp.zeros_like(product)
        for i in range(count):
            causal = causal + taps[i : i + 1] * delayed(product, count - 1 - i)
        return at, b_gate, c_gate, x_value, taps, product, causal

    def run(self):
        def step(j, carry):
            at, _, c_gate, _, _, _, causal = self.parts(j)
            self.y.ref[:, at] = (c_gate * causal).astype(BF)
            return carry

        lax.fori_loop(0, self.value.shape[1] // CONV_COLS, step, 0)


class ConvBack(Conv):
    def __init__(self, k, projected, value, kernel, d_y):
        self.projected, self.value, self.kernel, self.d_y = projected, value, kernel, d_y
        self.d_proj = k.vmem(projected.shape, BF)
        self.d_value = k.vmem(value.shape, BF)
        self.d_kernel = k.vmem(kernel.shape, F32)

    def run(self):
        channels = self.value.shape[1]

        def step(j, carry):
            at, b_gate, c_gate, x_value, taps, product, causal = self.parts(j)
            d_y = self.d_y.ref[:, at]
            d_causal = d_y * c_gate
            count = taps.shape[0]
            d_product = jnp.zeros_like(product)
            for i in range(count):
                by = count - 1 - i
                row = jnp.sum(d_causal * delayed(product, by), axis=0, keepdims=True)
                self.d_kernel.ref[i : i + 1, at] = row
                d_product = d_product + taps[i : i + 1] * advanced(d_causal, by)
            self.d_proj.ref[:, at] = (d_product * x_value).astype(BF)
            upper = block_of(j + channels // CONV_COLS, CONV_COLS)
            self.d_proj.ref[:, upper] = (d_y * causal).astype(BF)
            self.d_value.ref[:, at] = (d_product * b_gate).astype(BF)
            return carry

        lax.fori_loop(0, channels // CONV_COLS, step, 0)


def head_mean(values, head_size):
    width = values.shape[1]
    row = lax.broadcasted_iota(jnp.int32, (width, width), 0) // head_size
    col = lax.broadcasted_iota(jnp.int32, (width, width), 1) // head_size
    group = jnp.where(row == col, 1.0 / head_size, 0.0).astype(F32)
    return lax.dot_general(
        values, group, (((1,), (0,)), ((), ())),
        precision=lax.Precision.HIGHEST, preferred_element_type=F32,
    )


def turn(values, head_size, back):
    width, half = values.shape[1], head_size // 2
    lane = lax.broadcasted_iota(jnp.int32, values.shape, 1) % head_size
    upper = pltpu.roll(values, width - half, 1)
    lower = pltpu.roll(values, half, 1)
    return jnp.where(lane < half, upper, -lower) if back else jnp.where(lane < half, -upper, lower)


def head_norm(values, gain, head_size):
    return values * lax.rsqrt(head_mean(values * values, head_size) + EPS) * gain


def head_norm_back(values, gain, grad_in, head_size):
    row_scale = lax.rsqrt(head_mean(values * values, head_size) + EPS)
    normed = values * row_scale
    gain_grad = jnp.sum(grad_in * normed, axis=0, keepdims=True)
    scaled = grad_in * gain
    return row_scale * (scaled - normed * head_mean(scaled * normed, head_size)), gain_grad


def block_weights(q_rows, keys):
    scores = [contract(q_rows, k_rows, 1, 1) for k_rows in keys]
    query = lax.broadcasted_iota(jnp.int32, scores[-1].shape, 0)
    key = lax.broadcasted_iota(jnp.int32, scores[-1].shape, 1)
    scores[-1] = jnp.where(key <= query, scores[-1], MASKED)
    top = functools.reduce(
        jnp.maximum, [jnp.max(part, axis=1, keepdims=True) for part in scores]
    )
    exps = [jnp.exp(part - top) for part in scores]
    scale = 1.0 / sum(jnp.sum(part, axis=1, keepdims=True) for part in exps)
    return [part * scale for part in exps]


def key_blocks(i):
    blocks = [pl.ds(0, i * ROW_BLOCK)] if i else []
    return blocks + [pl.ds(i * ROW_BLOCK, ROW_BLOCK)]


class Heads:
    def __init__(self, projected, tables, size):
        assert size in (16, 64, 256), size
        self.projected, self.size = projected, size
        self.gain, self.cos, self.sin = (v.buf for v in tables)
        self.loads = tables
        self.length, width = projected.shape
        self.q_cols, self.k_cols = width // 2, width // 4
        self.heads, self.kv_heads = self.q_cols // size, self.k_cols // size
        self.share = self.heads // self.kv_heads

    def per_head(self, k, count, kind):
        return k.vmem((count, self.length, self.size), kind)

    def split(self, val, rows, values):
        for h in range(val.shape[0]):
            val.ref[h, rows, :] = values[:, h * self.size : (h + 1) * self.size]

    def join(self, val, rows):
        return jnp.concatenate([val.ref[h, rows, :] for h in range(val.shape[0])], axis=1)

    def angles(self, rows):
        c, n = self.cos.ref[rows, :], self.sin.ref[rows, :]
        repeat = self.q_cols // c.shape[1]
        return jnp.concatenate([c] * repeat, axis=1), jnp.concatenate([n] * repeat, axis=1)

    def blocks(self, step):
        lax.fori_loop(0, self.length // ROW_BLOCK, lambda p, c: step(block_of(p, ROW_BLOCK)) or c, 0)


class Attend(Heads):
    def __init__(self, k, projected, tables, size):
        super().__init__(projected, tables, size)
        self.q_rot = k.vmem((self.length, self.q_cols), BF)
        self.k_rot = k.vmem((self.length, self.k_cols), BF)
        self.y = k.vmem((self.length, self.q_cols), BF)
        self.q_h, self.y_h = (self.per_head(k, self.heads, BF) for _ in range(2))
        self.k_h, self.v_h = (self.per_head(k, self.kv_heads, BF) for _ in range(2))

    def run(self, *between):
        for load in self.loads:
            load.wait()
        size, q_cols, k_cols, proj = self.size, self.q_cols, self.k_cols, self.projected.ref

        def prepare(rows):
            c, n = self.angles(rows)
            q = head_norm(proj[rows, :q_cols], self.gain.ref[0:1, :], size)
            q = (q * c + turn(q, size, False) * n).astype(BF)
            k = head_norm(proj[rows, q_cols : q_cols + k_cols], self.gain.ref[1:2, :k_cols], size)
            k = (k * c[:, :k_cols] + turn(k, size, False) * n[:, :k_cols]).astype(BF)
            self.q_rot.ref[rows, :] = q
            self.k_rot.ref[rows, :] = k
            self.split(self.q_h, rows, (q.astype(F32) * size**-0.5).astype(BF))
            self.split(self.k_h, rows, k)
            self.split(self.v_h, rows, proj[rows, q_cols + k_cols :].astype(BF))

        self.blocks(prepare)

        def head(h, carry):
            g = h // self.share

            @pl.when(h == self.heads // 2)
            def _():
                for step in between:
                    step()

            for i in range(self.length // ROW_BLOCK):
                rows, seen = pl.ds(i * ROW_BLOCK, ROW_BLOCK), key_blocks(i)
                weights = block_weights(
                    self.q_h.ref[h, rows, :], [self.k_h.ref[g, at, :] for at in seen]
                )
                value = sum(
                    contract(part.astype(BF), self.v_h.ref[g, at, :], 1, 0)
                    for part, at in zip(weights, seen)
                )
                self.y_h.ref[h, rows, :] = value.astype(BF)
            return carry

        lax.fori_loop(0, self.heads, head, 0)

        def place(rows):
            self.y.ref[rows, :] = self.join(self.y_h, rows)

        self.blocks(place)


class AttendBack(Heads):
    def __init__(self, k, projected, tables, size, q_rot, k_rot, d_y):
        super().__init__(projected, tables, size)
        self.q_rot, self.k_rot, self.d_y = q_rot, k_rot, d_y
        self.q_h, self.dy_h = (self.per_head(k, self.heads, BF) for _ in range(2))
        self.k_h, self.v_h = (self.per_head(k, self.kv_heads, BF) for _ in range(2))
        self.dq_h = self.per_head(k, self.heads, F32)
        self.dk_h, self.dv_h = (self.per_head(k, self.kv_heads, F32) for _ in range(2))
        self.d_proj = k.vmem(projected.shape, BF)
        self.q_gain, self.k_gain = k.vmem((1, self.q_cols), F32), k.vmem((1, self.k_cols), F32)

    def run(self, *between):
        for load in self.loads:
            load.wait()
        size, q_cols, k_cols, proj = self.size, self.q_cols, self.k_cols, self.projected.ref
        scale = size**-0.5
        dq_h, dk_h, dv_h = self.dq_h.ref, self.dk_h.ref, self.dv_h.ref

        def prepare(rows):
            self.split(self.q_h, rows, (self.q_rot.ref[rows, :].astype(F32) * scale).astype(BF))
            self.split(self.dy_h, rows, self.d_y.ref[rows, :].astype(BF))
            self.split(self.k_h, rows, self.k_rot.ref[rows, :])
            self.split(self.v_h, rows, proj[rows, q_cols + k_cols :].astype(BF))

        self.blocks(prepare)

        def clear(rows):
            for val in (dk_h, dv_h):
                val[:, rows, :] = jnp.zeros((self.kv_heads, ROW_BLOCK, size), F32)

        self.blocks(clear)

        def head(h, carry):
            g = h // self.share

            @pl.when(h == self.heads // 2)
            def _():
                for step in between:
                    step()

            for i in range(self.length // ROW_BLOCK):
                rows, seen = pl.ds(i * ROW_BLOCK, ROW_BLOCK), key_blocks(i)
                q, low = self.q_h.ref[h, rows, :], self.dy_h.ref[h, rows, :]
                keys = [self.k_h.ref[g, at, :] for at in seen]
                probs = block_weights(q, keys)
                d_weights = [contract(low, self.v_h.ref[g, at, :], 1, 1) for at in seen]
                inner = sum(
                    jnp.sum(a * b, axis=1, keepdims=True) for a, b in zip(probs, d_weights)
                )
                d_q = 0.0
                for at, k, prob, d_weight in zip(seen, keys, probs, d_weights):
                    dv_h[g, at, :] += contract(prob.astype(BF), low, 0, 0)
                    d_scores = (prob * (d_weight - inner)).astype(BF)
                    d_q = d_q + contract(d_scores, k, 1, 0)
                    dk_h[g, at, :] += contract(d_scores, q, 0, 0)
                dq_h[h, rows, :] = d_q * scale
            return carry

        lax.fori_loop(0, self.heads, head, 0)
        self.q_gain.ref[...] = jnp.zeros_like(self.q_gain.ref)
        self.k_gain.ref[...] = jnp.zeros_like(self.k_gain.ref)

        def finish(rows):
            c, n = self.angles(rows)
            dq, dk, dv = (self.join(v, rows) for v in (self.dq_h, self.dk_h, self.dv_h))
            dq = dq * c + turn(dq * n, size, True)
            dk = dk * c[:, :k_cols] + turn(dk * n[:, :k_cols], size, True)
            dq, q_sum = head_norm_back(proj[rows, :q_cols], self.gain.ref[0:1, :], dq, size)
            dk, k_sum = head_norm_back(
                proj[rows, q_cols : q_cols + k_cols], self.gain.ref[1:2, :k_cols], dk, size
            )
            self.q_gain.ref[...] += q_sum
            self.k_gain.ref[...] += k_sum
            self.d_proj.ref[rows, :q_cols] = dq.astype(BF)
            self.d_proj.ref[rows, q_cols : q_cols + k_cols] = dk.astype(BF)
            self.d_proj.ref[rows, q_cols + k_cols :] = dv.astype(BF)

        self.blocks(finish)


def body(boundary, norm_gain, mix_in, mix_out, w_gate, w_up, w_down, conv_x, conv_kernel, qk_gain):
    first = lax.axis_index("section") == 0
    tensor_index = lax.axis_index("tensor")
    model_width = boundary.shape[3]
    channels = mix_out.shape[1]
    row_shape = boundary.shape[2:]
    length, size = 4 * row_shape[0], qk_gain.shape[1]

    seqs, own_gain = boundary[0], norm_gain[0]
    sh_in, sh_out, sh_gate, sh_up, sh_down = (v[0] for v in (mix_in, mix_out, w_gate, w_up, w_down))
    head_gain = jnp.tile(qk_gain, (1, channels // size))

    def gains_of(k, block, other, early=True):
        own, moved = k.input(own_gain), as_val(k, other)
        sources = lambda s, d, t: [(s == block, own.ref), (s == 1 - block, moved.ref)]
        return Load(k, sources, own.shape, F32, early)

    def start_rows(k, slot, other, early=True):
        own, moved = k.input(seqs), as_val(k, other)
        sources = lambda s, d, t: [(s == slot, own.ref.at[slot]), (s == 1 - slot, moved.ref)]
        return Load(k, sources, row_shape, BF, early)

    def wait(*items):
        return [item.wait for item in items]

    k = Kernel(0)
    t_seq = None
    seq_val = k.input(seqs)

    def seq_moves(s, d, t):
        return [([(None, seq_val.ref.at[1 - s])], t_seq.out.ref, {"section": 1 - s})], []

    t_in, t_out, t_up = (x_half(k, v) for v in (sh_in, sh_out, sh_up))
    gate_lo, gate_hi = (Part(sh_gate, i * (sh_gate.shape[0] // 2), sh_gate.shape[0] // 2) for i in range(2))
    down_lo, down_hi = (Part(sh_down, i * (sh_down.shape[0] // 2), sh_down.shape[0] // 2) for i in range(2))
    t_gate0a, t_gate0b = x_half(k, gate_lo, 0), x_move(k, gate_hi, 0)
    t_down0a, t_down0b = x_half(k, down_lo, 0), x_move(k, down_hi, 0)
    t_gate1, t_down1 = x_half(k, sh_gate, 1), x_move(k, sh_down, 1)
    t_seq = Task(k, row_shape, "section", seq_moves, 1)
    t_gain, z_cols = x_move(k, own_gain), z_gather(k, conv_x)
    z_in0, z_out0 = z_gather_half(k, sh_in, t_in.out, 0), z_gather_half(k, sh_out, t_out.out, 0)
    z_gate0a = z_gather_half(k, gate_lo, t_gate0a.out, 0)
    z_gate0b, x_gate0a = z_gather_whole(k, gate_hi, t_gate0b.out, 0), x_move(k, z_gate0a.out)
    z_up0 = z_gather_half(k, sh_up, t_up.out, 0)
    x_cols, x_in0, x_out0 = (x_move(k, v.out) for v in (z_cols, z_in0, z_out0))
    x_load, gain_load = start_rows(k, 0, t_seq.out, False), gains_of(k, 0, t_gain.out, False)
    taps = load_all(k, conv_kernel)
    angles = Angles(k, length, size, 128)
    w_in0, w_cols = Weight(k, "rows", (z_in0.out, x_in0.out)), Weight(k, "conv", (z_cols.out, x_cols.out))
    w_out0 = Weight(k, "cols", (z_out0.out, x_out0.out))
    g0 = Gather(k, x_load.buf, (gain_load.buf, 0), [w_in0, w_cols], save=(0, 1, 2))
    conv = Conv(k, g0.values[0], g0.values[1], taps.buf)
    y0 = Save(k, conv.y)
    s1 = Scatter(k, [conv.y], [w_out0], x_load.buf)
    mid0 = Save(k, s1.out)
    k.do(t_in.send, t_out.send, z_cols.send, t_gate0b.send, t_gate0a.send, t_gate1.send)
    k.do(t_gain.send, t_seq.send)
    k.do(t_in.wait, z_in0.send, t_out.wait, z_out0.send, z_cols.step, z_in0.step, z_out0.step)
    k.do(z_cols.step, z_in0.step, z_out0.step, t_gate0b.wait, z_gate0b.send)
    k.do(t_gate0a.wait, z_gate0a.send)
    k.do(z_cols.wait, x_cols.send, z_in0.wait, x_in0.send, z_out0.wait, x_out0.send, t_up.send)
    k.do(t_gain.wait, gain_load.start, t_seq.wait, x_load.start, gain_load.wait, x_load.wait)
    k.do(g0.begin, z_gate0b.step, z_gate0a.step, angles.run, z_gate0b.step, z_gate0a.step)
    k.do(x_cols.wait, w_cols.start, x_in0.wait, w_in0.start, z_gate0a.wait, x_gate0a.send)
    k.do(t_down0b.send, t_down0a.send, t_down1.send, t_up.wait, z_up0.send)
    k.do(g0.loop, z_up0.step, taps.wait, conv.run, y0.start)
    k.do(x_out0.wait, w_out0.start, s1.loop, z_up0.step, s1.finish, mid0.start)
    k.do(*wait(t_gate1, t_down0a, t_down0b, t_down1, z_gate0b, x_gate0a, z_up0))
    k.build()
    a0, proj0, value0 = (out for _, out, _ in g0.saved)
    table_arrays = [head_gain] + [v.out for v in angles.saves]
    y0, mid0 = y0.out, mid0.out

    k = Kernel(1)
    x_up0, z_gate1 = x_move(k, z_up0.out), z_gather_half(k, sh_gate, t_gate1.out, 1)
    z_down0a = z_gather_half(k, down_lo, t_down0a.out, 0)
    z_down0b = z_gather_whole(k, down_hi, t_down0b.out, 0)
    z_in1, z_out1 = z_gather_half(k, sh_in, t_in.out, 1), z_gather_half(k, sh_out, t_out.out, 1)
    x_down0a, x_in1, x_out1 = (x_move(k, v.out) for v in (z_down0a, z_in1, z_out1))
    rows, gain_load = load_all(k, mid0), gains_of(k, 0, t_gain.out)
    w_gate0 = Weight(k, "rows", (z_gate0a.out, x_gate0a.out), (z_gate0b.out, None), early=True)
    w_up0 = Weight(k, "rows", (z_up0.out, x_up0.out))
    w_down0 = Weight(k, "cols", (z_down0a.out, x_down0a.out), (z_down0b.out, None))
    g2 = Gather(
        k, rows.buf, (gain_load.buf, 1), [w_gate0, w_up0], epilogue="ffn", save=(0, 1, 2, 3)
    )
    s3 = Scatter(k, [g2.values[2]], [w_down0], rows.buf, low=True)
    z_rows = Save(k, s3.out)
    k.do(x_up0.send, z_down0a.send, z_down0b.send, rows.wait, gain_load.wait, g2.begin)
    k.do(z_in1.send, z_out1.send, z_down0a.step, z_in1.step, z_out1.step, z_down0b.step)
    k.do(z_down0a.step, z_in1.step, z_out1.step, z_gate1.send, z_down0a.wait, x_down0a.send)
    k.do(x_up0.wait, w_up0.start, z_down0b.step, g2.loop, z_gate1.step)
    k.do(z_in1.wait, x_in1.send, z_out1.wait, x_out1.send, z_down0b.wait, x_down0a.wait)
    k.do(w_down0.start, s3.loop, z_gate1.step, s3.finish, z_rows.start)
    k.do(*wait(x_in1, x_out1, z_gate1))
    k.build()
    m0, gate0, up0, hid0 = (out for _, out, _ in g2.saved)
    z_rows = z_rows.out

    k = Kernel(2)
    x_gate1, z_up1 = x_move(k, z_gate1.out), z_gather_half(k, sh_up, t_up.out, 1)
    z_down1a, z_down1b = (z_gather_whole(k, sh_down, t_down1.out, 1, i) for i in range(2))
    x_up1 = x_move(k, z_up1.out)
    rows, gain_load = load_all(k, z_rows), gains_of(k, 1, t_gain.out)
    tables = [load_all(k, v) for v in table_arrays]
    w_in1 = Weight(k, "rows", (z_in1.out, x_in1.out), early=True)
    w_out1 = Weight(k, "cols", (z_out1.out, x_out1.out), early=True)
    g4 = Gather(k, rows.buf, (gain_load.buf, 0), [w_in1], save=(0, 1))
    attend = Attend(k, g4.values[0], tables, size)
    kept = [Save(k, v) for v in (attend.q_rot, attend.k_rot, attend.y)]
    s5 = Scatter(k, [attend.y], [w_out1], rows.buf)
    mid1 = Save(k, s5.out)
    k.do(x_gate1.send, z_up1.send, rows.wait, gain_load.wait, g4.begin, z_up1.step)
    k.do(z_down1a.send, g4.loop, z_up1.step, z_down1b.send)
    k.do(lambda: attend.run(z_up1.wait, x_up1.send, z_down1a.step))
    k.do(*(v.start for v in kept))
    k.do(z_down1b.step, s5.loop, z_down1a.step, z_down1b.step, s5.finish, mid1.start)
    k.do(*wait(x_gate1, x_up1, z_down1a, z_down1b))
    k.build()
    a1, proj1 = (out for _, out, _ in g4.saved)
    q_rot, k_rot, y1 = (v.out for v in kept)
    mid1 = mid1.out

    k = Kernel(3)
    rows, gain_load = load_all(k, mid1), gains_of(k, 1, t_gain.out)
    cot = start_rows(k, 1, t_seq.out)
    w_gate1 = Weight(k, "rows", (z_gate1.out, x_gate1.out), early=True)
    w_up1 = Weight(k, "rows", (z_up1.out, x_up1.out), early=True)
    w_down1 = Weight(k, "cols", (z_down1a.out, None), (z_down1b.out, None), early=True)
    g6 = Gather(k, rows.buf, (gain_load.buf, 1), [w_gate1, w_up1], epilogue="ffn")
    g8 = Gather(
        k, cot.buf, None, [w_down1], [g6.values[0], g6.values[1]], trans=True, epilogue="ffn_back"
    )
    p_down1 = Product(k, g6.values[2], g8.full)
    p_gate1, p_up1 = Product(k, g6.full, g8.values[0]), Product(k, g6.full, g8.values[1])
    s9 = Scatter(k, g8.values, [w_gate1, w_up1], cot.buf, (rows.buf, (gain_load.buf, 1)), True)
    hid1 = Save(k, g6.values[2])
    d_mid1, gain11 = Save(k, s9.out), Save(k, s9.gain_grad)
    k.do(rows.wait, gain_load.wait, g6.begin, cot.wait, g8.begin, g6.loop, hid1.start, g8.loop)
    k.do(s9.loop, p_down1.run, p_gate1.run, p_up1.run)
    k.do(s9.finish, d_mid1.start, gain11.start, p_down1.wait, p_gate1.wait, p_up1.wait)
    k.build()
    hid1, d_mid1, gain11 = hid1.out, d_mid1.out, gain11.out

    k = Kernel(4)
    r_down1 = x_half(k, p_down1.out)
    r_gate1, q_up1 = x_slots(k, p_gate1.out, "rows"), sum_scatter(k, "rows", p_up1.out)
    rows, gain_load = load_all(k, d_mid1), gains_of(k, 1, t_gain.out)
    value = load_all(k, z_rows)
    tables = [load_all(k, v) for v in table_arrays]
    proj, q_load, k_load, y_load, a_load = (load_all(k, v) for v in (proj1, q_rot, k_rot, y1, a1))
    w_in1 = Weight(k, "rows", (z_in1.out, x_in1.out), early=True)
    w_out1 = Weight(k, "cols", (z_out1.out, x_out1.out), early=True)
    g10 = Gather(k, rows.buf, None, [w_out1], trans=True)
    p_out1 = Product(k, y_load.buf, g10.full)
    back = AttendBack(k, proj.buf, tables, size, q_load.buf, k_load.buf, g10.values[0])
    p_in1 = Product(k, a_load.buf, back.d_proj)
    r_out1 = x_half(k, p_out1.out)
    s11 = Scatter(
        k, [back.d_proj], [w_in1], rows.buf, (value.buf, (gain_load.buf, 0)), True, low=True
    )
    d_z, gain10 = Save(k, s11.out), Save(k, s11.gain_grad)
    head_gains = [Save(k, back.q_gain), Save(k, back.k_gain)]
    k.early.append(q_up1.load)
    k.do(r_down1.send, r_gate1.send, rows.wait, g10.begin, q_up1.send, g10.loop)
    k.do(y_load.wait, p_out1.run, q_up1.step, p_out1.wait, r_out1.send)
    k.do(proj.wait, q_load.wait, k_load.wait, lambda: back.run(q_up1.step))
    k.do(*(v.start for v in head_gains))
    k.do(gain_load.wait, value.wait, s11.loop, a_load.wait, p_in1.run)
    k.do(s11.finish, d_z.start, gain10.start, p_in1.wait)
    k.do(*wait(r_down1, q_up1, r_gate1, r_out1))
    k.build()
    d_z, gain10 = d_z.out, gain10.out
    q_gain, k_gain = (v.out for v in head_gains)

    k = Kernel(5)
    q_gate1, m_up1 = sum_scatter(k, "rows", p_gate1.out, r_gate1.out), x_move(k, q_up1.out, 0)
    q_out1 = sum_scatter(k, "cols", p_out1.out, r_out1.out)
    r_in1 = x_slots(k, p_in1.out, "rows")
    q_in1 = sum_scatter(k, "rows", p_in1.out, r_in1.out)
    q_down1 = sum_scatter(k, "cols", p_down1.out, r_down1.out)
    rows, value, gain_load = load_all(k, d_z), load_all(k, mid0), gains_of(k, 0, t_gain.out)
    gate_load, up_load, hid_load, m_load = (load_all(k, v) for v in (gate0, up0, hid0, m0))
    w_gate0 = Weight(k, "rows", (z_gate0a.out, x_gate0a.out), (z_gate0b.out, None), early=True)
    w_up0 = Weight(k, "rows", (z_up0.out, x_up0.out), early=True)
    w_down0 = Weight(k, "cols", (z_down0a.out, x_down0a.out), (z_down0b.out, None), early=True)
    g12 = Gather(
        k, rows.buf, None, [w_down0], [gate_load.buf, up_load.buf], trans=True, epilogue="ffn_back"
    )
    p_down0 = Product(k, hid_load.buf, g12.full)
    p_gate0, p_up0 = Product(k, m_load.buf, g12.values[0]), Product(k, m_load.buf, g12.values[1])
    r_down0 = x_half(k, p_down0.out)
    s13 = Scatter(
        k, g12.values, [w_gate0, w_up0], rows.buf, (value.buf, (gain_load.buf, 1)), True
    )
    d_mid0, gain01 = Save(k, s13.out), Save(k, s13.gain_grad)
    k.early += [q_gate1.load, q_down1.load, q_out1.load]
    k.do(r_in1.send, m_up1.send, rows.wait, g12.begin, q_gate1.send, q_down1.send, q_out1.send)
    k.do(gate_load.wait, up_load.wait, g12.loop, q_gate1.step, q_down1.step, q_out1.step)
    k.do(hid_load.wait, p_down0.run, p_down0.wait, r_down0.send, r_in1.wait, q_in1.add)
    k.do(s13.loop, q_gate1.step, q_down1.step, q_out1.step)
    k.do(m_load.wait, p_gate0.run, q_in1.step, p_up0.run, value.wait, gain_load.wait)
    k.do(s13.finish, d_mid0.start, gain01.start, q_in1.step, p_gate0.wait, p_up0.wait)
    k.do(*wait(q_gate1, q_out1, q_in1, q_down1, m_up1, r_down0))
    k.build()
    d_mid0, gain01 = d_mid0.out, gain01.out

    k = Kernel(6)
    r_gate0 = x_slots(k, p_gate0.out, "rows")
    q_gate0 = sum_scatter(k, "rows", p_gate0.out, r_gate0.out)
    q_down0 = sum_scatter(k, "cols", p_down0.out, r_down0.out)
    q_up0 = sum_scatter(k, "rows", p_up0.out)
    m_up0 = x_move(k, q_up0.out, 1)
    e_down1 = Finish(k, q_down1.out, 1)
    e_gate1, e_out1, e_in1 = (Finish(k, v.out, 1) for v in (q_gate1, q_out1, q_in1))
    rows, gain_load = load_all(k, d_mid0), gains_of(k, 0, t_gain.out)
    x_load, taps = start_rows(k, 0, t_seq.out), load_all(k, conv_kernel)
    y_load, a_load, proj, value = (load_all(k, v) for v in (y0, a0, proj0, value0))
    w_in0 = Weight(k, "rows", (z_in0.out, x_in0.out), early=True)
    w_cols = Weight(k, "conv", (z_cols.out, x_cols.out), early=True)
    w_out0 = Weight(k, "cols", (z_out0.out, x_out0.out), early=True)
    g14 = Gather(k, rows.buf, None, [w_out0], trans=True)
    p_out0 = Product(k, y_load.buf, g14.full)
    back = ConvBack(k, proj.buf, value.buf, taps.buf, g14.values[0])
    p_in0, p_cols = Product(k, a_load.buf, back.d_proj), Product(k, a_load.buf, back.d_value)
    r_out0, r_in0 = x_half(k, p_out0.out), x_slots(k, p_in0.out, "rows")
    r_cols = x_slots(k, p_cols.out, "conv")
    q_out0, q_in0 = sum_scatter(k, "cols", p_out0.out, r_out0.out), sum_scatter(k, "rows", p_in0.out, r_in0.out)
    q_cols = sum_scatter(k, "conv", p_cols.out, r_cols.out)
    e_down0, e_gate0, e_out0, e_in0 = (
        Finish(k, v.out, 0) for v in (q_down0, q_gate0, q_out0, q_in0)
    )
    s15 = Scatter(
        k, [back.d_proj, back.d_value], [w_in0, w_cols], rows.buf,
        (x_load.buf, (gain_load.buf, 0)), True, low=True,
    )
    d_x = Save(k, s15.out)
    tap_rows = conv_kernel.shape[0]
    small = k.vmem((8, model_width), F32)
    small_out = Save(k, small)
    ready = [load_all(k, v) for v in (gain01, gain10, gain11)]
    head_loads = [load_all(k, v) for v in (q_gain, k_gain)]

    def fill_small():
        t = lax.axis_index("tensor")
        small.ref[...] = jnp.zeros_like(small.ref)
        small.ref[0:1, :] = s15.gain_grad.ref[...]
        for i, load in enumerate(ready):
            load.wait()
            small.ref[i + 1 : i + 2, :] = load.buf.ref[...]
        small.ref[4 : 4 + tap_rows, block_of(t, channels)] = back.d_kernel.ref[...]
        at = 0
        for load in head_loads:
            load.wait()
            width = load.buf.shape[1]
            small.ref[7:8, at : at + width] = load.buf.ref[...]
            at += width
        small_out.start()

    t_small = x_move(k, small_out.out)
    z_small = SumShare(k, [small_out.out, t_small.out], "dp")
    t_total = SumShare(k, [z_small.out], "tensor", slotted=True)
    hid_load, mid_load = load_all(k, hid1), load_all(k, mid1)
    w_down1 = Weight(k, "cols", (z_down1a.out, None), (z_down1b.out, None), early=True)
    s7 = Scatter(k, [hid_load.buf], [w_down1], mid_load.buf, low=True)
    y_rows = Save(k, s7.out)
    t_x, t_y = x_move(k, d_x.out, 1), x_move(k, y_rows.out, 0)
    k.early += [q_up0.load, q_down0.load]
    k.early += [v.load for v in (e_down1, e_gate1, e_out1, e_in1)]
    k.do(r_gate0.send, rows.wait, g14.begin, q_up0.send, q_down0.send)
    k.do(e_down1.send, e_gate1.send, e_out1.send, e_in1.send, g14.loop)
    k.do(y_load.wait, p_out0.run, p_out0.wait, r_out0.send, q_up0.step)
    k.do(proj.wait, value.wait, taps.wait, back.run, q_down0.step, a_load.wait)
    k.do(p_in0.run, p_cols.run, p_in0.wait, r_in0.send, p_cols.wait, r_cols.send)
    k.do(r_gate0.wait, q_gate0.add, x_load.wait, gain_load.wait, s15.loop, q_up0.step)
    k.do(q_down0.step, s15.finish, d_x.start, fill_small, d_x.wait, t_x.send)
    k.do(small_out.wait, t_small.send, q_gate0.step, hid_load.wait, mid_load.wait, s7.loop)
    k.do(r_out0.wait, q_out0.add, r_in0.wait, q_in0.add)
    k.do(r_cols.wait, q_cols.add, q_up0.wait, m_up0.send, q_down0.wait, e_down0.add)
    k.do(s7.finish, y_rows.start, y_rows.wait, t_y.send)
    k.do(q_gate0.step, q_out0.step, q_in0.step, q_cols.step, t_small.wait, z_small.add)
    k.do(q_gate0.wait, e_gate0.add, q_out0.step, q_in0.step, q_cols.step)
    k.do(z_small.wait, t_total.add, q_out0.wait, e_out0.add, q_in0.wait, e_in0.add)
    rest = (e_down1, e_gate1, e_out1, e_in1, q_cols, e_down0, e_gate0, m_up0, e_out0, e_in0)
    k.do(*wait(*rest, t_total, t_x, t_y))
    k.build()

    owned = [
        ([e_in0], [e_in1], 1),
        ([e_out0], [e_out1], 1),
        ([e_gate0], [e_gate1], 1),
        ([q_up0, m_up0], [q_up1, m_up1], 1),
        ([e_down0], [e_down1], 1),
        ([q_cols], [q_cols], 0),
    ]
    return pack(
        [(zero, one, lead) for zero, one, lead in owned], t_total, d_x.out, y_rows.out, t_x, t_y,
        (norm_gain.shape, conv_kernel.shape, qk_gain.shape),
    )


def slot_free(val, shape):
    value = val.out.array
    if value.ndim == 3 and value.shape[0] * value.shape[1] != shape[0]:
        value = jnp.sum(value.astype(F32), axis=0).astype(BF)
    return value.reshape(shape)


def pack_kernel(plan, *refs):
    n_in, leads, terms, tap_rows = plan
    ins, rest = refs[:n_in], refs[n_in:]
    result, gain_out, *grads, cols, taps, heads = rest[: len(leads) + 4]
    grads = [*grads, cols]
    room = iter(rest[len(leads) + 4 :])
    own_v, moved_v, small_v, *bufs = (next(room) for _ in range(3 + len(terms)))
    out_v = [next(room) for _ in leads]
    load_sem, store_sem = room
    s, t = lax.axis_index("section"), lax.axis_index("tensor")
    small, d_x, y_rows, moved, moved_y, *parts = ins

    def either(cond, zero, one, dst, sem):
        if zero is not None:
            pl.when(cond)(pltpu.make_async_copy(zero, dst, sem).start)
        if one is not None:
            pl.when(jnp.logical_not(cond))(pltpu.make_async_copy(one, dst, sem).start)

    first = s == 0
    either(first, d_x, y_rows, own_v, load_sem.at[0])
    either(first, moved, moved_y, moved_v, load_sem.at[1])
    pltpu.make_async_copy(small, small_v, load_sem.at[2]).start()
    for j, (zero, one, _) in enumerate(terms):
        either(
            first,
            None if zero is None else parts[zero],
            None if one is None else parts[one],
            bufs[j],
            load_sem.at[3 + j],
        )
    for j, (zero, one, i) in enumerate(terms):
        arrive = pltpu.make_async_copy(parts[one if zero is None else zero], bufs[j], load_sem.at[3 + j])
        begins = j == 0 or terms[j - 1][2] != i

        def put(j=j, i=i, begins=begins):
            def add_rows(at):
                value = bufs[j][at, :].astype(F32)
                out_v[i][at, :] = value if begins else out_v[i][at, :] + value

            chunked(bufs[j].shape[0], add_rows)

        if zero is None or one is None:
            cond = first if one is None else jnp.logical_not(first)

            @pl.when(cond)
            def _(arrive=arrive, put=put):
                arrive.wait()
                put()
        else:
            arrive.wait()
            put()
        if j + 1 == len(terms) or terms[j + 1][2] != i:
            dst = grads[i].at[0] if leads[i] else grads[i]
            pltpu.make_async_copy(out_v[i], dst, store_sem.at[i]).start()
    pltpu.make_async_copy(d_x, own_v, load_sem.at[0]).wait()
    pltpu.make_async_copy(moved, moved_v, load_sem.at[1]).wait()
    n = len(leads)
    stores = [
        pltpu.make_async_copy(own_v, result.at[0, s], store_sem.at[n]),
        pltpu.make_async_copy(moved_v, result.at[0, 1 - s], store_sem.at[n + 1]),
    ]
    for store in stores:
        store.start()
    pltpu.make_async_copy(small, small_v, load_sem.at[2]).wait()
    total = small_v[0]
    for i in range(1, small_v.shape[0]):
        total = total + small_v[i]
    gain_out[0] = jnp.where(first, total[0:2], total[2:4])
    channels, size = taps.shape[1], heads.shape[1]
    chosen = total[4 : 4 + tap_rows, 0:channels]
    for i in range(1, total.shape[1] // channels):
        chosen = jnp.where(t == i, total[4 : 4 + tap_rows, i * channels : (i + 1) * channels], chosen)
    taps[...] = chosen
    at = 0
    for row, width in enumerate((channels, channels // 2)):
        value = total[7:8, at : at + size]
        for i in range(1, width // size):
            value = value + total[7:8, at + i * size : at + (i + 1) * size]
        heads[row : row + 1, :] = value
        at += width
    for i, store in enumerate(leads):
        dst = grads[i].at[0] if store else grads[i]
        pltpu.make_async_copy(out_v[i], dst, store_sem.at[i]).wait()
    for store in stores:
        store.wait()


def pack(owned, small, d_x, y_rows, moved_x, moved_y, shapes):
    gain_shape, tap_shape, head_shape = shapes
    parts, terms, leads, out_shapes = [], [], [], []
    for i, (zero, one, lead) in enumerate(owned):
        whole = zero[0].out.shape
        if lead and len(whole) == 3 and isinstance(zero[0], Finish):
            shape = (whole[0] * whole[1], whole[2])
        else:
            shape = whole[-2:]
        shape = tuple(shape)
        leads.append(lead)
        out_shapes.append(shape)
        for j in range(max(len(zero), len(one))):
            pair = []
            for side in (zero, one):
                if j < len(side):
                    parts.append(slot_free(side[j], shape))
                    pair.append(len(parts) - 1)
                else:
                    pair.append(None)
            terms.append((*pair, i))
    operands = [v.array for v in (small.out, d_x, y_rows, moved_x.out, moved_y.out)] + parts
    rows = d_x.shape
    smem = pl.BlockSpec(memory_space=pltpu.VMEM)
    out_shape = [jax.ShapeDtypeStruct((1, 2) + rows, BF), jax.ShapeDtypeStruct(gain_shape, F32)]
    out_shape += [
        jax.ShapeDtypeStruct((1,) + v if lead else v, F32) for v, lead in zip(out_shapes, leads)
    ]
    out_shape += [jax.ShapeDtypeStruct(v, F32) for v in (tap_shape, head_shape)]
    n = len(leads)
    return tuple(
        pl.pallas_call(
            functools.partial(
                pack_kernel, (len(operands), tuple(leads), tuple(terms), tap_shape[0])
            ),
            out_shape=out_shape,
            in_specs=[ANY] * len(operands),
            out_specs=[ANY, smem] + [ANY] * n + [smem] * 2,
            scratch_shapes=[pltpu.VMEM(rows, BF)] * 2
            + [pltpu.VMEM(small.out.shape, F32)]
            + [pltpu.VMEM(out_shapes[i], BF) for _, _, i in terms]
            + [pltpu.VMEM(v, F32) for v in out_shapes]
            + [DMA((3 + len(terms),)), DMA((n + 2,))],
            compiler_params=pltpu.CompilerParams(vmem_limit_bytes=VMEM_BYTES),
            name="pack",
        )(*operands)
    )


def solution(mesh):
    in_specs = (
        P("section", "dp", "tensor", None),
        P("section", None, None),
        P("section", "dp", "tensor"),
        P("section", "tensor", "dp"),
        P("section", "dp", "tensor"),
        P("section", "dp", "tensor"),
        P("section", "tensor", "dp"),
        P(("section", "dp"), "tensor"),
        P(None, "tensor"),
        P(),
    )
    out_specs = (
        P("section", "dp", "tensor", None),
        P("section", None, None),
        P("section", "dp", "tensor"),
        P("section", "tensor", "dp"),
        P("section", "dp", "tensor"),
        P("section", "dp", "tensor"),
        P("section", "tensor", "dp"),
        P(("section", "dp"), "tensor"),
        P(None, "tensor"),
        P(),
    )
    return jax.shard_map(body, mesh=mesh, in_specs=in_specs, out_specs=out_specs, check_vma=False)
```

```python
import functools

import jax
import jax.numpy as jnp
from jax import lax
from jax.experimental import pallas as pl
from jax.experimental.pallas import tpu as pltpu
from jax.sharding import PartitionSpec as P

HEADS = 16
KV_HEADS = 8

EPS = 1e-05
ROPE_BASE = 1000000.0
MASKED = -1e30

MESH = pl.DeviceIdType.MESH
ANY = pl.BlockSpec(memory_space=pl.ANY)
DMA = pltpu.SemaphoreType.DMA
VMEM_BYTES = 63 * 1024 * 1024
BF = jnp.bfloat16
F32 = jnp.float32
ROW_BLOCK = 256
STRIP = 32


def contract(left_op, right_op, left_dim, right_dim):
    return lax.dot_general(
        left_op, right_op, (((left_dim,), (right_dim,)), ((), ())), preferred_element_type=F32
    )


def norm_rows(values, gain):
    return values * lax.rsqrt(jnp.mean(values * values, axis=-1, keepdims=True) + EPS) * gain


def norm_back(values, gain, grad_in):
    row_scale = lax.rsqrt(jnp.mean(values * values, axis=-1, keepdims=True) + EPS)
    normed = values * row_scale
    gain_grad = jnp.sum(grad_in * normed, axis=0, keepdims=True)
    scaled = grad_in * gain
    value_grad = row_scale * (scaled - normed * jnp.mean(scaled * normed, axis=-1, keepdims=True))
    return (value_grad, gain_grad)


class Angles:
    def __init__(self, k, length, head_size, width):
        self.half = head_size // 2
        self.tables = [k.vmem((length, width), F32) for _ in range(2)]
        self.saves = [Save(k, v) for v in self.tables]

    def run(self):
        cos, sin = self.tables
        shape = (ROW_BLOCK, cos.shape[1])
        column = (lax.broadcasted_iota(jnp.int32, shape, 1) % self.half).astype(F32)
        frequency = ROPE_BASE ** (-(column / self.half))
        row = lax.broadcasted_iota(jnp.int32, shape, 0)

        def step(i, carry):
            rows = block_of(i, ROW_BLOCK)
            angle = (row + i * ROW_BLOCK).astype(F32) * frequency
            cos.ref[rows, :] = jnp.cos(angle)
            sin.ref[rows, :] = jnp.sin(angle)
            return carry

        lax.fori_loop(0, cos.shape[0] // ROW_BLOCK, step, 0)
        for save in self.saves:
            save.start()


def silu_parts(gate):
    sig = 1.0 / (1.0 + jnp.exp(-gate))
    return sig, gate * sig


def chunked(rows, step):
    size = next((n for n in (32, 16) if rows % n == 0), rows)
    if size == rows:
        step(pl.ds(0, rows))
    else:
        lax.fori_loop(0, rows // size, lambda i, c: step(block_of(i, size)) or c, 0)


def dp_size():
    return lax.axis_size("dp")


def spot():
    return tuple(lax.axis_index(a) for a in ("section", "dp", "tensor"))


def block_of(index, size):
    return pl.ds(pl.multiple_of(index * size, size), size)


class Val:
    def __init__(self, shape, dtype):
        self.shape, self.dtype = tuple(shape), dtype
        self.ref = self.array = None


class Kernel:
    def __init__(self, cid):
        self.cid, self.ins, self.arrays, self.outs, self.room = cid, [], [], [], []
        self.early, self.steps, self.late, self.axes = [], [], [], set()
        self.once = []

    def input(self, array):
        array = array.array if isinstance(array, Val) else array
        for val, known in zip(self.ins, self.arrays):
            if known is array:
                return val
        val = Val(array.shape, array.dtype)
        self.ins.append(val)
        self.arrays.append(array)
        return val

    def output(self, shape, dtype):
        val = Val(shape, dtype)
        self.outs.append(val)
        return val

    def vmem(self, shape, dtype):
        val = Val(shape, dtype)
        self.room.append((val, pltpu.VMEM(tuple(shape), dtype)))
        return val

    def sem(self, *shape):
        val = Val(shape, None)
        self.room.append((val, DMA(shape)))
        return val

    def do(self, *steps):
        self.steps += steps

    def body(self, *refs):
        vals = self.ins + self.outs + [val for val, _ in self.room]
        for val, ref in zip(vals, refs):
            val.ref = ref
        for item in self.once:
            item.waited = False
            item.phase = 0
        for step in self.early:
            step()
        self.greet()
        for step in self.steps + self.late:
            step()

    def greet(self):
        s, d, t = spot()
        _, sib, cross, diag = places()
        barrier = pltpu.get_barrier_semaphore()
        peers = [{"tensor": sib}, {"tensor": cross}]
        if "tensor" in self.axes:
            peers.append({"tensor": diag})
        if "section" in self.axes:
            peers.append({"section": 1 - s})
        if "dp" in self.axes:
            peers += [{"dp": (d + i) % dp_size()} for i in range(1, dp_size())]

        def signal(peer):
            pl.semaphore_signal(barrier, inc=1, device_id=peer, device_id_type=MESH)

        for peer in peers:
            signal(peer)
        expected = len(peers)
        if "line" in self.axes and "dp" not in self.axes:
            pl.when(d < 3)(lambda: signal({"dp": (d + 1) % 4}))
            pl.when(d > 0)(lambda: signal({"dp": (d + 3) % 4}))
            expected = expected + (d + 2) // 3 + (5 - d) // 3
        pl.semaphore_wait(barrier, expected)

    def build(self):
        result = pl.pallas_call(
            self.body,
            out_shape=[jax.ShapeDtypeStruct(v.shape, v.dtype) for v in self.outs],
            in_specs=[ANY] * len(self.ins),
            out_specs=[ANY] * len(self.outs),
            scratch_shapes=[room for _, room in self.room],
            compiler_params=pltpu.CompilerParams(
                collective_id=self.cid, has_side_effects=True, vmem_limit_bytes=VMEM_BYTES
            ),
            name=f"stage{self.cid}",
        )(*self.arrays)
        for val, array in zip(self.outs, result):
            val.array = array


def remote(src, dst, send_sem, recv_sem, peer):
    return pltpu.make_async_remote_copy(
        src_ref=src, dst_ref=dst, send_sem=send_sem, recv_sem=recv_sem,
        device_id=peer, device_id_type=MESH,
    )


class Load:
    def __init__(self, k, sources, shape, dtype, early=False):
        self.k, self.sources, self.waited = k, sources, False
        self.buf, self.sem = k.vmem(shape, dtype), k.sem(1)
        k.once.append(self)
        if early:
            k.early.append(self.start)

    def moves(self):
        for cond, source in self.sources(*spot()):
            yield cond, pltpu.make_async_copy(source, self.buf.ref, self.sem.ref.at[0])

    def start(self):
        for cond, move in self.moves():
            if cond is None:
                move.start()
            else:
                pl.when(cond)(move.start)

    def wait(self):
        if not self.waited:
            self.waited = True
            next(self.moves())[1].wait()


def load_all(k, array, early=True):
    val = k.input(array)
    return Load(k, lambda s, d, t: [(None, val.ref)], val.shape, val.dtype, early)


class Save:
    def __init__(self, k, buf):
        self.buf, self.out, self.sem = buf, k.output(buf.shape, buf.dtype), k.sem(1)
        self.waited = False
        k.once.append(self)
        k.late.append(self.wait)

    def move(self):
        return pltpu.make_async_copy(self.buf.ref, self.out.ref, self.sem.ref.at[0])

    def start(self):
        self.move().start()

    def wait(self):
        if not self.waited:
            self.waited = True
            self.move().wait()


class Task:
    final = None

    def __init__(self, k, out, axis, moves, count, n_local=1, out_dtype=BF):
        self.k, self.axis, self.make = k, axis, moves
        self.out = k.output(out, out_dtype)
        self.send_sem, self.recv_sem, self.local_sem = k.sem(count), k.sem(count), k.sem(n_local)
        self.waited = False
        k.axes.add(axis)
        k.once.append(self)

    def local(self, src, dst, i):
        return pltpu.make_async_copy(src, dst, self.local_sem.ref.at[i])

    def pairs(self, every):
        far, near = self.make(*spot())
        for i, (sources, dst, peer) in enumerate(far):
            for cond, src in sources if every else sources[:1]:
                yield cond, True, remote(
                    src, dst, self.send_sem.ref.at[i], self.recv_sem.ref.at[i], peer
                )
        for i, (sources, dst) in enumerate(near):
            for cond, src in sources if every else sources[:1]:
                yield cond, False, self.local(src, dst, i)

    def step(self):
        pass

    def send(self):
        for cond, far, move in self.pairs(True):
            if far and self.final is not None:
                cond = lax.axis_index("section") == 1 - self.final
            if cond is None:
                move.start()
            else:
                pl.when(cond)(move.start)

    def wait(self):
        if self.waited:
            return
        self.waited = True
        s = lax.axis_index("section")
        for _, far, move in self.pairs(False):
            if not far:
                move.wait()
            elif self.final is None:
                move.wait_recv()
                move.wait_send()
            else:
                pl.when(s == 1 - self.final)(move.wait_send)
                pl.when(s == self.final)(move.wait_recv)


class Part:
    def __init__(self, base, start, rows):
        self.base, self.start, self.rows = base, start, rows
        self.shape, self.dtype = (rows,) + tuple(base.shape[1:]), base.dtype
        self.array = None

    @property
    def ref(self):
        return self.base.ref.at[pl.ds(self.start, self.rows)]


def as_val(k, value):
    if isinstance(value, Part):
        return Part(as_val(k, value.base), value.start, value.rows)
    value = value.out if isinstance(value, Task) else value
    known = isinstance(value, Val) and (value.array is None)
    return value if known else k.input(value)


class Line(Task):
    def __init__(self, k, out, out_dtype=BF, n_local=1):
        super().__init__(k, out, "line", None, 6, n_local, out_dtype)
        self.send_sem, self.recv_sem = k.sem(2, 3), k.sem(2, 3)
        self.phase = 0

    def hop(self, j, way, src, dst):
        d = lax.axis_index("dp")
        peer = {"dp": (d + 1 if way == 0 else d + 3) % 4}
        return remote(src, dst, self.send_sem.ref.at[way, j], self.recv_sem.ref.at[way, j], peer)


class LineGather(Line):
    def __init__(self, k, sources, shape, dtype):
        super().__init__(k, (4,) + shape, dtype)
        self.sources = sources

    def ends(self, j, way):
        d = lax.axis_index("dp")
        if way == 0:
            return (d >= j) & (d < 3), d >= j + 1
        return (d <= 3 - j) & (d > 0), d <= 2 - j

    def copy(self, j, way, src=None):
        d = lax.axis_index("dp")
        slot = (d + 4 - j if way == 0 else d + j) % 4
        piece = self.out.ref.at[slot]
        return self.hop(j, way, piece if src is None else src, piece)

    def send(self):
        self.phase = 0
        for cond, src in self.sources(*spot()):
            own = self.local(src, self.out.ref.at[lax.axis_index("dp")], 0)
            moves = [(True if cond is None else cond, own)]
            for way in range(2):
                sends = self.ends(0, way)[0]
                moves.append((sends if cond is None else sends & cond, self.copy(0, way, src)))
            for when, move in moves:
                if when is True:
                    move.start()
                else:
                    pl.when(when)(move.start)

    def arrive(self, j):
        for way in range(2):
            pl.when(self.ends(j, way)[1])(self.copy(j, way).wait_recv)

    def step(self):
        self.arrive(self.phase)
        self.phase += 1
        for way in range(2):
            pl.when(self.ends(self.phase, way)[0])(self.copy(self.phase, way).start)

    def wait(self):
        if self.waited:
            return
        self.waited = True
        while self.phase < 2:
            self.step()
        self.arrive(2)
        for j in range(3):
            for way in range(2):
                pl.when(self.ends(j, way)[0])(self.copy(j, way).wait_send)
        d = lax.axis_index("dp")
        self.local(self.sources(*spot())[0][1], self.out.ref.at[d], 0).wait()


def z_gather_from(k, sources, shape, dtype):
    count = dp_size()
    if count == 4:
        return LineGather(k, sources, shape, dtype)

    def moves(s, d, t):
        dst, found = task.out.ref.at[d], sources(s, d, t)
        return [(found, dst, {"dp": (d + i) % count}) for i in range(1, count)], [(found, dst)]

    task = Task(k, (count,) + shape, "dp", moves, count - 1, out_dtype=dtype)
    return task


def z_gather(k, value):
    val = as_val(k, value)
    return z_gather_from(k, lambda s, d, t: [(None, val.ref)], val.shape, val.dtype)


def z_gather_half(k, shard, moved, block):
    shard, moved = as_val(k, shard), as_val(k, moved)
    rows = shard.shape[0] // 2

    def sources(s, d, t):
        own = shard.ref.at[pl.ds(block * rows, rows)]
        return [(s == block, own), (s == 1 - block, moved.ref)]

    return z_gather_from(k, sources, moved.shape, shard.dtype)


def one_way(task, sender):
    task.final = None if sender is None else 1 - sender
    return task


def z_gather_whole(k, shard, moved, block, half=None):
    shard, moved = as_val(k, shard), as_val(k, moved)
    rows = shard.shape[0] if half is None else shard.shape[0] // 2
    part = pl.ds(0 if half is None else half * rows, rows)

    def sources(s, d, t):
        return [(s == block, shard.ref.at[part]), (s == 1 - block, moved.ref.at[part])]

    return z_gather_from(k, sources, (rows,) + shard.shape[1:], shard.dtype)


def x_move(k, value, sender=None):
    val = as_val(k, value)

    def moves(s, d, t):
        return [([(None, val.ref)], task.out.ref, {"section": 1 - s})], []

    task = Task(k, val.shape, "section", moves, 1, out_dtype=val.dtype)
    return one_way(task, sender)


def x_half(k, value, sender=None):
    val = as_val(k, value)
    rows = val.shape[0] // 2

    def moves(s, d, t):
        src = val.ref.at[block_of(1 - s, rows)]
        return [([(None, src)], task.out.ref, {"section": 1 - s})], []

    task = Task(k, (rows,) + val.shape[1:], "section", moves, 1, out_dtype=val.dtype)
    return one_way(task, sender)


def x_slots(k, value, kind):
    val, count = as_val(k, value), dp_size()
    rows = val.shape[0] // (2 * count)

    def moves(s, d, t):
        far = []
        for i in range(count):
            slot = 2 * i + 1 - s if kind == "rows" else (1 - s) * count + i
            src = val.ref.at[block_of(slot, rows)]
            far.append(([(None, src)], task.out.ref.at[i], {"section": 1 - s}))
        return far, []

    task = Task(k, (count, rows) + val.shape[1:], "section", moves, count)
    return task


class Terms:
    def __init__(self, k, kind, grads, received, local):
        self.grads, self.local = as_val(k, grads), local
        self.kind, self.n = kind, dp_size()
        self.whole = received is None
        if self.whole:
            rows, cols = self.grads.shape
            self.rows = rows if kind == "cols" else rows // self.n
            self.cols = cols // self.n if kind == "cols" else cols
            self.shape = (self.n, self.rows, self.cols)
            self.aside = kind == "cols" and self.cols % 128 != 0
            self.total = k.vmem(self.shape, BF)
            self.kept = k.vmem(self.grads.shape, BF) if self.aside else self.total
            return
        self.received = as_val(k, received)
        if kind == "cols":
            self.rows, self.cols = self.grads.shape[0] // 2, self.grads.shape[1] // self.n
            held = (self.rows, self.grads.shape[1])
        else:
            self.rows, self.cols = self.grads.shape[0] // (2 * self.n), self.grads.shape[1]
            held = (self.n, self.rows, self.cols)
        self.kept, self.got = k.vmem(held, BF), k.vmem(held, BF)
        self.shape = (self.n, self.rows, self.cols)
        self.total = k.vmem(self.shape, BF) if kind == "cols" else self.kept

    def loads(self):
        s, grads, kept = lax.axis_index("section"), self.grads.ref, self.kept.ref
        if self.whole and self.aside:
            return [self.local(grads, kept, 2)]
        if self.whole:
            parts = [
                grads.at[:, pl.ds(i * self.cols, self.cols)]
                if self.kind == "cols"
                else grads.at[block_of(i, self.rows)]
                for i in range(self.n)
            ]
            return [self.local(part, kept.at[i], 2 + i) for i, part in enumerate(parts)]
        if self.kind == "cols":
            moves = [self.local(grads.at[block_of(s, self.rows)], kept, 2)]
        else:
            moves = []
            for i in range(self.n):
                slot = 2 * i + s if self.kind == "rows" else s * self.n + i
                moves.append(self.local(grads.at[block_of(slot, self.rows)], kept.at[i], 2 + i))
        return moves + [self.local(self.received.ref, self.got.ref, 1)]

    def load(self):
        for move in self.loads():
            move.start()

    def add(self):
        for move in self.loads():
            move.wait()
        if self.whole and self.aside:
            for i in range(self.n):
                self.total.ref[i] = self.kept.ref[:, i * self.cols : (i + 1) * self.cols]
        if self.whole:
            return
        kept, got, total = self.kept.ref, self.got.ref, self.total.ref
        if self.kind != "cols":

            def piece(i, carry):
                chunked(self.rows, lambda at: total.__setitem__(
                    (i, at), (kept[i, at, :].astype(F32) + got[i, at, :].astype(F32)).astype(BF)
                ))
                return carry

            lax.fori_loop(0, self.n, piece, 0)
            return

        def add_rows(at):
            for i in range(self.n):
                part = slice(i * self.cols, (i + 1) * self.cols)
                value = kept[at, part].astype(F32) + got[at, part].astype(F32)
                total[i, at, :] = value.astype(BF)

        chunked(self.rows, add_rows)


class DirectScatter(Task):
    def __init__(self, k, kind, grads, received):
        self.terms = Terms(k, kind, grads, received, lambda *a: self.local(*a))
        count = dp_size()

        def moves(s, d, t):
            total = self.terms.total.ref
            far = []
            for i in range(1, count):
                other = (d + i) % count
                far.append(([(None, total.at[other])], self.out.ref.at[d], {"dp": other}))
            return far, [([(None, total.at[d])], self.out.ref.at[d])]

        super().__init__(k, self.terms.shape, "dp", moves, count - 1, 2 + count)
        self.load = self.terms.load

    def send(self):
        self.terms.add()
        super().send()

    def add(self):
        self.load()
        self.send()


class LineScatter(Line):
    def __init__(self, k, kind, grads, received):
        self.terms = Terms(k, kind, grads, received, lambda *a: self.local(*a))
        super().__init__(k, self.terms.shape[1:], BF, 6)
        self.got = k.vmem((2, 3) + self.terms.shape[1:], BF)
        self.load = self.terms.load

    def ends(self, j, way):
        d = lax.axis_index("dp")
        if way == 0:
            return (d <= j) & (d < 3), (d >= 1) & (d <= j + 1)
        return (d >= 3 - j) & (d > 0), (d <= 2) & (d >= 2 - j)

    def copy(self, j, way):
        d = lax.axis_index("dp")
        to = (d + 3 - j if way == 0 else d + 1 + j) % 4
        return self.hop(j, way, self.terms.total.ref.at[to], self.got.ref.at[way, j])

    def send(self):
        self.phase = 0
        self.terms.add()
        for way in range(2):
            pl.when(self.ends(0, way)[0])(self.copy(0, way).start)

    def take(self, j, way):
        d = lax.axis_index("dp")
        to = (d + 2 - j if way == 0 else d + 2 + j) % 4
        self.copy(j, way).wait_recv()
        total, got = self.terms.total.ref, self.got.ref

        def add_rows(at):
            value = total[to, at, :].astype(F32) + got[way, j, at, :].astype(F32)
            total[to, at, :] = value.astype(BF)

        chunked(self.terms.rows, add_rows)

    def arrive(self, j):
        for way in range(2):
            pl.when(self.ends(j, way)[1])(functools.partial(self.take, j, way))

    def step(self):
        self.arrive(self.phase)
        self.phase += 1
        for way in range(2):
            pl.when(self.ends(self.phase, way)[0])(self.copy(self.phase, way).start)

    def wait(self):
        if self.waited:
            return
        self.waited = True
        while self.phase < 2:
            self.step()
        self.arrive(2)
        done = self.local(self.terms.total.ref.at[lax.axis_index("dp")], self.out.ref, 0)
        done.start()
        for j in range(3):
            for way in range(2):
                pl.when(self.ends(j, way)[0])(self.copy(j, way).wait_send)
        done.wait()

    def add(self):
        self.load()
        self.send()


def sum_scatter(k, kind, grads, received=None):
    return (LineScatter if dp_size() == 4 else DirectScatter)(k, kind, grads, received)


class Finish(Task):
    def __init__(self, k, pieces, block):
        self.pieces, self.final = as_val(k, pieces), block
        *slots, rows, cols = self.pieces.shape
        self.slots = slots[0] if slots else 0
        if slots:
            self.held, self.total = k.vmem(self.pieces.shape, BF), k.vmem((rows, cols), BF)
        else:
            self.total = self.pieces

        def moves(s, d, t):
            source, dst = [(None, self.total.ref)], self.out.ref.at[s]
            return [(source, dst, {"section": 1 - s})], [(source, dst)]

        super().__init__(k, (2, rows, cols), "section", moves, 1, 2)

    def load(self):
        if self.slots:
            self.local(self.pieces.ref, self.held.ref, 1).start()

    def send(self):
        if self.slots:
            self.local(self.pieces.ref, self.held.ref, 1).wait()
            acc = self.held.ref[0].astype(F32)
            for i in range(1, self.slots):
                acc = acc + self.held.ref[i].astype(F32)
            self.total.ref[...] = acc.astype(BF)
        super().send()

    def add(self):
        self.load()
        self.send()


class SumShare(Task):
    def __init__(self, k, terms, axis, slotted=False):
        self.terms = [as_val(k, v) for v in terms]
        shape = self.terms[0].shape[1:] if slotted else self.terms[0].shape
        count = dp_size() if axis == "dp" else 4
        self.slotted = slotted
        self.bufs = [k.vmem(v.shape, F32) for v in self.terms]
        self.total = k.vmem(shape, F32)

        def moves(s, d, t):
            source, me = [(None, self.total.ref)], d if axis == "dp" else t
            dst = self.out.ref.at[me]
            far = [(source, dst, {axis: (me + i) % count}) for i in range(1, count)]
            return far, [(source, dst)]

        super().__init__(k, (count,) + shape, axis, moves, count - 1, 3, out_dtype=F32)

    def add(self):
        loads = [self.local(v.ref, b.ref, 1 + i) for i, (v, b) in enumerate(zip(self.terms, self.bufs))]
        for load in loads:
            load.start()
        for load in loads:
            load.wait()
        if self.slotted:
            parts = [self.bufs[0].ref[i] for i in range(self.terms[0].shape[0])]
        else:
            parts = [buf.ref[...] for buf in self.bufs]
        acc = parts[0]
        for part in parts[1:]:
            acc = acc + part
        self.total.ref[...] = acc
        self.send()


class Weight:
    def __init__(self, k, kind, *segments, early=False):
        self.kind, self.waited = kind, False
        self.segments, start = [], 0
        for near, far in segments:
            near, far = as_val(k, near), None if far is None else as_val(k, far)
            self.segments.append((near, far, start))
            start += near.shape[1] * (1 if far is None else 2)
        self.count, _, self.cols = self.segments[0][0].shape
        self.rows = start
        if kind == "cols":
            shape = (self.rows, self.count * self.cols)
        else:
            shape = (self.count * self.rows, self.cols)
        self.aside = kind == "cols" and self.cols % 128 != 0
        self.buf = k.vmem(shape, BF)
        sides = [v for near, far, _ in self.segments for v in (near, far) if v is not None]
        self.sem = k.sem(len(sides), self.count)
        if self.aside:
            self.held = [k.vmem(v.shape, BF) for v in sides]
        k.once.append(self)
        if early:
            k.early.append(self.start)

    def sides(self):
        s = lax.axis_index("section")
        for near, far, start in self.segments:
            rows = near.shape[1]
            if far is None:
                yield near, start, None
            else:
                yield near, start + s * rows, s
                yield far, start + (1 - s) * rows, 1 - s

    def moves(self):
        dst = self.buf.ref
        for j, (val, start, sec) in enumerate(self.sides()):
            rows = val.shape[1]
            for i in range(self.count):
                if self.aside:
                    to = self.held[j].ref.at[i]
                elif self.kind == "cols":
                    at = pl.ds(pl.multiple_of(start, 16), rows)
                    to = dst.at[at, pl.ds(i * self.cols, self.cols)]
                else:
                    top = (sec * self.count + i) * rows if self.kind == "conv" else i * self.rows + start
                    to = dst.at[pl.ds(pl.multiple_of(top, 16), rows)]
                yield pltpu.make_async_copy(val.ref.at[i], to, self.sem.ref.at[j, i])

    def start(self):
        for move in self.moves():
            move.start()

    def wait(self):
        if self.waited:
            return
        self.waited = True
        for move in self.moves():
            move.wait()
        if self.aside:
            for j, (val, start, _) in enumerate(self.sides()):
                whole = jnp.concatenate([self.held[j].ref[i] for i in range(self.count)], axis=1)
                self.buf.ref[pl.ds(pl.multiple_of(start, 16), val.shape[1]), :] = whole


class Product:
    def __init__(self, k, left, right):
        self.left, self.right = left, right
        rows = left.shape[1]
        self.chunk = 384 if rows % 384 == 0 else 256
        self.count = rows // self.chunk
        self.buf = k.vmem((rows, right.shape[1]), BF)
        self.out, self.sem = k.output(self.buf.shape, BF), k.sem(self.count)

    def copy(self, i):
        part = block_of(i, self.chunk)
        return pltpu.make_async_copy(self.buf.ref.at[part], self.out.ref.at[part], self.sem.ref.at[i])

    def run(self):
        def step(i, carry):
            part = block_of(i, self.chunk)
            value = contract(self.left.ref[:, part], self.right.ref[...], 0, 0)
            self.buf.ref[part, :] = value.astype(BF)
            self.copy(i).start()
            return carry

        lax.fori_loop(0, self.count, step, 0)

    def wait(self):
        for i in range(self.count):
            self.copy(i).wait()


def places():
    me = lax.axis_index("tensor")
    sib = me + 1 - 2 * (me % 2)
    cross = (me + 2) % 4
    diag = (sib + 2) % 4
    return me, sib, cross, diag


class Gather:
    def __init__(self, k, x, gain, weights, extras=(), trans=False, epilogue="plain", save=()):
        rows, width = x.shape
        length = 4 * rows
        self.k, self.x, self.gain, self.weights, self.extras = k, x, gain, weights, extras
        self.trans, self.epilogue, self.rows, self.half = trans, epilogue, rows, rows // 2
        cols = [w.buf.shape[0 if trans else 1] for w in weights]
        kinds = {
            "plain": [(c, F32) for c in cols],
            "ffn": [(cols[0], BF)] * 3,
            "ffn_back": [(cols[0], BF)] * 2,
        }[epilogue]
        self.full = k.vmem((length, width), BF)
        self.values = [k.vmem((length, c), kind) for c, kind in kinds]
        kept = [self.full] + self.values
        self.saved = [(v, k.output(v.shape, v.dtype), k.sem(4, 2)) for v in kept if kept.index(v) in save]
        self.sems = [k.sem(2) for _ in range(6)]
        k.late.append(self.end)

    def span(self, owner, sub):
        return pl.ds(pl.multiple_of(owner * self.rows + sub * self.half, self.half), self.half)

    def move(self, kind, i):
        me, sib, cross, _ = places()
        full = self.full.ref
        owner, peer, at = {"cross": (me, cross, 0), "sib": (me, sib, 2), "relay": (cross, sib, 4)}[kind]
        part = full.at[self.span(owner, i)]
        return remote(
            part, part, self.sems[at].ref.at[i], self.sems[at + 1].ref.at[i], {"tensor": peer}
        )

    def begin(self):
        me = places()[0]
        for i in range(2):

            def put(j, carry):
                at = i * self.half + j * STRIP
                part = self.x.ref[pl.ds(pl.multiple_of(at, STRIP), STRIP), :].astype(F32)
                if self.gain is not None:
                    val, row = self.gain
                    part = norm_rows(part, val.ref[row : row + 1, :])
                to = pl.ds(pl.multiple_of(me * self.rows + at, STRIP), STRIP)
                self.full.ref[to, :] = part.astype(BF)
                return carry

            lax.fori_loop(0, self.half // STRIP, put, 0)
            self.move("cross", i).start()
            self.move("sib", i).start()

    def loop(self):
        me, sib, cross, diag = places()
        rows, half = self.rows, self.half
        for w in self.weights:
            w.wait()

        def step(p, carry):
            far, sub = p // 2, p % 2
            near = (1 - sub) * me + sub * sib
            first = (1 - far) * near * rows + far * (cross * rows + sub * half)
            second = (1 - far) * (near * rows + half) + far * (diag * rows + sub * half)
            pair = [pl.ds(pl.multiple_of(v, half), half) for v in (first, second)]

            @pl.when(p == 1)
            def _():
                self.move("sib", 0).wait_recv()
                self.move("sib", 1).wait_recv()

            for i in range(2):

                @pl.when(p == 2 + i)
                def _():
                    self.move("cross", i).wait_recv()
                    self.move("relay", i).start()
                    self.move("relay", i).wait_recv()

            def both(val):
                return jnp.concatenate([val.ref[pair[0], :], val.ref[pair[1], :]], axis=0)

            a = both(self.full)
            prods = [contract(a, w.buf.ref[...], 1, 1 if self.trans else 0) for w in self.weights]
            if self.epilogue == "plain":
                values = prods
            elif self.epilogue == "ffn":
                sig, silu = silu_parts(prods[0])
                values = [prods[0], prods[1], silu * prods[1]]
            else:
                gate, up = (both(v).astype(F32) for v in self.extras)
                sig, silu = silu_parts(gate)
                values = [prods[0] * up * sig * (1.0 + gate * (1.0 - sig)), prods[0] * silu]
            for val, value in zip(self.values, values):
                value = value.astype(val.dtype)
                for j in range(2):
                    val.ref[pair[j], :] = value[j * half : (j + 1) * half]
            for val, out, sem in self.saved:
                for j in range(2):
                    pltpu.make_async_copy(
                        val.ref.at[pair[j]], out.ref.at[pair[j]], sem.ref.at[p, j]
                    ).start()
            return carry

        lax.fori_loop(0, 4, step, 0)

    def end(self):
        for i in range(2):
            for kind in ("cross", "sib", "relay"):
                self.move(kind, i).wait_send()
        part = pl.ds(0, self.half)
        for val, out, sem in self.saved:
            for p in range(4):
                for j in range(2):
                    pltpu.make_async_copy(val.ref.at[part], out.ref.at[part], sem.ref.at[p, j]).wait()


class Scatter:
    def __init__(self, k, operands, weights, resid, back=None, trans=False, low=False):
        rows, width = resid.shape
        half = rows // 2
        self.operands, self.weights, self.resid, self.back = operands, weights, resid, back
        self.trans, self.low, self.rows, self.half = trans, low, rows, half
        self.keep, self.own = k.vmem((2, half, width), F32), k.vmem((rows, width), F32)
        self.to_s, self.from_s, self.to_c, self.from_c = (
            k.vmem((2, half, width), BF) for _ in range(4)
        )
        self.to_o, self.from_o = k.vmem((rows, width), BF), k.vmem((rows, width), BF)
        self.out = k.vmem((rows, width), BF if low else F32)
        self.gain_grad = k.vmem((1, width), F32) if back else None
        self.sems = [k.sem(2) for _ in range(4)] + [k.sem(1) for _ in range(2)]
        k.late.append(self.end)

    def move(self, kind, i=0):
        _, sib, cross, _ = places()
        at, src, dst, peer = {
            "diag": (0, self.to_s, self.from_s, sib),
            "cross": (2, self.to_c, self.from_c, cross),
            "near": (4, self.to_o, self.from_o, sib),
        }[kind]
        src, dst = (src.ref, dst.ref) if kind == "near" else (src.ref.at[i], dst.ref.at[i])
        return remote(
            src, dst, self.sems[at].ref.at[i], self.sems[at + 1].ref.at[i], {"tensor": peer}
        )

    def pass_on(self, i):
        self.move("diag", i).wait_recv()

        def add_rows(at):
            total = self.keep.ref[i, at, :] + self.from_s.ref[i, at, :].astype(F32)
            self.to_c.ref[i, at, :] = total.astype(BF)

        chunked(self.half, add_rows)
        self.move("cross", i).start()

    def loop(self):
        me, sib, cross, diag = places()
        rows, half = self.rows, self.half
        for w in self.weights:
            w.wait()

        def step(p, carry):
            near, sub = p // 2, p % 2
            base = near * ((1 - sub) * sib + sub * me) * rows
            first = base + (1 - near) * (cross * rows + sub * half)
            second = base + near * half + (1 - near) * (diag * rows + sub * half)
            pair = [pl.ds(pl.multiple_of(v, half), half) for v in (first, second)]
            total = None
            for y, w in zip(self.operands, self.weights):
                a = jnp.concatenate([y.ref[pair[0], :], y.ref[pair[1], :]], axis=0)
                prod = contract(a, w.buf.ref[...], 1, 1 if self.trans else 0)
                total = prod if total is None else total + prod

            self.own.ref[...] = total

            @pl.when(p < 2)
            def _():
                def put(at):
                    self.keep.ref[p, at, :] = self.own.ref[at, :]
                    lower = pl.ds(pl.multiple_of(at.start + half, 16), at.size)
                    self.to_s.ref[p, at, :] = self.own.ref[lower, :].astype(BF)

                chunked(half, put)
                self.move("diag", p).start()

            @pl.when(p == 2)
            def _():
                def put(at):
                    self.to_o.ref[at, :] = self.own.ref[at, :].astype(BF)

                chunked(rows, put)
                self.move("near").start()

            @pl.when((p == 1) | (p == 2))
            def _():
                self.pass_on(p - 1)

            return carry

        lax.fori_loop(0, 4, step, 0)

    def finish(self):
        self.move("near").wait_recv()
        if self.back:
            self.gain_grad.ref[...] = jnp.zeros_like(self.gain_grad.ref)
        for i in range(2):
            self.move("cross", i).wait_recv()

            def add_rows(j, carry):
                inner = block_of(j, STRIP)
                part = pl.ds(pl.multiple_of(i * self.half + j * STRIP, STRIP), STRIP)
                total = self.own.ref[part, :] + self.from_o.ref[part, :].astype(F32)
                total = total + self.from_c.ref[i, inner, :].astype(F32)
                resid = self.resid.ref[part, :].astype(F32)
                if self.back:
                    value, (gain, row) = self.back
                    total, gain_grad = norm_back(
                        value.ref[part, :].astype(F32), gain.ref[row : row + 1, :], total
                    )
                    self.gain_grad.ref[...] += gain_grad
                self.out.ref[part, :] = (resid + total).astype(self.out.dtype)
                return carry

            lax.fori_loop(0, self.half // STRIP, add_rows, 0)

    def end(self):
        self.move("near").wait_send()
        for i in range(2):
            self.move("diag", i).wait_send()
            self.move("cross", i).wait_send()


def delayed(values, by):
    if by == 0:
        return values
    row = lax.broadcasted_iota(jnp.int32, values.shape, 0)
    return jnp.where(row < by, 0.0, pltpu.roll(values, by, 0))


def advanced(values, by):
    if by == 0:
        return values
    length = values.shape[0]
    row = lax.broadcasted_iota(jnp.int32, values.shape, 0)
    return jnp.where(row >= length - by, 0.0, pltpu.roll(values, length - by, 0))


CONV_COLS = 128


class Conv:
    def __init__(self, k, projected, value, kernel):
        self.projected, self.value, self.kernel = projected, value, kernel
        self.y = k.vmem(value.shape, BF)

    def parts(self, j):
        channels = self.value.shape[1]
        at = block_of(j, CONV_COLS)
        b_gate = self.projected.ref[:, at]
        c_gate = self.projected.ref[:, block_of(j + channels // CONV_COLS, CONV_COLS)]
        x_value, taps = self.value.ref[:, at], self.kernel.ref[:, at]
        product = b_gate * x_value
        count = taps.shape[0]
        causal = jnp.zeros_like(product)
        for i in range(count):
            causal = causal + taps[i : i + 1] * delayed(product, count - 1 - i)
        return at, b_gate, c_gate, x_value, taps, product, causal

    def run(self):
        def step(j, carry):
            at, _, c_gate, _, _, _, causal = self.parts(j)
            self.y.ref[:, at] = (c_gate * causal).astype(BF)
            return carry

        lax.fori_loop(0, self.value.shape[1] // CONV_COLS, step, 0)


class ConvBack(Conv):
    def __init__(self, k, projected, value, kernel, d_y):
        self.projected, self.value, self.kernel, self.d_y = projected, value, kernel, d_y
        self.d_proj = k.vmem(projected.shape, BF)
        self.d_value = k.vmem(value.shape, BF)
        self.d_kernel = k.vmem(kernel.shape, F32)

    def run(self):
        channels = self.value.shape[1]

        def step(j, carry):
            at, b_gate, c_gate, x_value, taps, product, causal = self.parts(j)
            d_y = self.d_y.ref[:, at]
            d_causal = d_y * c_gate
            count = taps.shape[0]
            d_product = jnp.zeros_like(product)
            for i in range(count):
                by = count - 1 - i
                row = jnp.sum(d_causal * delayed(product, by), axis=0, keepdims=True)
                self.d_kernel.ref[i : i + 1, at] = row
                d_product = d_product + taps[i : i + 1] * advanced(d_causal, by)
            self.d_proj.ref[:, at] = (d_product * x_value).astype(BF)
            upper = block_of(j + channels // CONV_COLS, CONV_COLS)
            self.d_proj.ref[:, upper] = (d_y * causal).astype(BF)
            self.d_value.ref[:, at] = (d_product * b_gate).astype(BF)
            return carry

        lax.fori_loop(0, channels // CONV_COLS, step, 0)


def head_mean(values, head_size):
    width = values.shape[1]
    row = lax.broadcasted_iota(jnp.int32, (width, width), 0) // head_size
    col = lax.broadcasted_iota(jnp.int32, (width, width), 1) // head_size
    group = jnp.where(row == col, 1.0 / head_size, 0.0).astype(F32)
    return lax.dot_general(
        values, group, (((1,), (0,)), ((), ())),
        precision=lax.Precision.HIGHEST, preferred_element_type=F32,
    )


def turn(values, head_size, back):
    width, half = values.shape[1], head_size // 2
    lane = lax.broadcasted_iota(jnp.int32, values.shape, 1) % head_size
    upper = pltpu.roll(values, width - half, 1)
    lower = pltpu.roll(values, half, 1)
    return jnp.where(lane < half, upper, -lower) if back else jnp.where(lane < half, -upper, lower)


def head_norm(values, gain, head_size):
    return values * lax.rsqrt(head_mean(values * values, head_size) + EPS) * gain


def head_norm_back(values, gain, grad_in, head_size):
    row_scale = lax.rsqrt(head_mean(values * values, head_size) + EPS)
    normed = values * row_scale
    gain_grad = jnp.sum(grad_in * normed, axis=0, keepdims=True)
    scaled = grad_in * gain
    return row_scale * (scaled - normed * head_mean(scaled * normed, head_size)), gain_grad


def block_weights(q_rows, keys):
    scores = [contract(q_rows, k_rows, 1, 1) for k_rows in keys]
    query = lax.broadcasted_iota(jnp.int32, scores[-1].shape, 0)
    key = lax.broadcasted_iota(jnp.int32, scores[-1].shape, 1)
    scores[-1] = jnp.where(key <= query, scores[-1], MASKED)
    top = functools.reduce(
        jnp.maximum, [jnp.max(part, axis=1, keepdims=True) for part in scores]
    )
    exps = [jnp.exp(part - top) for part in scores]
    scale = 1.0 / sum(jnp.sum(part, axis=1, keepdims=True) for part in exps)
    return [part * scale for part in exps]


def key_blocks(i):
    blocks = [pl.ds(0, i * ROW_BLOCK)] if i else []
    return blocks + [pl.ds(i * ROW_BLOCK, ROW_BLOCK)]


class Heads:
    def __init__(self, projected, tables, size):
        assert size in (16, 64, 256), size
        self.projected, self.size = projected, size
        self.gain, self.cos, self.sin = (v.buf for v in tables)
        self.loads = tables
        self.length, width = projected.shape
        self.q_cols, self.k_cols = width // 2, width // 4
        self.heads, self.kv_heads = self.q_cols // size, self.k_cols // size
        self.share = self.heads // self.kv_heads

    def per_head(self, k, count, kind):
        return k.vmem((count, self.length, self.size), kind)

    def split(self, val, rows, values):
        for h in range(val.shape[0]):
            val.ref[h, rows, :] = values[:, h * self.size : (h + 1) * self.size]

    def join(self, val, rows):
        return jnp.concatenate([val.ref[h, rows, :] for h in range(val.shape[0])], axis=1)

    def gains(self):
        gain = self.gain.ref[...]
        return (
            jnp.concatenate([gain[0:1]] * self.heads, axis=1),
            jnp.concatenate([gain[1:2]] * self.kv_heads, axis=1),
        )

    def angles(self, rows):
        c, n = self.cos.ref[rows, :], self.sin.ref[rows, :]
        repeat = self.q_cols // c.shape[1]
        return jnp.concatenate([c] * repeat, axis=1), jnp.concatenate([n] * repeat, axis=1)

    def blocks(self, step):
        lax.fori_loop(0, self.length // ROW_BLOCK, lambda p, c: step(block_of(p, ROW_BLOCK)) or c, 0)


class Attend(Heads):
    def __init__(self, k, projected, tables, size):
        super().__init__(projected, tables, size)
        self.q_rot = k.vmem((self.length, self.q_cols), BF)
        self.k_rot = k.vmem((self.length, self.k_cols), BF)
        self.y = k.vmem((self.length, self.q_cols), BF)
        self.q_h, self.y_h = (self.per_head(k, self.heads, BF) for _ in range(2))
        self.k_h, self.v_h = (self.per_head(k, self.kv_heads, BF) for _ in range(2))

    def run(self, *between):
        for load in self.loads:
            load.wait()
        size, q_cols, k_cols, proj = self.size, self.q_cols, self.k_cols, self.projected.ref

        def prepare(rows):
            c, n = self.angles(rows)
            q_gain, k_gain = self.gains()
            q = head_norm(proj[rows, :q_cols], q_gain, size)
            q = (q * c + turn(q, size, False) * n).astype(BF)
            k = head_norm(proj[rows, q_cols : q_cols + k_cols], k_gain, size)
            k = (k * c[:, :k_cols] + turn(k, size, False) * n[:, :k_cols]).astype(BF)
            self.q_rot.ref[rows, :] = q
            self.k_rot.ref[rows, :] = k
            self.split(self.q_h, rows, (q.astype(F32) * size**-0.5).astype(BF))
            self.split(self.k_h, rows, k)
            self.split(self.v_h, rows, proj[rows, q_cols + k_cols :].astype(BF))

        self.blocks(prepare)

        def head(h, carry):
            g = h // self.share

            @pl.when(h == self.heads // 2)
            def _():
                for step in between:
                    step()

            for i in range(self.length // ROW_BLOCK):
                rows, seen = pl.ds(i * ROW_BLOCK, ROW_BLOCK), key_blocks(i)
                weights = block_weights(
                    self.q_h.ref[h, rows, :], [self.k_h.ref[g, at, :] for at in seen]
                )
                value = sum(
                    contract(part.astype(BF), self.v_h.ref[g, at, :], 1, 0)
                    for part, at in zip(weights, seen)
                )
                self.y_h.ref[h, rows, :] = value.astype(BF)
            return carry

        lax.fori_loop(0, self.heads, head, 0)

        def place(rows):
            self.y.ref[rows, :] = self.join(self.y_h, rows)

        self.blocks(place)


class AttendBack(Heads):
    def __init__(self, k, projected, tables, size, q_rot, k_rot, d_y):
        super().__init__(projected, tables, size)
        self.q_rot, self.k_rot, self.d_y = q_rot, k_rot, d_y
        self.q_h, self.dy_h = (self.per_head(k, self.heads, BF) for _ in range(2))
        self.k_h, self.v_h = (self.per_head(k, self.kv_heads, BF) for _ in range(2))
        self.dq_h = self.per_head(k, self.heads, F32)
        self.dk_h, self.dv_h = (self.per_head(k, self.kv_heads, F32) for _ in range(2))
        self.d_proj = k.vmem(projected.shape, BF)
        self.q_gain, self.k_gain = k.vmem((1, self.q_cols), F32), k.vmem((1, self.k_cols), F32)

    def run(self, *between):
        for load in self.loads:
            load.wait()
        size, q_cols, k_cols, proj = self.size, self.q_cols, self.k_cols, self.projected.ref
        scale = size**-0.5
        dq_h, dk_h, dv_h = self.dq_h.ref, self.dk_h.ref, self.dv_h.ref

        def prepare(rows):
            self.split(self.q_h, rows, (self.q_rot.ref[rows, :].astype(F32) * scale).astype(BF))
            self.split(self.dy_h, rows, self.d_y.ref[rows, :].astype(BF))
            self.split(self.k_h, rows, self.k_rot.ref[rows, :])
            self.split(self.v_h, rows, proj[rows, q_cols + k_cols :].astype(BF))

        self.blocks(prepare)

        def clear(rows):
            for val in (dk_h, dv_h):
                val[:, rows, :] = jnp.zeros((self.kv_heads, ROW_BLOCK, size), F32)

        self.blocks(clear)

        def head(h, carry):
            g = h // self.share

            @pl.when(h == self.heads // 2)
            def _():
                for step in between:
                    step()

            for i in range(self.length // ROW_BLOCK):
                rows, seen = pl.ds(i * ROW_BLOCK, ROW_BLOCK), key_blocks(i)
                q, low = self.q_h.ref[h, rows, :], self.dy_h.ref[h, rows, :]
                keys = [self.k_h.ref[g, at, :] for at in seen]
                probs = block_weights(q, keys)
                d_weights = [contract(low, self.v_h.ref[g, at, :], 1, 1) for at in seen]
                inner = sum(
                    jnp.sum(a * b, axis=1, keepdims=True) for a, b in zip(probs, d_weights)
                )
                d_q = 0.0
                for at, k, prob, d_weight in zip(seen, keys, probs, d_weights):
                    dv_h[g, at, :] += contract(prob.astype(BF), low, 0, 0)
                    d_scores = (prob * (d_weight - inner)).astype(BF)
                    d_q = d_q + contract(d_scores, k, 1, 0)
                    dk_h[g, at, :] += contract(d_scores, q, 0, 0)
                dq_h[h, rows, :] = d_q * scale
            return carry

        lax.fori_loop(0, self.heads, head, 0)
        self.q_gain.ref[...] = jnp.zeros_like(self.q_gain.ref)
        self.k_gain.ref[...] = jnp.zeros_like(self.k_gain.ref)

        def finish(rows):
            c, n = self.angles(rows)
            dq, dk, dv = (self.join(v, rows) for v in (self.dq_h, self.dk_h, self.dv_h))
            dq = dq * c + turn(dq * n, size, True)
            dk = dk * c[:, :k_cols] + turn(dk * n[:, :k_cols], size, True)
            q_gain, k_gain = self.gains()
            dq, q_sum = head_norm_back(proj[rows, :q_cols], q_gain, dq, size)
            dk, k_sum = head_norm_back(proj[rows, q_cols : q_cols + k_cols], k_gain, dk, size)
            self.q_gain.ref[...] += q_sum
            self.k_gain.ref[...] += k_sum
            self.d_proj.ref[rows, :q_cols] = dq.astype(BF)
            self.d_proj.ref[rows, q_cols : q_cols + k_cols] = dk.astype(BF)
            self.d_proj.ref[rows, q_cols + k_cols :] = dv.astype(BF)

        self.blocks(finish)


def body(boundary, norm_gain, mix_in, mix_out, w_gate, w_up, w_down, conv_x, conv_kernel, qk_gain):
    first = lax.axis_index("section") == 0
    tensor_index = lax.axis_index("tensor")
    model_width = boundary.shape[3]
    channels = mix_out.shape[1]
    row_shape = boundary.shape[2:]
    length, size = 4 * row_shape[0], qk_gain.shape[1]

    seqs, own_gain = boundary[0], norm_gain[0]
    sh_in, sh_out, sh_gate, sh_up, sh_down = (v[0] for v in (mix_in, mix_out, w_gate, w_up, w_down))

    def gains_of(k, block, other, early=True):
        own, moved = k.input(own_gain), as_val(k, other)
        sources = lambda s, d, t: [(s == block, own.ref), (s == 1 - block, moved.ref)]
        return Load(k, sources, own.shape, F32, early)

    def start_rows(k, slot, other, early=True):
        own, moved = k.input(seqs), as_val(k, other)
        sources = lambda s, d, t: [(s == slot, own.ref.at[slot]), (s == 1 - slot, moved.ref)]
        return Load(k, sources, row_shape, BF, early)

    def wait(*items):
        return [item.wait for item in items]

    k = Kernel(0)
    t_seq = None
    seq_val = k.input(seqs)

    def seq_moves(s, d, t):
        return [([(None, seq_val.ref.at[1 - s])], t_seq.out.ref, {"section": 1 - s})], []

    t_in, t_out, t_up = (x_half(k, v) for v in (sh_in, sh_out, sh_up))
    gate_lo, gate_hi = (Part(sh_gate, i * (sh_gate.shape[0] // 2), sh_gate.shape[0] // 2) for i in range(2))
    down_lo, down_hi = (Part(sh_down, i * (sh_down.shape[0] // 2), sh_down.shape[0] // 2) for i in range(2))
    t_gate0a, t_gate0b = x_half(k, gate_lo, 0), x_move(k, gate_hi, 0)
    t_down0a, t_down0b = x_half(k, down_lo, 0), x_move(k, down_hi, 0)
    t_gate1, t_down1 = x_half(k, sh_gate, 1), x_move(k, sh_down, 1)
    t_seq = Task(k, row_shape, "section", seq_moves, 1)
    t_gain, z_cols = x_move(k, own_gain), z_gather(k, conv_x)
    z_in0, z_out0 = z_gather_half(k, sh_in, t_in.out, 0), z_gather_half(k, sh_out, t_out.out, 0)
    z_gate0a = z_gather_half(k, gate_lo, t_gate0a.out, 0)
    z_gate0b, x_gate0a = z_gather_whole(k, gate_hi, t_gate0b.out, 0), x_move(k, z_gate0a.out)
    z_up0 = z_gather_half(k, sh_up, t_up.out, 0)
    x_cols, x_in0, x_out0 = (x_move(k, v.out) for v in (z_cols, z_in0, z_out0))
    x_load, gain_load = start_rows(k, 0, t_seq.out, False), gains_of(k, 0, t_gain.out, False)
    taps = load_all(k, conv_kernel)
    angles = Angles(k, length, size, 128)
    w_in0, w_cols = Weight(k, "rows", (z_in0.out, x_in0.out)), Weight(k, "conv", (z_cols.out, x_cols.out))
    w_out0 = Weight(k, "cols", (z_out0.out, x_out0.out))
    g0 = Gather(k, x_load.buf, (gain_load.buf, 0), [w_in0, w_cols], save=(0, 1, 2))
    conv = Conv(k, g0.values[0], g0.values[1], taps.buf)
    y0 = Save(k, conv.y)
    s1 = Scatter(k, [conv.y], [w_out0], x_load.buf)
    mid0 = Save(k, s1.out)
    k.do(t_in.send, t_out.send, z_cols.send, t_gate0b.send, t_gate0a.send, t_gate1.send)
    k.do(t_gain.send, t_seq.send)
    k.do(t_in.wait, z_in0.send, t_out.wait, z_out0.send, z_cols.step, z_in0.step, z_out0.step)
    k.do(z_cols.step, z_in0.step, z_out0.step, t_gate0b.wait, z_gate0b.send)
    k.do(t_gate0a.wait, z_gate0a.send)
    k.do(z_cols.wait, x_cols.send, z_in0.wait, x_in0.send, z_out0.wait, x_out0.send, t_up.send)
    k.do(t_gain.wait, gain_load.start, t_seq.wait, x_load.start, gain_load.wait, x_load.wait)
    k.do(g0.begin, z_gate0b.step, z_gate0a.step, angles.run, z_gate0b.step, z_gate0a.step)
    k.do(x_cols.wait, w_cols.start, x_in0.wait, w_in0.start, z_gate0a.wait, x_gate0a.send)
    k.do(t_down0b.send, t_down0a.send, t_down1.send, t_up.wait, z_up0.send)
    k.do(g0.loop, z_up0.step, taps.wait, conv.run, y0.start)
    k.do(x_out0.wait, w_out0.start, s1.loop, z_up0.step, s1.finish, mid0.start)
    k.do(*wait(t_gate1, t_down0a, t_down0b, t_down1, z_gate0b, x_gate0a, z_up0))
    k.build()
    a0, proj0, value0 = (out for _, out, _ in g0.saved)
    table_arrays = [qk_gain] + [v.out for v in angles.saves]
    y0, mid0 = y0.out, mid0.out

    k = Kernel(1)
    x_up0, z_gate1 = x_move(k, z_up0.out), z_gather_half(k, sh_gate, t_gate1.out, 1)
    z_down0a = z_gather_half(k, down_lo, t_down0a.out, 0)
    z_down0b = z_gather_whole(k, down_hi, t_down0b.out, 0)
    z_in1, z_out1 = z_gather_half(k, sh_in, t_in.out, 1), z_gather_half(k, sh_out, t_out.out, 1)
    x_down0a, x_in1, x_out1 = (x_move(k, v.out) for v in (z_down0a, z_in1, z_out1))
    rows, gain_load = load_all(k, mid0), gains_of(k, 0, t_gain.out)
    w_gate0 = Weight(k, "rows", (z_gate0a.out, x_gate0a.out), (z_gate0b.out, None), early=True)
    w_up0 = Weight(k, "rows", (z_up0.out, x_up0.out))
    w_down0 = Weight(k, "cols", (z_down0a.out, x_down0a.out), (z_down0b.out, None))
    g2 = Gather(
        k, rows.buf, (gain_load.buf, 1), [w_gate0, w_up0], epilogue="ffn", save=(0, 1, 2, 3)
    )
    s3 = Scatter(k, [g2.values[2]], [w_down0], rows.buf, low=True)
    z_rows = Save(k, s3.out)
    k.do(x_up0.send, z_down0a.send, z_down0b.send, rows.wait, gain_load.wait, g2.begin)
    k.do(z_in1.send, z_out1.send, z_down0a.step, z_in1.step, z_out1.step, z_down0b.step)
    k.do(z_down0a.step, z_in1.step, z_out1.step, z_gate1.send, z_down0a.wait, x_down0a.send)
    k.do(x_up0.wait, w_up0.start, z_down0b.step, g2.loop, z_gate1.step)
    k.do(z_in1.wait, x_in1.send, z_out1.wait, x_out1.send, z_down0b.wait, x_down0a.wait)
    k.do(w_down0.start, s3.loop, z_gate1.step, s3.finish, z_rows.start)
    k.do(*wait(x_in1, x_out1, z_gate1))
    k.build()
    m0, gate0, up0, hid0 = (out for _, out, _ in g2.saved)
    z_rows = z_rows.out

    k = Kernel(2)
    x_gate1, z_up1 = x_move(k, z_gate1.out), z_gather_half(k, sh_up, t_up.out, 1)
    z_down1a, z_down1b = (z_gather_whole(k, sh_down, t_down1.out, 1, i) for i in range(2))
    x_up1 = x_move(k, z_up1.out)
    rows, gain_load = load_all(k, z_rows), gains_of(k, 1, t_gain.out)
    tables = [load_all(k, v) for v in table_arrays]
    w_in1 = Weight(k, "rows", (z_in1.out, x_in1.out), early=True)
    w_out1 = Weight(k, "cols", (z_out1.out, x_out1.out), early=True)
    g4 = Gather(k, rows.buf, (gain_load.buf, 0), [w_in1], save=(0, 1))
    attend = Attend(k, g4.values[0], tables, size)
    kept = [Save(k, v) for v in (attend.q_rot, attend.k_rot, attend.y)]
    s5 = Scatter(k, [attend.y], [w_out1], rows.buf)
    mid1 = Save(k, s5.out)
    k.do(x_gate1.send, z_up1.send, rows.wait, gain_load.wait, g4.begin, z_up1.step)
    k.do(z_down1a.send, g4.loop, z_up1.step, z_down1b.send)
    k.do(lambda: attend.run(z_up1.wait, x_up1.send, z_down1a.step))
    k.do(*(v.start for v in kept))
    k.do(z_down1b.step, s5.loop, z_down1a.step, z_down1b.step, s5.finish, mid1.start)
    k.do(*wait(x_gate1, x_up1, z_down1a, z_down1b))
    k.build()
    a1, proj1 = (out for _, out, _ in g4.saved)
    q_rot, k_rot, y1 = (v.out for v in kept)
    mid1 = mid1.out

    k = Kernel(3)
    rows, gain_load = load_all(k, mid1), gains_of(k, 1, t_gain.out)
    cot = start_rows(k, 1, t_seq.out)
    w_gate1 = Weight(k, "rows", (z_gate1.out, x_gate1.out), early=True)
    w_up1 = Weight(k, "rows", (z_up1.out, x_up1.out), early=True)
    w_down1 = Weight(k, "cols", (z_down1a.out, None), (z_down1b.out, None), early=True)
    g6 = Gather(k, rows.buf, (gain_load.buf, 1), [w_gate1, w_up1], epilogue="ffn")
    g8 = Gather(
        k, cot.buf, None, [w_down1], [g6.values[0], g6.values[1]], trans=True, epilogue="ffn_back"
    )
    p_down1 = Product(k, g6.values[2], g8.full)
    p_gate1, p_up1 = Product(k, g6.full, g8.values[0]), Product(k, g6.full, g8.values[1])
    s9 = Scatter(k, g8.values, [w_gate1, w_up1], cot.buf, (rows.buf, (gain_load.buf, 1)), True)
    hid1 = Save(k, g6.values[2])
    d_mid1, gain11 = Save(k, s9.out), Save(k, s9.gain_grad)
    k.do(rows.wait, gain_load.wait, g6.begin, cot.wait, g8.begin, g6.loop, hid1.start, g8.loop)
    k.do(s9.loop, p_down1.run, p_gate1.run, p_up1.run)
    k.do(s9.finish, d_mid1.start, gain11.start, p_down1.wait, p_gate1.wait, p_up1.wait)
    k.build()
    hid1, d_mid1, gain11 = hid1.out, d_mid1.out, gain11.out

    k = Kernel(4)
    r_down1 = x_half(k, p_down1.out)
    r_gate1, q_up1 = x_slots(k, p_gate1.out, "rows"), sum_scatter(k, "rows", p_up1.out)
    q_gate1 = sum_scatter(k, "rows", p_gate1.out, r_gate1.out)
    rows, gain_load = load_all(k, d_mid1), gains_of(k, 1, t_gain.out)
    value = load_all(k, z_rows)
    tables = [load_all(k, v) for v in table_arrays]
    proj, q_load, k_load, y_load, a_load = (load_all(k, v) for v in (proj1, q_rot, k_rot, y1, a1))
    w_in1 = Weight(k, "rows", (z_in1.out, x_in1.out), early=True)
    w_out1 = Weight(k, "cols", (z_out1.out, x_out1.out), early=True)
    g10 = Gather(k, rows.buf, None, [w_out1], trans=True)
    p_out1 = Product(k, y_load.buf, g10.full)
    back = AttendBack(k, proj.buf, tables, size, q_load.buf, k_load.buf, g10.values[0])
    p_in1 = Product(k, a_load.buf, back.d_proj)
    s11 = Scatter(
        k, [back.d_proj], [w_in1], rows.buf, (value.buf, (gain_load.buf, 0)), True, low=True
    )
    d_z, gain10 = Save(k, s11.out), Save(k, s11.gain_grad)
    head_gains = [Save(k, back.q_gain), Save(k, back.k_gain)]
    k.early.append(q_up1.load)
    k.do(r_gate1.send, r_down1.send, rows.wait, g10.begin, q_up1.send, g10.loop)
    k.do(y_load.wait, p_out1.run, q_up1.step)
    k.do(proj.wait, q_load.wait, k_load.wait)
    k.do(lambda: back.run(r_gate1.wait, q_gate1.add, q_up1.step))
    k.do(q_gate1.step, *(v.start for v in head_gains))
    k.do(gain_load.wait, value.wait, s11.loop, a_load.wait, p_in1.run)
    k.do(s11.finish, d_z.start, gain10.start, q_gate1.step, p_out1.wait, p_in1.wait)
    k.do(*wait(r_down1, q_up1, q_gate1))
    k.build()
    d_z, gain10 = d_z.out, gain10.out
    q_gain, k_gain = (v.out for v in head_gains)

    k = Kernel(5)
    m_up1, r_out1 = x_move(k, q_up1.out, 0), x_half(k, p_out1.out)
    q_out1 = sum_scatter(k, "cols", p_out1.out, r_out1.out)
    r_in1 = x_slots(k, p_in1.out, "rows")
    q_in1 = sum_scatter(k, "rows", p_in1.out, r_in1.out)
    q_down1 = sum_scatter(k, "cols", p_down1.out, r_down1.out)
    rows, value, gain_load = load_all(k, d_z), load_all(k, mid0), gains_of(k, 0, t_gain.out)
    gate_load, up_load, hid_load, m_load = (load_all(k, v) for v in (gate0, up0, hid0, m0))
    w_gate0 = Weight(k, "rows", (z_gate0a.out, x_gate0a.out), (z_gate0b.out, None), early=True)
    w_up0 = Weight(k, "rows", (z_up0.out, x_up0.out), early=True)
    w_down0 = Weight(k, "cols", (z_down0a.out, x_down0a.out), (z_down0b.out, None), early=True)
    g12 = Gather(
        k, rows.buf, None, [w_down0], [gate_load.buf, up_load.buf], trans=True, epilogue="ffn_back"
    )
    p_down0 = Product(k, hid_load.buf, g12.full)
    p_gate0, p_up0 = Product(k, m_load.buf, g12.values[0]), Product(k, m_load.buf, g12.values[1])
    r_down0 = x_half(k, p_down0.out)
    s13 = Scatter(
        k, g12.values, [w_gate0, w_up0], rows.buf, (value.buf, (gain_load.buf, 1)), True
    )
    d_mid0, gain01 = Save(k, s13.out), Save(k, s13.gain_grad)
    k.early.append(q_down1.load)
    k.do(r_in1.send, r_out1.send, m_up1.send, rows.wait, g12.begin, q_down1.send)
    k.do(gate_load.wait, up_load.wait, g12.loop, q_down1.step)
    k.do(hid_load.wait, p_down0.run, p_down0.wait, r_down0.send)
    k.do(r_in1.wait, q_in1.add, r_out1.wait, q_out1.add, q_down1.step)
    k.do(s13.loop, q_in1.step, q_out1.step, m_load.wait, p_gate0.run, q_in1.step, q_out1.step)
    k.do(p_up0.run, value.wait, gain_load.wait)
    k.do(s13.finish, d_mid0.start, gain01.start, p_gate0.wait, p_up0.wait)
    k.do(*wait(q_out1, q_in1, q_down1, m_up1, r_down0))
    k.build()
    d_mid0, gain01 = d_mid0.out, gain01.out

    k = Kernel(6)
    r_gate0 = x_slots(k, p_gate0.out, "rows")
    q_gate0 = sum_scatter(k, "rows", p_gate0.out, r_gate0.out)
    q_down0 = sum_scatter(k, "cols", p_down0.out, r_down0.out)
    q_up0 = sum_scatter(k, "rows", p_up0.out)
    m_up0 = x_move(k, q_up0.out, 1)
    e_down1 = Finish(k, q_down1.out, 1)
    e_gate1, e_out1, e_in1 = (Finish(k, v.out, 1) for v in (q_gate1, q_out1, q_in1))
    rows, gain_load = load_all(k, d_mid0), gains_of(k, 0, t_gain.out)
    x_load, taps = start_rows(k, 0, t_seq.out), load_all(k, conv_kernel)
    y_load, a_load, proj, value = (load_all(k, v) for v in (y0, a0, proj0, value0))
    w_in0 = Weight(k, "rows", (z_in0.out, x_in0.out), early=True)
    w_cols = Weight(k, "conv", (z_cols.out, x_cols.out), early=True)
    w_out0 = Weight(k, "cols", (z_out0.out, x_out0.out), early=True)
    g14 = Gather(k, rows.buf, None, [w_out0], trans=True)
    p_out0 = Product(k, y_load.buf, g14.full)
    back = ConvBack(k, proj.buf, value.buf, taps.buf, g14.values[0])
    p_in0, p_cols = Product(k, a_load.buf, back.d_proj), Product(k, a_load.buf, back.d_value)
    r_out0, r_in0 = x_half(k, p_out0.out), x_slots(k, p_in0.out, "rows")
    r_cols = x_slots(k, p_cols.out, "conv")
    q_out0, q_in0 = sum_scatter(k, "cols", p_out0.out, r_out0.out), sum_scatter(k, "rows", p_in0.out, r_in0.out)
    q_cols = sum_scatter(k, "conv", p_cols.out, r_cols.out)
    e_down0, e_gate0, e_out0, e_in0 = (
        Finish(k, v.out, 0) for v in (q_down0, q_gate0, q_out0, q_in0)
    )
    s15 = Scatter(
        k, [back.d_proj, back.d_value], [w_in0, w_cols], rows.buf,
        (x_load.buf, (gain_load.buf, 0)), True, low=True,
    )
    d_x = Save(k, s15.out)
    tap_rows = conv_kernel.shape[0]
    small = k.vmem((8, model_width), F32)
    small_out = Save(k, small)
    ready = [load_all(k, v) for v in (gain01, gain10, gain11)]
    head_loads = [load_all(k, v) for v in (q_gain, k_gain)]

    def fill_small():
        t = lax.axis_index("tensor")
        small.ref[...] = jnp.zeros_like(small.ref)
        small.ref[0:1, :] = s15.gain_grad.ref[...]
        for i, load in enumerate(ready):
            load.wait()
            small.ref[i + 1 : i + 2, :] = load.buf.ref[...]
        small.ref[4 : 4 + tap_rows, block_of(t, channels)] = back.d_kernel.ref[...]
        at = 0
        for load in head_loads:
            load.wait()
            width = load.buf.shape[1]
            small.ref[7:8, at : at + width] = load.buf.ref[...]
            at += width
        small_out.start()

    t_small = x_move(k, small_out.out)
    z_small = SumShare(k, [small_out.out, t_small.out], "dp")
    t_total = SumShare(k, [z_small.out], "tensor", slotted=True)
    hid_load, mid_load = load_all(k, hid1), load_all(k, mid1)
    w_down1 = Weight(k, "cols", (z_down1a.out, None), (z_down1b.out, None), early=True)
    s7 = Scatter(k, [hid_load.buf], [w_down1], mid_load.buf, low=True)
    y_rows = Save(k, s7.out)
    t_x, t_y = x_move(k, d_x.out, 1), x_move(k, y_rows.out, 0)
    k.early += [q_up0.load, q_down0.load]
    k.early += [v.load for v in (e_down1, e_gate1, e_out1, e_in1)]
    k.do(r_gate0.send, rows.wait, g14.begin, q_up0.send, q_down0.send)
    k.do(e_down1.send, e_gate1.send, e_out1.send, e_in1.send, g14.loop)
    k.do(y_load.wait, p_out0.run, p_out0.wait, r_out0.send, q_up0.step)
    k.do(proj.wait, value.wait, taps.wait, back.run, q_down0.step, a_load.wait)
    k.do(p_in0.run, p_cols.run, p_in0.wait, r_in0.send, p_cols.wait, r_cols.send)
    k.do(r_gate0.wait, q_gate0.add, x_load.wait, gain_load.wait, s15.loop, q_up0.step)
    k.do(q_down0.step, s15.finish, d_x.start, fill_small, d_x.wait, t_x.send)
    k.do(small_out.wait, t_small.send, q_gate0.step, hid_load.wait, mid_load.wait, s7.loop)
    k.do(r_out0.wait, q_out0.add, r_in0.wait, q_in0.add)
    k.do(r_cols.wait, q_cols.add, q_up0.wait, m_up0.send, q_down0.wait, e_down0.add)
    k.do(s7.finish, y_rows.start, y_rows.wait, t_y.send)
    k.do(q_gate0.step, q_out0.step, q_in0.step, q_cols.step, t_small.wait, z_small.add)
    k.do(q_gate0.wait, e_gate0.add, q_out0.step, q_in0.step, q_cols.step)
    k.do(z_small.wait, t_total.add, q_out0.wait, e_out0.add, q_in0.wait, e_in0.add)
    rest = (e_down1, e_gate1, e_out1, e_in1, q_cols, e_down0, e_gate0, m_up0, e_out0, e_in0)
    k.do(*wait(*rest, t_total, t_x, t_y))
    k.build()

    owned = [
        ([e_in0], [e_in1], 1),
        ([e_out0], [e_out1], 1),
        ([e_gate0], [e_gate1], 1),
        ([q_up0, m_up0], [q_up1, m_up1], 1),
        ([e_down0], [e_down1], 1),
        ([q_cols], [q_cols], 0),
    ]
    return pack(
        [(zero, one, lead) for zero, one, lead in owned], t_total, d_x.out, y_rows.out, t_x, t_y,
        (norm_gain.shape, conv_kernel.shape, qk_gain.shape),
    )


def slot_free(val, shape):
    value = val.out.array
    if value.ndim == 3 and value.shape[0] * value.shape[1] != shape[0]:
        value = jnp.sum(value.astype(F32), axis=0).astype(BF)
    return value.reshape(shape)


def pack_kernel(plan, *refs):
    n_in, leads, terms, tap_rows = plan
    ins, rest = refs[:n_in], refs[n_in:]
    result, gain_out, *grads, cols, taps, heads = rest[: len(leads) + 4]
    grads = [*grads, cols]
    room = iter(rest[len(leads) + 4 :])
    own_v, moved_v, small_v, *bufs = (next(room) for _ in range(3 + len(terms)))
    out_v = [next(room) for _ in leads]
    load_sem, store_sem = room
    s, t = lax.axis_index("section"), lax.axis_index("tensor")
    small, d_x, y_rows, moved, moved_y, *parts = ins

    def either(cond, zero, one, dst, sem):
        if zero is not None:
            pl.when(cond)(pltpu.make_async_copy(zero, dst, sem).start)
        if one is not None:
            pl.when(jnp.logical_not(cond))(pltpu.make_async_copy(one, dst, sem).start)

    first = s == 0
    either(first, d_x, y_rows, own_v, load_sem.at[0])
    either(first, moved, moved_y, moved_v, load_sem.at[1])
    pltpu.make_async_copy(small, small_v, load_sem.at[2]).start()
    for j, (zero, one, _) in enumerate(terms):
        either(
            first,
            None if zero is None else parts[zero],
            None if one is None else parts[one],
            bufs[j],
            load_sem.at[3 + j],
        )
    for j, (zero, one, i) in enumerate(terms):
        arrive = pltpu.make_async_copy(parts[one if zero is None else zero], bufs[j], load_sem.at[3 + j])
        begins = j == 0 or terms[j - 1][2] != i

        def put(j=j, i=i, begins=begins):
            def add_rows(at):
                value = bufs[j][at, :].astype(F32)
                out_v[i][at, :] = value if begins else out_v[i][at, :] + value

            chunked(bufs[j].shape[0], add_rows)

        if zero is None or one is None:
            cond = first if one is None else jnp.logical_not(first)

            @pl.when(cond)
            def _(arrive=arrive, put=put):
                arrive.wait()
                put()
        else:
            arrive.wait()
            put()
        if j + 1 == len(terms) or terms[j + 1][2] != i:
            dst = grads[i].at[0] if leads[i] else grads[i]
            pltpu.make_async_copy(out_v[i], dst, store_sem.at[i]).start()
    pltpu.make_async_copy(d_x, own_v, load_sem.at[0]).wait()
    pltpu.make_async_copy(moved, moved_v, load_sem.at[1]).wait()
    n = len(leads)
    stores = [
        pltpu.make_async_copy(own_v, result.at[0, s], store_sem.at[n]),
        pltpu.make_async_copy(moved_v, result.at[0, 1 - s], store_sem.at[n + 1]),
    ]
    for store in stores:
        store.start()
    pltpu.make_async_copy(small, small_v, load_sem.at[2]).wait()
    total = small_v[0]
    for i in range(1, small_v.shape[0]):
        total = total + small_v[i]
    gain_out[0] = jnp.where(first, total[0:2], total[2:4])
    channels, size = taps.shape[1], heads.shape[1]
    chosen = total[4 : 4 + tap_rows, 0:channels]
    for i in range(1, total.shape[1] // channels):
        chosen = jnp.where(t == i, total[4 : 4 + tap_rows, i * channels : (i + 1) * channels], chosen)
    taps[...] = chosen
    at = 0
    for row, width in enumerate((channels, channels // 2)):
        value = total[7:8, at : at + size]
        for i in range(1, width // size):
            value = value + total[7:8, at + i * size : at + (i + 1) * size]
        heads[row : row + 1, :] = value
        at += width
    for i, store in enumerate(leads):
        dst = grads[i].at[0] if store else grads[i]
        pltpu.make_async_copy(out_v[i], dst, store_sem.at[i]).wait()
    for store in stores:
        store.wait()


def pack(owned, small, d_x, y_rows, moved_x, moved_y, shapes):
    gain_shape, tap_shape, head_shape = shapes
    parts, terms, leads, out_shapes = [], [], [], []
    for i, (zero, one, lead) in enumerate(owned):
        whole = zero[0].out.shape
        if lead and len(whole) == 3 and isinstance(zero[0], Finish):
            shape = (whole[0] * whole[1], whole[2])
        else:
            shape = whole[-2:]
        shape = tuple(shape)
        leads.append(lead)
        out_shapes.append(shape)
        for j in range(max(len(zero), len(one))):
            pair = []
            for side in (zero, one):
                if j < len(side):
                    parts.append(slot_free(side[j], shape))
                    pair.append(len(parts) - 1)
                else:
                    pair.append(None)
            terms.append((*pair, i))
    operands = [v.array for v in (small.out, d_x, y_rows, moved_x.out, moved_y.out)] + parts
    rows = d_x.shape
    smem = pl.BlockSpec(memory_space=pltpu.VMEM)
    out_shape = [jax.ShapeDtypeStruct((1, 2) + rows, BF), jax.ShapeDtypeStruct(gain_shape, F32)]
    out_shape += [
        jax.ShapeDtypeStruct((1,) + v if lead else v, F32) for v, lead in zip(out_shapes, leads)
    ]
    out_shape += [jax.ShapeDtypeStruct(v, F32) for v in (tap_shape, head_shape)]
    n = len(leads)
    return tuple(
        pl.pallas_call(
            functools.partial(
                pack_kernel, (len(operands), tuple(leads), tuple(terms), tap_shape[0])
            ),
            out_shape=out_shape,
            in_specs=[ANY] * len(operands),
            out_specs=[ANY, smem] + [ANY] * n + [smem] * 2,
            scratch_shapes=[pltpu.VMEM(rows, BF)] * 2
            + [pltpu.VMEM(small.out.shape, F32)]
            + [pltpu.VMEM(out_shapes[i], BF) for _, _, i in terms]
            + [pltpu.VMEM(v, F32) for v in out_shapes]
            + [DMA((3 + len(terms),)), DMA((n + 2,))],
            compiler_params=pltpu.CompilerParams(vmem_limit_bytes=VMEM_BYTES),
            name="pack",
        )(*operands)
    )


def solution(mesh):
    in_specs = (
        P("section", "dp", "tensor", None),
        P("section", None, None),
        P("section", "dp", "tensor"),
        P("section", "tensor", "dp"),
        P("section", "dp", "tensor"),
        P("section", "dp", "tensor"),
        P("section", "tensor", "dp"),
        P(("section", "dp"), "tensor"),
        P(None, "tensor"),
        P(),
    )
    out_specs = (
        P("section", "dp", "tensor", None),
        P("section", None, None),
        P("section", "dp", "tensor"),
        P("section", "tensor", "dp"),
        P("section", "dp", "tensor"),
        P("section", "dp", "tensor"),
        P("section", "tensor", "dp"),
        P(("section", "dp"), "tensor"),
        P(None, "tensor"),
        P(),
    )
    return jax.shard_map(body, mesh=mesh, in_specs=in_specs, out_specs=out_specs, check_vma=False)
```

```python
import functools

import jax
import jax.numpy as jnp
from jax import lax
from jax.experimental import pallas as pl
from jax.experimental.pallas import tpu as pltpu
from jax.sharding import PartitionSpec as P

HEADS = 16
KV_HEADS = 8

EPS = 1e-05
ROPE_BASE = 1000000.0
MASKED = -1e30

MESH = pl.DeviceIdType.MESH
ANY = pl.BlockSpec(memory_space=pl.ANY)
DMA = pltpu.SemaphoreType.DMA
VMEM_BYTES = 63 * 1024 * 1024
BF = jnp.bfloat16
F32 = jnp.float32
ROW_BLOCK = 256
STRIP = 32


def contract(left_op, right_op, left_dim, right_dim):
    return lax.dot_general(
        left_op, right_op, (((left_dim,), (right_dim,)), ((), ())), preferred_element_type=F32
    )


def norm_rows(values, gain):
    return values * lax.rsqrt(jnp.mean(values * values, axis=-1, keepdims=True) + EPS) * gain


def norm_back(values, gain, grad_in):
    row_scale = lax.rsqrt(jnp.mean(values * values, axis=-1, keepdims=True) + EPS)
    normed = values * row_scale
    gain_grad = jnp.sum(grad_in * normed, axis=0, keepdims=True)
    scaled = grad_in * gain
    value_grad = row_scale * (scaled - normed * jnp.mean(scaled * normed, axis=-1, keepdims=True))
    return (value_grad, gain_grad)


class Angles:
    def __init__(self, k, length, head_size, width):
        self.half = head_size // 2
        self.tables = [k.vmem((length, width), F32) for _ in range(2)]
        self.saves = [Save(k, v) for v in self.tables]

    def run(self):
        cos, sin = self.tables
        shape = (ROW_BLOCK, cos.shape[1])
        column = (lax.broadcasted_iota(jnp.int32, shape, 1) % self.half).astype(F32)
        frequency = ROPE_BASE ** (-(column / self.half))
        row = lax.broadcasted_iota(jnp.int32, shape, 0)

        def step(i, carry):
            rows = block_of(i, ROW_BLOCK)
            angle = (row + i * ROW_BLOCK).astype(F32) * frequency
            cos.ref[rows, :] = jnp.cos(angle)
            sin.ref[rows, :] = jnp.sin(angle)
            return carry

        lax.fori_loop(0, cos.shape[0] // ROW_BLOCK, step, 0)
        for save in self.saves:
            save.start()


def silu_parts(gate):
    sig = 1.0 / (1.0 + jnp.exp(-gate))
    return sig, gate * sig


def chunked(rows, step):
    size = next((n for n in (32, 16) if rows % n == 0), rows)
    if size == rows:
        step(pl.ds(0, rows))
    else:
        lax.fori_loop(0, rows // size, lambda i, c: step(block_of(i, size)) or c, 0)


def dp_size():
    return lax.axis_size("dp")


def spot():
    return tuple(lax.axis_index(a) for a in ("section", "dp", "tensor"))


def block_of(index, size):
    return pl.ds(pl.multiple_of(index * size, size), size)


class Val:
    def __init__(self, shape, dtype):
        self.shape, self.dtype = tuple(shape), dtype
        self.ref = self.array = None


class Kernel:
    def __init__(self, cid):
        self.cid, self.ins, self.arrays, self.outs, self.room = cid, [], [], [], []
        self.early, self.steps, self.late, self.axes = [], [], [], set()
        self.once = []

    def input(self, array):
        array = array.array if isinstance(array, Val) else array
        for val, known in zip(self.ins, self.arrays):
            if known is array:
                return val
        val = Val(array.shape, array.dtype)
        self.ins.append(val)
        self.arrays.append(array)
        return val

    def output(self, shape, dtype):
        val = Val(shape, dtype)
        self.outs.append(val)
        return val

    def vmem(self, shape, dtype):
        val = Val(shape, dtype)
        self.room.append((val, pltpu.VMEM(tuple(shape), dtype)))
        return val

    def sem(self, *shape):
        val = Val(shape, None)
        self.room.append((val, DMA(shape)))
        return val

    def do(self, *steps):
        self.steps += steps

    def body(self, *refs):
        vals = self.ins + self.outs + [val for val, _ in self.room]
        for val, ref in zip(vals, refs):
            val.ref = ref
        for item in self.once:
            item.waited = False
            item.phase = 0
        for step in self.early:
            step()
        self.greet()
        for step in self.steps + self.late:
            step()

    def greet(self):
        s, d, t = spot()
        _, sib, cross, diag = places()
        barrier = pltpu.get_barrier_semaphore()
        peers = [{"tensor": sib}, {"tensor": cross}]
        if "tensor" in self.axes:
            peers.append({"tensor": diag})
        if "section" in self.axes:
            peers.append({"section": 1 - s})
        if "dp" in self.axes:
            peers += [{"dp": (d + i) % dp_size()} for i in range(1, dp_size())]

        def signal(peer):
            pl.semaphore_signal(barrier, inc=1, device_id=peer, device_id_type=MESH)

        for peer in peers:
            signal(peer)
        expected = len(peers)
        if "line" in self.axes and "dp" not in self.axes:
            pl.when(d < 3)(lambda: signal({"dp": (d + 1) % 4}))
            pl.when(d > 0)(lambda: signal({"dp": (d + 3) % 4}))
            expected = expected + (d + 2) // 3 + (5 - d) // 3
        pl.semaphore_wait(barrier, expected)

    def build(self):
        result = pl.pallas_call(
            self.body,
            out_shape=[jax.ShapeDtypeStruct(v.shape, v.dtype) for v in self.outs],
            in_specs=[ANY] * len(self.ins),
            out_specs=[ANY] * len(self.outs),
            scratch_shapes=[room for _, room in self.room],
            compiler_params=pltpu.CompilerParams(
                collective_id=self.cid, has_side_effects=True, vmem_limit_bytes=VMEM_BYTES
            ),
            name=f"stage{self.cid}",
        )(*self.arrays)
        for val, array in zip(self.outs, result):
            val.array = array


def remote(src, dst, send_sem, recv_sem, peer):
    return pltpu.make_async_remote_copy(
        src_ref=src, dst_ref=dst, send_sem=send_sem, recv_sem=recv_sem,
        device_id=peer, device_id_type=MESH,
    )


class Load:
    def __init__(self, k, sources, shape, dtype, early=False):
        self.k, self.sources, self.waited = k, sources, False
        self.buf, self.sem = k.vmem(shape, dtype), k.sem(1)
        k.once.append(self)
        if early:
            k.early.append(self.start)

    def moves(self):
        for cond, source in self.sources(*spot()):
            yield cond, pltpu.make_async_copy(source, self.buf.ref, self.sem.ref.at[0])

    def start(self):
        for cond, move in self.moves():
            if cond is None:
                move.start()
            else:
                pl.when(cond)(move.start)

    def wait(self):
        if not self.waited:
            self.waited = True
            next(self.moves())[1].wait()


def load_all(k, array, early=True):
    val = k.input(array)
    return Load(k, lambda s, d, t: [(None, val.ref)], val.shape, val.dtype, early)


class Save:
    def __init__(self, k, buf):
        self.buf, self.out, self.sem = buf, k.output(buf.shape, buf.dtype), k.sem(1)
        self.waited = False
        k.once.append(self)
        k.late.append(self.wait)

    def move(self):
        return pltpu.make_async_copy(self.buf.ref, self.out.ref, self.sem.ref.at[0])

    def start(self):
        self.move().start()

    def wait(self):
        if not self.waited:
            self.waited = True
            self.move().wait()


class Task:
    final = None

    def __init__(self, k, out, axis, moves, count, n_local=1, out_dtype=BF):
        self.k, self.axis, self.make = k, axis, moves
        self.out = k.output(out, out_dtype)
        self.send_sem, self.recv_sem, self.local_sem = k.sem(count), k.sem(count), k.sem(n_local)
        self.waited = False
        k.axes.add(axis)
        k.once.append(self)

    def local(self, src, dst, i):
        return pltpu.make_async_copy(src, dst, self.local_sem.ref.at[i])

    def pairs(self, every):
        far, near = self.make(*spot())
        for i, (sources, dst, peer) in enumerate(far):
            for cond, src in sources if every else sources[:1]:
                yield cond, True, remote(
                    src, dst, self.send_sem.ref.at[i], self.recv_sem.ref.at[i], peer
                )
        for i, (sources, dst) in enumerate(near):
            for cond, src in sources if every else sources[:1]:
                yield cond, False, self.local(src, dst, i)

    def step(self):
        pass

    def send(self):
        for cond, far, move in self.pairs(True):
            if far and self.final is not None:
                cond = lax.axis_index("section") == 1 - self.final
            if cond is None:
                move.start()
            else:
                pl.when(cond)(move.start)

    def wait(self):
        if self.waited:
            return
        self.waited = True
        s = lax.axis_index("section")
        for _, far, move in self.pairs(False):
            if not far:
                move.wait()
            elif self.final is None:
                move.wait_recv()
                move.wait_send()
            else:
                pl.when(s == 1 - self.final)(move.wait_send)
                pl.when(s == self.final)(move.wait_recv)


class Part:
    def __init__(self, base, start, rows):
        self.base, self.start, self.rows = base, start, rows
        self.shape, self.dtype = (rows,) + tuple(base.shape[1:]), base.dtype
        self.array = None

    @property
    def ref(self):
        return self.base.ref.at[pl.ds(self.start, self.rows)]


def as_val(k, value):
    if isinstance(value, Part):
        return Part(as_val(k, value.base), value.start, value.rows)
    value = value.out if isinstance(value, Task) else value
    known = isinstance(value, Val) and (value.array is None)
    return value if known else k.input(value)


class Line(Task):
    def __init__(self, k, out, out_dtype=BF, n_local=1):
        super().__init__(k, out, "line", None, 6, n_local, out_dtype)
        self.send_sem, self.recv_sem = k.sem(2, 3), k.sem(2, 3)
        self.phase = 0

    def hop(self, j, way, src, dst):
        d = lax.axis_index("dp")
        peer = {"dp": (d + 1 if way == 0 else d + 3) % 4}
        return remote(src, dst, self.send_sem.ref.at[way, j], self.recv_sem.ref.at[way, j], peer)


class LineGather(Line):
    def __init__(self, k, sources, shape, dtype):
        super().__init__(k, (4,) + shape, dtype)
        self.sources = sources

    def ends(self, j, way):
        d = lax.axis_index("dp")
        if way == 0:
            return (d >= j) & (d < 3), d >= j + 1
        return (d <= 3 - j) & (d > 0), d <= 2 - j

    def copy(self, j, way, src=None):
        d = lax.axis_index("dp")
        slot = (d + 4 - j if way == 0 else d + j) % 4
        piece = self.out.ref.at[slot]
        return self.hop(j, way, piece if src is None else src, piece)

    def send(self):
        self.phase = 0
        for cond, src in self.sources(*spot()):
            own = self.local(src, self.out.ref.at[lax.axis_index("dp")], 0)
            moves = [(True if cond is None else cond, own)]
            for way in range(2):
                sends = self.ends(0, way)[0]
                moves.append((sends if cond is None else sends & cond, self.copy(0, way, src)))
            for when, move in moves:
                if when is True:
                    move.start()
                else:
                    pl.when(when)(move.start)

    def arrive(self, j):
        for way in range(2):
            pl.when(self.ends(j, way)[1])(self.copy(j, way).wait_recv)

    def step(self):
        self.arrive(self.phase)
        self.phase += 1
        for way in range(2):
            pl.when(self.ends(self.phase, way)[0])(self.copy(self.phase, way).start)

    def wait(self):
        if self.waited:
            return
        self.waited = True
        while self.phase < 2:
            self.step()
        self.arrive(2)
        for j in range(3):
            for way in range(2):
                pl.when(self.ends(j, way)[0])(self.copy(j, way).wait_send)
        d = lax.axis_index("dp")
        self.local(self.sources(*spot())[0][1], self.out.ref.at[d], 0).wait()


def z_gather_from(k, sources, shape, dtype):
    count = dp_size()
    if count == 4:
        return LineGather(k, sources, shape, dtype)

    def moves(s, d, t):
        dst, found = task.out.ref.at[d], sources(s, d, t)
        return [(found, dst, {"dp": (d + i) % count}) for i in range(1, count)], [(found, dst)]

    task = Task(k, (count,) + shape, "dp", moves, count - 1, out_dtype=dtype)
    return task


def z_gather(k, value):
    val = as_val(k, value)
    return z_gather_from(k, lambda s, d, t: [(None, val.ref)], val.shape, val.dtype)


def z_gather_half(k, shard, moved, block):
    shard, moved = as_val(k, shard), as_val(k, moved)
    rows = shard.shape[0] // 2

    def sources(s, d, t):
        own = shard.ref.at[pl.ds(block * rows, rows)]
        return [(s == block, own), (s == 1 - block, moved.ref)]

    return z_gather_from(k, sources, moved.shape, shard.dtype)


def one_way(task, sender):
    task.final = None if sender is None else 1 - sender
    return task


def z_gather_whole(k, shard, moved, block, half=None):
    shard, moved = as_val(k, shard), as_val(k, moved)
    rows = shard.shape[0] if half is None else shard.shape[0] // 2
    part = pl.ds(0 if half is None else half * rows, rows)

    def sources(s, d, t):
        return [(s == block, shard.ref.at[part]), (s == 1 - block, moved.ref.at[part])]

    return z_gather_from(k, sources, (rows,) + shard.shape[1:], shard.dtype)


def x_move(k, value, sender=None):
    val = as_val(k, value)

    def moves(s, d, t):
        return [([(None, val.ref)], task.out.ref, {"section": 1 - s})], []

    task = Task(k, val.shape, "section", moves, 1, out_dtype=val.dtype)
    return one_way(task, sender)


def x_half(k, value, sender=None):
    val = as_val(k, value)
    rows = val.shape[0] // 2

    def moves(s, d, t):
        src = val.ref.at[block_of(1 - s, rows)]
        return [([(None, src)], task.out.ref, {"section": 1 - s})], []

    task = Task(k, (rows,) + val.shape[1:], "section", moves, 1, out_dtype=val.dtype)
    return one_way(task, sender)


def x_slots(k, value, kind):
    val, count = as_val(k, value), dp_size()
    rows = val.shape[0] // (2 * count)

    def moves(s, d, t):
        far = []
        for i in range(count):
            slot = 2 * i + 1 - s if kind == "rows" else (1 - s) * count + i
            src = val.ref.at[block_of(slot, rows)]
            far.append(([(None, src)], task.out.ref.at[i], {"section": 1 - s}))
        return far, []

    task = Task(k, (count, rows) + val.shape[1:], "section", moves, count)
    return task


class Terms:
    def __init__(self, k, kind, grads, received, local):
        self.grads, self.local = as_val(k, grads), local
        self.kind, self.n = kind, dp_size()
        self.whole = received is None
        if self.whole:
            rows, cols = self.grads.shape
            self.rows = rows if kind == "cols" else rows // self.n
            self.cols = cols // self.n if kind == "cols" else cols
            self.shape = (self.n, self.rows, self.cols)
            self.aside = kind == "cols" and self.cols % 128 != 0
            self.total = k.vmem(self.shape, BF)
            self.kept = k.vmem(self.grads.shape, BF) if self.aside else self.total
            return
        self.received = as_val(k, received)
        if kind == "cols":
            self.rows, self.cols = self.grads.shape[0] // 2, self.grads.shape[1] // self.n
            held = (self.rows, self.grads.shape[1])
        else:
            self.rows, self.cols = self.grads.shape[0] // (2 * self.n), self.grads.shape[1]
            held = (self.n, self.rows, self.cols)
        self.kept, self.got = k.vmem(held, BF), k.vmem(held, BF)
        self.shape = (self.n, self.rows, self.cols)
        self.total = k.vmem(self.shape, BF) if kind == "cols" else self.kept

    def loads(self):
        s, grads, kept = lax.axis_index("section"), self.grads.ref, self.kept.ref
        if self.whole and self.aside:
            return [self.local(grads, kept, 2)]
        if self.whole:
            parts = [
                grads.at[:, pl.ds(i * self.cols, self.cols)]
                if self.kind == "cols"
                else grads.at[block_of(i, self.rows)]
                for i in range(self.n)
            ]
            return [self.local(part, kept.at[i], 2 + i) for i, part in enumerate(parts)]
        if self.kind == "cols":
            moves = [self.local(grads.at[block_of(s, self.rows)], kept, 2)]
        else:
            moves = []
            for i in range(self.n):
                slot = 2 * i + s if self.kind == "rows" else s * self.n + i
                moves.append(self.local(grads.at[block_of(slot, self.rows)], kept.at[i], 2 + i))
        return moves + [self.local(self.received.ref, self.got.ref, 1)]

    def load(self):
        for move in self.loads():
            move.start()

    def add(self):
        for move in self.loads():
            move.wait()
        if self.whole and self.aside:
            for i in range(self.n):
                self.total.ref[i] = self.kept.ref[:, i * self.cols : (i + 1) * self.cols]
        if self.whole:
            return
        kept, got, total = self.kept.ref, self.got.ref, self.total.ref
        if self.kind != "cols":

            def piece(i, carry):
                chunked(self.rows, lambda at: total.__setitem__(
                    (i, at), (kept[i, at, :].astype(F32) + got[i, at, :].astype(F32)).astype(BF)
                ))
                return carry

            lax.fori_loop(0, self.n, piece, 0)
            return

        def add_rows(at):
            for i in range(self.n):
                part = slice(i * self.cols, (i + 1) * self.cols)
                value = kept[at, part].astype(F32) + got[at, part].astype(F32)
                total[i, at, :] = value.astype(BF)

        chunked(self.rows, add_rows)


class DirectScatter(Task):
    def __init__(self, k, kind, grads, received):
        self.terms = Terms(k, kind, grads, received, lambda *a: self.local(*a))
        count = dp_size()

        def moves(s, d, t):
            total = self.terms.total.ref
            far = []
            for i in range(1, count):
                other = (d + i) % count
                far.append(([(None, total.at[other])], self.out.ref.at[d], {"dp": other}))
            return far, [([(None, total.at[d])], self.out.ref.at[d])]

        super().__init__(k, self.terms.shape, "dp", moves, count - 1, 2 + count)
        self.load = self.terms.load

    def send(self):
        self.terms.add()
        super().send()

    def add(self):
        self.load()
        self.send()


class LineScatter(Line):
    def __init__(self, k, kind, grads, received):
        self.terms = Terms(k, kind, grads, received, lambda *a: self.local(*a))
        super().__init__(k, self.terms.shape[1:], BF, 6)
        self.got = k.vmem((2, 3) + self.terms.shape[1:], BF)
        self.load = self.terms.load

    def ends(self, j, way):
        d = lax.axis_index("dp")
        if way == 0:
            return (d <= j) & (d < 3), (d >= 1) & (d <= j + 1)
        return (d >= 3 - j) & (d > 0), (d <= 2) & (d >= 2 - j)

    def copy(self, j, way):
        d = lax.axis_index("dp")
        to = (d + 3 - j if way == 0 else d + 1 + j) % 4
        return self.hop(j, way, self.terms.total.ref.at[to], self.got.ref.at[way, j])

    def send(self):
        self.phase = 0
        self.terms.add()
        for way in range(2):
            pl.when(self.ends(0, way)[0])(self.copy(0, way).start)

    def take(self, j, way):
        d = lax.axis_index("dp")
        to = (d + 2 - j if way == 0 else d + 2 + j) % 4
        self.copy(j, way).wait_recv()
        total, got = self.terms.total.ref, self.got.ref

        def add_rows(at):
            value = total[to, at, :].astype(F32) + got[way, j, at, :].astype(F32)
            total[to, at, :] = value.astype(BF)

        chunked(self.terms.rows, add_rows)

    def arrive(self, j):
        for way in range(2):
            pl.when(self.ends(j, way)[1])(functools.partial(self.take, j, way))

    def step(self):
        self.arrive(self.phase)
        self.phase += 1
        for way in range(2):
            pl.when(self.ends(self.phase, way)[0])(self.copy(self.phase, way).start)

    def wait(self):
        if self.waited:
            return
        self.waited = True
        while self.phase < 2:
            self.step()
        self.arrive(2)
        done = self.local(self.terms.total.ref.at[lax.axis_index("dp")], self.out.ref, 0)
        done.start()
        for j in range(3):
            for way in range(2):
                pl.when(self.ends(j, way)[0])(self.copy(j, way).wait_send)
        done.wait()

    def add(self):
        self.load()
        self.send()


def sum_scatter(k, kind, grads, received=None):
    return (LineScatter if dp_size() == 4 else DirectScatter)(k, kind, grads, received)


class Finish(Task):
    def __init__(self, k, pieces, block):
        self.pieces, self.final = as_val(k, pieces), block
        *slots, rows, cols = self.pieces.shape
        self.slots = slots[0] if slots else 0
        if slots:
            self.held, self.total = k.vmem(self.pieces.shape, BF), k.vmem((rows, cols), BF)
        else:
            self.total = self.pieces

        def moves(s, d, t):
            source, dst = [(None, self.total.ref)], self.out.ref.at[s]
            return [(source, dst, {"section": 1 - s})], [(source, dst)]

        super().__init__(k, (2, rows, cols), "section", moves, 1, 2)

    def load(self):
        if self.slots:
            self.local(self.pieces.ref, self.held.ref, 1).start()

    def send(self):
        if self.slots:
            self.local(self.pieces.ref, self.held.ref, 1).wait()
            acc = self.held.ref[0].astype(F32)
            for i in range(1, self.slots):
                acc = acc + self.held.ref[i].astype(F32)
            self.total.ref[...] = acc.astype(BF)
        super().send()

    def add(self):
        self.load()
        self.send()


class SumShare(Task):
    def __init__(self, k, terms, axis, slotted=False):
        self.terms = [as_val(k, v) for v in terms]
        shape = self.terms[0].shape[1:] if slotted else self.terms[0].shape
        count = dp_size() if axis == "dp" else 4
        self.slotted = slotted
        self.bufs = [k.vmem(v.shape, F32) for v in self.terms]
        self.total = k.vmem(shape, F32)

        def moves(s, d, t):
            source, me = [(None, self.total.ref)], d if axis == "dp" else t
            dst = self.out.ref.at[me]
            far = [(source, dst, {axis: (me + i) % count}) for i in range(1, count)]
            return far, [(source, dst)]

        super().__init__(k, (count,) + shape, axis, moves, count - 1, 3, out_dtype=F32)

    def add(self):
        loads = [self.local(v.ref, b.ref, 1 + i) for i, (v, b) in enumerate(zip(self.terms, self.bufs))]
        for load in loads:
            load.start()
        for load in loads:
            load.wait()
        if self.slotted:
            parts = [self.bufs[0].ref[i] for i in range(self.terms[0].shape[0])]
        else:
            parts = [buf.ref[...] for buf in self.bufs]
        acc = parts[0]
        for part in parts[1:]:
            acc = acc + part
        self.total.ref[...] = acc
        self.send()


class Weight:
    def __init__(self, k, kind, *segments, early=False):
        self.kind, self.waited = kind, False
        self.segments, start = [], 0
        for near, far in segments:
            near, far = as_val(k, near), None if far is None else as_val(k, far)
            self.segments.append((near, far, start))
            start += near.shape[1] * (1 if far is None else 2)
        self.count, _, self.cols = self.segments[0][0].shape
        self.rows = start
        if kind == "cols":
            shape = (self.rows, self.count * self.cols)
        else:
            shape = (self.count * self.rows, self.cols)
        self.aside = kind == "cols" and self.cols % 128 != 0
        self.buf = k.vmem(shape, BF)
        sides = [v for near, far, _ in self.segments for v in (near, far) if v is not None]
        self.sem = k.sem(len(sides), self.count)
        if self.aside:
            self.held = [k.vmem(v.shape, BF) for v in sides]
        k.once.append(self)
        if early:
            k.early.append(self.start)

    def sides(self):
        s = lax.axis_index("section")
        for near, far, start in self.segments:
            rows = near.shape[1]
            if far is None:
                yield near, start, None
            else:
                yield near, start + s * rows, s
                yield far, start + (1 - s) * rows, 1 - s

    def moves(self):
        dst = self.buf.ref
        for j, (val, start, sec) in enumerate(self.sides()):
            rows = val.shape[1]
            for i in range(self.count):
                if self.aside:
                    to = self.held[j].ref.at[i]
                elif self.kind == "cols":
                    at = pl.ds(pl.multiple_of(start, 16), rows)
                    to = dst.at[at, pl.ds(i * self.cols, self.cols)]
                else:
                    top = (sec * self.count + i) * rows if self.kind == "conv" else i * self.rows + start
                    to = dst.at[pl.ds(pl.multiple_of(top, 16), rows)]
                yield pltpu.make_async_copy(val.ref.at[i], to, self.sem.ref.at[j, i])

    def start(self):
        for move in self.moves():
            move.start()

    def wait(self):
        if self.waited:
            return
        self.waited = True
        for move in self.moves():
            move.wait()
        if self.aside:
            for j, (val, start, _) in enumerate(self.sides()):
                whole = jnp.concatenate([self.held[j].ref[i] for i in range(self.count)], axis=1)
                self.buf.ref[pl.ds(pl.multiple_of(start, 16), val.shape[1]), :] = whole


class Product:
    def __init__(self, k, left, right):
        self.left, self.right = left, right
        rows = left.shape[1]
        self.chunk = 384 if rows % 384 == 0 else 256
        self.count = rows // self.chunk
        self.buf = k.vmem((rows, right.shape[1]), BF)
        self.out, self.sem = k.output(self.buf.shape, BF), k.sem(self.count)

    def copy(self, i):
        part = block_of(i, self.chunk)
        return pltpu.make_async_copy(self.buf.ref.at[part], self.out.ref.at[part], self.sem.ref.at[i])

    def run(self):
        def step(i, carry):
            part = block_of(i, self.chunk)
            value = contract(self.left.ref[:, part], self.right.ref[...], 0, 0)
            self.buf.ref[part, :] = value.astype(BF)
            self.copy(i).start()
            return carry

        lax.fori_loop(0, self.count, step, 0)

    def wait(self):
        for i in range(self.count):
            self.copy(i).wait()


def places():
    me = lax.axis_index("tensor")
    sib = me + 1 - 2 * (me % 2)
    cross = (me + 2) % 4
    diag = (sib + 2) % 4
    return me, sib, cross, diag


class Gather:
    def __init__(self, k, x, gain, weights, extras=(), trans=False, epilogue="plain", save=()):
        rows, width = x.shape
        length = 4 * rows
        self.k, self.x, self.gain, self.weights, self.extras = k, x, gain, weights, extras
        self.trans, self.epilogue, self.rows, self.half = trans, epilogue, rows, rows // 2
        cols = [w.buf.shape[0 if trans else 1] for w in weights]
        kinds = {
            "plain": [(c, F32) for c in cols],
            "ffn": [(cols[0], BF)] * 3,
            "ffn_back": [(cols[0], BF)] * 2,
        }[epilogue]
        self.full = k.vmem((length, width), BF)
        self.values = [k.vmem((length, c), kind) for c, kind in kinds]
        kept = [self.full] + self.values
        self.saved = [(v, k.output(v.shape, v.dtype), k.sem(4, 2)) for v in kept if kept.index(v) in save]
        self.sems = [k.sem(2) for _ in range(6)]
        k.late.append(self.end)

    def span(self, owner, sub):
        return pl.ds(pl.multiple_of(owner * self.rows + sub * self.half, self.half), self.half)

    def move(self, kind, i):
        me, sib, cross, _ = places()
        full = self.full.ref
        owner, peer, at = {"cross": (me, cross, 0), "sib": (me, sib, 2), "relay": (cross, sib, 4)}[kind]
        part = full.at[self.span(owner, i)]
        return remote(
            part, part, self.sems[at].ref.at[i], self.sems[at + 1].ref.at[i], {"tensor": peer}
        )

    def begin(self):
        me = places()[0]
        for i in range(2):

            def put(j, carry):
                at = i * self.half + j * STRIP
                part = self.x.ref[pl.ds(pl.multiple_of(at, STRIP), STRIP), :].astype(F32)
                if self.gain is not None:
                    val, row = self.gain
                    part = norm_rows(part, val.ref[row : row + 1, :])
                to = pl.ds(pl.multiple_of(me * self.rows + at, STRIP), STRIP)
                self.full.ref[to, :] = part.astype(BF)
                return carry

            lax.fori_loop(0, self.half // STRIP, put, 0)
            self.move("cross", i).start()
            self.move("sib", i).start()

    def loop(self):
        me, sib, cross, diag = places()
        rows, half = self.rows, self.half
        for w in self.weights:
            w.wait()

        def step(p, carry):
            far, sub = p // 2, p % 2
            near = (1 - sub) * me + sub * sib
            first = (1 - far) * near * rows + far * (cross * rows + sub * half)
            second = (1 - far) * (near * rows + half) + far * (diag * rows + sub * half)
            pair = [pl.ds(pl.multiple_of(v, half), half) for v in (first, second)]

            @pl.when(p == 1)
            def _():
                self.move("sib", 0).wait_recv()
                self.move("sib", 1).wait_recv()

            for i in range(2):

                @pl.when(p == 2 + i)
                def _():
                    self.move("cross", i).wait_recv()
                    self.move("relay", i).start()
                    self.move("relay", i).wait_recv()

            def both(val):
                return jnp.concatenate([val.ref[pair[0], :], val.ref[pair[1], :]], axis=0)

            a = both(self.full)
            prods = [contract(a, w.buf.ref[...], 1, 1 if self.trans else 0) for w in self.weights]
            if self.epilogue == "plain":
                values = prods
            elif self.epilogue == "ffn":
                sig, silu = silu_parts(prods[0])
                values = [prods[0], prods[1], silu * prods[1]]
            else:
                gate, up = (both(v).astype(F32) for v in self.extras)
                sig, silu = silu_parts(gate)
                values = [prods[0] * up * sig * (1.0 + gate * (1.0 - sig)), prods[0] * silu]
            for val, value in zip(self.values, values):
                value = value.astype(val.dtype)
                for j in range(2):
                    val.ref[pair[j], :] = value[j * half : (j + 1) * half]
            for val, out, sem in self.saved:
                for j in range(2):
                    pltpu.make_async_copy(
                        val.ref.at[pair[j]], out.ref.at[pair[j]], sem.ref.at[p, j]
                    ).start()
            return carry

        lax.fori_loop(0, 4, step, 0)

    def end(self):
        for i in range(2):
            for kind in ("cross", "sib", "relay"):
                self.move(kind, i).wait_send()
        part = pl.ds(0, self.half)
        for val, out, sem in self.saved:
            for p in range(4):
                for j in range(2):
                    pltpu.make_async_copy(val.ref.at[part], out.ref.at[part], sem.ref.at[p, j]).wait()


class Scatter:
    def __init__(self, k, operands, weights, resid, back=None, trans=False, low=False):
        rows, width = resid.shape
        half = rows // 2
        self.operands, self.weights, self.resid, self.back = operands, weights, resid, back
        self.trans, self.low, self.rows, self.half = trans, low, rows, half
        self.keep, self.own = k.vmem((2, half, width), F32), k.vmem((rows, width), F32)
        self.to_s, self.from_s, self.to_c, self.from_c = (
            k.vmem((2, half, width), BF) for _ in range(4)
        )
        self.to_o, self.from_o = k.vmem((rows, width), BF), k.vmem((rows, width), BF)
        self.out = k.vmem((rows, width), BF if low else F32)
        self.gain_grad = k.vmem((1, width), F32) if back else None
        self.sems = [k.sem(2) for _ in range(4)] + [k.sem(1) for _ in range(2)]
        k.late.append(self.end)

    def move(self, kind, i=0):
        _, sib, cross, _ = places()
        at, src, dst, peer = {
            "diag": (0, self.to_s, self.from_s, sib),
            "cross": (2, self.to_c, self.from_c, cross),
            "near": (4, self.to_o, self.from_o, sib),
        }[kind]
        src, dst = (src.ref, dst.ref) if kind == "near" else (src.ref.at[i], dst.ref.at[i])
        return remote(
            src, dst, self.sems[at].ref.at[i], self.sems[at + 1].ref.at[i], {"tensor": peer}
        )

    def pass_on(self, i):
        self.move("diag", i).wait_recv()

        def add_rows(at):
            total = self.keep.ref[i, at, :] + self.from_s.ref[i, at, :].astype(F32)
            self.to_c.ref[i, at, :] = total.astype(BF)

        chunked(self.half, add_rows)
        self.move("cross", i).start()

    def loop(self):
        me, sib, cross, diag = places()
        rows, half = self.rows, self.half
        for w in self.weights:
            w.wait()

        def step(p, carry):
            near, sub = p // 2, p % 2
            base = near * ((1 - sub) * sib + sub * me) * rows
            first = base + (1 - near) * (cross * rows + sub * half)
            second = base + near * half + (1 - near) * (diag * rows + sub * half)
            pair = [pl.ds(pl.multiple_of(v, half), half) for v in (first, second)]
            total = None
            for y, w in zip(self.operands, self.weights):
                a = jnp.concatenate([y.ref[pair[0], :], y.ref[pair[1], :]], axis=0)
                prod = contract(a, w.buf.ref[...], 1, 1 if self.trans else 0)
                total = prod if total is None else total + prod

            self.own.ref[...] = total

            @pl.when(p < 2)
            def _():
                def put(at):
                    self.keep.ref[p, at, :] = self.own.ref[at, :]
                    lower = pl.ds(pl.multiple_of(at.start + half, 16), at.size)
                    self.to_s.ref[p, at, :] = self.own.ref[lower, :].astype(BF)

                chunked(half, put)
                self.move("diag", p).start()

            @pl.when(p == 2)
            def _():
                def put(at):
                    self.to_o.ref[at, :] = self.own.ref[at, :].astype(BF)

                chunked(rows, put)
                self.move("near").start()

            @pl.when((p == 1) | (p == 2))
            def _():
                self.pass_on(p - 1)

            return carry

        lax.fori_loop(0, 4, step, 0)

    def finish(self):
        self.move("near").wait_recv()
        if self.back:
            self.gain_grad.ref[...] = jnp.zeros_like(self.gain_grad.ref)
        for i in range(2):
            self.move("cross", i).wait_recv()

            def add_rows(j, carry):
                inner = block_of(j, STRIP)
                part = pl.ds(pl.multiple_of(i * self.half + j * STRIP, STRIP), STRIP)
                total = self.own.ref[part, :] + self.from_o.ref[part, :].astype(F32)
                total = total + self.from_c.ref[i, inner, :].astype(F32)
                resid = self.resid.ref[part, :].astype(F32)
                if self.back:
                    value, (gain, row) = self.back
                    total, gain_grad = norm_back(
                        value.ref[part, :].astype(F32), gain.ref[row : row + 1, :], total
                    )
                    self.gain_grad.ref[...] += gain_grad
                self.out.ref[part, :] = (resid + total).astype(self.out.dtype)
                return carry

            lax.fori_loop(0, self.half // STRIP, add_rows, 0)

    def end(self):
        self.move("near").wait_send()
        for i in range(2):
            self.move("diag", i).wait_send()
            self.move("cross", i).wait_send()


def delayed(values, by):
    if by == 0:
        return values
    row = lax.broadcasted_iota(jnp.int32, values.shape, 0)
    return jnp.where(row < by, 0.0, pltpu.roll(values, by, 0))


def advanced(values, by):
    if by == 0:
        return values
    length = values.shape[0]
    row = lax.broadcasted_iota(jnp.int32, values.shape, 0)
    return jnp.where(row >= length - by, 0.0, pltpu.roll(values, length - by, 0))


CONV_COLS = 128


class Conv:
    def __init__(self, k, projected, value, kernel):
        self.projected, self.value, self.kernel = projected, value, kernel
        self.y = k.vmem(value.shape, BF)

    def parts(self, j):
        channels = self.value.shape[1]
        at = block_of(j, CONV_COLS)
        b_gate = self.projected.ref[:, at]
        c_gate = self.projected.ref[:, block_of(j + channels // CONV_COLS, CONV_COLS)]
        x_value, taps = self.value.ref[:, at], self.kernel.ref[:, at]
        product = b_gate * x_value
        count = taps.shape[0]
        causal = jnp.zeros_like(product)
        for i in range(count):
            causal = causal + taps[i : i + 1] * delayed(product, count - 1 - i)
        return at, b_gate, c_gate, x_value, taps, product, causal

    def run(self):
        def step(j, carry):
            at, _, c_gate, _, _, _, causal = self.parts(j)
            self.y.ref[:, at] = (c_gate * causal).astype(BF)
            return carry

        lax.fori_loop(0, self.value.shape[1] // CONV_COLS, step, 0)


class ConvBack(Conv):
    def __init__(self, k, projected, value, kernel, d_y):
        self.projected, self.value, self.kernel, self.d_y = projected, value, kernel, d_y
        self.d_proj = k.vmem(projected.shape, BF)
        self.d_value = k.vmem(value.shape, BF)
        self.d_kernel = k.vmem(kernel.shape, F32)

    def run(self):
        channels = self.value.shape[1]

        def step(j, carry):
            at, b_gate, c_gate, x_value, taps, product, causal = self.parts(j)
            d_y = self.d_y.ref[:, at]
            d_causal = d_y * c_gate
            count = taps.shape[0]
            d_product = jnp.zeros_like(product)
            for i in range(count):
                by = count - 1 - i
                row = jnp.sum(d_causal * delayed(product, by), axis=0, keepdims=True)
                self.d_kernel.ref[i : i + 1, at] = row
                d_product = d_product + taps[i : i + 1] * advanced(d_causal, by)
            self.d_proj.ref[:, at] = (d_product * x_value).astype(BF)
            upper = block_of(j + channels // CONV_COLS, CONV_COLS)
            self.d_proj.ref[:, upper] = (d_y * causal).astype(BF)
            self.d_value.ref[:, at] = (d_product * b_gate).astype(BF)
            return carry

        lax.fori_loop(0, channels // CONV_COLS, step, 0)


def head_mean(values, head_size):
    width = values.shape[1]
    row = lax.broadcasted_iota(jnp.int32, (width, width), 0) // head_size
    col = lax.broadcasted_iota(jnp.int32, (width, width), 1) // head_size
    group = jnp.where(row == col, 1.0 / head_size, 0.0).astype(F32)
    return lax.dot_general(
        values, group, (((1,), (0,)), ((), ())),
        precision=lax.Precision.HIGHEST, preferred_element_type=F32,
    )


def turn(values, head_size, back):
    width, half = values.shape[1], head_size // 2
    lane = lax.broadcasted_iota(jnp.int32, values.shape, 1) % head_size
    upper = pltpu.roll(values, width - half, 1)
    lower = pltpu.roll(values, half, 1)
    return jnp.where(lane < half, upper, -lower) if back else jnp.where(lane < half, -upper, lower)


def head_norm(values, gain, head_size):
    return values * lax.rsqrt(head_mean(values * values, head_size) + EPS) * gain


def head_norm_back(values, gain, grad_in, head_size):
    row_scale = lax.rsqrt(head_mean(values * values, head_size) + EPS)
    normed = values * row_scale
    gain_grad = jnp.sum(grad_in * normed, axis=0, keepdims=True)
    scaled = grad_in * gain
    return row_scale * (scaled - normed * head_mean(scaled * normed, head_size)), gain_grad


def block_weights(q_rows, keys):
    scores = [contract(q_rows, k_rows, 1, 1) for k_rows in keys]
    query = lax.broadcasted_iota(jnp.int32, scores[-1].shape, 0)
    key = lax.broadcasted_iota(jnp.int32, scores[-1].shape, 1)
    scores[-1] = jnp.where(key <= query, scores[-1], MASKED)
    top = functools.reduce(
        jnp.maximum, [jnp.max(part, axis=1, keepdims=True) for part in scores]
    )
    exps = [jnp.exp(part - top) for part in scores]
    scale = 1.0 / sum(jnp.sum(part, axis=1, keepdims=True) for part in exps)
    return [part * scale for part in exps]


def key_blocks(i):
    blocks = [pl.ds(0, i * ROW_BLOCK)] if i else []
    return blocks + [pl.ds(i * ROW_BLOCK, ROW_BLOCK)]


class Heads:
    def __init__(self, projected, tables, size):
        assert size in (16, 64, 256), size
        self.projected, self.size = projected, size
        self.gain, self.cos, self.sin = (v.buf for v in tables)
        self.loads = tables
        self.length, width = projected.shape
        self.q_cols, self.k_cols = width // 2, width // 4
        self.heads, self.kv_heads = self.q_cols // size, self.k_cols // size
        self.share = self.heads // self.kv_heads

    def per_head(self, k, count, kind):
        return k.vmem((count, self.length, self.size), kind)

    def split(self, val, rows, values):
        for h in range(val.shape[0]):
            val.ref[h, rows, :] = values[:, h * self.size : (h + 1) * self.size]

    def join(self, val, rows):
        return jnp.concatenate([val.ref[h, rows, :] for h in range(val.shape[0])], axis=1)

    def gains(self):
        gain = self.gain.ref[...]
        return (
            jnp.concatenate([gain[0:1]] * self.heads, axis=1),
            jnp.concatenate([gain[1:2]] * self.kv_heads, axis=1),
        )

    def angles(self, rows):
        c, n = self.cos.ref[rows, :], self.sin.ref[rows, :]
        repeat = self.q_cols // c.shape[1]
        return jnp.concatenate([c] * repeat, axis=1), jnp.concatenate([n] * repeat, axis=1)

    def blocks(self, step):
        lax.fori_loop(0, self.length // ROW_BLOCK, lambda p, c: step(block_of(p, ROW_BLOCK)) or c, 0)


class Attend(Heads):
    def __init__(self, k, projected, tables, size):
        super().__init__(projected, tables, size)
        self.q_rot = k.vmem((self.length, self.q_cols), BF)
        self.k_rot = k.vmem((self.length, self.k_cols), BF)
        self.y = k.vmem((self.length, self.q_cols), BF)
        self.q_h, self.y_h = (self.per_head(k, self.heads, BF) for _ in range(2))
        self.k_h, self.v_h = (self.per_head(k, self.kv_heads, BF) for _ in range(2))

    def run(self, *between):
        for load in self.loads:
            load.wait()
        size, q_cols, k_cols, proj = self.size, self.q_cols, self.k_cols, self.projected.ref

        def prepare(rows):
            c, n = self.angles(rows)
            q_gain, k_gain = self.gains()
            q = head_norm(proj[rows, :q_cols], q_gain, size)
            q = (q * c + turn(q, size, False) * n).astype(BF)
            k = head_norm(proj[rows, q_cols : q_cols + k_cols], k_gain, size)
            k = (k * c[:, :k_cols] + turn(k, size, False) * n[:, :k_cols]).astype(BF)
            self.q_rot.ref[rows, :] = q
            self.k_rot.ref[rows, :] = k
            self.split(self.q_h, rows, (q.astype(F32) * size**-0.5).astype(BF))
            self.split(self.k_h, rows, k)
            self.split(self.v_h, rows, proj[rows, q_cols + k_cols :].astype(BF))

        self.blocks(prepare)

        def head(h, carry):
            g = h // self.share

            @pl.when(h == self.heads // 2)
            def _():
                for step in between:
                    step()

            for i in range(self.length // ROW_BLOCK):
                rows, seen = pl.ds(i * ROW_BLOCK, ROW_BLOCK), key_blocks(i)
                weights = block_weights(
                    self.q_h.ref[h, rows, :], [self.k_h.ref[g, at, :] for at in seen]
                )
                value = sum(
                    contract(part.astype(BF), self.v_h.ref[g, at, :], 1, 0)
                    for part, at in zip(weights, seen)
                )
                self.y_h.ref[h, rows, :] = value.astype(BF)
            return carry

        lax.fori_loop(0, self.heads, head, 0)

        def place(rows):
            self.y.ref[rows, :] = self.join(self.y_h, rows)

        self.blocks(place)


class AttendBack(Heads):
    def __init__(self, k, projected, tables, size, q_rot, k_rot, d_y):
        super().__init__(projected, tables, size)
        self.q_rot, self.k_rot, self.d_y = q_rot, k_rot, d_y
        self.q_h, self.dy_h = (self.per_head(k, self.heads, BF) for _ in range(2))
        self.k_h, self.v_h = (self.per_head(k, self.kv_heads, BF) for _ in range(2))
        self.dq_h = self.per_head(k, self.heads, F32)
        self.dk_h, self.dv_h = (self.per_head(k, self.kv_heads, F32) for _ in range(2))
        self.d_proj = k.vmem(projected.shape, BF)
        self.q_gain, self.k_gain = k.vmem((1, self.q_cols), F32), k.vmem((1, self.k_cols), F32)

    def run(self, *between):
        for load in self.loads:
            load.wait()
        size, q_cols, k_cols, proj = self.size, self.q_cols, self.k_cols, self.projected.ref
        scale = size**-0.5
        dq_h, dk_h, dv_h = self.dq_h.ref, self.dk_h.ref, self.dv_h.ref

        def prepare(rows):
            self.split(self.q_h, rows, (self.q_rot.ref[rows, :].astype(F32) * scale).astype(BF))
            self.split(self.dy_h, rows, self.d_y.ref[rows, :].astype(BF))
            self.split(self.k_h, rows, self.k_rot.ref[rows, :])
            self.split(self.v_h, rows, proj[rows, q_cols + k_cols :].astype(BF))

        self.blocks(prepare)

        def clear(rows):
            for val in (dk_h, dv_h):
                val[:, rows, :] = jnp.zeros((self.kv_heads, ROW_BLOCK, size), F32)

        self.blocks(clear)

        def head(h, carry):
            g = h // self.share

            @pl.when(h == self.heads // 2)
            def _():
                for step in between:
                    step()

            for i in range(self.length // ROW_BLOCK):
                rows, seen = pl.ds(i * ROW_BLOCK, ROW_BLOCK), key_blocks(i)
                q, low = self.q_h.ref[h, rows, :], self.dy_h.ref[h, rows, :]
                keys = [self.k_h.ref[g, at, :] for at in seen]
                probs = block_weights(q, keys)
                d_weights = [contract(low, self.v_h.ref[g, at, :], 1, 1) for at in seen]
                inner = sum(
                    jnp.sum(a * b, axis=1, keepdims=True) for a, b in zip(probs, d_weights)
                )
                d_q = 0.0
                for at, k, prob, d_weight in zip(seen, keys, probs, d_weights):
                    dv_h[g, at, :] += contract(prob.astype(BF), low, 0, 0)
                    d_scores = (prob * (d_weight - inner)).astype(BF)
                    d_q = d_q + contract(d_scores, k, 1, 0)
                    dk_h[g, at, :] += contract(d_scores, q, 0, 0)
                dq_h[h, rows, :] = d_q * scale
            return carry

        lax.fori_loop(0, self.heads, head, 0)
        self.q_gain.ref[...] = jnp.zeros_like(self.q_gain.ref)
        self.k_gain.ref[...] = jnp.zeros_like(self.k_gain.ref)

        def finish(rows):
            c, n = self.angles(rows)
            dq, dk, dv = (self.join(v, rows) for v in (self.dq_h, self.dk_h, self.dv_h))
            dq = dq * c + turn(dq * n, size, True)
            dk = dk * c[:, :k_cols] + turn(dk * n[:, :k_cols], size, True)
            q_gain, k_gain = self.gains()
            dq, q_sum = head_norm_back(proj[rows, :q_cols], q_gain, dq, size)
            dk, k_sum = head_norm_back(proj[rows, q_cols : q_cols + k_cols], k_gain, dk, size)
            self.q_gain.ref[...] += q_sum
            self.k_gain.ref[...] += k_sum
            self.d_proj.ref[rows, :q_cols] = dq.astype(BF)
            self.d_proj.ref[rows, q_cols : q_cols + k_cols] = dk.astype(BF)
            self.d_proj.ref[rows, q_cols + k_cols :] = dv.astype(BF)

        self.blocks(finish)


def body(boundary, norm_gain, mix_in, mix_out, w_gate, w_up, w_down, conv_x, conv_kernel, qk_gain):
    first = lax.axis_index("section") == 0
    tensor_index = lax.axis_index("tensor")
    model_width = boundary.shape[3]
    channels = mix_out.shape[1]
    row_shape = boundary.shape[2:]
    length, size = 4 * row_shape[0], qk_gain.shape[1]

    seqs, own_gain = boundary[0], norm_gain[0]
    sh_in, sh_out, sh_gate, sh_up, sh_down = (v[0] for v in (mix_in, mix_out, w_gate, w_up, w_down))

    def gains_of(k, block, other, early=True):
        own, moved = k.input(own_gain), as_val(k, other)
        sources = lambda s, d, t: [(s == block, own.ref), (s == 1 - block, moved.ref)]
        return Load(k, sources, own.shape, F32, early)

    def start_rows(k, slot, other, early=True):
        own, moved = k.input(seqs), as_val(k, other)
        sources = lambda s, d, t: [(s == slot, own.ref.at[slot]), (s == 1 - slot, moved.ref)]
        return Load(k, sources, row_shape, BF, early)

    def wait(*items):
        return [item.wait for item in items]

    k = Kernel(0)
    t_seq = None
    seq_val = k.input(seqs)

    def seq_moves(s, d, t):
        return [([(None, seq_val.ref.at[1 - s])], t_seq.out.ref, {"section": 1 - s})], []

    t_in, t_out, t_up = (x_half(k, v) for v in (sh_in, sh_out, sh_up))
    gate_lo, gate_hi = (Part(sh_gate, i * (sh_gate.shape[0] // 2), sh_gate.shape[0] // 2) for i in range(2))
    down_lo, down_hi = (Part(sh_down, i * (sh_down.shape[0] // 2), sh_down.shape[0] // 2) for i in range(2))
    t_gate0a, t_gate0b = x_half(k, gate_lo, 0), x_move(k, gate_hi, 0)
    t_down0a, t_down0b = x_half(k, down_lo, 0), x_move(k, down_hi, 0)
    t_gate1, t_down1 = x_half(k, sh_gate, 1), x_move(k, sh_down, 1)
    t_seq = Task(k, row_shape, "section", seq_moves, 1)
    t_gain, z_cols = x_move(k, own_gain), z_gather(k, conv_x)
    z_in0, z_out0 = z_gather_half(k, sh_in, t_in.out, 0), z_gather_half(k, sh_out, t_out.out, 0)
    z_gate0a = z_gather_half(k, gate_lo, t_gate0a.out, 0)
    z_gate0b, x_gate0a = z_gather_whole(k, gate_hi, t_gate0b.out, 0), x_move(k, z_gate0a.out)
    z_up0 = z_gather_half(k, sh_up, t_up.out, 0)
    x_cols, x_in0, x_out0 = (x_move(k, v.out) for v in (z_cols, z_in0, z_out0))
    x_load, gain_load = start_rows(k, 0, t_seq.out, False), gains_of(k, 0, t_gain.out, False)
    taps = load_all(k, conv_kernel)
    angles = Angles(k, length, size, 128)
    w_in0, w_cols = Weight(k, "rows", (z_in0.out, x_in0.out)), Weight(k, "conv", (z_cols.out, x_cols.out))
    w_out0 = Weight(k, "cols", (z_out0.out, x_out0.out))
    g0 = Gather(k, x_load.buf, (gain_load.buf, 0), [w_in0, w_cols], save=(0, 1, 2))
    conv = Conv(k, g0.values[0], g0.values[1], taps.buf)
    y0 = Save(k, conv.y)
    s1 = Scatter(k, [conv.y], [w_out0], x_load.buf)
    mid0 = Save(k, s1.out)
    k.do(t_in.send, t_out.send, z_cols.send, t_gate0b.send, t_gate0a.send, t_gate1.send)
    k.do(t_gain.send, t_seq.send)
    k.do(t_in.wait, z_in0.send, t_out.wait, z_out0.send, z_cols.step, z_in0.step, z_out0.step)
    k.do(z_cols.step, z_in0.step, z_out0.step, t_gate0b.wait, z_gate0b.send)
    k.do(t_gate0a.wait, z_gate0a.send)
    k.do(z_cols.wait, x_cols.send, z_in0.wait, x_in0.send, z_out0.wait, x_out0.send, t_up.send)
    k.do(t_gain.wait, gain_load.start, t_seq.wait, x_load.start, gain_load.wait, x_load.wait)
    k.do(g0.begin, z_gate0b.step, z_gate0a.step, angles.run, z_gate0b.step, z_gate0a.step)
    k.do(x_cols.wait, w_cols.start, x_in0.wait, w_in0.start, z_gate0a.wait, x_gate0a.send)
    k.do(t_down0b.send, t_down0a.send, t_down1.send, t_up.wait, z_up0.send)
    k.do(g0.loop, z_up0.step, taps.wait, conv.run, y0.start)
    k.do(x_out0.wait, w_out0.start, s1.loop, z_up0.step, s1.finish, mid0.start)
    k.do(*wait(t_gate1, t_down0a, t_down0b, t_down1, z_gate0b, x_gate0a, z_up0))
    k.build()
    a0, proj0, value0 = (out for _, out, _ in g0.saved)
    table_arrays = [qk_gain] + [v.out for v in angles.saves]
    y0, mid0 = y0.out, mid0.out

    k = Kernel(1)
    x_up0, z_gate1 = x_move(k, z_up0.out), z_gather_half(k, sh_gate, t_gate1.out, 1)
    z_down0a = z_gather_half(k, down_lo, t_down0a.out, 0)
    z_down0b = z_gather_whole(k, down_hi, t_down0b.out, 0)
    z_in1, z_out1 = z_gather_half(k, sh_in, t_in.out, 1), z_gather_half(k, sh_out, t_out.out, 1)
    x_down0a, x_in1, x_out1 = (x_move(k, v.out) for v in (z_down0a, z_in1, z_out1))
    rows, gain_load = load_all(k, mid0), gains_of(k, 0, t_gain.out)
    w_gate0 = Weight(k, "rows", (z_gate0a.out, x_gate0a.out), (z_gate0b.out, None), early=True)
    w_up0 = Weight(k, "rows", (z_up0.out, x_up0.out))
    w_down0 = Weight(k, "cols", (z_down0a.out, x_down0a.out), (z_down0b.out, None))
    g2 = Gather(
        k, rows.buf, (gain_load.buf, 1), [w_gate0, w_up0], epilogue="ffn", save=(0, 1, 2, 3)
    )
    s3 = Scatter(k, [g2.values[2]], [w_down0], rows.buf, low=True)
    z_rows = Save(k, s3.out)
    k.do(x_up0.send, z_down0a.send, z_down0b.send, rows.wait, gain_load.wait, g2.begin)
    k.do(z_in1.send, z_out1.send, z_down0a.step, z_in1.step, z_out1.step, z_down0b.step)
    k.do(z_down0a.step, z_in1.step, z_out1.step, z_gate1.send, z_down0a.wait, x_down0a.send)
    k.do(x_up0.wait, w_up0.start, z_down0b.step, g2.loop, z_gate1.step)
    k.do(z_in1.wait, x_in1.send, z_out1.wait, x_out1.send, z_down0b.wait, x_down0a.wait)
    k.do(w_down0.start, s3.loop, z_gate1.step, s3.finish, z_rows.start)
    k.do(*wait(x_in1, x_out1, z_gate1))
    k.build()
    m0, gate0, up0, hid0 = (out for _, out, _ in g2.saved)
    z_rows = z_rows.out

    k = Kernel(2)
    x_gate1, z_up1 = x_move(k, z_gate1.out), z_gather_half(k, sh_up, t_up.out, 1)
    z_down1a, z_down1b = (z_gather_whole(k, sh_down, t_down1.out, 1, i) for i in range(2))
    x_up1 = x_move(k, z_up1.out)
    rows, gain_load = load_all(k, z_rows), gains_of(k, 1, t_gain.out)
    tables = [load_all(k, v) for v in table_arrays]
    w_in1 = Weight(k, "rows", (z_in1.out, x_in1.out), early=True)
    w_out1 = Weight(k, "cols", (z_out1.out, x_out1.out), early=True)
    g4 = Gather(k, rows.buf, (gain_load.buf, 0), [w_in1], save=(0, 1))
    attend = Attend(k, g4.values[0], tables, size)
    kept = [Save(k, v) for v in (attend.q_rot, attend.k_rot, attend.y)]
    s5 = Scatter(k, [attend.y], [w_out1], rows.buf)
    mid1 = Save(k, s5.out)
    k.do(x_gate1.send, z_up1.send, rows.wait, gain_load.wait, g4.begin, z_up1.step)
    k.do(z_down1a.send, g4.loop, z_up1.step, z_down1b.send)
    k.do(lambda: attend.run(z_up1.wait, x_up1.send, z_down1a.step))
    k.do(*(v.start for v in kept))
    k.do(z_down1b.step, s5.loop, z_down1a.step, z_down1b.step, s5.finish, mid1.start)
    k.do(*wait(x_gate1, x_up1, z_down1a, z_down1b))
    k.build()
    a1, proj1 = (out for _, out, _ in g4.saved)
    q_rot, k_rot, y1 = (v.out for v in kept)
    mid1 = mid1.out

    k = Kernel(3)
    rows, gain_load = load_all(k, mid1), gains_of(k, 1, t_gain.out)
    cot = start_rows(k, 1, t_seq.out)
    w_gate1 = Weight(k, "rows", (z_gate1.out, x_gate1.out), early=True)
    w_up1 = Weight(k, "rows", (z_up1.out, x_up1.out), early=True)
    w_down1 = Weight(k, "cols", (z_down1a.out, None), (z_down1b.out, None), early=True)
    g6 = Gather(k, rows.buf, (gain_load.buf, 1), [w_gate1, w_up1], epilogue="ffn")
    g8 = Gather(
        k, cot.buf, None, [w_down1], [g6.values[0], g6.values[1]], trans=True, epilogue="ffn_back"
    )
    p_down1 = Product(k, g6.values[2], g8.full)
    p_gate1, p_up1 = Product(k, g6.full, g8.values[0]), Product(k, g6.full, g8.values[1])
    s9 = Scatter(k, g8.values, [w_gate1, w_up1], cot.buf, (rows.buf, (gain_load.buf, 1)), True)
    hid1 = Save(k, g6.values[2])
    d_mid1, gain11 = Save(k, s9.out), Save(k, s9.gain_grad)
    k.do(rows.wait, gain_load.wait, g6.begin, cot.wait, g8.begin, g6.loop, hid1.start, g8.loop)
    k.do(s9.loop, p_down1.run, p_gate1.run, p_up1.run)
    k.do(s9.finish, d_mid1.start, gain11.start, p_down1.wait, p_gate1.wait, p_up1.wait)
    k.build()
    hid1, d_mid1, gain11 = hid1.out, d_mid1.out, gain11.out

    k = Kernel(4)
    r_down1 = x_half(k, p_down1.out)
    r_gate1, q_up1 = x_slots(k, p_gate1.out, "rows"), sum_scatter(k, "rows", p_up1.out)
    rows, gain_load = load_all(k, d_mid1), gains_of(k, 1, t_gain.out)
    value = load_all(k, z_rows)
    tables = [load_all(k, v) for v in table_arrays]
    proj, q_load, k_load, y_load, a_load = (load_all(k, v) for v in (proj1, q_rot, k_rot, y1, a1))
    w_in1 = Weight(k, "rows", (z_in1.out, x_in1.out), early=True)
    w_out1 = Weight(k, "cols", (z_out1.out, x_out1.out), early=True)
    g10 = Gather(k, rows.buf, None, [w_out1], trans=True)
    p_out1 = Product(k, y_load.buf, g10.full)
    back = AttendBack(k, proj.buf, tables, size, q_load.buf, k_load.buf, g10.values[0])
    p_in1 = Product(k, a_load.buf, back.d_proj)
    s11 = Scatter(
        k, [back.d_proj], [w_in1], rows.buf, (value.buf, (gain_load.buf, 0)), True, low=True
    )
    d_z, gain10 = Save(k, s11.out), Save(k, s11.gain_grad)
    head_gains = [Save(k, back.q_gain), Save(k, back.k_gain)]
    k.early.append(q_up1.load)
    k.do(r_down1.send, r_gate1.send, rows.wait, g10.begin, q_up1.send, g10.loop)
    k.do(y_load.wait, p_out1.run, q_up1.step)
    k.do(proj.wait, q_load.wait, k_load.wait, lambda: back.run(q_up1.step))
    k.do(*(v.start for v in head_gains))
    k.do(gain_load.wait, value.wait, s11.loop, a_load.wait, p_in1.run)
    k.do(s11.finish, d_z.start, gain10.start, p_out1.wait, p_in1.wait)
    k.do(*wait(r_down1, r_gate1, q_up1))
    k.build()
    d_z, gain10 = d_z.out, gain10.out
    q_gain, k_gain = (v.out for v in head_gains)

    k = Kernel(5)
    q_gate1 = sum_scatter(k, "rows", p_gate1.out, r_gate1.out)
    m_up1, r_out1 = x_move(k, q_up1.out, 0), x_half(k, p_out1.out)
    q_out1 = sum_scatter(k, "cols", p_out1.out, r_out1.out)
    r_in1 = x_slots(k, p_in1.out, "rows")
    q_in1 = sum_scatter(k, "rows", p_in1.out, r_in1.out)
    q_down1 = sum_scatter(k, "cols", p_down1.out, r_down1.out)
    rows, value, gain_load = load_all(k, d_z), load_all(k, mid0), gains_of(k, 0, t_gain.out)
    gate_load, up_load, hid_load, m_load = (load_all(k, v) for v in (gate0, up0, hid0, m0))
    w_gate0 = Weight(k, "rows", (z_gate0a.out, x_gate0a.out), (z_gate0b.out, None), early=True)
    w_up0 = Weight(k, "rows", (z_up0.out, x_up0.out), early=True)
    w_down0 = Weight(k, "cols", (z_down0a.out, x_down0a.out), (z_down0b.out, None), early=True)
    g12 = Gather(
        k, rows.buf, None, [w_down0], [gate_load.buf, up_load.buf], trans=True, epilogue="ffn_back"
    )
    p_down0 = Product(k, hid_load.buf, g12.full)
    p_gate0, p_up0 = Product(k, m_load.buf, g12.values[0]), Product(k, m_load.buf, g12.values[1])
    r_down0 = x_half(k, p_down0.out)
    s13 = Scatter(
        k, g12.values, [w_gate0, w_up0], rows.buf, (value.buf, (gain_load.buf, 1)), True
    )
    d_mid0, gain01 = Save(k, s13.out), Save(k, s13.gain_grad)
    k.early += [q_gate1.load, q_down1.load]
    k.do(r_in1.send, r_out1.send, m_up1.send, q_gate1.send, rows.wait, g12.begin, q_down1.send)
    k.do(gate_load.wait, up_load.wait, g12.loop, q_gate1.step, q_down1.step)
    k.do(hid_load.wait, p_down0.run, p_down0.wait, r_down0.send)
    k.do(r_in1.wait, q_in1.add, r_out1.wait, q_out1.add)
    k.do(s13.loop, q_gate1.step, q_down1.step, q_in1.step, q_out1.step)
    k.do(m_load.wait, p_gate0.run, p_up0.run, value.wait, gain_load.wait)
    k.do(s13.finish, d_mid0.start, gain01.start, q_in1.step, q_out1.step)
    k.do(p_gate0.wait, p_up0.wait, *wait(q_gate1, q_out1, q_in1, q_down1, m_up1, r_down0))
    k.build()
    d_mid0, gain01 = d_mid0.out, gain01.out

    k = Kernel(6)
    r_gate0 = x_slots(k, p_gate0.out, "rows")
    q_gate0 = sum_scatter(k, "rows", p_gate0.out, r_gate0.out)
    q_down0 = sum_scatter(k, "cols", p_down0.out, r_down0.out)
    q_up0 = sum_scatter(k, "rows", p_up0.out)
    m_up0 = x_move(k, q_up0.out, 1)
    e_down1 = Finish(k, q_down1.out, 1)
    e_gate1, e_out1, e_in1 = (Finish(k, v.out, 1) for v in (q_gate1, q_out1, q_in1))
    rows, gain_load = load_all(k, d_mid0), gains_of(k, 0, t_gain.out)
    x_load, taps = start_rows(k, 0, t_seq.out), load_all(k, conv_kernel)
    y_load, a_load, proj, value = (load_all(k, v) for v in (y0, a0, proj0, value0))
    w_in0 = Weight(k, "rows", (z_in0.out, x_in0.out), early=True)
    w_cols = Weight(k, "conv", (z_cols.out, x_cols.out), early=True)
    w_out0 = Weight(k, "cols", (z_out0.out, x_out0.out), early=True)
    g14 = Gather(k, rows.buf, None, [w_out0], trans=True)
    p_out0 = Product(k, y_load.buf, g14.full)
    back = ConvBack(k, proj.buf, value.buf, taps.buf, g14.values[0])
    p_in0, p_cols = Product(k, a_load.buf, back.d_proj), Product(k, a_load.buf, back.d_value)
    r_out0, r_in0 = x_half(k, p_out0.out), x_slots(k, p_in0.out, "rows")
    r_cols = x_slots(k, p_cols.out, "conv")
    q_out0, q_in0 = sum_scatter(k, "cols", p_out0.out, r_out0.out), sum_scatter(k, "rows", p_in0.out, r_in0.out)
    q_cols = sum_scatter(k, "conv", p_cols.out, r_cols.out)
    e_down0, e_gate0, e_out0, e_in0 = (
        Finish(k, v.out, 0) for v in (q_down0, q_gate0, q_out0, q_in0)
    )
    s15 = Scatter(
        k, [back.d_proj, back.d_value], [w_in0, w_cols], rows.buf,
        (x_load.buf, (gain_load.buf, 0)), True, low=True,
    )
    d_x = Save(k, s15.out)
    tap_rows = conv_kernel.shape[0]
    small = k.vmem((8, model_width), F32)
    small_out = Save(k, small)
    ready = [load_all(k, v) for v in (gain01, gain10, gain11)]
    head_loads = [load_all(k, v) for v in (q_gain, k_gain)]

    def fill_small():
        t = lax.axis_index("tensor")
        small.ref[...] = jnp.zeros_like(small.ref)
        small.ref[0:1, :] = s15.gain_grad.ref[...]
        for i, load in enumerate(ready):
            load.wait()
            small.ref[i + 1 : i + 2, :] = load.buf.ref[...]
        small.ref[4 : 4 + tap_rows, block_of(t, channels)] = back.d_kernel.ref[...]
        at = 0
        for load in head_loads:
            load.wait()
            width = load.buf.shape[1]
            small.ref[7:8, at : at + width] = load.buf.ref[...]
            at += width
        small_out.start()

    t_small = x_move(k, small_out.out)
    z_small = SumShare(k, [small_out.out, t_small.out], "dp")
    t_total = SumShare(k, [z_small.out], "tensor", slotted=True)
    hid_load, mid_load = load_all(k, hid1), load_all(k, mid1)
    w_down1 = Weight(k, "cols", (z_down1a.out, None), (z_down1b.out, None), early=True)
    s7 = Scatter(k, [hid_load.buf], [w_down1], mid_load.buf, low=True)
    y_rows = Save(k, s7.out)
    t_x, t_y = x_move(k, d_x.out, 1), x_move(k, y_rows.out, 0)
    k.early += [q_up0.load, q_down0.load]
    k.early += [v.load for v in (e_down1, e_gate1, e_out1, e_in1)]
    k.do(r_gate0.send, q_up0.send, rows.wait, g14.begin, q_down0.send)
    k.do(e_down1.send, e_gate1.send, e_out1.send, e_in1.send, g14.loop)
    k.do(y_load.wait, p_out0.run, p_out0.wait, r_out0.send, q_up0.step)
    k.do(proj.wait, value.wait, taps.wait, back.run, q_down0.step, a_load.wait)
    k.do(p_in0.run, p_cols.run, p_in0.wait, r_in0.send, p_cols.wait, r_cols.send)
    k.do(r_gate0.wait, q_gate0.add, x_load.wait, gain_load.wait, s15.loop, q_up0.step)
    k.do(q_down0.step, s15.finish, d_x.start, fill_small, d_x.wait, t_x.send)
    k.do(small_out.wait, t_small.send, q_gate0.step, hid_load.wait, mid_load.wait, s7.loop)
    k.do(r_out0.wait, q_out0.add, r_in0.wait, q_in0.add)
    k.do(r_cols.wait, q_cols.add, q_up0.wait, m_up0.send, q_down0.wait, e_down0.add)
    k.do(s7.finish, y_rows.start, y_rows.wait, t_y.send)
    k.do(q_gate0.step, q_out0.step, q_in0.step, q_cols.step, t_small.wait, z_small.add)
    k.do(q_gate0.wait, e_gate0.add, q_out0.step, q_in0.step, q_cols.step)
    k.do(z_small.wait, t_total.add, q_out0.wait, e_out0.add, q_in0.wait, e_in0.add)
    rest = (e_down1, e_gate1, e_out1, e_in1, q_cols, e_down0, e_gate0, m_up0, e_out0, e_in0)
    k.do(*wait(*rest, t_total, t_x, t_y))
    k.build()

    owned = [
        ([e_in0], [e_in1], 1),
        ([e_out0], [e_out1], 1),
        ([e_gate0], [e_gate1], 1),
        ([q_up0, m_up0], [q_up1, m_up1], 1),
        ([e_down0], [e_down1], 1),
        ([q_cols], [q_cols], 0),
    ]
    return pack(
        [(zero, one, lead) for zero, one, lead in owned], t_total, d_x.out, y_rows.out, t_x, t_y,
        (norm_gain.shape, conv_kernel.shape, qk_gain.shape),
    )


def slot_free(val, shape):
    value = val.out.array
    if value.ndim == 3 and value.shape[0] * value.shape[1] != shape[0]:
        value = jnp.sum(value.astype(F32), axis=0).astype(BF)
    return value.reshape(shape)


def pack_kernel(plan, *refs):
    n_in, leads, terms, tap_rows = plan
    ins, rest = refs[:n_in], refs[n_in:]
    result, gain_out, *grads, cols, taps, heads = rest[: len(leads) + 4]
    grads = [*grads, cols]
    room = iter(rest[len(leads) + 4 :])
    own_v, moved_v, small_v, *bufs = (next(room) for _ in range(3 + len(terms)))
    out_v = [next(room) for _ in leads]
    load_sem, store_sem = room
    s, t = lax.axis_index("section"), lax.axis_index("tensor")
    small, d_x, y_rows, moved, moved_y, *parts = ins

    def either(cond, zero, one, dst, sem):
        if zero is not None:
            pl.when(cond)(pltpu.make_async_copy(zero, dst, sem).start)
        if one is not None:
            pl.when(jnp.logical_not(cond))(pltpu.make_async_copy(one, dst, sem).start)

    first = s == 0
    either(first, d_x, y_rows, own_v, load_sem.at[0])
    either(first, moved, moved_y, moved_v, load_sem.at[1])
    pltpu.make_async_copy(small, small_v, load_sem.at[2]).start()
    for j, (zero, one, _) in enumerate(terms):
        either(
            first,
            None if zero is None else parts[zero],
            None if one is None else parts[one],
            bufs[j],
            load_sem.at[3 + j],
        )
    for j, (zero, one, i) in enumerate(terms):
        arrive = pltpu.make_async_copy(parts[one if zero is None else zero], bufs[j], load_sem.at[3 + j])
        begins = j == 0 or terms[j - 1][2] != i

        def put(j=j, i=i, begins=begins):
            def add_rows(at):
                value = bufs[j][at, :].astype(F32)
                out_v[i][at, :] = value if begins else out_v[i][at, :] + value

            chunked(bufs[j].shape[0], add_rows)

        if zero is None or one is None:
            cond = first if one is None else jnp.logical_not(first)

            @pl.when(cond)
            def _(arrive=arrive, put=put):
                arrive.wait()
                put()
        else:
            arrive.wait()
            put()
        if j + 1 == len(terms) or terms[j + 1][2] != i:
            dst = grads[i].at[0] if leads[i] else grads[i]
            pltpu.make_async_copy(out_v[i], dst, store_sem.at[i]).start()
    pltpu.make_async_copy(d_x, own_v, load_sem.at[0]).wait()
    pltpu.make_async_copy(moved, moved_v, load_sem.at[1]).wait()
    n = len(leads)
    stores = [
        pltpu.make_async_copy(own_v, result.at[0, s], store_sem.at[n]),
        pltpu.make_async_copy(moved_v, result.at[0, 1 - s], store_sem.at[n + 1]),
    ]
    for store in stores:
        store.start()
    pltpu.make_async_copy(small, small_v, load_sem.at[2]).wait()
    total = small_v[0]
    for i in range(1, small_v.shape[0]):
        total = total + small_v[i]
    gain_out[0] = jnp.where(first, total[0:2], total[2:4])
    channels, size = taps.shape[1], heads.shape[1]
    chosen = total[4 : 4 + tap_rows, 0:channels]
    for i in range(1, total.shape[1] // channels):
        chosen = jnp.where(t == i, total[4 : 4 + tap_rows, i * channels : (i + 1) * channels], chosen)
    taps[...] = chosen
    at = 0
    for row, width in enumerate((channels, channels // 2)):
        value = total[7:8, at : at + size]
        for i in range(1, width // size):
            value = value + total[7:8, at + i * size : at + (i + 1) * size]
        heads[row : row + 1, :] = value
        at += width
    for i, store in enumerate(leads):
        dst = grads[i].at[0] if store else grads[i]
        pltpu.make_async_copy(out_v[i], dst, store_sem.at[i]).wait()
    for store in stores:
        store.wait()


def pack(owned, small, d_x, y_rows, moved_x, moved_y, shapes):
    gain_shape, tap_shape, head_shape = shapes
    parts, terms, leads, out_shapes = [], [], [], []
    for i, (zero, one, lead) in enumerate(owned):
        whole = zero[0].out.shape
        if lead and len(whole) == 3 and isinstance(zero[0], Finish):
            shape = (whole[0] * whole[1], whole[2])
        else:
            shape = whole[-2:]
        shape = tuple(shape)
        leads.append(lead)
        out_shapes.append(shape)
        for j in range(max(len(zero), len(one))):
            pair = []
            for side in (zero, one):
                if j < len(side):
                    parts.append(slot_free(side[j], shape))
                    pair.append(len(parts) - 1)
                else:
                    pair.append(None)
            terms.append((*pair, i))
    operands = [v.array for v in (small.out, d_x, y_rows, moved_x.out, moved_y.out)] + parts
    rows = d_x.shape
    smem = pl.BlockSpec(memory_space=pltpu.VMEM)
    out_shape = [jax.ShapeDtypeStruct((1, 2) + rows, BF), jax.ShapeDtypeStruct(gain_shape, F32)]
    out_shape += [
        jax.ShapeDtypeStruct((1,) + v if lead else v, F32) for v, lead in zip(out_shapes, leads)
    ]
    out_shape += [jax.ShapeDtypeStruct(v, F32) for v in (tap_shape, head_shape)]
    n = len(leads)
    return tuple(
        pl.pallas_call(
            functools.partial(
                pack_kernel, (len(operands), tuple(leads), tuple(terms), tap_shape[0])
            ),
            out_shape=out_shape,
            in_specs=[ANY] * len(operands),
            out_specs=[ANY, smem] + [ANY] * n + [smem] * 2,
            scratch_shapes=[pltpu.VMEM(rows, BF)] * 2
            + [pltpu.VMEM(small.out.shape, F32)]
            + [pltpu.VMEM(out_shapes[i], BF) for _, _, i in terms]
            + [pltpu.VMEM(v, F32) for v in out_shapes]
            + [DMA((3 + len(terms),)), DMA((n + 2,))],
            compiler_params=pltpu.CompilerParams(vmem_limit_bytes=VMEM_BYTES),
            name="pack",
        )(*operands)
    )


def solution(mesh):
    in_specs = (
        P("section", "dp", "tensor", None),
        P("section", None, None),
        P("section", "dp", "tensor"),
        P("section", "tensor", "dp"),
        P("section", "dp", "tensor"),
        P("section", "dp", "tensor"),
        P("section", "tensor", "dp"),
        P(("section", "dp"), "tensor"),
        P(None, "tensor"),
        P(),
    )
    out_specs = (
        P("section", "dp", "tensor", None),
        P("section", None, None),
        P("section", "dp", "tensor"),
        P("section", "tensor", "dp"),
        P("section", "dp", "tensor"),
        P("section", "dp", "tensor"),
        P("section", "tensor", "dp"),
        P(("section", "dp"), "tensor"),
        P(None, "tensor"),
        P(),
    )
    return jax.shard_map(body, mesh=mesh, in_specs=in_specs, out_specs=out_specs, check_vma=False)
```

```python
import functools

import jax
import jax.numpy as jnp
from jax import lax
from jax.experimental import pallas as pl
from jax.experimental.pallas import tpu as pltpu
from jax.sharding import PartitionSpec as P

HEADS = 16
KV_HEADS = 8

EPS = 1e-05
ROPE_BASE = 1000000.0
MASKED = -1e30

MESH = pl.DeviceIdType.MESH
ANY = pl.BlockSpec(memory_space=pl.ANY)
DMA = pltpu.SemaphoreType.DMA
VMEM_BYTES = 63 * 1024 * 1024
BF = jnp.bfloat16
F32 = jnp.float32
ROW_BLOCK = 256
STRIP = 32


def contract(left_op, right_op, left_dim, right_dim):
    return lax.dot_general(
        left_op, right_op, (((left_dim,), (right_dim,)), ((), ())), preferred_element_type=F32
    )


def norm_rows(values, gain):
    return values * lax.rsqrt(jnp.mean(values * values, axis=-1, keepdims=True) + EPS) * gain


def norm_back(values, gain, grad_in):
    row_scale = lax.rsqrt(jnp.mean(values * values, axis=-1, keepdims=True) + EPS)
    normed = values * row_scale
    gain_grad = jnp.sum(grad_in * normed, axis=0, keepdims=True)
    scaled = grad_in * gain
    value_grad = row_scale * (scaled - normed * jnp.mean(scaled * normed, axis=-1, keepdims=True))
    return (value_grad, gain_grad)


class Angles:
    def __init__(self, k, length, head_size, width):
        self.half = head_size // 2
        self.tables = [k.vmem((length, width), F32) for _ in range(2)]
        self.saves = [Save(k, v) for v in self.tables]

    def run(self):
        cos, sin = self.tables
        shape = (ROW_BLOCK, cos.shape[1])
        column = (lax.broadcasted_iota(jnp.int32, shape, 1) % self.half).astype(F32)
        frequency = ROPE_BASE ** (-(column / self.half))
        row = lax.broadcasted_iota(jnp.int32, shape, 0)

        def step(i, carry):
            rows = block_of(i, ROW_BLOCK)
            angle = (row + i * ROW_BLOCK).astype(F32) * frequency
            cos.ref[rows, :] = jnp.cos(angle)
            sin.ref[rows, :] = jnp.sin(angle)
            return carry

        lax.fori_loop(0, cos.shape[0] // ROW_BLOCK, step, 0)
        for save in self.saves:
            save.start()


def silu_parts(gate):
    sig = 1.0 / (1.0 + jnp.exp(-gate))
    return sig, gate * sig


def chunked(rows, step):
    size = next((n for n in (32, 16) if rows % n == 0), rows)
    if size == rows:
        step(pl.ds(0, rows))
    else:
        lax.fori_loop(0, rows // size, lambda i, c: step(block_of(i, size)) or c, 0)


def dp_size():
    return lax.axis_size("dp")


def spot():
    return tuple(lax.axis_index(a) for a in ("section", "dp", "tensor"))


def block_of(index, size):
    return pl.ds(pl.multiple_of(index * size, size), size)


class Val:
    def __init__(self, shape, dtype):
        self.shape, self.dtype = tuple(shape), dtype
        self.ref = self.array = None


class Kernel:
    def __init__(self, cid):
        self.cid, self.ins, self.arrays, self.outs, self.room = cid, [], [], [], []
        self.early, self.steps, self.late, self.axes = [], [], [], set()
        self.once = []

    def input(self, array):
        array = array.array if isinstance(array, Val) else array
        for val, known in zip(self.ins, self.arrays):
            if known is array:
                return val
        val = Val(array.shape, array.dtype)
        self.ins.append(val)
        self.arrays.append(array)
        return val

    def output(self, shape, dtype):
        val = Val(shape, dtype)
        self.outs.append(val)
        return val

    def vmem(self, shape, dtype):
        val = Val(shape, dtype)
        self.room.append((val, pltpu.VMEM(tuple(shape), dtype)))
        return val

    def sem(self, *shape):
        val = Val(shape, None)
        self.room.append((val, DMA(shape)))
        return val

    def do(self, *steps):
        self.steps += steps

    def body(self, *refs):
        vals = self.ins + self.outs + [val for val, _ in self.room]
        for val, ref in zip(vals, refs):
            val.ref = ref
        for item in self.once:
            item.waited = False
            item.phase = 0
        for step in self.early:
            step()
        self.greet()
        for step in self.steps + self.late:
            step()

    def greet(self):
        s, d, t = spot()
        _, sib, cross, diag = places()
        barrier = pltpu.get_barrier_semaphore()
        peers = [{"tensor": sib}, {"tensor": cross}]
        if "tensor" in self.axes:
            peers.append({"tensor": diag})
        if "section" in self.axes:
            peers.append({"section": 1 - s})
        if "dp" in self.axes:
            peers += [{"dp": (d + i) % dp_size()} for i in range(1, dp_size())]

        def signal(peer):
            pl.semaphore_signal(barrier, inc=1, device_id=peer, device_id_type=MESH)

        for peer in peers:
            signal(peer)
        expected = len(peers)
        if "line" in self.axes and "dp" not in self.axes:
            pl.when(d < 3)(lambda: signal({"dp": (d + 1) % 4}))
            pl.when(d > 0)(lambda: signal({"dp": (d + 3) % 4}))
            expected = expected + (d + 2) // 3 + (5 - d) // 3
        pl.semaphore_wait(barrier, expected)

    def build(self):
        result = pl.pallas_call(
            self.body,
            out_shape=[jax.ShapeDtypeStruct(v.shape, v.dtype) for v in self.outs],
            in_specs=[ANY] * len(self.ins),
            out_specs=[ANY] * len(self.outs),
            scratch_shapes=[room for _, room in self.room],
            compiler_params=pltpu.CompilerParams(
                collective_id=self.cid, has_side_effects=True, vmem_limit_bytes=VMEM_BYTES
            ),
            name=f"stage{self.cid}",
        )(*self.arrays)
        for val, array in zip(self.outs, result):
            val.array = array


def remote(src, dst, send_sem, recv_sem, peer):
    return pltpu.make_async_remote_copy(
        src_ref=src, dst_ref=dst, send_sem=send_sem, recv_sem=recv_sem,
        device_id=peer, device_id_type=MESH,
    )


class Load:
    def __init__(self, k, sources, shape, dtype, early=False):
        self.k, self.sources, self.waited = k, sources, False
        self.buf, self.sem = k.vmem(shape, dtype), k.sem(1)
        k.once.append(self)
        if early:
            k.early.append(self.start)

    def moves(self):
        for cond, source in self.sources(*spot()):
            yield cond, pltpu.make_async_copy(source, self.buf.ref, self.sem.ref.at[0])

    def start(self):
        for cond, move in self.moves():
            if cond is None:
                move.start()
            else:
                pl.when(cond)(move.start)

    def wait(self):
        if not self.waited:
            self.waited = True
            next(self.moves())[1].wait()


def load_all(k, array, early=True):
    val = k.input(array)
    return Load(k, lambda s, d, t: [(None, val.ref)], val.shape, val.dtype, early)


class Save:
    def __init__(self, k, buf):
        self.buf, self.out, self.sem = buf, k.output(buf.shape, buf.dtype), k.sem(1)
        self.waited = False
        k.once.append(self)
        k.late.append(self.wait)

    def move(self):
        return pltpu.make_async_copy(self.buf.ref, self.out.ref, self.sem.ref.at[0])

    def start(self):
        self.move().start()

    def wait(self):
        if not self.waited:
            self.waited = True
            self.move().wait()


class Task:
    final = None

    def __init__(self, k, out, axis, moves, count, n_local=1, out_dtype=BF):
        self.k, self.axis, self.make = k, axis, moves
        self.out = k.output(out, out_dtype)
        self.send_sem, self.recv_sem, self.local_sem = k.sem(count), k.sem(count), k.sem(n_local)
        self.waited = False
        k.axes.add(axis)
        k.once.append(self)

    def local(self, src, dst, i):
        return pltpu.make_async_copy(src, dst, self.local_sem.ref.at[i])

    def pairs(self, every):
        far, near = self.make(*spot())
        for i, (sources, dst, peer) in enumerate(far):
            for cond, src in sources if every else sources[:1]:
                yield cond, True, remote(
                    src, dst, self.send_sem.ref.at[i], self.recv_sem.ref.at[i], peer
                )
        for i, (sources, dst) in enumerate(near):
            for cond, src in sources if every else sources[:1]:
                yield cond, False, self.local(src, dst, i)

    def step(self):
        pass

    def send(self):
        for cond, far, move in self.pairs(True):
            if far and self.final is not None:
                cond = lax.axis_index("section") == 1 - self.final
            if cond is None:
                move.start()
            else:
                pl.when(cond)(move.start)

    def wait(self):
        if self.waited:
            return
        self.waited = True
        s = lax.axis_index("section")
        for _, far, move in self.pairs(False):
            if not far:
                move.wait()
            elif self.final is None:
                move.wait_recv()
                move.wait_send()
            else:
                pl.when(s == 1 - self.final)(move.wait_send)
                pl.when(s == self.final)(move.wait_recv)


class Part:
    def __init__(self, base, start, rows):
        self.base, self.start, self.rows = base, start, rows
        self.shape, self.dtype = (rows,) + tuple(base.shape[1:]), base.dtype
        self.array = None

    @property
    def ref(self):
        return self.base.ref.at[pl.ds(self.start, self.rows)]


def as_val(k, value):
    if isinstance(value, Part):
        return Part(as_val(k, value.base), value.start, value.rows)
    value = value.out if isinstance(value, Task) else value
    known = isinstance(value, Val) and (value.array is None)
    return value if known else k.input(value)


class Line(Task):
    def __init__(self, k, out, out_dtype=BF, n_local=1):
        super().__init__(k, out, "line", None, 6, n_local, out_dtype)
        self.send_sem, self.recv_sem = k.sem(2, 3), k.sem(2, 3)
        self.phase = 0

    def hop(self, j, way, src, dst):
        d = lax.axis_index("dp")
        peer = {"dp": (d + 1 if way == 0 else d + 3) % 4}
        return remote(src, dst, self.send_sem.ref.at[way, j], self.recv_sem.ref.at[way, j], peer)


class LineGather(Line):
    def __init__(self, k, sources, shape, dtype):
        super().__init__(k, (4,) + shape, dtype)
        self.sources = sources

    def ends(self, j, way):
        d = lax.axis_index("dp")
        if way == 0:
            return (d >= j) & (d < 3), d >= j + 1
        return (d <= 3 - j) & (d > 0), d <= 2 - j

    def copy(self, j, way, src=None):
        d = lax.axis_index("dp")
        slot = (d + 4 - j if way == 0 else d + j) % 4
        piece = self.out.ref.at[slot]
        return self.hop(j, way, piece if src is None else src, piece)

    def send(self):
        self.phase = 0
        for cond, src in self.sources(*spot()):
            own = self.local(src, self.out.ref.at[lax.axis_index("dp")], 0)
            moves = [(True if cond is None else cond, own)]
            for way in range(2):
                sends = self.ends(0, way)[0]
                moves.append((sends if cond is None else sends & cond, self.copy(0, way, src)))
            for when, move in moves:
                if when is True:
                    move.start()
                else:
                    pl.when(when)(move.start)

    def arrive(self, j):
        for way in range(2):
            pl.when(self.ends(j, way)[1])(self.copy(j, way).wait_recv)

    def step(self):
        self.arrive(self.phase)
        self.phase += 1
        for way in range(2):
            pl.when(self.ends(self.phase, way)[0])(self.copy(self.phase, way).start)

    def wait(self):
        if self.waited:
            return
        self.waited = True
        while self.phase < 2:
            self.step()
        self.arrive(2)
        for j in range(3):
            for way in range(2):
                pl.when(self.ends(j, way)[0])(self.copy(j, way).wait_send)
        d = lax.axis_index("dp")
        self.local(self.sources(*spot())[0][1], self.out.ref.at[d], 0).wait()


def z_gather_from(k, sources, shape, dtype):
    count = dp_size()
    if count == 4:
        return LineGather(k, sources, shape, dtype)

    def moves(s, d, t):
        dst, found = task.out.ref.at[d], sources(s, d, t)
        return [(found, dst, {"dp": (d + i) % count}) for i in range(1, count)], [(found, dst)]

    task = Task(k, (count,) + shape, "dp", moves, count - 1, out_dtype=dtype)
    return task


def z_gather(k, value):
    val = as_val(k, value)
    return z_gather_from(k, lambda s, d, t: [(None, val.ref)], val.shape, val.dtype)


def z_gather_half(k, shard, moved, block):
    shard, moved = as_val(k, shard), as_val(k, moved)
    rows = shard.shape[0] // 2

    def sources(s, d, t):
        own = shard.ref.at[pl.ds(block * rows, rows)]
        return [(s == block, own), (s == 1 - block, moved.ref)]

    return z_gather_from(k, sources, moved.shape, shard.dtype)


def one_way(task, sender):
    task.final = None if sender is None else 1 - sender
    return task


def z_gather_whole(k, shard, moved, block, half=None):
    shard, moved = as_val(k, shard), as_val(k, moved)
    rows = shard.shape[0] if half is None else shard.shape[0] // 2
    part = pl.ds(0 if half is None else half * rows, rows)

    def sources(s, d, t):
        return [(s == block, shard.ref.at[part]), (s == 1 - block, moved.ref.at[part])]

    return z_gather_from(k, sources, (rows,) + shard.shape[1:], shard.dtype)


def x_move(k, value, sender=None):
    val = as_val(k, value)

    def moves(s, d, t):
        return [([(None, val.ref)], task.out.ref, {"section": 1 - s})], []

    task = Task(k, val.shape, "section", moves, 1, out_dtype=val.dtype)
    return one_way(task, sender)


def x_half(k, value, sender=None):
    val = as_val(k, value)
    rows = val.shape[0] // 2

    def moves(s, d, t):
        src = val.ref.at[block_of(1 - s, rows)]
        return [([(None, src)], task.out.ref, {"section": 1 - s})], []

    task = Task(k, (rows,) + val.shape[1:], "section", moves, 1, out_dtype=val.dtype)
    return one_way(task, sender)


def x_slots(k, value, kind):
    val, count = as_val(k, value), dp_size()
    rows = val.shape[0] // (2 * count)

    def moves(s, d, t):
        far = []
        for i in range(count):
            slot = 2 * i + 1 - s if kind == "rows" else (1 - s) * count + i
            src = val.ref.at[block_of(slot, rows)]
            far.append(([(None, src)], task.out.ref.at[i], {"section": 1 - s}))
        return far, []

    task = Task(k, (count, rows) + val.shape[1:], "section", moves, count)
    return task


class Terms:
    def __init__(self, k, kind, grads, received, local):
        self.grads, self.local = as_val(k, grads), local
        self.kind, self.n = kind, dp_size()
        self.whole = received is None
        if self.whole:
            rows, cols = self.grads.shape
            self.rows = rows if kind == "cols" else rows // self.n
            self.cols = cols // self.n if kind == "cols" else cols
            self.shape = (self.n, self.rows, self.cols)
            self.aside = kind == "cols" and self.cols % 128 != 0
            self.total = k.vmem(self.shape, BF)
            self.kept = k.vmem(self.grads.shape, BF) if self.aside else self.total
            return
        self.received = as_val(k, received)
        if kind == "cols":
            self.rows, self.cols = self.grads.shape[0] // 2, self.grads.shape[1] // self.n
            held = (self.rows, self.grads.shape[1])
        else:
            self.rows, self.cols = self.grads.shape[0] // (2 * self.n), self.grads.shape[1]
            held = (self.n, self.rows, self.cols)
        self.kept, self.got = k.vmem(held, BF), k.vmem(held, BF)
        self.shape = (self.n, self.rows, self.cols)
        self.total = k.vmem(self.shape, BF) if kind == "cols" else self.kept

    def loads(self):
        s, grads, kept = lax.axis_index("section"), self.grads.ref, self.kept.ref
        if self.whole and self.aside:
            return [self.local(grads, kept, 2)]
        if self.whole:
            parts = [
                grads.at[:, pl.ds(i * self.cols, self.cols)]
                if self.kind == "cols"
                else grads.at[block_of(i, self.rows)]
                for i in range(self.n)
            ]
            return [self.local(part, kept.at[i], 2 + i) for i, part in enumerate(parts)]
        if self.kind == "cols":
            moves = [self.local(grads.at[block_of(s, self.rows)], kept, 2)]
        else:
            moves = []
            for i in range(self.n):
                slot = 2 * i + s if self.kind == "rows" else s * self.n + i
                moves.append(self.local(grads.at[block_of(slot, self.rows)], kept.at[i], 2 + i))
        return moves + [self.local(self.received.ref, self.got.ref, 1)]

    def load(self):
        for move in self.loads():
            move.start()

    def add(self):
        for move in self.loads():
            move.wait()
        if self.whole and self.aside:
            for i in range(self.n):
                self.total.ref[i] = self.kept.ref[:, i * self.cols : (i + 1) * self.cols]
        if self.whole:
            return
        kept, got, total = self.kept.ref, self.got.ref, self.total.ref
        if self.kind != "cols":

            def piece(i, carry):
                chunked(self.rows, lambda at: total.__setitem__(
                    (i, at), (kept[i, at, :].astype(F32) + got[i, at, :].astype(F32)).astype(BF)
                ))
                return carry

            lax.fori_loop(0, self.n, piece, 0)
            return

        def add_rows(at):
            for i in range(self.n):
                part = slice(i * self.cols, (i + 1) * self.cols)
                value = kept[at, part].astype(F32) + got[at, part].astype(F32)
                total[i, at, :] = value.astype(BF)

        chunked(self.rows, add_rows)


class DirectScatter(Task):
    def __init__(self, k, kind, grads, received):
        self.terms = Terms(k, kind, grads, received, lambda *a: self.local(*a))
        count = dp_size()

        def moves(s, d, t):
            total = self.terms.total.ref
            far = []
            for i in range(1, count):
                other = (d + i) % count
                far.append(([(None, total.at[other])], self.out.ref.at[d], {"dp": other}))
            return far, [([(None, total.at[d])], self.out.ref.at[d])]

        super().__init__(k, self.terms.shape, "dp", moves, count - 1, 2 + count)
        self.load = self.terms.load

    def send(self):
        self.terms.add()
        super().send()

    def add(self):
        self.load()
        self.send()


class LineScatter(Line):
    def __init__(self, k, kind, grads, received):
        self.terms = Terms(k, kind, grads, received, lambda *a: self.local(*a))
        super().__init__(k, self.terms.shape[1:], BF, 6)
        self.got = k.vmem((2, 3) + self.terms.shape[1:], BF)
        self.load = self.terms.load

    def ends(self, j, way):
        d = lax.axis_index("dp")
        if way == 0:
            return (d <= j) & (d < 3), (d >= 1) & (d <= j + 1)
        return (d >= 3 - j) & (d > 0), (d <= 2) & (d >= 2 - j)

    def copy(self, j, way):
        d = lax.axis_index("dp")
        to = (d + 3 - j if way == 0 else d + 1 + j) % 4
        return self.hop(j, way, self.terms.total.ref.at[to], self.got.ref.at[way, j])

    def send(self):
        self.phase = 0
        self.terms.add()
        for way in range(2):
            pl.when(self.ends(0, way)[0])(self.copy(0, way).start)

    def take(self, j, way):
        d = lax.axis_index("dp")
        to = (d + 2 - j if way == 0 else d + 2 + j) % 4
        self.copy(j, way).wait_recv()
        total, got = self.terms.total.ref, self.got.ref

        def add_rows(at):
            value = total[to, at, :].astype(F32) + got[way, j, at, :].astype(F32)
            total[to, at, :] = value.astype(BF)

        chunked(self.terms.rows, add_rows)

    def arrive(self, j):
        for way in range(2):
            pl.when(self.ends(j, way)[1])(functools.partial(self.take, j, way))

    def step(self):
        self.arrive(self.phase)
        self.phase += 1
        for way in range(2):
            pl.when(self.ends(self.phase, way)[0])(self.copy(self.phase, way).start)

    def wait(self):
        if self.waited:
            return
        self.waited = True
        while self.phase < 2:
            self.step()
        self.arrive(2)
        done = self.local(self.terms.total.ref.at[lax.axis_index("dp")], self.out.ref, 0)
        done.start()
        for j in range(3):
            for way in range(2):
                pl.when(self.ends(j, way)[0])(self.copy(j, way).wait_send)
        done.wait()

    def add(self):
        self.load()
        self.send()


def sum_scatter(k, kind, grads, received=None):
    return (LineScatter if dp_size() == 4 else DirectScatter)(k, kind, grads, received)


class Finish(Task):
    def __init__(self, k, pieces, block):
        self.pieces, self.final = as_val(k, pieces), block
        *slots, rows, cols = self.pieces.shape
        self.slots = slots[0] if slots else 0
        if slots:
            self.held, self.total = k.vmem(self.pieces.shape, BF), k.vmem((rows, cols), BF)
        else:
            self.total = self.pieces

        def moves(s, d, t):
            source, dst = [(None, self.total.ref)], self.out.ref.at[s]
            return [(source, dst, {"section": 1 - s})], [(source, dst)]

        super().__init__(k, (2, rows, cols), "section", moves, 1, 2)

    def load(self):
        if self.slots:
            self.local(self.pieces.ref, self.held.ref, 1).start()

    def send(self):
        if self.slots:
            self.local(self.pieces.ref, self.held.ref, 1).wait()
            acc = self.held.ref[0].astype(F32)
            for i in range(1, self.slots):
                acc = acc + self.held.ref[i].astype(F32)
            self.total.ref[...] = acc.astype(BF)
        super().send()

    def add(self):
        self.load()
        self.send()


class SumShare(Task):
    def __init__(self, k, terms, axis, slotted=False):
        self.terms = [as_val(k, v) for v in terms]
        shape = self.terms[0].shape[1:] if slotted else self.terms[0].shape
        count = dp_size() if axis == "dp" else 4
        self.slotted = slotted
        self.bufs = [k.vmem(v.shape, F32) for v in self.terms]
        self.total = k.vmem(shape, F32)

        def moves(s, d, t):
            source, me = [(None, self.total.ref)], d if axis == "dp" else t
            dst = self.out.ref.at[me]
            far = [(source, dst, {axis: (me + i) % count}) for i in range(1, count)]
            return far, [(source, dst)]

        super().__init__(k, (count,) + shape, axis, moves, count - 1, 3, out_dtype=F32)

    def add(self):
        loads = [self.local(v.ref, b.ref, 1 + i) for i, (v, b) in enumerate(zip(self.terms, self.bufs))]
        for load in loads:
            load.start()
        for load in loads:
            load.wait()
        if self.slotted:
            parts = [self.bufs[0].ref[i] for i in range(self.terms[0].shape[0])]
        else:
            parts = [buf.ref[...] for buf in self.bufs]
        acc = parts[0]
        for part in parts[1:]:
            acc = acc + part
        self.total.ref[...] = acc
        self.send()


class Weight:
    def __init__(self, k, kind, *segments, early=False):
        self.kind, self.waited = kind, False
        self.segments, start = [], 0
        for near, far in segments:
            near, far = as_val(k, near), None if far is None else as_val(k, far)
            self.segments.append((near, far, start))
            start += near.shape[1] * (1 if far is None else 2)
        self.count, _, self.cols = self.segments[0][0].shape
        self.rows = start
        if kind == "cols":
            shape = (self.rows, self.count * self.cols)
        else:
            shape = (self.count * self.rows, self.cols)
        self.aside = kind == "cols" and self.cols % 128 != 0
        self.buf = k.vmem(shape, BF)
        sides = [v for near, far, _ in self.segments for v in (near, far) if v is not None]
        self.sem = k.sem(len(sides), self.count)
        if self.aside:
            self.held = [k.vmem(v.shape, BF) for v in sides]
        k.once.append(self)
        if early:
            k.early.append(self.start)

    def sides(self):
        s = lax.axis_index("section")
        for near, far, start in self.segments:
            rows = near.shape[1]
            if far is None:
                yield near, start, None
            else:
                yield near, start + s * rows, s
                yield far, start + (1 - s) * rows, 1 - s

    def moves(self):
        dst = self.buf.ref
        for j, (val, start, sec) in enumerate(self.sides()):
            rows = val.shape[1]
            for i in range(self.count):
                if self.aside:
                    to = self.held[j].ref.at[i]
                elif self.kind == "cols":
                    at = pl.ds(pl.multiple_of(start, 16), rows)
                    to = dst.at[at, pl.ds(i * self.cols, self.cols)]
                else:
                    top = (sec * self.count + i) * rows if self.kind == "conv" else i * self.rows + start
                    to = dst.at[pl.ds(pl.multiple_of(top, 16), rows)]
                yield pltpu.make_async_copy(val.ref.at[i], to, self.sem.ref.at[j, i])

    def start(self):
        for move in self.moves():
            move.start()

    def wait(self):
        if self.waited:
            return
        self.waited = True
        for move in self.moves():
            move.wait()
        if self.aside:
            for j, (val, start, _) in enumerate(self.sides()):
                whole = jnp.concatenate([self.held[j].ref[i] for i in range(self.count)], axis=1)
                self.buf.ref[pl.ds(pl.multiple_of(start, 16), val.shape[1]), :] = whole


class Product:
    def __init__(self, k, left, right):
        self.left, self.right = left, right
        rows = left.shape[1]
        self.chunk = 384 if rows % 384 == 0 else 256
        self.count = rows // self.chunk
        self.buf = k.vmem((rows, right.shape[1]), BF)
        self.out, self.sem = k.output(self.buf.shape, BF), k.sem(self.count)

    def copy(self, i):
        part = block_of(i, self.chunk)
        return pltpu.make_async_copy(self.buf.ref.at[part], self.out.ref.at[part], self.sem.ref.at[i])

    def run(self):
        def step(i, carry):
            part = block_of(i, self.chunk)
            value = contract(self.left.ref[:, part], self.right.ref[...], 0, 0)
            self.buf.ref[part, :] = value.astype(BF)
            self.copy(i).start()
            return carry

        lax.fori_loop(0, self.count, step, 0)

    def wait(self):
        for i in range(self.count):
            self.copy(i).wait()


def places():
    me = lax.axis_index("tensor")
    sib = me + 1 - 2 * (me % 2)
    cross = (me + 2) % 4
    diag = (sib + 2) % 4
    return me, sib, cross, diag


class Gather:
    def __init__(self, k, x, gain, weights, extras=(), trans=False, epilogue="plain", save=()):
        rows, width = x.shape
        length = 4 * rows
        self.k, self.x, self.gain, self.weights, self.extras = k, x, gain, weights, extras
        self.trans, self.epilogue, self.rows, self.half = trans, epilogue, rows, rows // 2
        cols = [w.buf.shape[0 if trans else 1] for w in weights]
        kinds = {
            "plain": [(c, F32) for c in cols],
            "ffn": [(cols[0], BF)] * 3,
            "ffn_back": [(cols[0], BF)] * 2,
        }[epilogue]
        self.full = k.vmem((length, width), BF)
        self.values = [k.vmem((length, c), kind) for c, kind in kinds]
        kept = [self.full] + self.values
        self.saved = [(v, k.output(v.shape, v.dtype), k.sem(4, 2)) for v in kept if kept.index(v) in save]
        self.sems = [k.sem(2) for _ in range(6)]
        k.late.append(self.end)

    def span(self, owner, sub):
        return pl.ds(pl.multiple_of(owner * self.rows + sub * self.half, self.half), self.half)

    def move(self, kind, i):
        me, sib, cross, _ = places()
        full = self.full.ref
        owner, peer, at = {"cross": (me, cross, 0), "sib": (me, sib, 2), "relay": (cross, sib, 4)}[kind]
        part = full.at[self.span(owner, i)]
        return remote(
            part, part, self.sems[at].ref.at[i], self.sems[at + 1].ref.at[i], {"tensor": peer}
        )

    def begin(self):
        me = places()[0]
        for i in range(2):

            def put(j, carry):
                at = i * self.half + j * STRIP
                part = self.x.ref[pl.ds(pl.multiple_of(at, STRIP), STRIP), :].astype(F32)
                if self.gain is not None:
                    val, row = self.gain
                    part = norm_rows(part, val.ref[row : row + 1, :])
                to = pl.ds(pl.multiple_of(me * self.rows + at, STRIP), STRIP)
                self.full.ref[to, :] = part.astype(BF)
                return carry

            lax.fori_loop(0, self.half // STRIP, put, 0)
            self.move("cross", i).start()
            self.move("sib", i).start()

    def loop(self):
        me, sib, cross, diag = places()
        rows, half = self.rows, self.half
        for w in self.weights:
            w.wait()

        def step(p, carry):
            far, sub = p // 2, p % 2
            near = (1 - sub) * me + sub * sib
            first = (1 - far) * near * rows + far * (cross * rows + sub * half)
            second = (1 - far) * (near * rows + half) + far * (diag * rows + sub * half)
            pair = [pl.ds(pl.multiple_of(v, half), half) for v in (first, second)]

            @pl.when(p == 1)
            def _():
                self.move("sib", 0).wait_recv()
                self.move("sib", 1).wait_recv()

            for i in range(2):

                @pl.when(p == 2 + i)
                def _():
                    self.move("cross", i).wait_recv()
                    self.move("relay", i).start()
                    self.move("relay", i).wait_recv()

            def both(val):
                return jnp.concatenate([val.ref[pair[0], :], val.ref[pair[1], :]], axis=0)

            a = both(self.full)
            prods = [contract(a, w.buf.ref[...], 1, 1 if self.trans else 0) for w in self.weights]
            if self.epilogue == "plain":
                values = prods
            elif self.epilogue == "ffn":
                sig, silu = silu_parts(prods[0])
                values = [prods[0], prods[1], silu * prods[1]]
            else:
                gate, up = (both(v).astype(F32) for v in self.extras)
                sig, silu = silu_parts(gate)
                values = [prods[0] * up * sig * (1.0 + gate * (1.0 - sig)), prods[0] * silu]
            for val, value in zip(self.values, values):
                value = value.astype(val.dtype)
                for j in range(2):
                    val.ref[pair[j], :] = value[j * half : (j + 1) * half]
            for val, out, sem in self.saved:
                for j in range(2):
                    pltpu.make_async_copy(
                        val.ref.at[pair[j]], out.ref.at[pair[j]], sem.ref.at[p, j]
                    ).start()
            return carry

        lax.fori_loop(0, 4, step, 0)

    def end(self):
        for i in range(2):
            for kind in ("cross", "sib", "relay"):
                self.move(kind, i).wait_send()
        part = pl.ds(0, self.half)
        for val, out, sem in self.saved:
            for p in range(4):
                for j in range(2):
                    pltpu.make_async_copy(val.ref.at[part], out.ref.at[part], sem.ref.at[p, j]).wait()


class Scatter:
    def __init__(self, k, operands, weights, resid, back=None, trans=False, low=False):
        rows, width = resid.shape
        half = rows // 2
        self.operands, self.weights, self.resid, self.back = operands, weights, resid, back
        self.trans, self.low, self.rows, self.half = trans, low, rows, half
        self.keep, self.own = k.vmem((2, half, width), F32), k.vmem((rows, width), F32)
        self.to_s, self.from_s, self.to_c, self.from_c = (
            k.vmem((2, half, width), BF) for _ in range(4)
        )
        self.to_o, self.from_o = k.vmem((rows, width), BF), k.vmem((rows, width), BF)
        self.out = k.vmem((rows, width), BF if low else F32)
        self.gain_grad = k.vmem((1, width), F32) if back else None
        self.sems = [k.sem(2) for _ in range(4)] + [k.sem(1) for _ in range(2)]
        k.late.append(self.end)

    def move(self, kind, i=0):
        _, sib, cross, _ = places()
        at, src, dst, peer = {
            "diag": (0, self.to_s, self.from_s, sib),
            "cross": (2, self.to_c, self.from_c, cross),
            "near": (4, self.to_o, self.from_o, sib),
        }[kind]
        src, dst = (src.ref, dst.ref) if kind == "near" else (src.ref.at[i], dst.ref.at[i])
        return remote(
            src, dst, self.sems[at].ref.at[i], self.sems[at + 1].ref.at[i], {"tensor": peer}
        )

    def pass_on(self, i):
        self.move("diag", i).wait_recv()

        def add_rows(at):
            total = self.keep.ref[i, at, :] + self.from_s.ref[i, at, :].astype(F32)
            self.to_c.ref[i, at, :] = total.astype(BF)

        chunked(self.half, add_rows)
        self.move("cross", i).start()

    def loop(self):
        me, sib, cross, diag = places()
        rows, half = self.rows, self.half
        for w in self.weights:
            w.wait()

        def step(p, carry):
            near, sub = p // 2, p % 2
            base = near * ((1 - sub) * sib + sub * me) * rows
            first = base + (1 - near) * (cross * rows + sub * half)
            second = base + near * half + (1 - near) * (diag * rows + sub * half)
            pair = [pl.ds(pl.multiple_of(v, half), half) for v in (first, second)]
            total = None
            for y, w in zip(self.operands, self.weights):
                a = jnp.concatenate([y.ref[pair[0], :], y.ref[pair[1], :]], axis=0)
                prod = contract(a, w.buf.ref[...], 1, 1 if self.trans else 0)
                total = prod if total is None else total + prod

            self.own.ref[...] = total

            @pl.when(p < 2)
            def _():
                def put(at):
                    self.keep.ref[p, at, :] = self.own.ref[at, :]
                    lower = pl.ds(pl.multiple_of(at.start + half, 16), at.size)
                    self.to_s.ref[p, at, :] = self.own.ref[lower, :].astype(BF)

                chunked(half, put)
                self.move("diag", p).start()

            @pl.when(p == 2)
            def _():
                def put(at):
                    self.to_o.ref[at, :] = self.own.ref[at, :].astype(BF)

                chunked(rows, put)
                self.move("near").start()

            @pl.when((p == 1) | (p == 2))
            def _():
                self.pass_on(p - 1)

            return carry

        lax.fori_loop(0, 4, step, 0)

    def finish(self):
        self.move("near").wait_recv()
        if self.back:
            self.gain_grad.ref[...] = jnp.zeros_like(self.gain_grad.ref)
        for i in range(2):
            self.move("cross", i).wait_recv()

            def add_rows(j, carry):
                inner = block_of(j, STRIP)
                part = pl.ds(pl.multiple_of(i * self.half + j * STRIP, STRIP), STRIP)
                total = self.own.ref[part, :] + self.from_o.ref[part, :].astype(F32)
                total = total + self.from_c.ref[i, inner, :].astype(F32)
                resid = self.resid.ref[part, :].astype(F32)
                if self.back:
                    value, (gain, row) = self.back
                    total, gain_grad = norm_back(
                        value.ref[part, :].astype(F32), gain.ref[row : row + 1, :], total
                    )
                    self.gain_grad.ref[...] += gain_grad
                self.out.ref[part, :] = (resid + total).astype(self.out.dtype)
                return carry

            lax.fori_loop(0, self.half // STRIP, add_rows, 0)

    def end(self):
        self.move("near").wait_send()
        for i in range(2):
            self.move("diag", i).wait_send()
            self.move("cross", i).wait_send()


def delayed(values, by):
    if by == 0:
        return values
    row = lax.broadcasted_iota(jnp.int32, values.shape, 0)
    return jnp.where(row < by, 0.0, pltpu.roll(values, by, 0))


def advanced(values, by):
    if by == 0:
        return values
    length = values.shape[0]
    row = lax.broadcasted_iota(jnp.int32, values.shape, 0)
    return jnp.where(row >= length - by, 0.0, pltpu.roll(values, length - by, 0))


CONV_COLS = 128


class Conv:
    def __init__(self, k, projected, value, kernel):
        self.projected, self.value, self.kernel = projected, value, kernel
        self.y = k.vmem(value.shape, BF)

    def parts(self, j):
        channels = self.value.shape[1]
        at = block_of(j, CONV_COLS)
        b_gate = self.projected.ref[:, at]
        c_gate = self.projected.ref[:, block_of(j + channels // CONV_COLS, CONV_COLS)]
        x_value, taps = self.value.ref[:, at], self.kernel.ref[:, at]
        product = b_gate * x_value
        count = taps.shape[0]
        causal = jnp.zeros_like(product)
        for i in range(count):
            causal = causal + taps[i : i + 1] * delayed(product, count - 1 - i)
        return at, b_gate, c_gate, x_value, taps, product, causal

    def run(self):
        def step(j, carry):
            at, _, c_gate, _, _, _, causal = self.parts(j)
            self.y.ref[:, at] = (c_gate * causal).astype(BF)
            return carry

        lax.fori_loop(0, self.value.shape[1] // CONV_COLS, step, 0)


class ConvBack(Conv):
    def __init__(self, k, projected, value, kernel, d_y):
        self.projected, self.value, self.kernel, self.d_y = projected, value, kernel, d_y
        self.d_proj = k.vmem(projected.shape, BF)
        self.d_value = k.vmem(value.shape, BF)
        self.d_kernel = k.vmem(kernel.shape, F32)

    def run(self):
        channels = self.value.shape[1]

        def step(j, carry):
            at, b_gate, c_gate, x_value, taps, product, causal = self.parts(j)
            d_y = self.d_y.ref[:, at]
            d_causal = d_y * c_gate
            count = taps.shape[0]
            d_product = jnp.zeros_like(product)
            for i in range(count):
                by = count - 1 - i
                row = jnp.sum(d_causal * delayed(product, by), axis=0, keepdims=True)
                self.d_kernel.ref[i : i + 1, at] = row
                d_product = d_product + taps[i : i + 1] * advanced(d_causal, by)
            self.d_proj.ref[:, at] = (d_product * x_value).astype(BF)
            upper = block_of(j + channels // CONV_COLS, CONV_COLS)
            self.d_proj.ref[:, upper] = (d_y * causal).astype(BF)
            self.d_value.ref[:, at] = (d_product * b_gate).astype(BF)
            return carry

        lax.fori_loop(0, channels // CONV_COLS, step, 0)


def head_mean(values, head_size):
    width = values.shape[1]
    row = lax.broadcasted_iota(jnp.int32, (width, width), 0) // head_size
    col = lax.broadcasted_iota(jnp.int32, (width, width), 1) // head_size
    group = jnp.where(row == col, 1.0 / head_size, 0.0).astype(F32)
    return lax.dot_general(
        values, group, (((1,), (0,)), ((), ())),
        precision=lax.Precision.HIGHEST, preferred_element_type=F32,
    )


def turn(values, head_size, back):
    width, half = values.shape[1], head_size // 2
    lane = lax.broadcasted_iota(jnp.int32, values.shape, 1) % head_size
    upper = pltpu.roll(values, width - half, 1)
    lower = pltpu.roll(values, half, 1)
    return jnp.where(lane < half, upper, -lower) if back else jnp.where(lane < half, -upper, lower)


def head_norm(values, gain, head_size):
    return values * lax.rsqrt(head_mean(values * values, head_size) + EPS) * gain


def head_norm_back(values, gain, grad_in, head_size):
    row_scale = lax.rsqrt(head_mean(values * values, head_size) + EPS)
    normed = values * row_scale
    gain_grad = jnp.sum(grad_in * normed, axis=0, keepdims=True)
    scaled = grad_in * gain
    return row_scale * (scaled - normed * head_mean(scaled * normed, head_size)), gain_grad


def block_weights(q_rows, keys):
    scores = [contract(q_rows, k_rows, 1, 1) for k_rows in keys]
    query = lax.broadcasted_iota(jnp.int32, scores[-1].shape, 0)
    key = lax.broadcasted_iota(jnp.int32, scores[-1].shape, 1)
    scores[-1] = jnp.where(key <= query, scores[-1], MASKED)
    top = functools.reduce(
        jnp.maximum, [jnp.max(part, axis=1, keepdims=True) for part in scores]
    )
    exps = [jnp.exp(part - top) for part in scores]
    scale = 1.0 / sum(jnp.sum(part, axis=1, keepdims=True) for part in exps)
    return [part * scale for part in exps]


def key_blocks(i):
    blocks = [pl.ds(0, i * ROW_BLOCK)] if i else []
    return blocks + [pl.ds(i * ROW_BLOCK, ROW_BLOCK)]


class Heads:
    def __init__(self, projected, tables, size):
        assert size in (16, 64, 256), size
        self.projected, self.size = projected, size
        self.gain, self.cos, self.sin = (v.buf for v in tables)
        self.loads = tables
        self.length, width = projected.shape
        self.q_cols, self.k_cols = width // 2, width // 4
        self.heads, self.kv_heads = self.q_cols // size, self.k_cols // size
        self.share = self.heads // self.kv_heads

    def per_head(self, k, count, kind):
        return k.vmem((count, self.length, self.size), kind)

    def split(self, val, rows, values):
        for h in range(val.shape[0]):
            val.ref[h, rows, :] = values[:, h * self.size : (h + 1) * self.size]

    def join(self, val, rows):
        return jnp.concatenate([val.ref[h, rows, :] for h in range(val.shape[0])], axis=1)

    def gains(self):
        gain = self.gain.ref[...]
        return (
            jnp.concatenate([gain[0:1]] * self.heads, axis=1),
            jnp.concatenate([gain[1:2]] * self.kv_heads, axis=1),
        )

    def angles(self, rows):
        c, n = self.cos.ref[rows, :], self.sin.ref[rows, :]
        repeat = self.q_cols // c.shape[1]
        return jnp.concatenate([c] * repeat, axis=1), jnp.concatenate([n] * repeat, axis=1)

    def blocks(self, step):
        lax.fori_loop(0, self.length // ROW_BLOCK, lambda p, c: step(block_of(p, ROW_BLOCK)) or c, 0)


class Attend(Heads):
    def __init__(self, k, projected, tables, size):
        super().__init__(projected, tables, size)
        self.q_rot = k.vmem((self.length, self.q_cols), BF)
        self.k_rot = k.vmem((self.length, self.k_cols), BF)
        self.y = k.vmem((self.length, self.q_cols), BF)
        self.q_h, self.y_h = (self.per_head(k, self.heads, BF) for _ in range(2))
        self.k_h, self.v_h = (self.per_head(k, self.kv_heads, BF) for _ in range(2))

    def run(self, *between):
        for load in self.loads:
            load.wait()
        size, q_cols, k_cols, proj = self.size, self.q_cols, self.k_cols, self.projected.ref

        def prepare(rows):
            c, n = self.angles(rows)
            q_gain, k_gain = self.gains()
            q = head_norm(proj[rows, :q_cols], q_gain, size)
            q = (q * c + turn(q, size, False) * n).astype(BF)
            k = head_norm(proj[rows, q_cols : q_cols + k_cols], k_gain, size)
            k = (k * c[:, :k_cols] + turn(k, size, False) * n[:, :k_cols]).astype(BF)
            self.q_rot.ref[rows, :] = q
            self.k_rot.ref[rows, :] = k
            self.split(self.q_h, rows, (q.astype(F32) * size**-0.5).astype(BF))
            self.split(self.k_h, rows, k)
            self.split(self.v_h, rows, proj[rows, q_cols + k_cols :].astype(BF))

        self.blocks(prepare)

        def head(h, carry):
            g = h // self.share

            @pl.when(h == self.heads // 2)
            def _():
                for step in between:
                    step()

            for i in range(self.length // ROW_BLOCK):
                rows, seen = pl.ds(i * ROW_BLOCK, ROW_BLOCK), key_blocks(i)
                weights = block_weights(
                    self.q_h.ref[h, rows, :], [self.k_h.ref[g, at, :] for at in seen]
                )
                value = sum(
                    contract(part.astype(BF), self.v_h.ref[g, at, :], 1, 0)
                    for part, at in zip(weights, seen)
                )
                self.y_h.ref[h, rows, :] = value.astype(BF)
            return carry

        lax.fori_loop(0, self.heads, head, 0)

        def place(rows):
            self.y.ref[rows, :] = self.join(self.y_h, rows)

        self.blocks(place)


class AttendBack(Heads):
    def __init__(self, k, projected, tables, size, q_rot, k_rot, d_y):
        super().__init__(projected, tables, size)
        self.q_rot, self.k_rot, self.d_y = q_rot, k_rot, d_y
        self.q_h, self.dy_h = (self.per_head(k, self.heads, BF) for _ in range(2))
        self.k_h, self.v_h = (self.per_head(k, self.kv_heads, BF) for _ in range(2))
        self.dq_h = self.per_head(k, self.heads, F32)
        self.dk_h, self.dv_h = (self.per_head(k, self.kv_heads, F32) for _ in range(2))
        self.d_proj = k.vmem(projected.shape, BF)
        self.q_gain, self.k_gain = k.vmem((1, self.q_cols), F32), k.vmem((1, self.k_cols), F32)

    def run(self, *between):
        for load in self.loads:
            load.wait()
        size, q_cols, k_cols, proj = self.size, self.q_cols, self.k_cols, self.projected.ref
        scale = size**-0.5
        dq_h, dk_h, dv_h = self.dq_h.ref, self.dk_h.ref, self.dv_h.ref

        def prepare(rows):
            self.split(self.q_h, rows, (self.q_rot.ref[rows, :].astype(F32) * scale).astype(BF))
            self.split(self.dy_h, rows, self.d_y.ref[rows, :].astype(BF))
            self.split(self.k_h, rows, self.k_rot.ref[rows, :])
            self.split(self.v_h, rows, proj[rows, q_cols + k_cols :].astype(BF))

        self.blocks(prepare)

        def clear(rows):
            for val in (dk_h, dv_h):
                val[:, rows, :] = jnp.zeros((self.kv_heads, ROW_BLOCK, size), F32)

        self.blocks(clear)

        def head(h, carry):
            g = h // self.share

            @pl.when(h == self.heads // 2)
            def _():
                for step in between:
                    step()

            for i in range(self.length // ROW_BLOCK):
                rows, seen = pl.ds(i * ROW_BLOCK, ROW_BLOCK), key_blocks(i)
                q, low = self.q_h.ref[h, rows, :], self.dy_h.ref[h, rows, :]
                keys = [self.k_h.ref[g, at, :] for at in seen]
                probs = block_weights(q, keys)
                d_weights = [contract(low, self.v_h.ref[g, at, :], 1, 1) for at in seen]
                inner = sum(
                    jnp.sum(a * b, axis=1, keepdims=True) for a, b in zip(probs, d_weights)
                )
                d_q = 0.0
                for at, k, prob, d_weight in zip(seen, keys, probs, d_weights):
                    dv_h[g, at, :] += contract(prob.astype(BF), low, 0, 0)
                    d_scores = (prob * (d_weight - inner)).astype(BF)
                    d_q = d_q + contract(d_scores, k, 1, 0)
                    dk_h[g, at, :] += contract(d_scores, q, 0, 0)
                dq_h[h, rows, :] = d_q * scale
            return carry

        lax.fori_loop(0, self.heads, head, 0)
        self.q_gain.ref[...] = jnp.zeros_like(self.q_gain.ref)
        self.k_gain.ref[...] = jnp.zeros_like(self.k_gain.ref)

        def finish(rows):
            c, n = self.angles(rows)
            dq, dk, dv = (self.join(v, rows) for v in (self.dq_h, self.dk_h, self.dv_h))
            dq = dq * c + turn(dq * n, size, True)
            dk = dk * c[:, :k_cols] + turn(dk * n[:, :k_cols], size, True)
            q_gain, k_gain = self.gains()
            dq, q_sum = head_norm_back(proj[rows, :q_cols], q_gain, dq, size)
            dk, k_sum = head_norm_back(proj[rows, q_cols : q_cols + k_cols], k_gain, dk, size)
            self.q_gain.ref[...] += q_sum
            self.k_gain.ref[...] += k_sum
            self.d_proj.ref[rows, :q_cols] = dq.astype(BF)
            self.d_proj.ref[rows, q_cols : q_cols + k_cols] = dk.astype(BF)
            self.d_proj.ref[rows, q_cols + k_cols :] = dv.astype(BF)

        self.blocks(finish)


def body(boundary, norm_gain, mix_in, mix_out, w_gate, w_up, w_down, conv_x, conv_kernel, qk_gain):
    first = lax.axis_index("section") == 0
    tensor_index = lax.axis_index("tensor")
    model_width = boundary.shape[3]
    channels = mix_out.shape[1]
    row_shape = boundary.shape[2:]
    length, size = 4 * row_shape[0], qk_gain.shape[1]

    seqs, own_gain = boundary[0], norm_gain[0]
    sh_in, sh_out, sh_gate, sh_up, sh_down = (v[0] for v in (mix_in, mix_out, w_gate, w_up, w_down))

    def gains_of(k, block, other, early=True):
        own, moved = k.input(own_gain), as_val(k, other)
        sources = lambda s, d, t: [(s == block, own.ref), (s == 1 - block, moved.ref)]
        return Load(k, sources, own.shape, F32, early)

    def start_rows(k, slot, other, early=True):
        own, moved = k.input(seqs), as_val(k, other)
        sources = lambda s, d, t: [(s == slot, own.ref.at[slot]), (s == 1 - slot, moved.ref)]
        return Load(k, sources, row_shape, BF, early)

    def wait(*items):
        return [item.wait for item in items]

    k = Kernel(0)
    t_seq = None
    seq_val = k.input(seqs)

    def seq_moves(s, d, t):
        return [([(None, seq_val.ref.at[1 - s])], t_seq.out.ref, {"section": 1 - s})], []

    t_in, t_out, t_up = (x_half(k, v) for v in (sh_in, sh_out, sh_up))
    gate_lo, gate_hi = (Part(sh_gate, i * (sh_gate.shape[0] // 2), sh_gate.shape[0] // 2) for i in range(2))
    down_lo, down_hi = (Part(sh_down, i * (sh_down.shape[0] // 2), sh_down.shape[0] // 2) for i in range(2))
    t_gate0a, t_gate0b = x_half(k, gate_lo, 0), x_move(k, gate_hi, 0)
    t_down0a, t_down0b = x_half(k, down_lo, 0), x_move(k, down_hi, 0)
    t_gate1, t_down1 = x_half(k, sh_gate, 1), x_move(k, sh_down, 1)
    t_seq = Task(k, row_shape, "section", seq_moves, 1)
    t_gain, z_cols = x_move(k, own_gain), z_gather(k, conv_x)
    z_in0, z_out0 = z_gather_half(k, sh_in, t_in.out, 0), z_gather_half(k, sh_out, t_out.out, 0)
    z_gate0a = z_gather_half(k, gate_lo, t_gate0a.out, 0)
    z_gate0b, x_gate0a = z_gather_whole(k, gate_hi, t_gate0b.out, 0), x_move(k, z_gate0a.out)
    z_up0 = z_gather_half(k, sh_up, t_up.out, 0)
    x_cols, x_in0, x_out0 = (x_move(k, v.out) for v in (z_cols, z_in0, z_out0))
    x_load, gain_load = start_rows(k, 0, t_seq.out, False), gains_of(k, 0, t_gain.out, False)
    taps = load_all(k, conv_kernel)
    angles = Angles(k, length, size, 128)
    w_in0, w_cols = Weight(k, "rows", (z_in0.out, x_in0.out)), Weight(k, "conv", (z_cols.out, x_cols.out))
    w_out0 = Weight(k, "cols", (z_out0.out, x_out0.out))
    g0 = Gather(k, x_load.buf, (gain_load.buf, 0), [w_in0, w_cols], save=(0, 1, 2))
    conv = Conv(k, g0.values[0], g0.values[1], taps.buf)
    y0 = Save(k, conv.y)
    s1 = Scatter(k, [conv.y], [w_out0], x_load.buf)
    mid0 = Save(k, s1.out)
    k.do(t_in.send, t_out.send, z_cols.send, t_gate0b.send, t_gate0a.send, t_gate1.send)
    k.do(t_gain.send, t_seq.send)
    k.do(t_in.wait, z_in0.send, t_out.wait, z_out0.send, z_cols.step, z_in0.step, z_out0.step)
    k.do(z_cols.step, z_in0.step, z_out0.step, t_gate0b.wait, z_gate0b.send)
    k.do(t_gate0a.wait, z_gate0a.send)
    k.do(z_cols.wait, x_cols.send, z_in0.wait, x_in0.send, z_out0.wait, x_out0.send, t_up.send)
    k.do(t_gain.wait, gain_load.start, t_seq.wait, x_load.start, gain_load.wait, x_load.wait)
    k.do(g0.begin, z_gate0b.step, z_gate0a.step, angles.run, z_gate0b.step, z_gate0a.step)
    k.do(x_cols.wait, w_cols.start, x_in0.wait, w_in0.start, z_gate0a.wait, x_gate0a.send)
    k.do(t_down0b.send, t_down0a.send, t_down1.send, t_up.wait, z_up0.send)
    k.do(g0.loop, z_up0.step, taps.wait, conv.run, y0.start)
    k.do(x_out0.wait, w_out0.start, s1.loop, z_up0.step, s1.finish, mid0.start)
    k.do(*wait(t_gate1, t_down0a, t_down0b, t_down1, z_gate0b, x_gate0a, z_up0))
    k.build()
    a0, proj0, value0 = (out for _, out, _ in g0.saved)
    table_arrays = [qk_gain] + [v.out for v in angles.saves]
    y0, mid0 = y0.out, mid0.out

    k = Kernel(1)
    x_up0, z_gate1 = x_move(k, z_up0.out), z_gather_half(k, sh_gate, t_gate1.out, 1)
    z_down0a = z_gather_half(k, down_lo, t_down0a.out, 0)
    z_down0b = z_gather_whole(k, down_hi, t_down0b.out, 0)
    z_in1, z_out1 = z_gather_half(k, sh_in, t_in.out, 1), z_gather_half(k, sh_out, t_out.out, 1)
    x_down0a, x_in1, x_out1 = (x_move(k, v.out) for v in (z_down0a, z_in1, z_out1))
    rows, gain_load = load_all(k, mid0), gains_of(k, 0, t_gain.out)
    w_gate0 = Weight(k, "rows", (z_gate0a.out, x_gate0a.out), (z_gate0b.out, None), early=True)
    w_up0 = Weight(k, "rows", (z_up0.out, x_up0.out))
    w_down0 = Weight(k, "cols", (z_down0a.out, x_down0a.out), (z_down0b.out, None))
    g2 = Gather(
        k, rows.buf, (gain_load.buf, 1), [w_gate0, w_up0], epilogue="ffn", save=(0, 1, 2, 3)
    )
    s3 = Scatter(k, [g2.values[2]], [w_down0], rows.buf, low=True)
    z_rows = Save(k, s3.out)
    k.do(x_up0.send, z_down0a.send, z_down0b.send, rows.wait, gain_load.wait, g2.begin)
    k.do(z_in1.send, z_out1.send, z_down0a.step, z_in1.step, z_out1.step, z_down0b.step)
    k.do(z_down0a.step, z_in1.step, z_out1.step, z_gate1.send, z_down0a.wait, x_down0a.send)
    k.do(x_up0.wait, w_up0.start, z_down0b.step, g2.loop, z_gate1.step)
    k.do(z_in1.wait, x_in1.send, z_out1.wait, x_out1.send, z_down0b.wait, x_down0a.wait)
    k.do(w_down0.start, s3.loop, z_gate1.step, s3.finish, z_rows.start)
    k.do(*wait(x_in1, x_out1, z_gate1))
    k.build()
    m0, gate0, up0, hid0 = (out for _, out, _ in g2.saved)
    z_rows = z_rows.out

    k = Kernel(2)
    x_gate1, z_up1 = x_move(k, z_gate1.out), z_gather_half(k, sh_up, t_up.out, 1)
    z_down1a, z_down1b = (z_gather_whole(k, sh_down, t_down1.out, 1, i) for i in range(2))
    x_up1 = x_move(k, z_up1.out)
    rows, gain_load = load_all(k, z_rows), gains_of(k, 1, t_gain.out)
    tables = [load_all(k, v) for v in table_arrays]
    w_in1 = Weight(k, "rows", (z_in1.out, x_in1.out), early=True)
    w_out1 = Weight(k, "cols", (z_out1.out, x_out1.out), early=True)
    g4 = Gather(k, rows.buf, (gain_load.buf, 0), [w_in1], save=(0, 1))
    attend = Attend(k, g4.values[0], tables, size)
    kept = [Save(k, v) for v in (attend.q_rot, attend.k_rot, attend.y)]
    s5 = Scatter(k, [attend.y], [w_out1], rows.buf)
    mid1 = Save(k, s5.out)
    k.do(x_gate1.send, z_up1.send, rows.wait, gain_load.wait, g4.begin, z_up1.step)
    k.do(z_down1a.send, g4.loop, z_up1.step, z_down1b.send)
    k.do(lambda: attend.run(z_up1.wait, x_up1.send, z_down1a.step))
    k.do(*(v.start for v in kept))
    k.do(z_down1b.step, s5.loop, z_down1a.step, z_down1b.step, s5.finish, mid1.start)
    k.do(*wait(x_gate1, x_up1, z_down1a, z_down1b))
    k.build()
    a1, proj1 = (out for _, out, _ in g4.saved)
    q_rot, k_rot, y1 = (v.out for v in kept)
    mid1 = mid1.out

    k = Kernel(3)
    rows, gain_load = load_all(k, mid1), gains_of(k, 1, t_gain.out)
    cot = start_rows(k, 1, t_seq.out)
    w_gate1 = Weight(k, "rows", (z_gate1.out, x_gate1.out), early=True)
    w_up1 = Weight(k, "rows", (z_up1.out, x_up1.out), early=True)
    w_down1 = Weight(k, "cols", (z_down1a.out, None), (z_down1b.out, None), early=True)
    g6 = Gather(k, rows.buf, (gain_load.buf, 1), [w_gate1, w_up1], epilogue="ffn")
    g8 = Gather(
        k, cot.buf, None, [w_down1], [g6.values[0], g6.values[1]], trans=True, epilogue="ffn_back"
    )
    p_down1 = Product(k, g6.values[2], g8.full)
    p_gate1, p_up1 = Product(k, g6.full, g8.values[0]), Product(k, g6.full, g8.values[1])
    s9 = Scatter(k, g8.values, [w_gate1, w_up1], cot.buf, (rows.buf, (gain_load.buf, 1)), True)
    hid1 = Save(k, g6.values[2])
    d_mid1, gain11 = Save(k, s9.out), Save(k, s9.gain_grad)
    k.do(rows.wait, gain_load.wait, g6.begin, cot.wait, g8.begin, g6.loop, hid1.start, g8.loop)
    k.do(s9.loop, p_down1.run, p_gate1.run, p_up1.run)
    k.do(s9.finish, d_mid1.start, gain11.start, p_down1.wait, p_gate1.wait, p_up1.wait)
    k.build()
    hid1, d_mid1, gain11 = hid1.out, d_mid1.out, gain11.out

    k = Kernel(4)
    r_down1 = x_half(k, p_down1.out)
    r_gate1, q_up1 = x_slots(k, p_gate1.out, "rows"), sum_scatter(k, "rows", p_up1.out)
    rows, gain_load = load_all(k, d_mid1), gains_of(k, 1, t_gain.out)
    value = load_all(k, z_rows)
    tables = [load_all(k, v) for v in table_arrays]
    proj, q_load, k_load, y_load, a_load = (load_all(k, v) for v in (proj1, q_rot, k_rot, y1, a1))
    w_in1 = Weight(k, "rows", (z_in1.out, x_in1.out), early=True)
    w_out1 = Weight(k, "cols", (z_out1.out, x_out1.out), early=True)
    g10 = Gather(k, rows.buf, None, [w_out1], trans=True)
    p_out1 = Product(k, y_load.buf, g10.full)
    back = AttendBack(k, proj.buf, tables, size, q_load.buf, k_load.buf, g10.values[0])
    p_in1 = Product(k, a_load.buf, back.d_proj)
    r_out1 = x_half(k, p_out1.out)
    s11 = Scatter(
        k, [back.d_proj], [w_in1], rows.buf, (value.buf, (gain_load.buf, 0)), True, low=True
    )
    d_z, gain10 = Save(k, s11.out), Save(k, s11.gain_grad)
    head_gains = [Save(k, back.q_gain), Save(k, back.k_gain)]
    k.early.append(q_up1.load)
    k.do(r_down1.send, r_gate1.send, rows.wait, g10.begin, q_up1.send, g10.loop)
    k.do(y_load.wait, p_out1.run, q_up1.step, p_out1.wait, r_out1.send)
    k.do(proj.wait, q_load.wait, k_load.wait, lambda: back.run(q_up1.step))
    k.do(*(v.start for v in head_gains))
    k.do(gain_load.wait, value.wait, s11.loop, a_load.wait, p_in1.run)
    k.do(s11.finish, d_z.start, gain10.start, p_in1.wait)
    k.do(*wait(r_down1, q_up1, r_gate1, r_out1))
    k.build()
    d_z, gain10 = d_z.out, gain10.out
    q_gain, k_gain = (v.out for v in head_gains)

    k = Kernel(5)
    q_gate1, m_up1 = sum_scatter(k, "rows", p_gate1.out, r_gate1.out), x_move(k, q_up1.out, 0)
    q_out1 = sum_scatter(k, "cols", p_out1.out, r_out1.out)
    r_in1 = x_slots(k, p_in1.out, "rows")
    q_in1 = sum_scatter(k, "rows", p_in1.out, r_in1.out)
    q_down1 = sum_scatter(k, "cols", p_down1.out, r_down1.out)
    rows, value, gain_load = load_all(k, d_z), load_all(k, mid0), gains_of(k, 0, t_gain.out)
    gate_load, up_load, hid_load, m_load = (load_all(k, v) for v in (gate0, up0, hid0, m0))
    w_gate0 = Weight(k, "rows", (z_gate0a.out, x_gate0a.out), (z_gate0b.out, None), early=True)
    w_up0 = Weight(k, "rows", (z_up0.out, x_up0.out), early=True)
    w_down0 = Weight(k, "cols", (z_down0a.out, x_down0a.out), (z_down0b.out, None), early=True)
    g12 = Gather(
        k, rows.buf, None, [w_down0], [gate_load.buf, up_load.buf], trans=True, epilogue="ffn_back"
    )
    p_down0 = Product(k, hid_load.buf, g12.full)
    p_gate0, p_up0 = Product(k, m_load.buf, g12.values[0]), Product(k, m_load.buf, g12.values[1])
    r_down0 = x_half(k, p_down0.out)
    s13 = Scatter(
        k, g12.values, [w_gate0, w_up0], rows.buf, (value.buf, (gain_load.buf, 1)), True
    )
    d_mid0, gain01 = Save(k, s13.out), Save(k, s13.gain_grad)
    k.early += [q_gate1.load, q_down1.load, q_out1.load]
    k.do(r_in1.send, m_up1.send, rows.wait, g12.begin, q_gate1.send, q_down1.send, q_out1.send)
    k.do(gate_load.wait, up_load.wait, g12.loop, q_gate1.step, q_down1.step, q_out1.step)
    k.do(hid_load.wait, p_down0.run, p_down0.wait, r_down0.send, r_in1.wait, q_in1.add)
    k.do(s13.loop, q_gate1.step, q_down1.step, q_out1.step)
    k.do(m_load.wait, p_gate0.run, q_in1.step, p_up0.run, value.wait, gain_load.wait)
    k.do(s13.finish, d_mid0.start, gain01.start, q_in1.step, p_gate0.wait, p_up0.wait)
    k.do(*wait(q_gate1, q_out1, q_in1, q_down1, m_up1, r_down0))
    k.build()
    d_mid0, gain01 = d_mid0.out, gain01.out

    k = Kernel(6)
    r_gate0 = x_slots(k, p_gate0.out, "rows")
    q_gate0 = sum_scatter(k, "rows", p_gate0.out, r_gate0.out)
    q_down0 = sum_scatter(k, "cols", p_down0.out, r_down0.out)
    q_up0 = sum_scatter(k, "rows", p_up0.out)
    m_up0 = x_move(k, q_up0.out, 1)
    e_down1 = Finish(k, q_down1.out, 1)
    e_gate1, e_out1, e_in1 = (Finish(k, v.out, 1) for v in (q_gate1, q_out1, q_in1))
    rows, gain_load = load_all(k, d_mid0), gains_of(k, 0, t_gain.out)
    x_load, taps = start_rows(k, 0, t_seq.out), load_all(k, conv_kernel)
    y_load, a_load, proj, value = (load_all(k, v) for v in (y0, a0, proj0, value0))
    w_in0 = Weight(k, "rows", (z_in0.out, x_in0.out), early=True)
    w_cols = Weight(k, "conv", (z_cols.out, x_cols.out), early=True)
    w_out0 = Weight(k, "cols", (z_out0.out, x_out0.out), early=True)
    g14 = Gather(k, rows.buf, None, [w_out0], trans=True)
    p_out0 = Product(k, y_load.buf, g14.full)
    back = ConvBack(k, proj.buf, value.buf, taps.buf, g14.values[0])
    p_in0, p_cols = Product(k, a_load.buf, back.d_proj), Product(k, a_load.buf, back.d_value)
    r_out0, r_in0 = x_half(k, p_out0.out), x_slots(k, p_in0.out, "rows")
    r_cols = x_slots(k, p_cols.out, "conv")
    q_out0, q_in0 = sum_scatter(k, "cols", p_out0.out, r_out0.out), sum_scatter(k, "rows", p_in0.out, r_in0.out)
    q_cols = sum_scatter(k, "conv", p_cols.out, r_cols.out)
    e_down0, e_gate0, e_out0, e_in0 = (
        Finish(k, v.out, 0) for v in (q_down0, q_gate0, q_out0, q_in0)
    )
    s15 = Scatter(
        k, [back.d_proj, back.d_value], [w_in0, w_cols], rows.buf,
        (x_load.buf, (gain_load.buf, 0)), True, low=True,
    )
    d_x = Save(k, s15.out)
    tap_rows = conv_kernel.shape[0]
    small = k.vmem((8, model_width), F32)
    small_out = Save(k, small)
    ready = [load_all(k, v) for v in (gain01, gain10, gain11)]
    head_loads = [load_all(k, v) for v in (q_gain, k_gain)]

    def fill_small():
        t = lax.axis_index("tensor")
        small.ref[...] = jnp.zeros_like(small.ref)
        small.ref[0:1, :] = s15.gain_grad.ref[...]
        for i, load in enumerate(ready):
            load.wait()
            small.ref[i + 1 : i + 2, :] = load.buf.ref[...]
        small.ref[4 : 4 + tap_rows, block_of(t, channels)] = back.d_kernel.ref[...]
        at = 0
        for load in head_loads:
            load.wait()
            width = load.buf.shape[1]
            small.ref[7:8, at : at + width] = load.buf.ref[...]
            at += width
        small_out.start()

    t_small = x_move(k, small_out.out)
    z_small = SumShare(k, [small_out.out, t_small.out], "dp")
    t_total = SumShare(k, [z_small.out], "tensor", slotted=True)
    hid_load, mid_load = load_all(k, hid1), load_all(k, mid1)
    w_down1 = Weight(k, "cols", (z_down1a.out, None), (z_down1b.out, None), early=True)
    s7 = Scatter(k, [hid_load.buf], [w_down1], mid_load.buf, low=True)
    y_rows = Save(k, s7.out)
    t_x, t_y = x_move(k, d_x.out, 1), x_move(k, y_rows.out, 0)
    k.early += [q_up0.load, q_down0.load]
    k.early += [v.load for v in (e_down1, e_gate1, e_out1, e_in1)]
    k.do(r_gate0.send, q_up0.send, rows.wait, g14.begin, q_down0.send)
    k.do(e_down1.send, e_gate1.send, e_out1.send, e_in1.send, g14.loop)
    k.do(y_load.wait, p_out0.run, p_out0.wait, r_out0.send, q_up0.step)
    k.do(proj.wait, value.wait, taps.wait, back.run, q_down0.step, a_load.wait)
    k.do(p_in0.run, p_cols.run, p_in0.wait, r_in0.send, p_cols.wait, r_cols.send)
    k.do(r_gate0.wait, q_gate0.add, x_load.wait, gain_load.wait, s15.loop, q_up0.step)
    k.do(q_down0.step, s15.finish, d_x.start, fill_small, d_x.wait, t_x.send)
    k.do(small_out.wait, t_small.send, q_gate0.step, hid_load.wait, mid_load.wait, s7.loop)
    k.do(r_out0.wait, q_out0.add, r_in0.wait, q_in0.add)
    k.do(r_cols.wait, q_cols.add, q_up0.wait, m_up0.send, q_down0.wait, e_down0.add)
    k.do(s7.finish, y_rows.start, y_rows.wait, t_y.send)
    k.do(q_gate0.step, q_out0.step, q_in0.step, q_cols.step, t_small.wait, z_small.add)
    k.do(q_gate0.wait, e_gate0.add, q_out0.step, q_in0.step, q_cols.step)
    k.do(z_small.wait, t_total.add, q_out0.wait, e_out0.add, q_in0.wait, e_in0.add)
    rest = (e_down1, e_gate1, e_out1, e_in1, q_cols, e_down0, e_gate0, m_up0, e_out0, e_in0)
    k.do(*wait(*rest, t_total, t_x, t_y))
    k.build()

    owned = [
        ([e_in0], [e_in1], 1),
        ([e_out0], [e_out1], 1),
        ([e_gate0], [e_gate1], 1),
        ([q_up0, m_up0], [q_up1, m_up1], 1),
        ([e_down0], [e_down1], 1),
        ([q_cols], [q_cols], 0),
    ]
    return pack(
        [(zero, one, lead) for zero, one, lead in owned], t_total, d_x.out, y_rows.out, t_x, t_y,
        (norm_gain.shape, conv_kernel.shape, qk_gain.shape),
    )


def slot_free(val, shape):
    value = val.out.array
    if value.ndim == 3 and value.shape[0] * value.shape[1] != shape[0]:
        value = jnp.sum(value.astype(F32), axis=0).astype(BF)
    return value.reshape(shape)


def pack_kernel(plan, *refs):
    n_in, leads, terms, tap_rows = plan
    ins, rest = refs[:n_in], refs[n_in:]
    result, gain_out, *grads, cols, taps, heads = rest[: len(leads) + 4]
    grads = [*grads, cols]
    room = iter(rest[len(leads) + 4 :])
    own_v, moved_v, small_v, *bufs = (next(room) for _ in range(3 + len(terms)))
    out_v = [next(room) for _ in leads]
    load_sem, store_sem = room
    s, t = lax.axis_index("section"), lax.axis_index("tensor")
    small, d_x, y_rows, moved, moved_y, *parts = ins

    def either(cond, zero, one, dst, sem):
        if zero is not None:
            pl.when(cond)(pltpu.make_async_copy(zero, dst, sem).start)
        if one is not None:
            pl.when(jnp.logical_not(cond))(pltpu.make_async_copy(one, dst, sem).start)

    first = s == 0
    either(first, d_x, y_rows, own_v, load_sem.at[0])
    either(first, moved, moved_y, moved_v, load_sem.at[1])
    pltpu.make_async_copy(small, small_v, load_sem.at[2]).start()
    for j, (zero, one, _) in enumerate(terms):
        either(
            first,
            None if zero is None else parts[zero],
            None if one is None else parts[one],
            bufs[j],
            load_sem.at[3 + j],
        )
    for j, (zero, one, i) in enumerate(terms):
        arrive = pltpu.make_async_copy(parts[one if zero is None else zero], bufs[j], load_sem.at[3 + j])
        begins = j == 0 or terms[j - 1][2] != i

        def put(j=j, i=i, begins=begins):
            def add_rows(at):
                value = bufs[j][at, :].astype(F32)
                out_v[i][at, :] = value if begins else out_v[i][at, :] + value

            chunked(bufs[j].shape[0], add_rows)

        if zero is None or one is None:
            cond = first if one is None else jnp.logical_not(first)

            @pl.when(cond)
            def _(arrive=arrive, put=put):
                arrive.wait()
                put()
        else:
            arrive.wait()
            put()
        if j + 1 == len(terms) or terms[j + 1][2] != i:
            dst = grads[i].at[0] if leads[i] else grads[i]
            pltpu.make_async_copy(out_v[i], dst, store_sem.at[i]).start()
    pltpu.make_async_copy(d_x, own_v, load_sem.at[0]).wait()
    pltpu.make_async_copy(moved, moved_v, load_sem.at[1]).wait()
    n = len(leads)
    stores = [
        pltpu.make_async_copy(own_v, result.at[0, s], store_sem.at[n]),
        pltpu.make_async_copy(moved_v, result.at[0, 1 - s], store_sem.at[n + 1]),
    ]
    for store in stores:
        store.start()
    pltpu.make_async_copy(small, small_v, load_sem.at[2]).wait()
    total = small_v[0]
    for i in range(1, small_v.shape[0]):
        total = total + small_v[i]
    gain_out[0] = jnp.where(first, total[0:2], total[2:4])
    channels, size = taps.shape[1], heads.shape[1]
    chosen = total[4 : 4 + tap_rows, 0:channels]
    for i in range(1, total.shape[1] // channels):
        chosen = jnp.where(t == i, total[4 : 4 + tap_rows, i * channels : (i + 1) * channels], chosen)
    taps[...] = chosen
    at = 0
    for row, width in enumerate((channels, channels // 2)):
        value = total[7:8, at : at + size]
        for i in range(1, width // size):
            value = value + total[7:8, at + i * size : at + (i + 1) * size]
        heads[row : row + 1, :] = value
        at += width
    for i, store in enumerate(leads):
        dst = grads[i].at[0] if store else grads[i]
        pltpu.make_async_copy(out_v[i], dst, store_sem.at[i]).wait()
    for store in stores:
        store.wait()


def pack(owned, small, d_x, y_rows, moved_x, moved_y, shapes):
    gain_shape, tap_shape, head_shape = shapes
    parts, terms, leads, out_shapes = [], [], [], []
    for i, (zero, one, lead) in enumerate(owned):
        whole = zero[0].out.shape
        if lead and len(whole) == 3 and isinstance(zero[0], Finish):
            shape = (whole[0] * whole[1], whole[2])
        else:
            shape = whole[-2:]
        shape = tuple(shape)
        leads.append(lead)
        out_shapes.append(shape)
        for j in range(max(len(zero), len(one))):
            pair = []
            for side in (zero, one):
                if j < len(side):
                    parts.append(slot_free(side[j], shape))
                    pair.append(len(parts) - 1)
                else:
                    pair.append(None)
            terms.append((*pair, i))
    operands = [v.array for v in (small.out, d_x, y_rows, moved_x.out, moved_y.out)] + parts
    rows = d_x.shape
    smem = pl.BlockSpec(memory_space=pltpu.VMEM)
    out_shape = [jax.ShapeDtypeStruct((1, 2) + rows, BF), jax.ShapeDtypeStruct(gain_shape, F32)]
    out_shape += [
        jax.ShapeDtypeStruct((1,) + v if lead else v, F32) for v, lead in zip(out_shapes, leads)
    ]
    out_shape += [jax.ShapeDtypeStruct(v, F32) for v in (tap_shape, head_shape)]
    n = len(leads)
    return tuple(
        pl.pallas_call(
            functools.partial(
                pack_kernel, (len(operands), tuple(leads), tuple(terms), tap_shape[0])
            ),
            out_shape=out_shape,
            in_specs=[ANY] * len(operands),
            out_specs=[ANY, smem] + [ANY] * n + [smem] * 2,
            scratch_shapes=[pltpu.VMEM(rows, BF)] * 2
            + [pltpu.VMEM(small.out.shape, F32)]
            + [pltpu.VMEM(out_shapes[i], BF) for _, _, i in terms]
            + [pltpu.VMEM(v, F32) for v in out_shapes]
            + [DMA((3 + len(terms),)), DMA((n + 2,))],
            compiler_params=pltpu.CompilerParams(vmem_limit_bytes=VMEM_BYTES),
            name="pack",
        )(*operands)
    )


def solution(mesh):
    in_specs = (
        P("section", "dp", "tensor", None),
        P("section", None, None),
        P("section", "dp", "tensor"),
        P("section", "tensor", "dp"),
        P("section", "dp", "tensor"),
        P("section", "dp", "tensor"),
        P("section", "tensor", "dp"),
        P(("section", "dp"), "tensor"),
        P(None, "tensor"),
        P(),
    )
    out_specs = (
        P("section", "dp", "tensor", None),
        P("section", None, None),
        P("section", "dp", "tensor"),
        P("section", "tensor", "dp"),
        P("section", "dp", "tensor"),
        P("section", "dp", "tensor"),
        P("section", "tensor", "dp"),
        P(("section", "dp"), "tensor"),
        P(None, "tensor"),
        P(),
    )
    return jax.shard_map(body, mesh=mesh, in_specs=in_specs, out_specs=out_specs, check_vma=False)
```

```python
import functools

import jax
import jax.numpy as jnp
from jax import lax
from jax.experimental import pallas as pl
from jax.experimental.pallas import tpu as pltpu
from jax.sharding import PartitionSpec as P

HEADS = 16
KV_HEADS = 8

EPS = 1e-05
ROPE_BASE = 1000000.0
MASKED = -1e30

MESH = pl.DeviceIdType.MESH
ANY = pl.BlockSpec(memory_space=pl.ANY)
DMA = pltpu.SemaphoreType.DMA
VMEM_BYTES = 63 * 1024 * 1024
BF = jnp.bfloat16
F32 = jnp.float32
ROW_BLOCK = 256
STRIP = 32


def contract(left_op, right_op, left_dim, right_dim):
    return lax.dot_general(
        left_op, right_op, (((left_dim,), (right_dim,)), ((), ())), preferred_element_type=F32
    )


def norm_rows(values, gain):
    return values * lax.rsqrt(jnp.mean(values * values, axis=-1, keepdims=True) + EPS) * gain


def norm_back(values, gain, grad_in):
    row_scale = lax.rsqrt(jnp.mean(values * values, axis=-1, keepdims=True) + EPS)
    normed = values * row_scale
    gain_grad = jnp.sum(grad_in * normed, axis=0, keepdims=True)
    scaled = grad_in * gain
    value_grad = row_scale * (scaled - normed * jnp.mean(scaled * normed, axis=-1, keepdims=True))
    return (value_grad, gain_grad)


class Angles:
    def __init__(self, k, length, head_size, width):
        self.half = head_size // 2
        self.tables = [k.vmem((length, width), F32) for _ in range(2)]
        self.saves = [Save(k, v) for v in self.tables]

    def run(self):
        cos, sin = self.tables
        shape = (ROW_BLOCK, cos.shape[1])
        column = (lax.broadcasted_iota(jnp.int32, shape, 1) % self.half).astype(F32)
        frequency = ROPE_BASE ** (-(column / self.half))
        row = lax.broadcasted_iota(jnp.int32, shape, 0)

        def step(i, carry):
            rows = block_of(i, ROW_BLOCK)
            angle = (row + i * ROW_BLOCK).astype(F32) * frequency
            cos.ref[rows, :] = jnp.cos(angle)
            sin.ref[rows, :] = jnp.sin(angle)
            return carry

        lax.fori_loop(0, cos.shape[0] // ROW_BLOCK, step, 0)
        for save in self.saves:
            save.start()


def silu_parts(gate):
    sig = 1.0 / (1.0 + jnp.exp(-gate))
    return sig, gate * sig


def chunked(rows, step):
    size = next((n for n in (32, 16) if rows % n == 0), rows)
    if size == rows:
        step(pl.ds(0, rows))
    else:
        lax.fori_loop(0, rows // size, lambda i, c: step(block_of(i, size)) or c, 0)


def dp_size():
    return lax.axis_size("dp")


def spot():
    return tuple(lax.axis_index(a) for a in ("section", "dp", "tensor"))


def block_of(index, size):
    return pl.ds(pl.multiple_of(index * size, size), size)


class Val:
    def __init__(self, shape, dtype):
        self.shape, self.dtype = tuple(shape), dtype
        self.ref = self.array = None


class Kernel:
    def __init__(self, cid):
        self.cid, self.ins, self.arrays, self.outs, self.room = cid, [], [], [], []
        self.early, self.steps, self.late, self.axes = [], [], [], set()
        self.once = []

    def input(self, array):
        array = array.array if isinstance(array, Val) else array
        for val, known in zip(self.ins, self.arrays):
            if known is array:
                return val
        val = Val(array.shape, array.dtype)
        self.ins.append(val)
        self.arrays.append(array)
        return val

    def output(self, shape, dtype):
        val = Val(shape, dtype)
        self.outs.append(val)
        return val

    def vmem(self, shape, dtype):
        val = Val(shape, dtype)
        self.room.append((val, pltpu.VMEM(tuple(shape), dtype)))
        return val

    def sem(self, *shape):
        val = Val(shape, None)
        self.room.append((val, DMA(shape)))
        return val

    def do(self, *steps):
        self.steps += steps

    def body(self, *refs):
        vals = self.ins + self.outs + [val for val, _ in self.room]
        for val, ref in zip(vals, refs):
            val.ref = ref
        for item in self.once:
            item.waited = False
            item.phase = 0
        for step in self.early:
            step()
        self.greet()
        for step in self.steps + self.late:
            step()

    def greet(self):
        s, d, t = spot()
        _, sib, cross, diag = places()
        barrier = pltpu.get_barrier_semaphore()
        peers = [{"tensor": sib}, {"tensor": cross}]
        if "tensor" in self.axes:
            peers.append({"tensor": diag})
        if "section" in self.axes:
            peers.append({"section": 1 - s})
        if "dp" in self.axes:
            peers += [{"dp": (d + i) % dp_size()} for i in range(1, dp_size())]

        def signal(peer):
            pl.semaphore_signal(barrier, inc=1, device_id=peer, device_id_type=MESH)

        for peer in peers:
            signal(peer)
        expected = len(peers)
        if "line" in self.axes and "dp" not in self.axes:
            pl.when(d < 3)(lambda: signal({"dp": (d + 1) % 4}))
            pl.when(d > 0)(lambda: signal({"dp": (d + 3) % 4}))
            expected = expected + (d + 2) // 3 + (5 - d) // 3
        pl.semaphore_wait(barrier, expected)

    def build(self):
        result = pl.pallas_call(
            self.body,
            out_shape=[jax.ShapeDtypeStruct(v.shape, v.dtype) for v in self.outs],
            in_specs=[ANY] * len(self.ins),
            out_specs=[ANY] * len(self.outs),
            scratch_shapes=[room for _, room in self.room],
            compiler_params=pltpu.CompilerParams(
                collective_id=self.cid, has_side_effects=True, vmem_limit_bytes=VMEM_BYTES
            ),
            name=f"stage{self.cid}",
        )(*self.arrays)
        for val, array in zip(self.outs, result):
            val.array = array


def remote(src, dst, send_sem, recv_sem, peer):
    return pltpu.make_async_remote_copy(
        src_ref=src, dst_ref=dst, send_sem=send_sem, recv_sem=recv_sem,
        device_id=peer, device_id_type=MESH,
    )


class Load:
    def __init__(self, k, sources, shape, dtype, early=False):
        self.k, self.sources, self.waited = k, sources, False
        self.buf, self.sem = k.vmem(shape, dtype), k.sem(1)
        k.once.append(self)
        if early:
            k.early.append(self.start)

    def moves(self):
        for cond, source in self.sources(*spot()):
            yield cond, pltpu.make_async_copy(source, self.buf.ref, self.sem.ref.at[0])

    def start(self):
        for cond, move in self.moves():
            if cond is None:
                move.start()
            else:
                pl.when(cond)(move.start)

    def wait(self):
        if not self.waited:
            self.waited = True
            next(self.moves())[1].wait()


def load_all(k, array, early=True):
    val = k.input(array)
    return Load(k, lambda s, d, t: [(None, val.ref)], val.shape, val.dtype, early)


class Save:
    def __init__(self, k, buf):
        self.buf, self.out, self.sem = buf, k.output(buf.shape, buf.dtype), k.sem(1)
        self.waited = False
        k.once.append(self)
        k.late.append(self.wait)

    def move(self):
        return pltpu.make_async_copy(self.buf.ref, self.out.ref, self.sem.ref.at[0])

    def start(self):
        self.move().start()

    def wait(self):
        if not self.waited:
            self.waited = True
            self.move().wait()


class Task:
    final = None

    def __init__(self, k, out, axis, moves, count, n_local=1, out_dtype=BF):
        self.k, self.axis, self.make = k, axis, moves
        self.out = k.output(out, out_dtype)
        self.send_sem, self.recv_sem, self.local_sem = k.sem(count), k.sem(count), k.sem(n_local)
        self.waited = False
        k.axes.add(axis)
        k.once.append(self)

    def local(self, src, dst, i):
        return pltpu.make_async_copy(src, dst, self.local_sem.ref.at[i])

    def pairs(self, every):
        far, near = self.make(*spot())
        for i, (sources, dst, peer) in enumerate(far):
            for cond, src in sources if every else sources[:1]:
                yield cond, True, remote(
                    src, dst, self.send_sem.ref.at[i], self.recv_sem.ref.at[i], peer
                )
        for i, (sources, dst) in enumerate(near):
            for cond, src in sources if every else sources[:1]:
                yield cond, False, self.local(src, dst, i)

    def step(self):
        pass

    def send(self):
        for cond, far, move in self.pairs(True):
            if far and self.final is not None:
                cond = lax.axis_index("section") == 1 - self.final
            if cond is None:
                move.start()
            else:
                pl.when(cond)(move.start)

    def wait(self):
        if self.waited:
            return
        self.waited = True
        s = lax.axis_index("section")
        for _, far, move in self.pairs(False):
            if not far:
                move.wait()
            elif self.final is None:
                move.wait_recv()
                move.wait_send()
            else:
                pl.when(s == 1 - self.final)(move.wait_send)
                pl.when(s == self.final)(move.wait_recv)


class Part:
    def __init__(self, base, start, rows):
        self.base, self.start, self.rows = base, start, rows
        self.shape, self.dtype = (rows,) + tuple(base.shape[1:]), base.dtype
        self.array = None

    @property
    def ref(self):
        return self.base.ref.at[pl.ds(self.start, self.rows)]


def as_val(k, value):
    if isinstance(value, Part):
        return Part(as_val(k, value.base), value.start, value.rows)
    value = value.out if isinstance(value, Task) else value
    known = isinstance(value, Val) and (value.array is None)
    return value if known else k.input(value)


class Line(Task):
    def __init__(self, k, out, out_dtype=BF, n_local=1):
        super().__init__(k, out, "line", None, 6, n_local, out_dtype)
        self.send_sem, self.recv_sem = k.sem(2, 3), k.sem(2, 3)
        self.phase = 0

    def hop(self, j, way, src, dst):
        d = lax.axis_index("dp")
        peer = {"dp": (d + 1 if way == 0 else d + 3) % 4}
        return remote(src, dst, self.send_sem.ref.at[way, j], self.recv_sem.ref.at[way, j], peer)


class LineGather(Line):
    def __init__(self, k, sources, shape, dtype):
        super().__init__(k, (4,) + shape, dtype)
        self.sources = sources

    def ends(self, j, way):
        d = lax.axis_index("dp")
        if way == 0:
            return (d >= j) & (d < 3), d >= j + 1
        return (d <= 3 - j) & (d > 0), d <= 2 - j

    def copy(self, j, way, src=None):
        d = lax.axis_index("dp")
        slot = (d + 4 - j if way == 0 else d + j) % 4
        piece = self.out.ref.at[slot]
        return self.hop(j, way, piece if src is None else src, piece)

    def send(self):
        self.phase = 0
        for cond, src in self.sources(*spot()):
            own = self.local(src, self.out.ref.at[lax.axis_index("dp")], 0)
            moves = [(True if cond is None else cond, own)]
            for way in range(2):
                sends = self.ends(0, way)[0]
                moves.append((sends if cond is None else sends & cond, self.copy(0, way, src)))
            for when, move in moves:
                if when is True:
                    move.start()
                else:
                    pl.when(when)(move.start)

    def arrive(self, j):
        for way in range(2):
            pl.when(self.ends(j, way)[1])(self.copy(j, way).wait_recv)

    def step(self):
        self.arrive(self.phase)
        self.phase += 1
        for way in range(2):
            pl.when(self.ends(self.phase, way)[0])(self.copy(self.phase, way).start)

    def wait(self):
        if self.waited:
            return
        self.waited = True
        while self.phase < 2:
            self.step()
        self.arrive(2)
        for j in range(3):
            for way in range(2):
                pl.when(self.ends(j, way)[0])(self.copy(j, way).wait_send)
        d = lax.axis_index("dp")
        self.local(self.sources(*spot())[0][1], self.out.ref.at[d], 0).wait()


def z_gather_from(k, sources, shape, dtype):
    count = dp_size()
    if count == 4:
        return LineGather(k, sources, shape, dtype)

    def moves(s, d, t):
        dst, found = task.out.ref.at[d], sources(s, d, t)
        return [(found, dst, {"dp": (d + i) % count}) for i in range(1, count)], [(found, dst)]

    task = Task(k, (count,) + shape, "dp", moves, count - 1, out_dtype=dtype)
    return task


def z_gather(k, value):
    val = as_val(k, value)
    return z_gather_from(k, lambda s, d, t: [(None, val.ref)], val.shape, val.dtype)


def z_gather_half(k, shard, moved, block):
    shard, moved = as_val(k, shard), as_val(k, moved)
    rows = shard.shape[0] // 2

    def sources(s, d, t):
        own = shard.ref.at[pl.ds(block * rows, rows)]
        return [(s == block, own), (s == 1 - block, moved.ref)]

    return z_gather_from(k, sources, moved.shape, shard.dtype)


def one_way(task, sender):
    task.final = None if sender is None else 1 - sender
    return task


def z_gather_whole(k, shard, moved, block, half=None):
    shard, moved = as_val(k, shard), as_val(k, moved)
    rows = shard.shape[0] if half is None else shard.shape[0] // 2
    part = pl.ds(0 if half is None else half * rows, rows)

    def sources(s, d, t):
        return [(s == block, shard.ref.at[part]), (s == 1 - block, moved.ref.at[part])]

    return z_gather_from(k, sources, (rows,) + shard.shape[1:], shard.dtype)


def x_move(k, value, sender=None):
    val = as_val(k, value)

    def moves(s, d, t):
        return [([(None, val.ref)], task.out.ref, {"section": 1 - s})], []

    task = Task(k, val.shape, "section", moves, 1, out_dtype=val.dtype)
    return one_way(task, sender)


def x_half(k, value, sender=None):
    val = as_val(k, value)
    rows = val.shape[0] // 2

    def moves(s, d, t):
        src = val.ref.at[block_of(1 - s, rows)]
        return [([(None, src)], task.out.ref, {"section": 1 - s})], []

    task = Task(k, (rows,) + val.shape[1:], "section", moves, 1, out_dtype=val.dtype)
    return one_way(task, sender)


def x_slots(k, value, kind):
    val, count = as_val(k, value), dp_size()
    rows = val.shape[0] // (2 * count)

    def moves(s, d, t):
        far = []
        for i in range(count):
            slot = 2 * i + 1 - s if kind == "rows" else (1 - s) * count + i
            src = val.ref.at[block_of(slot, rows)]
            far.append(([(None, src)], task.out.ref.at[i], {"section": 1 - s}))
        return far, []

    task = Task(k, (count, rows) + val.shape[1:], "section", moves, count)
    return task


class Terms:
    def __init__(self, k, kind, grads, received, local):
        self.grads, self.local = as_val(k, grads), local
        self.kind, self.n = kind, dp_size()
        self.whole = received is None
        if self.whole:
            rows, cols = self.grads.shape
            self.rows = rows if kind == "cols" else rows // self.n
            self.cols = cols // self.n if kind == "cols" else cols
            self.shape = (self.n, self.rows, self.cols)
            self.aside = kind == "cols" and self.cols % 128 != 0
            self.total = k.vmem(self.shape, BF)
            self.kept = k.vmem(self.grads.shape, BF) if self.aside else self.total
            return
        self.received = as_val(k, received)
        if kind == "cols":
            self.rows, self.cols = self.grads.shape[0] // 2, self.grads.shape[1] // self.n
            held = (self.rows, self.grads.shape[1])
        else:
            self.rows, self.cols = self.grads.shape[0] // (2 * self.n), self.grads.shape[1]
            held = (self.n, self.rows, self.cols)
        self.kept, self.got = k.vmem(held, BF), k.vmem(held, BF)
        self.shape = (self.n, self.rows, self.cols)
        self.total = k.vmem(self.shape, BF) if kind == "cols" else self.kept

    def loads(self):
        s, grads, kept = lax.axis_index("section"), self.grads.ref, self.kept.ref
        if self.whole and self.aside:
            return [self.local(grads, kept, 2)]
        if self.whole:
            parts = [
                grads.at[:, pl.ds(i * self.cols, self.cols)]
                if self.kind == "cols"
                else grads.at[block_of(i, self.rows)]
                for i in range(self.n)
            ]
            return [self.local(part, kept.at[i], 2 + i) for i, part in enumerate(parts)]
        if self.kind == "cols":
            moves = [self.local(grads.at[block_of(s, self.rows)], kept, 2)]
        else:
            moves = []
            for i in range(self.n):
                slot = 2 * i + s if self.kind == "rows" else s * self.n + i
                moves.append(self.local(grads.at[block_of(slot, self.rows)], kept.at[i], 2 + i))
        return moves + [self.local(self.received.ref, self.got.ref, 1)]

    def load(self):
        for move in self.loads():
            move.start()

    def add(self):
        for move in self.loads():
            move.wait()
        if self.whole and self.aside:
            for i in range(self.n):
                self.total.ref[i] = self.kept.ref[:, i * self.cols : (i + 1) * self.cols]
        if self.whole:
            return
        kept, got, total = self.kept.ref, self.got.ref, self.total.ref
        if self.kind != "cols":

            def piece(i, carry):
                chunked(self.rows, lambda at: total.__setitem__(
                    (i, at), (kept[i, at, :].astype(F32) + got[i, at, :].astype(F32)).astype(BF)
                ))
                return carry

            lax.fori_loop(0, self.n, piece, 0)
            return

        def add_rows(at):
            for i in range(self.n):
                part = slice(i * self.cols, (i + 1) * self.cols)
                value = kept[at, part].astype(F32) + got[at, part].astype(F32)
                total[i, at, :] = value.astype(BF)

        chunked(self.rows, add_rows)


class DirectScatter(Task):
    def __init__(self, k, kind, grads, received):
        self.terms = Terms(k, kind, grads, received, lambda *a: self.local(*a))
        count = dp_size()

        def moves(s, d, t):
            total = self.terms.total.ref
            far = []
            for i in range(1, count):
                other = (d + i) % count
                far.append(([(None, total.at[other])], self.out.ref.at[d], {"dp": other}))
            return far, [([(None, total.at[d])], self.out.ref.at[d])]

        super().__init__(k, self.terms.shape, "dp", moves, count - 1, 2 + count)
        self.load = self.terms.load

    def send(self):
        self.terms.add()
        super().send()

    def add(self):
        self.load()
        self.send()


class LineScatter(Line):
    def __init__(self, k, kind, grads, received):
        self.terms = Terms(k, kind, grads, received, lambda *a: self.local(*a))
        super().__init__(k, self.terms.shape[1:], BF, 6)
        self.got = k.vmem((2, 3) + self.terms.shape[1:], BF)
        self.load = self.terms.load

    def ends(self, j, way):
        d = lax.axis_index("dp")
        if way == 0:
            return (d <= j) & (d < 3), (d >= 1) & (d <= j + 1)
        return (d >= 3 - j) & (d > 0), (d <= 2) & (d >= 2 - j)

    def copy(self, j, way):
        d = lax.axis_index("dp")
        to = (d + 3 - j if way == 0 else d + 1 + j) % 4
        return self.hop(j, way, self.terms.total.ref.at[to], self.got.ref.at[way, j])

    def send(self):
        self.phase = 0
        self.terms.add()
        for way in range(2):
            pl.when(self.ends(0, way)[0])(self.copy(0, way).start)

    def take(self, j, way):
        d = lax.axis_index("dp")
        to = (d + 2 - j if way == 0 else d + 2 + j) % 4
        self.copy(j, way).wait_recv()
        total, got = self.terms.total.ref, self.got.ref

        def add_rows(at):
            value = total[to, at, :].astype(F32) + got[way, j, at, :].astype(F32)
            total[to, at, :] = value.astype(BF)

        chunked(self.terms.rows, add_rows)

    def arrive(self, j):
        for way in range(2):
            pl.when(self.ends(j, way)[1])(functools.partial(self.take, j, way))

    def step(self):
        self.arrive(self.phase)
        self.phase += 1
        for way in range(2):
            pl.when(self.ends(self.phase, way)[0])(self.copy(self.phase, way).start)

    def wait(self):
        if self.waited:
            return
        self.waited = True
        while self.phase < 2:
            self.step()
        self.arrive(2)
        done = self.local(self.terms.total.ref.at[lax.axis_index("dp")], self.out.ref, 0)
        done.start()
        for j in range(3):
            for way in range(2):
                pl.when(self.ends(j, way)[0])(self.copy(j, way).wait_send)
        done.wait()

    def add(self):
        self.load()
        self.send()


def sum_scatter(k, kind, grads, received=None):
    return (LineScatter if dp_size() == 4 else DirectScatter)(k, kind, grads, received)


class Finish(Task):
    def __init__(self, k, pieces, block):
        self.pieces, self.final = as_val(k, pieces), block
        *slots, rows, cols = self.pieces.shape
        self.slots = slots[0] if slots else 0
        if slots:
            self.held, self.total = k.vmem(self.pieces.shape, BF), k.vmem((rows, cols), BF)
        else:
            self.total = self.pieces

        def moves(s, d, t):
            source, dst = [(None, self.total.ref)], self.out.ref.at[s]
            return [(source, dst, {"section": 1 - s})], [(source, dst)]

        super().__init__(k, (2, rows, cols), "section", moves, 1, 2)

    def load(self):
        if self.slots:
            self.local(self.pieces.ref, self.held.ref, 1).start()

    def send(self):
        if self.slots:
            self.local(self.pieces.ref, self.held.ref, 1).wait()
            acc = self.held.ref[0].astype(F32)
            for i in range(1, self.slots):
                acc = acc + self.held.ref[i].astype(F32)
            self.total.ref[...] = acc.astype(BF)
        super().send()

    def add(self):
        self.load()
        self.send()


class SumShare(Task):
    def __init__(self, k, terms, axis, slotted=False):
        self.terms = [as_val(k, v) for v in terms]
        shape = self.terms[0].shape[1:] if slotted else self.terms[0].shape
        count = dp_size() if axis == "dp" else 4
        self.slotted = slotted
        self.bufs = [k.vmem(v.shape, F32) for v in self.terms]
        self.total = k.vmem(shape, F32)

        def moves(s, d, t):
            source, me = [(None, self.total.ref)], d if axis == "dp" else t
            dst = self.out.ref.at[me]
            far = [(source, dst, {axis: (me + i) % count}) for i in range(1, count)]
            return far, [(source, dst)]

        super().__init__(k, (count,) + shape, axis, moves, count - 1, 3, out_dtype=F32)

    def add(self):
        loads = [self.local(v.ref, b.ref, 1 + i) for i, (v, b) in enumerate(zip(self.terms, self.bufs))]
        for load in loads:
            load.start()
        for load in loads:
            load.wait()
        if self.slotted:
            parts = [self.bufs[0].ref[i] for i in range(self.terms[0].shape[0])]
        else:
            parts = [buf.ref[...] for buf in self.bufs]
        acc = parts[0]
        for part in parts[1:]:
            acc = acc + part
        self.total.ref[...] = acc
        self.send()


class Weight:
    def __init__(self, k, kind, *segments, early=False):
        self.kind, self.waited = kind, False
        self.segments, start = [], 0
        for near, far in segments:
            near, far = as_val(k, near), None if far is None else as_val(k, far)
            self.segments.append((near, far, start))
            start += near.shape[1] * (1 if far is None else 2)
        self.count, _, self.cols = self.segments[0][0].shape
        self.rows = start
        if kind == "cols":
            shape = (self.rows, self.count * self.cols)
        else:
            shape = (self.count * self.rows, self.cols)
        self.aside = kind == "cols" and self.cols % 128 != 0
        self.buf = k.vmem(shape, BF)
        sides = [v for near, far, _ in self.segments for v in (near, far) if v is not None]
        self.sem = k.sem(len(sides), self.count)
        if self.aside:
            self.held = [k.vmem(v.shape, BF) for v in sides]
        k.once.append(self)
        if early:
            k.early.append(self.start)

    def sides(self):
        s = lax.axis_index("section")
        for near, far, start in self.segments:
            rows = near.shape[1]
            if far is None:
                yield near, start, None
            else:
                yield near, start + s * rows, s
                yield far, start + (1 - s) * rows, 1 - s

    def moves(self):
        dst = self.buf.ref
        for j, (val, start, sec) in enumerate(self.sides()):
            rows = val.shape[1]
            for i in range(self.count):
                if self.aside:
                    to = self.held[j].ref.at[i]
                elif self.kind == "cols":
                    at = pl.ds(pl.multiple_of(start, 16), rows)
                    to = dst.at[at, pl.ds(i * self.cols, self.cols)]
                else:
                    top = (sec * self.count + i) * rows if self.kind == "conv" else i * self.rows + start
                    to = dst.at[pl.ds(pl.multiple_of(top, 16), rows)]
                yield pltpu.make_async_copy(val.ref.at[i], to, self.sem.ref.at[j, i])

    def start(self):
        for move in self.moves():
            move.start()

    def wait(self):
        if self.waited:
            return
        self.waited = True
        for move in self.moves():
            move.wait()
        if self.aside:
            for j, (val, start, _) in enumerate(self.sides()):
                whole = jnp.concatenate([self.held[j].ref[i] for i in range(self.count)], axis=1)
                self.buf.ref[pl.ds(pl.multiple_of(start, 16), val.shape[1]), :] = whole


class Product:
    def __init__(self, k, left, right):
        self.left, self.right = left, right
        rows = left.shape[1]
        self.chunk = 384 if rows % 384 == 0 else 256
        self.count = rows // self.chunk
        self.buf = k.vmem((rows, right.shape[1]), BF)
        self.out, self.sem = k.output(self.buf.shape, BF), k.sem(self.count)

    def copy(self, i):
        part = block_of(i, self.chunk)
        return pltpu.make_async_copy(self.buf.ref.at[part], self.out.ref.at[part], self.sem.ref.at[i])

    def run(self):
        def step(i, carry):
            part = block_of(i, self.chunk)
            value = contract(self.left.ref[:, part], self.right.ref[...], 0, 0)
            self.buf.ref[part, :] = value.astype(BF)
            self.copy(i).start()
            return carry

        lax.fori_loop(0, self.count, step, 0)

    def wait(self):
        for i in range(self.count):
            self.copy(i).wait()


def places():
    me = lax.axis_index("tensor")
    sib = me + 1 - 2 * (me % 2)
    cross = (me + 2) % 4
    diag = (sib + 2) % 4
    return me, sib, cross, diag


class Gather:
    def __init__(self, k, x, gain, weights, extras=(), trans=False, epilogue="plain", save=()):
        rows, width = x.shape
        length = 4 * rows
        self.k, self.x, self.gain, self.weights, self.extras = k, x, gain, weights, extras
        self.trans, self.epilogue, self.rows, self.half = trans, epilogue, rows, rows // 2
        cols = [w.buf.shape[0 if trans else 1] for w in weights]
        kinds = {
            "plain": [(c, F32) for c in cols],
            "ffn": [(cols[0], BF)] * 3,
            "ffn_back": [(cols[0], BF)] * 2,
        }[epilogue]
        self.full = k.vmem((length, width), BF)
        self.values = [k.vmem((length, c), kind) for c, kind in kinds]
        kept = [self.full] + self.values
        self.saved = [(v, k.output(v.shape, v.dtype), k.sem(4, 2)) for v in kept if kept.index(v) in save]
        self.sems = [k.sem(2) for _ in range(6)]
        k.late.append(self.end)

    def span(self, owner, sub):
        return pl.ds(pl.multiple_of(owner * self.rows + sub * self.half, self.half), self.half)

    def move(self, kind, i):
        me, sib, cross, _ = places()
        full = self.full.ref
        owner, peer, at = {"cross": (me, cross, 0), "sib": (me, sib, 2), "relay": (cross, sib, 4)}[kind]
        part = full.at[self.span(owner, i)]
        return remote(
            part, part, self.sems[at].ref.at[i], self.sems[at + 1].ref.at[i], {"tensor": peer}
        )

    def begin(self):
        me = places()[0]
        for i in range(2):

            def put(j, carry):
                at = i * self.half + j * STRIP
                part = self.x.ref[pl.ds(pl.multiple_of(at, STRIP), STRIP), :].astype(F32)
                if self.gain is not None:
                    val, row = self.gain
                    part = norm_rows(part, val.ref[row : row + 1, :])
                to = pl.ds(pl.multiple_of(me * self.rows + at, STRIP), STRIP)
                self.full.ref[to, :] = part.astype(BF)
                return carry

            lax.fori_loop(0, self.half // STRIP, put, 0)
            self.move("cross", i).start()
            self.move("sib", i).start()

    def loop(self):
        me, sib, cross, diag = places()
        rows, half = self.rows, self.half
        for w in self.weights:
            w.wait()

        def step(p, carry):
            far, sub = p // 2, p % 2
            near = (1 - sub) * me + sub * sib
            first = (1 - far) * near * rows + far * (cross * rows + sub * half)
            second = (1 - far) * (near * rows + half) + far * (diag * rows + sub * half)
            pair = [pl.ds(pl.multiple_of(v, half), half) for v in (first, second)]

            @pl.when(p == 1)
            def _():
                self.move("sib", 0).wait_recv()
                self.move("sib", 1).wait_recv()

            for i in range(2):

                @pl.when(p == 2 + i)
                def _():
                    self.move("cross", i).wait_recv()
                    self.move("relay", i).start()
                    self.move("relay", i).wait_recv()

            def both(val):
                return jnp.concatenate([val.ref[pair[0], :], val.ref[pair[1], :]], axis=0)

            a = both(self.full)
            prods = [contract(a, w.buf.ref[...], 1, 1 if self.trans else 0) for w in self.weights]
            if self.epilogue == "plain":
                values = prods
            elif self.epilogue == "ffn":
                sig, silu = silu_parts(prods[0])
                values = [prods[0], prods[1], silu * prods[1]]
            else:
                gate, up = (both(v).astype(F32) for v in self.extras)
                sig, silu = silu_parts(gate)
                values = [prods[0] * up * sig * (1.0 + gate * (1.0 - sig)), prods[0] * silu]
            for val, value in zip(self.values, values):
                value = value.astype(val.dtype)
                for j in range(2):
                    val.ref[pair[j], :] = value[j * half : (j + 1) * half]
            for val, out, sem in self.saved:
                for j in range(2):
                    pltpu.make_async_copy(
                        val.ref.at[pair[j]], out.ref.at[pair[j]], sem.ref.at[p, j]
                    ).start()
            return carry

        lax.fori_loop(0, 4, step, 0)

    def end(self):
        for i in range(2):
            for kind in ("cross", "sib", "relay"):
                self.move(kind, i).wait_send()
        part = pl.ds(0, self.half)
        for val, out, sem in self.saved:
            for p in range(4):
                for j in range(2):
                    pltpu.make_async_copy(val.ref.at[part], out.ref.at[part], sem.ref.at[p, j]).wait()


class Scatter:
    def __init__(self, k, operands, weights, resid, back=None, trans=False, low=False):
        rows, width = resid.shape
        half = rows // 2
        self.operands, self.weights, self.resid, self.back = operands, weights, resid, back
        self.trans, self.low, self.rows, self.half = trans, low, rows, half
        self.keep, self.own = k.vmem((2, half, width), F32), k.vmem((rows, width), F32)
        self.to_s, self.from_s, self.to_c, self.from_c = (
            k.vmem((2, half, width), BF) for _ in range(4)
        )
        self.to_o, self.from_o = k.vmem((rows, width), BF), k.vmem((rows, width), BF)
        self.out = k.vmem((rows, width), BF if low else F32)
        self.gain_grad = k.vmem((1, width), F32) if back else None
        self.sems = [k.sem(2) for _ in range(4)] + [k.sem(1) for _ in range(2)]
        k.late.append(self.end)

    def move(self, kind, i=0):
        _, sib, cross, _ = places()
        at, src, dst, peer = {
            "diag": (0, self.to_s, self.from_s, sib),
            "cross": (2, self.to_c, self.from_c, cross),
            "near": (4, self.to_o, self.from_o, sib),
        }[kind]
        src, dst = (src.ref, dst.ref) if kind == "near" else (src.ref.at[i], dst.ref.at[i])
        return remote(
            src, dst, self.sems[at].ref.at[i], self.sems[at + 1].ref.at[i], {"tensor": peer}
        )

    def pass_on(self, i):
        self.move("diag", i).wait_recv()

        def add_rows(at):
            total = self.keep.ref[i, at, :] + self.from_s.ref[i, at, :].astype(F32)
            self.to_c.ref[i, at, :] = total.astype(BF)

        chunked(self.half, add_rows)
        self.move("cross", i).start()

    def loop(self):
        me, sib, cross, diag = places()
        rows, half = self.rows, self.half
        for w in self.weights:
            w.wait()

        def step(p, carry):
            near, sub = p // 2, p % 2
            base = near * ((1 - sub) * sib + sub * me) * rows
            first = base + (1 - near) * (cross * rows + sub * half)
            second = base + near * half + (1 - near) * (diag * rows + sub * half)
            pair = [pl.ds(pl.multiple_of(v, half), half) for v in (first, second)]
            total = None
            for y, w in zip(self.operands, self.weights):
                a = jnp.concatenate([y.ref[pair[0], :], y.ref[pair[1], :]], axis=0)
                prod = contract(a, w.buf.ref[...], 1, 1 if self.trans else 0)
                total = prod if total is None else total + prod

            self.own.ref[...] = total

            @pl.when(p < 2)
            def _():
                def put(at):
                    self.keep.ref[p, at, :] = self.own.ref[at, :]
                    lower = pl.ds(pl.multiple_of(at.start + half, 16), at.size)
                    self.to_s.ref[p, at, :] = self.own.ref[lower, :].astype(BF)

                chunked(half, put)
                self.move("diag", p).start()

            @pl.when(p == 2)
            def _():
                def put(at):
                    self.to_o.ref[at, :] = self.own.ref[at, :].astype(BF)

                chunked(rows, put)
                self.move("near").start()

            @pl.when((p == 1) | (p == 2))
            def _():
                self.pass_on(p - 1)

            return carry

        lax.fori_loop(0, 4, step, 0)

    def finish(self):
        self.move("near").wait_recv()
        if self.back:
            self.gain_grad.ref[...] = jnp.zeros_like(self.gain_grad.ref)
        for i in range(2):
            self.move("cross", i).wait_recv()

            def add_rows(j, carry):
                inner = block_of(j, STRIP)
                part = pl.ds(pl.multiple_of(i * self.half + j * STRIP, STRIP), STRIP)
                total = self.own.ref[part, :] + self.from_o.ref[part, :].astype(F32)
                total = total + self.from_c.ref[i, inner, :].astype(F32)
                resid = self.resid.ref[part, :].astype(F32)
                if self.back:
                    value, (gain, row) = self.back
                    total, gain_grad = norm_back(
                        value.ref[part, :].astype(F32), gain.ref[row : row + 1, :], total
                    )
                    self.gain_grad.ref[...] += gain_grad
                self.out.ref[part, :] = (resid + total).astype(self.out.dtype)
                return carry

            lax.fori_loop(0, self.half // STRIP, add_rows, 0)

    def end(self):
        self.move("near").wait_send()
        for i in range(2):
            self.move("diag", i).wait_send()
            self.move("cross", i).wait_send()


def delayed(values, by):
    if by == 0:
        return values
    row = lax.broadcasted_iota(jnp.int32, values.shape, 0)
    return jnp.where(row < by, 0.0, pltpu.roll(values, by, 0))


def advanced(values, by):
    if by == 0:
        return values
    length = values.shape[0]
    row = lax.broadcasted_iota(jnp.int32, values.shape, 0)
    return jnp.where(row >= length - by, 0.0, pltpu.roll(values, length - by, 0))


CONV_COLS = 128


class Conv:
    def __init__(self, k, projected, value, kernel):
        self.projected, self.value, self.kernel = projected, value, kernel
        self.y = k.vmem(value.shape, BF)

    def parts(self, j):
        channels = self.value.shape[1]
        at = block_of(j, CONV_COLS)
        b_gate = self.projected.ref[:, at]
        c_gate = self.projected.ref[:, block_of(j + channels // CONV_COLS, CONV_COLS)]
        x_value, taps = self.value.ref[:, at], self.kernel.ref[:, at]
        product = b_gate * x_value
        count = taps.shape[0]
        causal = jnp.zeros_like(product)
        for i in range(count):
            causal = causal + taps[i : i + 1] * delayed(product, count - 1 - i)
        return at, b_gate, c_gate, x_value, taps, product, causal

    def run(self):
        def step(j, carry):
            at, _, c_gate, _, _, _, causal = self.parts(j)
            self.y.ref[:, at] = (c_gate * causal).astype(BF)
            return carry

        lax.fori_loop(0, self.value.shape[1] // CONV_COLS, step, 0)


class ConvBack(Conv):
    def __init__(self, k, projected, value, kernel, d_y):
        self.projected, self.value, self.kernel, self.d_y = projected, value, kernel, d_y
        self.d_proj = k.vmem(projected.shape, BF)
        self.d_value = k.vmem(value.shape, BF)
        self.d_kernel = k.vmem(kernel.shape, F32)

    def run(self):
        channels = self.value.shape[1]

        def step(j, carry):
            at, b_gate, c_gate, x_value, taps, product, causal = self.parts(j)
            d_y = self.d_y.ref[:, at]
            d_causal = d_y * c_gate
            count = taps.shape[0]
            d_product = jnp.zeros_like(product)
            for i in range(count):
                by = count - 1 - i
                row = jnp.sum(d_causal * delayed(product, by), axis=0, keepdims=True)
                self.d_kernel.ref[i : i + 1, at] = row
                d_product = d_product + taps[i : i + 1] * advanced(d_causal, by)
            self.d_proj.ref[:, at] = (d_product * x_value).astype(BF)
            upper = block_of(j + channels // CONV_COLS, CONV_COLS)
            self.d_proj.ref[:, upper] = (d_y * causal).astype(BF)
            self.d_value.ref[:, at] = (d_product * b_gate).astype(BF)
            return carry

        lax.fori_loop(0, channels // CONV_COLS, step, 0)


def head_mean(values, head_size):
    width = values.shape[1]
    row = lax.broadcasted_iota(jnp.int32, (width, width), 0) // head_size
    col = lax.broadcasted_iota(jnp.int32, (width, width), 1) // head_size
    group = jnp.where(row == col, 1.0 / head_size, 0.0).astype(F32)
    return lax.dot_general(
        values, group, (((1,), (0,)), ((), ())),
        precision=lax.Precision.HIGHEST, preferred_element_type=F32,
    )


def turn(values, head_size, back):
    width, half = values.shape[1], head_size // 2
    lane = lax.broadcasted_iota(jnp.int32, values.shape, 1) % head_size
    upper = pltpu.roll(values, width - half, 1)
    lower = pltpu.roll(values, half, 1)
    return jnp.where(lane < half, upper, -lower) if back else jnp.where(lane < half, -upper, lower)


def head_norm(values, gain, head_size):
    return values * lax.rsqrt(head_mean(values * values, head_size) + EPS) * gain


def head_norm_back(values, gain, grad_in, head_size):
    row_scale = lax.rsqrt(head_mean(values * values, head_size) + EPS)
    normed = values * row_scale
    gain_grad = jnp.sum(grad_in * normed, axis=0, keepdims=True)
    scaled = grad_in * gain
    return row_scale * (scaled - normed * head_mean(scaled * normed, head_size)), gain_grad


def block_weights(q_rows, keys):
    scores = [contract(q_rows, k_rows, 1, 1) for k_rows in keys]
    query = lax.broadcasted_iota(jnp.int32, scores[-1].shape, 0)
    key = lax.broadcasted_iota(jnp.int32, scores[-1].shape, 1)
    scores[-1] = jnp.where(key <= query, scores[-1], MASKED)
    top = functools.reduce(
        jnp.maximum, [jnp.max(part, axis=1, keepdims=True) for part in scores]
    )
    exps = [jnp.exp(part - top) for part in scores]
    scale = 1.0 / sum(jnp.sum(part, axis=1, keepdims=True) for part in exps)
    return [part * scale for part in exps]


def key_blocks(i):
    blocks = [pl.ds(0, i * ROW_BLOCK)] if i else []
    return blocks + [pl.ds(i * ROW_BLOCK, ROW_BLOCK)]


class Heads:
    def __init__(self, projected, tables, size):
        assert size in (16, 64, 256), size
        self.projected, self.size = projected, size
        self.gain, self.cos, self.sin = (v.buf for v in tables)
        self.loads = tables
        self.length, width = projected.shape
        self.q_cols, self.k_cols = width // 2, width // 4
        self.heads, self.kv_heads = self.q_cols // size, self.k_cols // size
        self.share = self.heads // self.kv_heads

    def per_head(self, k, count, kind):
        return k.vmem((count, self.length, self.size), kind)

    def split(self, val, rows, values):
        for h in range(val.shape[0]):
            val.ref[h, rows, :] = values[:, h * self.size : (h + 1) * self.size]

    def join(self, val, rows):
        return jnp.concatenate([val.ref[h, rows, :] for h in range(val.shape[0])], axis=1)

    def gains(self):
        gain = self.gain.ref[...]
        return (
            jnp.concatenate([gain[0:1]] * self.heads, axis=1),
            jnp.concatenate([gain[1:2]] * self.kv_heads, axis=1),
        )

    def angles(self, rows):
        c, n = self.cos.ref[rows, :], self.sin.ref[rows, :]
        repeat = self.q_cols // c.shape[1]
        return jnp.concatenate([c] * repeat, axis=1), jnp.concatenate([n] * repeat, axis=1)

    def blocks(self, step):
        lax.fori_loop(0, self.length // ROW_BLOCK, lambda p, c: step(block_of(p, ROW_BLOCK)) or c, 0)


class Attend(Heads):
    def __init__(self, k, projected, tables, size):
        super().__init__(projected, tables, size)
        self.q_rot = k.vmem((self.length, self.q_cols), BF)
        self.k_rot = k.vmem((self.length, self.k_cols), BF)
        self.y = k.vmem((self.length, self.q_cols), BF)
        self.q_h, self.y_h = (self.per_head(k, self.heads, BF) for _ in range(2))
        self.k_h, self.v_h = (self.per_head(k, self.kv_heads, BF) for _ in range(2))

    def run(self, *between):
        for load in self.loads:
            load.wait()
        size, q_cols, k_cols, proj = self.size, self.q_cols, self.k_cols, self.projected.ref

        def prepare(rows):
            c, n = self.angles(rows)
            q_gain, k_gain = self.gains()
            q = head_norm(proj[rows, :q_cols], q_gain, size)
            q = (q * c + turn(q, size, False) * n).astype(BF)
            k = head_norm(proj[rows, q_cols : q_cols + k_cols], k_gain, size)
            k = (k * c[:, :k_cols] + turn(k, size, False) * n[:, :k_cols]).astype(BF)
            self.q_rot.ref[rows, :] = q
            self.k_rot.ref[rows, :] = k
            self.split(self.q_h, rows, (q.astype(F32) * size**-0.5).astype(BF))
            self.split(self.k_h, rows, k)
            self.split(self.v_h, rows, proj[rows, q_cols + k_cols :].astype(BF))

        self.blocks(prepare)

        def head(h, carry):
            g = h // self.share

            @pl.when(h == self.heads // 2)
            def _():
                for step in between:
                    step()

            for i in range(self.length // ROW_BLOCK):
                rows, seen = pl.ds(i * ROW_BLOCK, ROW_BLOCK), key_blocks(i)
                weights = block_weights(
                    self.q_h.ref[h, rows, :], [self.k_h.ref[g, at, :] for at in seen]
                )
                value = sum(
                    contract(part.astype(BF), self.v_h.ref[g, at, :], 1, 0)
                    for part, at in zip(weights, seen)
                )
                self.y_h.ref[h, rows, :] = value.astype(BF)
            return carry

        lax.fori_loop(0, self.heads, head, 0)

        def place(rows):
            self.y.ref[rows, :] = self.join(self.y_h, rows)

        self.blocks(place)


class AttendBack(Heads):
    def __init__(self, k, projected, tables, size, q_rot, k_rot, d_y):
        super().__init__(projected, tables, size)
        self.q_rot, self.k_rot, self.d_y = q_rot, k_rot, d_y
        self.q_h, self.dy_h = (self.per_head(k, self.heads, BF) for _ in range(2))
        self.k_h, self.v_h = (self.per_head(k, self.kv_heads, BF) for _ in range(2))
        self.dq_h = self.per_head(k, self.heads, F32)
        self.dk_h, self.dv_h = (self.per_head(k, self.kv_heads, F32) for _ in range(2))
        self.d_proj = k.vmem(projected.shape, BF)
        self.q_gain, self.k_gain = k.vmem((1, self.q_cols), F32), k.vmem((1, self.k_cols), F32)

    def run(self, *between):
        for load in self.loads:
            load.wait()
        size, q_cols, k_cols, proj = self.size, self.q_cols, self.k_cols, self.projected.ref
        scale = size**-0.5
        dq_h, dk_h, dv_h = self.dq_h.ref, self.dk_h.ref, self.dv_h.ref

        def prepare(rows):
            self.split(self.q_h, rows, (self.q_rot.ref[rows, :].astype(F32) * scale).astype(BF))
            self.split(self.dy_h, rows, self.d_y.ref[rows, :].astype(BF))
            self.split(self.k_h, rows, self.k_rot.ref[rows, :])
            self.split(self.v_h, rows, proj[rows, q_cols + k_cols :].astype(BF))

        self.blocks(prepare)

        def clear(rows):
            for val in (dk_h, dv_h):
                val[:, rows, :] = jnp.zeros((self.kv_heads, ROW_BLOCK, size), F32)

        self.blocks(clear)

        def head(h, carry):
            g = h // self.share

            @pl.when(h == self.heads // 2)
            def _():
                for step in between:
                    step()

            for i in range(self.length // ROW_BLOCK):
                rows, seen = pl.ds(i * ROW_BLOCK, ROW_BLOCK), key_blocks(i)
                q, low = self.q_h.ref[h, rows, :], self.dy_h.ref[h, rows, :]
                keys = [self.k_h.ref[g, at, :] for at in seen]
                probs = block_weights(q, keys)
                d_weights = [contract(low, self.v_h.ref[g, at, :], 1, 1) for at in seen]
                inner = sum(
                    jnp.sum(a * b, axis=1, keepdims=True) for a, b in zip(probs, d_weights)
                )
                d_q = 0.0
                for at, k, prob, d_weight in zip(seen, keys, probs, d_weights):
                    dv_h[g, at, :] += contract(prob.astype(BF), low, 0, 0)
                    d_scores = (prob * (d_weight - inner)).astype(BF)
                    d_q = d_q + contract(d_scores, k, 1, 0)
                    dk_h[g, at, :] += contract(d_scores, q, 0, 0)
                dq_h[h, rows, :] = d_q * scale
            return carry

        lax.fori_loop(0, self.heads, head, 0)
        self.q_gain.ref[...] = jnp.zeros_like(self.q_gain.ref)
        self.k_gain.ref[...] = jnp.zeros_like(self.k_gain.ref)

        def finish(rows):
            c, n = self.angles(rows)
            dq, dk, dv = (self.join(v, rows) for v in (self.dq_h, self.dk_h, self.dv_h))
            dq = dq * c + turn(dq * n, size, True)
            dk = dk * c[:, :k_cols] + turn(dk * n[:, :k_cols], size, True)
            q_gain, k_gain = self.gains()
            dq, q_sum = head_norm_back(proj[rows, :q_cols], q_gain, dq, size)
            dk, k_sum = head_norm_back(proj[rows, q_cols : q_cols + k_cols], k_gain, dk, size)
            self.q_gain.ref[...] += q_sum
            self.k_gain.ref[...] += k_sum
            self.d_proj.ref[rows, :q_cols] = dq.astype(BF)
            self.d_proj.ref[rows, q_cols : q_cols + k_cols] = dk.astype(BF)
            self.d_proj.ref[rows, q_cols + k_cols :] = dv.astype(BF)

        self.blocks(finish)


def body(boundary, norm_gain, mix_in, mix_out, w_gate, w_up, w_down, conv_x, conv_kernel, qk_gain):
    first = lax.axis_index("section") == 0
    tensor_index = lax.axis_index("tensor")
    model_width = boundary.shape[3]
    channels = mix_out.shape[1]
    row_shape = boundary.shape[2:]
    length, size = 4 * row_shape[0], qk_gain.shape[1]

    seqs, own_gain = boundary[0], norm_gain[0]
    sh_in, sh_out, sh_gate, sh_up, sh_down = (v[0] for v in (mix_in, mix_out, w_gate, w_up, w_down))

    def gains_of(k, block, other, early=True):
        own, moved = k.input(own_gain), as_val(k, other)
        sources = lambda s, d, t: [(s == block, own.ref), (s == 1 - block, moved.ref)]
        return Load(k, sources, own.shape, F32, early)

    def start_rows(k, slot, other, early=True):
        own, moved = k.input(seqs), as_val(k, other)
        sources = lambda s, d, t: [(s == slot, own.ref.at[slot]), (s == 1 - slot, moved.ref)]
        return Load(k, sources, row_shape, BF, early)

    def wait(*items):
        return [item.wait for item in items]

    k = Kernel(0)
    t_seq = None
    seq_val = k.input(seqs)

    def seq_moves(s, d, t):
        return [([(None, seq_val.ref.at[1 - s])], t_seq.out.ref, {"section": 1 - s})], []

    t_in, t_out, t_up = (x_half(k, v) for v in (sh_in, sh_out, sh_up))
    gate_lo, gate_hi = (Part(sh_gate, i * (sh_gate.shape[0] // 2), sh_gate.shape[0] // 2) for i in range(2))
    down_lo, down_hi = (Part(sh_down, i * (sh_down.shape[0] // 2), sh_down.shape[0] // 2) for i in range(2))
    t_gate0a, t_gate0b = x_half(k, gate_lo, 0), x_move(k, gate_hi, 0)
    t_down0a, t_down0b = x_half(k, down_lo, 0), x_move(k, down_hi, 0)
    t_gate1, t_down1 = x_half(k, sh_gate, 1), x_move(k, sh_down, 1)
    t_seq = Task(k, row_shape, "section", seq_moves, 1)
    t_gain, z_cols = x_move(k, own_gain), z_gather(k, conv_x)
    z_in0, z_out0 = z_gather_half(k, sh_in, t_in.out, 0), z_gather_half(k, sh_out, t_out.out, 0)
    z_gate0a = z_gather_half(k, gate_lo, t_gate0a.out, 0)
    z_gate0b, x_gate0a = z_gather_whole(k, gate_hi, t_gate0b.out, 0), x_move(k, z_gate0a.out)
    z_up0 = z_gather_half(k, sh_up, t_up.out, 0)
    x_cols, x_in0, x_out0 = (x_move(k, v.out) for v in (z_cols, z_in0, z_out0))
    x_load, gain_load = start_rows(k, 0, t_seq.out, False), gains_of(k, 0, t_gain.out, False)
    taps = load_all(k, conv_kernel)
    angles = Angles(k, length, size, 128)
    w_in0, w_cols = Weight(k, "rows", (z_in0.out, x_in0.out)), Weight(k, "conv", (z_cols.out, x_cols.out))
    w_out0 = Weight(k, "cols", (z_out0.out, x_out0.out))
    g0 = Gather(k, x_load.buf, (gain_load.buf, 0), [w_in0, w_cols], save=(0, 1, 2))
    conv = Conv(k, g0.values[0], g0.values[1], taps.buf)
    y0 = Save(k, conv.y)
    s1 = Scatter(k, [conv.y], [w_out0], x_load.buf)
    mid0 = Save(k, s1.out)
    k.do(t_in.send, t_out.send, z_cols.send, t_gate0b.send, t_gate0a.send, t_gate1.send)
    k.do(t_gain.send, t_seq.send)
    k.do(t_in.wait, z_in0.send, t_out.wait, z_out0.send, z_cols.step, z_in0.step, z_out0.step)
    k.do(z_cols.step, z_in0.step, z_out0.step, t_gate0b.wait, z_gate0b.send)
    k.do(t_gate0a.wait, z_gate0a.send)
    k.do(z_cols.wait, x_cols.send, z_in0.wait, x_in0.send, z_out0.wait, x_out0.send, t_up.send)
    k.do(t_gain.wait, gain_load.start, t_seq.wait, x_load.start, gain_load.wait, x_load.wait)
    k.do(g0.begin, z_gate0b.step, z_gate0a.step, angles.run, z_gate0b.step, z_gate0a.step)
    k.do(x_cols.wait, w_cols.start, x_in0.wait, w_in0.start, z_gate0a.wait, x_gate0a.send)
    k.do(t_down0b.send, t_down0a.send, t_down1.send, t_up.wait, z_up0.send)
    k.do(g0.loop, z_up0.step, taps.wait, conv.run, y0.start)
    k.do(x_out0.wait, w_out0.start, s1.loop, z_up0.step, s1.finish, mid0.start)
    k.do(*wait(t_gate1, t_down0a, t_down0b, t_down1, z_gate0b, x_gate0a, z_up0))
    k.build()
    a0, proj0, value0 = (out for _, out, _ in g0.saved)
    table_arrays = [qk_gain] + [v.out for v in angles.saves]
    y0, mid0 = y0.out, mid0.out

    k = Kernel(1)
    x_up0, z_gate1 = x_move(k, z_up0.out), z_gather_half(k, sh_gate, t_gate1.out, 1)
    z_down0a = z_gather_half(k, down_lo, t_down0a.out, 0)
    z_down0b = z_gather_whole(k, down_hi, t_down0b.out, 0)
    z_in1, z_out1 = z_gather_half(k, sh_in, t_in.out, 1), z_gather_half(k, sh_out, t_out.out, 1)
    x_down0a, x_in1, x_out1 = (x_move(k, v.out) for v in (z_down0a, z_in1, z_out1))
    rows, gain_load = load_all(k, mid0), gains_of(k, 0, t_gain.out)
    w_gate0 = Weight(k, "rows", (z_gate0a.out, x_gate0a.out), (z_gate0b.out, None), early=True)
    w_up0 = Weight(k, "rows", (z_up0.out, x_up0.out))
    w_down0 = Weight(k, "cols", (z_down0a.out, x_down0a.out), (z_down0b.out, None))
    g2 = Gather(
        k, rows.buf, (gain_load.buf, 1), [w_gate0, w_up0], epilogue="ffn", save=(0, 1, 2, 3)
    )
    s3 = Scatter(k, [g2.values[2]], [w_down0], rows.buf, low=True)
    z_rows = Save(k, s3.out)
    k.do(x_up0.send, z_down0a.send, z_down0b.send, rows.wait, gain_load.wait, g2.begin)
    k.do(z_in1.send, z_out1.send, z_down0a.step, z_in1.step, z_out1.step, z_down0b.step)
    k.do(z_down0a.step, z_in1.step, z_out1.step, z_gate1.send, z_down0a.wait, x_down0a.send)
    k.do(x_up0.wait, w_up0.start, z_down0b.step, g2.loop, z_gate1.step)
    k.do(z_in1.wait, x_in1.send, z_out1.wait, x_out1.send, z_down0b.wait, x_down0a.wait)
    k.do(w_down0.start, s3.loop, z_gate1.step, s3.finish, z_rows.start)
    k.do(*wait(x_in1, x_out1, z_gate1))
    k.build()
    m0, gate0, up0, hid0 = (out for _, out, _ in g2.saved)
    z_rows = z_rows.out

    k = Kernel(2)
    x_gate1, z_up1 = x_move(k, z_gate1.out), z_gather_half(k, sh_up, t_up.out, 1)
    z_down1a, z_down1b = (z_gather_whole(k, sh_down, t_down1.out, 1, i) for i in range(2))
    x_up1 = x_move(k, z_up1.out)
    rows, gain_load = load_all(k, z_rows), gains_of(k, 1, t_gain.out)
    tables = [load_all(k, v) for v in table_arrays]
    w_in1 = Weight(k, "rows", (z_in1.out, x_in1.out), early=True)
    w_out1 = Weight(k, "cols", (z_out1.out, x_out1.out), early=True)
    g4 = Gather(k, rows.buf, (gain_load.buf, 0), [w_in1], save=(0, 1))
    attend = Attend(k, g4.values[0], tables, size)
    kept = [Save(k, v) for v in (attend.q_rot, attend.k_rot, attend.y)]
    s5 = Scatter(k, [attend.y], [w_out1], rows.buf)
    mid1 = Save(k, s5.out)
    k.do(x_gate1.send, z_up1.send, rows.wait, gain_load.wait, g4.begin, z_up1.step)
    k.do(z_down1a.send, g4.loop, z_up1.step, z_down1b.send)
    k.do(lambda: attend.run(z_up1.wait, x_up1.send, z_down1a.step))
    k.do(*(v.start for v in kept))
    k.do(z_down1b.step, s5.loop, z_down1a.step, z_down1b.step, s5.finish, mid1.start)
    k.do(*wait(x_gate1, x_up1, z_down1a, z_down1b))
    k.build()
    a1, proj1 = (out for _, out, _ in g4.saved)
    q_rot, k_rot, y1 = (v.out for v in kept)
    mid1 = mid1.out

    k = Kernel(3)
    rows, gain_load = load_all(k, mid1), gains_of(k, 1, t_gain.out)
    cot = start_rows(k, 1, t_seq.out)
    w_gate1 = Weight(k, "rows", (z_gate1.out, x_gate1.out), early=True)
    w_up1 = Weight(k, "rows", (z_up1.out, x_up1.out), early=True)
    w_down1 = Weight(k, "cols", (z_down1a.out, None), (z_down1b.out, None), early=True)
    g6 = Gather(k, rows.buf, (gain_load.buf, 1), [w_gate1, w_up1], epilogue="ffn")
    g8 = Gather(
        k, cot.buf, None, [w_down1], [g6.values[0], g6.values[1]], trans=True, epilogue="ffn_back"
    )
    p_down1 = Product(k, g6.values[2], g8.full)
    p_gate1, p_up1 = Product(k, g6.full, g8.values[0]), Product(k, g6.full, g8.values[1])
    s9 = Scatter(k, g8.values, [w_gate1, w_up1], cot.buf, (rows.buf, (gain_load.buf, 1)), True)
    hid1 = Save(k, g6.values[2])
    d_mid1, gain11 = Save(k, s9.out), Save(k, s9.gain_grad)
    k.do(rows.wait, gain_load.wait, g6.begin, cot.wait, g8.begin, g6.loop, hid1.start, g8.loop)
    k.do(s9.loop, p_down1.run, p_gate1.run, p_up1.run)
    k.do(s9.finish, d_mid1.start, gain11.start, p_down1.wait, p_gate1.wait, p_up1.wait)
    k.build()
    hid1, d_mid1, gain11 = hid1.out, d_mid1.out, gain11.out

    k = Kernel(4)
    r_down1 = x_half(k, p_down1.out)
    r_gate1, q_up1 = x_slots(k, p_gate1.out, "rows"), sum_scatter(k, "rows", p_up1.out)
    rows, gain_load = load_all(k, d_mid1), gains_of(k, 1, t_gain.out)
    value = load_all(k, z_rows)
    tables = [load_all(k, v) for v in table_arrays]
    proj, q_load, k_load, y_load, a_load = (load_all(k, v) for v in (proj1, q_rot, k_rot, y1, a1))
    w_in1 = Weight(k, "rows", (z_in1.out, x_in1.out), early=True)
    w_out1 = Weight(k, "cols", (z_out1.out, x_out1.out), early=True)
    g10 = Gather(k, rows.buf, None, [w_out1], trans=True)
    p_out1 = Product(k, y_load.buf, g10.full)
    back = AttendBack(k, proj.buf, tables, size, q_load.buf, k_load.buf, g10.values[0])
    p_in1 = Product(k, a_load.buf, back.d_proj)
    r_out1 = x_half(k, p_out1.out)
    s11 = Scatter(
        k, [back.d_proj], [w_in1], rows.buf, (value.buf, (gain_load.buf, 0)), True, low=True
    )
    d_z, gain10 = Save(k, s11.out), Save(k, s11.gain_grad)
    head_gains = [Save(k, back.q_gain), Save(k, back.k_gain)]
    k.early.append(q_up1.load)
    k.do(r_down1.send, r_gate1.send, q_up1.send, rows.wait, g10.begin, g10.loop)
    k.do(y_load.wait, p_out1.run, q_up1.step, p_out1.wait, r_out1.send)
    k.do(proj.wait, q_load.wait, k_load.wait, lambda: back.run(q_up1.step))
    k.do(*(v.start for v in head_gains))
    k.do(gain_load.wait, value.wait, s11.loop, a_load.wait, p_in1.run)
    k.do(s11.finish, d_z.start, gain10.start, p_in1.wait)
    k.do(*wait(r_down1, q_up1, r_gate1, r_out1))
    k.build()
    d_z, gain10 = d_z.out, gain10.out
    q_gain, k_gain = (v.out for v in head_gains)

    k = Kernel(5)
    q_gate1, m_up1 = sum_scatter(k, "rows", p_gate1.out, r_gate1.out), x_move(k, q_up1.out, 0)
    q_out1 = sum_scatter(k, "cols", p_out1.out, r_out1.out)
    r_in1 = x_slots(k, p_in1.out, "rows")
    q_in1 = sum_scatter(k, "rows", p_in1.out, r_in1.out)
    q_down1 = sum_scatter(k, "cols", p_down1.out, r_down1.out)
    rows, value, gain_load = load_all(k, d_z), load_all(k, mid0), gains_of(k, 0, t_gain.out)
    gate_load, up_load, hid_load, m_load = (load_all(k, v) for v in (gate0, up0, hid0, m0))
    w_gate0 = Weight(k, "rows", (z_gate0a.out, x_gate0a.out), (z_gate0b.out, None), early=True)
    w_up0 = Weight(k, "rows", (z_up0.out, x_up0.out), early=True)
    w_down0 = Weight(k, "cols", (z_down0a.out, x_down0a.out), (z_down0b.out, None), early=True)
    g12 = Gather(
        k, rows.buf, None, [w_down0], [gate_load.buf, up_load.buf], trans=True, epilogue="ffn_back"
    )
    p_down0 = Product(k, hid_load.buf, g12.full)
    p_gate0, p_up0 = Product(k, m_load.buf, g12.values[0]), Product(k, m_load.buf, g12.values[1])
    r_down0 = x_half(k, p_down0.out)
    s13 = Scatter(
        k, g12.values, [w_gate0, w_up0], rows.buf, (value.buf, (gain_load.buf, 1)), True
    )
    d_mid0, gain01 = Save(k, s13.out), Save(k, s13.gain_grad)
    k.early += [q_gate1.load, q_down1.load, q_out1.load]
    k.do(r_in1.send, m_up1.send, q_gate1.send, rows.wait, g12.begin, q_down1.send, q_out1.send)
    k.do(gate_load.wait, up_load.wait, g12.loop, q_gate1.step, q_down1.step, q_out1.step)
    k.do(hid_load.wait, p_down0.run, p_down0.wait, r_down0.send, r_in1.wait, q_in1.add)
    k.do(s13.loop, q_gate1.step, q_down1.step, q_out1.step)
    k.do(m_load.wait, p_gate0.run, q_in1.step, p_up0.run, value.wait, gain_load.wait)
    k.do(s13.finish, d_mid0.start, gain01.start, q_in1.step, p_gate0.wait, p_up0.wait)
    k.do(*wait(q_gate1, q_out1, q_in1, q_down1, m_up1, r_down0))
    k.build()
    d_mid0, gain01 = d_mid0.out, gain01.out

    k = Kernel(6)
    r_gate0 = x_slots(k, p_gate0.out, "rows")
    q_gate0 = sum_scatter(k, "rows", p_gate0.out, r_gate0.out)
    q_down0 = sum_scatter(k, "cols", p_down0.out, r_down0.out)
    q_up0 = sum_scatter(k, "rows", p_up0.out)
    m_up0 = x_move(k, q_up0.out, 1)
    e_down1 = Finish(k, q_down1.out, 1)
    e_gate1, e_out1, e_in1 = (Finish(k, v.out, 1) for v in (q_gate1, q_out1, q_in1))
    rows, gain_load = load_all(k, d_mid0), gains_of(k, 0, t_gain.out)
    x_load, taps = start_rows(k, 0, t_seq.out), load_all(k, conv_kernel)
    y_load, a_load, proj, value = (load_all(k, v) for v in (y0, a0, proj0, value0))
    w_in0 = Weight(k, "rows", (z_in0.out, x_in0.out), early=True)
    w_cols = Weight(k, "conv", (z_cols.out, x_cols.out), early=True)
    w_out0 = Weight(k, "cols", (z_out0.out, x_out0.out), early=True)
    g14 = Gather(k, rows.buf, None, [w_out0], trans=True)
    p_out0 = Product(k, y_load.buf, g14.full)
    back = ConvBack(k, proj.buf, value.buf, taps.buf, g14.values[0])
    p_in0, p_cols = Product(k, a_load.buf, back.d_proj), Product(k, a_load.buf, back.d_value)
    r_out0, r_in0 = x_half(k, p_out0.out), x_slots(k, p_in0.out, "rows")
    r_cols = x_slots(k, p_cols.out, "conv")
    q_out0, q_in0 = sum_scatter(k, "cols", p_out0.out, r_out0.out), sum_scatter(k, "rows", p_in0.out, r_in0.out)
    q_cols = sum_scatter(k, "conv", p_cols.out, r_cols.out)
    e_down0, e_gate0, e_out0, e_in0 = (
        Finish(k, v.out, 0) for v in (q_down0, q_gate0, q_out0, q_in0)
    )
    s15 = Scatter(
        k, [back.d_proj, back.d_value], [w_in0, w_cols], rows.buf,
        (x_load.buf, (gain_load.buf, 0)), True, low=True,
    )
    d_x = Save(k, s15.out)
    tap_rows = conv_kernel.shape[0]
    small = k.vmem((8, model_width), F32)
    small_out = Save(k, small)
    ready = [load_all(k, v) for v in (gain01, gain10, gain11)]
    head_loads = [load_all(k, v) for v in (q_gain, k_gain)]

    def fill_small():
        t = lax.axis_index("tensor")
        small.ref[...] = jnp.zeros_like(small.ref)
        small.ref[0:1, :] = s15.gain_grad.ref[...]
        for i, load in enumerate(ready):
            load.wait()
            small.ref[i + 1 : i + 2, :] = load.buf.ref[...]
        small.ref[4 : 4 + tap_rows, block_of(t, channels)] = back.d_kernel.ref[...]
        at = 0
        for load in head_loads:
            load.wait()
            width = load.buf.shape[1]
            small.ref[7:8, at : at + width] = load.buf.ref[...]
            at += width
        small_out.start()

    t_small = x_move(k, small_out.out)
    z_small = SumShare(k, [small_out.out, t_small.out], "dp")
    t_total = SumShare(k, [z_small.out], "tensor", slotted=True)
    hid_load, mid_load = load_all(k, hid1), load_all(k, mid1)
    w_down1 = Weight(k, "cols", (z_down1a.out, None), (z_down1b.out, None), early=True)
    s7 = Scatter(k, [hid_load.buf], [w_down1], mid_load.buf, low=True)
    y_rows = Save(k, s7.out)
    t_x, t_y = x_move(k, d_x.out, 1), x_move(k, y_rows.out, 0)
    k.early += [q_up0.load, q_down0.load]
    k.early += [v.load for v in (e_down1, e_gate1, e_out1, e_in1)]
    k.do(r_gate0.send, q_up0.send, rows.wait, g14.begin, q_down0.send)
    k.do(e_down1.send, e_gate1.send, e_out1.send, e_in1.send, g14.loop)
    k.do(y_load.wait, p_out0.run, p_out0.wait, r_out0.send, q_up0.step)
    k.do(proj.wait, value.wait, taps.wait, back.run, q_down0.step, a_load.wait)
    k.do(p_in0.run, p_cols.run, p_in0.wait, r_in0.send, p_cols.wait, r_cols.send)
    k.do(r_gate0.wait, q_gate0.add, x_load.wait, gain_load.wait, s15.loop, q_up0.step)
    k.do(q_down0.step, s15.finish, d_x.start, fill_small, d_x.wait, t_x.send)
    k.do(small_out.wait, t_small.send, q_gate0.step, hid_load.wait, mid_load.wait, s7.loop)
    k.do(r_out0.wait, q_out0.add, r_in0.wait, q_in0.add)
    k.do(r_cols.wait, q_cols.add, q_up0.wait, m_up0.send, q_down0.wait, e_down0.add)
    k.do(s7.finish, y_rows.start, y_rows.wait, t_y.send)
    k.do(q_gate0.step, q_out0.step, q_in0.step, q_cols.step, t_small.wait, z_small.add)
    k.do(q_gate0.wait, e_gate0.add, q_out0.step, q_in0.step, q_cols.step)
    k.do(z_small.wait, t_total.add, q_out0.wait, e_out0.add, q_in0.wait, e_in0.add)
    rest = (e_down1, e_gate1, e_out1, e_in1, q_cols, e_down0, e_gate0, m_up0, e_out0, e_in0)
    k.do(*wait(*rest, t_total, t_x, t_y))
    k.build()

    owned = [
        ([e_in0], [e_in1], 1),
        ([e_out0], [e_out1], 1),
        ([e_gate0], [e_gate1], 1),
        ([q_up0, m_up0], [q_up1, m_up1], 1),
        ([e_down0], [e_down1], 1),
        ([q_cols], [q_cols], 0),
    ]
    return pack(
        [(zero, one, lead) for zero, one, lead in owned], t_total, d_x.out, y_rows.out, t_x, t_y,
        (norm_gain.shape, conv_kernel.shape, qk_gain.shape),
    )


def slot_free(val, shape):
    value = val.out.array
    if value.ndim == 3 and value.shape[0] * value.shape[1] != shape[0]:
        value = jnp.sum(value.astype(F32), axis=0).astype(BF)
    return value.reshape(shape)


def pack_kernel(plan, *refs):
    n_in, leads, terms, tap_rows = plan
    ins, rest = refs[:n_in], refs[n_in:]
    result, gain_out, *grads, cols, taps, heads = rest[: len(leads) + 4]
    grads = [*grads, cols]
    room = iter(rest[len(leads) + 4 :])
    own_v, moved_v, small_v, *bufs = (next(room) for _ in range(3 + len(terms)))
    out_v = [next(room) for _ in leads]
    load_sem, store_sem = room
    s, t = lax.axis_index("section"), lax.axis_index("tensor")
    small, d_x, y_rows, moved, moved_y, *parts = ins

    def either(cond, zero, one, dst, sem):
        if zero is not None:
            pl.when(cond)(pltpu.make_async_copy(zero, dst, sem).start)
        if one is not None:
            pl.when(jnp.logical_not(cond))(pltpu.make_async_copy(one, dst, sem).start)

    first = s == 0
    either(first, d_x, y_rows, own_v, load_sem.at[0])
    either(first, moved, moved_y, moved_v, load_sem.at[1])
    pltpu.make_async_copy(small, small_v, load_sem.at[2]).start()
    for j, (zero, one, _) in enumerate(terms):
        either(
            first,
            None if zero is None else parts[zero],
            None if one is None else parts[one],
            bufs[j],
            load_sem.at[3 + j],
        )
    for j, (zero, one, i) in enumerate(terms):
        arrive = pltpu.make_async_copy(parts[one if zero is None else zero], bufs[j], load_sem.at[3 + j])
        begins = j == 0 or terms[j - 1][2] != i

        def put(j=j, i=i, begins=begins):
            def add_rows(at):
                value = bufs[j][at, :].astype(F32)
                out_v[i][at, :] = value if begins else out_v[i][at, :] + value

            chunked(bufs[j].shape[0], add_rows)

        if zero is None or one is None:
            cond = first if one is None else jnp.logical_not(first)

            @pl.when(cond)
            def _(arrive=arrive, put=put):
                arrive.wait()
                put()
        else:
            arrive.wait()
            put()
        if j + 1 == len(terms) or terms[j + 1][2] != i:
            dst = grads[i].at[0] if leads[i] else grads[i]
            pltpu.make_async_copy(out_v[i], dst, store_sem.at[i]).start()
    pltpu.make_async_copy(d_x, own_v, load_sem.at[0]).wait()
    pltpu.make_async_copy(moved, moved_v, load_sem.at[1]).wait()
    n = len(leads)
    stores = [
        pltpu.make_async_copy(own_v, result.at[0, s], store_sem.at[n]),
        pltpu.make_async_copy(moved_v, result.at[0, 1 - s], store_sem.at[n + 1]),
    ]
    for store in stores:
        store.start()
    pltpu.make_async_copy(small, small_v, load_sem.at[2]).wait()
    total = small_v[0]
    for i in range(1, small_v.shape[0]):
        total = total + small_v[i]
    gain_out[0] = jnp.where(first, total[0:2], total[2:4])
    channels, size = taps.shape[1], heads.shape[1]
    chosen = total[4 : 4 + tap_rows, 0:channels]
    for i in range(1, total.shape[1] // channels):
        chosen = jnp.where(t == i, total[4 : 4 + tap_rows, i * channels : (i + 1) * channels], chosen)
    taps[...] = chosen
    at = 0
    for row, width in enumerate((channels, channels // 2)):
        value = total[7:8, at : at + size]
        for i in range(1, width // size):
            value = value + total[7:8, at + i * size : at + (i + 1) * size]
        heads[row : row + 1, :] = value
        at += width
    for i, store in enumerate(leads):
        dst = grads[i].at[0] if store else grads[i]
        pltpu.make_async_copy(out_v[i], dst, store_sem.at[i]).wait()
    for store in stores:
        store.wait()


def pack(owned, small, d_x, y_rows, moved_x, moved_y, shapes):
    gain_shape, tap_shape, head_shape = shapes
    parts, terms, leads, out_shapes = [], [], [], []
    for i, (zero, one, lead) in enumerate(owned):
        whole = zero[0].out.shape
        if lead and len(whole) == 3 and isinstance(zero[0], Finish):
            shape = (whole[0] * whole[1], whole[2])
        else:
            shape = whole[-2:]
        shape = tuple(shape)
        leads.append(lead)
        out_shapes.append(shape)
        for j in range(max(len(zero), len(one))):
            pair = []
            for side in (zero, one):
                if j < len(side):
                    parts.append(slot_free(side[j], shape))
                    pair.append(len(parts) - 1)
                else:
                    pair.append(None)
            terms.append((*pair, i))
    operands = [v.array for v in (small.out, d_x, y_rows, moved_x.out, moved_y.out)] + parts
    rows = d_x.shape
    smem = pl.BlockSpec(memory_space=pltpu.VMEM)
    out_shape = [jax.ShapeDtypeStruct((1, 2) + rows, BF), jax.ShapeDtypeStruct(gain_shape, F32)]
    out_shape += [
        jax.ShapeDtypeStruct((1,) + v if lead else v, F32) for v, lead in zip(out_shapes, leads)
    ]
    out_shape += [jax.ShapeDtypeStruct(v, F32) for v in (tap_shape, head_shape)]
    n = len(leads)
    return tuple(
        pl.pallas_call(
            functools.partial(
                pack_kernel, (len(operands), tuple(leads), tuple(terms), tap_shape[0])
            ),
            out_shape=out_shape,
            in_specs=[ANY] * len(operands),
            out_specs=[ANY, smem] + [ANY] * n + [smem] * 2,
            scratch_shapes=[pltpu.VMEM(rows, BF)] * 2
            + [pltpu.VMEM(small.out.shape, F32)]
            + [pltpu.VMEM(out_shapes[i], BF) for _, _, i in terms]
            + [pltpu.VMEM(v, F32) for v in out_shapes]
            + [DMA((3 + len(terms),)), DMA((n + 2,))],
            compiler_params=pltpu.CompilerParams(vmem_limit_bytes=VMEM_BYTES),
            name="pack",
        )(*operands)
    )


def solution(mesh):
    in_specs = (
        P("section", "dp", "tensor", None),
        P("section", None, None),
        P("section", "dp", "tensor"),
        P("section", "tensor", "dp"),
        P("section", "dp", "tensor"),
        P("section", "dp", "tensor"),
        P("section", "tensor", "dp"),
        P(("section", "dp"), "tensor"),
        P(None, "tensor"),
        P(),
    )
    out_specs = (
        P("section", "dp", "tensor", None),
        P("section", None, None),
        P("section", "dp", "tensor"),
        P("section", "tensor", "dp"),
        P("section", "dp", "tensor"),
        P("section", "dp", "tensor"),
        P("section", "tensor", "dp"),
        P(("section", "dp"), "tensor"),
        P(None, "tensor"),
        P(),
    )
    return jax.shard_map(body, mesh=mesh, in_specs=in_specs, out_specs=out_specs, check_vma=False)
```

```python
import functools

import jax
import jax.numpy as jnp
from jax import lax
from jax.experimental import pallas as pl
from jax.experimental.pallas import tpu as pltpu
from jax.sharding import PartitionSpec as P

HEADS = 16
KV_HEADS = 8

EPS = 1e-05
ROPE_BASE = 1000000.0
MASKED = -1e30

MESH = pl.DeviceIdType.MESH
ANY = pl.BlockSpec(memory_space=pl.ANY)
DMA = pltpu.SemaphoreType.DMA
VMEM_BYTES = 63 * 1024 * 1024
BF = jnp.bfloat16
F32 = jnp.float32
ROW_BLOCK = 256
STRIP = 32


def contract(left_op, right_op, left_dim, right_dim):
    return lax.dot_general(
        left_op, right_op, (((left_dim,), (right_dim,)), ((), ())), preferred_element_type=F32
    )


def norm_rows(values, gain):
    return values * lax.rsqrt(jnp.mean(values * values, axis=-1, keepdims=True) + EPS) * gain


def norm_back(values, gain, grad_in):
    row_scale = lax.rsqrt(jnp.mean(values * values, axis=-1, keepdims=True) + EPS)
    normed = values * row_scale
    gain_grad = jnp.sum(grad_in * normed, axis=0, keepdims=True)
    scaled = grad_in * gain
    value_grad = row_scale * (scaled - normed * jnp.mean(scaled * normed, axis=-1, keepdims=True))
    return (value_grad, gain_grad)


class Angles:
    def __init__(self, k, length, head_size, width):
        self.half = head_size // 2
        self.tables = [k.vmem((length, width), F32) for _ in range(2)]
        self.saves = [Save(k, v) for v in self.tables]

    def run(self):
        cos, sin = self.tables
        shape = (ROW_BLOCK, cos.shape[1])
        column = (lax.broadcasted_iota(jnp.int32, shape, 1) % self.half).astype(F32)
        frequency = ROPE_BASE ** (-(column / self.half))
        row = lax.broadcasted_iota(jnp.int32, shape, 0)

        def step(i, carry):
            rows = block_of(i, ROW_BLOCK)
            angle = (row + i * ROW_BLOCK).astype(F32) * frequency
            cos.ref[rows, :] = jnp.cos(angle)
            sin.ref[rows, :] = jnp.sin(angle)
            return carry

        lax.fori_loop(0, cos.shape[0] // ROW_BLOCK, step, 0)
        for save in self.saves:
            save.start()


def silu_parts(gate):
    sig = 1.0 / (1.0 + jnp.exp(-gate))
    return sig, gate * sig


def chunked(rows, step):
    size = next((n for n in (32, 16) if rows % n == 0), rows)
    if size == rows:
        step(pl.ds(0, rows))
    else:
        lax.fori_loop(0, rows // size, lambda i, c: step(block_of(i, size)) or c, 0)


def dp_size():
    return lax.axis_size("dp")


def spot():
    return tuple(lax.axis_index(a) for a in ("section", "dp", "tensor"))


def block_of(index, size):
    return pl.ds(pl.multiple_of(index * size, size), size)


class Val:
    def __init__(self, shape, dtype):
        self.shape, self.dtype = tuple(shape), dtype
        self.ref = self.array = None


class Kernel:
    def __init__(self, cid):
        self.cid, self.ins, self.arrays, self.outs, self.room = cid, [], [], [], []
        self.early, self.steps, self.late, self.axes = [], [], [], set()
        self.once = []

    def input(self, array):
        array = array.array if isinstance(array, Val) else array
        for val, known in zip(self.ins, self.arrays):
            if known is array:
                return val
        val = Val(array.shape, array.dtype)
        self.ins.append(val)
        self.arrays.append(array)
        return val

    def output(self, shape, dtype):
        val = Val(shape, dtype)
        self.outs.append(val)
        return val

    def vmem(self, shape, dtype):
        val = Val(shape, dtype)
        self.room.append((val, pltpu.VMEM(tuple(shape), dtype)))
        return val

    def sem(self, *shape):
        val = Val(shape, None)
        self.room.append((val, DMA(shape)))
        return val

    def do(self, *steps):
        self.steps += steps

    def body(self, *refs):
        vals = self.ins + self.outs + [val for val, _ in self.room]
        for val, ref in zip(vals, refs):
            val.ref = ref
        for item in self.once:
            item.waited = False
            item.phase = 0
        for step in self.early:
            step()
        self.greet()
        for step in self.steps + self.late:
            step()

    def greet(self):
        s, d, t = spot()
        _, sib, cross, diag = places()
        barrier = pltpu.get_barrier_semaphore()
        peers = [{"tensor": sib}, {"tensor": cross}]
        if "tensor" in self.axes:
            peers.append({"tensor": diag})
        if "section" in self.axes:
            peers.append({"section": 1 - s})
        if "dp" in self.axes:
            peers += [{"dp": (d + i) % dp_size()} for i in range(1, dp_size())]

        def signal(peer):
            pl.semaphore_signal(barrier, inc=1, device_id=peer, device_id_type=MESH)

        for peer in peers:
            signal(peer)
        expected = len(peers)
        if "line" in self.axes and "dp" not in self.axes:
            pl.when(d < 3)(lambda: signal({"dp": (d + 1) % 4}))
            pl.when(d > 0)(lambda: signal({"dp": (d + 3) % 4}))
            expected = expected + (d + 2) // 3 + (5 - d) // 3
        pl.semaphore_wait(barrier, expected)

    def build(self):
        result = pl.pallas_call(
            self.body,
            out_shape=[jax.ShapeDtypeStruct(v.shape, v.dtype) for v in self.outs],
            in_specs=[ANY] * len(self.ins),
            out_specs=[ANY] * len(self.outs),
            scratch_shapes=[room for _, room in self.room],
            compiler_params=pltpu.CompilerParams(
                collective_id=self.cid, has_side_effects=True, vmem_limit_bytes=VMEM_BYTES
            ),
            name=f"stage{self.cid}",
        )(*self.arrays)
        for val, array in zip(self.outs, result):
            val.array = array


def remote(src, dst, send_sem, recv_sem, peer):
    return pltpu.make_async_remote_copy(
        src_ref=src, dst_ref=dst, send_sem=send_sem, recv_sem=recv_sem,
        device_id=peer, device_id_type=MESH,
    )


class Load:
    def __init__(self, k, sources, shape, dtype, early=False):
        self.k, self.sources, self.waited = k, sources, False
        self.buf, self.sem = k.vmem(shape, dtype), k.sem(1)
        k.once.append(self)
        if early:
            k.early.append(self.start)

    def moves(self):
        for cond, source in self.sources(*spot()):
            yield cond, pltpu.make_async_copy(source, self.buf.ref, self.sem.ref.at[0])

    def start(self):
        for cond, move in self.moves():
            if cond is None:
                move.start()
            else:
                pl.when(cond)(move.start)

    def wait(self):
        if not self.waited:
            self.waited = True
            next(self.moves())[1].wait()


def load_all(k, array, early=True):
    val = k.input(array)
    return Load(k, lambda s, d, t: [(None, val.ref)], val.shape, val.dtype, early)


class Save:
    def __init__(self, k, buf):
        self.buf, self.out, self.sem = buf, k.output(buf.shape, buf.dtype), k.sem(1)
        self.waited = False
        k.once.append(self)
        k.late.append(self.wait)

    def move(self):
        return pltpu.make_async_copy(self.buf.ref, self.out.ref, self.sem.ref.at[0])

    def start(self):
        self.move().start()

    def wait(self):
        if not self.waited:
            self.waited = True
            self.move().wait()


class Task:
    final = None

    def __init__(self, k, out, axis, moves, count, n_local=1, out_dtype=BF):
        self.k, self.axis, self.make = k, axis, moves
        self.out = k.output(out, out_dtype)
        self.send_sem, self.recv_sem, self.local_sem = k.sem(count), k.sem(count), k.sem(n_local)
        self.waited = False
        k.axes.add(axis)
        k.once.append(self)

    def local(self, src, dst, i):
        return pltpu.make_async_copy(src, dst, self.local_sem.ref.at[i])

    def pairs(self, every):
        far, near = self.make(*spot())
        for i, (sources, dst, peer) in enumerate(far):
            for cond, src in sources if every else sources[:1]:
                yield cond, True, remote(
                    src, dst, self.send_sem.ref.at[i], self.recv_sem.ref.at[i], peer
                )
        for i, (sources, dst) in enumerate(near):
            for cond, src in sources if every else sources[:1]:
                yield cond, False, self.local(src, dst, i)

    def step(self):
        pass

    def send(self):
        for cond, far, move in self.pairs(True):
            if far and self.final is not None:
                cond = lax.axis_index("section") == 1 - self.final
            if cond is None:
                move.start()
            else:
                pl.when(cond)(move.start)

    def wait(self):
        if self.waited:
            return
        self.waited = True
        s = lax.axis_index("section")
        for _, far, move in self.pairs(False):
            if not far:
                move.wait()
            elif self.final is None:
                move.wait_recv()
                move.wait_send()
            else:
                pl.when(s == 1 - self.final)(move.wait_send)
                pl.when(s == self.final)(move.wait_recv)


class Part:
    def __init__(self, base, start, rows):
        self.base, self.start, self.rows = base, start, rows
        self.shape, self.dtype = (rows,) + tuple(base.shape[1:]), base.dtype
        self.array = None

    @property
    def ref(self):
        return self.base.ref.at[pl.ds(self.start, self.rows)]


def as_val(k, value):
    if isinstance(value, Part):
        return Part(as_val(k, value.base), value.start, value.rows)
    value = value.out if isinstance(value, Task) else value
    known = isinstance(value, Val) and (value.array is None)
    return value if known else k.input(value)


class Line(Task):
    def __init__(self, k, out, out_dtype=BF, n_local=1):
        super().__init__(k, out, "line", None, 6, n_local, out_dtype)
        self.send_sem, self.recv_sem = k.sem(2, 3), k.sem(2, 3)
        self.phase = 0

    def hop(self, j, way, src, dst):
        d = lax.axis_index("dp")
        peer = {"dp": (d + 1 if way == 0 else d + 3) % 4}
        return remote(src, dst, self.send_sem.ref.at[way, j], self.recv_sem.ref.at[way, j], peer)


class LineGather(Line):
    def __init__(self, k, sources, shape, dtype):
        super().__init__(k, (4,) + shape, dtype)
        self.sources = sources

    def ends(self, j, way):
        d = lax.axis_index("dp")
        if way == 0:
            return (d >= j) & (d < 3), d >= j + 1
        return (d <= 3 - j) & (d > 0), d <= 2 - j

    def copy(self, j, way, src=None):
        d = lax.axis_index("dp")
        slot = (d + 4 - j if way == 0 else d + j) % 4
        piece = self.out.ref.at[slot]
        return self.hop(j, way, piece if src is None else src, piece)

    def send(self):
        self.phase = 0
        for cond, src in self.sources(*spot()):
            own = self.local(src, self.out.ref.at[lax.axis_index("dp")], 0)
            moves = [(True if cond is None else cond, own)]
            for way in range(2):
                sends = self.ends(0, way)[0]
                moves.append((sends if cond is None else sends & cond, self.copy(0, way, src)))
            for when, move in moves:
                if when is True:
                    move.start()
                else:
                    pl.when(when)(move.start)

    def arrive(self, j):
        for way in range(2):
            pl.when(self.ends(j, way)[1])(self.copy(j, way).wait_recv)

    def step(self):
        self.arrive(self.phase)
        self.phase += 1
        for way in range(2):
            pl.when(self.ends(self.phase, way)[0])(self.copy(self.phase, way).start)

    def wait(self):
        if self.waited:
            return
        self.waited = True
        while self.phase < 2:
            self.step()
        self.arrive(2)
        for j in range(3):
            for way in range(2):
                pl.when(self.ends(j, way)[0])(self.copy(j, way).wait_send)
        d = lax.axis_index("dp")
        self.local(self.sources(*spot())[0][1], self.out.ref.at[d], 0).wait()


def z_gather_from(k, sources, shape, dtype):
    count = dp_size()
    if count == 4:
        return LineGather(k, sources, shape, dtype)

    def moves(s, d, t):
        dst, found = task.out.ref.at[d], sources(s, d, t)
        return [(found, dst, {"dp": (d + i) % count}) for i in range(1, count)], [(found, dst)]

    task = Task(k, (count,) + shape, "dp", moves, count - 1, out_dtype=dtype)
    return task


def z_gather(k, value):
    val = as_val(k, value)
    return z_gather_from(k, lambda s, d, t: [(None, val.ref)], val.shape, val.dtype)


def z_gather_half(k, shard, moved, block):
    shard, moved = as_val(k, shard), as_val(k, moved)
    rows = shard.shape[0] // 2

    def sources(s, d, t):
        own = shard.ref.at[pl.ds(block * rows, rows)]
        return [(s == block, own), (s == 1 - block, moved.ref)]

    return z_gather_from(k, sources, moved.shape, shard.dtype)


def one_way(task, sender):
    task.final = None if sender is None else 1 - sender
    return task


def z_gather_whole(k, shard, moved, block, half=None):
    shard, moved = as_val(k, shard), as_val(k, moved)
    rows = shard.shape[0] if half is None else shard.shape[0] // 2
    part = pl.ds(0 if half is None else half * rows, rows)

    def sources(s, d, t):
        return [(s == block, shard.ref.at[part]), (s == 1 - block, moved.ref.at[part])]

    return z_gather_from(k, sources, (rows,) + shard.shape[1:], shard.dtype)


def x_move(k, value, sender=None):
    val = as_val(k, value)

    def moves(s, d, t):
        return [([(None, val.ref)], task.out.ref, {"section": 1 - s})], []

    task = Task(k, val.shape, "section", moves, 1, out_dtype=val.dtype)
    return one_way(task, sender)


def x_half(k, value, sender=None):
    val = as_val(k, value)
    rows = val.shape[0] // 2

    def moves(s, d, t):
        src = val.ref.at[block_of(1 - s, rows)]
        return [([(None, src)], task.out.ref, {"section": 1 - s})], []

    task = Task(k, (rows,) + val.shape[1:], "section", moves, 1, out_dtype=val.dtype)
    return one_way(task, sender)


def x_slots(k, value, kind):
    val, count = as_val(k, value), dp_size()
    rows = val.shape[0] // (2 * count)

    def moves(s, d, t):
        far = []
        for i in range(count):
            slot = 2 * i + 1 - s if kind == "rows" else (1 - s) * count + i
            src = val.ref.at[block_of(slot, rows)]
            far.append(([(None, src)], task.out.ref.at[i], {"section": 1 - s}))
        return far, []

    task = Task(k, (count, rows) + val.shape[1:], "section", moves, count)
    return task


class Terms:
    def __init__(self, k, kind, grads, received, local):
        self.grads, self.local = as_val(k, grads), local
        self.kind, self.n = kind, dp_size()
        self.whole = received is None
        if self.whole:
            rows, cols = self.grads.shape
            self.rows = rows if kind == "cols" else rows // self.n
            self.cols = cols // self.n if kind == "cols" else cols
            self.shape = (self.n, self.rows, self.cols)
            self.aside = kind == "cols" and self.cols % 128 != 0
            self.total = k.vmem(self.shape, BF)
            self.kept = k.vmem(self.grads.shape, BF) if self.aside else self.total
            return
        self.received = as_val(k, received)
        if kind == "cols":
            self.rows, self.cols = self.grads.shape[0] // 2, self.grads.shape[1] // self.n
            held = (self.rows, self.grads.shape[1])
        else:
            self.rows, self.cols = self.grads.shape[0] // (2 * self.n), self.grads.shape[1]
            held = (self.n, self.rows, self.cols)
        self.kept, self.got = k.vmem(held, BF), k.vmem(held, BF)
        self.shape = (self.n, self.rows, self.cols)
        self.total = k.vmem(self.shape, BF) if kind == "cols" else self.kept

    def loads(self):
        s, grads, kept = lax.axis_index("section"), self.grads.ref, self.kept.ref
        if self.whole and self.aside:
            return [self.local(grads, kept, 2)]
        if self.whole:
            parts = [
                grads.at[:, pl.ds(i * self.cols, self.cols)]
                if self.kind == "cols"
                else grads.at[block_of(i, self.rows)]
                for i in range(self.n)
            ]
            return [self.local(part, kept.at[i], 2 + i) for i, part in enumerate(parts)]
        if self.kind == "cols":
            moves = [self.local(grads.at[block_of(s, self.rows)], kept, 2)]
        else:
            moves = []
            for i in range(self.n):
                slot = 2 * i + s if self.kind == "rows" else s * self.n + i
                moves.append(self.local(grads.at[block_of(slot, self.rows)], kept.at[i], 2 + i))
        return moves + [self.local(self.received.ref, self.got.ref, 1)]

    def load(self):
        for move in self.loads():
            move.start()

    def add(self):
        for move in self.loads():
            move.wait()
        if self.whole and self.aside:
            for i in range(self.n):
                self.total.ref[i] = self.kept.ref[:, i * self.cols : (i + 1) * self.cols]
        if self.whole:
            return
        kept, got, total = self.kept.ref, self.got.ref, self.total.ref
        if self.kind != "cols":

            def piece(i, carry):
                chunked(self.rows, lambda at: total.__setitem__(
                    (i, at), (kept[i, at, :].astype(F32) + got[i, at, :].astype(F32)).astype(BF)
                ))
                return carry

            lax.fori_loop(0, self.n, piece, 0)
            return

        def add_rows(at):
            for i in range(self.n):
                part = slice(i * self.cols, (i + 1) * self.cols)
                value = kept[at, part].astype(F32) + got[at, part].astype(F32)
                total[i, at, :] = value.astype(BF)

        chunked(self.rows, add_rows)


class DirectScatter(Task):
    def __init__(self, k, kind, grads, received):
        self.terms = Terms(k, kind, grads, received, lambda *a: self.local(*a))
        count = dp_size()

        def moves(s, d, t):
            total = self.terms.total.ref
            far = []
            for i in range(1, count):
                other = (d + i) % count
                far.append(([(None, total.at[other])], self.out.ref.at[d], {"dp": other}))
            return far, [([(None, total.at[d])], self.out.ref.at[d])]

        super().__init__(k, self.terms.shape, "dp", moves, count - 1, 2 + count)
        self.load = self.terms.load

    def send(self):
        self.terms.add()
        super().send()

    def add(self):
        self.load()
        self.send()


class LineScatter(Line):
    def __init__(self, k, kind, grads, received):
        self.terms = Terms(k, kind, grads, received, lambda *a: self.local(*a))
        super().__init__(k, self.terms.shape[1:], BF, 6)
        self.got = k.vmem((2, 3) + self.terms.shape[1:], BF)
        self.load = self.terms.load

    def ends(self, j, way):
        d = lax.axis_index("dp")
        if way == 0:
            return (d <= j) & (d < 3), (d >= 1) & (d <= j + 1)
        return (d >= 3 - j) & (d > 0), (d <= 2) & (d >= 2 - j)

    def copy(self, j, way):
        d = lax.axis_index("dp")
        to = (d + 3 - j if way == 0 else d + 1 + j) % 4
        return self.hop(j, way, self.terms.total.ref.at[to], self.got.ref.at[way, j])

    def send(self):
        self.phase = 0
        self.terms.add()
        for way in range(2):
            pl.when(self.ends(0, way)[0])(self.copy(0, way).start)

    def take(self, j, way):
        d = lax.axis_index("dp")
        to = (d + 2 - j if way == 0 else d + 2 + j) % 4
        self.copy(j, way).wait_recv()
        total, got = self.terms.total.ref, self.got.ref

        def add_rows(at):
            value = total[to, at, :].astype(F32) + got[way, j, at, :].astype(F32)
            total[to, at, :] = value.astype(BF)

        chunked(self.terms.rows, add_rows)

    def arrive(self, j):
        for way in range(2):
            pl.when(self.ends(j, way)[1])(functools.partial(self.take, j, way))

    def step(self):
        self.arrive(self.phase)
        self.phase += 1
        for way in range(2):
            pl.when(self.ends(self.phase, way)[0])(self.copy(self.phase, way).start)

    def wait(self):
        if self.waited:
            return
        self.waited = True
        while self.phase < 2:
            self.step()
        self.arrive(2)
        done = self.local(self.terms.total.ref.at[lax.axis_index("dp")], self.out.ref, 0)
        done.start()
        for j in range(3):
            for way in range(2):
                pl.when(self.ends(j, way)[0])(self.copy(j, way).wait_send)
        done.wait()

    def add(self):
        self.load()
        self.send()


def sum_scatter(k, kind, grads, received=None):
    return (LineScatter if dp_size() == 4 else DirectScatter)(k, kind, grads, received)


class Finish(Task):
    def __init__(self, k, pieces, block):
        self.pieces, self.final = as_val(k, pieces), block
        *slots, rows, cols = self.pieces.shape
        self.slots = slots[0] if slots else 0
        if slots:
            self.held, self.total = k.vmem(self.pieces.shape, BF), k.vmem((rows, cols), BF)
        else:
            self.total = self.pieces

        def moves(s, d, t):
            source, dst = [(None, self.total.ref)], self.out.ref.at[s]
            return [(source, dst, {"section": 1 - s})], [(source, dst)]

        super().__init__(k, (2, rows, cols), "section", moves, 1, 2)

    def load(self):
        if self.slots:
            self.local(self.pieces.ref, self.held.ref, 1).start()

    def send(self):
        if self.slots:
            self.local(self.pieces.ref, self.held.ref, 1).wait()
            acc = self.held.ref[0].astype(F32)
            for i in range(1, self.slots):
                acc = acc + self.held.ref[i].astype(F32)
            self.total.ref[...] = acc.astype(BF)
        super().send()

    def add(self):
        self.load()
        self.send()


class SumShare(Task):
    def __init__(self, k, terms, axis, slotted=False):
        self.terms = [as_val(k, v) for v in terms]
        shape = self.terms[0].shape[1:] if slotted else self.terms[0].shape
        count = dp_size() if axis == "dp" else 4
        self.slotted = slotted
        self.bufs = [k.vmem(v.shape, F32) for v in self.terms]
        self.total = k.vmem(shape, F32)

        def moves(s, d, t):
            source, me = [(None, self.total.ref)], d if axis == "dp" else t
            dst = self.out.ref.at[me]
            far = [(source, dst, {axis: (me + i) % count}) for i in range(1, count)]
            return far, [(source, dst)]

        super().__init__(k, (count,) + shape, axis, moves, count - 1, 3, out_dtype=F32)

    def add(self):
        loads = [self.local(v.ref, b.ref, 1 + i) for i, (v, b) in enumerate(zip(self.terms, self.bufs))]
        for load in loads:
            load.start()
        for load in loads:
            load.wait()
        if self.slotted:
            parts = [self.bufs[0].ref[i] for i in range(self.terms[0].shape[0])]
        else:
            parts = [buf.ref[...] for buf in self.bufs]
        acc = parts[0]
        for part in parts[1:]:
            acc = acc + part
        self.total.ref[...] = acc
        self.send()


class Weight:
    def __init__(self, k, kind, *segments, early=False):
        self.kind, self.waited = kind, False
        self.segments, start = [], 0
        for near, far in segments:
            near, far = as_val(k, near), None if far is None else as_val(k, far)
            self.segments.append((near, far, start))
            start += near.shape[1] * (1 if far is None else 2)
        self.count, _, self.cols = self.segments[0][0].shape
        self.rows = start
        if kind == "cols":
            shape = (self.rows, self.count * self.cols)
        else:
            shape = (self.count * self.rows, self.cols)
        self.aside = kind == "cols" and self.cols % 128 != 0
        self.buf = k.vmem(shape, BF)
        sides = [v for near, far, _ in self.segments for v in (near, far) if v is not None]
        self.sem = k.sem(len(sides), self.count)
        if self.aside:
            self.held = [k.vmem(v.shape, BF) for v in sides]
        k.once.append(self)
        if early:
            k.early.append(self.start)

    def sides(self):
        s = lax.axis_index("section")
        for near, far, start in self.segments:
            rows = near.shape[1]
            if far is None:
                yield near, start, None
            else:
                yield near, start + s * rows, s
                yield far, start + (1 - s) * rows, 1 - s

    def moves(self):
        dst = self.buf.ref
        for j, (val, start, sec) in enumerate(self.sides()):
            rows = val.shape[1]
            for i in range(self.count):
                if self.aside:
                    to = self.held[j].ref.at[i]
                elif self.kind == "cols":
                    at = pl.ds(pl.multiple_of(start, 16), rows)
                    to = dst.at[at, pl.ds(i * self.cols, self.cols)]
                else:
                    top = (sec * self.count + i) * rows if self.kind == "conv" else i * self.rows + start
                    to = dst.at[pl.ds(pl.multiple_of(top, 16), rows)]
                yield pltpu.make_async_copy(val.ref.at[i], to, self.sem.ref.at[j, i])

    def start(self):
        for move in self.moves():
            move.start()

    def wait(self):
        if self.waited:
            return
        self.waited = True
        for move in self.moves():
            move.wait()
        if self.aside:
            for j, (val, start, _) in enumerate(self.sides()):
                whole = jnp.concatenate([self.held[j].ref[i] for i in range(self.count)], axis=1)
                self.buf.ref[pl.ds(pl.multiple_of(start, 16), val.shape[1]), :] = whole


class Product:
    def __init__(self, k, left, right):
        self.left, self.right = left, right
        rows = left.shape[1]
        self.chunk = 384 if rows % 384 == 0 else 256
        self.count = rows // self.chunk
        self.buf = k.vmem((rows, right.shape[1]), BF)
        self.out, self.sem = k.output(self.buf.shape, BF), k.sem(self.count)

    def copy(self, i):
        part = block_of(i, self.chunk)
        return pltpu.make_async_copy(self.buf.ref.at[part], self.out.ref.at[part], self.sem.ref.at[i])

    def run(self):
        def step(i, carry):
            part = block_of(i, self.chunk)
            value = contract(self.left.ref[:, part], self.right.ref[...], 0, 0)
            self.buf.ref[part, :] = value.astype(BF)
            self.copy(i).start()
            return carry

        lax.fori_loop(0, self.count, step, 0)

    def wait(self):
        for i in range(self.count):
            self.copy(i).wait()


def places():
    me = lax.axis_index("tensor")
    sib = me + 1 - 2 * (me % 2)
    cross = (me + 2) % 4
    diag = (sib + 2) % 4
    return me, sib, cross, diag


class Gather:
    def __init__(self, k, x, gain, weights, extras=(), trans=False, epilogue="plain", save=()):
        rows, width = x.shape
        length = 4 * rows
        self.k, self.x, self.gain, self.weights, self.extras = k, x, gain, weights, extras
        self.trans, self.epilogue, self.rows, self.half = trans, epilogue, rows, rows // 2
        cols = [w.buf.shape[0 if trans else 1] for w in weights]
        kinds = {
            "plain": [(c, F32) for c in cols],
            "ffn": [(cols[0], BF)] * 3,
            "ffn_back": [(cols[0], BF)] * 2,
        }[epilogue]
        self.full = k.vmem((length, width), BF)
        self.values = [k.vmem((length, c), kind) for c, kind in kinds]
        kept = [self.full] + self.values
        self.saved = [(v, k.output(v.shape, v.dtype), k.sem(4, 2)) for v in kept if kept.index(v) in save]
        self.sems = [k.sem(2) for _ in range(6)]
        k.late.append(self.end)

    def span(self, owner, sub):
        return pl.ds(pl.multiple_of(owner * self.rows + sub * self.half, self.half), self.half)

    def move(self, kind, i):
        me, sib, cross, _ = places()
        full = self.full.ref
        owner, peer, at = {"cross": (me, cross, 0), "sib": (me, sib, 2), "relay": (cross, sib, 4)}[kind]
        part = full.at[self.span(owner, i)]
        return remote(
            part, part, self.sems[at].ref.at[i], self.sems[at + 1].ref.at[i], {"tensor": peer}
        )

    def begin(self):
        me = places()[0]
        for i in range(2):

            def put(j, carry):
                at = i * self.half + j * STRIP
                part = self.x.ref[pl.ds(pl.multiple_of(at, STRIP), STRIP), :].astype(F32)
                if self.gain is not None:
                    val, row = self.gain
                    part = norm_rows(part, val.ref[row : row + 1, :])
                to = pl.ds(pl.multiple_of(me * self.rows + at, STRIP), STRIP)
                self.full.ref[to, :] = part.astype(BF)
                return carry

            lax.fori_loop(0, self.half // STRIP, put, 0)
            self.move("cross", i).start()
            self.move("sib", i).start()

    def loop(self):
        me, sib, cross, diag = places()
        rows, half = self.rows, self.half
        for w in self.weights:
            w.wait()

        def step(p, carry):
            far, sub = p // 2, p % 2
            near = (1 - sub) * me + sub * sib
            first = (1 - far) * near * rows + far * (cross * rows + sub * half)
            second = (1 - far) * (near * rows + half) + far * (diag * rows + sub * half)
            pair = [pl.ds(pl.multiple_of(v, half), half) for v in (first, second)]

            @pl.when(p == 1)
            def _():
                self.move("sib", 0).wait_recv()
                self.move("sib", 1).wait_recv()

            for i in range(2):

                @pl.when(p == 2 + i)
                def _():
                    self.move("cross", i).wait_recv()
                    self.move("relay", i).start()
                    self.move("relay", i).wait_recv()

            def both(val):
                return jnp.concatenate([val.ref[pair[0], :], val.ref[pair[1], :]], axis=0)

            a = both(self.full)
            prods = [contract(a, w.buf.ref[...], 1, 1 if self.trans else 0) for w in self.weights]
            if self.epilogue == "plain":
                values = prods
            elif self.epilogue == "ffn":
                sig, silu = silu_parts(prods[0])
                values = [prods[0], prods[1], silu * prods[1]]
            else:
                gate, up = (both(v).astype(F32) for v in self.extras)
                sig, silu = silu_parts(gate)
                values = [prods[0] * up * sig * (1.0 + gate * (1.0 - sig)), prods[0] * silu]
            for val, value in zip(self.values, values):
                value = value.astype(val.dtype)
                for j in range(2):
                    val.ref[pair[j], :] = value[j * half : (j + 1) * half]
            for val, out, sem in self.saved:
                for j in range(2):
                    pltpu.make_async_copy(
                        val.ref.at[pair[j]], out.ref.at[pair[j]], sem.ref.at[p, j]
                    ).start()
            return carry

        lax.fori_loop(0, 4, step, 0)

    def end(self):
        for i in range(2):
            for kind in ("cross", "sib", "relay"):
                self.move(kind, i).wait_send()
        part = pl.ds(0, self.half)
        for val, out, sem in self.saved:
            for p in range(4):
                for j in range(2):
                    pltpu.make_async_copy(val.ref.at[part], out.ref.at[part], sem.ref.at[p, j]).wait()


class Scatter:
    def __init__(self, k, operands, weights, resid, back=None, trans=False, low=False):
        rows, width = resid.shape
        half = rows // 2
        self.operands, self.weights, self.resid, self.back = operands, weights, resid, back
        self.trans, self.low, self.rows, self.half = trans, low, rows, half
        self.keep, self.own = k.vmem((2, half, width), F32), k.vmem((rows, width), F32)
        self.to_s, self.from_s, self.to_c, self.from_c = (
            k.vmem((2, half, width), BF) for _ in range(4)
        )
        self.to_o, self.from_o = k.vmem((rows, width), BF), k.vmem((rows, width), BF)
        self.out = k.vmem((rows, width), BF if low else F32)
        self.gain_grad = k.vmem((1, width), F32) if back else None
        self.sems = [k.sem(2) for _ in range(4)] + [k.sem(1) for _ in range(2)]
        k.late.append(self.end)

    def move(self, kind, i=0):
        _, sib, cross, _ = places()
        at, src, dst, peer = {
            "diag": (0, self.to_s, self.from_s, sib),
            "cross": (2, self.to_c, self.from_c, cross),
            "near": (4, self.to_o, self.from_o, sib),
        }[kind]
        src, dst = (src.ref, dst.ref) if kind == "near" else (src.ref.at[i], dst.ref.at[i])
        return remote(
            src, dst, self.sems[at].ref.at[i], self.sems[at + 1].ref.at[i], {"tensor": peer}
        )

    def pass_on(self, i):
        self.move("diag", i).wait_recv()

        def add_rows(at):
            total = self.keep.ref[i, at, :] + self.from_s.ref[i, at, :].astype(F32)
            self.to_c.ref[i, at, :] = total.astype(BF)

        chunked(self.half, add_rows)
        self.move("cross", i).start()

    def loop(self):
        me, sib, cross, diag = places()
        rows, half = self.rows, self.half
        for w in self.weights:
            w.wait()

        def step(p, carry):
            near, sub = p // 2, p % 2
            base = near * ((1 - sub) * sib + sub * me) * rows
            first = base + (1 - near) * (cross * rows + sub * half)
            second = base + near * half + (1 - near) * (diag * rows + sub * half)
            pair = [pl.ds(pl.multiple_of(v, half), half) for v in (first, second)]
            total = None
            for y, w in zip(self.operands, self.weights):
                a = jnp.concatenate([y.ref[pair[0], :], y.ref[pair[1], :]], axis=0)
                prod = contract(a, w.buf.ref[...], 1, 1 if self.trans else 0)
                total = prod if total is None else total + prod

            self.own.ref[...] = total

            @pl.when(p < 2)
            def _():
                def put(at):
                    self.keep.ref[p, at, :] = self.own.ref[at, :]
                    lower = pl.ds(pl.multiple_of(at.start + half, 16), at.size)
                    self.to_s.ref[p, at, :] = self.own.ref[lower, :].astype(BF)

                chunked(half, put)
                self.move("diag", p).start()

            @pl.when(p == 2)
            def _():
                def put(at):
                    self.to_o.ref[at, :] = self.own.ref[at, :].astype(BF)

                chunked(rows, put)
                self.move("near").start()

            @pl.when((p == 1) | (p == 2))
            def _():
                self.pass_on(p - 1)

            return carry

        lax.fori_loop(0, 4, step, 0)

    def finish(self):
        self.move("near").wait_recv()
        if self.back:
            self.gain_grad.ref[...] = jnp.zeros_like(self.gain_grad.ref)
        for i in range(2):
            self.move("cross", i).wait_recv()

            def add_rows(j, carry):
                inner = block_of(j, STRIP)
                part = pl.ds(pl.multiple_of(i * self.half + j * STRIP, STRIP), STRIP)
                total = self.own.ref[part, :] + self.from_o.ref[part, :].astype(F32)
                total = total + self.from_c.ref[i, inner, :].astype(F32)
                resid = self.resid.ref[part, :].astype(F32)
                if self.back:
                    value, (gain, row) = self.back
                    total, gain_grad = norm_back(
                        value.ref[part, :].astype(F32), gain.ref[row : row + 1, :], total
                    )
                    self.gain_grad.ref[...] += gain_grad
                self.out.ref[part, :] = (resid + total).astype(self.out.dtype)
                return carry

            lax.fori_loop(0, self.half // STRIP, add_rows, 0)

    def end(self):
        self.move("near").wait_send()
        for i in range(2):
            self.move("diag", i).wait_send()
            self.move("cross", i).wait_send()


def delayed(values, by):
    if by == 0:
        return values
    row = lax.broadcasted_iota(jnp.int32, values.shape, 0)
    return jnp.where(row < by, 0.0, pltpu.roll(values, by, 0))


def advanced(values, by):
    if by == 0:
        return values
    length = values.shape[0]
    row = lax.broadcasted_iota(jnp.int32, values.shape, 0)
    return jnp.where(row >= length - by, 0.0, pltpu.roll(values, length - by, 0))


CONV_COLS = 128


class Conv:
    def __init__(self, k, projected, value, kernel):
        self.projected, self.value, self.kernel = projected, value, kernel
        self.y = k.vmem(value.shape, BF)

    def parts(self, j):
        channels = self.value.shape[1]
        at = block_of(j, CONV_COLS)
        b_gate = self.projected.ref[:, at]
        c_gate = self.projected.ref[:, block_of(j + channels // CONV_COLS, CONV_COLS)]
        x_value, taps = self.value.ref[:, at], self.kernel.ref[:, at]
        product = b_gate * x_value
        count = taps.shape[0]
        causal = jnp.zeros_like(product)
        for i in range(count):
            causal = causal + taps[i : i + 1] * delayed(product, count - 1 - i)
        return at, b_gate, c_gate, x_value, taps, product, causal

    def run(self):
        def step(j, carry):
            at, _, c_gate, _, _, _, causal = self.parts(j)
            self.y.ref[:, at] = (c_gate * causal).astype(BF)
            return carry

        lax.fori_loop(0, self.value.shape[1] // CONV_COLS, step, 0)


class ConvBack(Conv):
    def __init__(self, k, projected, value, kernel, d_y):
        self.projected, self.value, self.kernel, self.d_y = projected, value, kernel, d_y
        self.d_proj = k.vmem(projected.shape, BF)
        self.d_value = k.vmem(value.shape, BF)
        self.d_kernel = k.vmem(kernel.shape, F32)

    def run(self):
        channels = self.value.shape[1]

        def step(j, carry):
            at, b_gate, c_gate, x_value, taps, product, causal = self.parts(j)
            d_y = self.d_y.ref[:, at]
            d_causal = d_y * c_gate
            count = taps.shape[0]
            d_product = jnp.zeros_like(product)
            for i in range(count):
                by = count - 1 - i
                row = jnp.sum(d_causal * delayed(product, by), axis=0, keepdims=True)
                self.d_kernel.ref[i : i + 1, at] = row
                d_product = d_product + taps[i : i + 1] * advanced(d_causal, by)
            self.d_proj.ref[:, at] = (d_product * x_value).astype(BF)
            upper = block_of(j + channels // CONV_COLS, CONV_COLS)
            self.d_proj.ref[:, upper] = (d_y * causal).astype(BF)
            self.d_value.ref[:, at] = (d_product * b_gate).astype(BF)
            return carry

        lax.fori_loop(0, channels // CONV_COLS, step, 0)


def head_mean(values, head_size):
    width = values.shape[1]
    row = lax.broadcasted_iota(jnp.int32, (width, width), 0) // head_size
    col = lax.broadcasted_iota(jnp.int32, (width, width), 1) // head_size
    group = jnp.where(row == col, 1.0 / head_size, 0.0).astype(F32)
    return lax.dot_general(
        values, group, (((1,), (0,)), ((), ())),
        precision=lax.Precision.HIGHEST, preferred_element_type=F32,
    )


def turn(values, head_size, back):
    width, half = values.shape[1], head_size // 2
    lane = lax.broadcasted_iota(jnp.int32, values.shape, 1) % head_size
    upper = pltpu.roll(values, width - half, 1)
    lower = pltpu.roll(values, half, 1)
    return jnp.where(lane < half, upper, -lower) if back else jnp.where(lane < half, -upper, lower)


def head_norm(values, gain, head_size):
    return values * lax.rsqrt(head_mean(values * values, head_size) + EPS) * gain


def head_norm_back(values, gain, grad_in, head_size):
    row_scale = lax.rsqrt(head_mean(values * values, head_size) + EPS)
    normed = values * row_scale
    gain_grad = jnp.sum(grad_in * normed, axis=0, keepdims=True)
    scaled = grad_in * gain
    return row_scale * (scaled - normed * head_mean(scaled * normed, head_size)), gain_grad


def block_weights(q_rows, keys):
    scores = [contract(q_rows, k_rows, 1, 1) for k_rows in keys]
    query = lax.broadcasted_iota(jnp.int32, scores[-1].shape, 0)
    key = lax.broadcasted_iota(jnp.int32, scores[-1].shape, 1)
    scores[-1] = jnp.where(key <= query, scores[-1], MASKED)
    top = functools.reduce(
        jnp.maximum, [jnp.max(part, axis=1, keepdims=True) for part in scores]
    )
    exps = [jnp.exp(part - top) for part in scores]
    scale = 1.0 / sum(jnp.sum(part, axis=1, keepdims=True) for part in exps)
    return [part * scale for part in exps]


def key_blocks(i):
    blocks = [pl.ds(0, i * ROW_BLOCK)] if i else []
    return blocks + [pl.ds(i * ROW_BLOCK, ROW_BLOCK)]


class Heads:
    def __init__(self, projected, tables, size):
        assert size in (16, 64, 256), size
        self.projected, self.size = projected, size
        self.gain, self.cos, self.sin = (v.buf for v in tables)
        self.loads = tables
        self.length, width = projected.shape
        self.q_cols, self.k_cols = width // 2, width // 4
        self.heads, self.kv_heads = self.q_cols // size, self.k_cols // size
        self.share = self.heads // self.kv_heads

    def per_head(self, k, count, kind):
        return k.vmem((count, self.length, self.size), kind)

    def split(self, val, rows, values):
        for h in range(val.shape[0]):
            val.ref[h, rows, :] = values[:, h * self.size : (h + 1) * self.size]

    def join(self, val, rows):
        return jnp.concatenate([val.ref[h, rows, :] for h in range(val.shape[0])], axis=1)

    def gains(self):
        gain = self.gain.ref[...]
        return (
            jnp.concatenate([gain[0:1]] * self.heads, axis=1),
            jnp.concatenate([gain[1:2]] * self.kv_heads, axis=1),
        )

    def angles(self, rows):
        c, n = self.cos.ref[rows, :], self.sin.ref[rows, :]
        repeat = self.q_cols // c.shape[1]
        return jnp.concatenate([c] * repeat, axis=1), jnp.concatenate([n] * repeat, axis=1)

    def blocks(self, step):
        lax.fori_loop(0, self.length // ROW_BLOCK, lambda p, c: step(block_of(p, ROW_BLOCK)) or c, 0)


class Attend(Heads):
    def __init__(self, k, projected, tables, size):
        super().__init__(projected, tables, size)
        self.q_rot = k.vmem((self.length, self.q_cols), BF)
        self.k_rot = k.vmem((self.length, self.k_cols), BF)
        self.y = k.vmem((self.length, self.q_cols), BF)
        self.q_h, self.y_h = (self.per_head(k, self.heads, BF) for _ in range(2))
        self.k_h, self.v_h = (self.per_head(k, self.kv_heads, BF) for _ in range(2))

    def run(self, *between):
        for load in self.loads:
            load.wait()
        size, q_cols, k_cols, proj = self.size, self.q_cols, self.k_cols, self.projected.ref

        def prepare(rows):
            c, n = self.angles(rows)
            q_gain, k_gain = self.gains()
            q = head_norm(proj[rows, :q_cols], q_gain, size)
            q = (q * c + turn(q, size, False) * n).astype(BF)
            k = head_norm(proj[rows, q_cols : q_cols + k_cols], k_gain, size)
            k = (k * c[:, :k_cols] + turn(k, size, False) * n[:, :k_cols]).astype(BF)
            self.q_rot.ref[rows, :] = q
            self.k_rot.ref[rows, :] = k
            self.split(self.q_h, rows, (q.astype(F32) * size**-0.5).astype(BF))
            self.split(self.k_h, rows, k)
            self.split(self.v_h, rows, proj[rows, q_cols + k_cols :].astype(BF))

        self.blocks(prepare)

        def head(h, carry):
            g = h // self.share

            @pl.when(h == self.heads // 2)
            def _():
                for step in between:
                    step()

            for i in range(self.length // ROW_BLOCK):
                rows, seen = pl.ds(i * ROW_BLOCK, ROW_BLOCK), key_blocks(i)
                weights = block_weights(
                    self.q_h.ref[h, rows, :], [self.k_h.ref[g, at, :] for at in seen]
                )
                value = sum(
                    contract(part.astype(BF), self.v_h.ref[g, at, :], 1, 0)
                    for part, at in zip(weights, seen)
                )
                self.y_h.ref[h, rows, :] = value.astype(BF)
            return carry

        lax.fori_loop(0, self.heads, head, 0)

        def place(rows):
            self.y.ref[rows, :] = self.join(self.y_h, rows)

        self.blocks(place)


class AttendBack(Heads):
    def __init__(self, k, projected, tables, size, q_rot, k_rot, d_y):
        super().__init__(projected, tables, size)
        self.q_rot, self.k_rot, self.d_y = q_rot, k_rot, d_y
        self.q_h, self.dy_h = (self.per_head(k, self.heads, BF) for _ in range(2))
        self.k_h, self.v_h = (self.per_head(k, self.kv_heads, BF) for _ in range(2))
        self.dq_h = self.per_head(k, self.heads, F32)
        self.dk_h, self.dv_h = (self.per_head(k, self.kv_heads, F32) for _ in range(2))
        self.d_proj = k.vmem(projected.shape, BF)
        self.q_gain, self.k_gain = k.vmem((1, self.q_cols), F32), k.vmem((1, self.k_cols), F32)

    def run(self, *between):
        for load in self.loads:
            load.wait()
        size, q_cols, k_cols, proj = self.size, self.q_cols, self.k_cols, self.projected.ref
        scale = size**-0.5
        dq_h, dk_h, dv_h = self.dq_h.ref, self.dk_h.ref, self.dv_h.ref

        def prepare(rows):
            self.split(self.q_h, rows, (self.q_rot.ref[rows, :].astype(F32) * scale).astype(BF))
            self.split(self.dy_h, rows, self.d_y.ref[rows, :].astype(BF))
            self.split(self.k_h, rows, self.k_rot.ref[rows, :])
            self.split(self.v_h, rows, proj[rows, q_cols + k_cols :].astype(BF))

        self.blocks(prepare)

        def clear(rows):
            for val in (dk_h, dv_h):
                val[:, rows, :] = jnp.zeros((self.kv_heads, ROW_BLOCK, size), F32)

        self.blocks(clear)

        def head(h, carry):
            g = h // self.share

            @pl.when(h == self.heads // 2)
            def _():
                for step in between:
                    step()

            for i in range(self.length // ROW_BLOCK):
                rows, seen = pl.ds(i * ROW_BLOCK, ROW_BLOCK), key_blocks(i)
                q, low = self.q_h.ref[h, rows, :], self.dy_h.ref[h, rows, :]
                keys = [self.k_h.ref[g, at, :] for at in seen]
                probs = block_weights(q, keys)
                d_weights = [contract(low, self.v_h.ref[g, at, :], 1, 1) for at in seen]
                inner = sum(
                    jnp.sum(a * b, axis=1, keepdims=True) for a, b in zip(probs, d_weights)
                )
                d_q = 0.0
                for at, k, prob, d_weight in zip(seen, keys, probs, d_weights):
                    dv_h[g, at, :] += contract(prob.astype(BF), low, 0, 0)
                    d_scores = (prob * (d_weight - inner)).astype(BF)
                    d_q = d_q + contract(d_scores, k, 1, 0)
                    dk_h[g, at, :] += contract(d_scores, q, 0, 0)
                dq_h[h, rows, :] = d_q * scale
            return carry

        lax.fori_loop(0, self.heads, head, 0)
        self.q_gain.ref[...] = jnp.zeros_like(self.q_gain.ref)
        self.k_gain.ref[...] = jnp.zeros_like(self.k_gain.ref)

        def finish(rows):
            c, n = self.angles(rows)
            dq, dk, dv = (self.join(v, rows) for v in (self.dq_h, self.dk_h, self.dv_h))
            dq = dq * c + turn(dq * n, size, True)
            dk = dk * c[:, :k_cols] + turn(dk * n[:, :k_cols], size, True)
            q_gain, k_gain = self.gains()
            dq, q_sum = head_norm_back(proj[rows, :q_cols], q_gain, dq, size)
            dk, k_sum = head_norm_back(proj[rows, q_cols : q_cols + k_cols], k_gain, dk, size)
            self.q_gain.ref[...] += q_sum
            self.k_gain.ref[...] += k_sum
            self.d_proj.ref[rows, :q_cols] = dq.astype(BF)
            self.d_proj.ref[rows, q_cols : q_cols + k_cols] = dk.astype(BF)
            self.d_proj.ref[rows, q_cols + k_cols :] = dv.astype(BF)

        self.blocks(finish)


def body(boundary, norm_gain, mix_in, mix_out, w_gate, w_up, w_down, conv_x, conv_kernel, qk_gain):
    first = lax.axis_index("section") == 0
    tensor_index = lax.axis_index("tensor")
    model_width = boundary.shape[3]
    channels = mix_out.shape[1]
    row_shape = boundary.shape[2:]
    length, size = 4 * row_shape[0], qk_gain.shape[1]

    seqs, own_gain = boundary[0], norm_gain[0]
    sh_in, sh_out, sh_gate, sh_up, sh_down = (v[0] for v in (mix_in, mix_out, w_gate, w_up, w_down))

    def gains_of(k, block, other, early=True):
        own, moved = k.input(own_gain), as_val(k, other)
        sources = lambda s, d, t: [(s == block, own.ref), (s == 1 - block, moved.ref)]
        return Load(k, sources, own.shape, F32, early)

    def start_rows(k, slot, other, early=True):
        own, moved = k.input(seqs), as_val(k, other)
        sources = lambda s, d, t: [(s == slot, own.ref.at[slot]), (s == 1 - slot, moved.ref)]
        return Load(k, sources, row_shape, BF, early)

    def wait(*items):
        return [item.wait for item in items]

    k = Kernel(0)
    t_seq = None
    seq_val = k.input(seqs)

    def seq_moves(s, d, t):
        return [([(None, seq_val.ref.at[1 - s])], t_seq.out.ref, {"section": 1 - s})], []

    t_in, t_out, t_up = (x_half(k, v) for v in (sh_in, sh_out, sh_up))
    gate_lo, gate_hi = (Part(sh_gate, i * (sh_gate.shape[0] // 2), sh_gate.shape[0] // 2) for i in range(2))
    down_lo, down_hi = (Part(sh_down, i * (sh_down.shape[0] // 2), sh_down.shape[0] // 2) for i in range(2))
    t_gate0a, t_gate0b = x_half(k, gate_lo, 0), x_move(k, gate_hi, 0)
    t_down0a, t_down0b = x_half(k, down_lo, 0), x_move(k, down_hi, 0)
    t_gate1, t_down1 = x_half(k, sh_gate, 1), x_move(k, sh_down, 1)
    t_seq = Task(k, row_shape, "section", seq_moves, 1)
    t_gain, z_cols = x_move(k, own_gain), z_gather(k, conv_x)
    z_in0, z_out0 = z_gather_half(k, sh_in, t_in.out, 0), z_gather_half(k, sh_out, t_out.out, 0)
    z_gate0a = z_gather_half(k, gate_lo, t_gate0a.out, 0)
    z_gate0b, x_gate0a = z_gather_whole(k, gate_hi, t_gate0b.out, 0), x_move(k, z_gate0a.out)
    z_up0 = z_gather_half(k, sh_up, t_up.out, 0)
    x_cols, x_in0, x_out0 = (x_move(k, v.out) for v in (z_cols, z_in0, z_out0))
    x_load, gain_load = start_rows(k, 0, t_seq.out, False), gains_of(k, 0, t_gain.out, False)
    taps = load_all(k, conv_kernel)
    angles = Angles(k, length, size, 128)
    w_in0, w_cols = Weight(k, "rows", (z_in0.out, x_in0.out)), Weight(k, "conv", (z_cols.out, x_cols.out))
    w_out0 = Weight(k, "cols", (z_out0.out, x_out0.out))
    g0 = Gather(k, x_load.buf, (gain_load.buf, 0), [w_in0, w_cols], save=(0, 1, 2))
    conv = Conv(k, g0.values[0], g0.values[1], taps.buf)
    y0 = Save(k, conv.y)
    s1 = Scatter(k, [conv.y], [w_out0], x_load.buf)
    mid0 = Save(k, s1.out)
    k.do(t_in.send, t_out.send, z_cols.send, t_gate0b.send, t_gate0a.send, t_gate1.send)
    k.do(t_gain.send, t_seq.send)
    k.do(t_in.wait, z_in0.send, t_out.wait, z_out0.send, z_cols.step, z_in0.step, z_out0.step)
    k.do(z_cols.step, z_in0.step, z_out0.step, t_gate0b.wait, z_gate0b.send)
    k.do(t_gate0a.wait, z_gate0a.send)
    k.do(z_cols.wait, x_cols.send, z_in0.wait, x_in0.send, z_out0.wait, x_out0.send, t_up.send)
    k.do(t_gain.wait, gain_load.start, t_seq.wait, x_load.start, gain_load.wait, x_load.wait)
    k.do(g0.begin, z_gate0b.step, z_gate0a.step, angles.run, z_gate0b.step, z_gate0a.step)
    k.do(x_cols.wait, w_cols.start, x_in0.wait, w_in0.start, z_gate0a.wait, x_gate0a.send)
    k.do(t_down0b.send, t_down0a.send, t_down1.send, t_up.wait, z_up0.send)
    k.do(g0.loop, z_up0.step, taps.wait, conv.run, y0.start)
    k.do(x_out0.wait, w_out0.start, s1.loop, z_up0.step, s1.finish, mid0.start)
    k.do(*wait(t_gate1, t_down0a, t_down0b, t_down1, z_gate0b, x_gate0a, z_up0))
    k.build()
    a0, proj0, value0 = (out for _, out, _ in g0.saved)
    table_arrays = [qk_gain] + [v.out for v in angles.saves]
    y0, mid0 = y0.out, mid0.out

    k = Kernel(1)
    x_up0, z_gate1 = x_move(k, z_up0.out), z_gather_half(k, sh_gate, t_gate1.out, 1)
    z_down0a = z_gather_half(k, down_lo, t_down0a.out, 0)
    z_down0b = z_gather_whole(k, down_hi, t_down0b.out, 0)
    z_in1, z_out1 = z_gather_half(k, sh_in, t_in.out, 1), z_gather_half(k, sh_out, t_out.out, 1)
    x_down0a, x_in1, x_out1 = (x_move(k, v.out) for v in (z_down0a, z_in1, z_out1))
    rows, gain_load = load_all(k, mid0), gains_of(k, 0, t_gain.out)
    w_gate0 = Weight(k, "rows", (z_gate0a.out, x_gate0a.out), (z_gate0b.out, None), early=True)
    w_up0 = Weight(k, "rows", (z_up0.out, x_up0.out))
    w_down0 = Weight(k, "cols", (z_down0a.out, x_down0a.out), (z_down0b.out, None))
    g2 = Gather(
        k, rows.buf, (gain_load.buf, 1), [w_gate0, w_up0], epilogue="ffn", save=(0, 1, 2, 3)
    )
    s3 = Scatter(k, [g2.values[2]], [w_down0], rows.buf, low=True)
    z_rows = Save(k, s3.out)
    k.do(x_up0.send, z_down0a.send, z_down0b.send, rows.wait, gain_load.wait, g2.begin)
    k.do(z_in1.send, z_out1.send, z_down0a.step, z_in1.step, z_out1.step, z_down0b.step)
    k.do(z_down0a.step, z_in1.step, z_out1.step, z_gate1.send, z_down0a.wait, x_down0a.send)
    k.do(x_up0.wait, w_up0.start, z_down0b.step, g2.loop, z_gate1.step)
    k.do(z_in1.wait, x_in1.send, z_out1.wait, x_out1.send, z_down0b.wait, x_down0a.wait)
    k.do(w_down0.start, s3.loop, z_gate1.step, s3.finish, z_rows.start)
    k.do(*wait(x_in1, x_out1, z_gate1))
    k.build()
    m0, gate0, up0, hid0 = (out for _, out, _ in g2.saved)
    z_rows = z_rows.out

    k = Kernel(2)
    x_gate1, z_up1 = x_move(k, z_gate1.out), z_gather_half(k, sh_up, t_up.out, 1)
    z_down1a, z_down1b = (z_gather_whole(k, sh_down, t_down1.out, 1, i) for i in range(2))
    x_up1 = x_move(k, z_up1.out)
    rows, gain_load = load_all(k, z_rows), gains_of(k, 1, t_gain.out)
    tables = [load_all(k, v) for v in table_arrays]
    w_in1 = Weight(k, "rows", (z_in1.out, x_in1.out), early=True)
    w_out1 = Weight(k, "cols", (z_out1.out, x_out1.out), early=True)
    g4 = Gather(k, rows.buf, (gain_load.buf, 0), [w_in1], save=(0, 1))
    attend = Attend(k, g4.values[0], tables, size)
    kept = [Save(k, v) for v in (attend.q_rot, attend.k_rot, attend.y)]
    s5 = Scatter(k, [attend.y], [w_out1], rows.buf)
    mid1 = Save(k, s5.out)
    k.do(x_gate1.send, z_up1.send, rows.wait, gain_load.wait, g4.begin, z_up1.step)
    k.do(z_down1a.send, g4.loop, z_up1.step, z_down1b.send)
    k.do(lambda: attend.run(z_up1.wait, x_up1.send, z_down1a.step))
    k.do(*(v.start for v in kept))
    k.do(z_down1b.step, s5.loop, z_down1a.step, z_down1b.step, s5.finish, mid1.start)
    k.do(*wait(x_gate1, x_up1, z_down1a, z_down1b))
    k.build()
    a1, proj1 = (out for _, out, _ in g4.saved)
    q_rot, k_rot, y1 = (v.out for v in kept)
    mid1 = mid1.out

    k = Kernel(3)
    rows, gain_load = load_all(k, mid1), gains_of(k, 1, t_gain.out)
    cot = start_rows(k, 1, t_seq.out)
    w_gate1 = Weight(k, "rows", (z_gate1.out, x_gate1.out), early=True)
    w_up1 = Weight(k, "rows", (z_up1.out, x_up1.out), early=True)
    w_down1 = Weight(k, "cols", (z_down1a.out, None), (z_down1b.out, None), early=True)
    g6 = Gather(k, rows.buf, (gain_load.buf, 1), [w_gate1, w_up1], epilogue="ffn")
    g8 = Gather(
        k, cot.buf, None, [w_down1], [g6.values[0], g6.values[1]], trans=True, epilogue="ffn_back"
    )
    p_down1 = Product(k, g6.values[2], g8.full)
    p_gate1, p_up1 = Product(k, g6.full, g8.values[0]), Product(k, g6.full, g8.values[1])
    s9 = Scatter(k, g8.values, [w_gate1, w_up1], cot.buf, (rows.buf, (gain_load.buf, 1)), True)
    hid1 = Save(k, g6.values[2])
    d_mid1, gain11 = Save(k, s9.out), Save(k, s9.gain_grad)
    k.do(rows.wait, gain_load.wait, g6.begin, cot.wait, g8.begin, g6.loop, hid1.start, g8.loop)
    k.do(s9.loop, p_down1.run, p_gate1.run, p_up1.run)
    k.do(s9.finish, d_mid1.start, gain11.start, p_down1.wait, p_gate1.wait, p_up1.wait)
    k.build()
    hid1, d_mid1, gain11 = hid1.out, d_mid1.out, gain11.out

    k = Kernel(4)
    r_down1 = x_half(k, p_down1.out)
    r_gate1, q_up1 = x_slots(k, p_gate1.out, "rows"), sum_scatter(k, "rows", p_up1.out)
    rows, gain_load = load_all(k, d_mid1), gains_of(k, 1, t_gain.out)
    value = load_all(k, z_rows)
    tables = [load_all(k, v) for v in table_arrays]
    proj, q_load, k_load, y_load, a_load = (load_all(k, v) for v in (proj1, q_rot, k_rot, y1, a1))
    w_in1 = Weight(k, "rows", (z_in1.out, x_in1.out), early=True)
    w_out1 = Weight(k, "cols", (z_out1.out, x_out1.out), early=True)
    g10 = Gather(k, rows.buf, None, [w_out1], trans=True)
    p_out1 = Product(k, y_load.buf, g10.full)
    back = AttendBack(k, proj.buf, tables, size, q_load.buf, k_load.buf, g10.values[0])
    p_in1 = Product(k, a_load.buf, back.d_proj)
    r_out1 = x_half(k, p_out1.out)
    s11 = Scatter(
        k, [back.d_proj], [w_in1], rows.buf, (value.buf, (gain_load.buf, 0)), True, low=True
    )
    d_z, gain10 = Save(k, s11.out), Save(k, s11.gain_grad)
    head_gains = [Save(k, back.q_gain), Save(k, back.k_gain)]
    k.early.append(q_up1.load)
    k.do(r_down1.send, r_gate1.send, rows.wait, g10.begin, q_up1.send, g10.loop)
    k.do(y_load.wait, p_out1.run, q_up1.step, p_out1.wait, r_out1.send)
    k.do(proj.wait, q_load.wait, k_load.wait, lambda: back.run(q_up1.step))
    k.do(*(v.start for v in head_gains))
    k.do(gain_load.wait, value.wait, s11.loop, a_load.wait, p_in1.run)
    k.do(s11.finish, d_z.start, gain10.start, p_in1.wait)
    k.do(*wait(r_down1, q_up1, r_gate1, r_out1))
    k.build()
    d_z, gain10 = d_z.out, gain10.out
    q_gain, k_gain = (v.out for v in head_gains)

    k = Kernel(5)
    q_gate1, m_up1 = sum_scatter(k, "rows", p_gate1.out, r_gate1.out), x_move(k, q_up1.out, 0)
    q_out1 = sum_scatter(k, "cols", p_out1.out, r_out1.out)
    r_in1 = x_slots(k, p_in1.out, "rows")
    q_in1 = sum_scatter(k, "rows", p_in1.out, r_in1.out)
    q_down1 = sum_scatter(k, "cols", p_down1.out, r_down1.out)
    rows, value, gain_load = load_all(k, d_z), load_all(k, mid0), gains_of(k, 0, t_gain.out)
    gate_load, up_load, hid_load, m_load = (load_all(k, v) for v in (gate0, up0, hid0, m0))
    w_gate0 = Weight(k, "rows", (z_gate0a.out, x_gate0a.out), (z_gate0b.out, None), early=True)
    w_up0 = Weight(k, "rows", (z_up0.out, x_up0.out), early=True)
    w_down0 = Weight(k, "cols", (z_down0a.out, x_down0a.out), (z_down0b.out, None), early=True)
    g12 = Gather(
        k, rows.buf, None, [w_down0], [gate_load.buf, up_load.buf], trans=True, epilogue="ffn_back"
    )
    p_down0 = Product(k, hid_load.buf, g12.full)
    p_gate0, p_up0 = Product(k, m_load.buf, g12.values[0]), Product(k, m_load.buf, g12.values[1])
    r_down0 = x_half(k, p_down0.out)
    s13 = Scatter(
        k, g12.values, [w_gate0, w_up0], rows.buf, (value.buf, (gain_load.buf, 1)), True
    )
    d_mid0, gain01 = Save(k, s13.out), Save(k, s13.gain_grad)
    k.early += [q_gate1.load, q_down1.load, q_out1.load]
    k.do(r_in1.send, m_up1.send, rows.wait, g12.begin, q_gate1.send, q_down1.send, q_out1.send)
    k.do(gate_load.wait, up_load.wait, g12.loop, hid_load.wait, p_down0.run)
    k.do(q_gate1.step, p_down0.wait, r_down0.send, q_down1.step, q_out1.step, r_in1.wait, q_in1.add)
    k.do(s13.loop, q_gate1.step, q_down1.step, q_out1.step)
    k.do(m_load.wait, p_gate0.run, q_in1.step, p_up0.run, value.wait, gain_load.wait)
    k.do(s13.finish, d_mid0.start, gain01.start, q_in1.step, p_gate0.wait, p_up0.wait)
    k.do(*wait(q_gate1, q_out1, q_in1, q_down1, m_up1, r_down0))
    k.build()
    d_mid0, gain01 = d_mid0.out, gain01.out

    k = Kernel(6)
    r_gate0 = x_slots(k, p_gate0.out, "rows")
    q_gate0 = sum_scatter(k, "rows", p_gate0.out, r_gate0.out)
    q_down0 = sum_scatter(k, "cols", p_down0.out, r_down0.out)
    q_up0 = sum_scatter(k, "rows", p_up0.out)
    m_up0 = x_move(k, q_up0.out, 1)
    e_down1 = Finish(k, q_down1.out, 1)
    e_gate1, e_out1, e_in1 = (Finish(k, v.out, 1) for v in (q_gate1, q_out1, q_in1))
    rows, gain_load = load_all(k, d_mid0), gains_of(k, 0, t_gain.out)
    x_load, taps = start_rows(k, 0, t_seq.out), load_all(k, conv_kernel)
    y_load, a_load, proj, value = (load_all(k, v) for v in (y0, a0, proj0, value0))
    w_in0 = Weight(k, "rows", (z_in0.out, x_in0.out), early=True)
    w_cols = Weight(k, "conv", (z_cols.out, x_cols.out), early=True)
    w_out0 = Weight(k, "cols", (z_out0.out, x_out0.out), early=True)
    g14 = Gather(k, rows.buf, None, [w_out0], trans=True)
    p_out0 = Product(k, y_load.buf, g14.full)
    back = ConvBack(k, proj.buf, value.buf, taps.buf, g14.values[0])
    p_in0, p_cols = Product(k, a_load.buf, back.d_proj), Product(k, a_load.buf, back.d_value)
    r_out0, r_in0 = x_half(k, p_out0.out), x_slots(k, p_in0.out, "rows")
    r_cols = x_slots(k, p_cols.out, "conv")
    q_out0, q_in0 = sum_scatter(k, "cols", p_out0.out, r_out0.out), sum_scatter(k, "rows", p_in0.out, r_in0.out)
    q_cols = sum_scatter(k, "conv", p_cols.out, r_cols.out)
    e_down0, e_gate0, e_out0, e_in0 = (
        Finish(k, v.out, 0) for v in (q_down0, q_gate0, q_out0, q_in0)
    )
    s15 = Scatter(
        k, [back.d_proj, back.d_value], [w_in0, w_cols], rows.buf,
        (x_load.buf, (gain_load.buf, 0)), True, low=True,
    )
    d_x = Save(k, s15.out)
    tap_rows = conv_kernel.shape[0]
    small = k.vmem((8, model_width), F32)
    small_out = Save(k, small)
    ready = [load_all(k, v) for v in (gain01, gain10, gain11)]
    head_loads = [load_all(k, v) for v in (q_gain, k_gain)]

    def fill_small():
        t = lax.axis_index("tensor")
        small.ref[...] = jnp.zeros_like(small.ref)
        small.ref[0:1, :] = s15.gain_grad.ref[...]
        for i, load in enumerate(ready):
            load.wait()
            small.ref[i + 1 : i + 2, :] = load.buf.ref[...]
        small.ref[4 : 4 + tap_rows, block_of(t, channels)] = back.d_kernel.ref[...]
        at = 0
        for load in head_loads:
            load.wait()
            width = load.buf.shape[1]
            small.ref[7:8, at : at + width] = load.buf.ref[...]
            at += width
        small_out.start()

    t_small = x_move(k, small_out.out)
    z_small = SumShare(k, [small_out.out, t_small.out], "dp")
    t_total = SumShare(k, [z_small.out], "tensor", slotted=True)
    hid_load, mid_load = load_all(k, hid1), load_all(k, mid1)
    w_down1 = Weight(k, "cols", (z_down1a.out, None), (z_down1b.out, None), early=True)
    s7 = Scatter(k, [hid_load.buf], [w_down1], mid_load.buf, low=True)
    y_rows = Save(k, s7.out)
    t_x, t_y = x_move(k, d_x.out, 1), x_move(k, y_rows.out, 0)
    k.early += [q_up0.load, q_down0.load]
    k.early += [v.load for v in (e_down1, e_gate1, e_out1, e_in1)]
    k.do(r_gate0.send, q_up0.send, rows.wait, g14.begin, q_down0.send)
    k.do(e_down1.send, e_gate1.send, e_out1.send, e_in1.send, g14.loop)
    k.do(y_load.wait, p_out0.run, p_out0.wait, r_out0.send, q_up0.step)
    k.do(proj.wait, value.wait, taps.wait, back.run, q_down0.step, a_load.wait)
    k.do(p_in0.run, p_cols.run, p_in0.wait, r_in0.send, p_cols.wait, r_cols.send)
    k.do(r_gate0.wait, q_gate0.add, x_load.wait, gain_load.wait, s15.loop, q_up0.step)
    k.do(q_down0.step, s15.finish, d_x.start, fill_small, d_x.wait, t_x.send)
    k.do(small_out.wait, t_small.send, q_gate0.step, hid_load.wait, mid_load.wait, s7.loop)
    k.do(r_out0.wait, q_out0.add, r_in0.wait, q_in0.add)
    k.do(r_cols.wait, q_cols.add, q_up0.wait, m_up0.send, q_down0.wait, e_down0.add)
    k.do(s7.finish, y_rows.start, y_rows.wait, t_y.send)
    k.do(q_gate0.step, q_out0.step, q_in0.step, q_cols.step, t_small.wait, z_small.add)
    k.do(q_gate0.wait, e_gate0.add, q_out0.step, q_in0.step, q_cols.step)
    k.do(z_small.wait, t_total.add, q_out0.wait, e_out0.add, q_in0.wait, e_in0.add)
    rest = (e_down1, e_gate1, e_out1, e_in1, q_cols, e_down0, e_gate0, m_up0, e_out0, e_in0)
    k.do(*wait(*rest, t_total, t_x, t_y))
    k.build()

    owned = [
        ([e_in0], [e_in1], 1),
        ([e_out0], [e_out1], 1),
        ([e_gate0], [e_gate1], 1),
        ([q_up0, m_up0], [q_up1, m_up1], 1),
        ([e_down0], [e_down1], 1),
        ([q_cols], [q_cols], 0),
    ]
    return pack(
        [(zero, one, lead) for zero, one, lead in owned], t_total, d_x.out, y_rows.out, t_x, t_y,
        (norm_gain.shape, conv_kernel.shape, qk_gain.shape),
    )


def slot_free(val, shape):
    value = val.out.array
    if value.ndim == 3 and value.shape[0] * value.shape[1] != shape[0]:
        value = jnp.sum(value.astype(F32), axis=0).astype(BF)
    return value.reshape(shape)


def pack_kernel(plan, *refs):
    n_in, leads, terms, tap_rows = plan
    ins, rest = refs[:n_in], refs[n_in:]
    result, gain_out, *grads, cols, taps, heads = rest[: len(leads) + 4]
    grads = [*grads, cols]
    room = iter(rest[len(leads) + 4 :])
    own_v, moved_v, small_v, *bufs = (next(room) for _ in range(3 + len(terms)))
    out_v = [next(room) for _ in leads]
    load_sem, store_sem = room
    s, t = lax.axis_index("section"), lax.axis_index("tensor")
    small, d_x, y_rows, moved, moved_y, *parts = ins

    def either(cond, zero, one, dst, sem):
        if zero is not None:
            pl.when(cond)(pltpu.make_async_copy(zero, dst, sem).start)
        if one is not None:
            pl.when(jnp.logical_not(cond))(pltpu.make_async_copy(one, dst, sem).start)

    first = s == 0
    either(first, d_x, y_rows, own_v, load_sem.at[0])
    either(first, moved, moved_y, moved_v, load_sem.at[1])
    pltpu.make_async_copy(small, small_v, load_sem.at[2]).start()
    for j, (zero, one, _) in enumerate(terms):
        either(
            first,
            None if zero is None else parts[zero],
            None if one is None else parts[one],
            bufs[j],
            load_sem.at[3 + j],
        )
    for j, (zero, one, i) in enumerate(terms):
        arrive = pltpu.make_async_copy(parts[one if zero is None else zero], bufs[j], load_sem.at[3 + j])
        begins = j == 0 or terms[j - 1][2] != i

        def put(j=j, i=i, begins=begins):
            def add_rows(at):
                value = bufs[j][at, :].astype(F32)
                out_v[i][at, :] = value if begins else out_v[i][at, :] + value

            chunked(bufs[j].shape[0], add_rows)

        if zero is None or one is None:
            cond = first if one is None else jnp.logical_not(first)

            @pl.when(cond)
            def _(arrive=arrive, put=put):
                arrive.wait()
                put()
        else:
            arrive.wait()
            put()
        if j + 1 == len(terms) or terms[j + 1][2] != i:
            dst = grads[i].at[0] if leads[i] else grads[i]
            pltpu.make_async_copy(out_v[i], dst, store_sem.at[i]).start()
    pltpu.make_async_copy(d_x, own_v, load_sem.at[0]).wait()
    pltpu.make_async_copy(moved, moved_v, load_sem.at[1]).wait()
    n = len(leads)
    stores = [
        pltpu.make_async_copy(own_v, result.at[0, s], store_sem.at[n]),
        pltpu.make_async_copy(moved_v, result.at[0, 1 - s], store_sem.at[n + 1]),
    ]
    for store in stores:
        store.start()
    pltpu.make_async_copy(small, small_v, load_sem.at[2]).wait()
    total = small_v[0]
    for i in range(1, small_v.shape[0]):
        total = total + small_v[i]
    gain_out[0] = jnp.where(first, total[0:2], total[2:4])
    channels, size = taps.shape[1], heads.shape[1]
    chosen = total[4 : 4 + tap_rows, 0:channels]
    for i in range(1, total.shape[1] // channels):
        chosen = jnp.where(t == i, total[4 : 4 + tap_rows, i * channels : (i + 1) * channels], chosen)
    taps[...] = chosen
    at = 0
    for row, width in enumerate((channels, channels // 2)):
        value = total[7:8, at : at + size]
        for i in range(1, width // size):
            value = value + total[7:8, at + i * size : at + (i + 1) * size]
        heads[row : row + 1, :] = value
        at += width
    for i, store in enumerate(leads):
        dst = grads[i].at[0] if store else grads[i]
        pltpu.make_async_copy(out_v[i], dst, store_sem.at[i]).wait()
    for store in stores:
        store.wait()


def pack(owned, small, d_x, y_rows, moved_x, moved_y, shapes):
    gain_shape, tap_shape, head_shape = shapes
    parts, terms, leads, out_shapes = [], [], [], []
    for i, (zero, one, lead) in enumerate(owned):
        whole = zero[0].out.shape
        if lead and len(whole) == 3 and isinstance(zero[0], Finish):
            shape = (whole[0] * whole[1], whole[2])
        else:
            shape = whole[-2:]
        shape = tuple(shape)
        leads.append(lead)
        out_shapes.append(shape)
        for j in range(max(len(zero), len(one))):
            pair = []
            for side in (zero, one):
                if j < len(side):
                    parts.append(slot_free(side[j], shape))
                    pair.append(len(parts) - 1)
                else:
                    pair.append(None)
            terms.append((*pair, i))
    operands = [v.array for v in (small.out, d_x, y_rows, moved_x.out, moved_y.out)] + parts
    rows = d_x.shape
    smem = pl.BlockSpec(memory_space=pltpu.VMEM)
    out_shape = [jax.ShapeDtypeStruct((1, 2) + rows, BF), jax.ShapeDtypeStruct(gain_shape, F32)]
    out_shape += [
        jax.ShapeDtypeStruct((1,) + v if lead else v, F32) for v, lead in zip(out_shapes, leads)
    ]
    out_shape += [jax.ShapeDtypeStruct(v, F32) for v in (tap_shape, head_shape)]
    n = len(leads)
    return tuple(
        pl.pallas_call(
            functools.partial(
                pack_kernel, (len(operands), tuple(leads), tuple(terms), tap_shape[0])
            ),
            out_shape=out_shape,
            in_specs=[ANY] * len(operands),
            out_specs=[ANY, smem] + [ANY] * n + [smem] * 2,
            scratch_shapes=[pltpu.VMEM(rows, BF)] * 2
            + [pltpu.VMEM(small.out.shape, F32)]
            + [pltpu.VMEM(out_shapes[i], BF) for _, _, i in terms]
            + [pltpu.VMEM(v, F32) for v in out_shapes]
            + [DMA((3 + len(terms),)), DMA((n + 2,))],
            compiler_params=pltpu.CompilerParams(vmem_limit_bytes=VMEM_BYTES),
            name="pack",
        )(*operands)
    )


def solution(mesh):
    in_specs = (
        P("section", "dp", "tensor", None),
        P("section", None, None),
        P("section", "dp", "tensor"),
        P("section", "tensor", "dp"),
        P("section", "dp", "tensor"),
        P("section", "dp", "tensor"),
        P("section", "tensor", "dp"),
        P(("section", "dp"), "tensor"),
        P(None, "tensor"),
        P(),
    )
    out_specs = (
        P("section", "dp", "tensor", None),
        P("section", None, None),
        P("section", "dp", "tensor"),
        P("section", "tensor", "dp"),
        P("section", "dp", "tensor"),
        P("section", "dp", "tensor"),
        P("section", "tensor", "dp"),
        P(("section", "dp"), "tensor"),
        P(None, "tensor"),
        P(),
    )
    return jax.shard_map(body, mesh=mesh, in_specs=in_specs, out_specs=out_specs, check_vma=False)
```

```python
import functools

import jax
import jax.numpy as jnp
from jax import lax
from jax.experimental import pallas as pl
from jax.experimental.pallas import tpu as pltpu
from jax.sharding import PartitionSpec as P

HEADS = 16
KV_HEADS = 8

EPS = 1e-05
ROPE_BASE = 1000000.0
MASKED = -1e30

MESH = pl.DeviceIdType.MESH
ANY = pl.BlockSpec(memory_space=pl.ANY)
DMA = pltpu.SemaphoreType.DMA
VMEM_BYTES = 63 * 1024 * 1024
BF = jnp.bfloat16
F32 = jnp.float32
ROW_BLOCK = 256
STRIP = 32


def contract(left_op, right_op, left_dim, right_dim):
    return lax.dot_general(
        left_op, right_op, (((left_dim,), (right_dim,)), ((), ())), preferred_element_type=F32
    )


def norm_rows(values, gain):
    return values * lax.rsqrt(jnp.mean(values * values, axis=-1, keepdims=True) + EPS) * gain


def norm_back(values, gain, grad_in):
    row_scale = lax.rsqrt(jnp.mean(values * values, axis=-1, keepdims=True) + EPS)
    normed = values * row_scale
    gain_grad = jnp.sum(grad_in * normed, axis=0, keepdims=True)
    scaled = grad_in * gain
    value_grad = row_scale * (scaled - normed * jnp.mean(scaled * normed, axis=-1, keepdims=True))
    return (value_grad, gain_grad)


class Angles:
    def __init__(self, k, length, head_size, width):
        self.half = head_size // 2
        self.tables = [k.vmem((length, width), F32) for _ in range(2)]
        self.saves = [Save(k, v) for v in self.tables]

    def run(self):
        cos, sin = self.tables
        shape = (ROW_BLOCK, cos.shape[1])
        column = (lax.broadcasted_iota(jnp.int32, shape, 1) % self.half).astype(F32)
        frequency = ROPE_BASE ** (-(column / self.half))
        row = lax.broadcasted_iota(jnp.int32, shape, 0)

        def step(i, carry):
            rows = block_of(i, ROW_BLOCK)
            angle = (row + i * ROW_BLOCK).astype(F32) * frequency
            cos.ref[rows, :] = jnp.cos(angle)
            sin.ref[rows, :] = jnp.sin(angle)
            return carry

        lax.fori_loop(0, cos.shape[0] // ROW_BLOCK, step, 0)
        for save in self.saves:
            save.start()


def silu_parts(gate):
    sig = 1.0 / (1.0 + jnp.exp(-gate))
    return sig, gate * sig


def chunked(rows, step):
    size = next((n for n in (32, 16) if rows % n == 0), rows)
    if size == rows:
        step(pl.ds(0, rows))
    else:
        lax.fori_loop(0, rows // size, lambda i, c: step(block_of(i, size)) or c, 0)


def dp_size():
    return lax.axis_size("dp")


def spot():
    return tuple(lax.axis_index(a) for a in ("section", "dp", "tensor"))


def block_of(index, size):
    return pl.ds(pl.multiple_of(index * size, size), size)


class Val:
    def __init__(self, shape, dtype):
        self.shape, self.dtype = tuple(shape), dtype
        self.ref = self.array = None


class Kernel:
    def __init__(self, cid):
        self.cid, self.ins, self.arrays, self.outs, self.room = cid, [], [], [], []
        self.early, self.steps, self.late, self.axes = [], [], [], set()
        self.once = []

    def input(self, array):
        array = array.array if isinstance(array, Val) else array
        for val, known in zip(self.ins, self.arrays):
            if known is array:
                return val
        val = Val(array.shape, array.dtype)
        self.ins.append(val)
        self.arrays.append(array)
        return val

    def output(self, shape, dtype):
        val = Val(shape, dtype)
        self.outs.append(val)
        return val

    def vmem(self, shape, dtype):
        val = Val(shape, dtype)
        self.room.append((val, pltpu.VMEM(tuple(shape), dtype)))
        return val

    def sem(self, *shape):
        val = Val(shape, None)
        self.room.append((val, DMA(shape)))
        return val

    def do(self, *steps):
        self.steps += steps

    def body(self, *refs):
        vals = self.ins + self.outs + [val for val, _ in self.room]
        for val, ref in zip(vals, refs):
            val.ref = ref
        for item in self.once:
            item.waited = False
            item.phase = 0
        for step in self.early:
            step()
        self.greet()
        for step in self.steps + self.late:
            step()

    def greet(self):
        s, d, t = spot()
        _, sib, cross, diag = places()
        barrier = pltpu.get_barrier_semaphore()
        peers = [{"tensor": sib}, {"tensor": cross}]
        if "tensor" in self.axes:
            peers.append({"tensor": diag})
        if "section" in self.axes:
            peers.append({"section": 1 - s})
        if "dp" in self.axes:
            peers += [{"dp": (d + i) % dp_size()} for i in range(1, dp_size())]

        def signal(peer):
            pl.semaphore_signal(barrier, inc=1, device_id=peer, device_id_type=MESH)

        for peer in peers:
            signal(peer)
        expected = len(peers)
        if "line" in self.axes and "dp" not in self.axes:
            pl.when(d < 3)(lambda: signal({"dp": (d + 1) % 4}))
            pl.when(d > 0)(lambda: signal({"dp": (d + 3) % 4}))
            expected = expected + (d + 2) // 3 + (5 - d) // 3
        pl.semaphore_wait(barrier, expected)

    def build(self):
        result = pl.pallas_call(
            self.body,
            out_shape=[jax.ShapeDtypeStruct(v.shape, v.dtype) for v in self.outs],
            in_specs=[ANY] * len(self.ins),
            out_specs=[ANY] * len(self.outs),
            scratch_shapes=[room for _, room in self.room],
            compiler_params=pltpu.CompilerParams(
                collective_id=self.cid, has_side_effects=True, vmem_limit_bytes=VMEM_BYTES
            ),
            name=f"stage{self.cid}",
        )(*self.arrays)
        for val, array in zip(self.outs, result):
            val.array = array


def remote(src, dst, send_sem, recv_sem, peer):
    return pltpu.make_async_remote_copy(
        src_ref=src, dst_ref=dst, send_sem=send_sem, recv_sem=recv_sem,
        device_id=peer, device_id_type=MESH,
    )


class Load:
    def __init__(self, k, sources, shape, dtype, early=False):
        self.k, self.sources, self.waited = k, sources, False
        self.buf, self.sem = k.vmem(shape, dtype), k.sem(1)
        k.once.append(self)
        if early:
            k.early.append(self.start)

    def moves(self):
        for cond, source in self.sources(*spot()):
            yield cond, pltpu.make_async_copy(source, self.buf.ref, self.sem.ref.at[0])

    def start(self):
        for cond, move in self.moves():
            if cond is None:
                move.start()
            else:
                pl.when(cond)(move.start)

    def wait(self):
        if not self.waited:
            self.waited = True
            next(self.moves())[1].wait()


def load_all(k, array, early=True):
    val = k.input(array)
    return Load(k, lambda s, d, t: [(None, val.ref)], val.shape, val.dtype, early)


class Save:
    def __init__(self, k, buf):
        self.buf, self.out, self.sem = buf, k.output(buf.shape, buf.dtype), k.sem(1)
        self.waited = False
        k.once.append(self)
        k.late.append(self.wait)

    def move(self):
        return pltpu.make_async_copy(self.buf.ref, self.out.ref, self.sem.ref.at[0])

    def start(self):
        self.move().start()

    def wait(self):
        if not self.waited:
            self.waited = True
            self.move().wait()


class Task:
    final = None

    def __init__(self, k, out, axis, moves, count, n_local=1, out_dtype=BF):
        self.k, self.axis, self.make = k, axis, moves
        self.out = k.output(out, out_dtype)
        self.send_sem, self.recv_sem, self.local_sem = k.sem(count), k.sem(count), k.sem(n_local)
        self.waited = False
        k.axes.add(axis)
        k.once.append(self)

    def local(self, src, dst, i):
        return pltpu.make_async_copy(src, dst, self.local_sem.ref.at[i])

    def pairs(self, every):
        far, near = self.make(*spot())
        for i, (sources, dst, peer) in enumerate(far):
            for cond, src in sources if every else sources[:1]:
                yield cond, True, remote(
                    src, dst, self.send_sem.ref.at[i], self.recv_sem.ref.at[i], peer
                )
        for i, (sources, dst) in enumerate(near):
            for cond, src in sources if every else sources[:1]:
                yield cond, False, self.local(src, dst, i)

    def step(self):
        pass

    def send(self):
        for cond, far, move in self.pairs(True):
            if far and self.final is not None:
                cond = lax.axis_index("section") == 1 - self.final
            if cond is None:
                move.start()
            else:
                pl.when(cond)(move.start)

    def wait(self):
        if self.waited:
            return
        self.waited = True
        s = lax.axis_index("section")
        for _, far, move in self.pairs(False):
            if not far:
                move.wait()
            elif self.final is None:
                move.wait_recv()
                move.wait_send()
            else:
                pl.when(s == 1 - self.final)(move.wait_send)
                pl.when(s == self.final)(move.wait_recv)


class Part:
    def __init__(self, base, start, rows):
        self.base, self.start, self.rows = base, start, rows
        self.shape, self.dtype = (rows,) + tuple(base.shape[1:]), base.dtype
        self.array = None

    @property
    def ref(self):
        return self.base.ref.at[pl.ds(self.start, self.rows)]


def as_val(k, value):
    if isinstance(value, Part):
        return Part(as_val(k, value.base), value.start, value.rows)
    value = value.out if isinstance(value, Task) else value
    known = isinstance(value, Val) and (value.array is None)
    return value if known else k.input(value)


class Line(Task):
    def __init__(self, k, out, out_dtype=BF, n_local=1):
        super().__init__(k, out, "line", None, 6, n_local, out_dtype)
        self.send_sem, self.recv_sem = k.sem(2, 3), k.sem(2, 3)
        self.phase = 0

    def hop(self, j, way, src, dst):
        d = lax.axis_index("dp")
        peer = {"dp": (d + 1 if way == 0 else d + 3) % 4}
        return remote(src, dst, self.send_sem.ref.at[way, j], self.recv_sem.ref.at[way, j], peer)


class LineGather(Line):
    def __init__(self, k, sources, shape, dtype):
        super().__init__(k, (4,) + shape, dtype)
        self.sources = sources

    def ends(self, j, way):
        d = lax.axis_index("dp")
        if way == 0:
            return (d >= j) & (d < 3), d >= j + 1
        return (d <= 3 - j) & (d > 0), d <= 2 - j

    def copy(self, j, way, src=None):
        d = lax.axis_index("dp")
        slot = (d + 4 - j if way == 0 else d + j) % 4
        piece = self.out.ref.at[slot]
        return self.hop(j, way, piece if src is None else src, piece)

    def send(self):
        self.phase = 0
        for cond, src in self.sources(*spot()):
            own = self.local(src, self.out.ref.at[lax.axis_index("dp")], 0)
            moves = [(True if cond is None else cond, own)]
            for way in range(2):
                sends = self.ends(0, way)[0]
                moves.append((sends if cond is None else sends & cond, self.copy(0, way, src)))
            for when, move in moves:
                if when is True:
                    move.start()
                else:
                    pl.when(when)(move.start)

    def arrive(self, j):
        for way in range(2):
            pl.when(self.ends(j, way)[1])(self.copy(j, way).wait_recv)

    def step(self):
        self.arrive(self.phase)
        self.phase += 1
        for way in range(2):
            pl.when(self.ends(self.phase, way)[0])(self.copy(self.phase, way).start)

    def wait(self):
        if self.waited:
            return
        self.waited = True
        while self.phase < 2:
            self.step()
        self.arrive(2)
        for j in range(3):
            for way in range(2):
                pl.when(self.ends(j, way)[0])(self.copy(j, way).wait_send)
        d = lax.axis_index("dp")
        self.local(self.sources(*spot())[0][1], self.out.ref.at[d], 0).wait()


def z_gather_from(k, sources, shape, dtype):
    count = dp_size()
    if count == 4:
        return LineGather(k, sources, shape, dtype)

    def moves(s, d, t):
        dst, found = task.out.ref.at[d], sources(s, d, t)
        return [(found, dst, {"dp": (d + i) % count}) for i in range(1, count)], [(found, dst)]

    task = Task(k, (count,) + shape, "dp", moves, count - 1, out_dtype=dtype)
    return task


def z_gather(k, value):
    val = as_val(k, value)
    return z_gather_from(k, lambda s, d, t: [(None, val.ref)], val.shape, val.dtype)


def z_gather_half(k, shard, moved, block):
    shard, moved = as_val(k, shard), as_val(k, moved)
    rows = shard.shape[0] // 2

    def sources(s, d, t):
        own = shard.ref.at[pl.ds(block * rows, rows)]
        return [(s == block, own), (s == 1 - block, moved.ref)]

    return z_gather_from(k, sources, moved.shape, shard.dtype)


def one_way(task, sender):
    task.final = None if sender is None else 1 - sender
    return task


def z_gather_whole(k, shard, moved, block, half=None):
    shard, moved = as_val(k, shard), as_val(k, moved)
    rows = shard.shape[0] if half is None else shard.shape[0] // 2
    part = pl.ds(0 if half is None else half * rows, rows)

    def sources(s, d, t):
        return [(s == block, shard.ref.at[part]), (s == 1 - block, moved.ref.at[part])]

    return z_gather_from(k, sources, (rows,) + shard.shape[1:], shard.dtype)


def x_move(k, value, sender=None):
    val = as_val(k, value)

    def moves(s, d, t):
        return [([(None, val.ref)], task.out.ref, {"section": 1 - s})], []

    task = Task(k, val.shape, "section", moves, 1, out_dtype=val.dtype)
    return one_way(task, sender)


def x_half(k, value, sender=None):
    val = as_val(k, value)
    rows = val.shape[0] // 2

    def moves(s, d, t):
        src = val.ref.at[block_of(1 - s, rows)]
        return [([(None, src)], task.out.ref, {"section": 1 - s})], []

    task = Task(k, (rows,) + val.shape[1:], "section", moves, 1, out_dtype=val.dtype)
    return one_way(task, sender)


def x_slots(k, value, kind):
    val, count = as_val(k, value), dp_size()
    rows = val.shape[0] // (2 * count)

    def moves(s, d, t):
        far = []
        for i in range(count):
            slot = 2 * i + 1 - s if kind == "rows" else (1 - s) * count + i
            src = val.ref.at[block_of(slot, rows)]
            far.append(([(None, src)], task.out.ref.at[i], {"section": 1 - s}))
        return far, []

    task = Task(k, (count, rows) + val.shape[1:], "section", moves, count)
    return task


class Terms:
    def __init__(self, k, kind, grads, received, local):
        self.grads, self.local = as_val(k, grads), local
        self.kind, self.n = kind, dp_size()
        self.whole = received is None
        if self.whole:
            rows, cols = self.grads.shape
            self.rows = rows if kind == "cols" else rows // self.n
            self.cols = cols // self.n if kind == "cols" else cols
            self.shape = (self.n, self.rows, self.cols)
            self.aside = kind == "cols" and self.cols % 128 != 0
            self.total = k.vmem(self.shape, BF)
            self.kept = k.vmem(self.grads.shape, BF) if self.aside else self.total
            return
        self.received = as_val(k, received)
        if kind == "cols":
            self.rows, self.cols = self.grads.shape[0] // 2, self.grads.shape[1] // self.n
            held = (self.rows, self.grads.shape[1])
        else:
            self.rows, self.cols = self.grads.shape[0] // (2 * self.n), self.grads.shape[1]
            held = (self.n, self.rows, self.cols)
        self.kept, self.got = k.vmem(held, BF), k.vmem(held, BF)
        self.shape = (self.n, self.rows, self.cols)
        self.total = k.vmem(self.shape, BF) if kind == "cols" else self.kept

    def loads(self):
        s, grads, kept = lax.axis_index("section"), self.grads.ref, self.kept.ref
        if self.whole and self.aside:
            return [self.local(grads, kept, 2)]
        if self.whole:
            parts = [
                grads.at[:, pl.ds(i * self.cols, self.cols)]
                if self.kind == "cols"
                else grads.at[block_of(i, self.rows)]
                for i in range(self.n)
            ]
            return [self.local(part, kept.at[i], 2 + i) for i, part in enumerate(parts)]
        if self.kind == "cols":
            moves = [self.local(grads.at[block_of(s, self.rows)], kept, 2)]
        else:
            moves = []
            for i in range(self.n):
                slot = 2 * i + s if self.kind == "rows" else s * self.n + i
                moves.append(self.local(grads.at[block_of(slot, self.rows)], kept.at[i], 2 + i))
        return moves + [self.local(self.received.ref, self.got.ref, 1)]

    def load(self):
        for move in self.loads():
            move.start()

    def add(self):
        for move in self.loads():
            move.wait()
        if self.whole and self.aside:
            for i in range(self.n):
                self.total.ref[i] = self.kept.ref[:, i * self.cols : (i + 1) * self.cols]
        if self.whole:
            return
        kept, got, total = self.kept.ref, self.got.ref, self.total.ref
        if self.kind != "cols":

            def piece(i, carry):
                chunked(self.rows, lambda at: total.__setitem__(
                    (i, at), (kept[i, at, :].astype(F32) + got[i, at, :].astype(F32)).astype(BF)
                ))
                return carry

            lax.fori_loop(0, self.n, piece, 0)
            return

        def add_rows(at):
            for i in range(self.n):
                part = slice(i * self.cols, (i + 1) * self.cols)
                value = kept[at, part].astype(F32) + got[at, part].astype(F32)
                total[i, at, :] = value.astype(BF)

        chunked(self.rows, add_rows)


class DirectScatter(Task):
    def __init__(self, k, kind, grads, received):
        self.terms = Terms(k, kind, grads, received, lambda *a: self.local(*a))
        count = dp_size()

        def moves(s, d, t):
            total = self.terms.total.ref
            far = []
            for i in range(1, count):
                other = (d + i) % count
                far.append(([(None, total.at[other])], self.out.ref.at[d], {"dp": other}))
            return far, [([(None, total.at[d])], self.out.ref.at[d])]

        super().__init__(k, self.terms.shape, "dp", moves, count - 1, 2 + count)
        self.load = self.terms.load

    def send(self):
        self.terms.add()
        super().send()

    def add(self):
        self.load()
        self.send()


class LineScatter(Line):
    def __init__(self, k, kind, grads, received):
        self.terms = Terms(k, kind, grads, received, lambda *a: self.local(*a))
        super().__init__(k, self.terms.shape[1:], BF, 6)
        self.got = k.vmem((2, 3) + self.terms.shape[1:], BF)
        self.load = self.terms.load

    def ends(self, j, way):
        d = lax.axis_index("dp")
        if way == 0:
            return (d <= j) & (d < 3), (d >= 1) & (d <= j + 1)
        return (d >= 3 - j) & (d > 0), (d <= 2) & (d >= 2 - j)

    def copy(self, j, way):
        d = lax.axis_index("dp")
        to = (d + 3 - j if way == 0 else d + 1 + j) % 4
        return self.hop(j, way, self.terms.total.ref.at[to], self.got.ref.at[way, j])

    def send(self):
        self.phase = 0
        self.terms.add()
        for way in range(2):
            pl.when(self.ends(0, way)[0])(self.copy(0, way).start)

    def take(self, j, way):
        d = lax.axis_index("dp")
        to = (d + 2 - j if way == 0 else d + 2 + j) % 4
        self.copy(j, way).wait_recv()
        total, got = self.terms.total.ref, self.got.ref

        def add_rows(at):
            value = total[to, at, :].astype(F32) + got[way, j, at, :].astype(F32)
            total[to, at, :] = value.astype(BF)

        chunked(self.terms.rows, add_rows)

    def arrive(self, j):
        for way in range(2):
            pl.when(self.ends(j, way)[1])(functools.partial(self.take, j, way))

    def step(self):
        self.arrive(self.phase)
        self.phase += 1
        for way in range(2):
            pl.when(self.ends(self.phase, way)[0])(self.copy(self.phase, way).start)

    def wait(self):
        if self.waited:
            return
        self.waited = True
        while self.phase < 2:
            self.step()
        self.arrive(2)
        done = self.local(self.terms.total.ref.at[lax.axis_index("dp")], self.out.ref, 0)
        done.start()
        for j in range(3):
            for way in range(2):
                pl.when(self.ends(j, way)[0])(self.copy(j, way).wait_send)
        done.wait()

    def add(self):
        self.load()
        self.send()


def sum_scatter(k, kind, grads, received=None):
    return (LineScatter if dp_size() == 4 else DirectScatter)(k, kind, grads, received)


class Finish(Task):
    def __init__(self, k, pieces, block):
        self.pieces, self.final = as_val(k, pieces), block
        *slots, rows, cols = self.pieces.shape
        self.slots = slots[0] if slots else 0
        if slots:
            self.held, self.total = k.vmem(self.pieces.shape, BF), k.vmem((rows, cols), BF)
        else:
            self.total = self.pieces

        def moves(s, d, t):
            source, dst = [(None, self.total.ref)], self.out.ref.at[s]
            return [(source, dst, {"section": 1 - s})], [(source, dst)]

        super().__init__(k, (2, rows, cols), "section", moves, 1, 2)

    def load(self):
        if self.slots:
            self.local(self.pieces.ref, self.held.ref, 1).start()

    def send(self):
        if self.slots:
            self.local(self.pieces.ref, self.held.ref, 1).wait()
            acc = self.held.ref[0].astype(F32)
            for i in range(1, self.slots):
                acc = acc + self.held.ref[i].astype(F32)
            self.total.ref[...] = acc.astype(BF)
        super().send()

    def add(self):
        self.load()
        self.send()


class SumShare(Task):
    def __init__(self, k, terms, axis, slotted=False):
        self.terms = [as_val(k, v) for v in terms]
        shape = self.terms[0].shape[1:] if slotted else self.terms[0].shape
        count = dp_size() if axis == "dp" else 4
        self.slotted = slotted
        self.bufs = [k.vmem(v.shape, F32) for v in self.terms]
        self.total = k.vmem(shape, F32)

        def moves(s, d, t):
            source, me = [(None, self.total.ref)], d if axis == "dp" else t
            dst = self.out.ref.at[me]
            far = [(source, dst, {axis: (me + i) % count}) for i in range(1, count)]
            return far, [(source, dst)]

        super().__init__(k, (count,) + shape, axis, moves, count - 1, 3, out_dtype=F32)

    def add(self):
        loads = [self.local(v.ref, b.ref, 1 + i) for i, (v, b) in enumerate(zip(self.terms, self.bufs))]
        for load in loads:
            load.start()
        for load in loads:
            load.wait()
        if self.slotted:
            parts = [self.bufs[0].ref[i] for i in range(self.terms[0].shape[0])]
        else:
            parts = [buf.ref[...] for buf in self.bufs]
        acc = parts[0]
        for part in parts[1:]:
            acc = acc + part
        self.total.ref[...] = acc
        self.send()


class Weight:
    def __init__(self, k, kind, *segments, early=False):
        self.kind, self.waited = kind, False
        self.segments, start = [], 0
        for near, far in segments:
            near, far = as_val(k, near), None if far is None else as_val(k, far)
            self.segments.append((near, far, start))
            start += near.shape[1] * (1 if far is None else 2)
        self.count, _, self.cols = self.segments[0][0].shape
        self.rows = start
        if kind == "cols":
            shape = (self.rows, self.count * self.cols)
        else:
            shape = (self.count * self.rows, self.cols)
        self.aside = kind == "cols" and self.cols % 128 != 0
        self.buf = k.vmem(shape, BF)
        sides = [v for near, far, _ in self.segments for v in (near, far) if v is not None]
        self.sem = k.sem(len(sides), self.count)
        if self.aside:
            self.held = [k.vmem(v.shape, BF) for v in sides]
        k.once.append(self)
        if early:
            k.early.append(self.start)

    def sides(self):
        s = lax.axis_index("section")
        for near, far, start in self.segments:
            rows = near.shape[1]
            if far is None:
                yield near, start, None
            else:
                yield near, start + s * rows, s
                yield far, start + (1 - s) * rows, 1 - s

    def moves(self):
        dst = self.buf.ref
        for j, (val, start, sec) in enumerate(self.sides()):
            rows = val.shape[1]
            for i in range(self.count):
                if self.aside:
                    to = self.held[j].ref.at[i]
                elif self.kind == "cols":
                    at = pl.ds(pl.multiple_of(start, 16), rows)
                    to = dst.at[at, pl.ds(i * self.cols, self.cols)]
                else:
                    top = (sec * self.count + i) * rows if self.kind == "conv" else i * self.rows + start
                    to = dst.at[pl.ds(pl.multiple_of(top, 16), rows)]
                yield pltpu.make_async_copy(val.ref.at[i], to, self.sem.ref.at[j, i])

    def start(self):
        for move in self.moves():
            move.start()

    def wait(self):
        if self.waited:
            return
        self.waited = True
        for move in self.moves():
            move.wait()
        if self.aside:
            for j, (val, start, _) in enumerate(self.sides()):
                whole = jnp.concatenate([self.held[j].ref[i] for i in range(self.count)], axis=1)
                self.buf.ref[pl.ds(pl.multiple_of(start, 16), val.shape[1]), :] = whole


class Product:
    def __init__(self, k, left, right):
        self.left, self.right = left, right
        rows = left.shape[1]
        self.chunk = 384 if rows % 384 == 0 else 256
        self.count = rows // self.chunk
        self.buf = k.vmem((rows, right.shape[1]), BF)
        self.out, self.sem = k.output(self.buf.shape, BF), k.sem(self.count)

    def copy(self, i):
        part = block_of(i, self.chunk)
        return pltpu.make_async_copy(self.buf.ref.at[part], self.out.ref.at[part], self.sem.ref.at[i])

    def run(self):
        def step(i, carry):
            part = block_of(i, self.chunk)
            value = contract(self.left.ref[:, part], self.right.ref[...], 0, 0)
            self.buf.ref[part, :] = value.astype(BF)
            self.copy(i).start()
            return carry

        lax.fori_loop(0, self.count, step, 0)

    def wait(self):
        for i in range(self.count):
            self.copy(i).wait()


def places():
    me = lax.axis_index("tensor")
    sib = me + 1 - 2 * (me % 2)
    cross = (me + 2) % 4
    diag = (sib + 2) % 4
    return me, sib, cross, diag


class Gather:
    def __init__(self, k, x, gain, weights, extras=(), trans=False, epilogue="plain", save=()):
        rows, width = x.shape
        length = 4 * rows
        self.k, self.x, self.gain, self.weights, self.extras = k, x, gain, weights, extras
        self.trans, self.epilogue, self.rows, self.half = trans, epilogue, rows, rows // 2
        cols = [w.buf.shape[0 if trans else 1] for w in weights]
        kinds = {
            "plain": [(c, F32) for c in cols],
            "ffn": [(cols[0], BF)] * 3,
            "ffn_back": [(cols[0], BF)] * 2,
        }[epilogue]
        self.full = k.vmem((length, width), BF)
        self.values = [k.vmem((length, c), kind) for c, kind in kinds]
        kept = [self.full] + self.values
        self.saved = [(v, k.output(v.shape, v.dtype), k.sem(4, 2)) for v in kept if kept.index(v) in save]
        self.sems = [k.sem(2) for _ in range(6)]
        k.late.append(self.end)

    def span(self, owner, sub):
        return pl.ds(pl.multiple_of(owner * self.rows + sub * self.half, self.half), self.half)

    def move(self, kind, i):
        me, sib, cross, _ = places()
        full = self.full.ref
        owner, peer, at = {"cross": (me, cross, 0), "sib": (me, sib, 2), "relay": (cross, sib, 4)}[kind]
        part = full.at[self.span(owner, i)]
        return remote(
            part, part, self.sems[at].ref.at[i], self.sems[at + 1].ref.at[i], {"tensor": peer}
        )

    def begin(self):
        me = places()[0]
        for i in range(2):

            def put(j, carry):
                at = i * self.half + j * STRIP
                part = self.x.ref[pl.ds(pl.multiple_of(at, STRIP), STRIP), :].astype(F32)
                if self.gain is not None:
                    val, row = self.gain
                    part = norm_rows(part, val.ref[row : row + 1, :])
                to = pl.ds(pl.multiple_of(me * self.rows + at, STRIP), STRIP)
                self.full.ref[to, :] = part.astype(BF)
                return carry

            lax.fori_loop(0, self.half // STRIP, put, 0)
            self.move("cross", i).start()
            self.move("sib", i).start()

    def loop(self):
        me, sib, cross, diag = places()
        rows, half = self.rows, self.half
        for w in self.weights:
            w.wait()

        def step(p, carry):
            far, sub = p // 2, p % 2
            near = (1 - sub) * me + sub * sib
            first = (1 - far) * near * rows + far * (cross * rows + sub * half)
            second = (1 - far) * (near * rows + half) + far * (diag * rows + sub * half)
            pair = [pl.ds(pl.multiple_of(v, half), half) for v in (first, second)]

            @pl.when(p == 1)
            def _():
                self.move("sib", 0).wait_recv()
                self.move("sib", 1).wait_recv()

            for i in range(2):

                @pl.when(p == 2 + i)
                def _():
                    self.move("cross", i).wait_recv()
                    self.move("relay", i).start()
                    self.move("relay", i).wait_recv()

            def both(val):
                return jnp.concatenate([val.ref[pair[0], :], val.ref[pair[1], :]], axis=0)

            a = both(self.full)
            prods = [contract(a, w.buf.ref[...], 1, 1 if self.trans else 0) for w in self.weights]
            if self.epilogue == "plain":
                values = prods
            elif self.epilogue == "ffn":
                sig, silu = silu_parts(prods[0])
                values = [prods[0], prods[1], silu * prods[1]]
            else:
                gate, up = (both(v).astype(F32) for v in self.extras)
                sig, silu = silu_parts(gate)
                values = [prods[0] * up * sig * (1.0 + gate * (1.0 - sig)), prods[0] * silu]
            for val, value in zip(self.values, values):
                value = value.astype(val.dtype)
                for j in range(2):
                    val.ref[pair[j], :] = value[j * half : (j + 1) * half]
            for val, out, sem in self.saved:
                for j in range(2):
                    pltpu.make_async_copy(
                        val.ref.at[pair[j]], out.ref.at[pair[j]], sem.ref.at[p, j]
                    ).start()
            return carry

        lax.fori_loop(0, 4, step, 0)

    def end(self):
        for i in range(2):
            for kind in ("cross", "sib", "relay"):
                self.move(kind, i).wait_send()
        part = pl.ds(0, self.half)
        for val, out, sem in self.saved:
            for p in range(4):
                for j in range(2):
                    pltpu.make_async_copy(val.ref.at[part], out.ref.at[part], sem.ref.at[p, j]).wait()


class Scatter:
    def __init__(self, k, operands, weights, resid, back=None, trans=False, low=False):
        rows, width = resid.shape
        half = rows // 2
        self.operands, self.weights, self.resid, self.back = operands, weights, resid, back
        self.trans, self.low, self.rows, self.half = trans, low, rows, half
        self.keep, self.own = k.vmem((2, half, width), F32), k.vmem((rows, width), F32)
        self.to_s, self.from_s, self.to_c, self.from_c = (
            k.vmem((2, half, width), BF) for _ in range(4)
        )
        self.to_o, self.from_o = k.vmem((rows, width), BF), k.vmem((rows, width), BF)
        self.out = k.vmem((rows, width), BF if low else F32)
        self.gain_grad = k.vmem((1, width), F32) if back else None
        self.sems = [k.sem(2) for _ in range(4)] + [k.sem(1) for _ in range(2)]
        k.late.append(self.end)

    def move(self, kind, i=0):
        _, sib, cross, _ = places()
        at, src, dst, peer = {
            "diag": (0, self.to_s, self.from_s, sib),
            "cross": (2, self.to_c, self.from_c, cross),
            "near": (4, self.to_o, self.from_o, sib),
        }[kind]
        src, dst = (src.ref, dst.ref) if kind == "near" else (src.ref.at[i], dst.ref.at[i])
        return remote(
            src, dst, self.sems[at].ref.at[i], self.sems[at + 1].ref.at[i], {"tensor": peer}
        )

    def pass_on(self, i):
        self.move("diag", i).wait_recv()

        def add_rows(at):
            total = self.keep.ref[i, at, :] + self.from_s.ref[i, at, :].astype(F32)
            self.to_c.ref[i, at, :] = total.astype(BF)

        chunked(self.half, add_rows)
        self.move("cross", i).start()

    def loop(self):
        me, sib, cross, diag = places()
        rows, half = self.rows, self.half
        for w in self.weights:
            w.wait()

        def step(p, carry):
            near, sub = p // 2, p % 2
            base = near * ((1 - sub) * sib + sub * me) * rows
            first = base + (1 - near) * (cross * rows + sub * half)
            second = base + near * half + (1 - near) * (diag * rows + sub * half)
            pair = [pl.ds(pl.multiple_of(v, half), half) for v in (first, second)]
            total = None
            for y, w in zip(self.operands, self.weights):
                a = jnp.concatenate([y.ref[pair[0], :], y.ref[pair[1], :]], axis=0)
                prod = contract(a, w.buf.ref[...], 1, 1 if self.trans else 0)
                total = prod if total is None else total + prod

            self.own.ref[...] = total

            @pl.when(p < 2)
            def _():
                def put(at):
                    self.keep.ref[p, at, :] = self.own.ref[at, :]
                    lower = pl.ds(pl.multiple_of(at.start + half, 16), at.size)
                    self.to_s.ref[p, at, :] = self.own.ref[lower, :].astype(BF)

                chunked(half, put)
                self.move("diag", p).start()

            @pl.when(p == 2)
            def _():
                def put(at):
                    self.to_o.ref[at, :] = self.own.ref[at, :].astype(BF)

                chunked(rows, put)
                self.move("near").start()

            @pl.when((p == 1) | (p == 2))
            def _():
                self.pass_on(p - 1)

            return carry

        lax.fori_loop(0, 4, step, 0)

    def finish(self):
        self.move("near").wait_recv()
        if self.back:
            self.gain_grad.ref[...] = jnp.zeros_like(self.gain_grad.ref)
        for i in range(2):
            self.move("cross", i).wait_recv()

            def add_rows(j, carry):
                inner = block_of(j, STRIP)
                part = pl.ds(pl.multiple_of(i * self.half + j * STRIP, STRIP), STRIP)
                total = self.own.ref[part, :] + self.from_o.ref[part, :].astype(F32)
                total = total + self.from_c.ref[i, inner, :].astype(F32)
                resid = self.resid.ref[part, :].astype(F32)
                if self.back:
                    value, (gain, row) = self.back
                    total, gain_grad = norm_back(
                        value.ref[part, :].astype(F32), gain.ref[row : row + 1, :], total
                    )
                    self.gain_grad.ref[...] += gain_grad
                self.out.ref[part, :] = (resid + total).astype(self.out.dtype)
                return carry

            lax.fori_loop(0, self.half // STRIP, add_rows, 0)

    def end(self):
        self.move("near").wait_send()
        for i in range(2):
            self.move("diag", i).wait_send()
            self.move("cross", i).wait_send()


def delayed(values, by):
    if by == 0:
        return values
    row = lax.broadcasted_iota(jnp.int32, values.shape, 0)
    return jnp.where(row < by, 0.0, pltpu.roll(values, by, 0))


def advanced(values, by):
    if by == 0:
        return values
    length = values.shape[0]
    row = lax.broadcasted_iota(jnp.int32, values.shape, 0)
    return jnp.where(row >= length - by, 0.0, pltpu.roll(values, length - by, 0))


CONV_COLS = 128


class Conv:
    def __init__(self, k, projected, value, kernel):
        self.projected, self.value, self.kernel = projected, value, kernel
        self.y = k.vmem(value.shape, BF)

    def parts(self, j):
        channels = self.value.shape[1]
        at = block_of(j, CONV_COLS)
        b_gate = self.projected.ref[:, at]
        c_gate = self.projected.ref[:, block_of(j + channels // CONV_COLS, CONV_COLS)]
        x_value, taps = self.value.ref[:, at], self.kernel.ref[:, at]
        product = b_gate * x_value
        count = taps.shape[0]
        causal = jnp.zeros_like(product)
        for i in range(count):
            causal = causal + taps[i : i + 1] * delayed(product, count - 1 - i)
        return at, b_gate, c_gate, x_value, taps, product, causal

    def run(self):
        def step(j, carry):
            at, _, c_gate, _, _, _, causal = self.parts(j)
            self.y.ref[:, at] = (c_gate * causal).astype(BF)
            return carry

        lax.fori_loop(0, self.value.shape[1] // CONV_COLS, step, 0)


class ConvBack(Conv):
    def __init__(self, k, projected, value, kernel, d_y):
        self.projected, self.value, self.kernel, self.d_y = projected, value, kernel, d_y
        self.d_proj = k.vmem(projected.shape, BF)
        self.d_value = k.vmem(value.shape, BF)
        self.d_kernel = k.vmem(kernel.shape, F32)

    def run(self):
        channels = self.value.shape[1]

        def step(j, carry):
            at, b_gate, c_gate, x_value, taps, product, causal = self.parts(j)
            d_y = self.d_y.ref[:, at]
            d_causal = d_y * c_gate
            count = taps.shape[0]
            d_product = jnp.zeros_like(product)
            for i in range(count):
                by = count - 1 - i
                row = jnp.sum(d_causal * delayed(product, by), axis=0, keepdims=True)
                self.d_kernel.ref[i : i + 1, at] = row
                d_product = d_product + taps[i : i + 1] * advanced(d_causal, by)
            self.d_proj.ref[:, at] = (d_product * x_value).astype(BF)
            upper = block_of(j + channels // CONV_COLS, CONV_COLS)
            self.d_proj.ref[:, upper] = (d_y * causal).astype(BF)
            self.d_value.ref[:, at] = (d_product * b_gate).astype(BF)
            return carry

        lax.fori_loop(0, channels // CONV_COLS, step, 0)


def head_mean(values, head_size):
    width = values.shape[1]
    row = lax.broadcasted_iota(jnp.int32, (width, width), 0) // head_size
    col = lax.broadcasted_iota(jnp.int32, (width, width), 1) // head_size
    group = jnp.where(row == col, 1.0 / head_size, 0.0).astype(F32)
    return lax.dot_general(
        values, group, (((1,), (0,)), ((), ())),
        precision=lax.Precision.HIGHEST, preferred_element_type=F32,
    )


def turn(values, head_size, back):
    width, half = values.shape[1], head_size // 2
    lane = lax.broadcasted_iota(jnp.int32, values.shape, 1) % head_size
    upper = pltpu.roll(values, width - half, 1)
    lower = pltpu.roll(values, half, 1)
    return jnp.where(lane < half, upper, -lower) if back else jnp.where(lane < half, -upper, lower)


def head_norm(values, gain, head_size):
    return values * lax.rsqrt(head_mean(values * values, head_size) + EPS) * gain


def head_norm_back(values, gain, grad_in, head_size):
    row_scale = lax.rsqrt(head_mean(values * values, head_size) + EPS)
    normed = values * row_scale
    gain_grad = jnp.sum(grad_in * normed, axis=0, keepdims=True)
    scaled = grad_in * gain
    return row_scale * (scaled - normed * head_mean(scaled * normed, head_size)), gain_grad


def block_weights(q_rows, keys):
    scores = [contract(q_rows, k_rows, 1, 1) for k_rows in keys]
    query = lax.broadcasted_iota(jnp.int32, scores[-1].shape, 0)
    key = lax.broadcasted_iota(jnp.int32, scores[-1].shape, 1)
    scores[-1] = jnp.where(key <= query, scores[-1], MASKED)
    top = functools.reduce(
        jnp.maximum, [jnp.max(part, axis=1, keepdims=True) for part in scores]
    )
    exps = [jnp.exp(part - top) for part in scores]
    scale = 1.0 / sum(jnp.sum(part, axis=1, keepdims=True) for part in exps)
    return [part * scale for part in exps]


def key_blocks(i):
    blocks = [pl.ds(0, i * ROW_BLOCK)] if i else []
    return blocks + [pl.ds(i * ROW_BLOCK, ROW_BLOCK)]


class Heads:
    def __init__(self, projected, tables, size):
        assert size in (16, 64, 256), size
        self.projected, self.size = projected, size
        self.gain, self.cos, self.sin = (v.buf for v in tables)
        self.loads = tables
        self.length, width = projected.shape
        self.q_cols, self.k_cols = width // 2, width // 4
        self.heads, self.kv_heads = self.q_cols // size, self.k_cols // size
        self.share = self.heads // self.kv_heads

    def per_head(self, k, count, kind):
        return k.vmem((count, self.length, self.size), kind)

    def split(self, val, rows, values):
        for h in range(val.shape[0]):
            val.ref[h, rows, :] = values[:, h * self.size : (h + 1) * self.size]

    def join(self, val, rows):
        return jnp.concatenate([val.ref[h, rows, :] for h in range(val.shape[0])], axis=1)

    def gains(self):
        gain = self.gain.ref[...]
        return (
            jnp.concatenate([gain[0:1]] * self.heads, axis=1),
            jnp.concatenate([gain[1:2]] * self.kv_heads, axis=1),
        )

    def angles(self, rows):
        c, n = self.cos.ref[rows, :], self.sin.ref[rows, :]
        repeat = self.q_cols // c.shape[1]
        return jnp.concatenate([c] * repeat, axis=1), jnp.concatenate([n] * repeat, axis=1)

    def blocks(self, step):
        lax.fori_loop(0, self.length // ROW_BLOCK, lambda p, c: step(block_of(p, ROW_BLOCK)) or c, 0)


class Attend(Heads):
    def __init__(self, k, projected, tables, size):
        super().__init__(projected, tables, size)
        self.q_rot = k.vmem((self.length, self.q_cols), BF)
        self.k_rot = k.vmem((self.length, self.k_cols), BF)
        self.y = k.vmem((self.length, self.q_cols), BF)
        self.q_h, self.y_h = (self.per_head(k, self.heads, BF) for _ in range(2))
        self.k_h, self.v_h = (self.per_head(k, self.kv_heads, BF) for _ in range(2))

    def run(self, *between):
        for load in self.loads:
            load.wait()
        size, q_cols, k_cols, proj = self.size, self.q_cols, self.k_cols, self.projected.ref

        def prepare(rows):
            c, n = self.angles(rows)
            q_gain, k_gain = self.gains()
            q = head_norm(proj[rows, :q_cols], q_gain, size)
            q = (q * c + turn(q, size, False) * n).astype(BF)
            k = head_norm(proj[rows, q_cols : q_cols + k_cols], k_gain, size)
            k = (k * c[:, :k_cols] + turn(k, size, False) * n[:, :k_cols]).astype(BF)
            self.q_rot.ref[rows, :] = q
            self.k_rot.ref[rows, :] = k
            self.split(self.q_h, rows, (q.astype(F32) * size**-0.5).astype(BF))
            self.split(self.k_h, rows, k)
            self.split(self.v_h, rows, proj[rows, q_cols + k_cols :].astype(BF))

        self.blocks(prepare)

        def head(h, carry):
            g = h // self.share

            @pl.when(h == self.heads // 2)
            def _():
                for step in between:
                    step()

            for i in range(self.length // ROW_BLOCK):
                rows, seen = pl.ds(i * ROW_BLOCK, ROW_BLOCK), key_blocks(i)
                weights = block_weights(
                    self.q_h.ref[h, rows, :], [self.k_h.ref[g, at, :] for at in seen]
                )
                value = sum(
                    contract(part.astype(BF), self.v_h.ref[g, at, :], 1, 0)
                    for part, at in zip(weights, seen)
                )
                self.y_h.ref[h, rows, :] = value.astype(BF)
            return carry

        lax.fori_loop(0, self.heads, head, 0)

        def place(rows):
            self.y.ref[rows, :] = self.join(self.y_h, rows)

        self.blocks(place)


class AttendBack(Heads):
    def __init__(self, k, projected, tables, size, q_rot, k_rot, d_y):
        super().__init__(projected, tables, size)
        self.q_rot, self.k_rot, self.d_y = q_rot, k_rot, d_y
        self.q_h, self.dy_h = (self.per_head(k, self.heads, BF) for _ in range(2))
        self.k_h, self.v_h = (self.per_head(k, self.kv_heads, BF) for _ in range(2))
        self.dq_h = self.per_head(k, self.heads, F32)
        self.dk_h, self.dv_h = (self.per_head(k, self.kv_heads, F32) for _ in range(2))
        self.d_proj = k.vmem(projected.shape, BF)
        self.q_gain, self.k_gain = k.vmem((1, self.q_cols), F32), k.vmem((1, self.k_cols), F32)

    def run(self, *between):
        for load in self.loads:
            load.wait()
        size, q_cols, k_cols, proj = self.size, self.q_cols, self.k_cols, self.projected.ref
        scale = size**-0.5
        dq_h, dk_h, dv_h = self.dq_h.ref, self.dk_h.ref, self.dv_h.ref

        def prepare(rows):
            self.split(self.q_h, rows, (self.q_rot.ref[rows, :].astype(F32) * scale).astype(BF))
            self.split(self.dy_h, rows, self.d_y.ref[rows, :].astype(BF))
            self.split(self.k_h, rows, self.k_rot.ref[rows, :])
            self.split(self.v_h, rows, proj[rows, q_cols + k_cols :].astype(BF))

        self.blocks(prepare)

        def clear(rows):
            for val in (dk_h, dv_h):
                val[:, rows, :] = jnp.zeros((self.kv_heads, ROW_BLOCK, size), F32)

        self.blocks(clear)

        def head(h, carry):
            g = h // self.share

            @pl.when(h == self.heads // 2)
            def _():
                for step in between:
                    step()

            for i in range(self.length // ROW_BLOCK):
                rows, seen = pl.ds(i * ROW_BLOCK, ROW_BLOCK), key_blocks(i)
                q, low = self.q_h.ref[h, rows, :], self.dy_h.ref[h, rows, :]
                keys = [self.k_h.ref[g, at, :] for at in seen]
                probs = block_weights(q, keys)
                d_weights = [contract(low, self.v_h.ref[g, at, :], 1, 1) for at in seen]
                inner = sum(
                    jnp.sum(a * b, axis=1, keepdims=True) for a, b in zip(probs, d_weights)
                )
                d_q = 0.0
                for at, k, prob, d_weight in zip(seen, keys, probs, d_weights):
                    dv_h[g, at, :] += contract(prob.astype(BF), low, 0, 0)
                    d_scores = (prob * (d_weight - inner)).astype(BF)
                    d_q = d_q + contract(d_scores, k, 1, 0)
                    dk_h[g, at, :] += contract(d_scores, q, 0, 0)
                dq_h[h, rows, :] = d_q * scale
            return carry

        lax.fori_loop(0, self.heads, head, 0)
        self.q_gain.ref[...] = jnp.zeros_like(self.q_gain.ref)
        self.k_gain.ref[...] = jnp.zeros_like(self.k_gain.ref)

        def finish(rows):
            c, n = self.angles(rows)
            dq, dk, dv = (self.join(v, rows) for v in (self.dq_h, self.dk_h, self.dv_h))
            dq = dq * c + turn(dq * n, size, True)
            dk = dk * c[:, :k_cols] + turn(dk * n[:, :k_cols], size, True)
            q_gain, k_gain = self.gains()
            dq, q_sum = head_norm_back(proj[rows, :q_cols], q_gain, dq, size)
            dk, k_sum = head_norm_back(proj[rows, q_cols : q_cols + k_cols], k_gain, dk, size)
            self.q_gain.ref[...] += q_sum
            self.k_gain.ref[...] += k_sum
            self.d_proj.ref[rows, :q_cols] = dq.astype(BF)
            self.d_proj.ref[rows, q_cols : q_cols + k_cols] = dk.astype(BF)
            self.d_proj.ref[rows, q_cols + k_cols :] = dv.astype(BF)

        self.blocks(finish)


def body(boundary, norm_gain, mix_in, mix_out, w_gate, w_up, w_down, conv_x, conv_kernel, qk_gain):
    first = lax.axis_index("section") == 0
    tensor_index = lax.axis_index("tensor")
    model_width = boundary.shape[3]
    channels = mix_out.shape[1]
    row_shape = boundary.shape[2:]
    length, size = 4 * row_shape[0], qk_gain.shape[1]

    seqs, own_gain = boundary[0], norm_gain[0]
    sh_in, sh_out, sh_gate, sh_up, sh_down = (v[0] for v in (mix_in, mix_out, w_gate, w_up, w_down))

    def gains_of(k, block, other, early=True):
        own, moved = k.input(own_gain), as_val(k, other)
        sources = lambda s, d, t: [(s == block, own.ref), (s == 1 - block, moved.ref)]
        return Load(k, sources, own.shape, F32, early)

    def start_rows(k, slot, other, early=True):
        own, moved = k.input(seqs), as_val(k, other)
        sources = lambda s, d, t: [(s == slot, own.ref.at[slot]), (s == 1 - slot, moved.ref)]
        return Load(k, sources, row_shape, BF, early)

    def wait(*items):
        return [item.wait for item in items]

    k = Kernel(0)
    t_seq = None
    seq_val = k.input(seqs)

    def seq_moves(s, d, t):
        return [([(None, seq_val.ref.at[1 - s])], t_seq.out.ref, {"section": 1 - s})], []

    t_in, t_out, t_up = (x_half(k, v) for v in (sh_in, sh_out, sh_up))
    gate_lo, gate_hi = (Part(sh_gate, i * (sh_gate.shape[0] // 2), sh_gate.shape[0] // 2) for i in range(2))
    down_lo, down_hi = (Part(sh_down, i * (sh_down.shape[0] // 2), sh_down.shape[0] // 2) for i in range(2))
    t_gate0a, t_gate0b = x_half(k, gate_lo, 0), x_move(k, gate_hi, 0)
    t_down0a, t_down0b = x_half(k, down_lo, 0), x_move(k, down_hi, 0)
    t_gate1, t_down1 = x_half(k, sh_gate, 1), x_move(k, sh_down, 1)
    t_seq = Task(k, row_shape, "section", seq_moves, 1)
    t_gain, z_cols = x_move(k, own_gain), z_gather(k, conv_x)
    z_in0, z_out0 = z_gather_half(k, sh_in, t_in.out, 0), z_gather_half(k, sh_out, t_out.out, 0)
    z_gate0a = z_gather_half(k, gate_lo, t_gate0a.out, 0)
    z_gate0b, x_gate0a = z_gather_whole(k, gate_hi, t_gate0b.out, 0), x_move(k, z_gate0a.out)
    z_up0 = z_gather_half(k, sh_up, t_up.out, 0)
    x_cols, x_in0, x_out0 = (x_move(k, v.out) for v in (z_cols, z_in0, z_out0))
    x_load, gain_load = start_rows(k, 0, t_seq.out, False), gains_of(k, 0, t_gain.out, False)
    taps = load_all(k, conv_kernel)
    angles = Angles(k, length, size, 128)
    w_in0, w_cols = Weight(k, "rows", (z_in0.out, x_in0.out)), Weight(k, "conv", (z_cols.out, x_cols.out))
    w_out0 = Weight(k, "cols", (z_out0.out, x_out0.out))
    g0 = Gather(k, x_load.buf, (gain_load.buf, 0), [w_in0, w_cols], save=(0, 1, 2))
    conv = Conv(k, g0.values[0], g0.values[1], taps.buf)
    y0 = Save(k, conv.y)
    s1 = Scatter(k, [conv.y], [w_out0], x_load.buf)
    mid0 = Save(k, s1.out)
    k.do(t_in.send, t_out.send, z_cols.send, t_gate0b.send, t_gate0a.send, t_gate1.send)
    k.do(t_gain.send, t_seq.send)
    k.do(t_in.wait, z_in0.send, t_out.wait, z_out0.send, z_cols.step, z_in0.step, z_out0.step)
    k.do(z_cols.step, z_in0.step, z_out0.step, t_gate0b.wait, z_gate0b.send)
    k.do(t_gate0a.wait, z_gate0a.send)
    k.do(z_cols.wait, x_cols.send, z_in0.wait, x_in0.send, z_out0.wait, x_out0.send, t_up.send)
    k.do(t_gain.wait, gain_load.start, t_seq.wait, x_load.start, gain_load.wait, x_load.wait)
    k.do(g0.begin, z_gate0b.step, z_gate0a.step, angles.run, z_gate0b.step, z_gate0a.step)
    k.do(x_cols.wait, w_cols.start, x_in0.wait, w_in0.start, z_gate0a.wait, x_gate0a.send)
    k.do(t_down0b.send, t_down0a.send, t_down1.send, t_up.wait, z_up0.send)
    k.do(g0.loop, z_up0.step, taps.wait, conv.run, y0.start)
    k.do(x_out0.wait, w_out0.start, s1.loop, z_up0.step, s1.finish, mid0.start)
    k.do(*wait(t_gate1, t_down0a, t_down0b, t_down1, z_gate0b, x_gate0a, z_up0))
    k.build()
    a0, proj0, value0 = (out for _, out, _ in g0.saved)
    table_arrays = [qk_gain] + [v.out for v in angles.saves]
    y0, mid0 = y0.out, mid0.out

    k = Kernel(1)
    x_up0, z_gate1 = x_move(k, z_up0.out), z_gather_half(k, sh_gate, t_gate1.out, 1)
    z_down0a = z_gather_half(k, down_lo, t_down0a.out, 0)
    z_down0b = z_gather_whole(k, down_hi, t_down0b.out, 0)
    z_in1, z_out1 = z_gather_half(k, sh_in, t_in.out, 1), z_gather_half(k, sh_out, t_out.out, 1)
    x_down0a, x_in1, x_out1 = (x_move(k, v.out) for v in (z_down0a, z_in1, z_out1))
    rows, gain_load = load_all(k, mid0), gains_of(k, 0, t_gain.out)
    w_gate0 = Weight(k, "rows", (z_gate0a.out, x_gate0a.out), (z_gate0b.out, None), early=True)
    w_up0 = Weight(k, "rows", (z_up0.out, x_up0.out))
    w_down0 = Weight(k, "cols", (z_down0a.out, x_down0a.out), (z_down0b.out, None))
    g2 = Gather(
        k, rows.buf, (gain_load.buf, 1), [w_gate0, w_up0], epilogue="ffn", save=(0, 1, 2, 3)
    )
    s3 = Scatter(k, [g2.values[2]], [w_down0], rows.buf, low=True)
    z_rows = Save(k, s3.out)
    k.do(x_up0.send, z_down0a.send, z_down0b.send, rows.wait, gain_load.wait, g2.begin)
    k.do(z_in1.send, z_out1.send, z_down0a.step, z_in1.step, z_out1.step, z_down0b.step)
    k.do(z_down0a.step, z_in1.step, z_out1.step, z_gate1.send, z_down0a.wait, x_down0a.send)
    k.do(x_up0.wait, w_up0.start, z_down0b.step, g2.loop, z_gate1.step)
    k.do(z_in1.wait, x_in1.send, z_out1.wait, x_out1.send, z_down0b.wait, x_down0a.wait)
    k.do(w_down0.start, s3.loop, z_gate1.step, s3.finish, z_rows.start)
    k.do(*wait(x_in1, x_out1, z_gate1))
    k.build()
    m0, gate0, up0, hid0 = (out for _, out, _ in g2.saved)
    z_rows = z_rows.out

    k = Kernel(2)
    x_gate1, z_up1 = x_move(k, z_gate1.out), z_gather_half(k, sh_up, t_up.out, 1)
    z_down1a, z_down1b = (z_gather_whole(k, sh_down, t_down1.out, 1, i) for i in range(2))
    x_up1 = x_move(k, z_up1.out)
    rows, gain_load = load_all(k, z_rows), gains_of(k, 1, t_gain.out)
    tables = [load_all(k, v) for v in table_arrays]
    w_in1 = Weight(k, "rows", (z_in1.out, x_in1.out), early=True)
    w_out1 = Weight(k, "cols", (z_out1.out, x_out1.out), early=True)
    g4 = Gather(k, rows.buf, (gain_load.buf, 0), [w_in1], save=(0, 1))
    attend = Attend(k, g4.values[0], tables, size)
    kept = [Save(k, v) for v in (attend.q_rot, attend.k_rot, attend.y)]
    s5 = Scatter(k, [attend.y], [w_out1], rows.buf)
    mid1 = Save(k, s5.out)
    k.do(x_gate1.send, z_up1.send, rows.wait, gain_load.wait, g4.begin, z_up1.step)
    k.do(z_down1a.send, g4.loop, z_up1.step, z_down1b.send)
    k.do(lambda: attend.run(z_up1.wait, x_up1.send, z_down1a.step))
    k.do(*(v.start for v in kept))
    k.do(z_down1b.step, s5.loop, z_down1a.step, z_down1b.step, s5.finish, mid1.start)
    k.do(*wait(x_gate1, x_up1, z_down1a, z_down1b))
    k.build()
    a1, proj1 = (out for _, out, _ in g4.saved)
    q_rot, k_rot, y1 = (v.out for v in kept)
    mid1 = mid1.out

    k = Kernel(3)
    rows, gain_load = load_all(k, mid1), gains_of(k, 1, t_gain.out)
    cot = start_rows(k, 1, t_seq.out)
    w_gate1 = Weight(k, "rows", (z_gate1.out, x_gate1.out), early=True)
    w_up1 = Weight(k, "rows", (z_up1.out, x_up1.out), early=True)
    w_down1 = Weight(k, "cols", (z_down1a.out, None), (z_down1b.out, None), early=True)
    g6 = Gather(k, rows.buf, (gain_load.buf, 1), [w_gate1, w_up1], epilogue="ffn")
    g8 = Gather(
        k, cot.buf, None, [w_down1], [g6.values[0], g6.values[1]], trans=True, epilogue="ffn_back"
    )
    p_down1 = Product(k, g6.values[2], g8.full)
    p_gate1, p_up1 = Product(k, g6.full, g8.values[0]), Product(k, g6.full, g8.values[1])
    s9 = Scatter(k, g8.values, [w_gate1, w_up1], cot.buf, (rows.buf, (gain_load.buf, 1)), True)
    hid1 = Save(k, g6.values[2])
    d_mid1, gain11 = Save(k, s9.out), Save(k, s9.gain_grad)
    k.do(rows.wait, gain_load.wait, g6.begin, cot.wait, g8.begin, g6.loop, hid1.start, g8.loop)
    k.do(s9.loop, p_down1.run, p_gate1.run, p_up1.run)
    k.do(s9.finish, d_mid1.start, gain11.start, p_down1.wait, p_gate1.wait, p_up1.wait)
    k.build()
    hid1, d_mid1, gain11 = hid1.out, d_mid1.out, gain11.out

    k = Kernel(4)
    r_down1 = x_half(k, p_down1.out)
    r_gate1, q_up1 = x_slots(k, p_gate1.out, "rows"), sum_scatter(k, "rows", p_up1.out)
    rows, gain_load = load_all(k, d_mid1), gains_of(k, 1, t_gain.out)
    value = load_all(k, z_rows)
    tables = [load_all(k, v) for v in table_arrays]
    proj, q_load, k_load, y_load, a_load = (load_all(k, v) for v in (proj1, q_rot, k_rot, y1, a1))
    w_in1 = Weight(k, "rows", (z_in1.out, x_in1.out), early=True)
    w_out1 = Weight(k, "cols", (z_out1.out, x_out1.out), early=True)
    g10 = Gather(k, rows.buf, None, [w_out1], trans=True)
    p_out1 = Product(k, y_load.buf, g10.full)
    back = AttendBack(k, proj.buf, tables, size, q_load.buf, k_load.buf, g10.values[0])
    p_in1 = Product(k, a_load.buf, back.d_proj)
    r_out1 = x_half(k, p_out1.out)
    s11 = Scatter(
        k, [back.d_proj], [w_in1], rows.buf, (value.buf, (gain_load.buf, 0)), True, low=True
    )
    d_z, gain10 = Save(k, s11.out), Save(k, s11.gain_grad)
    head_gains = [Save(k, back.q_gain), Save(k, back.k_gain)]
    k.early.append(q_up1.load)
    k.do(r_down1.send, r_gate1.send, rows.wait, g10.begin, q_up1.send, g10.loop)
    k.do(y_load.wait, p_out1.run, q_up1.step, p_out1.wait, r_out1.send)
    k.do(proj.wait, q_load.wait, k_load.wait, lambda: back.run(q_up1.step))
    k.do(*(v.start for v in head_gains))
    k.do(gain_load.wait, value.wait, s11.loop, a_load.wait, p_in1.run)
    k.do(s11.finish, d_z.start, gain10.start, p_in1.wait)
    k.do(*wait(r_down1, q_up1, r_gate1, r_out1))
    k.build()
    d_z, gain10 = d_z.out, gain10.out
    q_gain, k_gain = (v.out for v in head_gains)

    k = Kernel(5)
    q_gate1, m_up1 = sum_scatter(k, "rows", p_gate1.out, r_gate1.out), x_move(k, q_up1.out, 0)
    q_out1 = sum_scatter(k, "cols", p_out1.out, r_out1.out)
    r_in1 = x_slots(k, p_in1.out, "rows")
    q_in1 = sum_scatter(k, "rows", p_in1.out, r_in1.out)
    q_down1 = sum_scatter(k, "cols", p_down1.out, r_down1.out)
    rows, value, gain_load = load_all(k, d_z), load_all(k, mid0), gains_of(k, 0, t_gain.out)
    gate_load, up_load, hid_load, m_load = (load_all(k, v) for v in (gate0, up0, hid0, m0))
    w_gate0 = Weight(k, "rows", (z_gate0a.out, x_gate0a.out), (z_gate0b.out, None), early=True)
    w_up0 = Weight(k, "rows", (z_up0.out, x_up0.out), early=True)
    w_down0 = Weight(k, "cols", (z_down0a.out, x_down0a.out), (z_down0b.out, None), early=True)
    g12 = Gather(
        k, rows.buf, None, [w_down0], [gate_load.buf, up_load.buf], trans=True, epilogue="ffn_back"
    )
    p_down0 = Product(k, hid_load.buf, g12.full)
    p_gate0, p_up0 = Product(k, m_load.buf, g12.values[0]), Product(k, m_load.buf, g12.values[1])
    r_down0 = x_half(k, p_down0.out)
    s13 = Scatter(
        k, g12.values, [w_gate0, w_up0], rows.buf, (value.buf, (gain_load.buf, 1)), True
    )
    d_mid0, gain01 = Save(k, s13.out), Save(k, s13.gain_grad)
    k.early += [q_gate1.load, q_down1.load, q_out1.load]
    k.do(r_in1.send, m_up1.send, rows.wait, g12.begin, q_gate1.send, q_down1.send, q_out1.send)
    k.do(gate_load.wait, up_load.wait, g12.loop, q_gate1.step, q_down1.step, q_out1.step)
    k.do(hid_load.wait, p_down0.run, p_down0.wait, r_down0.send, r_in1.wait, q_in1.add)
    k.do(s13.loop, q_gate1.step, q_down1.step, q_out1.step)
    k.do(m_load.wait, p_gate0.run, q_in1.step, p_up0.run, value.wait, gain_load.wait)
    k.do(s13.finish, d_mid0.start, gain01.start, q_in1.step, p_gate0.wait, p_up0.wait)
    k.do(*wait(q_gate1, q_out1, q_in1, q_down1, m_up1, r_down0))
    k.build()
    d_mid0, gain01 = d_mid0.out, gain01.out

    k = Kernel(6)
    r_gate0 = x_slots(k, p_gate0.out, "rows")
    q_gate0 = sum_scatter(k, "rows", p_gate0.out, r_gate0.out)
    q_down0 = sum_scatter(k, "cols", p_down0.out, r_down0.out)
    q_up0 = sum_scatter(k, "rows", p_up0.out)
    m_up0 = x_move(k, q_up0.out, 1)
    e_down1 = Finish(k, q_down1.out, 1)
    e_gate1, e_out1, e_in1 = (Finish(k, v.out, 1) for v in (q_gate1, q_out1, q_in1))
    rows, gain_load = load_all(k, d_mid0), gains_of(k, 0, t_gain.out)
    x_load, taps = start_rows(k, 0, t_seq.out), load_all(k, conv_kernel)
    y_load, a_load, proj, value = (load_all(k, v) for v in (y0, a0, proj0, value0))
    w_in0 = Weight(k, "rows", (z_in0.out, x_in0.out), early=True)
    w_cols = Weight(k, "conv", (z_cols.out, x_cols.out), early=True)
    w_out0 = Weight(k, "cols", (z_out0.out, x_out0.out), early=True)
    g14 = Gather(k, rows.buf, None, [w_out0], trans=True)
    p_out0 = Product(k, y_load.buf, g14.full)
    back = ConvBack(k, proj.buf, value.buf, taps.buf, g14.values[0])
    p_in0, p_cols = Product(k, a_load.buf, back.d_proj), Product(k, a_load.buf, back.d_value)
    r_out0, r_in0 = x_half(k, p_out0.out), x_slots(k, p_in0.out, "rows")
    r_cols = x_slots(k, p_cols.out, "conv")
    q_out0, q_in0 = sum_scatter(k, "cols", p_out0.out, r_out0.out), sum_scatter(k, "rows", p_in0.out, r_in0.out)
    q_cols = sum_scatter(k, "conv", p_cols.out, r_cols.out)
    e_down0, e_gate0, e_out0, e_in0 = (
        Finish(k, v.out, 0) for v in (q_down0, q_gate0, q_out0, q_in0)
    )
    s15 = Scatter(
        k, [back.d_proj, back.d_value], [w_in0, w_cols], rows.buf,
        (x_load.buf, (gain_load.buf, 0)), True, low=True,
    )
    d_x = Save(k, s15.out)
    tap_rows = conv_kernel.shape[0]
    small = k.vmem((8, model_width), F32)
    small_out = Save(k, small)
    ready = [load_all(k, v) for v in (gain01, gain10, gain11)]
    head_loads = [load_all(k, v) for v in (q_gain, k_gain)]

    def fill_small():
        t = lax.axis_index("tensor")
        small.ref[...] = jnp.zeros_like(small.ref)
        small.ref[0:1, :] = s15.gain_grad.ref[...]
        for i, load in enumerate(ready):
            load.wait()
            small.ref[i + 1 : i + 2, :] = load.buf.ref[...]
        small.ref[4 : 4 + tap_rows, block_of(t, channels)] = back.d_kernel.ref[...]
        at = 0
        for load in head_loads:
            load.wait()
            width = load.buf.shape[1]
            small.ref[7:8, at : at + width] = load.buf.ref[...]
            at += width
        small_out.start()

    t_small = x_move(k, small_out.out)
    z_small = SumShare(k, [small_out.out, t_small.out], "dp")
    t_total = SumShare(k, [z_small.out], "tensor", slotted=True)
    hid_load, mid_load = load_all(k, hid1), load_all(k, mid1)
    w_down1 = Weight(k, "cols", (z_down1a.out, None), (z_down1b.out, None), early=True)
    s7 = Scatter(k, [hid_load.buf], [w_down1], mid_load.buf, low=True)
    y_rows = Save(k, s7.out)
    t_x, t_y = x_move(k, d_x.out, 1), x_move(k, y_rows.out, 0)
    k.early += [q_up0.load, q_down0.load]
    k.early += [v.load for v in (e_down1, e_gate1, e_out1, e_in1)]
    k.do(r_gate0.send, q_up0.send, rows.wait, g14.begin, q_down0.send)
    k.do(e_down1.send, e_gate1.send, e_out1.send, e_in1.send, g14.loop)
    k.do(y_load.wait, p_out0.run, p_out0.wait, r_out0.send, q_up0.step)
    k.do(proj.wait, value.wait, taps.wait, back.run, q_down0.step, a_load.wait)
    k.do(p_in0.run, p_cols.run, p_in0.wait, r_in0.send, p_cols.wait, r_cols.send)
    k.do(r_gate0.wait, q_gate0.add, x_load.wait, gain_load.wait, s15.loop, q_up0.step)
    k.do(q_down0.step, s15.finish, d_x.start, fill_small, d_x.wait, t_x.send)
    k.do(small_out.wait, t_small.send, q_gate0.step, r_out0.wait, q_out0.add, r_in0.wait, q_in0.add)
    k.do(r_cols.wait, q_cols.add, q_up0.wait, m_up0.send, hid_load.wait, mid_load.wait, s7.loop)
    k.do(q_down0.wait, e_down0.add, s7.finish, y_rows.start, y_rows.wait, t_y.send)
    k.do(q_gate0.step, q_out0.step, q_in0.step, q_cols.step, t_small.wait, z_small.add)
    k.do(q_gate0.wait, e_gate0.add, q_out0.step, q_in0.step, q_cols.step)
    k.do(z_small.wait, t_total.add, q_out0.wait, e_out0.add, q_in0.wait, e_in0.add)
    rest = (e_down1, e_gate1, e_out1, e_in1, q_cols, e_down0, e_gate0, m_up0, e_out0, e_in0)
    k.do(*wait(*rest, t_total, t_x, t_y))
    k.build()

    owned = [
        ([e_in0], [e_in1], 1),
        ([e_out0], [e_out1], 1),
        ([e_gate0], [e_gate1], 1),
        ([q_up0, m_up0], [q_up1, m_up1], 1),
        ([e_down0], [e_down1], 1),
        ([q_cols], [q_cols], 0),
    ]
    return pack(
        [(zero, one, lead) for zero, one, lead in owned], t_total, d_x.out, y_rows.out, t_x, t_y,
        (norm_gain.shape, conv_kernel.shape, qk_gain.shape),
    )


def slot_free(val, shape):
    value = val.out.array
    if value.ndim == 3 and value.shape[0] * value.shape[1] != shape[0]:
        value = jnp.sum(value.astype(F32), axis=0).astype(BF)
    return value.reshape(shape)


def pack_kernel(plan, *refs):
    n_in, leads, terms, tap_rows = plan
    ins, rest = refs[:n_in], refs[n_in:]
    result, gain_out, *grads, cols, taps, heads = rest[: len(leads) + 4]
    grads = [*grads, cols]
    room = iter(rest[len(leads) + 4 :])
    own_v, moved_v, small_v, *bufs = (next(room) for _ in range(3 + len(terms)))
    out_v = [next(room) for _ in leads]
    load_sem, store_sem = room
    s, t = lax.axis_index("section"), lax.axis_index("tensor")
    small, d_x, y_rows, moved, moved_y, *parts = ins

    def either(cond, zero, one, dst, sem):
        if zero is not None:
            pl.when(cond)(pltpu.make_async_copy(zero, dst, sem).start)
        if one is not None:
            pl.when(jnp.logical_not(cond))(pltpu.make_async_copy(one, dst, sem).start)

    first = s == 0
    either(first, d_x, y_rows, own_v, load_sem.at[0])
    either(first, moved, moved_y, moved_v, load_sem.at[1])
    pltpu.make_async_copy(small, small_v, load_sem.at[2]).start()
    for j, (zero, one, _) in enumerate(terms):
        either(
            first,
            None if zero is None else parts[zero],
            None if one is None else parts[one],
            bufs[j],
            load_sem.at[3 + j],
        )
    for j, (zero, one, i) in enumerate(terms):
        arrive = pltpu.make_async_copy(parts[one if zero is None else zero], bufs[j], load_sem.at[3 + j])
        begins = j == 0 or terms[j - 1][2] != i

        def put(j=j, i=i, begins=begins):
            def add_rows(at):
                value = bufs[j][at, :].astype(F32)
                out_v[i][at, :] = value if begins else out_v[i][at, :] + value

            chunked(bufs[j].shape[0], add_rows)

        if zero is None or one is None:
            cond = first if one is None else jnp.logical_not(first)

            @pl.when(cond)
            def _(arrive=arrive, put=put):
                arrive.wait()
                put()
        else:
            arrive.wait()
            put()
        if j + 1 == len(terms) or terms[j + 1][2] != i:
            dst = grads[i].at[0] if leads[i] else grads[i]
            pltpu.make_async_copy(out_v[i], dst, store_sem.at[i]).start()
    pltpu.make_async_copy(d_x, own_v, load_sem.at[0]).wait()
    pltpu.make_async_copy(moved, moved_v, load_sem.at[1]).wait()
    n = len(leads)
    stores = [
        pltpu.make_async_copy(own_v, result.at[0, s], store_sem.at[n]),
        pltpu.make_async_copy(moved_v, result.at[0, 1 - s], store_sem.at[n + 1]),
    ]
    for store in stores:
        store.start()
    pltpu.make_async_copy(small, small_v, load_sem.at[2]).wait()
    total = small_v[0]
    for i in range(1, small_v.shape[0]):
        total = total + small_v[i]
    gain_out[0] = jnp.where(first, total[0:2], total[2:4])
    channels, size = taps.shape[1], heads.shape[1]
    chosen = total[4 : 4 + tap_rows, 0:channels]
    for i in range(1, total.shape[1] // channels):
        chosen = jnp.where(t == i, total[4 : 4 + tap_rows, i * channels : (i + 1) * channels], chosen)
    taps[...] = chosen
    at = 0
    for row, width in enumerate((channels, channels // 2)):
        value = total[7:8, at : at + size]
        for i in range(1, width // size):
            value = value + total[7:8, at + i * size : at + (i + 1) * size]
        heads[row : row + 1, :] = value
        at += width
    for i, store in enumerate(leads):
        dst = grads[i].at[0] if store else grads[i]
        pltpu.make_async_copy(out_v[i], dst, store_sem.at[i]).wait()
    for store in stores:
        store.wait()


def pack(owned, small, d_x, y_rows, moved_x, moved_y, shapes):
    gain_shape, tap_shape, head_shape = shapes
    parts, terms, leads, out_shapes = [], [], [], []
    for i, (zero, one, lead) in enumerate(owned):
        whole = zero[0].out.shape
        if lead and len(whole) == 3 and isinstance(zero[0], Finish):
            shape = (whole[0] * whole[1], whole[2])
        else:
            shape = whole[-2:]
        shape = tuple(shape)
        leads.append(lead)
        out_shapes.append(shape)
        for j in range(max(len(zero), len(one))):
            pair = []
            for side in (zero, one):
                if j < len(side):
                    parts.append(slot_free(side[j], shape))
                    pair.append(len(parts) - 1)
                else:
                    pair.append(None)
            terms.append((*pair, i))
    operands = [v.array for v in (small.out, d_x, y_rows, moved_x.out, moved_y.out)] + parts
    rows = d_x.shape
    smem = pl.BlockSpec(memory_space=pltpu.VMEM)
    out_shape = [jax.ShapeDtypeStruct((1, 2) + rows, BF), jax.ShapeDtypeStruct(gain_shape, F32)]
    out_shape += [
        jax.ShapeDtypeStruct((1,) + v if lead else v, F32) for v, lead in zip(out_shapes, leads)
    ]
    out_shape += [jax.ShapeDtypeStruct(v, F32) for v in (tap_shape, head_shape)]
    n = len(leads)
    return tuple(
        pl.pallas_call(
            functools.partial(
                pack_kernel, (len(operands), tuple(leads), tuple(terms), tap_shape[0])
            ),
            out_shape=out_shape,
            in_specs=[ANY] * len(operands),
            out_specs=[ANY, smem] + [ANY] * n + [smem] * 2,
            scratch_shapes=[pltpu.VMEM(rows, BF)] * 2
            + [pltpu.VMEM(small.out.shape, F32)]
            + [pltpu.VMEM(out_shapes[i], BF) for _, _, i in terms]
            + [pltpu.VMEM(v, F32) for v in out_shapes]
            + [DMA((3 + len(terms),)), DMA((n + 2,))],
            compiler_params=pltpu.CompilerParams(vmem_limit_bytes=VMEM_BYTES),
            name="pack",
        )(*operands)
    )


def solution(mesh):
    in_specs = (
        P("section", "dp", "tensor", None),
        P("section", None, None),
        P("section", "dp", "tensor"),
        P("section", "tensor", "dp"),
        P("section", "dp", "tensor"),
        P("section", "dp", "tensor"),
        P("section", "tensor", "dp"),
        P(("section", "dp"), "tensor"),
        P(None, "tensor"),
        P(),
    )
    out_specs = (
        P("section", "dp", "tensor", None),
        P("section", None, None),
        P("section", "dp", "tensor"),
        P("section", "tensor", "dp"),
        P("section", "dp", "tensor"),
        P("section", "dp", "tensor"),
        P("section", "tensor", "dp"),
        P(("section", "dp"), "tensor"),
        P(None, "tensor"),
        P(),
    )
    return jax.shard_map(body, mesh=mesh, in_specs=in_specs, out_specs=out_specs, check_vma=False)
```
